32 devices in a mesh: batch: 1 (over z), row: 4 (over y), col: 8 (over x, core).
Axes of the slice: x: 4, y: 4, z: 1, core: 2. Of those that a mesh axis runs over, the one named last changes fastest.
The devices are a block of a 4x4x8 slice.
Arguments:
- spd_blocks: float32 [32, 256, 8192], P(('batch', 'row'), None, 'col')
Outputs:
- output: float32 [32, 256, 8192], P(('batch', 'row'), None, 'col')
All inputs are finite; a program needn't handle non-finite values.
Results may differ from the reference program's by a relative error of at most 0.001.
Values are sent between devices in bfloat16 or wider.
A program may use at most 768 MiB of HBM per device.

```python
import math
import jax
import jax.numpy as jnp
from jax import lax

BLOCK = 256
ORDER = 8192
ROW_DEVS = 4
COL_DEVS = 8

BLOCK_COUNT = ORDER // BLOCK


def to_logical(a_cyc):
    by_rows = a_cyc.reshape(ROW_DEVS, BLOCK_COUNT // ROW_DEVS, BLOCK, ORDER).transpose(1, 0, 2, 3)
    by_cols = by_rows.reshape(ORDER, COL_DEVS, BLOCK_COUNT // COL_DEVS, BLOCK).transpose(0, 2, 1, 3)
    return by_cols.reshape(ORDER, ORDER)


def to_cyclic(matrix):
    by_rows = matrix.reshape(BLOCK_COUNT // ROW_DEVS, ROW_DEVS, BLOCK, ORDER).transpose(1, 0, 2, 3)
    by_cols = by_rows.reshape(ORDER, BLOCK_COUNT // COL_DEVS, COL_DEVS, BLOCK).transpose(0, 2, 1, 3)
    return by_cols.reshape(BLOCK_COUNT, BLOCK, ORDER)


def setup_inputs(seed: int = 0, part: int = 0) -> dict:
    rng_key = jax.random.fold_in(jax.random.key(seed), part)
    gauss_draw = jax.random.normal(rng_key, (ORDER, ORDER), jnp.float32)
    sym_part = (gauss_draw + gauss_draw.T) * math.sqrt(0.5 / ORDER)
    matrix = (sym_part + 2.2 * jnp.eye(ORDER, dtype=jnp.float32)) * ORDER
    return {"spd_blocks": to_cyclic(matrix)}


def reference(spd_blocks):
    trailing = to_logical(spd_blocks)
    columns = []
    for step_idx in range(BLOCK_COUNT):
        diag_fac = jnp.tril(jnp.linalg.cholesky(trailing[:BLOCK, :BLOCK]))
        pieces = [jnp.zeros((step_idx * BLOCK, BLOCK), jnp.float32), diag_fac]
        if step_idx + 1 < BLOCK_COUNT:
            panel_f32 = lax.linalg.triangular_solve(diag_fac, trailing[BLOCK:, :BLOCK], left_side=False, lower=True, transpose_a=True)
            pieces.append(panel_f32)
            panel_b16 = panel_f32.astype(jnp.bfloat16)
            trailing = trailing[BLOCK:, BLOCK:] - jnp.dot(panel_b16, panel_b16.T, preferred_element_type=jnp.float32)
        columns.append(jnp.concatenate(pieces, axis=0))
    return to_cyclic(jnp.concatenate(columns, axis=1))
```

```python
import functools

import jax
import jax.numpy as jnp
from jax import lax
from jax.experimental import pallas as pl
from jax.experimental.pallas import tpu as pltpu
from jax.sharding import PartitionSpec as P

F32 = jnp.float32
BF16 = jnp.bfloat16
MESH = pl.DeviceIdType.MESH
SUB = 8
LANE = 128
BASE = 16


def sub_bcast(x, q):
    return jnp.broadcast_to(x[q : q + 1, :], (SUB, LANE))


def lane_bcast(x, lane):
    return jnp.take_along_axis(x, jnp.full((SUB, LANE), lane, jnp.int32), axis=1)


def split3(x):
    high = x.astype(BF16)
    rest = x - high.astype(F32)
    mid = rest.astype(BF16)
    return high, mid, (rest - mid.astype(F32)).astype(BF16)


def swap_rows(x, bit, row_id):
    if bit == SUB // 2:
        return pltpu.roll(x, bit, 0)
    return jnp.where((row_id & bit) == 0, pltpu.roll(x, SUB - bit, 0), pltpu.roll(x, bit, 0))


def stack_sums(parts):
    row_id = lax.broadcasted_iota(jnp.int32, (SUB, LANE), 0)
    for bit in (4, 2, 1):
        low = (row_id & bit) == 0
        half = len(parts) // 2
        parts = [
            jnp.where(low, parts[n], parts[n + half]) + swap_rows(jnp.where(low, parts[n + half], parts[n]), bit, row_id)
            for n in range(half)
        ]
    return parts[0]


def eliminate(rows, lane0):
    row_id = lax.broadcasted_iota(jnp.int32, (SUB, LANE), 0)
    rows = [list(rows[0]), list(rows[1])]
    cols = [
        [lane_bcast(rows[0][0], lane0 + j) for j in range(SUB)],
        [lane_bcast(rows[1][0], lane0 + j) for j in range(BASE)],
    ]
    scale = [jnp.zeros((SUB, LANE), F32), jnp.zeros((SUB, LANE), F32)]
    pivot = sub_bcast(cols[0][0], 0)
    for j in range(BASE):
        t, q = divmod(j, SUB)
        inv = lax.rsqrt(pivot)
        scale[t] = jnp.where(row_id == q, inv, scale[t])
        if j + 1 < BASE:
            tn, qn = divmod(j + 1, SUB)
            near = sub_bcast(cols[tn][j], qn) * inv
            pivot = sub_bcast(cols[tn][j + 1], qn) - near * near
        below = cols[1][j] * inv
        here = cols[0][j] * inv if t == 0 else None
        for n in range(j + 1, BASE):
            tn, qn = divmod(n, SUB)
            other = sub_bcast(cols[tn][j], qn) * inv
            if t == 0 and tn == 0:
                cols[0][n] = cols[0][n] - here * other
            cols[1][n] = cols[1][n] - below * other
        masked = jnp.where(row_id > q, here if t == 0 else below, 0.0)
        for v in range(len(rows[0])):
            pivot_row = sub_bcast(rows[t][v], q) * inv
            rows[t][v] = rows[t][v] - masked * pivot_row
            if t == 0:
                rows[1][v] = rows[1][v] - below * pivot_row
    return [[x * scale[t] for x in rows[t]] for t in range(2)]


def factor_block(work, winv, prev):
    size = work.shape[1]
    prev[...] = jnp.zeros(prev.shape, F32)
    for half in range(size // LANE):
        views = [(work, 0), (work, 1), (winv, 0)] if half == 0 else [(work, 1), (winv, 0), (winv, 1)]
        first = half * LANE
        if half == 1:
            mid_part, inv_part = prev[:, LANE : 2 * LANE], prev[:, 2 * LANE :]
            prev[:, :LANE] = mid_part
            prev[:, LANE : 2 * LANE] = inv_part
            prev[:, 2 * LANE :] = jnp.zeros((BASE, LANE), F32)

        def body(s, carry, views=views, first=first):
            lane0 = s * BASE
            row0 = pl.multiple_of(first + lane0, BASE)

            def rows_at(row, t):
                return pl.ds(pl.multiple_of(row + SUB * t, SUB), SUB)

            rows = [[ref[rows_at(row0, t), LANE * g : LANE * (g + 1)] for ref, g in views] for t in range(2)]
            hi, mid, lo = split3(prev[...])
            lane = lax.broadcasted_iota(jnp.int32, (BASE, size - first), 1) + first
            after = lane >= row0 + BASE
            lhi, lmid, llo = [jnp.where(after, x[:, : size - first], jnp.zeros((), BF16)) for x in (hi, mid, lo)]
            update = lax.dot_general(
                jnp.concatenate([lhi, lhi, lmid, lhi, llo, lmid], axis=0),
                jnp.concatenate([hi, mid, hi, lo, hi, mid], axis=0),
                (((0,), (0,)), ((), ())),
                preferred_element_type=F32,
            )
            for v, (ref, g) in enumerate(views):
                ref[first:size, LANE * g : LANE * (g + 1)] -= update[:, LANE * v : LANE * (v + 1)]
            done = eliminate(rows, lane0)
            for t in range(2):
                for v, (ref, g) in enumerate(views):
                    ref[rows_at(row0, t), LANE * g : LANE * (g + 1)] = done[t][v]
                    prev[SUB * t : SUB * (t + 1), LANE * v : LANE * (v + 1)] = done[t][v]
            if first == 0:
                source = [jnp.where(s == LANE // BASE - 1, done[t][1], done[t][0]) for t in range(2)]
            else:
                source = [done[t][0] for t in range(2)]
            next_lane = (lane0 + BASE) % LANE
            for t in range(2):
                factor = [[lane_bcast(source[m], next_lane + SUB * t + n) for n in range(SUB)] for m in range(2)]
                for v, (ref, g) in enumerate(views):
                    parts = [factor[0][n] * done[0][v] + factor[1][n] * done[1][v] for n in range(SUB)]
                    ref[rows_at(row0 + BASE, t), LANE * g : LANE * (g + 1)] -= stack_sums(parts)
            return carry

        lax.fori_loop(0, LANE // BASE, body, 0)


def kernel(n_row, n_col, batch_axis, a_ref, o_ref, share, diag, panel, work, winv, prev, load_sem, store_sem, seed_send, seed_recv,
           send_sem, recv_sem):
    row_blocks, size, local_cols = a_ref.shape
    col_blocks = local_cols // size
    ratio = n_col // n_row
    steps = row_blocks * n_row
    batch = lax.axis_index(batch_axis)
    row = lax.axis_index("row")
    col = lax.axis_index("col")
    on_diag = lax.rem(col, n_row) == row
    row_slots = n_row * (row_blocks * (row_blocks + 1) // 2)

    def at(dev_row, dev_col):
        return (batch, dev_row, dev_col)

    def row_slot(k, a):
        g = k // n_row
        return n_row * (row_blocks * g - (g * (g - 1)) // 2) + (k - g * n_row) * (row_blocks - g) + a - g

    def col_slot(k, b):
        h = k // n_col
        return row_slots + n_col * (col_blocks * h - (h * (h - 1)) // 2) + (k - h * n_col) * (col_blocks - h) + b - h

    def first_a(k):
        return (k + n_row - row) // n_row

    def first_b(k):
        return (k + n_col - col) // n_col

    def home(ref, a, b):
        return ref.at[a, :, pl.ds(pl.multiple_of(b * size, size), size)]

    def col_of(k, b):
        return jnp.where(on_diag, row_slot(k, ratio * b + col // n_row), col_slot(k, b))

    def arrived(slot):
        pltpu.make_async_remote_copy(
            src_ref=panel.at[slot], dst_ref=panel.at[slot], send_sem=send_sem.at[0], recv_sem=recv_sem.at[slot],
            device_id=at(row, col), device_id_type=MESH,
        ).wait_recv()

    for a in range(row_blocks):
        for b in range(col_blocks):
            pltpu.make_async_copy(home(a_ref, a, b), share.at[a * col_blocks + b], load_sem).start()

    barrier = pltpu.get_barrier_semaphore()
    n_dev = n_row * n_col

    def greet(n, carry):
        other = lax.rem(row * n_col + col + n, n_dev)
        pl.semaphore_signal(barrier, inc=1, device_id=at(other // n_col, lax.rem(other, n_col)), device_id_type=MESH)
        return carry

    lax.fori_loop(1, n_dev, greet, 0)
    pl.semaphore_wait(barrier, n_dev - 1)
    pltpu.make_async_copy(share, share, load_sem).wait()

    def seed_copy(b, dev_row):
        block = (ratio * b + col // n_row) * col_blocks + b
        return pltpu.make_async_remote_copy(
            src_ref=share.at[block], dst_ref=diag.at[b], send_sem=seed_send.at[b, lax.rem(dev_row - row + n_row, n_row)],
            recv_sem=seed_recv.at[b], device_id=at(dev_row, col), device_id_type=MESH,
        )

    @pl.when(on_diag)
    def _():
        for b in range(col_blocks):
            for d in (1, n_row - 1, 2):
                seed_copy(b, lax.rem(row + d, n_row)).start()
        for b in range(col_blocks):
            diag[b] = share[(ratio * b + col // n_row) * col_blocks + b]

    def seed_arrived(b):
        @pl.when(jnp.logical_not(on_diag))
        def _():
            seed_copy(b, row).wait_recv()

    seed_arrived(0)

    def clear(n, carry):
        a, b = n // col_blocks, lax.rem(n, col_blocks)

        @pl.when(a * n_row + row < b * n_col + col)
        def _():
            share[n] = jnp.zeros((size, size), F32)
            pltpu.make_async_copy(share.at[n], home(o_ref, a, b), store_sem).start()

        return carry

    lax.fori_loop(0, row_blocks * col_blocks, clear, 0)

    def times_t(x, y):
        return lax.dot_general(x, y, (((1,), (1,)), ((), ())), preferred_element_type=F32)

    def send_block(k, a):
        i = a * n_row + row
        slot = row_slot(k, a)
        to_col, to_b = lax.rem(i, n_col), i // n_col
        for d in range(1, n_row):
            pltpu.make_async_remote_copy(
                src_ref=panel.at[slot], dst_ref=panel.at[col_slot(k, to_b)], send_sem=send_sem.at[a],
                recv_sem=recv_sem.at[col_slot(k, to_b)], device_id=at(lax.rem(row + d, n_row), to_col), device_id_type=MESH,
            ).start()
        for d in range(1, n_col):
            pltpu.make_async_remote_copy(
                src_ref=panel.at[slot], dst_ref=panel.at[slot], send_sem=send_sem.at[a], recv_sem=recv_sem.at[slot],
                device_id=at(row, lax.rem(col + d, n_col)), device_id_type=MESH,
            ).start()

    copies = n_row - 1 + n_col - 1

    def sends_done(k):
        def one(a, carry):
            every = panel.at[pl.ds(0, copies)]
            pltpu.make_async_copy(every, every, send_sem.at[a]).wait()
            return carry

        lax.fori_loop(first_a(k), row_blocks, one, 0)

    def step(k, carry):
        mine = col == lax.rem(k, n_col)
        kb = k // n_col

        @pl.when(mine)
        def _():
            work[0:size, :] = diag[kb]
            work[size:, :] = jnp.zeros((BASE, size), F32)
            r_id = lax.broadcasted_iota(jnp.int32, (size + BASE, size), 0)
            c_id = lax.broadcasted_iota(jnp.int32, (size + BASE, size), 1)
            winv[...] = jnp.where(r_id == c_id, 1.0, 0.0).astype(F32)
            factor_block(work, winv, prev)

            def solve(a, carry):
                n = a * col_blocks + kb

                @pl.when(k > 0)
                def _():
                    arrived(row_slot(k - 1, a))
                    share[n] -= times_t(panel[row_slot(k - 1, a)], panel[col_of(k - 1, kb)])

                x = lax.dot_general(
                    share[n], winv[0:size, :], (((1,), (1,)), ((), ())), precision=lax.Precision.HIGHEST,
                    preferred_element_type=F32,
                )
                panel[row_slot(k, a)] = x.astype(BF16)
                share[n] = x
                send_block(k, a)
                pltpu.make_async_copy(share.at[n], home(o_ref, a, kb), store_sem).start()
                return carry

            lax.fori_loop(first_a(k), row_blocks, solve, 0)

            @pl.when(row == lax.rem(k, n_row))
            def _():
                for d in range(1, n_row):
                    seed_copy(kb, lax.rem(row + d, n_row)).wait_send()
                r_id = lax.broadcasted_iota(jnp.int32, (size, size), 0)
                c_id = lax.broadcasted_iota(jnp.int32, (size, size), 1)
                n = (k // n_row) * col_blocks + kb
                share[n] = jnp.where(r_id >= c_id, work[0:size, :].T, 0.0)
                pltpu.make_async_copy(share.at[n], home(o_ref, k // n_row, kb), store_sem).start()

        @pl.when(k > 0)
        def _():
            p = k - 1
            owner = col == lax.rem(p, n_col)

            @pl.when(k == 1)
            def _():
                for b in range(1, col_blocks):
                    seed_arrived(b)

            @pl.when(jnp.logical_not(jnp.logical_or(owner, mine)))
            def _():
                lax.fori_loop(first_a(p), row_blocks, lambda a, c: (arrived(row_slot(p, a)), c)[1], 0)

            def column(b, carry):
                @pl.when(jnp.logical_not(on_diag))
                def _():
                    arrived(col_slot(p, b))

                other = col_of(p, b)
                diag[b] -= times_t(panel[other], panel[other])

                def block(a, carry):
                    share[a * col_blocks + b] -= times_t(panel[row_slot(p, a)], panel[other])
                    return carry

                lax.fori_loop(first_a(b * n_col + col), row_blocks, block, 0)
                return carry

            lax.fori_loop(jnp.where(mine, kb + 1, first_b(p)), col_blocks, column, 0)

        @pl.when(jnp.logical_and(col == lax.rem(k + 1, n_col), k + 1 < steps))
        def _():
            nb = (k + 1) // n_col
            slot = col_of(k, nb)
            arrived(slot)
            diag[nb] -= times_t(panel[slot], panel[slot])

        @pl.when(jnp.logical_and(k >= n_col // 2, col == lax.rem(k + n_col // 2, n_col)))
        def _():
            sends_done(k - n_col // 2)

        return carry

    lax.fori_loop(0, steps, step, 0)

    for m in range(n_col // 2):
        k = steps - n_col // 2 + m

        @pl.when(col == k % n_col)
        def _():
            sends_done(k)

    pltpu.make_async_copy(share, share, store_sem).wait()


def solution(mesh):
    n_row = mesh.shape["row"]
    n_col = mesh.shape["col"]

    def factor_local(a_loc):
        row_blocks, size, local_cols = a_loc.shape
        col_blocks = local_cols // size
        slots = n_row * (row_blocks * (row_blocks + 1) // 2) + n_col * (col_blocks * (col_blocks + 1) // 2)
        return pl.pallas_call(
            functools.partial(kernel, n_row, n_col, "batch"),
            out_shape=jax.ShapeDtypeStruct(a_loc.shape, F32),
            in_specs=[pl.BlockSpec(memory_space=pl.ANY)],
            out_specs=pl.BlockSpec(memory_space=pl.ANY),
            scratch_shapes=[
                pltpu.VMEM((row_blocks * col_blocks, size, size), F32),
                pltpu.VMEM((col_blocks, size, size), F32),
                pltpu.VMEM((slots, size, size), BF16),
                pltpu.VMEM((size + BASE, size), F32),
                pltpu.VMEM((size + BASE, size), F32),
                pltpu.VMEM((BASE, 3 * LANE), F32),
                pltpu.SemaphoreType.DMA,
                pltpu.SemaphoreType.DMA,
                pltpu.SemaphoreType.DMA((col_blocks, n_row)),
                pltpu.SemaphoreType.DMA((col_blocks,)),
                pltpu.SemaphoreType.DMA((row_blocks,)),
                pltpu.SemaphoreType.DMA((slots,)),
            ],
            compiler_params=pltpu.CompilerParams(
                collective_id=0, has_side_effects=True, vmem_limit_bytes=60 * 1024 * 1024
            ),
            name="cholesky",
        )(a_loc)

    blk_spec = P(("batch", "row"), None, "col")
    return jax.shard_map(factor_local, mesh=mesh, in_specs=(blk_spec,), out_specs=blk_spec, check_vma=False)
```

```python
import functools

import jax
import jax.numpy as jnp
from jax import lax
from jax.experimental import pallas as pl
from jax.experimental.pallas import tpu as pltpu
from jax.sharding import PartitionSpec as P

F32 = jnp.float32
BF16 = jnp.bfloat16
MESH = pl.DeviceIdType.MESH
SUB = 8
LANE = 128
BASE = 16


def sub_bcast(x, q):
    return jnp.broadcast_to(x[q : q + 1, :], (SUB, LANE))


def lane_bcast(x, lane):
    return jnp.take_along_axis(x, jnp.full((SUB, LANE), lane, jnp.int32), axis=1)


def split3(x):
    high = x.astype(BF16)
    rest = x - high.astype(F32)
    mid = rest.astype(BF16)
    return high, mid, (rest - mid.astype(F32)).astype(BF16)


def swap_rows(x, bit, row_id):
    if bit == SUB // 2:
        return pltpu.roll(x, bit, 0)
    return jnp.where((row_id & bit) == 0, pltpu.roll(x, SUB - bit, 0), pltpu.roll(x, bit, 0))


def stack_sums(parts):
    row_id = lax.broadcasted_iota(jnp.int32, (SUB, LANE), 0)
    for bit in (4, 2, 1):
        low = (row_id & bit) == 0
        half = len(parts) // 2
        parts = [
            jnp.where(low, parts[n], parts[n + half]) + swap_rows(jnp.where(low, parts[n + half], parts[n]), bit, row_id)
            for n in range(half)
        ]
    return parts[0]


def eliminate(rows, lane0):
    row_id = lax.broadcasted_iota(jnp.int32, (SUB, LANE), 0)
    rows = [list(rows[0]), list(rows[1])]
    cols = [
        [lane_bcast(rows[0][0], lane0 + j) for j in range(SUB)],
        [lane_bcast(rows[1][0], lane0 + j) for j in range(BASE)],
    ]
    scale = [jnp.zeros((SUB, LANE), F32), jnp.zeros((SUB, LANE), F32)]
    pivot = sub_bcast(cols[0][0], 0)
    for j in range(BASE):
        t, q = divmod(j, SUB)
        inv = lax.rsqrt(pivot)
        scale[t] = jnp.where(row_id == q, inv, scale[t])
        if j + 1 < BASE:
            tn, qn = divmod(j + 1, SUB)
            near = sub_bcast(cols[tn][j], qn) * inv
            pivot = sub_bcast(cols[tn][j + 1], qn) - near * near
        below = cols[1][j] * inv
        here = cols[0][j] * inv if t == 0 else None
        for n in range(j + 1, BASE):
            tn, qn = divmod(n, SUB)
            other = sub_bcast(cols[tn][j], qn) * inv
            if t == 0 and tn == 0:
                cols[0][n] = cols[0][n] - here * other
            cols[1][n] = cols[1][n] - below * other
        masked = jnp.where(row_id > q, here if t == 0 else below, 0.0)
        for v in range(len(rows[0])):
            pivot_row = sub_bcast(rows[t][v], q) * inv
            rows[t][v] = rows[t][v] - masked * pivot_row
            if t == 0:
                rows[1][v] = rows[1][v] - below * pivot_row
    return [[x * scale[t] for x in rows[t]] for t in range(2)]


def factor_block(work, winv, prev):
    size = work.shape[1]
    prev[...] = jnp.zeros(prev.shape, F32)
    for half in range(size // LANE):
        views = [(work, 0), (work, 1), (winv, 0)] if half == 0 else [(work, 1), (winv, 0), (winv, 1)]
        first = half * LANE
        if half == 1:
            mid_part, inv_part = prev[:, LANE : 2 * LANE], prev[:, 2 * LANE :]
            prev[:, :LANE] = mid_part
            prev[:, LANE : 2 * LANE] = inv_part
            prev[:, 2 * LANE :] = jnp.zeros((BASE, LANE), F32)

        def body(s, carry, views=views, first=first):
            lane0 = s * BASE
            row0 = pl.multiple_of(first + lane0, BASE)

            def rows_at(row, t):
                return pl.ds(pl.multiple_of(row + SUB * t, SUB), SUB)

            rows = [[ref[rows_at(row0, t), LANE * g : LANE * (g + 1)] for ref, g in views] for t in range(2)]
            hi, mid, lo = split3(prev[...])
            lane = lax.broadcasted_iota(jnp.int32, (BASE, size - first), 1) + first
            after = lane >= row0 + BASE
            lhi, lmid, llo = [jnp.where(after, x[:, : size - first], jnp.zeros((), BF16)) for x in (hi, mid, lo)]
            update = lax.dot_general(
                jnp.concatenate([lhi, lhi, lmid, lhi, llo, lmid], axis=0),
                jnp.concatenate([hi, mid, hi, lo, hi, mid], axis=0),
                (((0,), (0,)), ((), ())),
                preferred_element_type=F32,
            )
            for v, (ref, g) in enumerate(views):
                ref[first:size, LANE * g : LANE * (g + 1)] -= update[:, LANE * v : LANE * (v + 1)]
            done = eliminate(rows, lane0)
            for t in range(2):
                for v, (ref, g) in enumerate(views):
                    ref[rows_at(row0, t), LANE * g : LANE * (g + 1)] = done[t][v]
                    prev[SUB * t : SUB * (t + 1), LANE * v : LANE * (v + 1)] = done[t][v]
            if first == 0:
                source = [jnp.where(s == LANE // BASE - 1, done[t][1], done[t][0]) for t in range(2)]
            else:
                source = [done[t][0] for t in range(2)]
            next_lane = (lane0 + BASE) % LANE
            for t in range(2):
                factor = [[lane_bcast(source[m], next_lane + SUB * t + n) for n in range(SUB)] for m in range(2)]
                for v, (ref, g) in enumerate(views):
                    parts = [factor[0][n] * done[0][v] + factor[1][n] * done[1][v] for n in range(SUB)]
                    ref[rows_at(row0 + BASE, t), LANE * g : LANE * (g + 1)] -= stack_sums(parts)
            return carry

        lax.fori_loop(0, LANE // BASE, body, 0)


def kernel(n_row, n_col, batch_axis, a_ref, o_ref, share, diag, panel, work, winv, prev, load_sem, store_sem, seed_send, seed_recv,
           send_sem, pass_sem, recv_sem):
    row_blocks, size, local_cols = a_ref.shape
    col_blocks = local_cols // size
    ratio = n_col // n_row
    steps = row_blocks * n_row
    depth = pass_sem.shape[0]
    batch = lax.axis_index(batch_axis)
    row = lax.axis_index("row")
    col = lax.axis_index("col")
    odd = lax.rem(col, 2)
    on_diag = lax.rem(col, n_row) == row
    row_slots = n_row * (row_blocks * (row_blocks + 1) // 2)

    def at(dev_row, dev_col):
        return (batch, dev_row, dev_col)

    def row_slot(k, a):
        g = k // n_row
        return n_row * (row_blocks * g - (g * (g - 1)) // 2) + (k - g * n_row) * (row_blocks - g) + a - g

    def col_slot(k, b):
        h = k // n_col
        return row_slots + n_col * (col_blocks * h - (h * (h - 1)) // 2) + (k - h * n_col) * (col_blocks - h) + b - h

    def first_a(k):
        return (k + n_row - row) // n_row

    def first_b(k):
        return (k + n_col - col) // n_col

    def home(ref, a, b):
        return ref.at[a, :, pl.ds(pl.multiple_of(b * size, size), size)]

    def spot(a, b):
        return b * row_blocks + a

    def col_of(k, b):
        return jnp.where(on_diag, row_slot(k, ratio * b + col // n_row), col_slot(k, b))

    def copy(src_slot, dst_slot, sem, device):
        return pltpu.make_async_remote_copy(
            src_ref=panel.at[src_slot], dst_ref=panel.at[dst_slot], send_sem=sem, recv_sem=recv_sem.at[dst_slot],
            device_id=device, device_id_type=MESH,
        )

    def arrived(slot):
        copy(slot, slot, send_sem.at[0, 0], at(row, col)).wait_recv()

    def start(c):
        c.start()

    def finish(c):
        c.wait_send()

    def down_column(k, a, sems, target, act):
        slot = row_slot(k, a)
        dst = col_slot(k, (a * n_row + row) // n_col)
        for m, d in enumerate((1, n_row - 1, 2)):
            act(copy(slot, dst, sems[m], at(lax.rem(row + d, n_row), target)))

    def source_sends(k, a, act):
        ahead = a * n_row + row - k
        slot = row_slot(k, a)

        @pl.when(jnp.logical_or(ahead <= 2, lax.rem(ahead, n_col) == 0))
        def _():
            down_column(k, a, [send_sem.at[a, m] for m in range(3)], lax.rem(col + ahead, n_col), act)

        @pl.when(jnp.logical_or(odd == 0, jnp.logical_or(ahead == 1, ahead >= n_col - 1)))
        def _():
            up = jnp.logical_or(odd == 0, ahead == 1)
            act(copy(slot, slot, send_sem.at[a, 3], at(row, lax.rem(jnp.where(up, col + 1, col - 1), n_col))))

        @pl.when(ahead >= 2)
        def _():
            act(copy(slot, slot, send_sem.at[a, 4], at(row, lax.rem(col - odd + 3, n_col))))

        @pl.when(ahead >= n_col - 2 - odd)
        def _():
            act(copy(slot, slot, send_sem.at[a, 5], at(row, lax.rem(col - odd - 1 + n_col, n_col))))

    def lead(p):
        return lax.rem(col - lax.rem(p, n_col) + n_col, n_col)

    def hops(p):
        return lax.rem(col // 2 - lax.rem(p, n_col) // 2 + n_col // 2, n_col // 2)

    def passes(p):
        return jnp.logical_and(odd == 1, hops(p) != 0)

    def first_passed(p):
        low = jnp.where(passes(p), jnp.maximum(lead(p) - 1, 2), lead(p))
        return (p + low - row + n_row - 1) // n_row

    def pass_on(p, a, act):
        i = a * n_row + row
        ahead = i - p
        slot = row_slot(p, a)
        sems = pass_sem.at[lax.rem(p, depth), a]
        src_odd = lax.rem(p, 2)
        far = n_col - 2 - src_odd

        @pl.when(passes(p))
        def _():
            h = hops(p)
            via_prev = jnp.logical_and(lax.rem(a, 2) == 1, ahead >= far)
            mine_to_pass = jnp.logical_or(
                jnp.logical_and(h == 1, jnp.logical_not(via_prev)), jnp.logical_and(h == n_col // 2 - 1, via_prev)
            )

            @pl.when(jnp.logical_and(mine_to_pass, ahead >= n_col // 2 - src_odd))
            def _():
                act(copy(slot, slot, sems.at[4], at(row, lax.rem(jnp.where(h == 1, col + 2, col - 2 + n_col), n_col))))

            act(copy(slot, slot, sems.at[3], at(row, col - 1)))

        @pl.when(jnp.logical_and(lax.rem(i, n_col) == col, ahead >= 3))
        def _():
            down_column(p, a, [sems.at[m] for m in range(3)], col, act)

    def receive(p, a):
        arrived(row_slot(p, a))
        pass_on(p, a, start)

    def loop(lo, hi, fn):
        lax.fori_loop(lo, hi, lambda n, c: (fn(n), c)[1], 0)

    for a in range(row_blocks):
        for b in range(col_blocks):
            pltpu.make_async_copy(home(a_ref, a, b), share.at[spot(a, b)], load_sem).start()

    barrier = pltpu.get_barrier_semaphore()
    n_dev = n_row * n_col

    def greet(n):
        other = lax.rem(row * n_col + col + n, n_dev)
        pl.semaphore_signal(barrier, inc=1, device_id=at(other // n_col, lax.rem(other, n_col)), device_id_type=MESH)

    loop(1, n_dev, greet)
    pl.semaphore_wait(barrier, n_dev - 1)
    pltpu.make_async_copy(share, share, load_sem).wait()

    def seed_copy(b, dev_row):
        return pltpu.make_async_remote_copy(
            src_ref=share.at[spot(ratio * b + col // n_row, b)], dst_ref=diag.at[b],
            send_sem=seed_send.at[b, lax.rem(dev_row - row + n_row, n_row)],
            recv_sem=seed_recv.at[b], device_id=at(dev_row, col), device_id_type=MESH,
        )

    @pl.when(on_diag)
    def _():
        for b in range(col_blocks):
            for d in (1, n_row - 1, 2):
                seed_copy(b, lax.rem(row + d, n_row)).start()
        for b in range(col_blocks):
            diag[b] = share[spot(ratio * b + col // n_row, b)]

    def seed_arrived(b):
        @pl.when(jnp.logical_not(on_diag))
        def _():
            seed_copy(b, row).wait_recv()

    seed_arrived(0)

    def clear(n):
        a, b = lax.rem(n, row_blocks), n // row_blocks

        @pl.when(a * n_row + row < b * n_col + col)
        def _():
            share[n] = jnp.zeros((size, size), F32)
            pltpu.make_async_copy(share.at[n], home(o_ref, a, b), store_sem).start()

    loop(0, row_blocks * col_blocks, clear)

    def times_t(x, y):
        return lax.dot_general(x, y, (((1,), (1,)), ((), ())), preferred_element_type=F32)

    def update_block(p, a, b):
        share[spot(a, b)] -= times_t(panel[row_slot(p, a)], panel[col_of(p, b)])

    def update_diag(p, b):
        other = panel[col_of(p, b)]
        diag[b] -= times_t(other, other)

    def column_arrived(p, b):
        @pl.when(jnp.logical_not(on_diag))
        def _():
            arrived(col_slot(p, b))

    def trail(p, b_from):
        def column(b):
            column_arrived(p, b)
            update_diag(p, b)
            lo = first_a(b * n_col + col)
            lone = lax.rem(row_blocks - lo, 2)

            @pl.when(lone == 1)
            def _():
                update_block(p, lo, b)

            def pair(m):
                a = lo + lone + 2 * m
                both = pl.ds(spot(a, b), 2)
                left = panel[pl.ds(row_slot(p, a), 2)].reshape(2 * size, size)
                share[both] -= times_t(left, panel[col_of(p, b)]).reshape(2, size, size)

            loop(0, (row_blocks - lo) // 2, pair)

        loop(b_from, col_blocks, column)

    def step(k):
        mine = col == lax.rem(k, n_col)
        kb = k // n_col
        last = k - 1
        soon = jnp.logical_and(col == lax.rem(k + 1, n_col), k + 1 < steps)

        @pl.when(jnp.logical_and(k > depth, lead(last - depth + n_col) != 0))
        def _():
            loop(first_passed(last - depth), row_blocks, lambda a: pass_on(last - depth, a, finish))

        @pl.when(k == 1)
        def _():
            for b in range(1, col_blocks):
                seed_arrived(b)

        @pl.when(mine)
        def _():
            work[0:size, :] = diag[kb]
            work[size:, :] = jnp.zeros((BASE, size), F32)
            r_id = lax.broadcasted_iota(jnp.int32, (size + BASE, size), 0)
            c_id = lax.broadcasted_iota(jnp.int32, (size + BASE, size), 1)
            winv[...] = jnp.where(r_id == c_id, 1.0, 0.0).astype(F32)
            factor_block(work, winv, prev)

            def solve(a):
                n = spot(a, kb)

                @pl.when(k > 1)
                def _():
                    update_block(k - 2, a, kb)

                @pl.when(k > 0)
                def _():
                    receive(last, a)
                    update_block(last, a, kb)

                x = lax.dot_general(
                    share[n], winv[0:size, :], (((1,), (1,)), ((), ())), precision=lax.Precision.HIGHEST,
                    preferred_element_type=F32,
                )
                panel[row_slot(k, a)] = x.astype(BF16)
                share[n] = x
                source_sends(k, a, start)
                pltpu.make_async_copy(share.at[n], home(o_ref, a, kb), store_sem).start()

            loop(first_a(k), row_blocks, solve)

            @pl.when(row == lax.rem(k, n_row))
            def _():
                for d in range(1, n_row):
                    seed_copy(kb, lax.rem(row + d, n_row)).wait_send()
                r_id = lax.broadcasted_iota(jnp.int32, (size, size), 0)
                c_id = lax.broadcasted_iota(jnp.int32, (size, size), 1)
                n = spot(k // n_row, kb)
                share[n] = jnp.where(r_id >= c_id, work[0:size, :].T, 0.0)
                pltpu.make_async_copy(share.at[n], home(o_ref, k // n_row, kb), store_sem).start()

            @pl.when(k > 1)
            def _():
                trail(k - 2, kb + 1)

            @pl.when(k > 0)
            def _():
                trail(last, kb + 1)

        @pl.when(jnp.logical_and(k > 0, jnp.logical_not(mine)))
        def _():
            @pl.when(col != lax.rem(last, n_col))
            def _():
                loop(first_passed(last), row_blocks, lambda a: receive(last, a))

            @pl.when(jnp.logical_not(soon))
            def _():
                trail(last, first_b(last))

        @pl.when(soon)
        def _():
            nb = (k + 1) // n_col

            @pl.when(k > 0)
            def _():
                column_arrived(last, nb)
                update_diag(last, nb)

            arrived(col_of(k, nb))
            update_diag(k, nb)

        @pl.when(jnp.logical_and(k >= n_col // 2, col == lax.rem(k + n_col // 2, n_col)))
        def _():
            loop(first_a(k - n_col // 2), row_blocks, lambda a: source_sends(k - n_col // 2, a, finish))

    loop(0, steps, step)

    def last_passes(p):
        @pl.when(lead(p) != 0)
        def _():
            loop(first_passed(p), row_blocks, lambda a: pass_on(p, a, finish))

    loop(steps - 1 - depth, steps - 1, last_passes)

    def last_sends(k):
        @pl.when(col == lax.rem(k, n_col))
        def _():
            loop(first_a(k), row_blocks, lambda a: source_sends(k, a, finish))

    loop(steps - n_col // 2, steps, last_sends)
    pltpu.make_async_copy(share, share, store_sem).wait()


def solution(mesh):
    n_row = mesh.shape["row"]
    n_col = mesh.shape["col"]

    def factor_local(a_loc):
        row_blocks, size, local_cols = a_loc.shape
        col_blocks = local_cols // size
        slots = n_row * (row_blocks * (row_blocks + 1) // 2) + n_col * (col_blocks * (col_blocks + 1) // 2)
        return pl.pallas_call(
            functools.partial(kernel, n_row, n_col, "batch"),
            out_shape=jax.ShapeDtypeStruct(a_loc.shape, F32),
            in_specs=[pl.BlockSpec(memory_space=pl.ANY)],
            out_specs=pl.BlockSpec(memory_space=pl.ANY),
            scratch_shapes=[
                pltpu.VMEM((row_blocks * col_blocks, size, size), F32),
                pltpu.VMEM((col_blocks, size, size), F32),
                pltpu.VMEM((slots, size, size), BF16),
                pltpu.VMEM((size + BASE, size), F32),
                pltpu.VMEM((size + BASE, size), F32),
                pltpu.VMEM((BASE, 3 * LANE), F32),
                pltpu.SemaphoreType.DMA,
                pltpu.SemaphoreType.DMA,
                pltpu.SemaphoreType.DMA((col_blocks, n_row)),
                pltpu.SemaphoreType.DMA((col_blocks,)),
                pltpu.SemaphoreType.DMA((row_blocks, 6)),
                pltpu.SemaphoreType.DMA((4, row_blocks, 5)),
                pltpu.SemaphoreType.DMA((slots,)),
            ],
            compiler_params=pltpu.CompilerParams(
                collective_id=0, has_side_effects=True, vmem_limit_bytes=60 * 1024 * 1024
            ),
            name="cholesky",
        )(a_loc)

    blk_spec = P(("batch", "row"), None, "col")
    return jax.shard_map(factor_local, mesh=mesh, in_specs=(blk_spec,), out_specs=blk_spec, check_vma=False)
```

```python
import functools

import jax
import jax.numpy as jnp
from jax import lax
from jax.experimental import pallas as pl
from jax.experimental.pallas import tpu as pltpu
from jax.sharding import PartitionSpec as P

F32 = jnp.float32
BF16 = jnp.bfloat16
MESH = pl.DeviceIdType.MESH
SUB = 8
LANE = 128
BASE = 16


def sub_bcast(x, q):
    return jnp.broadcast_to(x[q : q + 1, :], (SUB, LANE))


def lane_bcast(x, lane):
    return jnp.take_along_axis(x, jnp.full((SUB, LANE), lane, jnp.int32), axis=1)


def split3(x):
    high = x.astype(BF16)
    rest = x - high.astype(F32)
    mid = rest.astype(BF16)
    return high, mid, (rest - mid.astype(F32)).astype(BF16)


def swap_rows(x, bit, row_id):
    if bit == SUB // 2:
        return pltpu.roll(x, bit, 0)
    return jnp.where((row_id & bit) == 0, pltpu.roll(x, SUB - bit, 0), pltpu.roll(x, bit, 0))


def stack_sums(parts):
    row_id = lax.broadcasted_iota(jnp.int32, (SUB, LANE), 0)
    for bit in (4, 2, 1):
        low = (row_id & bit) == 0
        half = len(parts) // 2
        parts = [
            jnp.where(low, parts[n], parts[n + half]) + swap_rows(jnp.where(low, parts[n + half], parts[n]), bit, row_id)
            for n in range(half)
        ]
    return parts[0]


def eliminate(rows, lane0):
    row_id = lax.broadcasted_iota(jnp.int32, (SUB, LANE), 0)
    rows = [list(rows[0]), list(rows[1])]
    cols = [
        [lane_bcast(rows[0][0], lane0 + j) for j in range(SUB)],
        [lane_bcast(rows[1][0], lane0 + j) for j in range(BASE)],
    ]
    scale = [jnp.zeros((SUB, LANE), F32), jnp.zeros((SUB, LANE), F32)]
    pivot = sub_bcast(cols[0][0], 0)
    for j in range(BASE):
        t, q = divmod(j, SUB)
        inv = lax.rsqrt(pivot)
        scale[t] = jnp.where(row_id == q, inv, scale[t])
        if j + 1 < BASE:
            tn, qn = divmod(j + 1, SUB)
            near = sub_bcast(cols[tn][j], qn) * inv
            pivot = sub_bcast(cols[tn][j + 1], qn) - near * near
        below = cols[1][j] * inv
        here = cols[0][j] * inv if t == 0 else None
        for n in range(j + 1, BASE):
            tn, qn = divmod(n, SUB)
            other = sub_bcast(cols[tn][j], qn) * inv
            if t == 0 and tn == 0:
                cols[0][n] = cols[0][n] - here * other
            cols[1][n] = cols[1][n] - below * other
        masked = jnp.where(row_id > q, here if t == 0 else below, 0.0)
        for v in range(len(rows[0])):
            pivot_row = sub_bcast(rows[t][v], q) * inv
            rows[t][v] = rows[t][v] - masked * pivot_row
            if t == 0:
                rows[1][v] = rows[1][v] - below * pivot_row
    return [[x * scale[t] for x in rows[t]] for t in range(2)]


def factor_block(work, winv, prev):
    size = work.shape[1]
    prev[...] = jnp.zeros(prev.shape, F32)
    for half in range(size // LANE):
        views = [(work, 0), (work, 1), (winv, 0)] if half == 0 else [(work, 1), (winv, 0), (winv, 1)]
        first = half * LANE
        if half == 1:
            mid_part, inv_part = prev[:, LANE : 2 * LANE], prev[:, 2 * LANE :]
            prev[:, :LANE] = mid_part
            prev[:, LANE : 2 * LANE] = inv_part
            prev[:, 2 * LANE :] = jnp.zeros((BASE, LANE), F32)

        def body(s, carry, views=views, first=first):
            lane0 = s * BASE
            row0 = pl.multiple_of(first + lane0, BASE)

            def rows_at(row, t):
                return pl.ds(pl.multiple_of(row + SUB * t, SUB), SUB)

            rows = [[ref[rows_at(row0, t), LANE * g : LANE * (g + 1)] for ref, g in views] for t in range(2)]
            hi, mid, lo = split3(prev[...])
            lane = lax.broadcasted_iota(jnp.int32, (BASE, size - first), 1) + first
            after = lane >= row0 + BASE
            lhi, lmid, llo = [jnp.where(after, x[:, : size - first], jnp.zeros((), BF16)) for x in (hi, mid, lo)]
            update = lax.dot_general(
                jnp.concatenate([lhi, lhi, lmid, lhi, llo, lmid], axis=0),
                jnp.concatenate([hi, mid, hi, lo, hi, mid], axis=0),
                (((0,), (0,)), ((), ())),
                preferred_element_type=F32,
            )
            for v, (ref, g) in enumerate(views):
                ref[first:size, LANE * g : LANE * (g + 1)] -= update[:, LANE * v : LANE * (v + 1)]
            done = eliminate(rows, lane0)
            for t in range(2):
                for v, (ref, g) in enumerate(views):
                    ref[rows_at(row0, t), LANE * g : LANE * (g + 1)] = done[t][v]
                    prev[SUB * t : SUB * (t + 1), LANE * v : LANE * (v + 1)] = done[t][v]
            if first == 0:
                source = [jnp.where(s == LANE // BASE - 1, done[t][1], done[t][0]) for t in range(2)]
            else:
                source = [done[t][0] for t in range(2)]
            next_lane = (lane0 + BASE) % LANE
            for t in range(2):
                factor = [[lane_bcast(source[m], next_lane + SUB * t + n) for n in range(SUB)] for m in range(2)]
                for v, (ref, g) in enumerate(views):
                    parts = [factor[0][n] * done[0][v] + factor[1][n] * done[1][v] for n in range(SUB)]
                    ref[rows_at(row0 + BASE, t), LANE * g : LANE * (g + 1)] -= stack_sums(parts)
            return carry

        lax.fori_loop(0, LANE // BASE, body, 0)


def kernel(n_row, n_col, batch_axis, a_ref, o_ref, share, diag, panel, work, winv, winv3, prev, load_sem, store_sem, seed_send, seed_recv,
           send_sem, pass_sem, recv_sem):
    row_blocks, size, local_cols = a_ref.shape
    col_blocks = local_cols // size
    ratio = n_col // n_row
    steps = row_blocks * n_row
    depth = pass_sem.shape[0]
    batch = lax.axis_index(batch_axis)
    row = lax.axis_index("row")
    col = lax.axis_index("col")
    odd = lax.rem(col, 2)
    on_diag = lax.rem(col, n_row) == row
    row_slots = n_row * (row_blocks * (row_blocks + 1) // 2)

    def at(dev_row, dev_col):
        return (batch, dev_row, dev_col)

    def row_slot(k, a):
        g = k // n_row
        return n_row * (row_blocks * g - (g * (g - 1)) // 2) + (k - g * n_row) * (row_blocks - g) + a - g

    def col_slot(k, b):
        h = k // n_col
        return row_slots + n_col * (col_blocks * h - (h * (h - 1)) // 2) + (k - h * n_col) * (col_blocks - h) + b - h

    def first_a(k):
        return (k + n_row - row) // n_row

    def first_b(k):
        return (k + n_col - col) // n_col

    def home(ref, a, b):
        return ref.at[a, :, pl.ds(pl.multiple_of(b * size, size), size)]

    def spot(a, b):
        return b * row_blocks + a

    def col_of(k, b):
        return jnp.where(on_diag, row_slot(k, ratio * b + col // n_row), col_slot(k, b))

    def copy(src_slot, dst_slot, sem, device):
        return pltpu.make_async_remote_copy(
            src_ref=panel.at[src_slot], dst_ref=panel.at[dst_slot], send_sem=sem, recv_sem=recv_sem.at[dst_slot],
            device_id=device, device_id_type=MESH,
        )

    def arrived(slot):
        copy(slot, slot, send_sem.at[0, 0], at(row, col)).wait_recv()

    def start(c):
        c.start()

    def finish(c):
        c.wait_send()

    def down_column(k, a, ways, sems, target, act):
        slot = row_slot(k, a)
        dst = col_slot(k, (a * n_row + row) // n_col)
        for m, d in enumerate(ways):
            act(copy(slot, dst, sems[m], at(lax.rem(row + d, n_row), target)))

    def source_sends(k, a, act):
        ahead = a * n_row + row - k
        slot = row_slot(k, a)

        @pl.when(ahead == 1)
        def _():
            dst = col_slot(k, (k + 1) // n_col)
            act(copy(slot, dst, send_sem.at[a, 0], at(lax.rem(row + 1, n_row), lax.rem(col + 1, n_col))))

        @pl.when(lax.rem(ahead, n_col) == 0)
        def _():
            down_column(k, a, (1, n_row - 1, 2), [send_sem.at[a, m] for m in range(3)], col, act)

        @pl.when(jnp.logical_or(odd == 0, jnp.logical_or(ahead == 1, ahead >= n_col - 1)))
        def _():
            up = jnp.logical_or(odd == 0, ahead == 1)
            act(copy(slot, slot, send_sem.at[a, 3], at(row, lax.rem(jnp.where(up, col + 1, col - 1), n_col))))

        @pl.when(ahead >= 2)
        def _():
            act(copy(slot, slot, send_sem.at[a, 4], at(row, lax.rem(col - odd + 3, n_col))))

        @pl.when(ahead >= n_col - 2 - odd)
        def _():
            act(copy(slot, slot, send_sem.at[a, 5], at(row, lax.rem(col - odd - 1 + n_col, n_col))))

    def lead(p):
        return lax.rem(col - lax.rem(p, n_col) + n_col, n_col)

    def hops(p):
        return lax.rem(col // 2 - lax.rem(p, n_col) // 2 + n_col // 2, n_col // 2)

    def passes(p):
        return jnp.logical_and(odd == 1, hops(p) != 0)

    def first_passed(p):
        low = jnp.where(passes(p), jnp.maximum(lead(p) - 1, 2), lead(p))
        return (p + low - row + n_row - 1) // n_row

    def pass_on(p, a, act):
        i = a * n_row + row
        ahead = i - p
        slot = row_slot(p, a)
        sems = pass_sem.at[lax.rem(p, depth), a]
        src_odd = lax.rem(p, 2)
        far = n_col - 2 - src_odd

        @pl.when(passes(p))
        def _():
            h = hops(p)
            via_prev = jnp.logical_and(lax.rem(a, 2) == 1, ahead >= far)
            mine_to_pass = jnp.logical_or(
                jnp.logical_and(h == 1, jnp.logical_not(via_prev)), jnp.logical_and(h == n_col // 2 - 1, via_prev)
            )

            @pl.when(jnp.logical_and(mine_to_pass, ahead >= n_col // 2 - src_odd))
            def _():
                act(copy(slot, slot, sems.at[4], at(row, lax.rem(jnp.where(h == 1, col + 2, col - 2 + n_col), n_col))))

            act(copy(slot, slot, sems.at[3], at(row, col - 1)))

        own = lax.rem(i, n_col) == col

        @pl.when(jnp.logical_and(own, ahead == 1))
        def _():
            down_column(p, a, (n_row - 1, 2), [sems.at[m] for m in range(2)], col, act)

        @pl.when(jnp.logical_and(own, ahead > 1))
        def _():
            down_column(p, a, (1, n_row - 1, 2), [sems.at[m] for m in range(3)], col, act)

    def passed(p):
        @pl.when(lead(p) != 0)
        def _():
            loop(first_passed(p), row_blocks, lambda a: pass_on(p, a, finish))

    def receive(p, a):
        arrived(row_slot(p, a))
        pass_on(p, a, start)

    def loop(lo, hi, fn):
        lax.fori_loop(lo, hi, lambda n, c: (fn(n), c)[1], 0)

    for a in range(row_blocks):
        for b in range(col_blocks):
            pltpu.make_async_copy(home(a_ref, a, b), share.at[spot(a, b)], load_sem).start()

    barrier = pltpu.get_barrier_semaphore()
    n_dev = n_row * n_col

    def greet(n):
        other = lax.rem(row * n_col + col + n, n_dev)
        pl.semaphore_signal(barrier, inc=1, device_id=at(other // n_col, lax.rem(other, n_col)), device_id_type=MESH)

    loop(1, n_dev, greet)
    pl.semaphore_wait(barrier, n_dev - 1)
    pltpu.make_async_copy(share, share, load_sem).wait()

    def seed_copy(b, dev_row):
        return pltpu.make_async_remote_copy(
            src_ref=share.at[spot(ratio * b + col // n_row, b)], dst_ref=diag.at[b],
            send_sem=seed_send.at[b, lax.rem(dev_row - row + n_row, n_row)],
            recv_sem=seed_recv.at[b], device_id=at(dev_row, col), device_id_type=MESH,
        )

    @pl.when(on_diag)
    def _():
        for b in range(col_blocks):
            for d in (1, n_row - 1, 2):
                seed_copy(b, lax.rem(row + d, n_row)).start()
        for b in range(col_blocks):
            diag[b] = share[spot(ratio * b + col // n_row, b)]

    def seed_arrived(b):
        @pl.when(jnp.logical_not(on_diag))
        def _():
            seed_copy(b, row).wait_recv()

    seed_arrived(0)

    def clear(n):
        a, b = lax.rem(n, row_blocks), n // row_blocks

        @pl.when(a * n_row + row < b * n_col + col)
        def _():
            share[n] = jnp.zeros((size, size), F32)
            pltpu.make_async_copy(share.at[n], home(o_ref, a, b), store_sem).start()

    loop(0, row_blocks * col_blocks, clear)

    def times_t(x, y):
        return lax.dot_general(x, y, (((1,), (1,)), ((), ())), preferred_element_type=F32)

    def update_block(p, a, b):
        share[spot(a, b)] -= times_t(panel[row_slot(p, a)], panel[col_of(p, b)])

    def update_diag(p, b):
        other = panel[col_of(p, b)]
        diag[b] -= times_t(other, other)

    def column_arrived(p, b):
        @pl.when(jnp.logical_not(on_diag))
        def _():
            arrived(col_slot(p, b))

    def trail(p, b_from):
        def column(b):
            column_arrived(p, b)
            update_diag(p, b)
            lo = first_a(b * n_col + col)
            lone = lax.rem(row_blocks - lo, 2)

            @pl.when(lone == 1)
            def _():
                update_block(p, lo, b)

            def pair(m):
                a = lo + lone + 2 * m
                both = pl.ds(spot(a, b), 2)
                left = panel[pl.ds(row_slot(p, a), 2)].reshape(2 * size, size)
                share[both] -= times_t(left, panel[col_of(p, b)]).reshape(2, size, size)

            loop(0, (row_blocks - lo) // 2, pair)

        loop(b_from, col_blocks, column)

    def prepare(b):
        work[size:, :] = jnp.zeros((BASE, size), F32)
        r_id = lax.broadcasted_iota(jnp.int32, (size + BASE, size), 0)
        c_id = lax.broadcasted_iota(jnp.int32, (size + BASE, size), 1)
        winv[...] = jnp.where(r_id == c_id, 1.0, 0.0).astype(F32)

    def times_winv_t(x):
        hi, mid, lo = split3(x)
        whi, wmid, wlo = winv3[0], winv3[1], winv3[2]
        small = times_t(lo, whi) + times_t(mid, wmid) + times_t(hi, wlo)
        return small + (times_t(mid, whi) + times_t(hi, wmid)) + times_t(hi, whi)

    def solve(k, a, count):
        kb = k // n_col
        here = pl.ds(spot(a, kb), count)

        @pl.when(k > 0)
        def _():
            last = k - 1
            for m in range(count):
                receive(last, a + m)
            left = panel[pl.ds(row_slot(last, a), count)].reshape(count * size, size)
            share[here] -= times_t(left, panel[col_of(last, kb)]).reshape(count, size, size)

        x = times_winv_t(share[here].reshape(count * size, size)).reshape(count, size, size)
        panel[pl.ds(row_slot(k, a), count)] = x.astype(BF16)
        share[here] = x
        for m in range(count):
            source_sends(k, a + m, start)
        for m in range(count):
            pltpu.make_async_copy(share.at[spot(a + m, kb)], home(o_ref, a + m, kb), store_sem).start()

    @pl.when(col == 0)
    def _():
        prepare(0)
        work[0:size, :] = diag[0]

    def step(k):
        mine = col == lax.rem(k, n_col)
        kb = k // n_col
        last = k - 1
        soon = jnp.logical_and(col == lax.rem(k + 1, n_col), k + 1 < steps)

        @pl.when(mine)
        def _():
            factor_block(work, winv, prev)
            for n, part in enumerate(split3(winv[0:size, :])):
                winv3[n] = part
            lo = first_a(k)
            single = jnp.minimum(lo + 1 + lax.rem(row_blocks - lo + 1, 2), row_blocks)
            loop(lo, single, lambda a: solve(k, a, 1))
            loop(0, (row_blocks - single) // 2, lambda m: solve(k, single + 2 * m, 2))

        @pl.when(k >= depth)
        def _():
            passed(k - depth)

        @pl.when(k == 1)
        def _():
            for b in range(1, col_blocks):
                seed_arrived(b)

        @pl.when(mine)
        def _():
            @pl.when(row == lax.rem(k, n_row))
            def _():
                for d in range(1, n_row):
                    seed_copy(kb, lax.rem(row + d, n_row)).wait_send()
                r_id = lax.broadcasted_iota(jnp.int32, (size, size), 0)
                c_id = lax.broadcasted_iota(jnp.int32, (size, size), 1)
                n = spot(k // n_row, kb)
                share[n] = jnp.where(r_id >= c_id, work[0:size, :].T, 0.0)
                pltpu.make_async_copy(share.at[n], home(o_ref, k // n_row, kb), store_sem).start()

            @pl.when(k > 1)
            def _():
                trail(k - 2, kb + 1)

            @pl.when(k > 0)
            def _():
                trail(last, kb + 1)

        @pl.when(jnp.logical_and(k > 0, jnp.logical_not(jnp.logical_or(mine, soon))))
        def _():
            @pl.when(col != lax.rem(last, n_col))
            def _():
                loop(first_passed(last), row_blocks, lambda a: receive(last, a))

            trail(last, first_b(last))

        @pl.when(soon)
        def _():
            nb = (k + 1) // n_col

            @pl.when(k > 0)
            def _():
                @pl.when(on_diag)
                def _():
                    receive(last, (k + 1) // n_row)

                column_arrived(last, nb)
                update_diag(last, nb)

                def catch_up(a):
                    receive(last, a)
                    update_block(last, a, nb)

                loop(first_a(k + 1), row_blocks, catch_up)

            prepare(nb)
            slot = col_of(k, nb)
            arrived(slot)

            @pl.when(on_diag)
            def _():
                pass_on(k, (k + 1) // n_row, start)

            other = panel[slot]
            work[0:size, :] = diag[nb] - times_t(other, other)

        @pl.when(jnp.logical_and(k >= n_col // 2, col == lax.rem(k + n_col // 2, n_col)))
        def _():
            loop(first_a(k - n_col // 2), row_blocks, lambda a: source_sends(k - n_col // 2, a, finish))

    loop(0, steps, step)

    loop(steps - depth, steps, passed)

    def last_sends(k):
        @pl.when(col == lax.rem(k, n_col))
        def _():
            loop(first_a(k), row_blocks, lambda a: source_sends(k, a, finish))

    loop(steps - n_col // 2, steps, last_sends)
    pltpu.make_async_copy(share, share, store_sem).wait()


def solution(mesh):
    n_row = mesh.shape["row"]
    n_col = mesh.shape["col"]

    def factor_local(a_loc):
        row_blocks, size, local_cols = a_loc.shape
        col_blocks = local_cols // size
        slots = n_row * (row_blocks * (row_blocks + 1) // 2) + n_col * (col_blocks * (col_blocks + 1) // 2)
        return pl.pallas_call(
            functools.partial(kernel, n_row, n_col, "batch"),
            out_shape=jax.ShapeDtypeStruct(a_loc.shape, F32),
            in_specs=[pl.BlockSpec(memory_space=pl.ANY)],
            out_specs=pl.BlockSpec(memory_space=pl.ANY),
            scratch_shapes=[
                pltpu.VMEM((row_blocks * col_blocks, size, size), F32),
                pltpu.VMEM((col_blocks, size, size), F32),
                pltpu.VMEM((slots, size, size), BF16),
                pltpu.VMEM((size + BASE, size), F32),
                pltpu.VMEM((size + BASE, size), F32),
                pltpu.VMEM((3, size, size), BF16),
                pltpu.VMEM((BASE, 3 * LANE), F32),
                pltpu.SemaphoreType.DMA,
                pltpu.SemaphoreType.DMA,
                pltpu.SemaphoreType.DMA((col_blocks, n_row)),
                pltpu.SemaphoreType.DMA((col_blocks,)),
                pltpu.SemaphoreType.DMA((row_blocks, 6)),
                pltpu.SemaphoreType.DMA((4, row_blocks, 5)),
                pltpu.SemaphoreType.DMA((slots,)),
            ],
            compiler_params=pltpu.CompilerParams(
                collective_id=0, has_side_effects=True, vmem_limit_bytes=60 * 1024 * 1024
            ),
            name="cholesky",
        )(a_loc)

    blk_spec = P(("batch", "row"), None, "col")
    return jax.shard_map(factor_local, mesh=mesh, in_specs=(blk_spec,), out_specs=blk_spec, check_vma=False)
```

```python
import functools

import jax
import jax.numpy as jnp
from jax import lax
from jax.experimental import pallas as pl
from jax.experimental.pallas import tpu as pltpu
from jax.sharding import PartitionSpec as P

F32 = jnp.float32
BF16 = jnp.bfloat16
MESH = pl.DeviceIdType.MESH
SUB = 8
LANE = 128
BASE = 16


def sub_bcast(x, q):
    return jnp.broadcast_to(x[q : q + 1, :], (SUB, LANE))


def lane_bcast(x, lane):
    return jnp.take_along_axis(x, jnp.full((SUB, LANE), lane, jnp.int32), axis=1)


def split3(x):
    high = x.astype(BF16)
    rest = x - high.astype(F32)
    mid = rest.astype(BF16)
    return high, mid, (rest - mid.astype(F32)).astype(BF16)


def swap_rows(x, bit, row_id):
    if bit == SUB // 2:
        return pltpu.roll(x, bit, 0)
    return jnp.where((row_id & bit) == 0, pltpu.roll(x, SUB - bit, 0), pltpu.roll(x, bit, 0))


def stack_sums(parts):
    row_id = lax.broadcasted_iota(jnp.int32, (SUB, LANE), 0)
    for bit in (4, 2, 1):
        low = (row_id & bit) == 0
        half = len(parts) // 2
        parts = [
            jnp.where(low, parts[n], parts[n + half]) + swap_rows(jnp.where(low, parts[n + half], parts[n]), bit, row_id)
            for n in range(half)
        ]
    return parts[0]


def eliminate(rows, lane0):
    row_id = lax.broadcasted_iota(jnp.int32, (SUB, LANE), 0)
    rows = [list(rows[0]), list(rows[1])]
    cols = [
        [lane_bcast(rows[0][0], lane0 + j) for j in range(SUB)],
        [lane_bcast(rows[1][0], lane0 + j) for j in range(BASE)],
    ]
    scale = [jnp.zeros((SUB, LANE), F32), jnp.zeros((SUB, LANE), F32)]
    pivot = sub_bcast(cols[0][0], 0)
    for j in range(BASE):
        t, q = divmod(j, SUB)
        inv = lax.rsqrt(pivot)
        scale[t] = jnp.where(row_id == q, inv, scale[t])
        if j + 1 < BASE:
            tn, qn = divmod(j + 1, SUB)
            near = sub_bcast(cols[tn][j], qn) * inv
            pivot = sub_bcast(cols[tn][j + 1], qn) - near * near
        below = cols[1][j] * inv
        here = cols[0][j] * inv if t == 0 else None
        for n in range(j + 1, BASE):
            tn, qn = divmod(n, SUB)
            other = sub_bcast(cols[tn][j], qn) * inv
            if t == 0 and tn == 0:
                cols[0][n] = cols[0][n] - here * other
            cols[1][n] = cols[1][n] - below * other
        masked = jnp.where(row_id > q, here if t == 0 else below, 0.0)
        for v in range(len(rows[0])):
            pivot_row = sub_bcast(rows[t][v], q) * inv
            rows[t][v] = rows[t][v] - masked * pivot_row
            if t == 0:
                rows[1][v] = rows[1][v] - below * pivot_row
    return [[x * scale[t] for x in rows[t]] for t in range(2)]


def factor_block(work, winv, prev):
    size = work.shape[1]
    prev[...] = jnp.zeros(prev.shape, F32)
    for half in range(size // LANE):
        views = [(work, 0), (work, 1), (winv, 0)] if half == 0 else [(work, 1), (winv, 0), (winv, 1)]
        first = half * LANE
        if half == 1:
            mid_part, inv_part = prev[:, LANE : 2 * LANE], prev[:, 2 * LANE :]
            prev[:, :LANE] = mid_part
            prev[:, LANE : 2 * LANE] = inv_part
            prev[:, 2 * LANE :] = jnp.zeros((BASE, LANE), F32)

        def body(s, carry, views=views, first=first):
            lane0 = s * BASE
            row0 = pl.multiple_of(first + lane0, BASE)

            def rows_at(row, t):
                return pl.ds(pl.multiple_of(row + SUB * t, SUB), SUB)

            rows = [[ref[rows_at(row0, t), LANE * g : LANE * (g + 1)] for ref, g in views] for t in range(2)]
            hi, mid, lo = split3(prev[...])
            lane = lax.broadcasted_iota(jnp.int32, (BASE, size - first), 1) + first
            after = lane >= row0 + BASE
            lhi, lmid, llo = [jnp.where(after, x[:, : size - first], jnp.zeros((), BF16)) for x in (hi, mid, lo)]
            update = lax.dot_general(
                jnp.concatenate([lhi, lhi, lmid, lhi, llo, lmid], axis=0),
                jnp.concatenate([hi, mid, hi, lo, hi, mid], axis=0),
                (((0,), (0,)), ((), ())),
                preferred_element_type=F32,
            )
            for v, (ref, g) in enumerate(views):
                ref[first:size, LANE * g : LANE * (g + 1)] -= update[:, LANE * v : LANE * (v + 1)]
            done = eliminate(rows, lane0)
            for t in range(2):
                for v, (ref, g) in enumerate(views):
                    ref[rows_at(row0, t), LANE * g : LANE * (g + 1)] = done[t][v]
                    prev[SUB * t : SUB * (t + 1), LANE * v : LANE * (v + 1)] = done[t][v]
            if first == 0:
                source = [jnp.where(s == LANE // BASE - 1, done[t][1], done[t][0]) for t in range(2)]
            else:
                source = [done[t][0] for t in range(2)]
            next_lane = (lane0 + BASE) % LANE
            for t in range(2):
                factor = [[lane_bcast(source[m], next_lane + SUB * t + n) for n in range(SUB)] for m in range(2)]
                for v, (ref, g) in enumerate(views):
                    parts = [factor[0][n] * done[0][v] + factor[1][n] * done[1][v] for n in range(SUB)]
                    ref[rows_at(row0 + BASE, t), LANE * g : LANE * (g + 1)] -= stack_sums(parts)
            return carry

        lax.fori_loop(0, LANE // BASE, body, 0)


def kernel(n_row, n_col, batch_axis, a_ref, o_ref, share, diag, panel, work, winv, winv3, prev, load_sem, store_sem, seed_send, seed_recv,
           send_sem, pass_sem, column_sem, recv_sem):
    row_blocks, size, local_cols = a_ref.shape
    col_blocks = local_cols // size
    ratio = n_col // n_row
    steps = row_blocks * n_row
    depth = pass_sem.shape[0]
    batch = lax.axis_index(batch_axis)
    row = lax.axis_index("row")
    col = lax.axis_index("col")
    odd = lax.rem(col, 2)
    on_diag = lax.rem(col, n_row) == row
    row_slots = n_row * (row_blocks * (row_blocks + 1) // 2)

    def at(dev_row, dev_col):
        return (batch, dev_row, dev_col)

    def row_slot(k, a):
        g = k // n_row
        return n_row * (row_blocks * g - (g * (g - 1)) // 2) + (k - g * n_row) * (row_blocks - g) + a - g

    def col_slot(k, b):
        h = k // n_col
        return row_slots + n_col * (col_blocks * h - (h * (h - 1)) // 2) + (k - h * n_col) * (col_blocks - h) + b - h

    def first_a(k):
        return (k + n_row - row) // n_row

    def first_b(k):
        return (k + n_col - col) // n_col

    def home(ref, a, b):
        return ref.at[a, :, pl.ds(pl.multiple_of(b * size, size), size)]

    def spot(a, b):
        return b * row_blocks + a

    def col_of(k, b):
        return jnp.where(on_diag, row_slot(k, ratio * b + col // n_row), col_slot(k, b))

    def copy(src_slot, dst_slot, sem, device):
        return pltpu.make_async_remote_copy(
            src_ref=panel.at[src_slot], dst_ref=panel.at[dst_slot], send_sem=sem, recv_sem=recv_sem.at[dst_slot],
            device_id=device, device_id_type=MESH,
        )

    def arrived(slot):
        copy(slot, slot, send_sem.at[0, 0], at(row, col)).wait_recv()

    def start(c):
        c.start()

    def finish(c):
        c.wait_send()

    def down_column(k, a, ways, sems, target, act):
        slot = row_slot(k, a)
        dst = col_slot(k, (a * n_row + row) // n_col)
        for m, d in enumerate(ways):
            act(copy(slot, dst, sems[m], at(lax.rem(row + d, n_row), target)))

    def source_sends(k, a, act):
        ahead = a * n_row + row - k
        slot = row_slot(k, a)

        @pl.when(ahead == 1)
        def _():
            dst = col_slot(k, (k + 1) // n_col)
            act(copy(slot, dst, send_sem.at[a, 0], at(lax.rem(row + 1, n_row), lax.rem(col + 1, n_col))))

        @pl.when(lax.rem(ahead, n_col) == 0)
        def _():
            down_column(k, a, (1, n_row - 1), [send_sem.at[a, m] for m in range(2)], col, act)

        @pl.when(jnp.logical_or(odd == 0, jnp.logical_or(ahead == 1, ahead >= n_col - 1)))
        def _():
            up = jnp.logical_or(odd == 0, ahead == 1)
            act(copy(slot, slot, send_sem.at[a, 3], at(row, lax.rem(jnp.where(up, col + 1, col - 1), n_col))))

        @pl.when(ahead >= 2)
        def _():
            act(copy(slot, slot, send_sem.at[a, 4], at(row, lax.rem(col - odd + 3, n_col))))

        @pl.when(ahead >= n_col - 2 - odd)
        def _():
            act(copy(slot, slot, send_sem.at[a, 5], at(row, lax.rem(col - odd - 1 + n_col, n_col))))

    def lead(p):
        return lax.rem(col - lax.rem(p, n_col) + n_col, n_col)

    def hops(p):
        return lax.rem(col // 2 - lax.rem(p, n_col) // 2 + n_col // 2, n_col // 2)

    def passes(p):
        return jnp.logical_and(odd == 1, hops(p) != 0)

    def first_passed(p):
        low = jnp.where(passes(p), jnp.maximum(lead(p) - 1, 2), lead(p))
        return (p + low - row + n_row - 1) // n_row

    def pass_on(p, a, act):
        i = a * n_row + row
        ahead = i - p
        slot = row_slot(p, a)
        sems = pass_sem.at[lax.rem(p, depth), a]
        src_odd = lax.rem(p, 2)
        far = n_col - 2 - src_odd

        @pl.when(passes(p))
        def _():
            h = hops(p)
            via_prev = jnp.logical_and(lax.rem(a, 2) == 1, ahead >= far)
            mine_to_pass = jnp.logical_or(
                jnp.logical_and(h == 1, jnp.logical_not(via_prev)), jnp.logical_and(h == n_col // 2 - 1, via_prev)
            )

            @pl.when(jnp.logical_and(mine_to_pass, ahead >= n_col // 2 - src_odd))
            def _():
                act(copy(slot, slot, sems.at[4], at(row, lax.rem(jnp.where(h == 1, col + 2, col - 2 + n_col), n_col))))

            act(copy(slot, slot, sems.at[3], at(row, col - 1)))

        own = lax.rem(i, n_col) == col

        @pl.when(jnp.logical_and(own, ahead == 1))
        def _():
            down_column(p, a, (n_row - 1, 2), [sems.at[m] for m in range(2)], col, act)

        @pl.when(jnp.logical_and(own, ahead > 1))
        def _():
            down_column(p, a, (1, n_row - 1), [sems.at[m] for m in range(2)], col, act)

    def column_pass_on(p, b, act):
        j = b * n_col + col
        away = lax.rem(row - lax.rem(j, n_row) + n_row, n_row)

        @pl.when(jnp.logical_and(j > p + 1, away == jnp.where(lax.rem(b, 2) == 0, 1, n_row - 1)))
        def _():
            slot = col_slot(p, b)
            act(copy(slot, slot, column_sem.at[lax.rem(p, depth), b], at(lax.rem(row + away, n_row), col)))

    def passed(p):
        @pl.when(lead(p) != 0)
        def _():
            loop(first_passed(p), row_blocks, lambda a: pass_on(p, a, finish))

        loop(first_b(p), col_blocks, lambda b: column_pass_on(p, b, finish))

    def receive(p, a):
        arrived(row_slot(p, a))
        pass_on(p, a, start)

    def loop(lo, hi, fn):
        lax.fori_loop(lo, hi, lambda n, c: (fn(n), c)[1], 0)

    for a in range(row_blocks):
        for b in range(col_blocks):
            pltpu.make_async_copy(home(a_ref, a, b), share.at[spot(a, b)], load_sem).start()

    barrier = pltpu.get_barrier_semaphore()
    n_dev = n_row * n_col

    def greet(n):
        other = lax.rem(row * n_col + col + n, n_dev)
        pl.semaphore_signal(barrier, inc=1, device_id=at(other // n_col, lax.rem(other, n_col)), device_id_type=MESH)

    loop(1, n_dev, greet)
    with jax.named_scope("all_here"):
        pl.semaphore_wait(barrier, n_dev - 1)
    with jax.named_scope("loaded"):
        pltpu.make_async_copy(share, share, load_sem).wait()

    def seed_copy(b, dev_row):
        return pltpu.make_async_remote_copy(
            src_ref=share.at[spot(ratio * b + col // n_row, b)], dst_ref=diag.at[b],
            send_sem=seed_send.at[b, lax.rem(dev_row - row + n_row, n_row)],
            recv_sem=seed_recv.at[b], device_id=at(dev_row, col), device_id_type=MESH,
        )

    @pl.when(on_diag)
    def _():
        for b in range(col_blocks):
            for d in (1, n_row - 1, 2):
                seed_copy(b, lax.rem(row + d, n_row)).start()
        for b in range(col_blocks):
            diag[b] = share[spot(ratio * b + col // n_row, b)]

    def seed_arrived(b):
        @pl.when(jnp.logical_not(on_diag))
        def _():
            seed_copy(b, row).wait_recv()

    with jax.named_scope("seed"):
        seed_arrived(0)

    def clear(n):
        a, b = lax.rem(n, row_blocks), n // row_blocks

        @pl.when(a * n_row + row < b * n_col + col)
        def _():
            share[n] = jnp.zeros((size, size), F32)
            pltpu.make_async_copy(share.at[n], home(o_ref, a, b), store_sem).start()

    loop(0, row_blocks * col_blocks, clear)

    def times_t(x, y):
        return lax.dot_general(x, y, (((1,), (1,)), ((), ())), preferred_element_type=F32)

    def update_block(p, a, b):
        share[spot(a, b)] -= times_t(panel[row_slot(p, a)], panel[col_of(p, b)])

    def update_diag(p, b):
        other = panel[col_of(p, b)]
        diag[b] -= times_t(other, other)

    def column_arrived(p, b):
        @pl.when(jnp.logical_not(on_diag))
        def _():
            arrived(col_slot(p, b))
            column_pass_on(p, b, start)

    def trail(p, b_from):
        def column(b):
            column_arrived(p, b)
            update_diag(p, b)
            lo = first_a(b * n_col + col)
            lone = lax.rem(row_blocks - lo, 2)

            @pl.when(lone == 1)
            def _():
                update_block(p, lo, b)

            def pair(m):
                a = lo + lone + 2 * m
                both = pl.ds(spot(a, b), 2)
                left = panel[pl.ds(row_slot(p, a), 2)].reshape(2 * size, size)
                share[both] -= times_t(left, panel[col_of(p, b)]).reshape(2, size, size)

            loop(0, (row_blocks - lo) // 2, pair)

        loop(b_from, col_blocks, column)

    def prepare(b):
        work[size:, :] = jnp.zeros((BASE, size), F32)
        r_id = lax.broadcasted_iota(jnp.int32, (size + BASE, size), 0)
        c_id = lax.broadcasted_iota(jnp.int32, (size + BASE, size), 1)
        winv[...] = jnp.where(r_id == c_id, 1.0, 0.0).astype(F32)

    def times_winv_t(x):
        hi, mid, lo = split3(x)
        whi, wmid, wlo = winv3[0], winv3[1], winv3[2]
        small = times_t(lo, whi) + times_t(mid, wmid) + times_t(hi, wlo)
        return small + (times_t(mid, whi) + times_t(hi, wmid)) + times_t(hi, whi)

    def solve(k, a, count):
        kb = k // n_col
        here = pl.ds(spot(a, kb), count)

        @pl.when(k > 0)
        def _():
            last = k - 1
            for m in range(count):
                receive(last, a + m)
            left = panel[pl.ds(row_slot(last, a), count)].reshape(count * size, size)
            share[here] -= times_t(left, panel[col_of(last, kb)]).reshape(count, size, size)

        x = times_winv_t(share[here].reshape(count * size, size)).reshape(count, size, size)
        panel[pl.ds(row_slot(k, a), count)] = x.astype(BF16)
        share[here] = x
        for m in range(count):
            source_sends(k, a + m, start)
        for m in range(count):
            pltpu.make_async_copy(share.at[spot(a + m, kb)], home(o_ref, a + m, kb), store_sem).start()

    @pl.when(col == 0)
    def _():
        prepare(0)
        work[0:size, :] = diag[0]

    def step(k):
        mine = col == lax.rem(k, n_col)
        kb = k // n_col
        last = k - 1
        soon = jnp.logical_and(col == lax.rem(k + 1, n_col), k + 1 < steps)

        @pl.when(mine)
        def _():
            with jax.named_scope("factor"):
                factor_block(work, winv, prev)
            for n, part in enumerate(split3(winv[0:size, :])):
                winv3[n] = part
            lo = first_a(k)
            single = jnp.minimum(lo + 1 + lax.rem(row_blocks - lo + 1, 2), row_blocks)
            with jax.named_scope("solve_one"):
                loop(lo, single, lambda a: solve(k, a, 1))
            with jax.named_scope("solve_two"):
              loop(0, (row_blocks - single) // 2, lambda m: solve(k, single + 2 * m, 2))

        @pl.when(k >= depth)
        def _():
            with jax.named_scope("passed"):
                passed(k - depth)

        @pl.when(k == 1)
        def _():
            for b in range(1, col_blocks):
                seed_arrived(b)

        @pl.when(mine)
        def _():
            @pl.when(row == lax.rem(k, n_row))
            def _():
                for d in range(1, n_row):
                    seed_copy(kb, lax.rem(row + d, n_row)).wait_send()
                r_id = lax.broadcasted_iota(jnp.int32, (size, size), 0)
                c_id = lax.broadcasted_iota(jnp.int32, (size, size), 1)
                n = spot(k // n_row, kb)
                share[n] = jnp.where(r_id >= c_id, work[0:size, :].T, 0.0)
                pltpu.make_async_copy(share.at[n], home(o_ref, k // n_row, kb), store_sem).start()

            @pl.when(k > 1)
            def _():
                with jax.named_scope("late_trail"):
                    trail(k - 2, kb + 1)

            @pl.when(k > 0)
            def _():
                with jax.named_scope("late_trail2"):
                    trail(last, kb + 1)

        @pl.when(jnp.logical_and(k > 0, jnp.logical_not(jnp.logical_or(mine, soon))))
        def _():
            @pl.when(col != lax.rem(last, n_col))
            def _():
                with jax.named_scope("receive"):
                    loop(first_passed(last), row_blocks, lambda a: receive(last, a))

            with jax.named_scope("trail"):
                trail(last, first_b(last))

        @pl.when(soon)
        def _():
            nb = (k + 1) // n_col

            @pl.when(k > 0)
            def _():
                @pl.when(on_diag)
                def _():
                    receive(last, (k + 1) // n_row)

                column_arrived(last, nb)
                update_diag(last, nb)

                def catch_up(a):
                    receive(last, a)
                    update_block(last, a, nb)

                with jax.named_scope("catch_up"):
                    loop(first_a(k + 1), row_blocks, catch_up)

            prepare(nb)
            slot = col_of(k, nb)
            with jax.named_scope("first_block"):
                arrived(slot)

            @pl.when(on_diag)
            def _():
                pass_on(k, (k + 1) // n_row, start)

            other = panel[slot]
            work[0:size, :] = diag[nb] - times_t(other, other)

        @pl.when(jnp.logical_and(k >= n_col // 2, col == lax.rem(k + n_col // 2, n_col)))
        def _():
            with jax.named_scope("sends_done"):
                loop(first_a(k - n_col // 2), row_blocks, lambda a: source_sends(k - n_col // 2, a, finish))

    loop(0, steps, step)

    loop(steps - depth, steps, passed)

    def last_sends(k):
        @pl.when(col == lax.rem(k, n_col))
        def _():
            loop(first_a(k), row_blocks, lambda a: source_sends(k, a, finish))

    loop(steps - n_col // 2, steps, last_sends)
    with jax.named_scope("stored"):
        pltpu.make_async_copy(share, share, store_sem).wait()


def solution(mesh):
    n_row = mesh.shape["row"]
    n_col = mesh.shape["col"]

    def factor_local(a_loc):
        row_blocks, size, local_cols = a_loc.shape
        col_blocks = local_cols // size
        slots = n_row * (row_blocks * (row_blocks + 1) // 2) + n_col * (col_blocks * (col_blocks + 1) // 2)
        return pl.pallas_call(
            functools.partial(kernel, n_row, n_col, "batch"),
            out_shape=jax.ShapeDtypeStruct(a_loc.shape, F32),
            in_specs=[pl.BlockSpec(memory_space=pl.ANY)],
            out_specs=pl.BlockSpec(memory_space=pl.ANY),
            scratch_shapes=[
                pltpu.VMEM((row_blocks * col_blocks, size, size), F32),
                pltpu.VMEM((col_blocks, size, size), F32),
                pltpu.VMEM((slots, size, size), BF16),
                pltpu.VMEM((size + BASE, size), F32),
                pltpu.VMEM((size + BASE, size), F32),
                pltpu.VMEM((3, size, size), BF16),
                pltpu.VMEM((BASE, 3 * LANE), F32),
                pltpu.SemaphoreType.DMA,
                pltpu.SemaphoreType.DMA,
                pltpu.SemaphoreType.DMA((col_blocks, n_row)),
                pltpu.SemaphoreType.DMA((col_blocks,)),
                pltpu.SemaphoreType.DMA((row_blocks, 6)),
                pltpu.SemaphoreType.DMA((4, row_blocks, 5)),
                pltpu.SemaphoreType.DMA((4, col_blocks)),
                pltpu.SemaphoreType.DMA((slots,)),
            ],
            compiler_params=pltpu.CompilerParams(
                collective_id=0, has_side_effects=True, vmem_limit_bytes=60 * 1024 * 1024
            ),
            name="cholesky",
        )(a_loc)

    blk_spec = P(("batch", "row"), None, "col")
    return jax.shard_map(factor_local, mesh=mesh, in_specs=(blk_spec,), out_specs=blk_spec, check_vma=False)
```

```python
import functools

import jax
import jax.numpy as jnp
from jax import lax
from jax.experimental import pallas as pl
from jax.experimental.pallas import tpu as pltpu
from jax.sharding import PartitionSpec as P

F32 = jnp.float32
BF16 = jnp.bfloat16
MESH = pl.DeviceIdType.MESH
SUB = 8
LANE = 128
BASE = 16


def sub_bcast(x, q):
    return jnp.broadcast_to(x[q : q + 1, :], (SUB, LANE))


def lane_bcast(x, lane):
    return jnp.take_along_axis(x, jnp.full((SUB, LANE), lane, jnp.int32), axis=1)


def split3(x):
    high = x.astype(BF16)
    rest = x - high.astype(F32)
    mid = rest.astype(BF16)
    return high, mid, (rest - mid.astype(F32)).astype(BF16)


def swap_rows(x, bit, row_id):
    if bit == SUB // 2:
        return pltpu.roll(x, bit, 0)
    return jnp.where((row_id & bit) == 0, pltpu.roll(x, SUB - bit, 0), pltpu.roll(x, bit, 0))


def stack_sums(parts):
    row_id = lax.broadcasted_iota(jnp.int32, (SUB, LANE), 0)
    for bit in (4, 2, 1):
        low = (row_id & bit) == 0
        half = len(parts) // 2
        parts = [
            jnp.where(low, parts[n], parts[n + half]) + swap_rows(jnp.where(low, parts[n + half], parts[n]), bit, row_id)
            for n in range(half)
        ]
    return parts[0]


def eliminate(rows, lane0):
    row_id = lax.broadcasted_iota(jnp.int32, (SUB, LANE), 0)
    rows = [list(rows[0]), list(rows[1])]
    cols = [
        [lane_bcast(rows[0][0], lane0 + j) for j in range(SUB)],
        [lane_bcast(rows[1][0], lane0 + j) for j in range(BASE)],
    ]
    scale = [jnp.zeros((SUB, LANE), F32), jnp.zeros((SUB, LANE), F32)]
    pivot = sub_bcast(cols[0][0], 0)
    for j in range(BASE):
        t, q = divmod(j, SUB)
        inv = lax.rsqrt(pivot)
        scale[t] = jnp.where(row_id == q, inv, scale[t])
        if j + 1 < BASE:
            tn, qn = divmod(j + 1, SUB)
            near = sub_bcast(cols[tn][j], qn) * inv
            pivot = sub_bcast(cols[tn][j + 1], qn) - near * near
        below = cols[1][j] * inv
        here = cols[0][j] * inv if t == 0 else None
        for n in range(j + 1, BASE):
            tn, qn = divmod(n, SUB)
            other = sub_bcast(cols[tn][j], qn) * inv
            if t == 0 and tn == 0:
                cols[0][n] = cols[0][n] - here * other
            cols[1][n] = cols[1][n] - below * other
        masked = jnp.where(row_id > q, here if t == 0 else below, 0.0)
        for v in range(len(rows[0])):
            pivot_row = sub_bcast(rows[t][v], q) * inv
            rows[t][v] = rows[t][v] - masked * pivot_row
            if t == 0:
                rows[1][v] = rows[1][v] - below * pivot_row
    return [[x * scale[t] for x in rows[t]] for t in range(2)]


def factor_block(work, winv, prev):
    size = work.shape[1]
    prev[...] = jnp.zeros(prev.shape, F32)
    for half in range(size // LANE):
        views = [(work, 0), (work, 1), (winv, 0)] if half == 0 else [(work, 1), (winv, 0), (winv, 1)]
        first = half * LANE
        if half == 1:
            mid_part, inv_part = prev[:, LANE : 2 * LANE], prev[:, 2 * LANE :]
            prev[:, :LANE] = mid_part
            prev[:, LANE : 2 * LANE] = inv_part
            prev[:, 2 * LANE :] = jnp.zeros((BASE, LANE), F32)

        def body(s, carry, views=views, first=first):
            lane0 = s * BASE
            row0 = pl.multiple_of(first + lane0, BASE)

            def rows_at(row, t):
                return pl.ds(pl.multiple_of(row + SUB * t, SUB), SUB)

            rows = [[ref[rows_at(row0, t), LANE * g : LANE * (g + 1)] for ref, g in views] for t in range(2)]
            hi, mid, lo = split3(prev[...])
            lane = lax.broadcasted_iota(jnp.int32, (BASE, size - first), 1) + first
            after = lane >= row0 + BASE
            lhi, lmid, llo = [jnp.where(after, x[:, : size - first], jnp.zeros((), BF16)) for x in (hi, mid, lo)]
            update = lax.dot_general(
                jnp.concatenate([lhi, lhi, lmid, lhi, llo, lmid], axis=0),
                jnp.concatenate([hi, mid, hi, lo, hi, mid], axis=0),
                (((0,), (0,)), ((), ())),
                preferred_element_type=F32,
            )
            for v, (ref, g) in enumerate(views):
                ref[first:size, LANE * g : LANE * (g + 1)] -= update[:, LANE * v : LANE * (v + 1)]
            done = eliminate(rows, lane0)
            for t in range(2):
                for v, (ref, g) in enumerate(views):
                    ref[rows_at(row0, t), LANE * g : LANE * (g + 1)] = done[t][v]
                    prev[SUB * t : SUB * (t + 1), LANE * v : LANE * (v + 1)] = done[t][v]
            if first == 0:
                source = [jnp.where(s == LANE // BASE - 1, done[t][1], done[t][0]) for t in range(2)]
            else:
                source = [done[t][0] for t in range(2)]
            next_lane = (lane0 + BASE) % LANE
            for t in range(2):
                factor = [[lane_bcast(source[m], next_lane + SUB * t + n) for n in range(SUB)] for m in range(2)]
                for v, (ref, g) in enumerate(views):
                    parts = [factor[0][n] * done[0][v] + factor[1][n] * done[1][v] for n in range(SUB)]
                    ref[rows_at(row0 + BASE, t), LANE * g : LANE * (g + 1)] -= stack_sums(parts)
            return carry

        lax.fori_loop(0, LANE // BASE, body, 0)


def kernel(n_row, n_col, batch_axis, a_ref, o_ref, share, diag, panel, work, winv, winv3, prev, load_sem, store_sem, seed_send, seed_recv,
           send_sem, pass_sem, column_sem, recv_sem):
    row_blocks, size, local_cols = a_ref.shape
    col_blocks = local_cols // size
    ratio = n_col // n_row
    steps = row_blocks * n_row
    depth = pass_sem.shape[0]
    batch = lax.axis_index(batch_axis)
    row = lax.axis_index("row")
    col = lax.axis_index("col")
    odd = lax.rem(col, 2)
    on_diag = lax.rem(col, n_row) == row
    row_slots = n_row * (row_blocks * (row_blocks + 1) // 2)

    def at(dev_row, dev_col):
        return (batch, dev_row, dev_col)

    def row_slot(k, a):
        g = k // n_row
        return n_row * (row_blocks * g - (g * (g - 1)) // 2) + (k - g * n_row) * (row_blocks - g) + a - g

    def col_slot(k, b):
        h = k // n_col
        return row_slots + n_col * (col_blocks * h - (h * (h - 1)) // 2) + (k - h * n_col) * (col_blocks - h) + b - h

    def first_a(k):
        return (k + n_row - row) // n_row

    def first_b(k):
        return (k + n_col - col) // n_col

    def home(ref, a, b):
        return ref.at[a, :, pl.ds(pl.multiple_of(b * size, size), size)]

    def spot(a, b):
        return b * row_blocks + a

    def col_of(k, b):
        return jnp.where(on_diag, row_slot(k, ratio * b + col // n_row), col_slot(k, b))

    def copy(src_slot, dst_slot, sem, device):
        return pltpu.make_async_remote_copy(
            src_ref=panel.at[src_slot], dst_ref=panel.at[dst_slot], send_sem=sem, recv_sem=recv_sem.at[dst_slot],
            device_id=device, device_id_type=MESH,
        )

    def arrived(slot):
        copy(slot, slot, send_sem.at[0, 0], at(row, col)).wait_recv()

    def start(c):
        c.start()

    def finish(c):
        c.wait_send()

    def down_column(k, a, ways, sems, target, act):
        slot = row_slot(k, a)
        dst = col_slot(k, (a * n_row + row) // n_col)
        for m, d in enumerate(ways):
            act(copy(slot, dst, sems[m], at(lax.rem(row + d, n_row), target)))

    def source_sends(k, a, act):
        ahead = a * n_row + row - k
        slot = row_slot(k, a)

        @pl.when(ahead == 1)
        def _():
            dst = col_slot(k, (k + 1) // n_col)
            act(copy(slot, dst, send_sem.at[a, 0], at(lax.rem(row + 1, n_row), lax.rem(col + 1, n_col))))

        @pl.when(lax.rem(ahead, n_col) == 0)
        def _():
            down_column(k, a, (1, n_row - 1), [send_sem.at[a, m] for m in range(2)], col, act)

        @pl.when(jnp.logical_or(odd == 0, jnp.logical_or(ahead == 1, ahead >= n_col - 1)))
        def _():
            up = jnp.logical_or(odd == 0, ahead == 1)
            act(copy(slot, slot, send_sem.at[a, 3], at(row, lax.rem(jnp.where(up, col + 1, col - 1), n_col))))

        @pl.when(ahead >= 2)
        def _():
            act(copy(slot, slot, send_sem.at[a, 4], at(row, lax.rem(col - odd + 3, n_col))))

        @pl.when(ahead >= n_col - 2 - odd)
        def _():
            act(copy(slot, slot, send_sem.at[a, 5], at(row, lax.rem(col - odd - 1 + n_col, n_col))))

    def lead(p):
        return lax.rem(col - lax.rem(p, n_col) + n_col, n_col)

    def hops(p):
        return lax.rem(col // 2 - lax.rem(p, n_col) // 2 + n_col // 2, n_col // 2)

    def passes(p):
        return jnp.logical_and(odd == 1, hops(p) != 0)

    def first_passed(p):
        low = jnp.where(passes(p), jnp.maximum(lead(p) - 1, 2), lead(p))
        return (p + low - row + n_row - 1) // n_row

    def pass_on(p, a, act):
        i = a * n_row + row
        ahead = i - p
        slot = row_slot(p, a)
        sems = pass_sem.at[lax.rem(p, depth), a]
        src_odd = lax.rem(p, 2)
        far = n_col - 2 - src_odd

        @pl.when(passes(p))
        def _():
            h = hops(p)
            via_prev = jnp.logical_and(lax.rem(a, 2) == 1, ahead >= far)
            mine_to_pass = jnp.logical_or(
                jnp.logical_and(h == 1, jnp.logical_not(via_prev)), jnp.logical_and(h == n_col // 2 - 1, via_prev)
            )

            @pl.when(jnp.logical_and(mine_to_pass, ahead >= n_col // 2 - src_odd))
            def _():
                act(copy(slot, slot, sems.at[4], at(row, lax.rem(jnp.where(h == 1, col + 2, col - 2 + n_col), n_col))))

            act(copy(slot, slot, sems.at[3], at(row, col - 1)))

        own = lax.rem(i, n_col) == col

        @pl.when(jnp.logical_and(own, ahead == 1))
        def _():
            down_column(p, a, (n_row - 1, 2), [sems.at[m] for m in range(2)], col, act)

        @pl.when(jnp.logical_and(own, ahead > 1))
        def _():
            down_column(p, a, (1, n_row - 1), [sems.at[m] for m in range(2)], col, act)

    def column_pass_on(p, b, act):
        j = b * n_col + col
        away = lax.rem(row - lax.rem(j, n_row) + n_row, n_row)

        @pl.when(jnp.logical_and(j > p + 1, away == jnp.where(lax.rem(b, 2) == 0, 1, n_row - 1)))
        def _():
            slot = col_slot(p, b)
            act(copy(slot, slot, column_sem.at[lax.rem(p, depth), b], at(lax.rem(row + away, n_row), col)))

    def passed(p):
        @pl.when(lead(p) != 0)
        def _():
            loop(first_passed(p), row_blocks, lambda a: pass_on(p, a, finish))

        loop(first_b(p), col_blocks, lambda b: column_pass_on(p, b, finish))

    def receive(p, a):
        arrived(row_slot(p, a))
        pass_on(p, a, start)

    def loop(lo, hi, fn):
        lax.fori_loop(lo, hi, lambda n, c: (fn(n), c)[1], 0)

    for a in range(row_blocks):
        for b in range(col_blocks):
            pltpu.make_async_copy(home(a_ref, a, b), share.at[spot(a, b)], load_sem).start()

    barrier = pltpu.get_barrier_semaphore()
    n_dev = n_row * n_col

    def greet(n):
        other = lax.rem(row * n_col + col + n, n_dev)
        pl.semaphore_signal(barrier, inc=1, device_id=at(other // n_col, lax.rem(other, n_col)), device_id_type=MESH)

    loop(1, n_dev, greet)
    with jax.named_scope("all_here"):
        pl.semaphore_wait(barrier, n_dev - 1)
    with jax.named_scope("loaded"):
        pltpu.make_async_copy(share, share, load_sem).wait()

    def seed_copy(b, dev_row):
        return pltpu.make_async_remote_copy(
            src_ref=share.at[spot(ratio * b + col // n_row, b)], dst_ref=diag.at[b],
            send_sem=seed_send.at[b, lax.rem(dev_row - row + n_row, n_row)],
            recv_sem=seed_recv.at[b], device_id=at(dev_row, col), device_id_type=MESH,
        )

    def hand_out(b):
        @pl.when(on_diag)
        def _():
            for d in (1, n_row - 1, 2):
                seed_copy(b, lax.rem(row + d, n_row)).start()
            diag[b] = share[spot(ratio * b + col // n_row, b)]

    hand_out(0)

    def seed_arrived(b):
        @pl.when(jnp.logical_not(on_diag))
        def _():
            seed_copy(b, row).wait_recv()

    with jax.named_scope("seed"):
        seed_arrived(0)

    def clear(n):
        a, b = lax.rem(n, row_blocks), n // row_blocks

        @pl.when(a * n_row + row < b * n_col + col)
        def _():
            share[n] = jnp.zeros((size, size), F32)
            pltpu.make_async_copy(share.at[n], home(o_ref, a, b), store_sem).start()

    loop(0, row_blocks * col_blocks, clear)

    def times_t(x, y):
        return lax.dot_general(x, y, (((1,), (1,)), ((), ())), preferred_element_type=F32)

    def update_block(p, a, b):
        share[spot(a, b)] -= times_t(panel[row_slot(p, a)], panel[col_of(p, b)])

    def update_diag(p, b):
        other = panel[col_of(p, b)]
        diag[b] -= times_t(other, other)

    def column_arrived(p, b):
        @pl.when(jnp.logical_not(on_diag))
        def _():
            arrived(col_slot(p, b))
            column_pass_on(p, b, start)

    def update_column(p, b, lo):
        lone = lax.rem(row_blocks - lo, 2)

        @pl.when(lone == 1)
        def _():
            update_block(p, lo, b)

        def pair(m):
            a = lo + lone + 2 * m
            both = pl.ds(spot(a, b), 2)
            left = panel[pl.ds(row_slot(p, a), 2)].reshape(2 * size, size)
            share[both] -= times_t(left, panel[col_of(p, b)]).reshape(2, size, size)

        loop(0, (row_blocks - lo) // 2, pair)

    def trail(p, b_from, near):
        loop(b_from, col_blocks, lambda b: update_column(p, b, first_a(b * n_col + col - jnp.where(b == near, 0, 1))))

    def columns_arrived(p, b_from):
        loop(b_from, col_blocks, lambda b: column_arrived(p, b))

    def prepare(b):
        work[size:, :] = jnp.zeros((BASE, size), F32)
        r_id = lax.broadcasted_iota(jnp.int32, (size + BASE, size), 0)
        c_id = lax.broadcasted_iota(jnp.int32, (size + BASE, size), 1)
        winv[...] = jnp.where(r_id == c_id, 1.0, 0.0).astype(F32)

    def times_winv_t(x):
        hi, mid, lo = split3(x)
        whi, wmid, wlo = winv3[0], winv3[1], winv3[2]
        small = times_t(lo, whi) + times_t(mid, wmid) + times_t(hi, wlo)
        return small + (times_t(mid, whi) + times_t(hi, wmid)) + times_t(hi, whi)

    def solve(k, a, count):
        kb = k // n_col
        here = pl.ds(spot(a, kb), count)

        @pl.when(k > 0)
        def _():
            last = k - 1
            for m in range(count):
                receive(last, a + m)
            left = panel[pl.ds(row_slot(last, a), count)].reshape(count * size, size)
            share[here] -= times_t(left, panel[col_of(last, kb)]).reshape(count, size, size)

        x = times_winv_t(share[here].reshape(count * size, size)).reshape(count, size, size)
        panel[pl.ds(row_slot(k, a), count)] = x.astype(BF16)
        share[here] = x
        for m in range(count):
            source_sends(k, a + m, start)
        for m in range(count):
            pltpu.make_async_copy(share.at[spot(a + m, kb)], home(o_ref, a + m, kb), store_sem).start()

    @pl.when(col == 0)
    def _():
        prepare(0)
        work[0:size, :] = diag[0]

    def step(k):
        mine = col == lax.rem(k, n_col)
        kb = k // n_col
        last = k - 1
        soon = jnp.logical_and(col == lax.rem(k + 1, n_col), k + 1 < steps)

        @pl.when(mine)
        def _():
            with jax.named_scope("factor"):
                factor_block(work, winv, prev)
            for n, part in enumerate(split3(winv[0:size, :])):
                winv3[n] = part
            lo = first_a(k)
            single = jnp.minimum(lo + 1 + lax.rem(row_blocks - lo + 1, 2), row_blocks)
            with jax.named_scope("solve_one"):
                loop(lo, single, lambda a: solve(k, a, 1))
            with jax.named_scope("solve_two"):
              loop(0, (row_blocks - single) // 2, lambda m: solve(k, single + 2 * m, 2))

        @pl.when(k >= depth)
        def _():
            with jax.named_scope("passed"):
                passed(k - depth)

        @pl.when(mine)
        def _():
            @pl.when(row == lax.rem(k, n_row))
            def _():
                for d in range(1, n_row):
                    seed_copy(kb, lax.rem(row + d, n_row)).wait_send()
                r_id = lax.broadcasted_iota(jnp.int32, (size, size), 0)
                c_id = lax.broadcasted_iota(jnp.int32, (size, size), 1)
                n = spot(k // n_row, kb)
                share[n] = jnp.where(r_id >= c_id, work[0:size, :].T, 0.0)
                pltpu.make_async_copy(share.at[n], home(o_ref, k // n_row, kb), store_sem).start()

            with jax.named_scope("late_trail"):

                def late(p):
                    columns_arrived(p, kb + 1)
                    trail(p, kb + 1, -1)

                loop(jnp.maximum(k - 3, 0), last, late)

            @pl.when(kb + 1 < col_blocks)
            def _():
                hand_out(kb + 1)

        @pl.when(jnp.logical_and(k > 0, jnp.logical_not(jnp.logical_or(mine, soon))))
        def _():
            @pl.when(col != lax.rem(last, n_col))
            def _():
                with jax.named_scope("receive"):
                    loop(first_passed(last), row_blocks, lambda a: receive(last, a))

            @pl.when(k > 1)
            def _():
                p = k - 2
                near = first_b(k)
                with jax.named_scope("columns"):
                    columns_arrived(p, near)

                @pl.when(near < col_blocks)
                def _():
                    age = k + n_col - (near * n_col + col)

                    @pl.when(jnp.logical_and(age == 3, near > 0))
                    def _():
                        with jax.named_scope("seed_late"):
                            seed_arrived(near)

                    @pl.when(age >= 3)
                    def _():
                        oldest = jnp.where(age == 3, jnp.maximum(k - 4, 0), p)
                        loop(oldest, last, lambda q: update_diag(q, near))

                with jax.named_scope("trail"):
                    trail(p, near, near)

        @pl.when(soon)
        def _():
            nb = (k + 1) // n_col

            @pl.when(k > 1)
            def _():
                with jax.named_scope("catch_up_old"):
                    column_arrived(k - 2, nb)
                    update_diag(k - 2, nb)
                    update_column(k - 2, nb, first_a(k + 1))

            @pl.when(k > 0)
            def _():
                @pl.when(on_diag)
                def _():
                    receive(last, (k + 1) // n_row)

                column_arrived(last, nb)
                update_diag(last, nb)

                def catch_up(a):
                    receive(last, a)
                    update_block(last, a, nb)

                with jax.named_scope("catch_up"):
                    loop(first_a(k + 1), row_blocks, catch_up)

            prepare(nb)
            slot = col_of(k, nb)
            with jax.named_scope("first_block"):
                arrived(slot)

            @pl.when(on_diag)
            def _():
                pass_on(k, (k + 1) // n_row, start)

            other = panel[slot]
            work[0:size, :] = diag[nb] - times_t(other, other)

        @pl.when(jnp.logical_and(k >= n_col // 2, col == lax.rem(k + n_col // 2, n_col)))
        def _():
            with jax.named_scope("sends_done"):
                loop(first_a(k - n_col // 2), row_blocks, lambda a: source_sends(k - n_col // 2, a, finish))

    loop(0, steps, step)

    loop(steps - depth, steps, passed)

    def last_sends(k):
        @pl.when(col == lax.rem(k, n_col))
        def _():
            loop(first_a(k), row_blocks, lambda a: source_sends(k, a, finish))

    loop(steps - n_col // 2, steps, last_sends)
    with jax.named_scope("stored"):
        pltpu.make_async_copy(share, share, store_sem).wait()


def solution(mesh):
    n_row = mesh.shape["row"]
    n_col = mesh.shape["col"]

    def factor_local(a_loc):
        row_blocks, size, local_cols = a_loc.shape
        col_blocks = local_cols // size
        slots = n_row * (row_blocks * (row_blocks + 1) // 2) + n_col * (col_blocks * (col_blocks + 1) // 2)
        return pl.pallas_call(
            functools.partial(kernel, n_row, n_col, "batch"),
            out_shape=jax.ShapeDtypeStruct(a_loc.shape, F32),
            in_specs=[pl.BlockSpec(memory_space=pl.ANY)],
            out_specs=pl.BlockSpec(memory_space=pl.ANY),
            scratch_shapes=[
                pltpu.VMEM((row_blocks * col_blocks, size, size), F32),
                pltpu.VMEM((col_blocks, size, size), F32),
                pltpu.VMEM((slots, size, size), BF16),
                pltpu.VMEM((size + BASE, size), F32),
                pltpu.VMEM((size + BASE, size), F32),
                pltpu.VMEM((3, size, size), BF16),
                pltpu.VMEM((BASE, 3 * LANE), F32),
                pltpu.SemaphoreType.DMA,
                pltpu.SemaphoreType.DMA,
                pltpu.SemaphoreType.DMA((col_blocks, n_row)),
                pltpu.SemaphoreType.DMA((col_blocks,)),
                pltpu.SemaphoreType.DMA((row_blocks, 6)),
                pltpu.SemaphoreType.DMA((4, row_blocks, 5)),
                pltpu.SemaphoreType.DMA((4, col_blocks)),
                pltpu.SemaphoreType.DMA((slots,)),
            ],
            compiler_params=pltpu.CompilerParams(
                collective_id=0, has_side_effects=True, vmem_limit_bytes=60 * 1024 * 1024
            ),
            name="cholesky",
        )(a_loc)

    blk_spec = P(("batch", "row"), None, "col")
    return jax.shard_map(factor_local, mesh=mesh, in_specs=(blk_spec,), out_specs=blk_spec, check_vma=False)
```

```python
import functools

import jax
import jax.numpy as jnp
from jax import lax
from jax.experimental import pallas as pl
from jax.experimental.pallas import tpu as pltpu
from jax.sharding import PartitionSpec as P

F32 = jnp.float32
BF16 = jnp.bfloat16
MESH = pl.DeviceIdType.MESH
SUB = 8
LANE = 128
BASE = 16
LAG = 3


def sub_bcast(x, q):
    return jnp.broadcast_to(x[q : q + 1, :], (SUB, LANE))


def lane_bcast(x, lane):
    return jnp.take_along_axis(x, jnp.full((SUB, LANE), lane, jnp.int32), axis=1)


def split3(x):
    high = x.astype(BF16)
    rest = x - high.astype(F32)
    mid = rest.astype(BF16)
    return high, mid, (rest - mid.astype(F32)).astype(BF16)


def swap_rows(x, bit, row_id):
    if bit == SUB // 2:
        return pltpu.roll(x, bit, 0)
    return jnp.where((row_id & bit) == 0, pltpu.roll(x, SUB - bit, 0), pltpu.roll(x, bit, 0))


def stack_sums(parts):
    row_id = lax.broadcasted_iota(jnp.int32, (SUB, LANE), 0)
    for bit in (4, 2, 1):
        low = (row_id & bit) == 0
        half = len(parts) // 2
        parts = [
            jnp.where(low, parts[n], parts[n + half]) + swap_rows(jnp.where(low, parts[n + half], parts[n]), bit, row_id)
            for n in range(half)
        ]
    return parts[0]


def eliminate(rows, lane0):
    row_id = lax.broadcasted_iota(jnp.int32, (SUB, LANE), 0)
    rows = [list(rows[0]), list(rows[1])]
    cols = [
        [lane_bcast(rows[0][0], lane0 + j) for j in range(SUB)],
        [lane_bcast(rows[1][0], lane0 + j) for j in range(BASE)],
    ]
    scale = [jnp.zeros((SUB, LANE), F32), jnp.zeros((SUB, LANE), F32)]
    pivot = sub_bcast(cols[0][0], 0)
    for j in range(BASE):
        t, q = divmod(j, SUB)
        inv = lax.rsqrt(pivot)
        scale[t] = jnp.where(row_id == q, inv, scale[t])
        if j + 1 < BASE:
            tn, qn = divmod(j + 1, SUB)
            near = sub_bcast(cols[tn][j], qn) * inv
            pivot = sub_bcast(cols[tn][j + 1], qn) - near * near
        below = cols[1][j] * inv
        here = cols[0][j] * inv if t == 0 else None
        for n in range(j + 1, BASE):
            tn, qn = divmod(n, SUB)
            other = sub_bcast(cols[tn][j], qn) * inv
            if t == 0 and tn == 0:
                cols[0][n] = cols[0][n] - here * other
            cols[1][n] = cols[1][n] - below * other
        masked = jnp.where(row_id > q, here if t == 0 else below, 0.0)
        for v in range(len(rows[0])):
            pivot_row = sub_bcast(rows[t][v], q) * inv
            rows[t][v] = rows[t][v] - masked * pivot_row
            if t == 0:
                rows[1][v] = rows[1][v] - below * pivot_row
    return [[x * scale[t] for x in rows[t]] for t in range(2)]


def factor_block(work, winv, prev):
    size = work.shape[1]
    prev[...] = jnp.zeros(prev.shape, F32)
    for half in range(size // LANE):
        views = [(work, 0), (work, 1), (winv, 0)] if half == 0 else [(work, 1), (winv, 0), (winv, 1)]
        first = half * LANE
        if half == 1:
            mid_part, inv_part = prev[:, LANE : 2 * LANE], prev[:, 2 * LANE :]
            prev[:, :LANE] = mid_part
            prev[:, LANE : 2 * LANE] = inv_part
            prev[:, 2 * LANE :] = jnp.zeros((BASE, LANE), F32)

        def body(s, carry, views=views, first=first):
            lane0 = s * BASE
            row0 = pl.multiple_of(first + lane0, BASE)

            def rows_at(row, t):
                return pl.ds(pl.multiple_of(row + SUB * t, SUB), SUB)

            rows = [[ref[rows_at(row0, t), LANE * g : LANE * (g + 1)] for ref, g in views] for t in range(2)]
            hi, mid, lo = split3(prev[...])
            lane = lax.broadcasted_iota(jnp.int32, (BASE, size - first), 1) + first
            after = lane >= row0 + BASE
            lhi, lmid, llo = [jnp.where(after, x[:, : size - first], jnp.zeros((), BF16)) for x in (hi, mid, lo)]
            update = lax.dot_general(
                jnp.concatenate([lhi, lhi, lmid, lhi, llo, lmid], axis=0),
                jnp.concatenate([hi, mid, hi, lo, hi, mid], axis=0),
                (((0,), (0,)), ((), ())),
                preferred_element_type=F32,
            )
            for v, (ref, g) in enumerate(views):
                ref[first:size, LANE * g : LANE * (g + 1)] -= update[:, LANE * v : LANE * (v + 1)]
            done = eliminate(rows, lane0)
            for t in range(2):
                for v, (ref, g) in enumerate(views):
                    ref[rows_at(row0, t), LANE * g : LANE * (g + 1)] = done[t][v]
                    prev[SUB * t : SUB * (t + 1), LANE * v : LANE * (v + 1)] = done[t][v]
            if first == 0:
                source = [jnp.where(s == LANE // BASE - 1, done[t][1], done[t][0]) for t in range(2)]
            else:
                source = [done[t][0] for t in range(2)]
            next_lane = (lane0 + BASE) % LANE
            for t in range(2):
                factor = [[lane_bcast(source[m], next_lane + SUB * t + n) for n in range(SUB)] for m in range(2)]
                for v, (ref, g) in enumerate(views):
                    parts = [factor[0][n] * done[0][v] + factor[1][n] * done[1][v] for n in range(SUB)]
                    ref[rows_at(row0 + BASE, t), LANE * g : LANE * (g + 1)] -= stack_sums(parts)
            return carry

        lax.fori_loop(0, LANE // BASE, body, 0)


def kernel(n_row, n_col, batch_axis, a_ref, o_ref, share, diag, panel, work, winv, winv3, prev, load_sem, store_sem, seed_send, seed_recv,
           send_sem, pass_sem, recv_sem):
    row_blocks, size, local_cols = a_ref.shape
    col_blocks = local_cols // size
    ratio = n_col // n_row
    steps = row_blocks * n_row
    depth = pass_sem.shape[0]
    batch = lax.axis_index(batch_axis)
    row = lax.axis_index("row")
    col = lax.axis_index("col")
    odd = lax.rem(col, 2)
    on_diag = lax.rem(col, n_row) == row
    row_slots = n_row * (row_blocks * (row_blocks + 1) // 2)

    def at(dev_row, dev_col):
        return (batch, dev_row, dev_col)

    def row_slot(k, a):
        g = k // n_row
        return n_row * (row_blocks * g - (g * (g - 1)) // 2) + (k - g * n_row) * (row_blocks - g) + a - g

    def col_slot(k, b):
        h = k // n_col
        return row_slots + n_col * (col_blocks * h - (h * (h - 1)) // 2) + (k - h * n_col) * (col_blocks - h) + b - h

    def first_a(k):
        return (k + n_row - row) // n_row

    def first_b(k):
        return (k + n_col - col) // n_col

    def home(ref, a, b):
        return ref.at[a, :, pl.ds(pl.multiple_of(b * size, size), size)]

    def spot(a, b):
        return b * row_blocks + a

    def col_of(k, b):
        return jnp.where(on_diag, row_slot(k, ratio * b + col // n_row), col_slot(k, b))

    def copy(src_slot, dst_slot, sem, device):
        return pltpu.make_async_remote_copy(
            src_ref=panel.at[src_slot], dst_ref=panel.at[dst_slot], send_sem=sem, recv_sem=recv_sem.at[dst_slot],
            device_id=device, device_id_type=MESH,
        )

    def arrived(slot):
        copy(slot, slot, send_sem.at[0, 0], at(row, col)).wait_recv()

    def start(c):
        c.start()

    def finish(c):
        c.wait_send()

    def down_column(k, a, ways, sems, target, act):
        slot = row_slot(k, a)
        dst = col_slot(k, (a * n_row + row) // n_col)
        for m, d in enumerate(ways):
            act(copy(slot, dst, sems[m], at(lax.rem(row + d, n_row), target)))

    def source_sends(k, a, act):
        ahead = a * n_row + row - k
        slot = row_slot(k, a)

        @pl.when(ahead == 1)
        def _():
            dst = col_slot(k, (k + 1) // n_col)
            act(copy(slot, dst, send_sem.at[a, 0], at(lax.rem(row + 1, n_row), lax.rem(col + 1, n_col))))

        @pl.when(lax.rem(ahead, n_col) == 0)
        def _():
            down_column(k, a, (1, n_row - 1, 2), [send_sem.at[a, m] for m in range(3)], col, act)

        @pl.when(jnp.logical_or(odd == 0, jnp.logical_or(ahead == 1, ahead >= n_col - 1)))
        def _():
            up = jnp.logical_or(odd == 0, ahead == 1)
            act(copy(slot, slot, send_sem.at[a, 3], at(row, lax.rem(jnp.where(up, col + 1, col - 1), n_col))))

        @pl.when(ahead >= 2)
        def _():
            act(copy(slot, slot, send_sem.at[a, 4], at(row, lax.rem(col - odd + 3, n_col))))

        @pl.when(ahead >= n_col - 2 - odd)
        def _():
            act(copy(slot, slot, send_sem.at[a, 5], at(row, lax.rem(col - odd - 1 + n_col, n_col))))

    def lead(p):
        return lax.rem(col - lax.rem(p, n_col) + n_col, n_col)

    def hops(p):
        return lax.rem(col // 2 - lax.rem(p, n_col) // 2 + n_col // 2, n_col // 2)

    def passes(p):
        return jnp.logical_and(odd == 1, hops(p) != 0)

    def first_passed(p):
        low = jnp.where(passes(p), jnp.maximum(lead(p) - 1, 2), lead(p))
        return (p + low - row + n_row - 1) // n_row

    def pass_on(p, a, act):
        i = a * n_row + row
        ahead = i - p
        slot = row_slot(p, a)
        sems = pass_sem.at[lax.rem(p, depth), a]
        src_odd = lax.rem(p, 2)
        far = n_col - 2 - src_odd

        @pl.when(passes(p))
        def _():
            h = hops(p)
            via_prev = jnp.logical_and(lax.rem(a, 2) == 1, ahead >= far)
            mine_to_pass = jnp.logical_or(
                jnp.logical_and(h == 1, jnp.logical_not(via_prev)), jnp.logical_and(h == n_col // 2 - 1, via_prev)
            )

            @pl.when(jnp.logical_and(mine_to_pass, ahead >= n_col // 2 - src_odd))
            def _():
                act(copy(slot, slot, sems.at[4], at(row, lax.rem(jnp.where(h == 1, col + 2, col - 2 + n_col), n_col))))

            act(copy(slot, slot, sems.at[3], at(row, col - 1)))

        own = lax.rem(i, n_col) == col

        @pl.when(jnp.logical_and(own, ahead == 1))
        def _():
            down_column(p, a, (n_row - 1, 2), [sems.at[m] for m in range(2)], col, act)

        @pl.when(jnp.logical_and(own, ahead > 1))
        def _():
            down_column(p, a, (1, n_row - 1, 2), [sems.at[m] for m in range(3)], col, act)

    def passed(p):
        @pl.when(lead(p) != 0)
        def _():
            loop(first_passed(p), row_blocks, lambda a: pass_on(p, a, finish))

    def receive(p, a):
        arrived(row_slot(p, a))
        pass_on(p, a, start)

    def loop(lo, hi, fn):
        lax.fori_loop(lo, hi, lambda n, c: (fn(n), c)[1], 0)

    for a in range(row_blocks):
        for b in range(col_blocks):
            pltpu.make_async_copy(home(a_ref, a, b), share.at[spot(a, b)], load_sem).start()

    barrier = pltpu.get_barrier_semaphore()
    n_dev = n_row * n_col

    def greet(n):
        other = lax.rem(row * n_col + col + n, n_dev)
        pl.semaphore_signal(barrier, inc=1, device_id=at(other // n_col, lax.rem(other, n_col)), device_id_type=MESH)

    loop(1, n_dev, greet)
    with jax.named_scope("all_here"):
        pl.semaphore_wait(barrier, n_dev - 1)
    with jax.named_scope("loaded"):
        pltpu.make_async_copy(share, share, load_sem).wait()

    def seed_copy(b, dev_row):
        return pltpu.make_async_remote_copy(
            src_ref=share.at[spot(ratio * b + col // n_row, b)], dst_ref=diag.at[b],
            send_sem=seed_send.at[b, lax.rem(dev_row - row + n_row, n_row)],
            recv_sem=seed_recv.at[b], device_id=at(dev_row, col), device_id_type=MESH,
        )

    def hand_out(b):
        @pl.when(on_diag)
        def _():
            for d in (1, n_row - 1, 2):
                seed_copy(b, lax.rem(row + d, n_row)).start()
            diag[b] = share[spot(ratio * b + col // n_row, b)]

    hand_out(0)

    def seed_arrived(b):
        @pl.when(jnp.logical_not(on_diag))
        def _():
            seed_copy(b, row).wait_recv()

    with jax.named_scope("seed"):
        seed_arrived(0)

    def clear(n):
        a, b = lax.rem(n, row_blocks), n // row_blocks

        @pl.when(a * n_row + row < b * n_col + col)
        def _():
            share[n] = jnp.zeros((size, size), F32)
            pltpu.make_async_copy(share.at[n], home(o_ref, a, b), store_sem).start()

    loop(0, row_blocks * col_blocks, clear)

    def times_t(x, y):
        return lax.dot_general(x, y, (((1,), (1,)), ((), ())), preferred_element_type=F32)

    def update_block(p, a, b):
        share[spot(a, b)] -= times_t(panel[row_slot(p, a)], panel[col_of(p, b)])

    def update_diag(p, b):
        other = panel[col_of(p, b)]
        diag[b] -= times_t(other, other)

    def column_arrived(p, b):
        @pl.when(jnp.logical_not(on_diag))
        def _():
            arrived(col_slot(p, b))

    def update_column(p, b, lo):
        lone = lax.rem(row_blocks - lo, 2)

        @pl.when(lone == 1)
        def _():
            update_block(p, lo, b)

        def pair(m):
            a = lo + lone + 2 * m
            both = pl.ds(spot(a, b), 2)
            left = panel[pl.ds(row_slot(p, a), 2)].reshape(2 * size, size)
            share[both] -= times_t(left, panel[col_of(p, b)]).reshape(2, size, size)

        loop(0, (row_blocks - lo) // 2, pair)

    def trail(p, b_from, near):
        loop(b_from, col_blocks, lambda b: update_column(p, b, first_a(b * n_col + col - jnp.where(b == near, 0, 1))))

    def columns_arrived(p, b_from):
        loop(b_from, col_blocks, lambda b: column_arrived(p, b))

    def prepare(b):
        work[size:, :] = jnp.zeros((BASE, size), F32)
        r_id = lax.broadcasted_iota(jnp.int32, (size + BASE, size), 0)
        c_id = lax.broadcasted_iota(jnp.int32, (size + BASE, size), 1)
        winv[...] = jnp.where(r_id == c_id, 1.0, 0.0).astype(F32)

    def times_winv_t(x):
        hi, mid, lo = split3(x)
        whi, wmid, wlo = winv3[0], winv3[1], winv3[2]
        small = times_t(lo, whi) + times_t(mid, wmid) + times_t(hi, wlo)
        return small + (times_t(mid, whi) + times_t(hi, wmid)) + times_t(hi, whi)

    def solve(k, a, count):
        kb = k // n_col
        here = pl.ds(spot(a, kb), count)

        @pl.when(k > 0)
        def _():
            last = k - 1
            for m in range(count):
                receive(last, a + m)
            left = panel[pl.ds(row_slot(last, a), count)].reshape(count * size, size)
            share[here] -= times_t(left, panel[col_of(last, kb)]).reshape(count, size, size)

        x = times_winv_t(share[here].reshape(count * size, size)).reshape(count, size, size)
        panel[pl.ds(row_slot(k, a), count)] = x.astype(BF16)
        share[here] = x
        for m in range(count):
            source_sends(k, a + m, start)
        for m in range(count):
            pltpu.make_async_copy(share.at[spot(a + m, kb)], home(o_ref, a + m, kb), store_sem).start()

    @pl.when(col == 0)
    def _():
        prepare(0)
        work[0:size, :] = diag[0]

    def step(k):
        mine = col == lax.rem(k, n_col)
        kb = k // n_col
        last = k - 1
        soon = jnp.logical_and(col == lax.rem(k + 1, n_col), k + 1 < steps)

        @pl.when(mine)
        def _():
            with jax.named_scope("factor"):
                factor_block(work, winv, prev)
            for n, part in enumerate(split3(winv[0:size, :])):
                winv3[n] = part
            lo = first_a(k)
            single = jnp.minimum(lo + 1 + lax.rem(row_blocks - lo + 1, 2), row_blocks)
            with jax.named_scope("solve_one"):
                loop(lo, single, lambda a: solve(k, a, 1))
            with jax.named_scope("solve_two"):
              loop(0, (row_blocks - single) // 2, lambda m: solve(k, single + 2 * m, 2))

        @pl.when(k >= depth)
        def _():
            with jax.named_scope("passed"):
                passed(k - depth)

        @pl.when(mine)
        def _():
            @pl.when(row == lax.rem(k, n_row))
            def _():
                for d in range(1, n_row):
                    seed_copy(kb, lax.rem(row + d, n_row)).wait_send()
                r_id = lax.broadcasted_iota(jnp.int32, (size, size), 0)
                c_id = lax.broadcasted_iota(jnp.int32, (size, size), 1)
                n = spot(k // n_row, kb)
                share[n] = jnp.where(r_id >= c_id, work[0:size, :].T, 0.0)
                pltpu.make_async_copy(share.at[n], home(o_ref, k // n_row, kb), store_sem).start()

            with jax.named_scope("late_trail"):

                def late(p):
                    columns_arrived(p, kb + 1)
                    trail(p, kb + 1, -1)

                loop(jnp.maximum(k - 1 - LAG, 0), k - LAG + 1, late)

            @pl.when(kb + 1 < col_blocks)
            def _():
                hand_out(kb + 1)

        @pl.when(jnp.logical_and(k > 0, jnp.logical_not(jnp.logical_or(mine, soon))))
        def _():
            @pl.when(col != lax.rem(last, n_col))
            def _():
                with jax.named_scope("receive"):
                    loop(first_passed(last), row_blocks, lambda a: receive(last, a))

            @pl.when(k >= LAG)
            def _():
                p = k - LAG
                near = first_b(k)
                with jax.named_scope("columns"):
                    columns_arrived(p, near)

                @pl.when(near < col_blocks)
                def _():
                    age = k + n_col - (near * n_col + col)

                    @pl.when(jnp.logical_and(age == 3, near > 0))
                    def _():
                        with jax.named_scope("seed_late"):
                            seed_arrived(near)

                    @pl.when(age >= 3)
                    def _():
                        oldest = jnp.where(age == 3, jnp.maximum(p - 2, 0), p)
                        loop(oldest, p + 1, lambda q: update_diag(q, near))

                with jax.named_scope("trail"):
                    trail(p, near, near)

        @pl.when(soon)
        def _():
            nb = (k + 1) // n_col

            oldest = jnp.maximum(k - LAG, 0)

            def old_diag(p):
                column_arrived(p, nb)
                update_diag(p, nb)

            def take(a):
                receive(last, a)

                @pl.when(a * n_row + row > k + 1)
                def _():
                    loop(oldest, last, lambda p: update_block(p, a, nb))

            @pl.when(k > 0)
            def _():
                with jax.named_scope("old_diag"):
                    loop(oldest, last, old_diag)
                with jax.named_scope("take"):
                    loop(first_a(k), row_blocks, take)
                with jax.named_scope("take_column"):
                    column_arrived(last, nb)
                with jax.named_scope("catch_up"):
                    update_diag(last, nb)
                    update_column(last, nb, first_a(k + 1))

            prepare(nb)
            slot = col_of(k, nb)
            with jax.named_scope("first_block"):
                arrived(slot)

            @pl.when(on_diag)
            def _():
                pass_on(k, (k + 1) // n_row, start)

            other = panel[slot]
            work[0:size, :] = diag[nb] - times_t(other, other)

        @pl.when(jnp.logical_and(k >= n_col // 2, col == lax.rem(k + n_col // 2, n_col)))
        def _():
            with jax.named_scope("sends_done"):
                loop(first_a(k - n_col // 2), row_blocks, lambda a: source_sends(k - n_col // 2, a, finish))

    loop(0, steps, step)

    loop(steps - depth, steps, passed)

    def last_sends(k):
        @pl.when(col == lax.rem(k, n_col))
        def _():
            loop(first_a(k), row_blocks, lambda a: source_sends(k, a, finish))

    loop(steps - n_col // 2, steps, last_sends)
    with jax.named_scope("stored"):
        pltpu.make_async_copy(share, share, store_sem).wait()


def solution(mesh):
    n_row = mesh.shape["row"]
    n_col = mesh.shape["col"]

    def factor_local(a_loc):
        row_blocks, size, local_cols = a_loc.shape
        col_blocks = local_cols // size
        slots = n_row * (row_blocks * (row_blocks + 1) // 2) + n_col * (col_blocks * (col_blocks + 1) // 2)
        return pl.pallas_call(
            functools.partial(kernel, n_row, n_col, "batch"),
            out_shape=jax.ShapeDtypeStruct(a_loc.shape, F32),
            in_specs=[pl.BlockSpec(memory_space=pl.ANY)],
            out_specs=pl.BlockSpec(memory_space=pl.ANY),
            scratch_shapes=[
                pltpu.VMEM((row_blocks * col_blocks, size, size), F32),
                pltpu.VMEM((col_blocks, size, size), F32),
                pltpu.VMEM((slots, size, size), BF16),
                pltpu.VMEM((size + BASE, size), F32),
                pltpu.VMEM((size + BASE, size), F32),
                pltpu.VMEM((3, size, size), BF16),
                pltpu.VMEM((BASE, 3 * LANE), F32),
                pltpu.SemaphoreType.DMA,
                pltpu.SemaphoreType.DMA,
                pltpu.SemaphoreType.DMA((col_blocks, n_row)),
                pltpu.SemaphoreType.DMA((col_blocks,)),
                pltpu.SemaphoreType.DMA((row_blocks, 6)),
                pltpu.SemaphoreType.DMA((4, row_blocks, 5)),
                pltpu.SemaphoreType.DMA((slots,)),
            ],
            compiler_params=pltpu.CompilerParams(
                collective_id=0, has_side_effects=True, vmem_limit_bytes=60 * 1024 * 1024
            ),
            name="cholesky",
        )(a_loc)

    blk_spec = P(("batch", "row"), None, "col")
    return jax.shard_map(factor_local, mesh=mesh, in_specs=(blk_spec,), out_specs=blk_spec, check_vma=False)
```

```python
import functools

import jax
import jax.numpy as jnp
from jax import lax
from jax.experimental import pallas as pl
from jax.experimental.pallas import tpu as pltpu
from jax.sharding import PartitionSpec as P

F32 = jnp.float32
BF16 = jnp.bfloat16
MESH = pl.DeviceIdType.MESH
SUB = 8
LANE = 128
BASE = 16
LAG = 3


def sub_bcast(x, q):
    return jnp.broadcast_to(x[q : q + 1, :], (SUB, LANE))


def lane_bcast(x, lane):
    return jnp.take_along_axis(x, jnp.full((SUB, LANE), lane, jnp.int32), axis=1)


def split3(x):
    high = x.astype(BF16)
    rest = x - high.astype(F32)
    mid = rest.astype(BF16)
    return high, mid, (rest - mid.astype(F32)).astype(BF16)


def swap_rows(x, bit, row_id):
    if bit == SUB // 2:
        return pltpu.roll(x, bit, 0)
    return jnp.where((row_id & bit) == 0, pltpu.roll(x, SUB - bit, 0), pltpu.roll(x, bit, 0))


def stack_sums(parts):
    row_id = lax.broadcasted_iota(jnp.int32, (SUB, LANE), 0)
    for bit in (4, 2, 1):
        low = (row_id & bit) == 0
        half = len(parts) // 2
        parts = [
            jnp.where(low, parts[n], parts[n + half]) + swap_rows(jnp.where(low, parts[n + half], parts[n]), bit, row_id)
            for n in range(half)
        ]
    return parts[0]


def eliminate(rows, lane0):
    row_id = lax.broadcasted_iota(jnp.int32, (SUB, LANE), 0)
    rows = [list(rows[0]), list(rows[1])]
    cols = [
        [lane_bcast(rows[0][0], lane0 + j) for j in range(SUB)],
        [lane_bcast(rows[1][0], lane0 + j) for j in range(BASE)],
    ]
    scale = [jnp.zeros((SUB, LANE), F32), jnp.zeros((SUB, LANE), F32)]
    pivot = sub_bcast(cols[0][0], 0)
    for j in range(BASE):
        t, q = divmod(j, SUB)
        inv = lax.rsqrt(pivot)
        scale[t] = jnp.where(row_id == q, inv, scale[t])
        if j + 1 < BASE:
            tn, qn = divmod(j + 1, SUB)
            near = sub_bcast(cols[tn][j], qn) * inv
            pivot = sub_bcast(cols[tn][j + 1], qn) - near * near
        below = cols[1][j] * inv
        here = cols[0][j] * inv if t == 0 else None
        for n in range(j + 1, BASE):
            tn, qn = divmod(n, SUB)
            other = sub_bcast(cols[tn][j], qn) * inv
            if t == 0 and tn == 0:
                cols[0][n] = cols[0][n] - here * other
            cols[1][n] = cols[1][n] - below * other
        masked = jnp.where(row_id > q, here if t == 0 else below, 0.0)
        for v in range(len(rows[0])):
            pivot_row = sub_bcast(rows[t][v], q) * inv
            rows[t][v] = rows[t][v] - masked * pivot_row
            if t == 0:
                rows[1][v] = rows[1][v] - below * pivot_row
    return [[x * scale[t] for x in rows[t]] for t in range(2)]


def factor_block(work, winv, prev):
    size = work.shape[1]
    prev[...] = jnp.zeros(prev.shape, F32)
    for half in range(size // LANE):
        views = [(work, 0), (work, 1), (winv, 0)] if half == 0 else [(work, 1), (winv, 0), (winv, 1)]
        first = half * LANE
        if half == 1:
            mid_part, inv_part = prev[:, LANE : 2 * LANE], prev[:, 2 * LANE :]
            prev[:, :LANE] = mid_part
            prev[:, LANE : 2 * LANE] = inv_part
            prev[:, 2 * LANE :] = jnp.zeros((BASE, LANE), F32)

        def body(s, carry, views=views, first=first):
            lane0 = s * BASE
            row0 = pl.multiple_of(first + lane0, BASE)

            def rows_at(row, t):
                return pl.ds(pl.multiple_of(row + SUB * t, SUB), SUB)

            rows = [[ref[rows_at(row0, t), LANE * g : LANE * (g + 1)] for ref, g in views] for t in range(2)]
            hi, mid, lo = split3(prev[...])
            lane = lax.broadcasted_iota(jnp.int32, (BASE, size - first), 1) + first
            after = lane >= row0 + BASE
            lhi, lmid, llo = [jnp.where(after, x[:, : size - first], jnp.zeros((), BF16)) for x in (hi, mid, lo)]
            update = lax.dot_general(
                jnp.concatenate([lhi, lhi, lmid, lhi, llo, lmid], axis=0),
                jnp.concatenate([hi, mid, hi, lo, hi, mid], axis=0),
                (((0,), (0,)), ((), ())),
                preferred_element_type=F32,
            )
            for v, (ref, g) in enumerate(views):
                ref[first:size, LANE * g : LANE * (g + 1)] -= update[:, LANE * v : LANE * (v + 1)]
            done = eliminate(rows, lane0)
            for t in range(2):
                for v, (ref, g) in enumerate(views):
                    ref[rows_at(row0, t), LANE * g : LANE * (g + 1)] = done[t][v]
                    prev[SUB * t : SUB * (t + 1), LANE * v : LANE * (v + 1)] = done[t][v]
            if first == 0:
                source = [jnp.where(s == LANE // BASE - 1, done[t][1], done[t][0]) for t in range(2)]
            else:
                source = [done[t][0] for t in range(2)]
            next_lane = (lane0 + BASE) % LANE
            for t in range(2):
                factor = [[lane_bcast(source[m], next_lane + SUB * t + n) for n in range(SUB)] for m in range(2)]
                for v, (ref, g) in enumerate(views):
                    parts = [factor[0][n] * done[0][v] + factor[1][n] * done[1][v] for n in range(SUB)]
                    ref[rows_at(row0 + BASE, t), LANE * g : LANE * (g + 1)] -= stack_sums(parts)
            return carry

        lax.fori_loop(0, LANE // BASE, body, 0)


def kernel(n_row, n_col, batch_axis, a_ref, o_ref, share, diag, panel, work, winv, winv3, prev, load_sem, store_sem, seed_send, seed_recv,
           send_sem, pass_sem, recv_sem):
    row_blocks, size, local_cols = a_ref.shape
    col_blocks = local_cols // size
    ratio = n_col // n_row
    steps = row_blocks * n_row
    depth = pass_sem.shape[0]
    batch = lax.axis_index(batch_axis)
    row = lax.axis_index("row")
    col = lax.axis_index("col")
    odd = lax.rem(col, 2)
    on_diag = lax.rem(col, n_row) == row
    row_slots = n_row * (row_blocks * (row_blocks + 1) // 2)

    def at(dev_row, dev_col):
        return (batch, dev_row, dev_col)

    def row_slot(k, a):
        g = k // n_row
        return n_row * (row_blocks * g - (g * (g - 1)) // 2) + (k - g * n_row) * (row_blocks - g) + a - g

    def col_slot(k, b):
        h = k // n_col
        return row_slots + n_col * (col_blocks * h - (h * (h - 1)) // 2) + (k - h * n_col) * (col_blocks - h) + b - h

    def first_a(k):
        return (k + n_row - row) // n_row

    def first_b(k):
        return (k + n_col - col) // n_col

    def home(ref, a, b):
        return ref.at[a, :, pl.ds(pl.multiple_of(b * size, size), size)]

    def spot(a, b):
        return b * row_blocks + a

    def col_of(k, b):
        return jnp.where(on_diag, row_slot(k, ratio * b + col // n_row), col_slot(k, b))

    def copy(src_slot, dst_slot, sem, device):
        return pltpu.make_async_remote_copy(
            src_ref=panel.at[src_slot], dst_ref=panel.at[dst_slot], send_sem=sem, recv_sem=recv_sem.at[dst_slot],
            device_id=device, device_id_type=MESH,
        )

    def arrived(slot):
        copy(slot, slot, send_sem.at[0, 0], at(row, col)).wait_recv()

    def start(c):
        c.start()

    def finish(c):
        c.wait_send()

    def down_column(k, a, ways, sems, target, act):
        slot = row_slot(k, a)
        dst = col_slot(k, (a * n_row + row) // n_col)
        for m, d in enumerate(ways):
            act(copy(slot, dst, sems[m], at(lax.rem(row + d, n_row), target)))

    def source_sends(k, a, act):
        ahead = a * n_row + row - k
        slot = row_slot(k, a)

        @pl.when(ahead == 1)
        def _():
            dst = col_slot(k, (k + 1) // n_col)
            act(copy(slot, dst, send_sem.at[a, 0], at(lax.rem(row + 1, n_row), lax.rem(col + 1, n_col))))

        @pl.when(lax.rem(ahead, n_col) == 0)
        def _():
            down_column(k, a, (1, n_row - 1, 2), [send_sem.at[a, m] for m in range(3)], col, act)

        @pl.when(jnp.logical_or(odd == 0, jnp.logical_or(ahead == 1, ahead >= n_col - 1)))
        def _():
            up = jnp.logical_or(odd == 0, ahead == 1)
            act(copy(slot, slot, send_sem.at[a, 3], at(row, lax.rem(jnp.where(up, col + 1, col - 1), n_col))))

        @pl.when(jnp.logical_and(odd == 1, ahead >= 2))
        def _():
            act(copy(slot, slot, send_sem.at[a, 6], at(row, lax.rem(col + 1, n_col))))

        @pl.when(ahead >= 2)
        def _():
            act(copy(slot, slot, send_sem.at[a, 4], at(row, lax.rem(col - odd + 3, n_col))))

        @pl.when(jnp.logical_and(odd == 1, jnp.logical_and(ahead >= n_col // 2 - 1, ahead < n_col - 3)))
        def _():
            act(copy(slot, slot, send_sem.at[a, 7], at(row, lax.rem(col + n_col // 2, n_col))))

        @pl.when(ahead >= n_col - 2 - odd)
        def _():
            act(copy(slot, slot, send_sem.at[a, 5], at(row, lax.rem(col - odd - 1 + n_col, n_col))))

    def lead(p):
        return lax.rem(col - lax.rem(p, n_col) + n_col, n_col)

    def hops(p):
        return lax.rem(col // 2 - lax.rem(p, n_col) // 2 + n_col // 2, n_col // 2)

    def passes(p):
        return jnp.logical_and(odd == 1, hops(p) != 0)

    def first_passed(p):
        low = jnp.where(passes(p), jnp.maximum(lead(p) - 1, 2), lead(p))
        return (p + low - row + n_row - 1) // n_row

    def pass_on(p, a, act):
        i = a * n_row + row
        ahead = i - p
        slot = row_slot(p, a)
        sems = pass_sem.at[lax.rem(p, depth), a]
        src_odd = lax.rem(p, 2)
        far = n_col - 2 - src_odd

        @pl.when(passes(p))
        def _():
            h = hops(p)
            via_prev = jnp.logical_or(src_odd == 1, jnp.logical_and(lax.rem(a, 2) == 1, ahead >= far))
            mine_to_pass = jnp.logical_or(
                jnp.logical_and(h == 1, jnp.logical_not(via_prev)), jnp.logical_and(h == n_col // 2 - 1, via_prev)
            )

            @pl.when(jnp.logical_and(mine_to_pass, ahead >= n_col // 2 - src_odd))
            def _():
                act(copy(slot, slot, sems.at[4], at(row, lax.rem(jnp.where(h == 1, col + 2, col - 2 + n_col), n_col))))

            @pl.when(jnp.logical_or(src_odd == 0, h != 1))
            def _():
                act(copy(slot, slot, sems.at[3], at(row, col - 1)))

        own = lax.rem(i, n_col) == col

        @pl.when(jnp.logical_and(own, ahead == 1))
        def _():
            down_column(p, a, (n_row - 1, 2), [sems.at[m] for m in range(2)], col, act)

        @pl.when(jnp.logical_and(own, ahead > 1))
        def _():
            down_column(p, a, (1, n_row - 1, 2), [sems.at[m] for m in range(3)], col, act)

    def passed(p):
        @pl.when(lead(p) != 0)
        def _():
            loop(first_passed(p), row_blocks, lambda a: pass_on(p, a, finish))

    def receive(p, a):
        arrived(row_slot(p, a))
        pass_on(p, a, start)

    def loop(lo, hi, fn):
        lax.fori_loop(lo, hi, lambda n, c: (fn(n), c)[1], 0)

    for a in range(row_blocks):
        for b in range(col_blocks):
            pltpu.make_async_copy(home(a_ref, a, b), share.at[spot(a, b)], load_sem).start()

    barrier = pltpu.get_barrier_semaphore()
    n_dev = n_row * n_col

    def greet(n):
        other = lax.rem(row * n_col + col + n, n_dev)
        pl.semaphore_signal(barrier, inc=1, device_id=at(other // n_col, lax.rem(other, n_col)), device_id_type=MESH)

    loop(1, n_dev, greet)
    with jax.named_scope("all_here"):
        pl.semaphore_wait(barrier, n_dev - 1)
    with jax.named_scope("loaded"):
        pltpu.make_async_copy(share, share, load_sem).wait()

    def seed_copy(b, dev_row):
        return pltpu.make_async_remote_copy(
            src_ref=share.at[spot(ratio * b + col // n_row, b)], dst_ref=diag.at[b],
            send_sem=seed_send.at[b, lax.rem(dev_row - row + n_row, n_row)],
            recv_sem=seed_recv.at[b], device_id=at(dev_row, col), device_id_type=MESH,
        )

    def hand_out(b):
        @pl.when(on_diag)
        def _():
            for d in (1, n_row - 1, 2):
                seed_copy(b, lax.rem(row + d, n_row)).start()
            diag[b] = share[spot(ratio * b + col // n_row, b)]

    hand_out(0)

    def seed_arrived(b):
        @pl.when(jnp.logical_not(on_diag))
        def _():
            seed_copy(b, row).wait_recv()

    with jax.named_scope("seed"):
        seed_arrived(0)

    def clear(n):
        a, b = lax.rem(n, row_blocks), n // row_blocks

        @pl.when(a * n_row + row < b * n_col + col)
        def _():
            share[n] = jnp.zeros((size, size), F32)
            pltpu.make_async_copy(share.at[n], home(o_ref, a, b), store_sem).start()

    loop(0, row_blocks * col_blocks, clear)

    def times_t(x, y):
        return lax.dot_general(x, y, (((1,), (1,)), ((), ())), preferred_element_type=F32)

    def update_block(p, a, b):
        share[spot(a, b)] -= times_t(panel[row_slot(p, a)], panel[col_of(p, b)])

    def update_diag(p, b):
        other = panel[col_of(p, b)]
        diag[b] -= times_t(other, other)

    def column_arrived(p, b):
        @pl.when(jnp.logical_not(on_diag))
        def _():
            arrived(col_slot(p, b))

    def update_column(p, b, lo):
        lone = lax.rem(row_blocks - lo, 2)

        @pl.when(lone == 1)
        def _():
            update_block(p, lo, b)

        def pair(m):
            a = lo + lone + 2 * m
            both = pl.ds(spot(a, b), 2)
            left = panel[pl.ds(row_slot(p, a), 2)].reshape(2 * size, size)
            share[both] -= times_t(left, panel[col_of(p, b)]).reshape(2, size, size)

        loop(0, (row_blocks - lo) // 2, pair)

    def trail(p, b_from, near):
        loop(b_from, col_blocks, lambda b: update_column(p, b, first_a(b * n_col + col - jnp.where(b == near, 0, 1))))

    def columns_arrived(p, b_from):
        loop(b_from, col_blocks, lambda b: column_arrived(p, b))

    def prepare(b):
        work[size:, :] = jnp.zeros((BASE, size), F32)
        r_id = lax.broadcasted_iota(jnp.int32, (size + BASE, size), 0)
        c_id = lax.broadcasted_iota(jnp.int32, (size + BASE, size), 1)
        winv[...] = jnp.where(r_id == c_id, 1.0, 0.0).astype(F32)

    def times_winv_t(x):
        hi, mid, lo = split3(x)
        whi, wmid, wlo = winv3[0], winv3[1], winv3[2]
        small = times_t(lo, whi) + times_t(mid, wmid) + times_t(hi, wlo)
        return small + (times_t(mid, whi) + times_t(hi, wmid)) + times_t(hi, whi)

    def solve(k, a, count, near):
        kb = k // n_col
        here = pl.ds(spot(a, kb), count)

        def apply(p):
            left = panel[pl.ds(row_slot(p, a), count)].reshape(count * size, size)
            share[here] -= times_t(left, panel[col_of(p, kb)]).reshape(count, size, size)

        if not near:

            @pl.when(k > 1)
            def _():
                for m in range(count):
                    receive(k - 2, a + m)

            loop(jnp.maximum(k - 1 - LAG, 0), k - 1, apply)

        @pl.when(k > 0)
        def _():
            for m in range(count):
                receive(k - 1, a + m)
            apply(k - 1)

        x = times_winv_t(share[here].reshape(count * size, size)).reshape(count, size, size)
        panel[pl.ds(row_slot(k, a), count)] = x.astype(BF16)
        share[here] = x
        for m in range(count):
            source_sends(k, a + m, start)
        for m in range(count):
            pltpu.make_async_copy(share.at[spot(a + m, kb)], home(o_ref, a + m, kb), store_sem).start()

    @pl.when(col == 0)
    def _():
        prepare(0)
        work[0:size, :] = diag[0]

    def step(k):
        mine = col == lax.rem(k, n_col)
        kb = k // n_col
        last = k - 1
        soon = jnp.logical_and(col == lax.rem(k + 1, n_col), k + 1 < steps)

        @pl.when(mine)
        def _():
            with jax.named_scope("factor"):
                factor_block(work, winv, prev)
            for n, part in enumerate(split3(winv[0:size, :])):
                winv3[n] = part
            lo = first_a(k)
            second = jnp.minimum(lo + 1, row_blocks)
            with jax.named_scope("solve_near"):
                loop(lo, second, lambda a: solve(k, a, 1, True))
            with jax.named_scope("solve_one"):
                third = second + lax.rem(row_blocks - second, 2)
                loop(second, third, lambda a: solve(k, a, 1, False))
            with jax.named_scope("solve_two"):
                loop(0, (row_blocks - third) // 2, lambda m: solve(k, third + 2 * m, 2, False))

        @pl.when(k >= depth)
        def _():
            with jax.named_scope("passed"):
                passed(k - depth)

        @pl.when(mine)
        def _():
            @pl.when(row == lax.rem(k, n_row))
            def _():
                for d in range(1, n_row):
                    seed_copy(kb, lax.rem(row + d, n_row)).wait_send()
                r_id = lax.broadcasted_iota(jnp.int32, (size, size), 0)
                c_id = lax.broadcasted_iota(jnp.int32, (size, size), 1)
                n = spot(k // n_row, kb)
                share[n] = jnp.where(r_id >= c_id, work[0:size, :].T, 0.0)
                pltpu.make_async_copy(share.at[n], home(o_ref, k // n_row, kb), store_sem).start()

            with jax.named_scope("late_trail"):

                def late(p):
                    columns_arrived(p, kb + 1)
                    trail(p, kb + 1, -1)

                loop(jnp.maximum(k - 1 - LAG, 0), k - LAG + 1, late)

            @pl.when(kb + 1 < col_blocks)
            def _():
                hand_out(kb + 1)

        @pl.when(jnp.logical_and(k > 0, jnp.logical_not(jnp.logical_or(mine, soon))))
        def _():
            @pl.when(col != lax.rem(last, n_col))
            def _():
                with jax.named_scope("receive"):
                    loop(first_passed(last), row_blocks, lambda a: receive(last, a))

            @pl.when(k >= LAG)
            def _():
                p = k - LAG
                near = first_b(k)
                with jax.named_scope("columns"):
                    columns_arrived(p, near)

                @pl.when(near < col_blocks)
                def _():
                    age = k + n_col - (near * n_col + col)

                    @pl.when(jnp.logical_and(age == 3, near > 0))
                    def _():
                        with jax.named_scope("seed_late"):
                            seed_arrived(near)

                    @pl.when(age >= 3)
                    def _():
                        oldest = jnp.where(age == 3, jnp.maximum(p - 2, 0), p)
                        loop(oldest, p + 1, lambda q: update_diag(q, near))

                with jax.named_scope("trail"):
                    trail(p, near, near)

        @pl.when(soon)
        def _():
            nb = (k + 1) // n_col

            oldest = jnp.maximum(k - LAG, 0)

            def old_diag(p):
                column_arrived(p, nb)
                update_diag(p, nb)

            def take(a):
                receive(last, a)

                @pl.when(a * n_row + row > k + 1)
                def _():
                    loop(oldest, last, lambda p: update_block(p, a, nb))

            @pl.when(k > 0)
            def _():
                with jax.named_scope("old_diag"):
                    loop(oldest, last, old_diag)
                with jax.named_scope("take"):
                    loop(first_a(k), jnp.minimum(first_a(k + 1) + 1, row_blocks), take)
                with jax.named_scope("take_column"):
                    column_arrived(last, nb)
                with jax.named_scope("catch_up"):
                    update_diag(last, nb)
                    loop(first_a(k + 1), jnp.minimum(first_a(k + 1) + 1, row_blocks), lambda a: update_block(last, a, nb))

            prepare(nb)
            slot = col_of(k, nb)
            with jax.named_scope("first_block"):
                arrived(slot)

            @pl.when(on_diag)
            def _():
                pass_on(k, (k + 1) // n_row, start)

            other = panel[slot]
            work[0:size, :] = diag[nb] - times_t(other, other)

        @pl.when(jnp.logical_and(k >= n_col // 2, col == lax.rem(k + n_col // 2, n_col)))
        def _():
            with jax.named_scope("sends_done"):
                loop(first_a(k - n_col // 2), row_blocks, lambda a: source_sends(k - n_col // 2, a, finish))

    loop(0, steps, step)

    loop(steps - depth, steps, passed)

    def last_sends(k):
        @pl.when(col == lax.rem(k, n_col))
        def _():
            loop(first_a(k), row_blocks, lambda a: source_sends(k, a, finish))

    loop(steps - n_col // 2, steps, last_sends)
    with jax.named_scope("stored"):
        pltpu.make_async_copy(share, share, store_sem).wait()


def solution(mesh):
    n_row = mesh.shape["row"]
    n_col = mesh.shape["col"]

    def factor_local(a_loc):
        row_blocks, size, local_cols = a_loc.shape
        col_blocks = local_cols // size
        slots = n_row * (row_blocks * (row_blocks + 1) // 2) + n_col * (col_blocks * (col_blocks + 1) // 2)
        return pl.pallas_call(
            functools.partial(kernel, n_row, n_col, "batch"),
            out_shape=jax.ShapeDtypeStruct(a_loc.shape, F32),
            in_specs=[pl.BlockSpec(memory_space=pl.ANY)],
            out_specs=pl.BlockSpec(memory_space=pl.ANY),
            scratch_shapes=[
                pltpu.VMEM((row_blocks * col_blocks, size, size), F32),
                pltpu.VMEM((col_blocks, size, size), F32),
                pltpu.VMEM((slots, size, size), BF16),
                pltpu.VMEM((size + BASE, size), F32),
                pltpu.VMEM((size + BASE, size), F32),
                pltpu.VMEM((3, size, size), BF16),
                pltpu.VMEM((BASE, 3 * LANE), F32),
                pltpu.SemaphoreType.DMA,
                pltpu.SemaphoreType.DMA,
                pltpu.SemaphoreType.DMA((col_blocks, n_row)),
                pltpu.SemaphoreType.DMA((col_blocks,)),
                pltpu.SemaphoreType.DMA((row_blocks, 8)),
                pltpu.SemaphoreType.DMA((4, row_blocks, 5)),
                pltpu.SemaphoreType.DMA((slots,)),
            ],
            compiler_params=pltpu.CompilerParams(
                collective_id=0, has_side_effects=True, vmem_limit_bytes=60 * 1024 * 1024
            ),
            name="cholesky",
        )(a_loc)

    blk_spec = P(("batch", "row"), None, "col")
    return jax.shard_map(factor_local, mesh=mesh, in_specs=(blk_spec,), out_specs=blk_spec, check_vma=False)
```

```python
import functools

import jax
import jax.numpy as jnp
from jax import lax
from jax.experimental import pallas as pl
from jax.experimental.pallas import tpu as pltpu
from jax.sharding import PartitionSpec as P

F32 = jnp.float32
BF16 = jnp.bfloat16
MESH = pl.DeviceIdType.MESH
SUB = 8
LANE = 128
BASE = 16
LEAD = 0
LAG = 3


def sub_bcast(x, q):
    return jnp.broadcast_to(x[q : q + 1, :], (SUB, LANE))


def lane_bcast(x, lane):
    return jnp.take_along_axis(x, jnp.full((SUB, LANE), lane, jnp.int32), axis=1)


def split3(x):
    high = x.astype(BF16)
    rest = x - high.astype(F32)
    mid = rest.astype(BF16)
    return high, mid, (rest - mid.astype(F32)).astype(BF16)


def swap_rows(x, bit, row_id):
    if bit == SUB // 2:
        return pltpu.roll(x, bit, 0)
    return jnp.where((row_id & bit) == 0, pltpu.roll(x, SUB - bit, 0), pltpu.roll(x, bit, 0))


def stack_sums(parts):
    row_id = lax.broadcasted_iota(jnp.int32, (SUB, LANE), 0)
    for bit in (4, 2, 1):
        low = (row_id & bit) == 0
        half = len(parts) // 2
        parts = [
            jnp.where(low, parts[n], parts[n + half]) + swap_rows(jnp.where(low, parts[n + half], parts[n]), bit, row_id)
            for n in range(half)
        ]
    return parts[0]


def eliminate(rows, lane0):
    row_id = lax.broadcasted_iota(jnp.int32, (SUB, LANE), 0)
    rows = [list(rows[0]), list(rows[1])]
    cols = [
        [lane_bcast(rows[0][0], lane0 + j) for j in range(SUB)],
        [lane_bcast(rows[1][0], lane0 + j) for j in range(BASE)],
    ]
    scale = [jnp.zeros((SUB, LANE), F32), jnp.zeros((SUB, LANE), F32)]
    pivot = sub_bcast(cols[0][0], 0)
    for j in range(BASE):
        t, q = divmod(j, SUB)
        inv = lax.rsqrt(pivot)
        scale[t] = jnp.where(row_id == q, inv, scale[t])
        if j + 1 < BASE:
            tn, qn = divmod(j + 1, SUB)
            near = sub_bcast(cols[tn][j], qn) * inv
            pivot = sub_bcast(cols[tn][j + 1], qn) - near * near
        below = cols[1][j] * inv
        here = cols[0][j] * inv if t == 0 else None
        for n in range(j + 1, BASE):
            tn, qn = divmod(n, SUB)
            other = sub_bcast(cols[tn][j], qn) * inv
            if t == 0 and tn == 0:
                cols[0][n] = cols[0][n] - here * other
            cols[1][n] = cols[1][n] - below * other
        masked = jnp.where(row_id > q, here if t == 0 else below, 0.0)
        for v in range(len(rows[0])):
            pivot_row = sub_bcast(rows[t][v], q) * inv
            rows[t][v] = rows[t][v] - masked * pivot_row
            if t == 0:
                rows[1][v] = rows[1][v] - below * pivot_row
    return [[x * scale[t] for x in rows[t]] for t in range(2)]


def factor_block(work, winv, prev):
    size = work.shape[1]
    prev[...] = jnp.zeros(prev.shape, F32)
    for half in range(size // LANE):
        views = [(work, 0), (work, 1), (winv, 0)] if half == 0 else [(work, 1), (winv, 0), (winv, 1)]
        first = half * LANE
        if half == 1:
            mid_part, inv_part = prev[:, LANE : 2 * LANE], prev[:, 2 * LANE :]
            prev[:, :LANE] = mid_part
            prev[:, LANE : 2 * LANE] = inv_part
            prev[:, 2 * LANE :] = jnp.zeros((BASE, LANE), F32)

        def body(s, carry, views=views, first=first):
            lane0 = s * BASE
            row0 = pl.multiple_of(first + lane0, BASE)

            def rows_at(row, t):
                return pl.ds(pl.multiple_of(row + SUB * t, SUB), SUB)

            rows = [[ref[rows_at(row0, t), LANE * g : LANE * (g + 1)] for ref, g in views] for t in range(2)]
            hi, mid, lo = split3(prev[...])
            lane = lax.broadcasted_iota(jnp.int32, (BASE, size - first), 1) + first
            after = lane >= row0 + BASE
            lhi, lmid, llo = [jnp.where(after, x[:, : size - first], jnp.zeros((), BF16)) for x in (hi, mid, lo)]
            update = lax.dot_general(
                jnp.concatenate([lhi, lhi, lmid, lhi, llo, lmid], axis=0),
                jnp.concatenate([hi, mid, hi, lo, hi, mid], axis=0),
                (((0,), (0,)), ((), ())),
                preferred_element_type=F32,
            )
            for v, (ref, g) in enumerate(views):
                ref[first:size, LANE * g : LANE * (g + 1)] -= update[:, LANE * v : LANE * (v + 1)]
            done = eliminate(rows, lane0)
            for t in range(2):
                for v, (ref, g) in enumerate(views):
                    ref[rows_at(row0, t), LANE * g : LANE * (g + 1)] = done[t][v]
                    prev[SUB * t : SUB * (t + 1), LANE * v : LANE * (v + 1)] = done[t][v]
            if first == 0:
                source = [jnp.where(s == LANE // BASE - 1, done[t][1], done[t][0]) for t in range(2)]
            else:
                source = [done[t][0] for t in range(2)]
            next_lane = (lane0 + BASE) % LANE
            for t in range(2):
                factor = [[lane_bcast(source[m], next_lane + SUB * t + n) for n in range(SUB)] for m in range(2)]
                for v, (ref, g) in enumerate(views):
                    parts = [factor[0][n] * done[0][v] + factor[1][n] * done[1][v] for n in range(SUB)]
                    ref[rows_at(row0 + BASE, t), LANE * g : LANE * (g + 1)] -= stack_sums(parts)
            return carry

        lax.fori_loop(0, LANE // BASE, body, 0)


def kernel(n_row, n_col, batch_axis, a_ref, o_ref, share, diag, edge, stage, first, panel, work, winv, winv3, prev, load_sem, store_sem,
           seed_send, seed_recv, edge_send, edge_recv, first_sem, send_sem, pass_sem, recv_sem):
    row_blocks, size, local_cols = a_ref.shape
    col_blocks = local_cols // size
    ratio = n_col // n_row
    steps = row_blocks * n_row
    depth = pass_sem.shape[0]
    batch = lax.axis_index(batch_axis)
    row = lax.axis_index("row")
    col = lax.axis_index("col")
    odd = lax.rem(col, 2)
    on_diag = lax.rem(col, n_row) == row
    row_slots = n_row * (row_blocks * (row_blocks + 1) // 2)
    edge_slots = row_slots + n_col * (col_blocks * (col_blocks + 1) // 2)
    leads = row == LEAD

    def at(dev_row, dev_col):
        return (batch, dev_row, dev_col)

    def row_slot(k, a):
        g = k // n_row
        return n_row * (row_blocks * g - (g * (g - 1)) // 2) + (k - g * n_row) * (row_blocks - g) + a - g

    def col_slot(k, b):
        h = k // n_col
        return row_slots + n_col * (col_blocks * h - (h * (h - 1)) // 2) + (k - h * n_col) * (col_blocks - h) + b - h

    def first_a(k):
        return (k + n_row - row) // n_row

    def first_b(k):
        return (k + n_col - col) // n_col

    def home(ref, a, b):
        return ref.at[a, :, pl.ds(pl.multiple_of(b * size, size), size)]

    def spot(a, b):
        return b * row_blocks + a

    def col_of(k, b):
        return jnp.where(on_diag, row_slot(k, ratio * b + col // n_row), col_slot(k, b))

    def edge_slot(k, j):
        return edge_slots + 2 * k + (j - k - 1) // n_col

    def edge_reach(ahead):
        return jnp.logical_and(ahead >= 2, jnp.logical_and(ahead <= n_col + LAG, row != LEAD))

    def copy(src_slot, dst_slot, sem, device):
        return pltpu.make_async_remote_copy(
            src_ref=panel.at[src_slot], dst_ref=panel.at[dst_slot], send_sem=sem, recv_sem=recv_sem.at[dst_slot],
            device_id=device, device_id_type=MESH,
        )

    def arrived(slot):
        copy(slot, slot, send_sem.at[0, 0], at(row, col)).wait_recv()

    def start(c):
        c.start()

    def finish(c):
        c.wait_send()

    def down_column(k, a, ways, sems, target, act):
        slot = row_slot(k, a)
        dst = col_slot(k, (a * n_row + row) // n_col)
        for m, d in enumerate(ways):
            act(copy(slot, dst, sems[m], at(lax.rem(row + d, n_row), target)))

    def to_edge(k, a, sem, act):
        i = a * n_row + row
        act(copy(row_slot(k, a), edge_slot(k, i - 1), sem, at(LEAD, lax.rem(i - 1, n_col))))

    def source_sends(k, a, act):
        ahead = a * n_row + row - k
        slot = row_slot(k, a)
        early = n_row

        @pl.when(jnp.logical_and(edge_reach(ahead), jnp.logical_or(ahead <= early, ahead == n_col)))
        def _():
            to_edge(k, a, send_sem.at[a, 5], act)

        @pl.when(lax.rem(ahead, n_col) == 0)
        def _():
            down_column(k, a, (1, n_row - 1, 2), [send_sem.at[a, m] for m in range(3)], col, act)

        @pl.when(jnp.logical_or(jnp.logical_and(odd == 0, ahead >= 2), ahead >= n_col - 1))
        def _():
            act(copy(slot, slot, send_sem.at[a, 3], at(row, lax.rem(jnp.where(odd == 0, col + 1, col - 1), n_col))))

        @pl.when(jnp.logical_and(odd == 1, ahead >= 2))
        def _():
            act(copy(slot, slot, send_sem.at[a, 6], at(row, lax.rem(col + 1, n_col))))

        @pl.when(ahead >= 2)
        def _():
            act(copy(slot, slot, send_sem.at[a, 4], at(row, lax.rem(col - odd + 3, n_col))))

        @pl.when(jnp.logical_and(odd == 1, jnp.logical_and(ahead >= n_col // 2 - 1, ahead < n_col - 3)))
        def _():
            act(copy(slot, slot, send_sem.at[a, 7], at(row, lax.rem(col + n_col // 2, n_col))))

        @pl.when(ahead >= n_col - 2 - odd)
        def _():
            act(copy(slot, slot, send_sem.at[a, 8], at(row, lax.rem(col - odd - 1 + n_col, n_col))))

    def lead(p):
        return lax.rem(col - lax.rem(p, n_col) + n_col, n_col)

    def hops(p):
        return lax.rem(col // 2 - lax.rem(p, n_col) // 2 + n_col // 2, n_col // 2)

    def passes(p):
        return jnp.logical_and(odd == 1, hops(p) != 0)

    def first_passed(p):
        low = jnp.where(passes(p), jnp.maximum(lead(p) - 1, 2), lead(p))
        return (p + low - row + n_row - 1) // n_row

    def pass_on(p, a, act):
        i = a * n_row + row
        ahead = i - p
        slot = row_slot(p, a)
        sems = pass_sem.at[lax.rem(p, depth), a]
        src_odd = lax.rem(p, 2)
        far = n_col - 2 - src_odd

        @pl.when(passes(p))
        def _():
            h = hops(p)
            via_prev = jnp.logical_or(src_odd == 1, jnp.logical_and(lax.rem(a, 2) == 1, ahead >= far))
            mine_to_pass = jnp.logical_or(
                jnp.logical_and(h == 1, jnp.logical_not(via_prev)), jnp.logical_and(h == n_col // 2 - 1, via_prev)
            )

            @pl.when(jnp.logical_and(mine_to_pass, ahead >= n_col // 2 - src_odd))
            def _():
                act(copy(slot, slot, sems.at[4], at(row, lax.rem(jnp.where(h == 1, col + 2, col - 2 + n_col), n_col))))

            @pl.when(jnp.logical_or(src_odd == 0, h != 1))
            def _():
                act(copy(slot, slot, sems.at[3], at(row, col - 1)))

        own = lax.rem(i, n_col) == col

        @pl.when(jnp.logical_and(own, jnp.logical_and(ahead > n_row, edge_reach(ahead))))
        def _():
            to_edge(p, a, sems.at[5], act)

        @pl.when(jnp.logical_and(own, ahead > 1))
        def _():
            down_column(p, a, (1, n_row - 1, 2), [sems.at[m] for m in range(3)], col, act)

    def passed(p):
        @pl.when(lead(p) != 0)
        def _():
            loop(first_passed(p), row_blocks, lambda a: pass_on(p, a, finish))

    def receive(p, a):
        arrived(row_slot(p, a))
        pass_on(p, a, start)

    def loop(lo, hi, fn):
        lax.fori_loop(lo, hi, lambda n, c: (fn(n), c)[1], 0)

    for a in range(row_blocks):
        for b in range(col_blocks):
            pltpu.make_async_copy(home(a_ref, a, b), share.at[spot(a, b)], load_sem).start()

    barrier = pltpu.get_barrier_semaphore()
    n_dev = n_row * n_col

    def greet(n):
        other = lax.rem(row * n_col + col + n, n_dev)
        pl.semaphore_signal(barrier, inc=1, device_id=at(other // n_col, lax.rem(other, n_col)), device_id_type=MESH)

    loop(1, n_dev, greet)
    with jax.named_scope("all_here"):
        pl.semaphore_wait(barrier, n_dev - 1)
    with jax.named_scope("loaded"):
        pltpu.make_async_copy(share, share, load_sem).wait()

    def seed_copy(b, dev_row):
        return pltpu.make_async_remote_copy(
            src_ref=share.at[spot(ratio * b + col // n_row, b)], dst_ref=diag.at[b],
            send_sem=seed_send.at[b, lax.rem(dev_row - row + n_row, n_row)],
            recv_sem=seed_recv.at[b], device_id=at(dev_row, col), device_id_type=MESH,
        )

    def hand_out(b):
        @pl.when(on_diag)
        def _():
            for d in (1, n_row - 1, 2):
                seed_copy(b, lax.rem(row + d, n_row)).start()
            diag[b] = share[spot(ratio * b + col // n_row, b)]

        @pl.when(jnp.logical_and(holds_edge(b), jnp.logical_not(leads)))
        def _():
            stage[b] = share[spot((b * n_col + col + 1) // n_row, b)]
            edge_copy(b).start()

    def holds_edge(b):
        j = b * n_col + col
        return jnp.logical_and(lax.rem(j + 1, n_row) == row, j + 1 < steps)

    def edge_copy(b):
        return pltpu.make_async_remote_copy(
            src_ref=stage.at[b], dst_ref=edge.at[b], send_sem=edge_send.at[b], recv_sem=edge_recv.at[b],
            device_id=at(LEAD, col), device_id_type=MESH,
        )

    def has_edge(b):
        from_other = jnp.logical_and(leads, lax.rem(col + 1, n_row) != LEAD)
        return jnp.logical_and(from_other, b * n_col + col + 1 < steps)

    def edge_seeded(b):
        @pl.when(has_edge(b))
        def _():
            edge_copy(b).wait_recv()

    def edge_arrived(p, b):
        j = b * n_col + col

        @pl.when(jnp.logical_and(has_edge(b), j + 1 - p <= n_col + LAG))
        def _():
            arrived(edge_slot(p, j))

    hand_out(0)

    def seed_arrived(b):
        @pl.when(jnp.logical_not(on_diag))
        def _():
            seed_copy(b, row).wait_recv()

    with jax.named_scope("seed"):
        seed_arrived(0)

        @pl.when(col != 0)
        def _():
            edge_seeded(0)

    def clear(n):
        a, b = lax.rem(n, row_blocks), n // row_blocks

        @pl.when(a * n_row + row < b * n_col + col)
        def _():
            share[n] = jnp.zeros((size, size), F32)
            pltpu.make_async_copy(share.at[n], home(o_ref, a, b), store_sem).start()

    loop(0, row_blocks * col_blocks, clear)

    def times_t(x, y):
        return lax.dot_general(x, y, (((1,), (1,)), ((), ())), preferred_element_type=F32)

    def update_block(p, a, b):
        share[spot(a, b)] -= times_t(panel[row_slot(p, a)], panel[col_of(p, b)])

    def update_diag(p, b):
        other = panel[col_of(p, b)]
        diag[b] -= times_t(other, other)

    def update_edge(p, b):
        @pl.when(has_edge(b))
        def _():
            edge[b] -= times_t(panel[edge_slot(p, b * n_col + col)], panel[col_of(p, b)])

    def column_arrived(p, b):
        @pl.when(jnp.logical_not(on_diag))
        def _():
            arrived(col_slot(p, b))

    def update_column(p, b, lo):
        lone = lax.rem(row_blocks - lo, 2)

        @pl.when(lone == 1)
        def _():
            update_block(p, lo, b)

        def pair(m):
            a = lo + lone + 2 * m
            both = pl.ds(spot(a, b), 2)
            left = panel[pl.ds(row_slot(p, a), 2)].reshape(2 * size, size)
            share[both] -= times_t(left, panel[col_of(p, b)]).reshape(2, size, size)

        loop(0, (row_blocks - lo) // 2, pair)

    def trail(p, b_from, near):
        loop(b_from, col_blocks, lambda b: update_column(p, b, first_a(b * n_col + col - jnp.where(b == near, 0, 1))))

    def columns_arrived(p, b_from):
        def one(b):
            column_arrived(p, b)
            edge_arrived(p, b)

        loop(b_from, col_blocks, one)

    def prepare(b):
        work[size:, :] = jnp.zeros((BASE, size), F32)
        r_id = lax.broadcasted_iota(jnp.int32, (size + BASE, size), 0)
        c_id = lax.broadcasted_iota(jnp.int32, (size + BASE, size), 1)
        winv[...] = jnp.where(r_id == c_id, 1.0, 0.0).astype(F32)

    def times_winv_t(x):
        hi, mid, lo = split3(x)
        whi, wmid, wlo = winv3[0], winv3[1], winv3[2]
        small = times_t(lo, whi) + times_t(mid, wmid) + times_t(hi, wlo)
        return small + (times_t(mid, whi) + times_t(hi, wmid)) + times_t(hi, whi)

    def solve(k, a, count, near):
        kb = k // n_col
        here = pl.ds(spot(a, kb), count)

        def apply(p):
            left = panel[pl.ds(row_slot(p, a), count)].reshape(count * size, size)
            share[here] -= times_t(left, panel[col_of(p, kb)]).reshape(count, size, size)

        if not near:

            @pl.when(k > 1)
            def _():
                for m in range(count):
                    receive(k - 2, a + m)

            loop(jnp.maximum(k - 1 - LAG, 0), k - 1, apply)

        @pl.when(k > 0)
        def _():
            for m in range(count):
                receive(k - 1, a + m)
            apply(k - 1)

        x = times_winv_t(share[here].reshape(count * size, size)).reshape(count, size, size)
        panel[pl.ds(row_slot(k, a), count)] = x.astype(BF16)
        share[here] = x
        if near:

            @pl.when(jnp.logical_and(leads, lax.rem(k + 1, n_row) == LEAD))
            def _():
                first[...] = panel[row_slot(k, a)]
                first_copy(k).start()

        for m in range(count):
            source_sends(k, a + m, start)
        for m in range(count):
            pltpu.make_async_copy(share.at[spot(a + m, kb)], home(o_ref, a + m, kb), store_sem).start()

    def update_near(p, b):
        update_diag(p, b)
        update_edge(p, b)

    def first_slot(k, dev_row):
        return jnp.where(lax.rem(k + 1, n_row) == dev_row, row_slot(k, (k + 1) // n_row), col_slot(k, (k + 1) // n_col))

    def first_copy(k):
        dst = first_slot(k, LEAD)
        return pltpu.make_async_remote_copy(
            src_ref=first, dst_ref=panel.at[dst], send_sem=first_sem.at[0], recv_sem=recv_sem.at[dst],
            device_id=at(LEAD, lax.rem(col + 1, n_col)), device_id_type=MESH,
        )

    def first_down(k, act):
        for d in range(1, n_row):
            act(copy(first_slot(k, LEAD), first_slot(k, (LEAD + d) % n_row), first_sem.at[d], at((LEAD + d) % n_row, col)))

    def firsts_done(k):
        @pl.when(jnp.logical_and(leads, k + 1 < steps))
        def _():
            first_copy(k).wait_send()

        @pl.when(jnp.logical_and(leads, k > 0))
        def _():
            first_down(k - 1, finish)

    @pl.when(col == 0)
    def _():
        prepare(0)
        work[0:size, :] = diag[0]

    def step(k):
        mine = col == lax.rem(k, n_col)
        kb = k // n_col
        last = k - 1
        soon = jnp.logical_and(col == lax.rem(k + 1, n_col), k + 1 < steps)

        @pl.when(mine)
        def _():
            with jax.named_scope("factor"):
                factor_block(work, winv, prev)
            for n, part in enumerate(split3(winv[0:size, :])):
                winv3[n] = part

            @pl.when(has_edge(kb))
            def _():
                with jax.named_scope("lead"):

                    @pl.when(k == 0)
                    def _():
                        edge_seeded(kb)

                    @pl.when(k > 0)
                    def _():
                        edge_arrived(last, kb)
                        update_edge(last, kb)

                    first[...] = times_winv_t(edge[kb]).astype(BF16)
                    first_copy(k).start()

            lo = first_a(k)
            second = jnp.minimum(lo + 1, row_blocks)
            with jax.named_scope("solve_near"):
                loop(lo, second, lambda a: solve(k, a, 1, True))
            with jax.named_scope("solve_one"):
                third = second + lax.rem(row_blocks - second, 2)
                loop(second, third, lambda a: solve(k, a, 1, False))
            with jax.named_scope("solve_two"):
                loop(0, (row_blocks - third) // 2, lambda m: solve(k, third + 2 * m, 2, False))

        @pl.when(k >= depth)
        def _():
            with jax.named_scope("passed"):
                passed(k - depth)

        @pl.when(mine)
        def _():
            @pl.when(row == lax.rem(k, n_row))
            def _():
                for d in range(1, n_row):
                    seed_copy(kb, lax.rem(row + d, n_row)).wait_send()
                r_id = lax.broadcasted_iota(jnp.int32, (size, size), 0)
                c_id = lax.broadcasted_iota(jnp.int32, (size, size), 1)
                n = spot(k // n_row, kb)
                share[n] = jnp.where(r_id >= c_id, work[0:size, :].T, 0.0)
                pltpu.make_async_copy(share.at[n], home(o_ref, k // n_row, kb), store_sem).start()

            with jax.named_scope("late_trail"):

                def late(p):
                    columns_arrived(p, kb + 1)
                    trail(p, kb + 1, -1)

                loop(jnp.maximum(k - 1 - LAG, 0), k - LAG + 1, late)

            @pl.when(kb + 1 < col_blocks)
            def _():
                hand_out(kb + 1)

        @pl.when(jnp.logical_and(k > 0, jnp.logical_not(jnp.logical_or(mine, soon))))
        def _():
            @pl.when(col != lax.rem(last, n_col))
            def _():
                with jax.named_scope("receive"):
                    loop(first_passed(last), row_blocks, lambda a: receive(last, a))

            @pl.when(k >= LAG)
            def _():
                p = k - LAG
                near = first_b(k)
                with jax.named_scope("columns"):
                    columns_arrived(p, near)

                @pl.when(near < col_blocks)
                def _():
                    age = k + n_col - (near * n_col + col)

                    @pl.when(jnp.logical_and(age == 3, near > 0))
                    def _():
                        with jax.named_scope("seed_late"):
                            seed_arrived(near)
                            edge_seeded(near)

                    @pl.when(age >= 3)
                    def _():
                        oldest = jnp.where(age == 3, jnp.maximum(p - 2, 0), p)
                        loop(oldest, p + 1, lambda q: update_near(q, near))

                with jax.named_scope("trail"):
                    trail(p, near, near)

        @pl.when(soon)
        def _():
            nb = (k + 1) // n_col

            oldest = jnp.maximum(k - LAG, 0)

            def old_diag(p):
                column_arrived(p, nb)
                edge_arrived(p, nb)
                update_near(p, nb)

            def take(a):
                receive(last, a)

                @pl.when(a * n_row + row > k + 1)
                def _():
                    loop(oldest, last, lambda p: update_block(p, a, nb))

            @pl.when(k > 0)
            def _():
                with jax.named_scope("old_diag"):
                    loop(oldest, last, old_diag)
                with jax.named_scope("take"):
                    loop(first_a(k), jnp.minimum(first_a(k + 1) + 1, row_blocks), take)
                with jax.named_scope("take_column"):
                    column_arrived(last, nb)
                    edge_arrived(last, nb)
                with jax.named_scope("catch_up"):
                    update_near(last, nb)
                    loop(first_a(k + 1), jnp.minimum(first_a(k + 1) + 1, row_blocks), lambda a: update_block(last, a, nb))

            prepare(nb)
            slot = col_of(k, nb)
            with jax.named_scope("first_block"):
                arrived(slot)

            @pl.when(leads)
            def _():
                first_down(k, start)

            other = panel[slot]
            work[0:size, :] = diag[nb] - times_t(other, other)

        @pl.when(jnp.logical_and(k >= n_col // 2, col == lax.rem(k + n_col // 2, n_col)))
        def _():
            with jax.named_scope("sends_done"):
                firsts_done(k - n_col // 2)
                loop(first_a(k - n_col // 2), row_blocks, lambda a: source_sends(k - n_col // 2, a, finish))

    loop(0, steps, step)

    loop(steps - depth, steps, passed)

    def last_sends(k):
        @pl.when(col == lax.rem(k, n_col))
        def _():
            firsts_done(k)
            loop(first_a(k), row_blocks, lambda a: source_sends(k, a, finish))

    loop(steps - n_col // 2, steps, last_sends)

    def edges_done(b):
        @pl.when(jnp.logical_and(holds_edge(b), jnp.logical_not(leads)))
        def _():
            edge_copy(b).wait_send()

    loop(0, col_blocks, edges_done)
    with jax.named_scope("stored"):
        pltpu.make_async_copy(share, share, store_sem).wait()


def solution(mesh):
    n_row = mesh.shape["row"]
    n_col = mesh.shape["col"]

    def factor_local(a_loc):
        row_blocks, size, local_cols = a_loc.shape
        col_blocks = local_cols // size
        slots = n_row * (row_blocks * (row_blocks + 1) // 2) + n_col * (col_blocks * (col_blocks + 1) // 2)
        slots += 2 * row_blocks * n_row
        return pl.pallas_call(
            functools.partial(kernel, n_row, n_col, "batch"),
            out_shape=jax.ShapeDtypeStruct(a_loc.shape, F32),
            in_specs=[pl.BlockSpec(memory_space=pl.ANY)],
            out_specs=pl.BlockSpec(memory_space=pl.ANY),
            scratch_shapes=[
                pltpu.VMEM((row_blocks * col_blocks, size, size), F32),
                pltpu.VMEM((col_blocks, size, size), F32),
                pltpu.VMEM((col_blocks, size, size), F32),
                pltpu.VMEM((col_blocks, size, size), F32),
                pltpu.VMEM((size, size), BF16),
                pltpu.VMEM((slots, size, size), BF16),
                pltpu.VMEM((size + BASE, size), F32),
                pltpu.VMEM((size + BASE, size), F32),
                pltpu.VMEM((3, size, size), BF16),
                pltpu.VMEM((BASE, 3 * LANE), F32),
                pltpu.SemaphoreType.DMA,
                pltpu.SemaphoreType.DMA,
                pltpu.SemaphoreType.DMA((col_blocks, n_row)),
                pltpu.SemaphoreType.DMA((col_blocks,)),
                pltpu.SemaphoreType.DMA((col_blocks,)),
                pltpu.SemaphoreType.DMA((col_blocks,)),
                pltpu.SemaphoreType.DMA((n_row,)),
                pltpu.SemaphoreType.DMA((row_blocks, 9)),
                pltpu.SemaphoreType.DMA((4, row_blocks, 6)),
                pltpu.SemaphoreType.DMA((slots,)),
            ],
            compiler_params=pltpu.CompilerParams(
                collective_id=0, has_side_effects=True, vmem_limit_bytes=60 * 1024 * 1024
            ),
            name="cholesky",
        )(a_loc)

    blk_spec = P(("batch", "row"), None, "col")
    return jax.shard_map(factor_local, mesh=mesh, in_specs=(blk_spec,), out_specs=blk_spec, check_vma=False)
```

```python
import functools

import jax
import jax.numpy as jnp
from jax import lax
from jax.experimental import pallas as pl
from jax.experimental.pallas import tpu as pltpu
from jax.sharding import PartitionSpec as P

F32 = jnp.float32
BF16 = jnp.bfloat16
MESH = pl.DeviceIdType.MESH
SUB = 8
LANE = 128
BASE = 16
LEAD = 1
LAG = 3


def sub_bcast(x, q):
    return jnp.broadcast_to(x[q : q + 1, :], (SUB, LANE))


def lane_bcast(x, lane):
    return jnp.take_along_axis(x, jnp.full((SUB, LANE), lane, jnp.int32), axis=1)


def split3(x):
    high = x.astype(BF16)
    rest = x - high.astype(F32)
    mid = rest.astype(BF16)
    return high, mid, (rest - mid.astype(F32)).astype(BF16)


def swap_rows(x, bit, row_id):
    if bit == SUB // 2:
        return pltpu.roll(x, bit, 0)
    return jnp.where((row_id & bit) == 0, pltpu.roll(x, SUB - bit, 0), pltpu.roll(x, bit, 0))


def stack_sums(parts):
    row_id = lax.broadcasted_iota(jnp.int32, (SUB, LANE), 0)
    for bit in (4, 2, 1):
        low = (row_id & bit) == 0
        half = len(parts) // 2
        parts = [
            jnp.where(low, parts[n], parts[n + half]) + swap_rows(jnp.where(low, parts[n + half], parts[n]), bit, row_id)
            for n in range(half)
        ]
    return parts[0]


def eliminate(rows, lane0):
    row_id = lax.broadcasted_iota(jnp.int32, (SUB, LANE), 0)
    rows = [list(rows[0]), list(rows[1])]
    cols = [
        [lane_bcast(rows[0][0], lane0 + j) for j in range(SUB)],
        [lane_bcast(rows[1][0], lane0 + j) for j in range(BASE)],
    ]
    scale = [jnp.zeros((SUB, LANE), F32), jnp.zeros((SUB, LANE), F32)]
    pivot = sub_bcast(cols[0][0], 0)
    for j in range(BASE):
        t, q = divmod(j, SUB)
        inv = lax.rsqrt(pivot)
        scale[t] = jnp.where(row_id == q, inv, scale[t])
        if j + 1 < BASE:
            tn, qn = divmod(j + 1, SUB)
            near = sub_bcast(cols[tn][j], qn) * inv
            pivot = sub_bcast(cols[tn][j + 1], qn) - near * near
        below = cols[1][j] * inv
        here = cols[0][j] * inv if t == 0 else None
        for n in range(j + 1, BASE):
            tn, qn = divmod(n, SUB)
            other = sub_bcast(cols[tn][j], qn) * inv
            if t == 0 and tn == 0:
                cols[0][n] = cols[0][n] - here * other
            cols[1][n] = cols[1][n] - below * other
        masked = jnp.where(row_id > q, here if t == 0 else below, 0.0)
        for v in range(len(rows[0])):
            pivot_row = sub_bcast(rows[t][v], q) * inv
            rows[t][v] = rows[t][v] - masked * pivot_row
            if t == 0:
                rows[1][v] = rows[1][v] - below * pivot_row
    return [[x * scale[t] for x in rows[t]] for t in range(2)]


def factor_block(work, winv, prev):
    size = work.shape[1]
    prev[...] = jnp.zeros(prev.shape, F32)
    for half in range(size // LANE):
        views = [(work, 0), (work, 1), (winv, 0)] if half == 0 else [(work, 1), (winv, 0), (winv, 1)]
        first = half * LANE
        if half == 1:
            mid_part, inv_part = prev[:, LANE : 2 * LANE], prev[:, 2 * LANE :]
            prev[:, :LANE] = mid_part
            prev[:, LANE : 2 * LANE] = inv_part
            prev[:, 2 * LANE :] = jnp.zeros((BASE, LANE), F32)

        def body(s, carry, views=views, first=first):
            lane0 = s * BASE
            row0 = pl.multiple_of(first + lane0, BASE)

            def rows_at(row, t):
                return pl.ds(pl.multiple_of(row + SUB * t, SUB), SUB)

            rows = [[ref[rows_at(row0, t), LANE * g : LANE * (g + 1)] for ref, g in views] for t in range(2)]
            hi, mid, lo = split3(prev[...])
            lane = lax.broadcasted_iota(jnp.int32, (BASE, size - first), 1) + first
            after = lane >= row0 + BASE
            lhi, lmid, llo = [jnp.where(after, x[:, : size - first], jnp.zeros((), BF16)) for x in (hi, mid, lo)]
            update = lax.dot_general(
                jnp.concatenate([lhi, lhi, lmid, lhi, llo, lmid], axis=0),
                jnp.concatenate([hi, mid, hi, lo, hi, mid], axis=0),
                (((0,), (0,)), ((), ())),
                preferred_element_type=F32,
            )
            for v, (ref, g) in enumerate(views):
                ref[first:size, LANE * g : LANE * (g + 1)] -= update[:, LANE * v : LANE * (v + 1)]
            done = eliminate(rows, lane0)
            for t in range(2):
                for v, (ref, g) in enumerate(views):
                    ref[rows_at(row0, t), LANE * g : LANE * (g + 1)] = done[t][v]
                    prev[SUB * t : SUB * (t + 1), LANE * v : LANE * (v + 1)] = done[t][v]
            if first == 0:
                source = [jnp.where(s == LANE // BASE - 1, done[t][1], done[t][0]) for t in range(2)]
            else:
                source = [done[t][0] for t in range(2)]
            next_lane = (lane0 + BASE) % LANE
            for t in range(2):
                factor = [[lane_bcast(source[m], next_lane + SUB * t + n) for n in range(SUB)] for m in range(2)]
                for v, (ref, g) in enumerate(views):
                    parts = [factor[0][n] * done[0][v] + factor[1][n] * done[1][v] for n in range(SUB)]
                    ref[rows_at(row0 + BASE, t), LANE * g : LANE * (g + 1)] -= stack_sums(parts)
            return carry

        lax.fori_loop(0, LANE // BASE, body, 0)


def kernel(n_row, n_col, batch_axis, a_ref, o_ref, share, diag, edge, stage, first, panel, work, winv, winv3, prev, load_sem, store_sem,
           seed_send, seed_recv, edge_send, edge_recv, first_sem, send_sem, pass_sem, recv_sem):
    row_blocks, size, local_cols = a_ref.shape
    col_blocks = local_cols // size
    ratio = n_col // n_row
    steps = row_blocks * n_row
    depth = pass_sem.shape[0]
    batch = lax.axis_index(batch_axis)
    row = lax.axis_index("row")
    col = lax.axis_index("col")
    odd = lax.rem(col, 2)
    on_diag = lax.rem(col, n_row) == row
    row_slots = n_row * (row_blocks * (row_blocks + 1) // 2)
    edge_slots = row_slots + n_col * (col_blocks * (col_blocks + 1) // 2)
    leads = row == LEAD

    def at(dev_row, dev_col):
        return (batch, dev_row, dev_col)

    def row_slot(k, a):
        g = k // n_row
        return n_row * (row_blocks * g - (g * (g - 1)) // 2) + (k - g * n_row) * (row_blocks - g) + a - g

    def col_slot(k, b):
        h = k // n_col
        return row_slots + n_col * (col_blocks * h - (h * (h - 1)) // 2) + (k - h * n_col) * (col_blocks - h) + b - h

    def first_a(k):
        return (k + n_row - row) // n_row

    def first_b(k):
        return (k + n_col - col) // n_col

    def home(ref, a, b):
        return ref.at[a, :, pl.ds(pl.multiple_of(b * size, size), size)]

    def spot(a, b):
        return b * row_blocks + a

    def col_of(k, b):
        return jnp.where(on_diag, row_slot(k, ratio * b + col // n_row), col_slot(k, b))

    def edge_slot(k, j):
        return edge_slots + 2 * k + (j - k - 1) // n_col

    def edge_reach(ahead):
        return jnp.logical_and(ahead >= 2, jnp.logical_and(ahead <= n_col + LAG, row != LEAD))

    def copy(src_slot, dst_slot, sem, device):
        return pltpu.make_async_remote_copy(
            src_ref=panel.at[src_slot], dst_ref=panel.at[dst_slot], send_sem=sem, recv_sem=recv_sem.at[dst_slot],
            device_id=device, device_id_type=MESH,
        )

    def arrived(slot):
        copy(slot, slot, send_sem.at[0, 0], at(row, col)).wait_recv()

    def start(c):
        c.start()

    def finish(c):
        c.wait_send()

    def to_lead(ahead):
        return jnp.logical_and(jnp.logical_and(ahead >= 2, ahead <= n_row), row != LEAD)

    def down_column(k, a, sems, act):
        i = a * n_row + row
        slot = row_slot(k, a)
        dst = col_slot(k, i // n_col)
        for m, d in enumerate((1, n_row - 1, 2)):
            there = lax.rem(row + d, n_row)

            @pl.when(jnp.logical_not(jnp.logical_and(there == LEAD, to_lead(i - k))))
            def _():
                act(copy(slot, dst, sems[m], at(there, col)))

    def to_edge(k, a, sem, act):
        i = a * n_row + row
        act(copy(row_slot(k, a), edge_slot(k, i - 1), sem, at(LEAD, lax.rem(i - 1, n_col))))

    def source_sends(k, a, act):
        ahead = a * n_row + row - k
        slot = row_slot(k, a)
        early = n_row

        @pl.when(jnp.logical_and(edge_reach(ahead), jnp.logical_or(ahead <= early, ahead == n_col)))
        def _():
            to_edge(k, a, send_sem.at[a, 5], act)

        @pl.when(to_lead(ahead))
        def _():
            act(copy(slot, col_slot(k, (k + ahead) // n_col), send_sem.at[a, 0], at(LEAD, lax.rem(k + ahead, n_col))))

        @pl.when(lax.rem(ahead, n_col) == 0)
        def _():
            down_column(k, a, [send_sem.at[a, m] for m in range(3)], act)

        @pl.when(jnp.logical_or(jnp.logical_and(odd == 0, ahead >= 2), ahead >= n_col - 1))
        def _():
            act(copy(slot, slot, send_sem.at[a, 3], at(row, lax.rem(jnp.where(odd == 0, col + 1, col - 1), n_col))))

        @pl.when(jnp.logical_and(odd == 1, ahead >= 2))
        def _():
            act(copy(slot, slot, send_sem.at[a, 6], at(row, lax.rem(col + 1, n_col))))

        @pl.when(ahead >= 2)
        def _():
            act(copy(slot, slot, send_sem.at[a, 4], at(row, lax.rem(col - odd + 3, n_col))))

        @pl.when(jnp.logical_and(odd == 1, jnp.logical_and(ahead >= n_col // 2 - 1, ahead < n_col - 3)))
        def _():
            act(copy(slot, slot, send_sem.at[a, 7], at(row, lax.rem(col + n_col // 2, n_col))))

        @pl.when(ahead >= n_col - 2 - odd)
        def _():
            act(copy(slot, slot, send_sem.at[a, 8], at(row, lax.rem(col - odd - 1 + n_col, n_col))))

    def lead(p):
        return lax.rem(col - lax.rem(p, n_col) + n_col, n_col)

    def hops(p):
        return lax.rem(col // 2 - lax.rem(p, n_col) // 2 + n_col // 2, n_col // 2)

    def passes(p):
        return jnp.logical_and(odd == 1, hops(p) != 0)

    def first_passed(p):
        low = jnp.where(passes(p), jnp.maximum(lead(p) - 1, 2), lead(p))
        return (p + low - row + n_row - 1) // n_row

    def pass_on(p, a, act):
        i = a * n_row + row
        ahead = i - p
        slot = row_slot(p, a)
        sems = pass_sem.at[lax.rem(p, depth), a]
        src_odd = lax.rem(p, 2)
        far = n_col - 2 - src_odd

        @pl.when(passes(p))
        def _():
            h = hops(p)
            via_prev = jnp.logical_or(src_odd == 1, jnp.logical_and(lax.rem(a, 2) == 1, ahead >= far))
            mine_to_pass = jnp.logical_or(
                jnp.logical_and(h == 1, jnp.logical_not(via_prev)), jnp.logical_and(h == n_col // 2 - 1, via_prev)
            )

            @pl.when(jnp.logical_and(mine_to_pass, ahead >= n_col // 2 - src_odd))
            def _():
                act(copy(slot, slot, sems.at[4], at(row, lax.rem(jnp.where(h == 1, col + 2, col - 2 + n_col), n_col))))

            @pl.when(jnp.logical_or(src_odd == 0, h != 1))
            def _():
                act(copy(slot, slot, sems.at[3], at(row, col - 1)))

        own = lax.rem(i, n_col) == col

        @pl.when(jnp.logical_and(own, jnp.logical_and(ahead > n_row, edge_reach(ahead))))
        def _():
            to_edge(p, a, sems.at[5], act)

        @pl.when(jnp.logical_and(own, ahead > 1))
        def _():
            down_column(p, a, [sems.at[m] for m in range(3)], act)

    def passed(p):
        @pl.when(lead(p) != 0)
        def _():
            loop(first_passed(p), row_blocks, lambda a: pass_on(p, a, finish))

    def receive(p, a):
        arrived(row_slot(p, a))
        pass_on(p, a, start)

    def loop(lo, hi, fn):
        lax.fori_loop(lo, hi, lambda n, c: (fn(n), c)[1], 0)

    for a in range(row_blocks):
        for b in range(col_blocks):
            pltpu.make_async_copy(home(a_ref, a, b), share.at[spot(a, b)], load_sem).start()

    barrier = pltpu.get_barrier_semaphore()
    n_dev = n_row * n_col

    def greet(n):
        other = lax.rem(row * n_col + col + n, n_dev)
        pl.semaphore_signal(barrier, inc=1, device_id=at(other // n_col, lax.rem(other, n_col)), device_id_type=MESH)

    loop(1, n_dev, greet)
    with jax.named_scope("all_here"):
        pl.semaphore_wait(barrier, n_dev - 1)
    with jax.named_scope("loaded"):
        pltpu.make_async_copy(share, share, load_sem).wait()

    def seed_copy(b, dev_row):
        return pltpu.make_async_remote_copy(
            src_ref=share.at[spot(ratio * b + col // n_row, b)], dst_ref=diag.at[b],
            send_sem=seed_send.at[b, lax.rem(dev_row - row + n_row, n_row)],
            recv_sem=seed_recv.at[b], device_id=at(dev_row, col), device_id_type=MESH,
        )

    def hand_out(b):
        @pl.when(on_diag)
        def _():
            for d in (1, n_row - 1, 2):
                seed_copy(b, lax.rem(row + d, n_row)).start()
            diag[b] = share[spot(ratio * b + col // n_row, b)]

        @pl.when(jnp.logical_and(holds_edge(b), jnp.logical_not(leads)))
        def _():
            stage[b] = share[spot((b * n_col + col + 1) // n_row, b)]
            edge_copy(b).start()

    def holds_edge(b):
        j = b * n_col + col
        return jnp.logical_and(lax.rem(j + 1, n_row) == row, j + 1 < steps)

    def edge_copy(b):
        return pltpu.make_async_remote_copy(
            src_ref=stage.at[b], dst_ref=edge.at[b], send_sem=edge_send.at[b], recv_sem=edge_recv.at[b],
            device_id=at(LEAD, col), device_id_type=MESH,
        )

    def has_edge(b):
        from_other = jnp.logical_and(leads, lax.rem(col + 1, n_row) != LEAD)
        return jnp.logical_and(from_other, b * n_col + col + 1 < steps)

    def edge_seeded(b):
        @pl.when(has_edge(b))
        def _():
            edge_copy(b).wait_recv()

    def edge_arrived(p, b):
        j = b * n_col + col

        @pl.when(jnp.logical_and(has_edge(b), j + 1 - p <= n_col + LAG))
        def _():
            arrived(edge_slot(p, j))

    hand_out(0)

    def seed_arrived(b):
        @pl.when(jnp.logical_not(on_diag))
        def _():
            seed_copy(b, row).wait_recv()

    with jax.named_scope("seed"):
        seed_arrived(0)

        @pl.when(col != 0)
        def _():
            edge_seeded(0)

    def clear(n):
        a, b = lax.rem(n, row_blocks), n // row_blocks

        @pl.when(a * n_row + row < b * n_col + col)
        def _():
            share[n] = jnp.zeros((size, size), F32)
            pltpu.make_async_copy(share.at[n], home(o_ref, a, b), store_sem).start()

    loop(0, row_blocks * col_blocks, clear)

    def times_t(x, y):
        return lax.dot_general(x, y, (((1,), (1,)), ((), ())), preferred_element_type=F32)

    def update_block(p, a, b):
        share[spot(a, b)] -= times_t(panel[row_slot(p, a)], panel[col_of(p, b)])

    def update_diag(p, b):
        other = panel[col_of(p, b)]
        diag[b] -= times_t(other, other)

    def update_edge(p, b):
        @pl.when(has_edge(b))
        def _():
            edge[b] -= times_t(panel[edge_slot(p, b * n_col + col)], panel[col_of(p, b)])

    def column_arrived(p, b):
        @pl.when(jnp.logical_not(on_diag))
        def _():
            arrived(col_slot(p, b))

    def update_column(p, b, lo):
        lone = lax.rem(row_blocks - lo, 2)

        @pl.when(lone == 1)
        def _():
            update_block(p, lo, b)

        def pair(m):
            a = lo + lone + 2 * m
            both = pl.ds(spot(a, b), 2)
            left = panel[pl.ds(row_slot(p, a), 2)].reshape(2 * size, size)
            share[both] -= times_t(left, panel[col_of(p, b)]).reshape(2, size, size)

        loop(0, (row_blocks - lo) // 2, pair)

    def trail(p, b_from, near):
        loop(b_from, col_blocks, lambda b: update_column(p, b, first_a(b * n_col + col - jnp.where(b == near, 0, 1))))

    def columns_arrived(p, b_from):
        def one(b):
            column_arrived(p, b)
            edge_arrived(p, b)

        loop(b_from, col_blocks, one)

    def prepare(b):
        work[size:, :] = jnp.zeros((BASE, size), F32)
        r_id = lax.broadcasted_iota(jnp.int32, (size + BASE, size), 0)
        c_id = lax.broadcasted_iota(jnp.int32, (size + BASE, size), 1)
        winv[...] = jnp.where(r_id == c_id, 1.0, 0.0).astype(F32)

    def times_winv_t(x):
        hi, mid, lo = split3(x)
        whi, wmid, wlo = winv3[0], winv3[1], winv3[2]
        small = times_t(lo, whi) + times_t(mid, wmid) + times_t(hi, wlo)
        return small + (times_t(mid, whi) + times_t(hi, wmid)) + times_t(hi, whi)

    def solve(k, a, count, near):
        kb = k // n_col
        here = pl.ds(spot(a, kb), count)

        def apply(p):
            left = panel[pl.ds(row_slot(p, a), count)].reshape(count * size, size)
            share[here] -= times_t(left, panel[col_of(p, kb)]).reshape(count, size, size)

        if not near:

            @pl.when(k > 1)
            def _():
                for m in range(count):
                    receive(k - 2, a + m)

            loop(jnp.maximum(k - 1 - LAG, 0), k - 1, apply)

        @pl.when(k > 0)
        def _():
            for m in range(count):
                receive(k - 1, a + m)
            apply(k - 1)

        x = times_winv_t(share[here].reshape(count * size, size)).reshape(count, size, size)
        panel[pl.ds(row_slot(k, a), count)] = x.astype(BF16)
        share[here] = x
        if near:

            @pl.when(jnp.logical_and(leads, lax.rem(k + 1, n_row) == LEAD))
            def _():
                first[...] = panel[row_slot(k, a)]
                first_out(k, start)

        for m in range(count):
            source_sends(k, a + m, start)
        for m in range(count):
            pltpu.make_async_copy(share.at[spot(a + m, kb)], home(o_ref, a + m, kb), store_sem).start()

    def update_near(p, b):
        update_diag(p, b)
        update_edge(p, b)

    def first_slot(k, dev_row):
        return jnp.where(lax.rem(k + 1, n_row) == dev_row, row_slot(k, (k + 1) // n_row), col_slot(k, (k + 1) // n_col))

    def first_copy(k, dev_row, sem):
        dst = first_slot(k, dev_row)
        return pltpu.make_async_remote_copy(
            src_ref=first, dst_ref=panel.at[dst], send_sem=sem, recv_sem=recv_sem.at[dst],
            device_id=at(dev_row, lax.rem(col + 1, n_col)), device_id_type=MESH,
        )

    def others_first(k, fn):
        urgent = lax.rem(k + 3, n_row)
        lone = urgent == LEAD
        for m in range(n_row - 1):
            fn(m, lax.rem(jnp.where(lone, LEAD + 1, urgent) + m + jnp.where(lax.rem(jnp.where(lone, LEAD + 1, urgent) - LEAD + n_row, n_row) + m >= n_row, 1, 0), n_row))

    def first_out(k, act):
        act(first_copy(k, LEAD, first_sem.at[0, 0]))

        @pl.when(odd == 0)
        def _():
            others_first(k, lambda m, r: act(first_copy(k, r, first_sem.at[0, 1 + m])))

    def first_down(k, act):
        @pl.when(odd == 0)
        def _():
            others_first(k, lambda m, r: act(copy(first_slot(k, LEAD), first_slot(k, r), first_sem.at[1, 1 + m], at(r, col))))

    def firsts_done(k):
        @pl.when(jnp.logical_and(leads, k + 1 < steps))
        def _():
            first_out(k, finish)

        @pl.when(jnp.logical_and(leads, k > 0))
        def _():
            first_down(k - 1, finish)

    @pl.when(col == 0)
    def _():
        prepare(0)
        work[0:size, :] = diag[0]

    def step(k):
        mine = col == lax.rem(k, n_col)
        kb = k // n_col
        last = k - 1
        soon = jnp.logical_and(col == lax.rem(k + 1, n_col), k + 1 < steps)

        @pl.when(mine)
        def _():
            with jax.named_scope("factor"):
                factor_block(work, winv, prev)
            for n, part in enumerate(split3(winv[0:size, :])):
                winv3[n] = part

            @pl.when(has_edge(kb))
            def _():
                with jax.named_scope("lead"):

                    @pl.when(k == 0)
                    def _():
                        edge_seeded(kb)

                    @pl.when(k > 0)
                    def _():
                        edge_arrived(last, kb)
                        update_edge(last, kb)

                    first[...] = times_winv_t(edge[kb]).astype(BF16)
                    first_out(k, start)

            lo = first_a(k)
            second = jnp.minimum(lo + 1, row_blocks)
            with jax.named_scope("solve_near"):
                loop(lo, second, lambda a: solve(k, a, 1, True))
            with jax.named_scope("solve_one"):
                third = second + lax.rem(row_blocks - second, 2)
                loop(second, third, lambda a: solve(k, a, 1, False))
            with jax.named_scope("solve_two"):
                loop(0, (row_blocks - third) // 2, lambda m: solve(k, third + 2 * m, 2, False))

        @pl.when(k >= depth)
        def _():
            with jax.named_scope("passed"):
                passed(k - depth)

        @pl.when(mine)
        def _():
            @pl.when(row == lax.rem(k, n_row))
            def _():
                for d in range(1, n_row):
                    seed_copy(kb, lax.rem(row + d, n_row)).wait_send()
                r_id = lax.broadcasted_iota(jnp.int32, (size, size), 0)
                c_id = lax.broadcasted_iota(jnp.int32, (size, size), 1)
                n = spot(k // n_row, kb)
                share[n] = jnp.where(r_id >= c_id, work[0:size, :].T, 0.0)
                pltpu.make_async_copy(share.at[n], home(o_ref, k // n_row, kb), store_sem).start()

            with jax.named_scope("late_trail"):

                def late(p):
                    columns_arrived(p, kb + 1)
                    trail(p, kb + 1, -1)

                loop(jnp.maximum(k - 1 - LAG, 0), k - LAG + 1, late)

            @pl.when(kb + 1 < col_blocks)
            def _():
                hand_out(kb + 1)

        @pl.when(jnp.logical_and(k > 0, jnp.logical_not(jnp.logical_or(mine, soon))))
        def _():
            @pl.when(col != lax.rem(last, n_col))
            def _():
                with jax.named_scope("receive"):
                    loop(first_passed(last), row_blocks, lambda a: receive(last, a))

            @pl.when(k >= LAG)
            def _():
                p = k - LAG
                near = first_b(k)
                with jax.named_scope("columns"):
                    columns_arrived(p, near)

                @pl.when(near < col_blocks)
                def _():
                    age = k + n_col - (near * n_col + col)

                    @pl.when(jnp.logical_and(age == 3, near > 0))
                    def _():
                        with jax.named_scope("seed_late"):
                            seed_arrived(near)
                            edge_seeded(near)

                    @pl.when(age >= 3)
                    def _():
                        oldest = jnp.where(age == 3, jnp.maximum(p - 2, 0), p)
                        loop(oldest, p + 1, lambda q: update_near(q, near))

                with jax.named_scope("trail"):
                    trail(p, near, near)

        @pl.when(soon)
        def _():
            nb = (k + 1) // n_col

            oldest = jnp.maximum(k - LAG, 0)

            def old_diag(p):
                column_arrived(p, nb)
                edge_arrived(p, nb)
                update_near(p, nb)

            def take(a):
                receive(last, a)

                @pl.when(a * n_row + row > k + 1)
                def _():
                    loop(oldest, last, lambda p: update_block(p, a, nb))

            @pl.when(k > 0)
            def _():
                with jax.named_scope("old_diag"):
                    loop(oldest, last, old_diag)
                with jax.named_scope("take"):
                    loop(first_a(k), jnp.minimum(first_a(k + 1) + 1, row_blocks), take)
                with jax.named_scope("take_column"):
                    column_arrived(last, nb)
                    edge_arrived(last, nb)
                with jax.named_scope("catch_up"):
                    update_near(last, nb)
                    loop(first_a(k + 1), jnp.minimum(first_a(k + 1) + 1, row_blocks), lambda a: update_block(last, a, nb))

            prepare(nb)
            slot = col_of(k, nb)
            with jax.named_scope("first_block"):
                arrived(slot)

            @pl.when(leads)
            def _():
                first_down(k, start)

            other = panel[slot]
            work[0:size, :] = diag[nb] - times_t(other, other)

        @pl.when(jnp.logical_and(k >= n_col // 2, col == lax.rem(k + n_col // 2, n_col)))
        def _():
            with jax.named_scope("sends_done"):
                firsts_done(k - n_col // 2)
                loop(first_a(k - n_col // 2), row_blocks, lambda a: source_sends(k - n_col // 2, a, finish))

    loop(0, steps, step)

    loop(steps - depth, steps, passed)

    def last_sends(k):
        @pl.when(col == lax.rem(k, n_col))
        def _():
            firsts_done(k)
            loop(first_a(k), row_blocks, lambda a: source_sends(k, a, finish))

    loop(steps - n_col // 2, steps, last_sends)

    def edges_done(b):
        @pl.when(jnp.logical_and(holds_edge(b), jnp.logical_not(leads)))
        def _():
            edge_copy(b).wait_send()

    loop(0, col_blocks, edges_done)
    with jax.named_scope("stored"):
        pltpu.make_async_copy(share, share, store_sem).wait()


def solution(mesh):
    n_row = mesh.shape["row"]
    n_col = mesh.shape["col"]

    def factor_local(a_loc):
        row_blocks, size, local_cols = a_loc.shape
        col_blocks = local_cols // size
        slots = n_row * (row_blocks * (row_blocks + 1) // 2) + n_col * (col_blocks * (col_blocks + 1) // 2)
        slots += 2 * row_blocks * n_row
        return pl.pallas_call(
            functools.partial(kernel, n_row, n_col, "batch"),
            out_shape=jax.ShapeDtypeStruct(a_loc.shape, F32),
            in_specs=[pl.BlockSpec(memory_space=pl.ANY)],
            out_specs=pl.BlockSpec(memory_space=pl.ANY),
            scratch_shapes=[
                pltpu.VMEM((row_blocks * col_blocks, size, size), F32),
                pltpu.VMEM((col_blocks, size, size), F32),
                pltpu.VMEM((col_blocks, size, size), F32),
                pltpu.VMEM((col_blocks, size, size), F32),
                pltpu.VMEM((size, size), BF16),
                pltpu.VMEM((slots, size, size), BF16),
                pltpu.VMEM((size + BASE, size), F32),
                pltpu.VMEM((size + BASE, size), F32),
                pltpu.VMEM((3, size, size), BF16),
                pltpu.VMEM((BASE, 3 * LANE), F32),
                pltpu.SemaphoreType.DMA,
                pltpu.SemaphoreType.DMA,
                pltpu.SemaphoreType.DMA((col_blocks, n_row)),
                pltpu.SemaphoreType.DMA((col_blocks,)),
                pltpu.SemaphoreType.DMA((col_blocks,)),
                pltpu.SemaphoreType.DMA((col_blocks,)),
                pltpu.SemaphoreType.DMA((2, n_row)),
                pltpu.SemaphoreType.DMA((row_blocks, 9)),
                pltpu.SemaphoreType.DMA((4, row_blocks, 6)),
                pltpu.SemaphoreType.DMA((slots,)),
            ],
            compiler_params=pltpu.CompilerParams(
                collective_id=0, has_side_effects=True, vmem_limit_bytes=60 * 1024 * 1024
            ),
            name="cholesky",
        )(a_loc)

    blk_spec = P(("batch", "row"), None, "col")
    return jax.shard_map(factor_local, mesh=mesh, in_specs=(blk_spec,), out_specs=blk_spec, check_vma=False)
```

```python
import functools

import jax
import jax.numpy as jnp
from jax import lax
from jax.experimental import pallas as pl
from jax.experimental.pallas import tpu as pltpu
from jax.sharding import PartitionSpec as P

F32 = jnp.float32
BF16 = jnp.bfloat16
MESH = pl.DeviceIdType.MESH
SUB = 8
LANE = 128
BASE = 16
LEAD = 1
SENT = 6
LAG = 3


def sub_bcast(x, q):
    return jnp.broadcast_to(x[q : q + 1, :], (SUB, LANE))


def lane_bcast(x, lane):
    return jnp.take_along_axis(x, jnp.full((SUB, LANE), lane, jnp.int32), axis=1)


def split3(x):
    high = x.astype(BF16)
    rest = x - high.astype(F32)
    mid = rest.astype(BF16)
    return high, mid, (rest - mid.astype(F32)).astype(BF16)


def swap_rows(x, bit, row_id):
    if bit == SUB // 2:
        return pltpu.roll(x, bit, 0)
    return jnp.where((row_id & bit) == 0, pltpu.roll(x, SUB - bit, 0), pltpu.roll(x, bit, 0))


def stack_sums(parts):
    row_id = lax.broadcasted_iota(jnp.int32, (SUB, LANE), 0)
    for bit in (4, 2, 1):
        low = (row_id & bit) == 0
        half = len(parts) // 2
        parts = [
            jnp.where(low, parts[n], parts[n + half]) + swap_rows(jnp.where(low, parts[n + half], parts[n]), bit, row_id)
            for n in range(half)
        ]
    return parts[0]


def eliminate(rows, lane0):
    row_id = lax.broadcasted_iota(jnp.int32, (SUB, LANE), 0)
    rows = [list(rows[0]), list(rows[1])]
    cols = [
        [lane_bcast(rows[0][0], lane0 + j) for j in range(SUB)],
        [lane_bcast(rows[1][0], lane0 + j) for j in range(BASE)],
    ]
    scale = [jnp.zeros((SUB, LANE), F32), jnp.zeros((SUB, LANE), F32)]
    pivot = sub_bcast(cols[0][0], 0)
    for j in range(BASE):
        t, q = divmod(j, SUB)
        inv = lax.rsqrt(pivot)
        scale[t] = jnp.where(row_id == q, inv, scale[t])
        if j + 1 < BASE:
            tn, qn = divmod(j + 1, SUB)
            near = sub_bcast(cols[tn][j], qn) * inv
            pivot = sub_bcast(cols[tn][j + 1], qn) - near * near
        below = cols[1][j] * inv
        here = cols[0][j] * inv if t == 0 else None
        for n in range(j + 1, BASE):
            tn, qn = divmod(n, SUB)
            other = sub_bcast(cols[tn][j], qn) * inv
            if t == 0 and tn == 0:
                cols[0][n] = cols[0][n] - here * other
            cols[1][n] = cols[1][n] - below * other
        masked = jnp.where(row_id > q, here if t == 0 else below, 0.0)
        for v in range(len(rows[0])):
            pivot_row = sub_bcast(rows[t][v], q) * inv
            rows[t][v] = rows[t][v] - masked * pivot_row
            if t == 0:
                rows[1][v] = rows[1][v] - below * pivot_row
    return [[x * scale[t] for x in rows[t]] for t in range(2)]


def factor_block(work, winv, prev):
    size = work.shape[1]
    prev[...] = jnp.zeros(prev.shape, F32)
    for half in range(size // LANE):
        views = [(work, 0), (work, 1), (winv, 0)] if half == 0 else [(work, 1), (winv, 0), (winv, 1)]
        first = half * LANE
        if half == 1:
            mid_part, inv_part = prev[:, LANE : 2 * LANE], prev[:, 2 * LANE :]
            prev[:, :LANE] = mid_part
            prev[:, LANE : 2 * LANE] = inv_part
            prev[:, 2 * LANE :] = jnp.zeros((BASE, LANE), F32)

        def body(s, carry, views=views, first=first):
            lane0 = s * BASE
            row0 = pl.multiple_of(first + lane0, BASE)

            def rows_at(row, t):
                return pl.ds(pl.multiple_of(row + SUB * t, SUB), SUB)

            rows = [[ref[rows_at(row0, t), LANE * g : LANE * (g + 1)] for ref, g in views] for t in range(2)]
            hi, mid, lo = split3(prev[...])
            lane = lax.broadcasted_iota(jnp.int32, (BASE, size - first), 1) + first
            after = lane >= row0 + BASE
            lhi, lmid, llo = [jnp.where(after, x[:, : size - first], jnp.zeros((), BF16)) for x in (hi, mid, lo)]
            update = lax.dot_general(
                jnp.concatenate([lhi, lhi, lmid, lhi, llo, lmid], axis=0),
                jnp.concatenate([hi, mid, hi, lo, hi, mid], axis=0),
                (((0,), (0,)), ((), ())),
                preferred_element_type=F32,
            )
            for v, (ref, g) in enumerate(views):
                ref[first:size, LANE * g : LANE * (g + 1)] -= update[:, LANE * v : LANE * (v + 1)]
            done = eliminate(rows, lane0)
            for t in range(2):
                for v, (ref, g) in enumerate(views):
                    ref[rows_at(row0, t), LANE * g : LANE * (g + 1)] = done[t][v]
                    prev[SUB * t : SUB * (t + 1), LANE * v : LANE * (v + 1)] = done[t][v]
            if first == 0:
                source = [jnp.where(s == LANE // BASE - 1, done[t][1], done[t][0]) for t in range(2)]
            else:
                source = [done[t][0] for t in range(2)]
            next_lane = (lane0 + BASE) % LANE
            for t in range(2):
                factor = [[lane_bcast(source[m], next_lane + SUB * t + n) for n in range(SUB)] for m in range(2)]
                for v, (ref, g) in enumerate(views):
                    parts = [factor[0][n] * done[0][v] + factor[1][n] * done[1][v] for n in range(SUB)]
                    ref[rows_at(row0 + BASE, t), LANE * g : LANE * (g + 1)] -= stack_sums(parts)
            return carry

        lax.fori_loop(0, LANE // BASE, body, 0)


def kernel(n_row, n_col, batch_axis, a_ref, o_ref, share, diag, edge, stage, first, panel, work, winv, winv3, prev, load_sem, store_sem,
           seed_send, seed_recv, edge_send, edge_recv, first_sem, send_sem, pass_sem, down_sem, recv_sem):
    row_blocks, size, local_cols = a_ref.shape
    col_blocks = local_cols // size
    ratio = n_col // n_row
    steps = row_blocks * n_row
    depth = pass_sem.shape[0]
    batch = lax.axis_index(batch_axis)
    row = lax.axis_index("row")
    col = lax.axis_index("col")
    odd = lax.rem(col, 2)
    on_diag = lax.rem(col, n_row) == row
    row_slots = n_row * (row_blocks * (row_blocks + 1) // 2)
    edge_slots = row_slots + n_col * (col_blocks * (col_blocks + 1) // 2)
    leads = row == LEAD

    def at(dev_row, dev_col):
        return (batch, dev_row, dev_col)

    def row_slot(k, a):
        g = k // n_row
        return n_row * (row_blocks * g - (g * (g - 1)) // 2) + (k - g * n_row) * (row_blocks - g) + a - g

    def col_slot(k, b):
        h = k // n_col
        return row_slots + n_col * (col_blocks * h - (h * (h - 1)) // 2) + (k - h * n_col) * (col_blocks - h) + b - h

    def first_a(k):
        return (k + n_row - row) // n_row

    def first_b(k):
        return (k + n_col - col) // n_col

    def home(ref, a, b):
        return ref.at[a, :, pl.ds(pl.multiple_of(b * size, size), size)]

    def spot(a, b):
        return b * row_blocks + a

    def col_of(k, b):
        return jnp.where(on_diag, row_slot(k, ratio * b + col // n_row), col_slot(k, b))

    def edge_slot(k, j):
        return edge_slots + 2 * k + (j - k - 1) // n_col

    def edge_reach(ahead):
        return jnp.logical_and(ahead >= 2, jnp.logical_and(ahead <= n_col + LAG, row != LEAD))

    def copy(src_slot, dst_slot, sem, device):
        return pltpu.make_async_remote_copy(
            src_ref=panel.at[src_slot], dst_ref=panel.at[dst_slot], send_sem=sem, recv_sem=recv_sem.at[dst_slot],
            device_id=device, device_id_type=MESH,
        )

    def arrived(slot):
        copy(slot, slot, send_sem.at[0, 0], at(row, col)).wait_recv()

    def start(c):
        c.start()

    def finish(c):
        c.wait_send()

    def to_lead(ahead):
        return jnp.logical_and(jnp.logical_and(ahead >= 2, ahead <= n_row), row != LEAD)

    def down_column(k, a, sems, act):
        i = a * n_row + row
        slot = row_slot(k, a)
        dst = col_slot(k, i // n_col)
        for m, d in enumerate((1, n_row - 1, 2)):
            there = lax.rem(row + d, n_row)

            @pl.when(jnp.logical_not(jnp.logical_and(there == LEAD, to_lead(i - k))))
            def _():
                act(copy(slot, dst, sems[m], at(there, col)))

    def to_edge(k, a, sem, act):
        i = a * n_row + row
        act(copy(row_slot(k, a), edge_slot(k, i - 1), sem, at(LEAD, lax.rem(i - 1, n_col))))

    def source_sends(k, a, act):
        ahead = a * n_row + row - k
        slot = row_slot(k, a)
        early = n_row

        @pl.when(jnp.logical_and(edge_reach(ahead), jnp.logical_or(ahead <= early, ahead == n_col)))
        def _():
            to_edge(k, a, send_sem.at[a, 5], act)

        @pl.when(to_lead(ahead))
        def _():
            act(copy(slot, col_slot(k, (k + ahead) // n_col), send_sem.at[a, 0], at(LEAD, lax.rem(k + ahead, n_col))))

        @pl.when(lax.rem(ahead, n_col) == 0)
        def _():
            down_column(k, a, [send_sem.at[a, m] for m in range(3)], act)

        @pl.when(jnp.logical_or(jnp.logical_and(odd == 0, ahead >= 2), ahead >= n_col - 1))
        def _():
            act(copy(slot, slot, send_sem.at[a, 3], at(row, lax.rem(jnp.where(odd == 0, col + 1, col - 1), n_col))))

        @pl.when(jnp.logical_and(odd == 1, ahead >= 2))
        def _():
            act(copy(slot, slot, send_sem.at[a, 6], at(row, lax.rem(col + 1, n_col))))

        @pl.when(ahead >= 2)
        def _():
            act(copy(slot, slot, send_sem.at[a, 4], at(row, lax.rem(col - odd + 3, n_col))))

        @pl.when(jnp.logical_and(odd == 1, jnp.logical_and(ahead >= n_col // 2 - 1, ahead < n_col - 3)))
        def _():
            act(copy(slot, slot, send_sem.at[a, 7], at(row, lax.rem(col + n_col // 2, n_col))))

        @pl.when(ahead >= n_col - 2 - odd)
        def _():
            act(copy(slot, slot, send_sem.at[a, 8], at(row, lax.rem(col - odd - 1 + n_col, n_col))))

    def lead(p):
        return lax.rem(col - lax.rem(p, n_col) + n_col, n_col)

    def hops(p):
        return lax.rem(col // 2 - lax.rem(p, n_col) // 2 + n_col // 2, n_col // 2)

    def passes(p):
        return jnp.logical_and(odd == 1, hops(p) != 0)

    def first_passed(p):
        low = jnp.where(passes(p), jnp.maximum(lead(p) - 1, 2), lead(p))
        return (p + low - row + n_row - 1) // n_row

    def pass_on(p, a, act):
        i = a * n_row + row
        ahead = i - p
        slot = row_slot(p, a)
        sems = pass_sem.at[lax.rem(p, depth), a]
        downs = down_sem.at[lax.rem(p, depth), i // n_col]
        src_odd = lax.rem(p, 2)
        far = n_col - 2 - src_odd

        @pl.when(passes(p))
        def _():
            h = hops(p)
            via_prev = jnp.logical_or(src_odd == 1, jnp.logical_and(lax.rem(a, 2) == 1, ahead >= far))
            mine_to_pass = jnp.logical_or(
                jnp.logical_and(h == 1, jnp.logical_not(via_prev)), jnp.logical_and(h == n_col // 2 - 1, via_prev)
            )

            @pl.when(jnp.logical_and(mine_to_pass, ahead >= n_col // 2 - src_odd))
            def _():
                act(copy(slot, slot, sems.at[1], at(row, lax.rem(jnp.where(h == 1, col + 2, col - 2 + n_col), n_col))))

            @pl.when(jnp.logical_or(src_odd == 0, h != 1))
            def _():
                act(copy(slot, slot, sems.at[0], at(row, col - 1)))

        own = lax.rem(i, n_col) == col

        @pl.when(jnp.logical_and(own, jnp.logical_and(ahead > n_row, edge_reach(ahead))))
        def _():
            to_edge(p, a, downs.at[3], act)

        @pl.when(jnp.logical_and(own, ahead > 1))
        def _():
            down_column(p, a, [downs.at[m] for m in range(3)], act)

    def passed(p):
        @pl.when(lead(p) != 0)
        def _():
            loop(first_passed(p), row_blocks, lambda a: pass_on(p, a, finish))

    def receive(p, a):
        arrived(row_slot(p, a))
        pass_on(p, a, start)

    def last_near(p):
        return first_a(p + 2)

    def loop(lo, hi, fn):
        lax.fori_loop(lo, hi, lambda n, c: (fn(n), c)[1], 0)

    for a in range(row_blocks):
        for b in range(col_blocks):
            pltpu.make_async_copy(home(a_ref, a, b), share.at[spot(a, b)], load_sem).start()

    barrier = pltpu.get_barrier_semaphore()
    n_dev = n_row * n_col

    def greet(n):
        other = lax.rem(row * n_col + col + n, n_dev)
        pl.semaphore_signal(barrier, inc=1, device_id=at(other // n_col, lax.rem(other, n_col)), device_id_type=MESH)

    loop(1, n_dev, greet)
    with jax.named_scope("all_here"):
        pl.semaphore_wait(barrier, n_dev - 1)
    with jax.named_scope("loaded"):
        pltpu.make_async_copy(share, share, load_sem).wait()

    def seed_copy(b, dev_row):
        return pltpu.make_async_remote_copy(
            src_ref=share.at[spot(ratio * b + col // n_row, b)], dst_ref=diag.at[b],
            send_sem=seed_send.at[b, lax.rem(dev_row - row + n_row, n_row)],
            recv_sem=seed_recv.at[b], device_id=at(dev_row, col), device_id_type=MESH,
        )

    def hand_out(b):
        @pl.when(on_diag)
        def _():
            for d in (1, n_row - 1, 2):
                seed_copy(b, lax.rem(row + d, n_row)).start()
            diag[b] = share[spot(ratio * b + col // n_row, b)]

        @pl.when(jnp.logical_and(holds_edge(b), jnp.logical_not(leads)))
        def _():
            stage[b] = share[spot((b * n_col + col + 1) // n_row, b)]
            edge_copy(b).start()

    def holds_edge(b):
        j = b * n_col + col
        return jnp.logical_and(lax.rem(j + 1, n_row) == row, j + 1 < steps)

    def edge_copy(b):
        return pltpu.make_async_remote_copy(
            src_ref=stage.at[b], dst_ref=edge.at[b], send_sem=edge_send.at[b], recv_sem=edge_recv.at[b],
            device_id=at(LEAD, col), device_id_type=MESH,
        )

    def has_edge(b):
        from_other = jnp.logical_and(leads, lax.rem(col + 1, n_row) != LEAD)
        return jnp.logical_and(from_other, b * n_col + col + 1 < steps)

    def edge_seeded(b):
        @pl.when(has_edge(b))
        def _():
            edge_copy(b).wait_recv()

    def edge_arrived(p, b):
        j = b * n_col + col

        @pl.when(jnp.logical_and(has_edge(b), j + 1 - p <= n_col + LAG))
        def _():
            arrived(edge_slot(p, j))

    hand_out(0)

    def seed_arrived(b):
        @pl.when(jnp.logical_not(on_diag))
        def _():
            seed_copy(b, row).wait_recv()

    with jax.named_scope("seed"):
        seed_arrived(0)

        @pl.when(col != 0)
        def _():
            edge_seeded(0)

    def clear(n):
        a, b = lax.rem(n, row_blocks), n // row_blocks

        @pl.when(a * n_row + row < b * n_col + col)
        def _():
            share[n] = jnp.zeros((size, size), F32)
            pltpu.make_async_copy(share.at[n], home(o_ref, a, b), store_sem).start()

    loop(0, row_blocks * col_blocks, clear)

    def times_t(x, y):
        return lax.dot_general(x, y, (((1,), (1,)), ((), ())), preferred_element_type=F32)

    def update_block(p, a, b):
        share[spot(a, b)] -= times_t(panel[row_slot(p, a)], panel[col_of(p, b)])

    def update_diag(p, b):
        other = panel[col_of(p, b)]
        diag[b] -= times_t(other, other)

    def update_edge(p, b):
        @pl.when(has_edge(b))
        def _():
            edge[b] -= times_t(panel[edge_slot(p, b * n_col + col)], panel[col_of(p, b)])

    def column_arrived(p, b):
        @pl.when(jnp.logical_not(on_diag))
        def _():
            arrived(col_slot(p, b))

    def update_column(p, b, lo):
        lone = lax.rem(row_blocks - lo, 2)

        @pl.when(lone == 1)
        def _():
            update_block(p, lo, b)

        def pair(m):
            a = lo + lone + 2 * m
            both = pl.ds(spot(a, b), 2)
            left = panel[pl.ds(row_slot(p, a), 2)].reshape(2 * size, size)
            share[both] -= times_t(left, panel[col_of(p, b)]).reshape(2, size, size)

        loop(0, (row_blocks - lo) // 2, pair)

    def trail(p, b_from, near):
        loop(b_from, col_blocks, lambda b: update_column(p, b, first_a(b * n_col + col - jnp.where(b == near, 0, 1))))

    def columns_arrived(p, b_from):
        def one(b):
            column_arrived(p, b)
            edge_arrived(p, b)

        loop(b_from, col_blocks, one)

    def prepare(b):
        work[size:, :] = jnp.zeros((BASE, size), F32)
        r_id = lax.broadcasted_iota(jnp.int32, (size + BASE, size), 0)
        c_id = lax.broadcasted_iota(jnp.int32, (size + BASE, size), 1)
        winv[...] = jnp.where(r_id == c_id, 1.0, 0.0).astype(F32)

    def times_winv_t(x):
        hi, mid, lo = split3(x)
        whi, wmid, wlo = winv3[0], winv3[1], winv3[2]
        small = times_t(lo, whi) + times_t(mid, wmid) + times_t(hi, wlo)
        return small + (times_t(mid, whi) + times_t(hi, wmid)) + times_t(hi, whi)

    def solve(k, a, count, near):
        kb = k // n_col
        here = pl.ds(spot(a, kb), count)

        def apply(p):
            left = panel[pl.ds(row_slot(p, a), count)].reshape(count * size, size)
            share[here] -= times_t(left, panel[col_of(p, kb)]).reshape(count, size, size)

        if not near:

            @pl.when(k > 1)
            def _():
                for m in range(count):
                    receive(k - 2, a + m)

            loop(jnp.maximum(k - 1 - LAG, 0), k - 1, apply)

        @pl.when(k > 0)
        def _():
            for m in range(count):
                receive(k - 1, a + m)
            apply(k - 1)

        x = times_winv_t(share[here].reshape(count * size, size)).reshape(count, size, size)
        panel[pl.ds(row_slot(k, a), count)] = x.astype(BF16)
        share[here] = x
        if near:

            @pl.when(jnp.logical_and(leads, lax.rem(k + 1, n_row) == LEAD))
            def _():
                first[...] = panel[row_slot(k, a)]
                first_out(k, start)

        for m in range(count):
            source_sends(k, a + m, start)
        for m in range(count):
            pltpu.make_async_copy(share.at[spot(a + m, kb)], home(o_ref, a + m, kb), store_sem).start()

    def update_near(p, b):
        update_diag(p, b)
        update_edge(p, b)

    def first_slot(k, dev_row):
        return jnp.where(lax.rem(k + 1, n_row) == dev_row, row_slot(k, (k + 1) // n_row), col_slot(k, (k + 1) // n_col))

    def first_copy(k, dev_row, sem):
        dst = first_slot(k, dev_row)
        return pltpu.make_async_remote_copy(
            src_ref=first, dst_ref=panel.at[dst], send_sem=sem, recv_sem=recv_sem.at[dst],
            device_id=at(dev_row, lax.rem(col + 1, n_col)), device_id_type=MESH,
        )

    def others_first(k, fn):
        urgent = lax.rem(k + 3, n_row)
        lone = urgent == LEAD
        for m in range(n_row - 1):
            fn(m, lax.rem(jnp.where(lone, LEAD + 1, urgent) + m + jnp.where(lax.rem(jnp.where(lone, LEAD + 1, urgent) - LEAD + n_row, n_row) + m >= n_row, 1, 0), n_row))

    def first_out(k, act):
        act(first_copy(k, LEAD, first_sem.at[0, 0]))

        @pl.when(odd == 0)
        def _():
            others_first(k, lambda m, r: act(first_copy(k, r, first_sem.at[0, 1 + m])))

    def first_down(k, act):
        @pl.when(odd == 0)
        def _():
            others_first(k, lambda m, r: act(copy(first_slot(k, LEAD), first_slot(k, r), first_sem.at[1, 1 + m], at(r, col))))

    def firsts_done(k):
        @pl.when(jnp.logical_and(leads, k + 1 < steps))
        def _():
            first_out(k, finish)

        @pl.when(jnp.logical_and(leads, k > 0))
        def _():
            first_down(k - 1, finish)

    @pl.when(col == 0)
    def _():
        prepare(0)
        work[0:size, :] = diag[0]

    def step(k):
        mine = col == lax.rem(k, n_col)
        kb = k // n_col
        last = k - 1
        soon = jnp.logical_and(col == lax.rem(k + 1, n_col), k + 1 < steps)

        @pl.when(mine)
        def _():
            with jax.named_scope("factor"):
                factor_block(work, winv, prev)
            for n, part in enumerate(split3(winv[0:size, :])):
                winv3[n] = part

            @pl.when(has_edge(kb))
            def _():
                with jax.named_scope("lead"):

                    @pl.when(k == 0)
                    def _():
                        edge_seeded(kb)

                    @pl.when(k > 0)
                    def _():
                        edge_arrived(last, kb)
                        update_edge(last, kb)

                    first[...] = times_winv_t(edge[kb]).astype(BF16)
                    first_out(k, start)

            lo = first_a(k)
            second = jnp.minimum(lo + 1, row_blocks)
            with jax.named_scope("solve_near"):
                loop(lo, second, lambda a: solve(k, a, 1, True))
            with jax.named_scope("solve_one"):
                third = second + lax.rem(row_blocks - second, 2)
                loop(second, third, lambda a: solve(k, a, 1, False))
            with jax.named_scope("solve_two"):
                loop(0, (row_blocks - third) // 2, lambda m: solve(k, third + 2 * m, 2, False))

        @pl.when(k >= depth)
        def _():
            with jax.named_scope("passed"):
                passed(k - depth)

        @pl.when(mine)
        def _():
            @pl.when(row == lax.rem(k, n_row))
            def _():
                for d in range(1, n_row):
                    seed_copy(kb, lax.rem(row + d, n_row)).wait_send()
                r_id = lax.broadcasted_iota(jnp.int32, (size, size), 0)
                c_id = lax.broadcasted_iota(jnp.int32, (size, size), 1)
                n = spot(k // n_row, kb)
                share[n] = jnp.where(r_id >= c_id, work[0:size, :].T, 0.0)
                pltpu.make_async_copy(share.at[n], home(o_ref, k // n_row, kb), store_sem).start()

            with jax.named_scope("late_trail"):

                def late(p):
                    columns_arrived(p, kb + 1)
                    trail(p, kb + 1, -1)

                loop(jnp.maximum(k - 1 - LAG, 0), k - LAG + 1, late)

            @pl.when(kb + 1 < col_blocks)
            def _():
                hand_out(kb + 1)

        @pl.when(jnp.logical_and(k > 0, jnp.logical_not(jnp.logical_or(mine, soon))))
        def _():
            def part(n):
                p = jnp.where(n == 1, k - 2, last)
                low = first_passed(p)
                split = last_near(p) + 1
                here = jnp.where(
                    n == 0, lead(last) != 0, jnp.where(n == 1, jnp.logical_and(k > 1, lead(k - 2 + n_col) > 3), lead(last) == 3)
                )
                begin = jnp.where(n == 0, low, jnp.maximum(low, split))
                end = jnp.where(n == 0, jnp.minimum(split, row_blocks), row_blocks)
                loop(begin, jnp.where(here, end, begin), lambda a: receive(p, a))

            with jax.named_scope("receive"):
                loop(0, 3, part)

            @pl.when(k >= LAG)
            def _():
                p = k - LAG
                near = first_b(k)
                with jax.named_scope("columns"):
                    columns_arrived(p, near)

                @pl.when(near < col_blocks)
                def _():
                    age = k + n_col - (near * n_col + col)

                    @pl.when(jnp.logical_and(age == 3, near > 0))
                    def _():
                        with jax.named_scope("seed_late"):
                            seed_arrived(near)
                            edge_seeded(near)

                    @pl.when(age >= 3)
                    def _():
                        oldest = jnp.where(age == 3, jnp.maximum(p - 2, 0), p)
                        loop(oldest, p + 1, lambda q: update_near(q, near))

                with jax.named_scope("trail"):
                    trail(p, near, near)

        @pl.when(soon)
        def _():
            nb = (k + 1) // n_col

            oldest = jnp.maximum(k - LAG, 0)

            def old_diag(p):
                column_arrived(p, nb)
                edge_arrived(p, nb)
                update_near(p, nb)

            def take(a):
                receive(last, a)

                @pl.when(a * n_row + row > k + 1)
                def _():
                    loop(oldest, last, lambda p: update_block(p, a, nb))

            @pl.when(k > 0)
            def _():
                with jax.named_scope("old_diag"):
                    loop(oldest, last, old_diag)
                with jax.named_scope("take"):
                    loop(first_a(k), jnp.minimum(first_a(k + 1) + 1, row_blocks), take)
                with jax.named_scope("take_column"):
                    column_arrived(last, nb)
                    edge_arrived(last, nb)
                with jax.named_scope("catch_up"):
                    update_near(last, nb)
                    loop(first_a(k + 1), jnp.minimum(first_a(k + 1) + 1, row_blocks), lambda a: update_block(last, a, nb))

            prepare(nb)
            slot = col_of(k, nb)
            with jax.named_scope("first_block"):
                arrived(slot)

            @pl.when(leads)
            def _():
                first_down(k, start)

            other = panel[slot]
            work[0:size, :] = diag[nb] - times_t(other, other)

        @pl.when(jnp.logical_and(k >= SENT, lead(k - SENT + n_col) == 0))
        def _():
            with jax.named_scope("sends_done"):
                firsts_done(k - SENT)
                loop(first_a(k - SENT), row_blocks, lambda a: source_sends(k - SENT, a, finish))

    loop(0, steps, step)

    loop(steps - depth, steps, passed)

    def last_sends(k):
        @pl.when(col == lax.rem(k, n_col))
        def _():
            firsts_done(k)
            loop(first_a(k), row_blocks, lambda a: source_sends(k, a, finish))

    loop(steps - SENT, steps, last_sends)

    def edges_done(b):
        @pl.when(jnp.logical_and(holds_edge(b), jnp.logical_not(leads)))
        def _():
            edge_copy(b).wait_send()

    loop(0, col_blocks, edges_done)
    with jax.named_scope("stored"):
        pltpu.make_async_copy(share, share, store_sem).wait()


def solution(mesh):
    n_row = mesh.shape["row"]
    n_col = mesh.shape["col"]

    def factor_local(a_loc):
        row_blocks, size, local_cols = a_loc.shape
        col_blocks = local_cols // size
        slots = n_row * (row_blocks * (row_blocks + 1) // 2) + n_col * (col_blocks * (col_blocks + 1) // 2)
        slots += 2 * row_blocks * n_row
        return pl.pallas_call(
            functools.partial(kernel, n_row, n_col, "batch"),
            out_shape=jax.ShapeDtypeStruct(a_loc.shape, F32),
            in_specs=[pl.BlockSpec(memory_space=pl.ANY)],
            out_specs=pl.BlockSpec(memory_space=pl.ANY),
            scratch_shapes=[
                pltpu.VMEM((row_blocks * col_blocks, size, size), F32),
                pltpu.VMEM((col_blocks, size, size), F32),
                pltpu.VMEM((col_blocks, size, size), F32),
                pltpu.VMEM((col_blocks, size, size), F32),
                pltpu.VMEM((size, size), BF16),
                pltpu.VMEM((slots, size, size), BF16),
                pltpu.VMEM((size + BASE, size), F32),
                pltpu.VMEM((size + BASE, size), F32),
                pltpu.VMEM((3, size, size), BF16),
                pltpu.VMEM((BASE, 3 * LANE), F32),
                pltpu.SemaphoreType.DMA,
                pltpu.SemaphoreType.DMA,
                pltpu.SemaphoreType.DMA((col_blocks, n_row)),
                pltpu.SemaphoreType.DMA((col_blocks,)),
                pltpu.SemaphoreType.DMA((col_blocks,)),
                pltpu.SemaphoreType.DMA((col_blocks,)),
                pltpu.SemaphoreType.DMA((2, n_row)),
                pltpu.SemaphoreType.DMA((row_blocks, 9)),
                pltpu.SemaphoreType.DMA((6, row_blocks, 2)),
                pltpu.SemaphoreType.DMA((6, col_blocks, 4)),
                pltpu.SemaphoreType.DMA((slots,)),
            ],
            compiler_params=pltpu.CompilerParams(
                collective_id=0, has_side_effects=True, vmem_limit_bytes=60 * 1024 * 1024
            ),
            name="cholesky",
        )(a_loc)

    blk_spec = P(("batch", "row"), None, "col")
    return jax.shard_map(factor_local, mesh=mesh, in_specs=(blk_spec,), out_specs=blk_spec, check_vma=False)
```

```python
import functools

import jax
import jax.numpy as jnp
from jax import lax
from jax.experimental import pallas as pl
from jax.experimental.pallas import tpu as pltpu
from jax.sharding import PartitionSpec as P

F32 = jnp.float32
BF16 = jnp.bfloat16
MESH = pl.DeviceIdType.MESH
SUB = 8
LANE = 128
BASE = 16
LEAD = 1
LAG = 3


def sub_bcast(x, q):
    return jnp.broadcast_to(x[q : q + 1, :], (SUB, LANE))


ALONG_LANES = lax.GatherDimensionNumbers(
    offset_dims=(), collapsed_slice_dims=(1,), start_index_map=(1,), operand_batching_dims=(0,), start_indices_batching_dims=(0,)
)


def lane_bcast(x, lane):
    index = jnp.full((SUB, LANE, 1), lane, jnp.int32)
    return lax.gather(x, index, ALONG_LANES, (1, 1), mode=lax.GatherScatterMode.PROMISE_IN_BOUNDS)


def split3(x):
    high = x.astype(BF16)
    rest = x - high.astype(F32)
    mid = rest.astype(BF16)
    return high, mid, (rest - mid.astype(F32)).astype(BF16)


def swap_rows(x, bit, row_id):
    if bit == SUB // 2:
        return pltpu.roll(x, bit, 0)
    return jnp.where((row_id & bit) == 0, pltpu.roll(x, SUB - bit, 0), pltpu.roll(x, bit, 0))


def stack_sums(parts):
    row_id = lax.broadcasted_iota(jnp.int32, (SUB, LANE), 0)
    for bit in (4, 2, 1):
        low = (row_id & bit) == 0
        half = len(parts) // 2
        parts = [
            jnp.where(low, parts[n], parts[n + half]) + swap_rows(jnp.where(low, parts[n + half], parts[n]), bit, row_id)
            for n in range(half)
        ]
    return parts[0]


def eliminate(rows, lane0):
    row_id = lax.broadcasted_iota(jnp.int32, (SUB, LANE), 0)
    rows = [list(rows[0]), list(rows[1])]
    cols = [
        [lane_bcast(rows[0][0], lane0 + j) for j in range(SUB)],
        [lane_bcast(rows[1][0], lane0 + j) for j in range(BASE)],
    ]
    scale = [jnp.zeros((SUB, LANE), F32), jnp.zeros((SUB, LANE), F32)]
    pivot = sub_bcast(cols[0][0], 0)
    for j in range(BASE):
        t, q = divmod(j, SUB)
        inv = lax.rsqrt(pivot)
        scale[t] = jnp.where(row_id == q, inv, scale[t])
        if j + 1 < BASE:
            tn, qn = divmod(j + 1, SUB)
            near = sub_bcast(cols[tn][j], qn) * inv
            pivot = sub_bcast(cols[tn][j + 1], qn) - near * near
        below = cols[1][j] * inv
        here = cols[0][j] * inv if t == 0 else None
        for n in range(j + 1, BASE):
            tn, qn = divmod(n, SUB)
            other = near if n == j + 1 else sub_bcast(here if tn == 0 else below, qn)
            if t == 0 and tn == 0:
                cols[0][n] = cols[0][n] - here * other
            cols[1][n] = cols[1][n] - below * other
        masked = jnp.where(row_id > q, here if t == 0 else below, 0.0)
        for v in range(len(rows[0])):
            pivot_row = sub_bcast(rows[t][v], q) * inv
            rows[t][v] = rows[t][v] - masked * pivot_row
            if t == 0:
                rows[1][v] = rows[1][v] - below * pivot_row
    return [[x * scale[t] for x in rows[t]] for t in range(2)]


def factor_block(work, winv, prev):
    size = work.shape[1]
    prev[...] = jnp.zeros(prev.shape, F32)
    for half in range(size // LANE):
        views = [(work, 0), (work, 1), (winv, 0)] if half == 0 else [(work, 1), (winv, 0), (winv, 1)]
        first = half * LANE
        if half == 1:
            mid_part, inv_part = prev[:, LANE : 2 * LANE], prev[:, 2 * LANE :]
            prev[:, :LANE] = mid_part
            prev[:, LANE : 2 * LANE] = inv_part
            prev[:, 2 * LANE :] = jnp.zeros((BASE, LANE), F32)

        def body(s, carry, views=views, first=first):
            lane0 = s * BASE
            row0 = pl.multiple_of(first + lane0, BASE)

            def rows_at(row, t):
                return pl.ds(pl.multiple_of(row + SUB * t, SUB), SUB)

            rows = [[ref[rows_at(row0, t), LANE * g : LANE * (g + 1)] for ref, g in views] for t in range(2)]
            hi, mid, lo = split3(prev[...])
            lane = lax.broadcasted_iota(jnp.int32, (BASE, size - first), 1) + first
            after = lane >= row0 + BASE
            lhi, lmid, llo = [jnp.where(after, x[:, : size - first], jnp.zeros((), BF16)) for x in (hi, mid, lo)]
            update = lax.dot_general(
                jnp.concatenate([lhi, lhi, lmid, lhi, llo, lmid], axis=0),
                jnp.concatenate([hi, mid, hi, lo, hi, mid], axis=0),
                (((0,), (0,)), ((), ())),
                preferred_element_type=F32,
            )
            for v, (ref, g) in enumerate(views):
                ref[first:size, LANE * g : LANE * (g + 1)] -= update[:, LANE * v : LANE * (v + 1)]
            done = eliminate(rows, lane0)
            for t in range(2):
                for v, (ref, g) in enumerate(views):
                    ref[rows_at(row0, t), LANE * g : LANE * (g + 1)] = done[t][v]
                    prev[SUB * t : SUB * (t + 1), LANE * v : LANE * (v + 1)] = done[t][v]
            if first == 0:
                source = [jnp.where(s == LANE // BASE - 1, done[t][1], done[t][0]) for t in range(2)]
            else:
                source = [done[t][0] for t in range(2)]
            next_lane = (lane0 + BASE) % LANE
            for t in range(2):
                factor = [[lane_bcast(source[m], next_lane + SUB * t + n) for n in range(SUB)] for m in range(2)]
                for v, (ref, g) in enumerate(views):
                    parts = [factor[0][n] * done[0][v] + factor[1][n] * done[1][v] for n in range(SUB)]
                    ref[rows_at(row0 + BASE, t), LANE * g : LANE * (g + 1)] -= stack_sums(parts)
            return carry

        lax.fori_loop(0, LANE // BASE, body, 0)


def kernel(n_row, n_col, batch_axis, a_ref, o_ref, share, diag, edge, stage, first, panel, work, winv, winv3, prev, load_sem, store_sem,
           seed_send, seed_recv, edge_send, edge_recv, first_sem, send_sem, pass_sem, recv_sem):
    row_blocks, size, local_cols = a_ref.shape
    col_blocks = local_cols // size
    ratio = n_col // n_row
    steps = row_blocks * n_row
    depth = pass_sem.shape[0]
    batch = lax.axis_index(batch_axis)
    row = lax.axis_index("row")
    col = lax.axis_index("col")
    odd = lax.rem(col, 2)
    on_diag = lax.rem(col, n_row) == row
    row_slots = n_row * (row_blocks * (row_blocks + 1) // 2)
    edge_slots = row_slots + n_col * (col_blocks * (col_blocks + 1) // 2)
    leads = row == LEAD

    def at(dev_row, dev_col):
        return (batch, dev_row, dev_col)

    def row_slot(k, a):
        g = k // n_row
        return n_row * (row_blocks * g - (g * (g - 1)) // 2) + (k - g * n_row) * (row_blocks - g) + a - g

    def col_slot(k, b):
        h = k // n_col
        return row_slots + n_col * (col_blocks * h - (h * (h - 1)) // 2) + (k - h * n_col) * (col_blocks - h) + b - h

    def first_a(k):
        return (k + n_row - row) // n_row

    def first_b(k):
        return (k + n_col - col) // n_col

    def home(ref, a, b):
        return ref.at[a, :, pl.ds(pl.multiple_of(b * size, size), size)]

    def spot(a, b):
        return b * row_blocks + a

    def col_of(k, b):
        return jnp.where(on_diag, row_slot(k, ratio * b + col // n_row), col_slot(k, b))

    def edge_slot(k, j):
        return edge_slots + 2 * k + (j - k - 1) // n_col

    def edge_reach(ahead):
        return jnp.logical_and(ahead >= 2, jnp.logical_and(ahead <= n_col + LAG, row != LEAD))

    def copy(src_slot, dst_slot, sem, device):
        return pltpu.make_async_remote_copy(
            src_ref=panel.at[src_slot], dst_ref=panel.at[dst_slot], send_sem=sem, recv_sem=recv_sem.at[dst_slot],
            device_id=device, device_id_type=MESH,
        )

    def arrived(slot):
        copy(slot, slot, send_sem.at[0, 0], at(row, col)).wait_recv()

    def start(c):
        c.start()

    def finish(c):
        c.wait_send()

    def down_column(k, a, sems, act):
        i = a * n_row + row
        slot = row_slot(k, a)
        dst = col_slot(k, i // n_col)
        swap = lax.rem(LEAD - row + n_row, n_row)
        for m, d in enumerate((1, n_row - 1, 2)):
            way = jnp.where(swap == 0, d, jnp.where(m == 0, swap, jnp.where(swap == d, 1, d)))
            act(copy(slot, dst, sems[m], at(lax.rem(row + way, n_row), lax.rem(i, n_col))))

    def to_edge(k, a, sem, act):
        i = a * n_row + row
        act(copy(row_slot(k, a), edge_slot(k, i - 1), sem, at(LEAD, lax.rem(i - 1, n_col))))

    def source_sends(k, a, act):
        ahead = a * n_row + row - k
        slot = row_slot(k, a)
        early = n_row

        @pl.when(jnp.logical_and(edge_reach(ahead), jnp.logical_or(ahead <= early, ahead == n_col)))
        def _():
            to_edge(k, a, send_sem.at[a, 5], act)

        near = jnp.logical_and(ahead >= 2, ahead <= early)

        @pl.when(jnp.logical_or(near, lax.rem(ahead, n_col) == 0))
        def _():
            down_column(k, a, [send_sem.at[a, m] for m in range(3)], act)

        @pl.when(jnp.logical_or(jnp.logical_and(odd == 0, ahead >= 2), ahead >= n_col - 1))
        def _():
            act(copy(slot, slot, send_sem.at[a, 3], at(row, lax.rem(jnp.where(odd == 0, col + 1, col - 1), n_col))))

        @pl.when(jnp.logical_and(odd == 1, ahead >= 2))
        def _():
            act(copy(slot, slot, send_sem.at[a, 6], at(row, lax.rem(col + 1, n_col))))

        @pl.when(ahead >= 2)
        def _():
            act(copy(slot, slot, send_sem.at[a, 4], at(row, lax.rem(col - odd + 3, n_col))))

        @pl.when(jnp.logical_and(odd == 1, jnp.logical_and(ahead >= n_col // 2 - 1, ahead < n_col - 3)))
        def _():
            act(copy(slot, slot, send_sem.at[a, 7], at(row, lax.rem(col + n_col // 2, n_col))))

        @pl.when(ahead >= n_col - 2 - odd)
        def _():
            act(copy(slot, slot, send_sem.at[a, 8], at(row, lax.rem(col - odd - 1 + n_col, n_col))))

    def lead(p):
        return lax.rem(col - lax.rem(p, n_col) + n_col, n_col)

    def hops(p):
        return lax.rem(col // 2 - lax.rem(p, n_col) // 2 + n_col // 2, n_col // 2)

    def passes(p):
        return jnp.logical_and(odd == 1, hops(p) != 0)

    def first_passed(p):
        low = jnp.where(passes(p), jnp.maximum(lead(p) - 1, 2), lead(p))
        return (p + low - row + n_row - 1) // n_row

    def pass_on(p, a, act):
        i = a * n_row + row
        ahead = i - p
        slot = row_slot(p, a)
        sems = pass_sem.at[lax.rem(p, depth), a]
        src_odd = lax.rem(p, 2)
        far = n_col - 2 - src_odd

        @pl.when(passes(p))
        def _():
            h = hops(p)
            via_prev = jnp.logical_or(src_odd == 1, jnp.logical_and(lax.rem(a, 2) == 1, ahead >= far))
            mine_to_pass = jnp.logical_or(
                jnp.logical_and(h == 1, jnp.logical_not(via_prev)), jnp.logical_and(h == n_col // 2 - 1, via_prev)
            )

            @pl.when(jnp.logical_and(mine_to_pass, ahead >= n_col // 2 - src_odd))
            def _():
                act(copy(slot, slot, sems.at[4], at(row, lax.rem(jnp.where(h == 1, col + 2, col - 2 + n_col), n_col))))

            @pl.when(jnp.logical_or(src_odd == 0, h != 1))
            def _():
                act(copy(slot, slot, sems.at[3], at(row, col - 1)))

        own = lax.rem(i, n_col) == col

        @pl.when(jnp.logical_and(own, jnp.logical_and(ahead > n_row, edge_reach(ahead))))
        def _():
            to_edge(p, a, sems.at[5], act)

        @pl.when(jnp.logical_and(own, ahead > n_row))
        def _():
            down_column(p, a, [sems.at[m] for m in range(3)], act)

    def passed(p):
        @pl.when(lead(p) != 0)
        def _():
            loop(first_passed(p), row_blocks, lambda a: pass_on(p, a, finish))

    def receive(p, a):
        arrived(row_slot(p, a))
        pass_on(p, a, start)

    def loop(lo, hi, fn):
        lax.fori_loop(lo, hi, lambda n, c: (fn(n), c)[1], 0)

    for a in range(row_blocks):
        for b in range(col_blocks):
            pltpu.make_async_copy(home(a_ref, a, b), share.at[spot(a, b)], load_sem).start()

    barrier = pltpu.get_barrier_semaphore()
    n_dev = n_row * n_col

    def greet(n):
        other = lax.rem(row * n_col + col + n, n_dev)
        pl.semaphore_signal(barrier, inc=1, device_id=at(other // n_col, lax.rem(other, n_col)), device_id_type=MESH)

    loop(1, n_dev, greet)
    with jax.named_scope("all_here"):
        pl.semaphore_wait(barrier, n_dev - 1)
    with jax.named_scope("loaded"):
        pltpu.make_async_copy(share, share, load_sem).wait()

    def seed_copy(b, dev_row):
        return pltpu.make_async_remote_copy(
            src_ref=share.at[spot(ratio * b + col // n_row, b)], dst_ref=diag.at[b],
            send_sem=seed_send.at[b, lax.rem(dev_row - row + n_row, n_row)],
            recv_sem=seed_recv.at[b], device_id=at(dev_row, col), device_id_type=MESH,
        )

    def hand_out(b):
        @pl.when(on_diag)
        def _():
            for d in (1, n_row - 1, 2):
                seed_copy(b, lax.rem(row + d, n_row)).start()
            diag[b] = share[spot(ratio * b + col // n_row, b)]

        @pl.when(jnp.logical_and(holds_edge(b), jnp.logical_not(leads)))
        def _():
            stage[b] = share[spot((b * n_col + col + 1) // n_row, b)]
            edge_copy(b).start()

    def holds_edge(b):
        j = b * n_col + col
        return jnp.logical_and(lax.rem(j + 1, n_row) == row, j + 1 < steps)

    def edge_copy(b):
        return pltpu.make_async_remote_copy(
            src_ref=stage.at[b], dst_ref=edge.at[b], send_sem=edge_send.at[b], recv_sem=edge_recv.at[b],
            device_id=at(LEAD, col), device_id_type=MESH,
        )

    def has_edge(b):
        from_other = jnp.logical_and(leads, lax.rem(col + 1, n_row) != LEAD)
        return jnp.logical_and(from_other, b * n_col + col + 1 < steps)

    def edge_seeded(b):
        @pl.when(has_edge(b))
        def _():
            edge_copy(b).wait_recv()

    def edge_arrived(p, b):
        j = b * n_col + col

        @pl.when(jnp.logical_and(has_edge(b), j + 1 - p <= n_col + LAG))
        def _():
            arrived(edge_slot(p, j))

    hand_out(0)

    def seed_arrived(b):
        @pl.when(jnp.logical_not(on_diag))
        def _():
            seed_copy(b, row).wait_recv()

    with jax.named_scope("seed"):
        seed_arrived(0)

        @pl.when(col != 0)
        def _():
            edge_seeded(0)

    def clear(n):
        a, b = lax.rem(n, row_blocks), n // row_blocks

        @pl.when(a * n_row + row < b * n_col + col)
        def _():
            share[n] = jnp.zeros((size, size), F32)
            pltpu.make_async_copy(share.at[n], home(o_ref, a, b), store_sem).start()

    loop(0, row_blocks * col_blocks, clear)

    def times_t(x, y):
        return lax.dot_general(x, y, (((1,), (1,)), ((), ())), preferred_element_type=F32)

    def update_block(p, a, b):
        share[spot(a, b)] -= times_t(panel[row_slot(p, a)], panel[col_of(p, b)])

    def update_diag(p, b):
        other = panel[col_of(p, b)]
        diag[b] -= times_t(other, other)

    def update_edge(p, b):
        @pl.when(has_edge(b))
        def _():
            edge[b] -= times_t(panel[edge_slot(p, b * n_col + col)], panel[col_of(p, b)])

    def column_arrived(p, b):
        @pl.when(jnp.logical_not(on_diag))
        def _():
            arrived(col_slot(p, b))

    def update_column(p, b, lo):
        lone = lax.rem(row_blocks - lo, 2)

        @pl.when(lone == 1)
        def _():
            update_block(p, lo, b)

        def pair(m):
            a = lo + lone + 2 * m
            both = pl.ds(spot(a, b), 2)
            left = panel[pl.ds(row_slot(p, a), 2)].reshape(2 * size, size)
            share[both] -= times_t(left, panel[col_of(p, b)]).reshape(2, size, size)

        loop(0, (row_blocks - lo) // 2, pair)

    def trail(p, b_from, near):
        loop(b_from, col_blocks, lambda b: update_column(p, b, first_a(b * n_col + col - jnp.where(b == near, 0, 1))))

    def columns_arrived(p, b_from):
        def one(b):
            column_arrived(p, b)
            edge_arrived(p, b)

        loop(b_from, col_blocks, one)

    def prepare(b):
        work[size:, :] = jnp.zeros((BASE, size), F32)
        r_id = lax.broadcasted_iota(jnp.int32, (size + BASE, size), 0)
        c_id = lax.broadcasted_iota(jnp.int32, (size + BASE, size), 1)
        winv[...] = jnp.where(r_id == c_id, 1.0, 0.0).astype(F32)

    def times_winv_t(x):
        hi, mid, lo = split3(x)
        whi, wmid, wlo = winv3[0], winv3[1], winv3[2]
        small = times_t(lo, whi) + times_t(mid, wmid) + times_t(hi, wlo)
        return small + (times_t(mid, whi) + times_t(hi, wmid)) + times_t(hi, whi)

    def solve(k, a, count, near):
        kb = k // n_col
        here = pl.ds(spot(a, kb), count)

        def apply(p):
            left = panel[pl.ds(row_slot(p, a), count)].reshape(count * size, size)
            share[here] -= times_t(left, panel[col_of(p, kb)]).reshape(count, size, size)

        if not near:

            @pl.when(k > 1)
            def _():
                for m in range(count):
                    receive(k - 2, a + m)

            loop(jnp.maximum(k - 1 - LAG, 0), k - 1, apply)

        @pl.when(k > 0)
        def _():
            for m in range(count):
                receive(k - 1, a + m)
            apply(k - 1)

        x = times_winv_t(share[here].reshape(count * size, size)).reshape(count, size, size)
        panel[pl.ds(row_slot(k, a), count)] = x.astype(BF16)
        share[here] = x
        if near:

            @pl.when(jnp.logical_and(leads, lax.rem(k + 1, n_row) == LEAD))
            def _():
                first[...] = panel[row_slot(k, a)]
                first_out(k, start)

        for m in range(count):
            source_sends(k, a + m, start)
        for m in range(count):
            pltpu.make_async_copy(share.at[spot(a + m, kb)], home(o_ref, a + m, kb), store_sem).start()

    def update_near(p, b):
        update_diag(p, b)
        update_edge(p, b)

    def first_slot(k, dev_row):
        return jnp.where(lax.rem(k + 1, n_row) == dev_row, row_slot(k, (k + 1) // n_row), col_slot(k, (k + 1) // n_col))

    def first_copy(k, dev_row, sem):
        dst = first_slot(k, dev_row)
        return pltpu.make_async_remote_copy(
            src_ref=first, dst_ref=panel.at[dst], send_sem=sem, recv_sem=recv_sem.at[dst],
            device_id=at(dev_row, lax.rem(col + 1, n_col)), device_id_type=MESH,
        )

    def others_first(k, fn):
        urgent = lax.rem(k + 3, n_row)
        lone = urgent == LEAD
        for m in range(n_row - 1):
            fn(m, lax.rem(jnp.where(lone, LEAD + 1, urgent) + m + jnp.where(lax.rem(jnp.where(lone, LEAD + 1, urgent) - LEAD + n_row, n_row) + m >= n_row, 1, 0), n_row))

    def first_out(k, act):
        act(first_copy(k, LEAD, first_sem.at[0, 0]))

        @pl.when(odd == 0)
        def _():
            others_first(k, lambda m, r: act(first_copy(k, r, first_sem.at[0, 1 + m])))

    def first_down(k, act):
        @pl.when(odd == 0)
        def _():
            others_first(k, lambda m, r: act(copy(first_slot(k, LEAD), first_slot(k, r), first_sem.at[1, 1 + m], at(r, col))))

    def firsts_done(k):
        @pl.when(jnp.logical_and(leads, k + 1 < steps))
        def _():
            first_out(k, finish)

        @pl.when(jnp.logical_and(leads, k > 0))
        def _():
            first_down(k - 1, finish)

    @pl.when(col == 0)
    def _():
        prepare(0)
        work[0:size, :] = diag[0]

    def step(k):
        mine = col == lax.rem(k, n_col)
        kb = k // n_col
        last = k - 1
        soon = jnp.logical_and(col == lax.rem(k + 1, n_col), k + 1 < steps)

        @pl.when(mine)
        def _():
            with jax.named_scope("factor"):
                factor_block(work, winv, prev)
            for n, part in enumerate(split3(winv[0:size, :])):
                winv3[n] = part

            @pl.when(has_edge(kb))
            def _():
                with jax.named_scope("lead"):

                    @pl.when(k == 0)
                    def _():
                        edge_seeded(kb)

                    @pl.when(k > 0)
                    def _():
                        edge_arrived(last, kb)
                        update_edge(last, kb)

                    first[...] = times_winv_t(edge[kb]).astype(BF16)
                    first_out(k, start)

            lo = first_a(k)
            second = jnp.minimum(lo + 1, row_blocks)
            with jax.named_scope("solve_near"):
                loop(lo, second, lambda a: solve(k, a, 1, True))
            with jax.named_scope("solve_one"):
                third = second + lax.rem(row_blocks - second, 2)
                loop(second, third, lambda a: solve(k, a, 1, False))
            with jax.named_scope("solve_two"):
                loop(0, (row_blocks - third) // 2, lambda m: solve(k, third + 2 * m, 2, False))

        @pl.when(k >= depth)
        def _():
            with jax.named_scope("passed"):
                passed(k - depth)

        @pl.when(mine)
        def _():
            @pl.when(row == lax.rem(k, n_row))
            def _():
                for d in range(1, n_row):
                    seed_copy(kb, lax.rem(row + d, n_row)).wait_send()
                r_id = lax.broadcasted_iota(jnp.int32, (size, size), 0)
                c_id = lax.broadcasted_iota(jnp.int32, (size, size), 1)
                n = spot(k // n_row, kb)
                share[n] = jnp.where(r_id >= c_id, work[0:size, :].T, 0.0)
                pltpu.make_async_copy(share.at[n], home(o_ref, k // n_row, kb), store_sem).start()

            with jax.named_scope("late_trail"):

                def late(p):
                    columns_arrived(p, kb + 1)
                    trail(p, kb + 1, -1)

                loop(jnp.maximum(k - 1 - LAG, 0), k - LAG + 1, late)

            @pl.when(kb + 1 < col_blocks)
            def _():
                hand_out(kb + 1)

        @pl.when(jnp.logical_and(k > 0, jnp.logical_not(jnp.logical_or(mine, soon))))
        def _():
            @pl.when(col != lax.rem(last, n_col))
            def _():
                with jax.named_scope("receive"):
                    loop(first_passed(last), row_blocks, lambda a: receive(last, a))

            @pl.when(k >= LAG)
            def _():
                p = k - LAG
                near = first_b(k)
                with jax.named_scope("columns"):
                    columns_arrived(p, near)

                @pl.when(near < col_blocks)
                def _():
                    age = k + n_col - (near * n_col + col)

                    @pl.when(jnp.logical_and(age == 3, near > 0))
                    def _():
                        with jax.named_scope("seed_late"):
                            seed_arrived(near)
                            edge_seeded(near)

                    @pl.when(age >= 3)
                    def _():
                        oldest = jnp.where(age == 3, jnp.maximum(p - 2, 0), p)
                        loop(oldest, p + 1, lambda q: update_near(q, near))

                with jax.named_scope("trail"):
                    trail(p, near, near)

        @pl.when(soon)
        def _():
            nb = (k + 1) // n_col

            oldest = jnp.maximum(k - LAG, 0)

            def old_diag(p):
                column_arrived(p, nb)
                edge_arrived(p, nb)
                update_near(p, nb)

            def take(a):
                receive(last, a)

                @pl.when(a * n_row + row > k + 1)
                def _():
                    loop(oldest, last, lambda p: update_block(p, a, nb))

            @pl.when(k > 0)
            def _():
                with jax.named_scope("old_diag"):
                    loop(oldest, last, old_diag)
                with jax.named_scope("take"):
                    loop(first_a(k), jnp.minimum(first_a(k + 1) + 1, row_blocks), take)
                with jax.named_scope("take_column"):
                    column_arrived(last, nb)
                    edge_arrived(last, nb)
                with jax.named_scope("catch_up"):
                    update_near(last, nb)
                    loop(first_a(k + 1), jnp.minimum(first_a(k + 1) + 1, row_blocks), lambda a: update_block(last, a, nb))

            prepare(nb)
            slot = col_of(k, nb)
            with jax.named_scope("first_block"):
                arrived(slot)

            @pl.when(leads)
            def _():
                first_down(k, start)

            other = panel[slot]
            work[0:size, :] = diag[nb] - times_t(other, other)

        @pl.when(jnp.logical_and(k >= n_col // 2, col == lax.rem(k + n_col // 2, n_col)))
        def _():
            with jax.named_scope("sends_done"):
                firsts_done(k - n_col // 2)
                loop(first_a(k - n_col // 2), row_blocks, lambda a: source_sends(k - n_col // 2, a, finish))

    loop(0, steps, step)

    loop(steps - depth, steps, passed)

    def last_sends(k):
        @pl.when(col == lax.rem(k, n_col))
        def _():
            firsts_done(k)
            loop(first_a(k), row_blocks, lambda a: source_sends(k, a, finish))

    loop(steps - n_col // 2, steps, last_sends)

    def edges_done(b):
        @pl.when(jnp.logical_and(holds_edge(b), jnp.logical_not(leads)))
        def _():
            edge_copy(b).wait_send()

    loop(0, col_blocks, edges_done)
    with jax.named_scope("stored"):
        pltpu.make_async_copy(share, share, store_sem).wait()


def solution(mesh):
    n_row = mesh.shape["row"]
    n_col = mesh.shape["col"]

    def factor_local(a_loc):
        row_blocks, size, local_cols = a_loc.shape
        col_blocks = local_cols // size
        slots = n_row * (row_blocks * (row_blocks + 1) // 2) + n_col * (col_blocks * (col_blocks + 1) // 2)
        slots += 2 * row_blocks * n_row
        return pl.pallas_call(
            functools.partial(kernel, n_row, n_col, "batch"),
            out_shape=jax.ShapeDtypeStruct(a_loc.shape, F32),
            in_specs=[pl.BlockSpec(memory_space=pl.ANY)],
            out_specs=pl.BlockSpec(memory_space=pl.ANY),
            scratch_shapes=[
                pltpu.VMEM((row_blocks * col_blocks, size, size), F32),
                pltpu.VMEM((col_blocks, size, size), F32),
                pltpu.VMEM((col_blocks, size, size), F32),
                pltpu.VMEM((col_blocks, size, size), F32),
                pltpu.VMEM((size, size), BF16),
                pltpu.VMEM((slots, size, size), BF16),
                pltpu.VMEM((size + BASE, size), F32),
                pltpu.VMEM((size + BASE, size), F32),
                pltpu.VMEM((3, size, size), BF16),
                pltpu.VMEM((BASE, 3 * LANE), F32),
                pltpu.SemaphoreType.DMA,
                pltpu.SemaphoreType.DMA,
                pltpu.SemaphoreType.DMA((col_blocks, n_row)),
                pltpu.SemaphoreType.DMA((col_blocks,)),
                pltpu.SemaphoreType.DMA((col_blocks,)),
                pltpu.SemaphoreType.DMA((col_blocks,)),
                pltpu.SemaphoreType.DMA((2, n_row)),
                pltpu.SemaphoreType.DMA((row_blocks, 9)),
                pltpu.SemaphoreType.DMA((4, row_blocks, 6)),
                pltpu.SemaphoreType.DMA((slots,)),
            ],
            compiler_params=pltpu.CompilerParams(
                collective_id=0, has_side_effects=True, vmem_limit_bytes=60 * 1024 * 1024
            ),
            name="cholesky",
        )(a_loc)

    blk_spec = P(("batch", "row"), None, "col")
    return jax.shard_map(factor_local, mesh=mesh, in_specs=(blk_spec,), out_specs=blk_spec, check_vma=False)
```

```python
import functools

import jax
import jax.numpy as jnp
from jax import lax
from jax.experimental import pallas as pl
from jax.experimental.pallas import tpu as pltpu
from jax.sharding import PartitionSpec as P

F32 = jnp.float32
BF16 = jnp.bfloat16
MESH = pl.DeviceIdType.MESH
SUB = 8
LANE = 128
BASE = 16
LEAD = 1
LAG = 3


def sub_bcast(x, q):
    return jnp.broadcast_to(x[q : q + 1, :], (SUB, LANE))


ALONG_LANES = lax.GatherDimensionNumbers(
    offset_dims=(), collapsed_slice_dims=(1,), start_index_map=(1,), operand_batching_dims=(0,), start_indices_batching_dims=(0,)
)


def lane_bcast(x, lane):
    index = jnp.full((SUB, LANE, 1), lane, jnp.int32)
    return lax.gather(x, index, ALONG_LANES, (1, 1), mode=lax.GatherScatterMode.PROMISE_IN_BOUNDS)


def split3(x):
    high = x.astype(BF16)
    rest = x - high.astype(F32)
    mid = rest.astype(BF16)
    return high, mid, (rest - mid.astype(F32)).astype(BF16)


def swap_rows(x, bit, row_id):
    if bit == SUB // 2:
        return pltpu.roll(x, bit, 0)
    return jnp.where((row_id & bit) == 0, pltpu.roll(x, SUB - bit, 0), pltpu.roll(x, bit, 0))


def stack_sums(parts):
    row_id = lax.broadcasted_iota(jnp.int32, (SUB, LANE), 0)
    for bit in (4, 2, 1):
        low = (row_id & bit) == 0
        half = len(parts) // 2
        parts = [
            jnp.where(low, parts[n], parts[n + half]) + swap_rows(jnp.where(low, parts[n + half], parts[n]), bit, row_id)
            for n in range(half)
        ]
    return parts[0]


def eliminate(rows, lane0):
    row_id = lax.broadcasted_iota(jnp.int32, (SUB, LANE), 0)
    rows = [list(rows[0]), list(rows[1])]
    cols = [
        [lane_bcast(rows[0][0], lane0 + j) for j in range(SUB)],
        [lane_bcast(rows[1][0], lane0 + j) for j in range(BASE)],
    ]
    scale = [jnp.zeros((SUB, LANE), F32), jnp.zeros((SUB, LANE), F32)]
    pivot = sub_bcast(cols[0][0], 0)
    for j in range(BASE):
        t, q = divmod(j, SUB)
        inv = lax.rsqrt(pivot)
        scale[t] = jnp.where(row_id == q, inv, scale[t])
        if j + 1 < BASE:
            tn, qn = divmod(j + 1, SUB)
            near = sub_bcast(cols[tn][j], qn) * inv
            pivot = sub_bcast(cols[tn][j + 1], qn) - near * near
        below = cols[1][j] * inv
        here = cols[0][j] * inv if t == 0 else None
        for n in range(j + 1, BASE):
            tn, qn = divmod(n, SUB)
            other = near if n == j + 1 else sub_bcast(here if tn == 0 else below, qn)
            if t == 0 and tn == 0:
                cols[0][n] = cols[0][n] - here * other
            cols[1][n] = cols[1][n] - below * other
        masked = jnp.where(row_id > q, here if t == 0 else below, 0.0)
        for v in range(len(rows[0])):
            pivot_row = sub_bcast(rows[t][v], q) * inv
            rows[t][v] = rows[t][v] - masked * pivot_row
            if t == 0:
                rows[1][v] = rows[1][v] - below * pivot_row
    return [[x * scale[t] for x in rows[t]] for t in range(2)]


def factor_block(work, winv, prev):
    size = work.shape[1]
    prev[...] = jnp.zeros(prev.shape, F32)
    for half in range(size // LANE):
        views = [(work, 0), (work, 1), (winv, 0)] if half == 0 else [(work, 1), (winv, 0), (winv, 1)]
        first = half * LANE
        if half == 1:
            mid_part, inv_part = prev[:, LANE : 2 * LANE], prev[:, 2 * LANE :]
            prev[:, :LANE] = mid_part
            prev[:, LANE : 2 * LANE] = inv_part
            prev[:, 2 * LANE :] = jnp.zeros((BASE, LANE), F32)

        def body(s, carry, views=views, first=first):
            lane0 = s * BASE
            row0 = pl.multiple_of(first + lane0, BASE)

            def rows_at(row, t):
                return pl.ds(pl.multiple_of(row + SUB * t, SUB), SUB)

            rows = [[ref[rows_at(row0, t), LANE * g : LANE * (g + 1)] for ref, g in views] for t in range(2)]
            hi, mid, lo = split3(prev[...])
            lane = lax.broadcasted_iota(jnp.int32, (BASE, size - first), 1) + first
            after = lane >= row0 + BASE
            lhi, lmid, llo = [jnp.where(after, x[:, : size - first], jnp.zeros((), BF16)) for x in (hi, mid, lo)]
            update = lax.dot_general(
                jnp.concatenate([lhi, lhi, lmid, lhi, llo, lmid], axis=0),
                jnp.concatenate([hi, mid, hi, lo, hi, mid], axis=0),
                (((0,), (0,)), ((), ())),
                preferred_element_type=F32,
            )
            for v, (ref, g) in enumerate(views):
                ref[first:size, LANE * g : LANE * (g + 1)] -= update[:, LANE * v : LANE * (v + 1)]
            done = eliminate(rows, lane0)
            for t in range(2):
                for v, (ref, g) in enumerate(views):
                    ref[rows_at(row0, t), LANE * g : LANE * (g + 1)] = done[t][v]
                    prev[SUB * t : SUB * (t + 1), LANE * v : LANE * (v + 1)] = done[t][v]
            if first == 0:
                source = [jnp.where(s == LANE // BASE - 1, done[t][1], done[t][0]) for t in range(2)]
            else:
                source = [done[t][0] for t in range(2)]
            next_lane = (lane0 + BASE) % LANE
            for t in range(2):
                factor = [[lane_bcast(source[m], next_lane + SUB * t + n) for n in range(SUB)] for m in range(2)]
                for v, (ref, g) in enumerate(views):
                    parts = [factor[0][n] * done[0][v] + factor[1][n] * done[1][v] for n in range(SUB)]
                    ref[rows_at(row0 + BASE, t), LANE * g : LANE * (g + 1)] -= stack_sums(parts)
            return carry

        lax.fori_loop(0, LANE // BASE, body, 0)


def kernel(n_row, n_col, batch_axis, a_ref, o_ref, share, diag, edge, stage, first, panel, work, winv, winv3, prev, load_sem, store_sem,
           seed_send, seed_recv, edge_send, edge_recv, first_sem, send_sem, pass_sem, recv_sem):
    row_blocks, size, local_cols = a_ref.shape
    col_blocks = local_cols // size
    ratio = n_col // n_row
    steps = row_blocks * n_row
    depth = pass_sem.shape[0]
    batch = lax.axis_index(batch_axis)
    row = lax.axis_index("row")
    col = lax.axis_index("col")
    odd = lax.rem(col, 2)
    on_diag = lax.rem(col, n_row) == row
    row_slots = n_row * (row_blocks * (row_blocks + 1) // 2)
    edge_slots = row_slots + n_col * (col_blocks * (col_blocks + 1) // 2)
    leads = row == LEAD

    def at(dev_row, dev_col):
        return (batch, dev_row, dev_col)

    def row_slot(k, a):
        g = k // n_row
        return n_row * (row_blocks * g - (g * (g - 1)) // 2) + (k - g * n_row) * (row_blocks - g) + a - g

    def col_slot(k, b):
        h = k // n_col
        return row_slots + n_col * (col_blocks * h - (h * (h - 1)) // 2) + (k - h * n_col) * (col_blocks - h) + b - h

    def first_a(k):
        return (k + n_row - row) // n_row

    def first_b(k):
        return (k + n_col - col) // n_col

    def home(ref, a, b):
        return ref.at[a, :, pl.ds(pl.multiple_of(b * size, size), size)]

    def spot(a, b):
        return b * row_blocks + a

    def col_of(k, b):
        return jnp.where(on_diag, row_slot(k, ratio * b + col // n_row), col_slot(k, b))

    def edge_slot(k, j):
        return edge_slots + 2 * k + (j - k - 1) // n_col

    def edge_reach(ahead):
        return jnp.logical_and(ahead >= 2, jnp.logical_and(ahead <= n_col + LAG, row != LEAD))

    def copy(src_slot, dst_slot, sem, device):
        return pltpu.make_async_remote_copy(
            src_ref=panel.at[src_slot], dst_ref=panel.at[dst_slot], send_sem=sem, recv_sem=recv_sem.at[dst_slot],
            device_id=device, device_id_type=MESH,
        )

    def arrived(slot):
        copy(slot, slot, send_sem.at[0, 0], at(row, col)).wait_recv()

    def start(c):
        c.start()

    def finish(c):
        c.wait_send()

    def from_maker(ahead, way):
        there = lax.rem(row + way, n_row)
        lead_near = jnp.logical_and(there == LEAD, jnp.logical_and(ahead >= 2, ahead <= n_row))
        soon_needed = jnp.logical_and(ahead == 2, way == 2)
        return jnp.logical_or(lead_near, soon_needed)

    def down_column(k, a, maker, sems, act):
        i = a * n_row + row
        slot = row_slot(k, a)
        dst = col_slot(k, i // n_col)
        for m, way in enumerate((1, n_row - 1, 2)):
            direct = from_maker(i - k, way)

            @pl.when(direct if maker else jnp.logical_not(direct))
            def _():
                act(copy(slot, dst, sems[m], at(lax.rem(row + way, n_row), lax.rem(i, n_col))))

    def to_edge(k, a, sem, act):
        i = a * n_row + row
        act(copy(row_slot(k, a), edge_slot(k, i - 1), sem, at(LEAD, lax.rem(i - 1, n_col))))

    def source_sends(k, a, act):
        ahead = a * n_row + row - k
        slot = row_slot(k, a)
        early = n_row

        @pl.when(jnp.logical_and(edge_reach(ahead), jnp.logical_or(ahead <= early, ahead == n_col)))
        def _():
            to_edge(k, a, send_sem.at[a, 5], act)

        @pl.when(jnp.logical_and(ahead >= 2, ahead <= early))
        def _():
            down_column(k, a, True, [send_sem.at[a, m] for m in range(3)], act)

        @pl.when(lax.rem(ahead, n_col) == 0)
        def _():
            down_column(k, a, False, [send_sem.at[a, m] for m in range(3)], act)

        @pl.when(jnp.logical_or(jnp.logical_and(odd == 0, ahead >= 2), ahead >= n_col - 1))
        def _():
            act(copy(slot, slot, send_sem.at[a, 3], at(row, lax.rem(jnp.where(odd == 0, col + 1, col - 1), n_col))))

        @pl.when(jnp.logical_and(odd == 1, ahead >= 2))
        def _():
            act(copy(slot, slot, send_sem.at[a, 6], at(row, lax.rem(col + 1, n_col))))

        @pl.when(ahead >= 2)
        def _():
            act(copy(slot, slot, send_sem.at[a, 4], at(row, lax.rem(col - odd + 3, n_col))))

        @pl.when(jnp.logical_and(odd == 1, jnp.logical_and(ahead >= n_col // 2 - 1, ahead < n_col - 3)))
        def _():
            act(copy(slot, slot, send_sem.at[a, 7], at(row, lax.rem(col + n_col // 2, n_col))))

        @pl.when(ahead >= n_col - 2 - odd)
        def _():
            act(copy(slot, slot, send_sem.at[a, 8], at(row, lax.rem(col - odd - 1 + n_col, n_col))))

    def lead(p):
        return lax.rem(col - lax.rem(p, n_col) + n_col, n_col)

    def hops(p):
        return lax.rem(col // 2 - lax.rem(p, n_col) // 2 + n_col // 2, n_col // 2)

    def passes(p):
        return jnp.logical_and(odd == 1, hops(p) != 0)

    def first_passed(p):
        low = jnp.where(passes(p), jnp.maximum(lead(p) - 1, 2), lead(p))
        return (p + low - row + n_row - 1) // n_row

    def pass_on(p, a, act):
        i = a * n_row + row
        ahead = i - p
        slot = row_slot(p, a)
        sems = pass_sem.at[lax.rem(p, depth), a]
        src_odd = lax.rem(p, 2)
        far = n_col - 2 - src_odd

        @pl.when(passes(p))
        def _():
            h = hops(p)
            via_prev = jnp.logical_or(src_odd == 1, jnp.logical_and(lax.rem(a, 2) == 1, ahead >= far))
            mine_to_pass = jnp.logical_or(
                jnp.logical_and(h == 1, jnp.logical_not(via_prev)), jnp.logical_and(h == n_col // 2 - 1, via_prev)
            )

            @pl.when(jnp.logical_and(mine_to_pass, ahead >= n_col // 2 - src_odd))
            def _():
                act(copy(slot, slot, sems.at[4], at(row, lax.rem(jnp.where(h == 1, col + 2, col - 2 + n_col), n_col))))

            @pl.when(jnp.logical_or(src_odd == 0, h != 1))
            def _():
                act(copy(slot, slot, sems.at[3], at(row, col - 1)))

        own = lax.rem(i, n_col) == col

        @pl.when(jnp.logical_and(own, jnp.logical_and(ahead > n_row, edge_reach(ahead))))
        def _():
            to_edge(p, a, sems.at[5], act)

        @pl.when(jnp.logical_and(own, ahead > 1))
        def _():
            down_column(p, a, False, [sems.at[m] for m in range(3)], act)

    def passed(p):
        @pl.when(lead(p) != 0)
        def _():
            loop(first_passed(p), row_blocks, lambda a: pass_on(p, a, finish))

    def receive(p, a):
        arrived(row_slot(p, a))
        pass_on(p, a, start)

    def loop(lo, hi, fn):
        lax.fori_loop(lo, hi, lambda n, c: (fn(n), c)[1], 0)

    for a in range(row_blocks):
        for b in range(col_blocks):
            pltpu.make_async_copy(home(a_ref, a, b), share.at[spot(a, b)], load_sem).start()

    barrier = pltpu.get_barrier_semaphore()
    n_dev = n_row * n_col

    def greet(n):
        other = lax.rem(row * n_col + col + n, n_dev)
        pl.semaphore_signal(barrier, inc=1, device_id=at(other // n_col, lax.rem(other, n_col)), device_id_type=MESH)

    loop(1, n_dev, greet)
    with jax.named_scope("all_here"):
        pl.semaphore_wait(barrier, n_dev - 1)
    with jax.named_scope("loaded"):
        pltpu.make_async_copy(share, share, load_sem).wait()

    def seed_copy(b, dev_row):
        return pltpu.make_async_remote_copy(
            src_ref=share.at[spot(ratio * b + col // n_row, b)], dst_ref=diag.at[b],
            send_sem=seed_send.at[b, lax.rem(dev_row - row + n_row, n_row)],
            recv_sem=seed_recv.at[b], device_id=at(dev_row, col), device_id_type=MESH,
        )

    def hand_out(b):
        @pl.when(on_diag)
        def _():
            for d in (1, n_row - 1, 2):
                seed_copy(b, lax.rem(row + d, n_row)).start()
            diag[b] = share[spot(ratio * b + col // n_row, b)]

        @pl.when(jnp.logical_and(holds_edge(b), jnp.logical_not(leads)))
        def _():
            stage[b] = share[spot((b * n_col + col + 1) // n_row, b)]
            edge_copy(b).start()

    def holds_edge(b):
        j = b * n_col + col
        return jnp.logical_and(lax.rem(j + 1, n_row) == row, j + 1 < steps)

    def edge_copy(b):
        return pltpu.make_async_remote_copy(
            src_ref=stage.at[b], dst_ref=edge.at[b], send_sem=edge_send.at[b], recv_sem=edge_recv.at[b],
            device_id=at(LEAD, col), device_id_type=MESH,
        )

    def has_edge(b):
        from_other = jnp.logical_and(leads, lax.rem(col + 1, n_row) != LEAD)
        return jnp.logical_and(from_other, b * n_col + col + 1 < steps)

    def edge_seeded(b):
        @pl.when(has_edge(b))
        def _():
            edge_copy(b).wait_recv()

    def edge_arrived(p, b):
        j = b * n_col + col

        @pl.when(jnp.logical_and(has_edge(b), j + 1 - p <= n_col + LAG))
        def _():
            arrived(edge_slot(p, j))

    hand_out(0)

    def seed_arrived(b):
        @pl.when(jnp.logical_not(on_diag))
        def _():
            seed_copy(b, row).wait_recv()

    with jax.named_scope("seed"):
        seed_arrived(0)

        @pl.when(col != 0)
        def _():
            edge_seeded(0)

    def clear(n):
        a, b = lax.rem(n, row_blocks), n // row_blocks

        @pl.when(a * n_row + row < b * n_col + col)
        def _():
            share[n] = jnp.zeros((size, size), F32)
            pltpu.make_async_copy(share.at[n], home(o_ref, a, b), store_sem).start()

    loop(0, row_blocks * col_blocks, clear)

    def times_t(x, y):
        return lax.dot_general(x, y, (((1,), (1,)), ((), ())), preferred_element_type=F32)

    def update_block(p, a, b):
        share[spot(a, b)] -= times_t(panel[row_slot(p, a)], panel[col_of(p, b)])

    def update_diag(p, b):
        other = panel[col_of(p, b)]
        diag[b] -= times_t(other, other)

    def update_edge(p, b):
        @pl.when(has_edge(b))
        def _():
            edge[b] -= times_t(panel[edge_slot(p, b * n_col + col)], panel[col_of(p, b)])

    def column_arrived(p, b):
        @pl.when(jnp.logical_not(on_diag))
        def _():
            arrived(col_slot(p, b))

    def update_column(p, b, lo):
        lone = lax.rem(row_blocks - lo, 2)

        @pl.when(lone == 1)
        def _():
            update_block(p, lo, b)

        def pair(m):
            a = lo + lone + 2 * m
            both = pl.ds(spot(a, b), 2)
            left = panel[pl.ds(row_slot(p, a), 2)].reshape(2 * size, size)
            share[both] -= times_t(left, panel[col_of(p, b)]).reshape(2, size, size)

        loop(0, (row_blocks - lo) // 2, pair)

    def trail(p, b_from, near):
        loop(b_from, col_blocks, lambda b: update_column(p, b, first_a(b * n_col + col - jnp.where(b == near, 0, 1))))

    def columns_arrived(p, b_from):
        def one(b):
            column_arrived(p, b)
            edge_arrived(p, b)

        loop(b_from, col_blocks, one)

    def prepare(b):
        work[size:, :] = jnp.zeros((BASE, size), F32)
        r_id = lax.broadcasted_iota(jnp.int32, (size + BASE, size), 0)
        c_id = lax.broadcasted_iota(jnp.int32, (size + BASE, size), 1)
        winv[...] = jnp.where(r_id == c_id, 1.0, 0.0).astype(F32)

    def times_winv_t(x):
        hi, mid, lo = split3(x)
        whi, wmid, wlo = winv3[0], winv3[1], winv3[2]
        small = times_t(lo, whi) + times_t(mid, wmid) + times_t(hi, wlo)
        return small + (times_t(mid, whi) + times_t(hi, wmid)) + times_t(hi, whi)

    def solve(k, a, count, near):
        kb = k // n_col
        here = pl.ds(spot(a, kb), count)

        def apply(p):
            left = panel[pl.ds(row_slot(p, a), count)].reshape(count * size, size)
            share[here] -= times_t(left, panel[col_of(p, kb)]).reshape(count, size, size)

        if not near:

            @pl.when(k > 1)
            def _():
                for m in range(count):
                    receive(k - 2, a + m)

            loop(jnp.maximum(k - 1 - LAG, 0), k - 1, apply)

        @pl.when(k > 0)
        def _():
            for m in range(count):
                receive(k - 1, a + m)
            apply(k - 1)

        x = times_winv_t(share[here].reshape(count * size, size)).reshape(count, size, size)
        panel[pl.ds(row_slot(k, a), count)] = x.astype(BF16)
        share[here] = x
        if near:

            @pl.when(jnp.logical_and(leads, lax.rem(k + 1, n_row) == LEAD))
            def _():
                first[...] = panel[row_slot(k, a)]
                first_out(k, start)

        for m in range(count):
            source_sends(k, a + m, start)
        for m in range(count):
            pltpu.make_async_copy(share.at[spot(a + m, kb)], home(o_ref, a + m, kb), store_sem).start()

    def update_near(p, b):
        update_diag(p, b)
        update_edge(p, b)

    def first_slot(k, dev_row):
        return jnp.where(lax.rem(k + 1, n_row) == dev_row, row_slot(k, (k + 1) // n_row), col_slot(k, (k + 1) // n_col))

    def first_copy(k, dev_row, sem):
        dst = first_slot(k, dev_row)
        return pltpu.make_async_remote_copy(
            src_ref=first, dst_ref=panel.at[dst], send_sem=sem, recv_sem=recv_sem.at[dst],
            device_id=at(dev_row, lax.rem(col + 1, n_col)), device_id_type=MESH,
        )

    def others_first(k, fn):
        urgent = lax.rem(k + 3, n_row)
        lone = urgent == LEAD
        for m in range(n_row - 1):
            fn(m, lax.rem(jnp.where(lone, LEAD + 1, urgent) + m + jnp.where(lax.rem(jnp.where(lone, LEAD + 1, urgent) - LEAD + n_row, n_row) + m >= n_row, 1, 0), n_row))

    def first_out(k, act):
        act(first_copy(k, LEAD, first_sem.at[0, 0]))

        @pl.when(odd == 0)
        def _():
            others_first(k, lambda m, r: act(first_copy(k, r, first_sem.at[0, 1 + m])))

    def first_down(k, act):
        @pl.when(odd == 0)
        def _():
            others_first(k, lambda m, r: act(copy(first_slot(k, LEAD), first_slot(k, r), first_sem.at[1, 1 + m], at(r, col))))

    def firsts_done(k):
        @pl.when(jnp.logical_and(leads, k + 1 < steps))
        def _():
            first_out(k, finish)

        @pl.when(jnp.logical_and(leads, k > 0))
        def _():
            first_down(k - 1, finish)

    @pl.when(col == 0)
    def _():
        prepare(0)
        work[0:size, :] = diag[0]

    def step(k):
        mine = col == lax.rem(k, n_col)
        kb = k // n_col
        last = k - 1
        soon = jnp.logical_and(col == lax.rem(k + 1, n_col), k + 1 < steps)

        @pl.when(mine)
        def _():
            with jax.named_scope("factor"):
                factor_block(work, winv, prev)
            for n, part in enumerate(split3(winv[0:size, :])):
                winv3[n] = part

            @pl.when(has_edge(kb))
            def _():
                with jax.named_scope("lead"):

                    @pl.when(k == 0)
                    def _():
                        edge_seeded(kb)

                    @pl.when(k > 0)
                    def _():
                        edge_arrived(last, kb)
                        update_edge(last, kb)

                    first[...] = times_winv_t(edge[kb]).astype(BF16)
                    first_out(k, start)

            lo = first_a(k)
            second = jnp.minimum(lo + 1, row_blocks)
            with jax.named_scope("solve_near"):
                loop(lo, second, lambda a: solve(k, a, 1, True))
            with jax.named_scope("solve_one"):
                third = second + lax.rem(row_blocks - second, 2)
                loop(second, third, lambda a: solve(k, a, 1, False))
            with jax.named_scope("solve_two"):
                loop(0, (row_blocks - third) // 2, lambda m: solve(k, third + 2 * m, 2, False))

        @pl.when(k >= depth)
        def _():
            with jax.named_scope("passed"):
                passed(k - depth)

        @pl.when(mine)
        def _():
            @pl.when(row == lax.rem(k, n_row))
            def _():
                for d in range(1, n_row):
                    seed_copy(kb, lax.rem(row + d, n_row)).wait_send()
                r_id = lax.broadcasted_iota(jnp.int32, (size, size), 0)
                c_id = lax.broadcasted_iota(jnp.int32, (size, size), 1)
                n = spot(k // n_row, kb)
                share[n] = jnp.where(r_id >= c_id, work[0:size, :].T, 0.0)
                pltpu.make_async_copy(share.at[n], home(o_ref, k // n_row, kb), store_sem).start()

            with jax.named_scope("late_trail"):

                def late(p):
                    columns_arrived(p, kb + 1)
                    trail(p, kb + 1, -1)

                loop(jnp.maximum(k - 1 - LAG, 0), k - LAG + 1, late)

            @pl.when(kb + 1 < col_blocks)
            def _():
                hand_out(kb + 1)

        @pl.when(jnp.logical_and(k > 0, jnp.logical_not(jnp.logical_or(mine, soon))))
        def _():
            @pl.when(col != lax.rem(last, n_col))
            def _():
                with jax.named_scope("receive"):
                    loop(first_passed(last), row_blocks, lambda a: receive(last, a))

            @pl.when(k >= LAG)
            def _():
                p = k - LAG
                near = first_b(k)
                with jax.named_scope("columns"):
                    columns_arrived(p, near)

                @pl.when(near < col_blocks)
                def _():
                    age = k + n_col - (near * n_col + col)

                    @pl.when(jnp.logical_and(age == 3, near > 0))
                    def _():
                        with jax.named_scope("seed_late"):
                            seed_arrived(near)
                            edge_seeded(near)

                    @pl.when(age >= 3)
                    def _():
                        oldest = jnp.where(age == 3, jnp.maximum(p - 2, 0), p)
                        loop(oldest, p + 1, lambda q: update_near(q, near))

                with jax.named_scope("trail"):
                    trail(p, near, near)

        @pl.when(soon)
        def _():
            nb = (k + 1) // n_col

            oldest = jnp.maximum(k - LAG, 0)

            def old_diag(p):
                column_arrived(p, nb)
                edge_arrived(p, nb)
                update_near(p, nb)

            def take(a):
                receive(last, a)

                @pl.when(a * n_row + row > k + 1)
                def _():
                    loop(oldest, last, lambda p: update_block(p, a, nb))

            @pl.when(k > 0)
            def _():
                with jax.named_scope("old_diag"):
                    loop(oldest, last, old_diag)
                with jax.named_scope("take"):
                    loop(first_a(k), jnp.minimum(first_a(k + 1) + 1, row_blocks), take)
                with jax.named_scope("take_column"):
                    column_arrived(last, nb)
                    edge_arrived(last, nb)
                with jax.named_scope("catch_up"):
                    update_near(last, nb)
                    loop(first_a(k + 1), jnp.minimum(first_a(k + 1) + 1, row_blocks), lambda a: update_block(last, a, nb))

            prepare(nb)
            slot = col_of(k, nb)
            with jax.named_scope("first_block"):
                arrived(slot)

            @pl.when(leads)
            def _():
                first_down(k, start)

            other = panel[slot]
            work[0:size, :] = diag[nb] - times_t(other, other)

        @pl.when(jnp.logical_and(k >= n_col // 2, col == lax.rem(k + n_col // 2, n_col)))
        def _():
            with jax.named_scope("sends_done"):
                firsts_done(k - n_col // 2)
                loop(first_a(k - n_col // 2), row_blocks, lambda a: source_sends(k - n_col // 2, a, finish))

    loop(0, steps, step)

    loop(steps - depth, steps, passed)

    def last_sends(k):
        @pl.when(col == lax.rem(k, n_col))
        def _():
            firsts_done(k)
            loop(first_a(k), row_blocks, lambda a: source_sends(k, a, finish))

    loop(steps - n_col // 2, steps, last_sends)

    def edges_done(b):
        @pl.when(jnp.logical_and(holds_edge(b), jnp.logical_not(leads)))
        def _():
            edge_copy(b).wait_send()

    loop(0, col_blocks, edges_done)
    with jax.named_scope("stored"):
        pltpu.make_async_copy(share, share, store_sem).wait()


def solution(mesh):
    n_row = mesh.shape["row"]
    n_col = mesh.shape["col"]

    def factor_local(a_loc):
        row_blocks, size, local_cols = a_loc.shape
        col_blocks = local_cols // size
        slots = n_row * (row_blocks * (row_blocks + 1) // 2) + n_col * (col_blocks * (col_blocks + 1) // 2)
        slots += 2 * row_blocks * n_row
        return pl.pallas_call(
            functools.partial(kernel, n_row, n_col, "batch"),
            out_shape=jax.ShapeDtypeStruct(a_loc.shape, F32),
            in_specs=[pl.BlockSpec(memory_space=pl.ANY)],
            out_specs=pl.BlockSpec(memory_space=pl.ANY),
            scratch_shapes=[
                pltpu.VMEM((row_blocks * col_blocks, size, size), F32),
                pltpu.VMEM((col_blocks, size, size), F32),
                pltpu.VMEM((col_blocks, size, size), F32),
                pltpu.VMEM((col_blocks, size, size), F32),
                pltpu.VMEM((size, size), BF16),
                pltpu.VMEM((slots, size, size), BF16),
                pltpu.VMEM((size + BASE, size), F32),
                pltpu.VMEM((size + BASE, size), F32),
                pltpu.VMEM((3, size, size), BF16),
                pltpu.VMEM((BASE, 3 * LANE), F32),
                pltpu.SemaphoreType.DMA,
                pltpu.SemaphoreType.DMA,
                pltpu.SemaphoreType.DMA((col_blocks, n_row)),
                pltpu.SemaphoreType.DMA((col_blocks,)),
                pltpu.SemaphoreType.DMA((col_blocks,)),
                pltpu.SemaphoreType.DMA((col_blocks,)),
                pltpu.SemaphoreType.DMA((2, n_row)),
                pltpu.SemaphoreType.DMA((row_blocks, 9)),
                pltpu.SemaphoreType.DMA((4, row_blocks, 6)),
                pltpu.SemaphoreType.DMA((slots,)),
            ],
            compiler_params=pltpu.CompilerParams(
                collective_id=0, has_side_effects=True, vmem_limit_bytes=60 * 1024 * 1024
            ),
            name="cholesky",
        )(a_loc)

    blk_spec = P(("batch", "row"), None, "col")
    return jax.shard_map(factor_local, mesh=mesh, in_specs=(blk_spec,), out_specs=blk_spec, check_vma=False)
```

```python
import functools

import jax
import jax.numpy as jnp
from jax import lax
from jax.experimental import pallas as pl
from jax.experimental.pallas import tpu as pltpu
from jax.sharding import PartitionSpec as P

F32 = jnp.float32
BF16 = jnp.bfloat16
MESH = pl.DeviceIdType.MESH
SUB = 8
LANE = 128
BASE = 16
LEAD = 1
LAG = 3


def sub_bcast(x, q):
    return jnp.broadcast_to(x[q : q + 1, :], (SUB, LANE))


ALONG_LANES = lax.GatherDimensionNumbers(
    offset_dims=(), collapsed_slice_dims=(1,), start_index_map=(1,), operand_batching_dims=(0,), start_indices_batching_dims=(0,)
)


def lane_bcast(x, lane):
    index = jnp.full((SUB, LANE, 1), lane, jnp.int32)
    return lax.gather(x, index, ALONG_LANES, (1, 1), mode=lax.GatherScatterMode.PROMISE_IN_BOUNDS)


def split3(x):
    high = x.astype(BF16)
    rest = x - high.astype(F32)
    mid = rest.astype(BF16)
    return high, mid, (rest - mid.astype(F32)).astype(BF16)


def swap_rows(x, bit, row_id):
    if bit == SUB // 2:
        return pltpu.roll(x, bit, 0)
    return jnp.where((row_id & bit) == 0, pltpu.roll(x, SUB - bit, 0), pltpu.roll(x, bit, 0))


def stack_sums(parts):
    row_id = lax.broadcasted_iota(jnp.int32, (SUB, LANE), 0)
    for bit in (4, 2, 1):
        low = (row_id & bit) == 0
        half = len(parts) // 2
        parts = [
            jnp.where(low, parts[n], parts[n + half]) + swap_rows(jnp.where(low, parts[n + half], parts[n]), bit, row_id)
            for n in range(half)
        ]
    return parts[0]


def eliminate(rows, lane0):
    row_id = lax.broadcasted_iota(jnp.int32, (SUB, LANE), 0)
    rows = [list(rows[0]), list(rows[1])]
    cols = [
        [lane_bcast(rows[0][0], lane0 + j) for j in range(SUB)],
        [lane_bcast(rows[1][0], lane0 + j) for j in range(BASE)],
    ]
    scale = [jnp.zeros((SUB, LANE), F32), jnp.zeros((SUB, LANE), F32)]
    pivot = sub_bcast(cols[0][0], 0)
    for j in range(BASE):
        t, q = divmod(j, SUB)
        inv = lax.rsqrt(pivot)
        scale[t] = jnp.where(row_id == q, inv, scale[t])
        if j + 1 < BASE:
            tn, qn = divmod(j + 1, SUB)
            near = sub_bcast(cols[tn][j], qn) * inv
            pivot = sub_bcast(cols[tn][j + 1], qn) - near * near
        below = cols[1][j] * inv
        here = cols[0][j] * inv if t == 0 else None
        for n in range(j + 1, BASE):
            tn, qn = divmod(n, SUB)
            other = near if n == j + 1 else sub_bcast(here if tn == 0 else below, qn)
            if t == 0 and tn == 0:
                cols[0][n] = cols[0][n] - here * other
            cols[1][n] = cols[1][n] - below * other
        masked = jnp.where(row_id > q, here if t == 0 else below, 0.0)
        for v in range(len(rows[0])):
            pivot_row = sub_bcast(rows[t][v], q) * inv
            rows[t][v] = rows[t][v] - masked * pivot_row
            if t == 0:
                rows[1][v] = rows[1][v] - below * pivot_row
    return [[x * scale[t] for x in rows[t]] for t in range(2)]


def factor_block(work, winv, winv3, prev, fac):
    size = work.shape[1]
    prev[...] = jnp.zeros(prev.shape, F32)
    fac[...] = jnp.zeros(fac.shape, F32)

    def group(v):
        return slice(LANE * v, LANE * (v + 1))

    def pending(factors, before, t, v):
        above, below = before[:SUB, group(v)], before[SUB:, group(v)]
        at = 2 * SUB * t
        return stack_sums([factors[at + n] * above + factors[at + SUB + n] * below for n in range(SUB)])

    for half in range(size // LANE):
        views = [(work, 0), (work, 1), (winv, 0)] if half == 0 else [(work, 1), (winv, 0), (winv, 1)]
        first = half * LANE
        if half == 1:
            factors, before = fac[...], prev[...]
            work[first : first + BASE, group(1)] -= jnp.concatenate([pending(factors, before, t, 1) for t in range(2)], axis=0)
            prev[...] = jnp.concatenate([before[:, group(1)], before[:, group(2)], jnp.zeros((BASE, LANE), F32)], axis=1)

        def body(s, carry, views=views, first=first):
            lane0 = s * BASE
            row0 = pl.multiple_of(first + lane0, BASE)

            here = pl.ds(row0, BASE)
            then = pl.ds(pl.multiple_of(row0 + BASE, BASE), BASE)
            both = [ref[here, group(g)] for ref, g in views]
            rows = [[x[SUB * t : SUB * (t + 1)] for x in both] for t in range(2)]
            factors, before = fac[...], prev[...]
            for t in range(2):
                for v in (1, 2):
                    rows[t][v] = rows[t][v] - pending(factors, before, t, v)
            hi, mid, lo = split3(before)
            lane = lax.broadcasted_iota(jnp.int32, (BASE, size - first), 1) + first
            after = lane >= row0 + BASE
            lhi, lmid, llo = [jnp.where(after, x[:, : size - first], jnp.zeros((), BF16)) for x in (hi, mid, lo)]
            update = lax.dot_general(
                jnp.concatenate([lhi, lhi, lmid, lhi, llo, lmid], axis=0),
                jnp.concatenate([hi, mid, hi, lo, hi, mid], axis=0),
                (((0,), (0,)), ((), ())),
                preferred_element_type=F32,
            )
            for v, (ref, g) in enumerate(views):
                ref[first:size, group(g)] -= update[:, group(v)]
            done = eliminate(rows, lane0)
            if first == 0:
                source = [jnp.where(s == LANE // BASE - 1, done[t][1], done[t][0]) for t in range(2)]
            else:
                source = [done[t][0] for t in range(2)]
            next_lane = (lane0 + BASE) % LANE
            factors, sums = [], []
            for t in range(2):
                factor = [[lane_bcast(source[m], next_lane + SUB * t + n) for n in range(SUB)] for m in range(2)]
                sums.append(stack_sums([factor[0][n] * done[0][0] + factor[1][n] * done[1][0] for n in range(SUB)]))
                factors += factor[0] + factor[1]
            ref, g = views[0]
            ref[then, group(g)] -= jnp.concatenate(sums, axis=0)
            fac[...] = jnp.stack(factors)
            whole = [jnp.concatenate([done[0][v], done[1][v]], axis=0) for v in range(3)]
            prev[...] = jnp.concatenate(whole, axis=1)
            for (ref, g), x in zip(views, whole):
                ref[here, group(g)] = x
                if ref is winv:
                    for n, part in enumerate(split3(x)):
                        winv3[n, here, group(g)] = part
            return carry

        lax.fori_loop(0, LANE // BASE, body, 0)


def kernel(n_row, n_col, batch_axis, a_ref, o_ref, share, diag, edge, stage, first, panel, work, winv, winv3, prev, fac, load_sem, store_sem,
           seed_send, seed_recv, edge_send, edge_recv, first_sem, send_sem, pass_sem, recv_sem):
    row_blocks, size, local_cols = a_ref.shape
    col_blocks = local_cols // size
    ratio = n_col // n_row
    steps = row_blocks * n_row
    depth = pass_sem.shape[0]
    batch = lax.axis_index(batch_axis)
    row = lax.axis_index("row")
    col = lax.axis_index("col")
    odd = lax.rem(col, 2)
    on_diag = lax.rem(col, n_row) == row
    row_slots = n_row * (row_blocks * (row_blocks + 1) // 2)
    edge_slots = row_slots + n_col * (col_blocks * (col_blocks + 1) // 2)
    leads = row == LEAD

    def at(dev_row, dev_col):
        return (batch, dev_row, dev_col)

    def row_slot(k, a):
        g = k // n_row
        return n_row * (row_blocks * g - (g * (g - 1)) // 2) + (k - g * n_row) * (row_blocks - g) + a - g

    def col_slot(k, b):
        h = k // n_col
        return row_slots + n_col * (col_blocks * h - (h * (h - 1)) // 2) + (k - h * n_col) * (col_blocks - h) + b - h

    def first_a(k):
        return (k + n_row - row) // n_row

    def first_b(k):
        return (k + n_col - col) // n_col

    def home(ref, a, b):
        return ref.at[a, :, pl.ds(pl.multiple_of(b * size, size), size)]

    def spot(a, b):
        return b * row_blocks + a

    def col_of(k, b):
        return jnp.where(on_diag, row_slot(k, ratio * b + col // n_row), col_slot(k, b))

    def edge_slot(k, j):
        return edge_slots + 2 * k + (j - k - 1) // n_col

    def edge_reach(ahead):
        return jnp.logical_and(ahead >= 2, jnp.logical_and(ahead <= n_col + LAG, row != LEAD))

    def copy(src_slot, dst_slot, sem, device):
        return pltpu.make_async_remote_copy(
            src_ref=panel.at[src_slot], dst_ref=panel.at[dst_slot], send_sem=sem, recv_sem=recv_sem.at[dst_slot],
            device_id=device, device_id_type=MESH,
        )

    def arrived(slot):
        copy(slot, slot, send_sem.at[0, 0], at(row, col)).wait_recv()

    def start(c):
        c.start()

    def finish(c):
        c.wait_send()

    def from_maker(ahead, way):
        there = lax.rem(row + way, n_row)
        lead_near = jnp.logical_and(there == LEAD, jnp.logical_and(ahead >= 2, ahead <= n_row))
        soon_needed = jnp.logical_and(ahead == 2, way == 2)
        return jnp.logical_or(lead_near, soon_needed)

    def down_column(k, a, maker, sems, act):
        i = a * n_row + row
        slot = row_slot(k, a)
        dst = col_slot(k, i // n_col)
        for m, way in enumerate((1, n_row - 1, 2)):
            direct = from_maker(i - k, way)

            @pl.when(direct if maker else jnp.logical_not(direct))
            def _():
                act(copy(slot, dst, sems[m], at(lax.rem(row + way, n_row), lax.rem(i, n_col))))

    def to_edge(k, a, sem, act):
        i = a * n_row + row
        act(copy(row_slot(k, a), edge_slot(k, i - 1), sem, at(LEAD, lax.rem(i - 1, n_col))))

    def source_sends(k, a, act):
        ahead = a * n_row + row - k
        slot = row_slot(k, a)
        early = n_row

        @pl.when(jnp.logical_and(edge_reach(ahead), jnp.logical_or(ahead <= early, ahead == n_col)))
        def _():
            to_edge(k, a, send_sem.at[a, 5], act)

        @pl.when(jnp.logical_and(ahead >= 2, ahead <= early))
        def _():
            down_column(k, a, True, [send_sem.at[a, m] for m in range(3)], act)

        @pl.when(lax.rem(ahead, n_col) == 0)
        def _():
            down_column(k, a, False, [send_sem.at[a, m] for m in range(3)], act)

        @pl.when(jnp.logical_or(jnp.logical_and(odd == 0, ahead >= 2), ahead >= n_col - 1))
        def _():
            act(copy(slot, slot, send_sem.at[a, 3], at(row, lax.rem(jnp.where(odd == 0, col + 1, col - 1), n_col))))

        @pl.when(jnp.logical_and(odd == 1, ahead >= 2))
        def _():
            act(copy(slot, slot, send_sem.at[a, 6], at(row, lax.rem(col + 1, n_col))))

        @pl.when(ahead >= 2)
        def _():
            act(copy(slot, slot, send_sem.at[a, 4], at(row, lax.rem(col - odd + 3, n_col))))

        @pl.when(jnp.logical_and(odd == 1, jnp.logical_and(ahead >= n_col // 2 - 1, ahead < n_col - 3)))
        def _():
            act(copy(slot, slot, send_sem.at[a, 7], at(row, lax.rem(col + n_col // 2, n_col))))

        @pl.when(ahead >= n_col - 2 - odd)
        def _():
            act(copy(slot, slot, send_sem.at[a, 8], at(row, lax.rem(col - odd - 1 + n_col, n_col))))

    def lead(p):
        return lax.rem(col - lax.rem(p, n_col) + n_col, n_col)

    def hops(p):
        return lax.rem(col // 2 - lax.rem(p, n_col) // 2 + n_col // 2, n_col // 2)

    def passes(p):
        return jnp.logical_and(odd == 1, hops(p) != 0)

    def first_passed(p):
        low = jnp.where(passes(p), jnp.maximum(lead(p) - 1, 2), lead(p))
        return (p + low - row + n_row - 1) // n_row

    def pass_on(p, a, act):
        i = a * n_row + row
        ahead = i - p
        slot = row_slot(p, a)
        sems = pass_sem.at[lax.rem(p, depth), a]
        src_odd = lax.rem(p, 2)
        far = n_col - 2 - src_odd

        @pl.when(passes(p))
        def _():
            h = hops(p)
            via_prev = jnp.logical_or(src_odd == 1, jnp.logical_and(lax.rem(a, 2) == 1, ahead >= far))
            mine_to_pass = jnp.logical_or(
                jnp.logical_and(h == 1, jnp.logical_not(via_prev)), jnp.logical_and(h == n_col // 2 - 1, via_prev)
            )

            @pl.when(jnp.logical_and(mine_to_pass, ahead >= n_col // 2 - src_odd))
            def _():
                act(copy(slot, slot, sems.at[4], at(row, lax.rem(jnp.where(h == 1, col + 2, col - 2 + n_col), n_col))))

            @pl.when(jnp.logical_or(src_odd == 0, h != 1))
            def _():
                act(copy(slot, slot, sems.at[3], at(row, col - 1)))

        own = lax.rem(i, n_col) == col

        @pl.when(jnp.logical_and(own, jnp.logical_and(ahead > n_row, edge_reach(ahead))))
        def _():
            to_edge(p, a, sems.at[5], act)

        @pl.when(jnp.logical_and(own, ahead > 1))
        def _():
            down_column(p, a, False, [sems.at[m] for m in range(3)], act)

    def passed(p):
        @pl.when(lead(p) != 0)
        def _():
            loop(first_passed(p), row_blocks, lambda a: pass_on(p, a, finish))

    def receive(p, a):
        arrived(row_slot(p, a))
        pass_on(p, a, start)

    def loop(lo, hi, fn):
        lax.fori_loop(lo, hi, lambda n, c: (fn(n), c)[1], 0)

    for a in range(row_blocks):
        for b in range(col_blocks):
            pltpu.make_async_copy(home(a_ref, a, b), share.at[spot(a, b)], load_sem).start()

    barrier = pltpu.get_barrier_semaphore()
    n_dev = n_row * n_col

    def greet(n):
        other = lax.rem(row * n_col + col + n, n_dev)
        pl.semaphore_signal(barrier, inc=1, device_id=at(other // n_col, lax.rem(other, n_col)), device_id_type=MESH)

    loop(1, n_dev, greet)
    with jax.named_scope("all_here"):
        pl.semaphore_wait(barrier, n_dev - 1)
    with jax.named_scope("loaded"):
        pltpu.make_async_copy(share, share, load_sem).wait()

    def seed_copy(b, dev_row):
        return pltpu.make_async_remote_copy(
            src_ref=share.at[spot(ratio * b + col // n_row, b)], dst_ref=diag.at[b],
            send_sem=seed_send.at[b, lax.rem(dev_row - row + n_row, n_row)],
            recv_sem=seed_recv.at[b], device_id=at(dev_row, col), device_id_type=MESH,
        )

    def hand_out(b):
        @pl.when(on_diag)
        def _():
            for d in (1, n_row - 1, 2):
                seed_copy(b, lax.rem(row + d, n_row)).start()
            diag[b] = share[spot(ratio * b + col // n_row, b)]

        @pl.when(jnp.logical_and(holds_edge(b), jnp.logical_not(leads)))
        def _():
            stage[b] = share[spot((b * n_col + col + 1) // n_row, b)]
            edge_copy(b).start()

    def holds_edge(b):
        j = b * n_col + col
        return jnp.logical_and(lax.rem(j + 1, n_row) == row, j + 1 < steps)

    def edge_copy(b):
        return pltpu.make_async_remote_copy(
            src_ref=stage.at[b], dst_ref=edge.at[b], send_sem=edge_send.at[b], recv_sem=edge_recv.at[b],
            device_id=at(LEAD, col), device_id_type=MESH,
        )

    def has_edge(b):
        from_other = jnp.logical_and(leads, lax.rem(col + 1, n_row) != LEAD)
        return jnp.logical_and(from_other, b * n_col + col + 1 < steps)

    def edge_seeded(b):
        @pl.when(has_edge(b))
        def _():
            edge_copy(b).wait_recv()

    def edge_arrived(p, b):
        j = b * n_col + col

        @pl.when(jnp.logical_and(has_edge(b), j + 1 - p <= n_col + LAG))
        def _():
            arrived(edge_slot(p, j))

    hand_out(0)
    winv3[...] = jnp.zeros(winv3.shape, BF16)

    def seed_arrived(b):
        @pl.when(jnp.logical_not(on_diag))
        def _():
            seed_copy(b, row).wait_recv()

    with jax.named_scope("seed"):
        seed_arrived(0)

        @pl.when(col != 0)
        def _():
            edge_seeded(0)

    def clear(n):
        a, b = lax.rem(n, row_blocks), n // row_blocks

        @pl.when(a * n_row + row < b * n_col + col)
        def _():
            share[n] = jnp.zeros((size, size), F32)
            pltpu.make_async_copy(share.at[n], home(o_ref, a, b), store_sem).start()

    loop(0, row_blocks * col_blocks, clear)

    def times_t(x, y):
        return lax.dot_general(x, y, (((1,), (1,)), ((), ())), preferred_element_type=F32)

    def update_block(p, a, b):
        share[spot(a, b)] -= times_t(panel[row_slot(p, a)], panel[col_of(p, b)])

    def update_diag(p, b):
        other = panel[col_of(p, b)]
        diag[b] -= times_t(other, other)

    def update_edge(p, b):
        @pl.when(has_edge(b))
        def _():
            edge[b] -= times_t(panel[edge_slot(p, b * n_col + col)], panel[col_of(p, b)])

    def column_arrived(p, b):
        @pl.when(jnp.logical_not(on_diag))
        def _():
            arrived(col_slot(p, b))

    def update_column(p, b, lo):
        lone = lax.rem(row_blocks - lo, 2)

        @pl.when(lone == 1)
        def _():
            update_block(p, lo, b)

        def pair(m):
            a = lo + lone + 2 * m
            both = pl.ds(spot(a, b), 2)
            left = panel[pl.ds(row_slot(p, a), 2)].reshape(2 * size, size)
            share[both] -= times_t(left, panel[col_of(p, b)]).reshape(2, size, size)

        loop(0, (row_blocks - lo) // 2, pair)

    def trail(p, b_from, near):
        loop(b_from, col_blocks, lambda b: update_column(p, b, first_a(b * n_col + col - jnp.where(b == near, 0, 1))))

    def columns_arrived(p, b_from):
        def one(b):
            column_arrived(p, b)
            edge_arrived(p, b)

        loop(b_from, col_blocks, one)

    def prepare(b):
        work[size:, :] = jnp.zeros((BASE, size), F32)
        r_id = lax.broadcasted_iota(jnp.int32, (size + BASE, size), 0)
        c_id = lax.broadcasted_iota(jnp.int32, (size + BASE, size), 1)
        winv[...] = jnp.where(r_id == c_id, 1.0, 0.0).astype(F32)

    def times_winv_t(x):
        hi, mid, lo = split3(x)
        whi, wmid, wlo = winv3[0], winv3[1], winv3[2]
        small = times_t(lo, whi) + times_t(mid, wmid) + times_t(hi, wlo)
        return small + (times_t(mid, whi) + times_t(hi, wmid)) + times_t(hi, whi)

    def solve(k, a, count, near):
        kb = k // n_col
        here = pl.ds(spot(a, kb), count)

        def apply(p):
            left = panel[pl.ds(row_slot(p, a), count)].reshape(count * size, size)
            share[here] -= times_t(left, panel[col_of(p, kb)]).reshape(count, size, size)

        if not near:

            @pl.when(k > 1)
            def _():
                for m in range(count):
                    receive(k - 2, a + m)

            loop(jnp.maximum(k - 1 - LAG, 0), k - 1, apply)

        @pl.when(k > 0)
        def _():
            for m in range(count):
                receive(k - 1, a + m)
            apply(k - 1)

        x = times_winv_t(share[here].reshape(count * size, size)).reshape(count, size, size)
        panel[pl.ds(row_slot(k, a), count)] = x.astype(BF16)
        share[here] = x
        if near:

            @pl.when(jnp.logical_and(leads, lax.rem(k + 1, n_row) == LEAD))
            def _():
                first[...] = panel[row_slot(k, a)]
                first_out(k, start)

        for m in range(count):
            source_sends(k, a + m, start)
        for m in range(count):
            pltpu.make_async_copy(share.at[spot(a + m, kb)], home(o_ref, a + m, kb), store_sem).start()

    def update_near(p, b):
        update_diag(p, b)
        update_edge(p, b)

    def first_slot(k, dev_row):
        return jnp.where(lax.rem(k + 1, n_row) == dev_row, row_slot(k, (k + 1) // n_row), col_slot(k, (k + 1) // n_col))

    def first_copy(k, dev_row, sem):
        dst = first_slot(k, dev_row)
        return pltpu.make_async_remote_copy(
            src_ref=first, dst_ref=panel.at[dst], send_sem=sem, recv_sem=recv_sem.at[dst],
            device_id=at(dev_row, lax.rem(col + 1, n_col)), device_id_type=MESH,
        )

    def others_first(k, fn):
        urgent = lax.rem(k + 3, n_row)
        lone = urgent == LEAD
        for m in range(n_row - 1):
            fn(m, lax.rem(jnp.where(lone, LEAD + 1, urgent) + m + jnp.where(lax.rem(jnp.where(lone, LEAD + 1, urgent) - LEAD + n_row, n_row) + m >= n_row, 1, 0), n_row))

    def first_out(k, act):
        act(first_copy(k, LEAD, first_sem.at[0, 0]))

        @pl.when(odd == 0)
        def _():
            others_first(k, lambda m, r: act(first_copy(k, r, first_sem.at[0, 1 + m])))

    def first_down(k, act):
        @pl.when(odd == 0)
        def _():
            others_first(k, lambda m, r: act(copy(first_slot(k, LEAD), first_slot(k, r), first_sem.at[1, 1 + m], at(r, col))))

    def firsts_done(k):
        @pl.when(jnp.logical_and(leads, k + 1 < steps))
        def _():
            first_out(k, finish)

        @pl.when(jnp.logical_and(leads, k > 0))
        def _():
            first_down(k - 1, finish)

    @pl.when(col == 0)
    def _():
        prepare(0)
        work[0:size, :] = diag[0]

    def step(k):
        mine = col == lax.rem(k, n_col)
        kb = k // n_col
        last = k - 1
        soon = jnp.logical_and(col == lax.rem(k + 1, n_col), k + 1 < steps)

        @pl.when(mine)
        def _():
            with jax.named_scope("factor"):
                factor_block(work, winv, winv3, prev, fac)

            @pl.when(has_edge(kb))
            def _():
                with jax.named_scope("lead"):

                    @pl.when(k == 0)
                    def _():
                        edge_seeded(kb)

                    @pl.when(k > 0)
                    def _():
                        edge_arrived(last, kb)
                        update_edge(last, kb)

                    first[...] = times_winv_t(edge[kb]).astype(BF16)
                    first_out(k, start)

            lo = first_a(k)
            second = jnp.minimum(lo + 1, row_blocks)
            with jax.named_scope("solve_near"):
                loop(lo, second, lambda a: solve(k, a, 1, True))
            with jax.named_scope("solve_one"):
                third = second + lax.rem(row_blocks - second, 2)
                loop(second, third, lambda a: solve(k, a, 1, False))
            with jax.named_scope("solve_two"):
                loop(0, (row_blocks - third) // 2, lambda m: solve(k, third + 2 * m, 2, False))

        @pl.when(k >= depth)
        def _():
            with jax.named_scope("passed"):
                passed(k - depth)

        @pl.when(mine)
        def _():
            @pl.when(row == lax.rem(k, n_row))
            def _():
                for d in range(1, n_row):
                    seed_copy(kb, lax.rem(row + d, n_row)).wait_send()
                r_id = lax.broadcasted_iota(jnp.int32, (size, size), 0)
                c_id = lax.broadcasted_iota(jnp.int32, (size, size), 1)
                n = spot(k // n_row, kb)
                share[n] = jnp.where(r_id >= c_id, work[0:size, :].T, 0.0)
                pltpu.make_async_copy(share.at[n], home(o_ref, k // n_row, kb), store_sem).start()

            with jax.named_scope("late_trail"):

                def late(p):
                    columns_arrived(p, kb + 1)
                    trail(p, kb + 1, -1)

                loop(jnp.maximum(k - 1 - LAG, 0), k - LAG + 1, late)

            @pl.when(kb + 1 < col_blocks)
            def _():
                hand_out(kb + 1)

        @pl.when(jnp.logical_and(k > 0, jnp.logical_not(jnp.logical_or(mine, soon))))
        def _():
            @pl.when(col != lax.rem(last, n_col))
            def _():
                with jax.named_scope("receive"):
                    loop(first_passed(last), row_blocks, lambda a: receive(last, a))

            @pl.when(k >= LAG)
            def _():
                p = k - LAG
                near = first_b(k)
                with jax.named_scope("columns"):
                    columns_arrived(p, near)

                @pl.when(near < col_blocks)
                def _():
                    age = k + n_col - (near * n_col + col)

                    @pl.when(jnp.logical_and(age == 3, near > 0))
                    def _():
                        with jax.named_scope("seed_late"):
                            seed_arrived(near)
                            edge_seeded(near)

                    @pl.when(age >= 3)
                    def _():
                        oldest = jnp.where(age == 3, jnp.maximum(p - 2, 0), p)
                        loop(oldest, p + 1, lambda q: update_near(q, near))

                with jax.named_scope("trail"):
                    trail(p, near, near)

        @pl.when(soon)
        def _():
            nb = (k + 1) // n_col

            oldest = jnp.maximum(k - LAG, 0)

            def old_diag(p):
                column_arrived(p, nb)
                edge_arrived(p, nb)
                update_near(p, nb)

            def take(a):
                receive(last, a)

                @pl.when(a * n_row + row > k + 1)
                def _():
                    loop(oldest, last, lambda p: update_block(p, a, nb))

            @pl.when(k > 0)
            def _():
                with jax.named_scope("old_diag"):
                    loop(oldest, last, old_diag)
                with jax.named_scope("take"):
                    loop(first_a(k), jnp.minimum(first_a(k + 1) + 1, row_blocks), take)
                with jax.named_scope("take_column"):
                    column_arrived(last, nb)
                    edge_arrived(last, nb)
                with jax.named_scope("catch_up"):
                    update_near(last, nb)
                    loop(first_a(k + 1), jnp.minimum(first_a(k + 1) + 1, row_blocks), lambda a: update_block(last, a, nb))

            prepare(nb)
            slot = col_of(k, nb)
            with jax.named_scope("first_block"):
                arrived(slot)

            @pl.when(leads)
            def _():
                first_down(k, start)

            other = panel[slot]
            work[0:size, :] = diag[nb] - times_t(other, other)

        @pl.when(jnp.logical_and(k >= n_col // 2, col == lax.rem(k + n_col // 2, n_col)))
        def _():
            with jax.named_scope("sends_done"):
                firsts_done(k - n_col // 2)
                loop(first_a(k - n_col // 2), row_blocks, lambda a: source_sends(k - n_col // 2, a, finish))

    loop(0, steps, step)

    loop(steps - depth, steps, passed)

    def last_sends(k):
        @pl.when(col == lax.rem(k, n_col))
        def _():
            firsts_done(k)
            loop(first_a(k), row_blocks, lambda a: source_sends(k, a, finish))

    loop(steps - n_col // 2, steps, last_sends)

    def edges_done(b):
        @pl.when(jnp.logical_and(holds_edge(b), jnp.logical_not(leads)))
        def _():
            edge_copy(b).wait_send()

    loop(0, col_blocks, edges_done)
    with jax.named_scope("stored"):
        pltpu.make_async_copy(share, share, store_sem).wait()


def solution(mesh):
    n_row = mesh.shape["row"]
    n_col = mesh.shape["col"]

    def factor_local(a_loc):
        row_blocks, size, local_cols = a_loc.shape
        col_blocks = local_cols // size
        slots = n_row * (row_blocks * (row_blocks + 1) // 2) + n_col * (col_blocks * (col_blocks + 1) // 2)
        slots += 2 * row_blocks * n_row
        return pl.pallas_call(
            functools.partial(kernel, n_row, n_col, "batch"),
            out_shape=jax.ShapeDtypeStruct(a_loc.shape, F32),
            in_specs=[pl.BlockSpec(memory_space=pl.ANY)],
            out_specs=pl.BlockSpec(memory_space=pl.ANY),
            scratch_shapes=[
                pltpu.VMEM((row_blocks * col_blocks, size, size), F32),
                pltpu.VMEM((col_blocks, size, size), F32),
                pltpu.VMEM((col_blocks, size, size), F32),
                pltpu.VMEM((col_blocks, size, size), F32),
                pltpu.VMEM((size, size), BF16),
                pltpu.VMEM((slots, size, size), BF16),
                pltpu.VMEM((size + BASE, size), F32),
                pltpu.VMEM((size + BASE, size), F32),
                pltpu.VMEM((3, size, size), BF16),
                pltpu.VMEM((BASE, 3 * LANE), F32),
                pltpu.VMEM((4 * SUB, SUB, LANE), F32),
                pltpu.SemaphoreType.DMA,
                pltpu.SemaphoreType.DMA,
                pltpu.SemaphoreType.DMA((col_blocks, n_row)),
                pltpu.SemaphoreType.DMA((col_blocks,)),
                pltpu.SemaphoreType.DMA((col_blocks,)),
                pltpu.SemaphoreType.DMA((col_blocks,)),
                pltpu.SemaphoreType.DMA((2, n_row)),
                pltpu.SemaphoreType.DMA((row_blocks, 9)),
                pltpu.SemaphoreType.DMA((4, row_blocks, 6)),
                pltpu.SemaphoreType.DMA((slots,)),
            ],
            compiler_params=pltpu.CompilerParams(
                collective_id=0, has_side_effects=True, vmem_limit_bytes=60 * 1024 * 1024
            ),
            name="cholesky",
        )(a_loc)

    blk_spec = P(("batch", "row"), None, "col")
    return jax.shard_map(factor_local, mesh=mesh, in_specs=(blk_spec,), out_specs=blk_spec, check_vma=False)
```

```python
import functools

import jax
import jax.numpy as jnp
from jax import lax
from jax.experimental import pallas as pl
from jax.experimental.pallas import tpu as pltpu
from jax.sharding import PartitionSpec as P

F32 = jnp.float32
BF16 = jnp.bfloat16
MESH = pl.DeviceIdType.MESH
SUB = 8
LANE = 128
BASE = 16
LEAD = 1
LAG = 3


def sub_bcast(x, q):
    return jnp.broadcast_to(x[q : q + 1, :], (SUB, LANE))


ALONG_LANES = lax.GatherDimensionNumbers(
    offset_dims=(), collapsed_slice_dims=(1,), start_index_map=(1,), operand_batching_dims=(0,), start_indices_batching_dims=(0,)
)


def lane_bcast(x, lane):
    index = jnp.full((SUB, LANE, 1), lane, jnp.int32)
    return lax.gather(x, index, ALONG_LANES, (1, 1), mode=lax.GatherScatterMode.PROMISE_IN_BOUNDS)


def split3(x):
    high = x.astype(BF16)
    rest = x - high.astype(F32)
    mid = rest.astype(BF16)
    return high, mid, (rest - mid.astype(F32)).astype(BF16)


def swap_rows(x, bit, row_id):
    if bit == SUB // 2:
        return pltpu.roll(x, bit, 0)
    return jnp.where((row_id & bit) == 0, pltpu.roll(x, SUB - bit, 0), pltpu.roll(x, bit, 0))


def stack_sums(parts):
    row_id = lax.broadcasted_iota(jnp.int32, (SUB, LANE), 0)
    for bit in (4, 2, 1):
        low = (row_id & bit) == 0
        half = len(parts) // 2
        parts = [
            jnp.where(low, parts[n], parts[n + half]) + swap_rows(jnp.where(low, parts[n + half], parts[n]), bit, row_id)
            for n in range(half)
        ]
    return parts[0]


def eliminate(rows, lane0):
    row_id = lax.broadcasted_iota(jnp.int32, (SUB, LANE), 0)
    rows = [list(rows[0]), list(rows[1])]
    cols = [
        [lane_bcast(rows[0][0], lane0 + j) for j in range(SUB)],
        [lane_bcast(rows[1][0], lane0 + j) for j in range(BASE)],
    ]
    scale = [jnp.zeros((SUB, LANE), F32), jnp.zeros((SUB, LANE), F32)]
    pivot = sub_bcast(cols[0][0], 0)
    for j in range(BASE):
        t, q = divmod(j, SUB)
        inv = lax.rsqrt(pivot)
        scale[t] = jnp.where(row_id == q, inv, scale[t])
        if j + 1 < BASE:
            tn, qn = divmod(j + 1, SUB)
            near = sub_bcast(cols[tn][j], qn) * inv
            pivot = sub_bcast(cols[tn][j + 1], qn) - near * near
        below = cols[1][j] * inv
        here = cols[0][j] * inv if t == 0 else None
        for n in range(j + 1, BASE):
            tn, qn = divmod(n, SUB)
            other = near if n == j + 1 else sub_bcast(here if tn == 0 else below, qn)
            if t == 0 and tn == 0:
                cols[0][n] = cols[0][n] - here * other
            cols[1][n] = cols[1][n] - below * other
        masked = jnp.where(row_id > q, here if t == 0 else below, 0.0)
        for v in range(len(rows[0])):
            pivot_row = sub_bcast(rows[t][v], q) * inv
            rows[t][v] = rows[t][v] - masked * pivot_row
            if t == 0:
                rows[1][v] = rows[1][v] - below * pivot_row
    return [[x * scale[t] for x in rows[t]] for t in range(2)]


def factor_block(work, winv, winv3, prev, fac):
    size = work.shape[1]
    prev[...] = jnp.zeros(prev.shape, F32)
    fac[...] = jnp.zeros(fac.shape, F32)

    def group(v):
        return slice(LANE * v, LANE * (v + 1))

    def pending(factors, before, t, v):
        above, below = before[:SUB, group(v)], before[SUB:, group(v)]
        at = 2 * SUB * t
        return stack_sums([factors[at + n] * above + factors[at + SUB + n] * below for n in range(SUB)])

    for half in range(size // LANE):
        views = [(work, 0), (work, 1), (winv, 0)] if half == 0 else [(work, 1), (winv, 0), (winv, 1)]
        first = half * LANE
        if half == 1:
            factors, before = fac[...], prev[...]
            work[first : first + BASE, group(1)] -= jnp.concatenate([pending(factors, before, t, 1) for t in range(2)], axis=0)
            prev[...] = jnp.concatenate([before[:, group(1)], before[:, group(2)], jnp.zeros((BASE, LANE), F32)], axis=1)

        def body(s, carry, views=views, first=first):
            lane0 = s * BASE
            row0 = pl.multiple_of(first + lane0, BASE)

            here = pl.ds(row0, BASE)
            then = pl.ds(pl.multiple_of(row0 + BASE, BASE), BASE)
            both = [ref[here, group(g)] for ref, g in views]
            rows = [[x[SUB * t : SUB * (t + 1)] for x in both] for t in range(2)]
            factors, before = fac[...], prev[...]
            for t in range(2):
                for v in (1, 2):
                    rows[t][v] = rows[t][v] - pending(factors, before, t, v)
            hi, mid, lo = split3(before)
            lane = lax.broadcasted_iota(jnp.int32, (BASE, size - first), 1) + first
            after = lane >= row0 + BASE
            lhi, lmid, llo = [jnp.where(after, x[:, : size - first], jnp.zeros((), BF16)) for x in (hi, mid, lo)]
            update = lax.dot_general(
                jnp.concatenate([lhi, lhi, lmid, lhi, llo, lmid], axis=0),
                jnp.concatenate([hi, mid, hi, lo, hi, mid], axis=0),
                (((0,), (0,)), ((), ())),
                preferred_element_type=F32,
            )
            for v, (ref, g) in enumerate(views):
                ref[first:size, group(g)] -= update[:, group(v)]
            done = eliminate(rows, lane0)
            if first == 0:
                source = [jnp.where(s == LANE // BASE - 1, done[t][1], done[t][0]) for t in range(2)]
            else:
                source = [done[t][0] for t in range(2)]
            next_lane = (lane0 + BASE) % LANE
            factors, sums = [], []
            for t in range(2):
                factor = [[lane_bcast(source[m], next_lane + SUB * t + n) for n in range(SUB)] for m in range(2)]
                sums.append(stack_sums([factor[0][n] * done[0][0] + factor[1][n] * done[1][0] for n in range(SUB)]))
                factors += factor[0] + factor[1]
            ref, g = views[0]
            ref[then, group(g)] -= jnp.concatenate(sums, axis=0)
            fac[...] = jnp.stack(factors)
            whole = [jnp.concatenate([done[0][v], done[1][v]], axis=0) for v in range(3)]
            prev[...] = jnp.concatenate(whole, axis=1)
            for (ref, g), x in zip(views, whole):
                ref[here, group(g)] = x
                if ref is winv:
                    for n, part in enumerate(split3(x)):
                        winv3[n, here, group(g)] = part
            return carry

        lax.fori_loop(0, LANE // BASE, body, 0)


def kernel(n_row, n_col, batch_axis, a_ref, o_ref, share, diag, edge, stage, first, panel, work, winv, winv3, prev, fac, load_sem, store_sem,
           seed_send, seed_recv, edge_send, edge_recv, first_sem, send_sem, pass_sem, recv_sem):
    row_blocks, size, local_cols = a_ref.shape
    col_blocks = local_cols // size
    ratio = n_col // n_row
    steps = row_blocks * n_row
    depth = pass_sem.shape[0]
    batch = lax.axis_index(batch_axis)
    row = lax.axis_index("row")
    col = lax.axis_index("col")
    odd = lax.rem(col, 2)
    on_diag = lax.rem(col, n_row) == row
    row_slots = n_row * (row_blocks * (row_blocks + 1) // 2)
    edge_slots = row_slots + n_col * (col_blocks * (col_blocks + 1) // 2)
    leads = row == LEAD

    def at(dev_row, dev_col):
        return (batch, dev_row, dev_col)

    def row_slot(k, a):
        g = k // n_row
        return n_row * (row_blocks * g - (g * (g - 1)) // 2) + (k - g * n_row) * (row_blocks - g) + a - g

    def col_slot(k, b):
        h = k // n_col
        return row_slots + n_col * (col_blocks * h - (h * (h - 1)) // 2) + (k - h * n_col) * (col_blocks - h) + b - h

    def first_a(k):
        return (k + n_row - row) // n_row

    def first_b(k):
        return (k + n_col - col) // n_col

    def home(ref, a, b):
        return ref.at[a, :, pl.ds(pl.multiple_of(b * size, size), size)]

    def spot(a, b):
        return b * row_blocks + a

    def col_of(k, b):
        return jnp.where(on_diag, row_slot(k, ratio * b + col // n_row), col_slot(k, b))

    def edge_slot(k, j):
        return edge_slots + 2 * k + (j - k - 1) // n_col

    def edge_reach(ahead):
        return jnp.logical_and(ahead >= 2, jnp.logical_and(ahead <= n_col + LAG, row != LEAD))

    def copy(src_slot, dst_slot, sem, device):
        return pltpu.make_async_remote_copy(
            src_ref=panel.at[src_slot], dst_ref=panel.at[dst_slot], send_sem=sem, recv_sem=recv_sem.at[dst_slot],
            device_id=device, device_id_type=MESH,
        )

    def arrived(slot):
        copy(slot, slot, send_sem.at[0, 0], at(row, col)).wait_recv()

    def start(c):
        c.start()

    def finish(c):
        c.wait_send()

    def from_maker(ahead, way):
        there = lax.rem(row + way, n_row)
        lead_near = jnp.logical_and(there == LEAD, jnp.logical_and(ahead >= 2, ahead <= n_row))
        soon_needed = jnp.logical_and(ahead == 2, way == 2)
        return jnp.logical_or(lead_near, soon_needed)

    def down_column(k, a, maker, sems, act):
        i = a * n_row + row
        slot = row_slot(k, a)
        dst = col_slot(k, i // n_col)
        for m, way in enumerate((1, n_row - 1, 2)):
            direct = from_maker(i - k, way)

            @pl.when(direct if maker else jnp.logical_not(direct))
            def _():
                act(copy(slot, dst, sems[m], at(lax.rem(row + way, n_row), lax.rem(i, n_col))))

    def to_edge(k, a, sem, act):
        i = a * n_row + row
        act(copy(row_slot(k, a), edge_slot(k, i - 1), sem, at(LEAD, lax.rem(i - 1, n_col))))

    def source_sends(k, a, act):
        ahead = a * n_row + row - k
        slot = row_slot(k, a)
        early = n_row

        @pl.when(jnp.logical_and(edge_reach(ahead), jnp.logical_or(ahead <= early, ahead == n_col)))
        def _():
            to_edge(k, a, send_sem.at[a, 5], act)

        @pl.when(jnp.logical_and(ahead >= 2, ahead <= early))
        def _():
            down_column(k, a, True, [send_sem.at[a, m] for m in range(3)], act)

        @pl.when(lax.rem(ahead, n_col) == 0)
        def _():
            down_column(k, a, False, [send_sem.at[a, m] for m in range(3)], act)

        @pl.when(jnp.logical_or(jnp.logical_and(odd == 0, ahead >= 2), ahead >= n_col - 1))
        def _():
            act(copy(slot, slot, send_sem.at[a, 3], at(row, lax.rem(jnp.where(odd == 0, col + 1, col - 1), n_col))))

        @pl.when(ahead >= 2)
        def _():
            act(copy(slot, slot, send_sem.at[a, 6], at(row, lax.rem(col - odd + 2, n_col))))

        @pl.when(ahead >= 3 - odd)
        def _():
            act(copy(slot, slot, send_sem.at[a, 4], at(row, lax.rem(col - odd + 3, n_col))))

        @pl.when(jnp.logical_and(ahead >= n_col // 2 - odd, ahead < n_col - 2 - odd))
        def _():
            act(copy(slot, slot, send_sem.at[a, 7], at(row, lax.rem(col - odd + 5, n_col))))

        @pl.when(ahead >= n_col - 2 - odd)
        def _():
            act(copy(slot, slot, send_sem.at[a, 8], at(row, lax.rem(col - odd - 1 + n_col, n_col))))

    def lead(p):
        return lax.rem(col - lax.rem(p, n_col) + n_col, n_col)

    def hops(p):
        return lax.rem(col // 2 - lax.rem(p, n_col) // 2 + n_col // 2, n_col // 2)

    def passes(p):
        return jnp.logical_and(odd == 1, hops(p) > 1)

    def first_passed(p):
        low = jnp.where(passes(p), jnp.maximum(lead(p) - 1, 2), lead(p))
        return (p + low - row + n_row - 1) // n_row

    def pass_down(p, a, act):
        i = a * n_row + row
        ahead = i - p
        sems = pass_sem.at[lax.rem(p, depth), a]

        @pl.when(jnp.logical_and(lax.rem(i, n_col) == col, ahead > 1))
        def _():
            @pl.when(jnp.logical_and(ahead > n_row, edge_reach(ahead)))
            def _():
                to_edge(p, a, sems.at[5], act)

            down_column(p, a, False, [sems.at[m] for m in range(3)], act)

    def pass_on(p, a, act):
        slot = row_slot(p, a)
        sems = pass_sem.at[lax.rem(p, depth), a]

        @pl.when(passes(p))
        def _():
            @pl.when(hops(p) == n_col // 2 - 1)
            def _():
                act(copy(slot, slot, sems.at[4], at(row, lax.rem(col - 2 + n_col, n_col))))

            act(copy(slot, slot, sems.at[3], at(row, col - 1)))

        pass_down(p, a, act)

    def passed(p):
        @pl.when(lead(p) != 0)
        def _():
            loop(first_passed(p), row_blocks, lambda a: pass_on(p, a, finish))

    def receive(p, a):
        arrived(row_slot(p, a))
        pass_down(p, a, start)

    def receive_any(p, a):
        arrived(row_slot(p, a))
        pass_on(p, a, start)

    def last_near(p):
        return first_a(p + 2)

    def loop(lo, hi, fn):
        lax.fori_loop(lo, hi, lambda n, c: (fn(n), c)[1], 0)

    for a in range(row_blocks):
        for b in range(col_blocks):
            pltpu.make_async_copy(home(a_ref, a, b), share.at[spot(a, b)], load_sem).start()

    barrier = pltpu.get_barrier_semaphore()
    n_dev = n_row * n_col

    def greet(n):
        other = lax.rem(row * n_col + col + n, n_dev)
        pl.semaphore_signal(barrier, inc=1, device_id=at(other // n_col, lax.rem(other, n_col)), device_id_type=MESH)

    loop(1, n_dev, greet)
    with jax.named_scope("all_here"):
        pl.semaphore_wait(barrier, n_dev - 1)
    with jax.named_scope("loaded"):
        pltpu.make_async_copy(share, share, load_sem).wait()

    def seed_copy(b, dev_row):
        return pltpu.make_async_remote_copy(
            src_ref=share.at[spot(ratio * b + col // n_row, b)], dst_ref=diag.at[b],
            send_sem=seed_send.at[b, lax.rem(dev_row - row + n_row, n_row)],
            recv_sem=seed_recv.at[b], device_id=at(dev_row, col), device_id_type=MESH,
        )

    def hand_out(b):
        @pl.when(on_diag)
        def _():
            for d in (1, n_row - 1, 2):
                seed_copy(b, lax.rem(row + d, n_row)).start()
            diag[b] = share[spot(ratio * b + col // n_row, b)]

        @pl.when(jnp.logical_and(holds_edge(b), jnp.logical_not(leads)))
        def _():
            stage[b] = share[spot((b * n_col + col + 1) // n_row, b)]
            edge_copy(b).start()

    def holds_edge(b):
        j = b * n_col + col
        return jnp.logical_and(lax.rem(j + 1, n_row) == row, j + 1 < steps)

    def edge_copy(b):
        return pltpu.make_async_remote_copy(
            src_ref=stage.at[b], dst_ref=edge.at[b], send_sem=edge_send.at[b], recv_sem=edge_recv.at[b],
            device_id=at(LEAD, col), device_id_type=MESH,
        )

    def has_edge(b):
        from_other = jnp.logical_and(leads, lax.rem(col + 1, n_row) != LEAD)
        return jnp.logical_and(from_other, b * n_col + col + 1 < steps)

    def edge_seeded(b):
        @pl.when(has_edge(b))
        def _():
            edge_copy(b).wait_recv()

    def edge_arrived(p, b):
        j = b * n_col + col

        @pl.when(jnp.logical_and(has_edge(b), j + 1 - p <= n_col + LAG))
        def _():
            arrived(edge_slot(p, j))

    hand_out(0)
    winv3[...] = jnp.zeros(winv3.shape, BF16)

    def seed_arrived(b):
        @pl.when(jnp.logical_not(on_diag))
        def _():
            seed_copy(b, row).wait_recv()

    with jax.named_scope("seed"):
        seed_arrived(0)

        @pl.when(col != 0)
        def _():
            edge_seeded(0)

    def clear(n):
        a, b = lax.rem(n, row_blocks), n // row_blocks

        @pl.when(a * n_row + row < b * n_col + col)
        def _():
            share[n] = jnp.zeros((size, size), F32)
            pltpu.make_async_copy(share.at[n], home(o_ref, a, b), store_sem).start()

    loop(0, row_blocks * col_blocks, clear)

    def times_t(x, y):
        return lax.dot_general(x, y, (((1,), (1,)), ((), ())), preferred_element_type=F32)

    def update_block(p, a, b):
        share[spot(a, b)] -= times_t(panel[row_slot(p, a)], panel[col_of(p, b)])

    def update_diag(p, b):
        other = panel[col_of(p, b)]
        diag[b] -= times_t(other, other)

    def update_edge(p, b):
        @pl.when(has_edge(b))
        def _():
            edge[b] -= times_t(panel[edge_slot(p, b * n_col + col)], panel[col_of(p, b)])

    def column_arrived(p, b):
        @pl.when(jnp.logical_not(on_diag))
        def _():
            arrived(col_slot(p, b))

    def update_column(p, b, lo):
        lone = lax.rem(row_blocks - lo, 2)

        @pl.when(lone == 1)
        def _():
            update_block(p, lo, b)

        def pair(m):
            a = lo + lone + 2 * m
            both = pl.ds(spot(a, b), 2)
            left = panel[pl.ds(row_slot(p, a), 2)].reshape(2 * size, size)
            share[both] -= times_t(left, panel[col_of(p, b)]).reshape(2, size, size)

        loop(0, (row_blocks - lo) // 2, pair)

    def trail(p, b_from, near):
        loop(b_from, col_blocks, lambda b: update_column(p, b, first_a(b * n_col + col - jnp.where(b == near, 0, 1))))

    def columns_arrived(p, b_from):
        def one(b):
            column_arrived(p, b)
            edge_arrived(p, b)

        loop(b_from, col_blocks, one)

    def prepare(b):
        work[size:, :] = jnp.zeros((BASE, size), F32)
        r_id = lax.broadcasted_iota(jnp.int32, (size + BASE, size), 0)
        c_id = lax.broadcasted_iota(jnp.int32, (size + BASE, size), 1)
        winv[...] = jnp.where(r_id == c_id, 1.0, 0.0).astype(F32)

    def times_winv_t(x):
        hi, mid, lo = split3(x)
        whi, wmid, wlo = winv3[0], winv3[1], winv3[2]
        small = times_t(lo, whi) + times_t(mid, wmid) + times_t(hi, wlo)
        return small + (times_t(mid, whi) + times_t(hi, wmid)) + times_t(hi, whi)

    def solve(k, a, count, near):
        kb = k // n_col
        here = pl.ds(spot(a, kb), count)

        def apply(p):
            left = panel[pl.ds(row_slot(p, a), count)].reshape(count * size, size)
            share[here] -= times_t(left, panel[col_of(p, kb)]).reshape(count, size, size)

        if not near:

            for back in (3, 2):

                @pl.when(k >= back)
                def _():
                    for m in range(count):
                        receive(k - back, a + m)

            loop(jnp.maximum(k - 2 - LAG, 0), k - 1, apply)

        @pl.when(k > 0)
        def _():
            for m in range(count):
                receive(k - 1, a + m)
            apply(k - 1)

        x = times_winv_t(share[here].reshape(count * size, size)).reshape(count, size, size)
        panel[pl.ds(row_slot(k, a), count)] = x.astype(BF16)
        share[here] = x
        if near:

            @pl.when(jnp.logical_and(leads, lax.rem(k + 1, n_row) == LEAD))
            def _():
                first[...] = panel[row_slot(k, a)]
                first_out(k, start)

        if count == 1:
            source_sends(k, a, start)
        else:
            loop(a, a + count, lambda n: source_sends(k, n, start))
        for m in range(count):
            pltpu.make_async_copy(share.at[spot(a + m, kb)], home(o_ref, a + m, kb), store_sem).start()

    def update_near(p, b):
        update_diag(p, b)
        update_edge(p, b)

    def first_slot(k, dev_row):
        return jnp.where(lax.rem(k + 1, n_row) == dev_row, row_slot(k, (k + 1) // n_row), col_slot(k, (k + 1) // n_col))

    def first_copy(k, dev_row, sem):
        dst = first_slot(k, dev_row)
        return pltpu.make_async_remote_copy(
            src_ref=first, dst_ref=panel.at[dst], send_sem=sem, recv_sem=recv_sem.at[dst],
            device_id=at(dev_row, lax.rem(col + 1, n_col)), device_id_type=MESH,
        )

    def others_first(k, fn):
        urgent = lax.rem(k + 3, n_row)
        lone = urgent == LEAD
        for m in range(n_row - 1):
            fn(m, lax.rem(jnp.where(lone, LEAD + 1, urgent) + m + jnp.where(lax.rem(jnp.where(lone, LEAD + 1, urgent) - LEAD + n_row, n_row) + m >= n_row, 1, 0), n_row))

    def first_out(k, act):
        act(first_copy(k, LEAD, first_sem.at[0, 0]))

        @pl.when(odd == 0)
        def _():
            others_first(k, lambda m, r: act(first_copy(k, r, first_sem.at[0, 1 + m])))

    def first_down(k, act):
        @pl.when(odd == 0)
        def _():
            others_first(k, lambda m, r: act(copy(first_slot(k, LEAD), first_slot(k, r), first_sem.at[1, 1 + m], at(r, col))))

    def firsts_done(k):
        @pl.when(jnp.logical_and(leads, k + 1 < steps))
        def _():
            first_out(k, finish)

        @pl.when(jnp.logical_and(leads, k > 0))
        def _():
            first_down(k - 1, finish)

    @pl.when(col == 0)
    def _():
        prepare(0)
        work[0:size, :] = diag[0]

    def step(k):
        mine = jnp.logical_and(col == lax.rem(k, n_col), k < steps)
        kb = k // n_col
        last = k - 1
        soon = jnp.logical_and(col == lax.rem(k + 1, n_col), k + 1 < steps)

        @pl.when(mine)
        def _():
            with jax.named_scope("factor"):
                factor_block(work, winv, winv3, prev, fac)

            @pl.when(has_edge(kb))
            def _():
                with jax.named_scope("lead"):

                    @pl.when(k == 0)
                    def _():
                        edge_seeded(kb)

                    @pl.when(k > 0)
                    def _():
                        edge_arrived(last, kb)
                        update_edge(last, kb)

                    first[...] = times_winv_t(edge[kb]).astype(BF16)
                    first_out(k, start)

            lo = first_a(k)
            second = jnp.minimum(lo + 1, row_blocks)
            with jax.named_scope("solve_near"):
                loop(lo, second, lambda a: solve(k, a, 1, True))
            with jax.named_scope("solve_one"):
                third = second + lax.rem(row_blocks - second, 2)
                loop(second, third, lambda a: solve(k, a, 1, False))
            with jax.named_scope("solve_two"):
                loop(0, (row_blocks - third) // 2, lambda m: solve(k, third + 2 * m, 2, False))

        @pl.when(k >= depth)
        def _():
            with jax.named_scope("passed"):
                passed(k - depth)

        @pl.when(mine)
        def _():
            @pl.when(row == lax.rem(k, n_row))
            def _():
                for d in range(1, n_row):
                    seed_copy(kb, lax.rem(row + d, n_row)).wait_send()
                r_id = lax.broadcasted_iota(jnp.int32, (size, size), 0)
                c_id = lax.broadcasted_iota(jnp.int32, (size, size), 1)
                n = spot(k // n_row, kb)
                share[n] = jnp.where(r_id >= c_id, work[0:size, :].T, 0.0)
                pltpu.make_async_copy(share.at[n], home(o_ref, k // n_row, kb), store_sem).start()

            with jax.named_scope("late_trail"):

                def late(p):
                    columns_arrived(p, kb + 1)
                    trail(p, kb + 1, -1)

                loop(jnp.maximum(k - 2 - LAG, 0), k - LAG + 1, late)

            @pl.when(kb + 1 < col_blocks)
            def _():
                hand_out(kb + 1)

        @pl.when(jnp.logical_and(k > 0, jnp.logical_not(jnp.logical_or(mine, soon))))
        def _():
            @pl.when(col != lax.rem(last, n_col))
            def _():
                with jax.named_scope("receive"):
                    end = jnp.where(lead(last) == 3, jnp.minimum(last_near(last) + 1, row_blocks), row_blocks)
                    loop(first_passed(last), end, lambda a: receive_any(last, a))

            @pl.when(jnp.logical_and(k >= LAG, lead(last) != 3))
            def _():
                p = k - LAG
                near = first_b(k)
                with jax.named_scope("columns"):
                    columns_arrived(p, near)

                @pl.when(near < col_blocks)
                def _():
                    age = k + n_col - (near * n_col + col)

                    @pl.when(jnp.logical_and(age == 3, near > 0))
                    def _():
                        with jax.named_scope("seed_late"):
                            seed_arrived(near)
                            edge_seeded(near)

                    @pl.when(age >= 3)
                    def _():
                        oldest = jnp.where(age == 3, jnp.maximum(p - 2, 0), p)
                        loop(oldest, p + 1, lambda q: update_near(q, near))

                with jax.named_scope("trail"):
                    trail(p, near, near)

        @pl.when(soon)
        def _():
            nb = (k + 1) // n_col

            oldest = jnp.maximum(k - 1 - LAG, 0)
            lo = first_a(k + 1)

            def old_diag(p):
                column_arrived(p, nb)
                edge_arrived(p, nb)
                update_near(p, nb)

            def take(a):
                receive(last, a)

                @pl.when(a * n_row + row > k + 1)
                def _():
                    loop(oldest, last, lambda p: update_block(p, a, nb))

            @pl.when(k > 0)
            def _():
                with jax.named_scope("old_diag"):
                    loop(oldest, last, old_diag)
                @pl.when(jnp.logical_and(k > 1, jnp.logical_and(lo > last_near(k - 2), lo < row_blocks)))
                def _():
                    receive(k - 2, lo)

                with jax.named_scope("take"):
                    loop(first_a(k), jnp.minimum(first_a(k + 1) + 1, row_blocks), take)
                with jax.named_scope("take_column"):
                    column_arrived(last, nb)
                    edge_arrived(last, nb)
                with jax.named_scope("catch_up"):
                    update_near(last, nb)
                    loop(first_a(k + 1), jnp.minimum(first_a(k + 1) + 1, row_blocks), lambda a: update_block(last, a, nb))

            prepare(nb)
            slot = col_of(k, nb)
            with jax.named_scope("first_block"):
                arrived(slot)

            @pl.when(leads)
            def _():
                first_down(k, start)

            other = panel[slot]
            work[0:size, :] = diag[nb] - times_t(other, other)

        @pl.when(jnp.logical_and(k >= n_col // 2, col == lax.rem(k + n_col // 2, n_col)))
        def _():
            with jax.named_scope("sends_done"):
                firsts_done(k - n_col // 2)
                loop(first_a(k - n_col // 2), row_blocks, lambda a: source_sends(k - n_col // 2, a, finish))

    loop(0, steps + n_col // 2, step)

    def edges_done(b):
        @pl.when(jnp.logical_and(holds_edge(b), jnp.logical_not(leads)))
        def _():
            edge_copy(b).wait_send()

    loop(0, col_blocks, edges_done)
    with jax.named_scope("stored"):
        pltpu.make_async_copy(share, share, store_sem).wait()


def solution(mesh):
    n_row = mesh.shape["row"]
    n_col = mesh.shape["col"]

    def factor_local(a_loc):
        row_blocks, size, local_cols = a_loc.shape
        col_blocks = local_cols // size
        slots = n_row * (row_blocks * (row_blocks + 1) // 2) + n_col * (col_blocks * (col_blocks + 1) // 2)
        slots += 2 * row_blocks * n_row
        return pl.pallas_call(
            functools.partial(kernel, n_row, n_col, "batch"),
            out_shape=jax.ShapeDtypeStruct(a_loc.shape, F32),
            in_specs=[pl.BlockSpec(memory_space=pl.ANY)],
            out_specs=pl.BlockSpec(memory_space=pl.ANY),
            scratch_shapes=[
                pltpu.VMEM((row_blocks * col_blocks, size, size), F32),
                pltpu.VMEM((col_blocks, size, size), F32),
                pltpu.VMEM((col_blocks, size, size), F32),
                pltpu.VMEM((col_blocks, size, size), F32),
                pltpu.VMEM((size, size), BF16),
                pltpu.VMEM((slots, size, size), BF16),
                pltpu.VMEM((size + BASE, size), F32),
                pltpu.VMEM((size + BASE, size), F32),
                pltpu.VMEM((3, size, size), BF16),
                pltpu.VMEM((BASE, 3 * LANE), F32),
                pltpu.VMEM((4 * SUB, SUB, LANE), F32),
                pltpu.SemaphoreType.DMA,
                pltpu.SemaphoreType.DMA,
                pltpu.SemaphoreType.DMA((col_blocks, n_row)),
                pltpu.SemaphoreType.DMA((col_blocks,)),
                pltpu.SemaphoreType.DMA((col_blocks,)),
                pltpu.SemaphoreType.DMA((col_blocks,)),
                pltpu.SemaphoreType.DMA((2, n_row)),
                pltpu.SemaphoreType.DMA((row_blocks, 9)),
                pltpu.SemaphoreType.DMA((4, row_blocks, 6)),
                pltpu.SemaphoreType.DMA((slots,)),
            ],
            compiler_params=pltpu.CompilerParams(
                collective_id=0, has_side_effects=True, vmem_limit_bytes=60 * 1024 * 1024
            ),
            name="cholesky",
        )(a_loc)

    blk_spec = P(("batch", "row"), None, "col")
    return jax.shard_map(factor_local, mesh=mesh, in_specs=(blk_spec,), out_specs=blk_spec, check_vma=False)
```

```python
import functools

import jax
import jax.numpy as jnp
from jax import lax
from jax.experimental import pallas as pl
from jax.experimental.pallas import tpu as pltpu
from jax.sharding import PartitionSpec as P

F32 = jnp.float32
BF16 = jnp.bfloat16
MESH = pl.DeviceIdType.MESH
SUB = 8
LANE = 128
BASE = 16
LEAD = 1
LAG = 3


def sub_bcast(x, q):
    return jnp.broadcast_to(x[q : q + 1, :], (SUB, LANE))


ALONG_LANES = lax.GatherDimensionNumbers(
    offset_dims=(), collapsed_slice_dims=(1,), start_index_map=(1,), operand_batching_dims=(0,), start_indices_batching_dims=(0,)
)


def lane_bcast(x, lane):
    index = jnp.full((SUB, LANE, 1), lane, jnp.int32)
    return lax.gather(x, index, ALONG_LANES, (1, 1), mode=lax.GatherScatterMode.PROMISE_IN_BOUNDS)


def split3(x):
    high = x.astype(BF16)
    rest = x - high.astype(F32)
    mid = rest.astype(BF16)
    return high, mid, (rest - mid.astype(F32)).astype(BF16)


def swap_rows(x, bit, row_id):
    if bit == SUB // 2:
        return pltpu.roll(x, bit, 0)
    return jnp.where((row_id & bit) == 0, pltpu.roll(x, SUB - bit, 0), pltpu.roll(x, bit, 0))


def stack_sums(parts):
    row_id = lax.broadcasted_iota(jnp.int32, (SUB, LANE), 0)
    for bit in (4, 2, 1):
        low = (row_id & bit) == 0
        half = len(parts) // 2
        parts = [
            jnp.where(low, parts[n], parts[n + half]) + swap_rows(jnp.where(low, parts[n + half], parts[n]), bit, row_id)
            for n in range(half)
        ]
    return parts[0]


def eliminate(rows, lane0):
    row_id = lax.broadcasted_iota(jnp.int32, (SUB, LANE), 0)
    rows = [list(rows[0]), list(rows[1])]
    cols = [
        [lane_bcast(rows[0][0], lane0 + j) for j in range(SUB)],
        [lane_bcast(rows[1][0], lane0 + j) for j in range(BASE)],
    ]
    scale = [jnp.zeros((SUB, LANE), F32), jnp.zeros((SUB, LANE), F32)]
    pivot = sub_bcast(cols[0][0], 0)
    for j in range(BASE):
        t, q = divmod(j, SUB)
        inv = lax.rsqrt(pivot)
        scale[t] = jnp.where(row_id == q, inv, scale[t])
        if j + 1 < BASE:
            tn, qn = divmod(j + 1, SUB)
            near = sub_bcast(cols[tn][j], qn) * inv
            pivot = sub_bcast(cols[tn][j + 1], qn) - near * near
        below = cols[1][j] * inv
        here = cols[0][j] * inv if t == 0 else None
        for n in range(j + 1, BASE):
            tn, qn = divmod(n, SUB)
            other = near if n == j + 1 else sub_bcast(here if tn == 0 else below, qn)
            if t == 0 and tn == 0:
                cols[0][n] = cols[0][n] - here * other
            cols[1][n] = cols[1][n] - below * other
        masked = jnp.where(row_id > q, here if t == 0 else below, 0.0)
        for v in range(len(rows[0])):
            pivot_row = sub_bcast(rows[t][v], q) * inv
            rows[t][v] = rows[t][v] - masked * pivot_row
            if t == 0:
                rows[1][v] = rows[1][v] - below * pivot_row
    return [[x * scale[t] for x in rows[t]] for t in range(2)]


def factor_block(work, winv, winv3, prev, fac):
    size = work.shape[1]
    prev[...] = jnp.zeros(prev.shape, F32)
    fac[...] = jnp.zeros(fac.shape, F32)

    def group(v):
        return slice(LANE * v, LANE * (v + 1))

    def pending(factors, before, t, v):
        above, below = before[:SUB, group(v)], before[SUB:, group(v)]
        at = 2 * SUB * t
        return stack_sums([factors[at + n] * above + factors[at + SUB + n] * below for n in range(SUB)])

    for half in range(size // LANE):
        views = [(work, 0), (work, 1), (winv, 0)] if half == 0 else [(work, 1), (winv, 0), (winv, 1)]
        first = half * LANE
        if half == 1:
            factors, before = fac[...], prev[...]
            work[first : first + BASE, group(1)] -= jnp.concatenate([pending(factors, before, t, 1) for t in range(2)], axis=0)
            prev[...] = jnp.concatenate([before[:, group(1)], before[:, group(2)], jnp.zeros((BASE, LANE), F32)], axis=1)

        def body(s, carry, views=views, first=first):
            lane0 = s * BASE
            row0 = pl.multiple_of(first + lane0, BASE)

            here = pl.ds(row0, BASE)
            then = pl.ds(pl.multiple_of(row0 + BASE, BASE), BASE)
            both = [ref[here, group(g)] for ref, g in views]
            rows = [[x[SUB * t : SUB * (t + 1)] for x in both] for t in range(2)]
            factors, before = fac[...], prev[...]
            for t in range(2):
                for v in (1, 2):
                    rows[t][v] = rows[t][v] - pending(factors, before, t, v)
            hi, mid, lo = split3(before)
            lane = lax.broadcasted_iota(jnp.int32, (BASE, size - first), 1) + first
            after = lane >= row0 + BASE
            lhi, lmid, llo = [jnp.where(after, x[:, : size - first], jnp.zeros((), BF16)) for x in (hi, mid, lo)]
            update = lax.dot_general(
                jnp.concatenate([lhi, lhi, lmid, lhi, llo, lmid], axis=0),
                jnp.concatenate([hi, mid, hi, lo, hi, mid], axis=0),
                (((0,), (0,)), ((), ())),
                preferred_element_type=F32,
            )
            for v, (ref, g) in enumerate(views):
                ref[first:size, group(g)] -= update[:, group(v)]
            done = eliminate(rows, lane0)
            if first == 0:
                source = [jnp.where(s == LANE // BASE - 1, done[t][1], done[t][0]) for t in range(2)]
            else:
                source = [done[t][0] for t in range(2)]
            next_lane = (lane0 + BASE) % LANE
            factors, sums = [], []
            for t in range(2):
                factor = [[lane_bcast(source[m], next_lane + SUB * t + n) for n in range(SUB)] for m in range(2)]
                sums.append(stack_sums([factor[0][n] * done[0][0] + factor[1][n] * done[1][0] for n in range(SUB)]))
                factors += factor[0] + factor[1]
            ref, g = views[0]
            ref[then, group(g)] -= jnp.concatenate(sums, axis=0)
            fac[...] = jnp.stack(factors)
            whole = [jnp.concatenate([done[0][v], done[1][v]], axis=0) for v in range(3)]
            prev[...] = jnp.concatenate(whole, axis=1)
            for (ref, g), x in zip(views, whole):
                ref[here, group(g)] = x
                if ref is winv:
                    for n, part in enumerate(split3(x)):
                        winv3[n, here, group(g)] = part
            return carry

        lax.fori_loop(0, LANE // BASE, body, 0)


def kernel(n_row, n_col, batch_axis, a_ref, o_ref, share, diag, edge, stage, first, panel, work, winv, winv3, prev, fac, load_sem, store_sem,
           seed_send, seed_recv, edge_send, edge_recv, first_sem, send_sem, pass_sem, recv_sem):
    row_blocks, size, local_cols = a_ref.shape
    col_blocks = local_cols // size
    ratio = n_col // n_row
    steps = row_blocks * n_row
    depth = pass_sem.shape[0]
    batch = lax.axis_index(batch_axis)
    row = lax.axis_index("row")
    col = lax.axis_index("col")
    odd = lax.rem(col, 2)
    on_diag = lax.rem(col, n_row) == row
    row_slots = n_row * (row_blocks * (row_blocks + 1) // 2)
    edge_slots = row_slots + n_col * (col_blocks * (col_blocks + 1) // 2)
    leads = row == LEAD

    def at(dev_row, dev_col):
        return (batch, dev_row, dev_col)

    def row_slot(k, a):
        g = k // n_row
        return n_row * (row_blocks * g - (g * (g - 1)) // 2) + (k - g * n_row) * (row_blocks - g) + a - g

    def col_slot(k, b):
        h = k // n_col
        return row_slots + n_col * (col_blocks * h - (h * (h - 1)) // 2) + (k - h * n_col) * (col_blocks - h) + b - h

    def first_a(k):
        return (k + n_row - row) // n_row

    def first_b(k):
        return (k + n_col - col) // n_col

    def home(ref, a, b):
        return ref.at[a, :, pl.ds(pl.multiple_of(b * size, size), size)]

    def spot(a, b):
        return b * row_blocks + a

    def col_of(k, b):
        return jnp.where(on_diag, row_slot(k, ratio * b + col // n_row), col_slot(k, b))

    def edge_slot(k, j):
        return edge_slots + 2 * k + (j - k - 1) // n_col

    def edge_reach(ahead):
        return jnp.logical_and(ahead >= 2, jnp.logical_and(ahead <= n_col + LAG, row != LEAD))

    def copy(src_slot, dst_slot, sem, device):
        return pltpu.make_async_remote_copy(
            src_ref=panel.at[src_slot], dst_ref=panel.at[dst_slot], send_sem=sem, recv_sem=recv_sem.at[dst_slot],
            device_id=device, device_id_type=MESH,
        )

    def arrived(slot):
        copy(slot, slot, send_sem.at[0, 0], at(row, col)).wait_recv()

    def start(c):
        c.start()

    def finish(c):
        c.wait_send()

    def from_maker(ahead, way):
        there = lax.rem(row + way, n_row)
        lead_near = jnp.logical_and(there == LEAD, jnp.logical_and(ahead >= 2, ahead <= n_row))
        soon_needed = jnp.logical_and(ahead == 2, way == 2)
        return jnp.logical_or(lead_near, soon_needed)

    def down_column(k, a, maker, sems, act):
        i = a * n_row + row
        slot = row_slot(k, a)
        dst = col_slot(k, i // n_col)
        for m, way in enumerate((1, n_row - 1, 2)):
            direct = from_maker(i - k, way)

            @pl.when(direct if maker else jnp.logical_not(direct))
            def _():
                act(copy(slot, dst, sems[m], at(lax.rem(row + way, n_row), lax.rem(i, n_col))))

    def last_near(p):
        return first_a(p + 3)

    def to_edge(k, a, sem, act):
        i = a * n_row + row
        act(copy(row_slot(k, a), edge_slot(k, i - 1), sem, at(LEAD, lax.rem(i - 1, n_col))))

    def source_sends(k, a, act):
        ahead = a * n_row + row - k
        slot = row_slot(k, a)
        early = n_row

        @pl.when(jnp.logical_and(edge_reach(ahead), jnp.logical_or(ahead <= early, ahead == n_col)))
        def _():
            to_edge(k, a, send_sem.at[a, 5], act)

        @pl.when(jnp.logical_and(ahead >= 2, ahead <= early))
        def _():
            down_column(k, a, True, [send_sem.at[a, m] for m in range(3)], act)

        @pl.when(lax.rem(ahead, n_col) == 0)
        def _():
            down_column(k, a, False, [send_sem.at[a, m] for m in range(3)], act)

        @pl.when(jnp.logical_or(jnp.logical_and(odd == 0, ahead >= 2), ahead >= n_col - 1))
        def _():
            act(copy(slot, slot, send_sem.at[a, 3], at(row, lax.rem(jnp.where(odd == 0, col + 1, col - 1), n_col))))

        @pl.when(ahead >= 2)
        def _():
            act(copy(slot, slot, send_sem.at[a, 6], at(row, lax.rem(col - odd + 2, n_col))))

        @pl.when(jnp.logical_and(ahead >= 3 - odd, a <= last_near(k)))
        def _():
            act(copy(slot, slot, send_sem.at[a, 4], at(row, lax.rem(col - odd + 3, n_col))))

        @pl.when(jnp.logical_and(ahead >= n_col // 2 - odd, ahead < n_col - 2 - odd))
        def _():
            act(copy(slot, slot, send_sem.at[a, 7], at(row, lax.rem(col - odd + 5, n_col))))

        @pl.when(ahead >= n_col - 2 - odd)
        def _():
            act(copy(slot, slot, send_sem.at[a, 8], at(row, lax.rem(col - odd - 1 + n_col, n_col))))

    def lead(p):
        return lax.rem(col - lax.rem(p, n_col) + n_col, n_col)

    def hops(p):
        return lax.rem(col // 2 - lax.rem(p, n_col) // 2 + n_col // 2, n_col // 2)

    def passes(p):
        return jnp.logical_and(odd == 1, hops(p) > 1)

    def first_passed(p):
        low = jnp.where(passes(p), jnp.maximum(lead(p) - 1, 2), lead(p))
        return (p + low - row + n_row - 1) // n_row

    def pass_down(p, a, act):
        i = a * n_row + row
        ahead = i - p
        sems = pass_sem.at[lax.rem(p, depth), a]

        @pl.when(jnp.logical_and(odd == 0, jnp.logical_and(lead(p) <= 2, a > last_near(p))))
        def _():
            act(copy(row_slot(p, a), row_slot(p, a), sems.at[3], at(row, col + 1)))

        @pl.when(jnp.logical_and(lax.rem(i, n_col) == col, ahead > 1))
        def _():
            @pl.when(jnp.logical_and(ahead > n_row, edge_reach(ahead)))
            def _():
                to_edge(p, a, sems.at[5], act)

            down_column(p, a, False, [sems.at[m] for m in range(3)], act)

    def pass_on(p, a, act):
        slot = row_slot(p, a)
        sems = pass_sem.at[lax.rem(p, depth), a]

        @pl.when(passes(p))
        def _():
            @pl.when(hops(p) == n_col // 2 - 1)
            def _():
                act(copy(slot, slot, sems.at[4], at(row, lax.rem(col - 2 + n_col, n_col))))

            act(copy(slot, slot, sems.at[3], at(row, col - 1)))

        pass_down(p, a, act)

    def passed(p):
        @pl.when(lead(p) != 0)
        def _():
            loop(first_passed(p), row_blocks, lambda a: pass_on(p, a, finish))

    def receive(p, a):
        arrived(row_slot(p, a))
        pass_down(p, a, start)

    def receive_any(p, a):
        arrived(row_slot(p, a))
        pass_on(p, a, start)

    def loop(lo, hi, fn):
        lax.fori_loop(lo, hi, lambda n, c: (fn(n), c)[1], 0)

    for a in range(row_blocks):
        for b in range(col_blocks):
            pltpu.make_async_copy(home(a_ref, a, b), share.at[spot(a, b)], load_sem).start()

    barrier = pltpu.get_barrier_semaphore()
    n_dev = n_row * n_col

    def greet(n):
        other = lax.rem(row * n_col + col + n, n_dev)
        pl.semaphore_signal(barrier, inc=1, device_id=at(other // n_col, lax.rem(other, n_col)), device_id_type=MESH)

    loop(1, n_dev, greet)
    with jax.named_scope("all_here"):
        pl.semaphore_wait(barrier, n_dev - 1)
    with jax.named_scope("loaded"):
        pltpu.make_async_copy(share, share, load_sem).wait()

    def seed_copy(b, dev_row):
        return pltpu.make_async_remote_copy(
            src_ref=share.at[spot(ratio * b + col // n_row, b)], dst_ref=diag.at[b],
            send_sem=seed_send.at[b, lax.rem(dev_row - row + n_row, n_row)],
            recv_sem=seed_recv.at[b], device_id=at(dev_row, col), device_id_type=MESH,
        )

    def hand_out(b):
        @pl.when(on_diag)
        def _():
            for d in (1, n_row - 1, 2):
                seed_copy(b, lax.rem(row + d, n_row)).start()
            diag[b] = share[spot(ratio * b + col // n_row, b)]

        @pl.when(jnp.logical_and(holds_edge(b), jnp.logical_not(leads)))
        def _():
            stage[b] = share[spot((b * n_col + col + 1) // n_row, b)]
            edge_copy(b).start()

    def holds_edge(b):
        j = b * n_col + col
        return jnp.logical_and(lax.rem(j + 1, n_row) == row, j + 1 < steps)

    def edge_copy(b):
        return pltpu.make_async_remote_copy(
            src_ref=stage.at[b], dst_ref=edge.at[b], send_sem=edge_send.at[b], recv_sem=edge_recv.at[b],
            device_id=at(LEAD, col), device_id_type=MESH,
        )

    def has_edge(b):
        from_other = jnp.logical_and(leads, lax.rem(col + 1, n_row) != LEAD)
        return jnp.logical_and(from_other, b * n_col + col + 1 < steps)

    def edge_seeded(b):
        @pl.when(has_edge(b))
        def _():
            edge_copy(b).wait_recv()

    def edge_arrived(p, b):
        j = b * n_col + col

        @pl.when(jnp.logical_and(has_edge(b), j + 1 - p <= n_col + LAG))
        def _():
            arrived(edge_slot(p, j))

    hand_out(0)
    winv3[...] = jnp.zeros(winv3.shape, BF16)

    def seed_arrived(b):
        @pl.when(jnp.logical_not(on_diag))
        def _():
            seed_copy(b, row).wait_recv()

    with jax.named_scope("seed"):
        seed_arrived(0)

        @pl.when(col != 0)
        def _():
            edge_seeded(0)

    def clear(n):
        a, b = lax.rem(n, row_blocks), n // row_blocks

        @pl.when(a * n_row + row < b * n_col + col)
        def _():
            share[n] = jnp.zeros((size, size), F32)
            pltpu.make_async_copy(share.at[n], home(o_ref, a, b), store_sem).start()

    loop(0, row_blocks * col_blocks, clear)

    def times_t(x, y):
        return lax.dot_general(x, y, (((1,), (1,)), ((), ())), preferred_element_type=F32)

    def update_block(p, a, b):
        share[spot(a, b)] -= times_t(panel[row_slot(p, a)], panel[col_of(p, b)])

    def update_diag(p, b):
        other = panel[col_of(p, b)]
        diag[b] -= times_t(other, other)

    def update_edge(p, b):
        @pl.when(has_edge(b))
        def _():
            edge[b] -= times_t(panel[edge_slot(p, b * n_col + col)], panel[col_of(p, b)])

    def column_arrived(p, b):
        @pl.when(jnp.logical_not(on_diag))
        def _():
            arrived(col_slot(p, b))

    def update_column(p, b, lo):
        lone = lax.rem(row_blocks - lo, 2)

        @pl.when(lone == 1)
        def _():
            update_block(p, lo, b)

        def pair(m):
            a = lo + lone + 2 * m
            both = pl.ds(spot(a, b), 2)
            left = panel[pl.ds(row_slot(p, a), 2)].reshape(2 * size, size)
            share[both] -= times_t(left, panel[col_of(p, b)]).reshape(2, size, size)

        loop(0, (row_blocks - lo) // 2, pair)

    def trail(p, b_from, near):
        loop(b_from, col_blocks, lambda b: update_column(p, b, first_a(b * n_col + col - jnp.where(b == near, 0, 1))))

    def columns_arrived(p, b_from):
        def one(b):
            column_arrived(p, b)
            edge_arrived(p, b)

        loop(b_from, col_blocks, one)

    def prepare(b):
        work[size:, :] = jnp.zeros((BASE, size), F32)
        r_id = lax.broadcasted_iota(jnp.int32, (size + BASE, size), 0)
        c_id = lax.broadcasted_iota(jnp.int32, (size + BASE, size), 1)
        winv[...] = jnp.where(r_id == c_id, 1.0, 0.0).astype(F32)

    def times_winv_t(x):
        hi, mid, lo = split3(x)
        whi, wmid, wlo = winv3[0], winv3[1], winv3[2]
        small = times_t(lo, whi) + times_t(mid, wmid) + times_t(hi, wlo)
        return small + (times_t(mid, whi) + times_t(hi, wmid)) + times_t(hi, whi)

    def solve(k, a, count, near):
        kb = k // n_col
        here = pl.ds(spot(a, kb), count)

        def apply(p):
            left = panel[pl.ds(row_slot(p, a), count)].reshape(count * size, size)
            share[here] -= times_t(left, panel[col_of(p, kb)]).reshape(count, size, size)

        if not near:

            for m in range(count):

                @pl.when(k >= 3)
                def _():
                    receive(k - 3, a + m)

                @pl.when(jnp.logical_and(k >= 2, a + m > last_near(k - 2)))
                def _():
                    receive(k - 2, a + m)

            loop(jnp.maximum(k - 2 - LAG, 0), k - 1, apply)

        @pl.when(k > 0)
        def _():
            for m in range(count):
                receive(k - 1, a + m)
            apply(k - 1)

        x = times_winv_t(share[here].reshape(count * size, size)).reshape(count, size, size)
        panel[pl.ds(row_slot(k, a), count)] = x.astype(BF16)
        share[here] = x
        if near:

            @pl.when(jnp.logical_and(leads, lax.rem(k + 1, n_row) == LEAD))
            def _():
                first[...] = panel[row_slot(k, a)]
                first_out(k, start)

        if count == 1:
            source_sends(k, a, start)
        else:
            loop(a, a + count, lambda n: source_sends(k, n, start))
        for m in range(count):
            pltpu.make_async_copy(share.at[spot(a + m, kb)], home(o_ref, a + m, kb), store_sem).start()

    def update_near(p, b):
        update_diag(p, b)
        update_edge(p, b)

    def first_slot(k, dev_row):
        return jnp.where(lax.rem(k + 1, n_row) == dev_row, row_slot(k, (k + 1) // n_row), col_slot(k, (k + 1) // n_col))

    def first_copy(k, dev_row, sem):
        dst = first_slot(k, dev_row)
        return pltpu.make_async_remote_copy(
            src_ref=first, dst_ref=panel.at[dst], send_sem=sem, recv_sem=recv_sem.at[dst],
            device_id=at(dev_row, lax.rem(col + 1, n_col)), device_id_type=MESH,
        )

    def others_first(k, fn):
        urgent = lax.rem(k + 3, n_row)
        lone = urgent == LEAD
        for m in range(n_row - 1):
            fn(m, lax.rem(jnp.where(lone, LEAD + 1, urgent) + m + jnp.where(lax.rem(jnp.where(lone, LEAD + 1, urgent) - LEAD + n_row, n_row) + m >= n_row, 1, 0), n_row))

    def first_out(k, act):
        act(first_copy(k, LEAD, first_sem.at[0, 0]))

        @pl.when(odd == 0)
        def _():
            others_first(k, lambda m, r: act(first_copy(k, r, first_sem.at[0, 1 + m])))

    def first_down(k, act):
        @pl.when(odd == 0)
        def _():
            others_first(k, lambda m, r: act(copy(first_slot(k, LEAD), first_slot(k, r), first_sem.at[1, 1 + m], at(r, col))))

    def firsts_done(k):
        @pl.when(jnp.logical_and(leads, k + 1 < steps))
        def _():
            first_out(k, finish)

        @pl.when(jnp.logical_and(leads, k > 0))
        def _():
            first_down(k - 1, finish)

    @pl.when(col == 0)
    def _():
        prepare(0)
        work[0:size, :] = diag[0]

    def step(k):
        mine = jnp.logical_and(col == lax.rem(k, n_col), k < steps)
        kb = k // n_col
        last = k - 1
        soon = jnp.logical_and(col == lax.rem(k + 1, n_col), k + 1 < steps)

        @pl.when(mine)
        def _():
            with jax.named_scope("factor"):
                factor_block(work, winv, winv3, prev, fac)

            @pl.when(has_edge(kb))
            def _():
                with jax.named_scope("lead"):

                    @pl.when(k == 0)
                    def _():
                        edge_seeded(kb)

                    @pl.when(k > 0)
                    def _():
                        edge_arrived(last, kb)
                        update_edge(last, kb)

                    first[...] = times_winv_t(edge[kb]).astype(BF16)
                    first_out(k, start)

            lo = first_a(k)
            second = jnp.minimum(lo + 1, row_blocks)
            with jax.named_scope("solve_near"):
                loop(lo, second, lambda a: solve(k, a, 1, True))
            with jax.named_scope("solve_one"):
                third = second + lax.rem(row_blocks - second, 2)
                loop(second, third, lambda a: solve(k, a, 1, False))
            with jax.named_scope("solve_two"):
                loop(0, (row_blocks - third) // 2, lambda m: solve(k, third + 2 * m, 2, False))

        @pl.when(k >= depth)
        def _():
            with jax.named_scope("passed"):
                passed(k - depth)

        @pl.when(mine)
        def _():
            @pl.when(row == lax.rem(k, n_row))
            def _():
                for d in range(1, n_row):
                    seed_copy(kb, lax.rem(row + d, n_row)).wait_send()
                r_id = lax.broadcasted_iota(jnp.int32, (size, size), 0)
                c_id = lax.broadcasted_iota(jnp.int32, (size, size), 1)
                n = spot(k // n_row, kb)
                share[n] = jnp.where(r_id >= c_id, work[0:size, :].T, 0.0)
                pltpu.make_async_copy(share.at[n], home(o_ref, k // n_row, kb), store_sem).start()

            with jax.named_scope("late_trail"):

                def late(p):
                    columns_arrived(p, kb + 1)
                    trail(p, kb + 1, -1)

                loop(jnp.maximum(k - 2 - LAG, 0), k - LAG + 1, late)

            @pl.when(kb + 1 < col_blocks)
            def _():
                hand_out(kb + 1)

        @pl.when(jnp.logical_and(k > 0, jnp.logical_not(jnp.logical_or(mine, soon))))
        def _():
            @pl.when(col != lax.rem(last, n_col))
            def _():
                with jax.named_scope("receive"):
                    end = jnp.where(lead(last) == 3, jnp.minimum(last_near(last) + 1, row_blocks), row_blocks)
                    loop(first_passed(last), end, lambda a: receive_any(last, a))

            @pl.when(jnp.logical_and(k >= LAG, lead(last) != 3))
            def _():
                p = k - LAG
                near = first_b(k)
                with jax.named_scope("columns"):
                    columns_arrived(p, near)

                @pl.when(near < col_blocks)
                def _():
                    age = k + n_col - (near * n_col + col)

                    @pl.when(jnp.logical_and(age == 3, near > 0))
                    def _():
                        with jax.named_scope("seed_late"):
                            seed_arrived(near)
                            edge_seeded(near)

                    @pl.when(age >= 3)
                    def _():
                        oldest = jnp.where(age == 3, jnp.maximum(p - 2, 0), p)
                        loop(oldest, p + 1, lambda q: update_near(q, near))

                with jax.named_scope("trail"):
                    trail(p, near, near)

        @pl.when(soon)
        def _():
            nb = (k + 1) // n_col

            oldest = jnp.maximum(k - 1 - LAG, 0)
            lo = first_a(k + 1)

            def old_diag(p):
                column_arrived(p, nb)
                edge_arrived(p, nb)
                update_near(p, nb)

            def take(a):
                receive(last, a)

                @pl.when(jnp.logical_and(a * n_row + row > k + 1, a <= lo))
                def _():
                    loop(oldest, last, lambda p: update_block(p, a, nb))

            @pl.when(k > 0)
            def _():
                with jax.named_scope("old_diag"):
                    loop(oldest, last, old_diag)
                with jax.named_scope("take"):
                    loop(first_a(k), jnp.minimum(last_near(last) + 1, row_blocks), take)
                with jax.named_scope("take_column"):
                    column_arrived(last, nb)
                    edge_arrived(last, nb)
                with jax.named_scope("catch_up"):
                    update_near(last, nb)
                    loop(first_a(k + 1), jnp.minimum(first_a(k + 1) + 1, row_blocks), lambda a: update_block(last, a, nb))

            prepare(nb)
            slot = col_of(k, nb)
            with jax.named_scope("first_block"):
                arrived(slot)

            @pl.when(leads)
            def _():
                first_down(k, start)

            other = panel[slot]
            work[0:size, :] = diag[nb] - times_t(other, other)

        @pl.when(jnp.logical_and(k >= n_col // 2, col == lax.rem(k + n_col // 2, n_col)))
        def _():
            with jax.named_scope("sends_done"):
                firsts_done(k - n_col // 2)
                loop(first_a(k - n_col // 2), row_blocks, lambda a: source_sends(k - n_col // 2, a, finish))

    loop(0, steps + n_col // 2, step)

    def edges_done(b):
        @pl.when(jnp.logical_and(holds_edge(b), jnp.logical_not(leads)))
        def _():
            edge_copy(b).wait_send()

    loop(0, col_blocks, edges_done)
    with jax.named_scope("stored"):
        pltpu.make_async_copy(share, share, store_sem).wait()


def solution(mesh):
    n_row = mesh.shape["row"]
    n_col = mesh.shape["col"]

    def factor_local(a_loc):
        row_blocks, size, local_cols = a_loc.shape
        col_blocks = local_cols // size
        slots = n_row * (row_blocks * (row_blocks + 1) // 2) + n_col * (col_blocks * (col_blocks + 1) // 2)
        slots += 2 * row_blocks * n_row
        return pl.pallas_call(
            functools.partial(kernel, n_row, n_col, "batch"),
            out_shape=jax.ShapeDtypeStruct(a_loc.shape, F32),
            in_specs=[pl.BlockSpec(memory_space=pl.ANY)],
            out_specs=pl.BlockSpec(memory_space=pl.ANY),
            scratch_shapes=[
                pltpu.VMEM((row_blocks * col_blocks, size, size), F32),
                pltpu.VMEM((col_blocks, size, size), F32),
                pltpu.VMEM((col_blocks, size, size), F32),
                pltpu.VMEM((col_blocks, size, size), F32),
                pltpu.VMEM((size, size), BF16),
                pltpu.VMEM((slots, size, size), BF16),
                pltpu.VMEM((size + BASE, size), F32),
                pltpu.VMEM((size + BASE, size), F32),
                pltpu.VMEM((3, size, size), BF16),
                pltpu.VMEM((BASE, 3 * LANE), F32),
                pltpu.VMEM((4 * SUB, SUB, LANE), F32),
                pltpu.SemaphoreType.DMA,
                pltpu.SemaphoreType.DMA,
                pltpu.SemaphoreType.DMA((col_blocks, n_row)),
                pltpu.SemaphoreType.DMA((col_blocks,)),
                pltpu.SemaphoreType.DMA((col_blocks,)),
                pltpu.SemaphoreType.DMA((col_blocks,)),
                pltpu.SemaphoreType.DMA((2, n_row)),
                pltpu.SemaphoreType.DMA((row_blocks, 9)),
                pltpu.SemaphoreType.DMA((4, row_blocks, 6)),
                pltpu.SemaphoreType.DMA((slots,)),
            ],
            compiler_params=pltpu.CompilerParams(
                collective_id=0, has_side_effects=True, vmem_limit_bytes=60 * 1024 * 1024
            ),
            name="cholesky",
        )(a_loc)

    blk_spec = P(("batch", "row"), None, "col")
    return jax.shard_map(factor_local, mesh=mesh, in_specs=(blk_spec,), out_specs=blk_spec, check_vma=False)
```

```python
import functools

import jax
import jax.numpy as jnp
from jax import lax
from jax.experimental import pallas as pl
from jax.experimental.pallas import tpu as pltpu
from jax.sharding import PartitionSpec as P

F32 = jnp.float32
BF16 = jnp.bfloat16
MESH = pl.DeviceIdType.MESH
SUB = 8
LANE = 128
BASE = 16
LEAD = 1
LAG = 3


def sub_bcast(x, q):
    return jnp.broadcast_to(x[q : q + 1, :], (SUB, LANE))


ALONG_LANES = lax.GatherDimensionNumbers(
    offset_dims=(), collapsed_slice_dims=(1,), start_index_map=(1,), operand_batching_dims=(0,), start_indices_batching_dims=(0,)
)


def lane_bcast(x, lane):
    index = jnp.full((SUB, LANE, 1), lane, jnp.int32)
    return lax.gather(x, index, ALONG_LANES, (1, 1), mode=lax.GatherScatterMode.PROMISE_IN_BOUNDS)


def split3(x):
    high = x.astype(BF16)
    rest = x - high.astype(F32)
    mid = rest.astype(BF16)
    return high, mid, (rest - mid.astype(F32)).astype(BF16)


def swap_rows(x, bit, row_id):
    if bit == SUB // 2:
        return pltpu.roll(x, bit, 0)
    return jnp.where((row_id & bit) == 0, pltpu.roll(x, SUB - bit, 0), pltpu.roll(x, bit, 0))


def stack_sums(parts):
    row_id = lax.broadcasted_iota(jnp.int32, (SUB, LANE), 0)
    for bit in (4, 2, 1):
        low = (row_id & bit) == 0
        half = len(parts) // 2
        parts = [
            jnp.where(low, parts[n], parts[n + half]) + swap_rows(jnp.where(low, parts[n + half], parts[n]), bit, row_id)
            for n in range(half)
        ]
    return parts[0]


def eliminate(rows, lane0):
    row_id = lax.broadcasted_iota(jnp.int32, (SUB, LANE), 0)
    rows = [list(rows[0]), list(rows[1])]
    cols = [
        [lane_bcast(rows[0][0], lane0 + j) for j in range(SUB)],
        [lane_bcast(rows[1][0], lane0 + j) for j in range(BASE)],
    ]
    scale = [jnp.zeros((SUB, LANE), F32), jnp.zeros((SUB, LANE), F32)]
    pivot = sub_bcast(cols[0][0], 0)
    for j in range(BASE):
        t, q = divmod(j, SUB)
        inv = lax.rsqrt(pivot)
        scale[t] = jnp.where(row_id == q, inv, scale[t])
        if j + 1 < BASE:
            tn, qn = divmod(j + 1, SUB)
            near = sub_bcast(cols[tn][j], qn) * inv
            pivot = sub_bcast(cols[tn][j + 1], qn) - near * near
        below = cols[1][j] * inv
        here = cols[0][j] * inv if t == 0 else None
        for n in range(j + 1, BASE):
            tn, qn = divmod(n, SUB)
            other = near if n == j + 1 else sub_bcast(here if tn == 0 else below, qn)
            if t == 0 and tn == 0:
                cols[0][n] = cols[0][n] - here * other
            cols[1][n] = cols[1][n] - below * other
        masked = jnp.where(row_id > q, here if t == 0 else below, 0.0)
        for v in range(len(rows[0])):
            pivot_row = sub_bcast(rows[t][v], q) * inv
            rows[t][v] = rows[t][v] - masked * pivot_row
            if t == 0:
                rows[1][v] = rows[1][v] - below * pivot_row
    return [[x * scale[t] for x in rows[t]] for t in range(2)]


def factor_block(work, winv, winv3, prev, fac):
    size = work.shape[1]
    prev[...] = jnp.zeros(prev.shape, F32)
    fac[...] = jnp.zeros(fac.shape, F32)

    def group(v):
        return slice(LANE * v, LANE * (v + 1))

    def pending(factors, before, t, v):
        above, below = before[:SUB, group(v)], before[SUB:, group(v)]
        at = 2 * SUB * t
        return stack_sums([factors[at + n] * above + factors[at + SUB + n] * below for n in range(SUB)])

    for half in range(size // LANE):
        views = [(work, 0), (work, 1), (winv, 0)] if half == 0 else [(work, 1), (winv, 0), (winv, 1)]
        first = half * LANE
        if half == 1:
            factors, before = fac[...], prev[...]
            work[first : first + BASE, group(1)] -= jnp.concatenate([pending(factors, before, t, 1) for t in range(2)], axis=0)
            prev[...] = jnp.concatenate([before[:, group(1)], before[:, group(2)], jnp.zeros((BASE, LANE), F32)], axis=1)

        def body(s, carry, views=views, first=first):
            lane0 = s * BASE
            row0 = pl.multiple_of(first + lane0, BASE)

            here = pl.ds(row0, BASE)
            then = pl.ds(pl.multiple_of(row0 + BASE, BASE), BASE)
            both = [ref[here, group(g)] for ref, g in views]
            rows = [[x[SUB * t : SUB * (t + 1)] for x in both] for t in range(2)]
            factors, before = fac[...], prev[...]
            for t in range(2):
                for v in (1, 2):
                    rows[t][v] = rows[t][v] - pending(factors, before, t, v)
            hi, mid, lo = split3(before)
            lane = lax.broadcasted_iota(jnp.int32, (BASE, size - first), 1) + first
            after = lane >= row0 + BASE
            lhi, lmid, llo = [jnp.where(after, x[:, : size - first], jnp.zeros((), BF16)) for x in (hi, mid, lo)]
            update = lax.dot_general(
                jnp.concatenate([lhi, lhi, lmid, lhi, llo, lmid], axis=0),
                jnp.concatenate([hi, mid, hi, lo, hi, mid], axis=0),
                (((0,), (0,)), ((), ())),
                preferred_element_type=F32,
            )
            for v, (ref, g) in enumerate(views):
                ref[first:size, group(g)] -= update[:, group(v)]
            done = eliminate(rows, lane0)
            if first == 0:
                source = [jnp.where(s == LANE // BASE - 1, done[t][1], done[t][0]) for t in range(2)]
            else:
                source = [done[t][0] for t in range(2)]
            next_lane = (lane0 + BASE) % LANE
            factors, sums = [], []
            for t in range(2):
                factor = [[lane_bcast(source[m], next_lane + SUB * t + n) for n in range(SUB)] for m in range(2)]
                sums.append(stack_sums([factor[0][n] * done[0][0] + factor[1][n] * done[1][0] for n in range(SUB)]))
                factors += factor[0] + factor[1]
            ref, g = views[0]
            ref[then, group(g)] -= jnp.concatenate(sums, axis=0)
            fac[...] = jnp.stack(factors)
            whole = [jnp.concatenate([done[0][v], done[1][v]], axis=0) for v in range(3)]
            prev[...] = jnp.concatenate(whole, axis=1)
            for (ref, g), x in zip(views, whole):
                ref[here, group(g)] = x
                if ref is winv:
                    for n, part in enumerate(split3(x)):
                        winv3[n, here, group(g)] = part
            return carry

        lax.fori_loop(0, LANE // BASE, body, 0)


def kernel(n_row, n_col, batch_axis, a_ref, o_ref, share, diag, edge, stage, first, panel, work, winv, winv3, prev, fac, load_sem, store_sem,
           seed_send, seed_recv, edge_send, edge_recv, first_sem, send_sem, pass_sem, recv_sem):
    row_blocks, size, local_cols = a_ref.shape
    col_blocks = local_cols // size
    ratio = n_col // n_row
    steps = row_blocks * n_row
    depth = pass_sem.shape[0]
    batch = lax.axis_index(batch_axis)
    row = lax.axis_index("row")
    col = lax.axis_index("col")
    odd = lax.rem(col, 2)
    on_diag = lax.rem(col, n_row) == row
    row_slots = n_row * (row_blocks * (row_blocks + 1) // 2)
    edge_slots = row_slots + n_col * (col_blocks * (col_blocks + 1) // 2)
    leads = row == LEAD

    def at(dev_row, dev_col):
        return (batch, dev_row, dev_col)

    def row_slot(k, a):
        g = k // n_row
        return n_row * (row_blocks * g - (g * (g - 1)) // 2) + (k - g * n_row) * (row_blocks - g) + a - g

    def col_slot(k, b):
        h = k // n_col
        return row_slots + n_col * (col_blocks * h - (h * (h - 1)) // 2) + (k - h * n_col) * (col_blocks - h) + b - h

    def first_a(k):
        return (k + n_row - row) // n_row

    def first_b(k):
        return (k + n_col - col) // n_col

    def home(ref, a, b):
        return ref.at[a, :, pl.ds(pl.multiple_of(b * size, size), size)]

    def spot(a, b):
        return b * row_blocks + a

    def col_of(k, b):
        return jnp.where(on_diag, row_slot(k, ratio * b + col // n_row), col_slot(k, b))

    def edge_slot(k, j):
        return edge_slots + 2 * k + (j - k - 1) // n_col

    def edge_reach(ahead):
        return jnp.logical_and(ahead >= 2, jnp.logical_and(ahead <= n_col + LAG, row != LEAD))

    def copy(src_slot, dst_slot, sem, device):
        return pltpu.make_async_remote_copy(
            src_ref=panel.at[src_slot], dst_ref=panel.at[dst_slot], send_sem=sem, recv_sem=recv_sem.at[dst_slot],
            device_id=device, device_id_type=MESH,
        )

    def arrived(slot):
        copy(slot, slot, send_sem.at[0, 0], at(row, col)).wait_recv()

    def start(c):
        c.start()

    def finish(c):
        c.wait_send()

    def from_maker(ahead, way):
        there = lax.rem(row + way, n_row)
        lead_near = jnp.logical_and(there == LEAD, jnp.logical_and(ahead >= 2, ahead <= n_row))
        soon_needed = jnp.logical_and(ahead == 2, way == 2)
        return jnp.logical_or(lead_near, soon_needed)

    def down_column(k, a, maker, sems, act):
        i = a * n_row + row
        slot = row_slot(k, a)
        dst = col_slot(k, i // n_col)
        for m, way in enumerate((1, n_row - 1, 2)):
            direct = from_maker(i - k, way)

            @pl.when(direct if maker else jnp.logical_not(direct))
            def _():
                act(copy(slot, dst, sems[m], at(lax.rem(row + way, n_row), lax.rem(i, n_col))))

    def last_near(p):
        return first_a(p + 3)

    def to_edge(k, a, sem, act):
        i = a * n_row + row
        act(copy(row_slot(k, a), edge_slot(k, i - 1), sem, at(LEAD, lax.rem(i - 1, n_col))))

    def source_sends(k, a, act):
        ahead = a * n_row + row - k
        slot = row_slot(k, a)
        early = n_row

        @pl.when(jnp.logical_and(edge_reach(ahead), jnp.logical_or(ahead <= early, ahead == n_col)))
        def _():
            to_edge(k, a, send_sem.at[a, 5], act)

        @pl.when(jnp.logical_and(ahead >= 2, ahead <= early))
        def _():
            down_column(k, a, True, [send_sem.at[a, m] for m in range(3)], act)

        @pl.when(lax.rem(ahead, n_col) == 0)
        def _():
            down_column(k, a, False, [send_sem.at[a, m] for m in range(3)], act)

        @pl.when(jnp.logical_or(jnp.logical_and(odd == 0, ahead >= 2), ahead >= n_col - 1))
        def _():
            act(copy(slot, slot, send_sem.at[a, 3], at(row, lax.rem(jnp.where(odd == 0, col + 1, col - 1), n_col))))

        @pl.when(ahead >= 2)
        def _():
            act(copy(slot, slot, send_sem.at[a, 6], at(row, lax.rem(col - odd + 2, n_col))))

        @pl.when(jnp.logical_and(ahead >= 3 - odd, a <= last_near(k)))
        def _():
            act(copy(slot, slot, send_sem.at[a, 4], at(row, lax.rem(col - odd + 3, n_col))))

        @pl.when(ahead >= n_col // 2 - odd)
        def _():
            act(copy(slot, slot, send_sem.at[a, 7], at(row, lax.rem(col - odd + 5, n_col))))

        @pl.when(ahead >= n_col - 2 - odd)
        def _():
            act(copy(slot, slot, send_sem.at[a, 8], at(row, lax.rem(col - odd - 1 + n_col, n_col))))

    def lead(p):
        return lax.rem(col - lax.rem(p, n_col) + n_col, n_col)

    def hops(p):
        return lax.rem(col // 2 - lax.rem(p, n_col) // 2 + n_col // 2, n_col // 2)

    def passes(p):
        return jnp.logical_and(odd == 1, hops(p) > 1)

    def first_passed(p):
        low = jnp.where(passes(p), jnp.maximum(lead(p) - 1, 2), lead(p))
        return (p + low - row + n_row - 1) // n_row

    def pass_down(p, a, act):
        i = a * n_row + row
        ahead = i - p
        sems = pass_sem.at[lax.rem(p, depth), a]

        @pl.when(jnp.logical_and(odd == 0, jnp.logical_and(lead(p) <= 2, a > last_near(p))))
        def _():
            act(copy(row_slot(p, a), row_slot(p, a), sems.at[3], at(row, col + 1)))

        @pl.when(jnp.logical_and(lax.rem(i, n_col) == col, ahead > 1))
        def _():
            @pl.when(jnp.logical_and(ahead > n_row, edge_reach(ahead)))
            def _():
                to_edge(p, a, sems.at[5], act)

            down_column(p, a, False, [sems.at[m] for m in range(3)], act)

    def pass_on(p, a, act):
        slot = row_slot(p, a)
        sems = pass_sem.at[lax.rem(p, depth), a]

        @pl.when(passes(p))
        def _():
            act(copy(slot, slot, sems.at[3], at(row, col - 1)))

        pass_down(p, a, act)

    def passed(p):
        @pl.when(lead(p) != 0)
        def _():
            loop(first_passed(p), row_blocks, lambda a: pass_on(p, a, finish))

    def receive(p, a):
        arrived(row_slot(p, a))
        pass_down(p, a, start)

    def receive_any(p, a):
        arrived(row_slot(p, a))
        pass_on(p, a, start)

    def loop(lo, hi, fn):
        lax.fori_loop(lo, hi, lambda n, c: (fn(n), c)[1], 0)

    for a in range(row_blocks):
        for b in range(col_blocks):
            pltpu.make_async_copy(home(a_ref, a, b), share.at[spot(a, b)], load_sem).start()

    barrier = pltpu.get_barrier_semaphore()
    n_dev = n_row * n_col

    def greet(n):
        other = lax.rem(row * n_col + col + n, n_dev)
        pl.semaphore_signal(barrier, inc=1, device_id=at(other // n_col, lax.rem(other, n_col)), device_id_type=MESH)

    loop(1, n_dev, greet)
    with jax.named_scope("all_here"):
        pl.semaphore_wait(barrier, n_dev - 1)
    with jax.named_scope("loaded"):
        pltpu.make_async_copy(share, share, load_sem).wait()

    def seed_copy(b, dev_row):
        return pltpu.make_async_remote_copy(
            src_ref=share.at[spot(ratio * b + col // n_row, b)], dst_ref=diag.at[b],
            send_sem=seed_send.at[b, lax.rem(dev_row - row + n_row, n_row)],
            recv_sem=seed_recv.at[b], device_id=at(dev_row, col), device_id_type=MESH,
        )

    def hand_out(b):
        @pl.when(on_diag)
        def _():
            for d in (1, n_row - 1, 2):
                seed_copy(b, lax.rem(row + d, n_row)).start()
            diag[b] = share[spot(ratio * b + col // n_row, b)]

        @pl.when(jnp.logical_and(holds_edge(b), jnp.logical_not(leads)))
        def _():
            stage[b] = share[spot((b * n_col + col + 1) // n_row, b)]
            edge_copy(b).start()

    def holds_edge(b):
        j = b * n_col + col
        return jnp.logical_and(lax.rem(j + 1, n_row) == row, j + 1 < steps)

    def edge_copy(b):
        return pltpu.make_async_remote_copy(
            src_ref=stage.at[b], dst_ref=edge.at[b], send_sem=edge_send.at[b], recv_sem=edge_recv.at[b],
            device_id=at(LEAD, col), device_id_type=MESH,
        )

    def has_edge(b):
        from_other = jnp.logical_and(leads, lax.rem(col + 1, n_row) != LEAD)
        return jnp.logical_and(from_other, b * n_col + col + 1 < steps)

    def edge_seeded(b):
        @pl.when(has_edge(b))
        def _():
            edge_copy(b).wait_recv()

    def edge_arrived(p, b):
        j = b * n_col + col

        @pl.when(jnp.logical_and(has_edge(b), j + 1 - p <= n_col + LAG))
        def _():
            arrived(edge_slot(p, j))

    hand_out(0)
    winv3[...] = jnp.zeros(winv3.shape, BF16)

    def seed_arrived(b):
        @pl.when(jnp.logical_not(on_diag))
        def _():
            seed_copy(b, row).wait_recv()

    with jax.named_scope("seed"):
        seed_arrived(0)

        @pl.when(col != 0)
        def _():
            edge_seeded(0)

    def clear(n):
        a, b = lax.rem(n, row_blocks), n // row_blocks

        @pl.when(a * n_row + row < b * n_col + col)
        def _():
            share[n] = jnp.zeros((size, size), F32)
            pltpu.make_async_copy(share.at[n], home(o_ref, a, b), store_sem).start()

    loop(0, row_blocks * col_blocks, clear)

    def times_t(x, y):
        return lax.dot_general(x, y, (((1,), (1,)), ((), ())), preferred_element_type=F32)

    def update_block(p, a, b):
        share[spot(a, b)] -= times_t(panel[row_slot(p, a)], panel[col_of(p, b)])

    def update_diag(p, b):
        other = panel[col_of(p, b)]
        diag[b] -= times_t(other, other)

    def update_edge(p, b):
        @pl.when(has_edge(b))
        def _():
            edge[b] -= times_t(panel[edge_slot(p, b * n_col + col)], panel[col_of(p, b)])

    def column_arrived(p, b):
        @pl.when(jnp.logical_not(on_diag))
        def _():
            arrived(col_slot(p, b))

    def update_column(p, b, lo):
        lone = lax.rem(row_blocks - lo, 2)

        @pl.when(lone == 1)
        def _():
            update_block(p, lo, b)

        def pair(m):
            a = lo + lone + 2 * m
            both = pl.ds(spot(a, b), 2)
            left = panel[pl.ds(row_slot(p, a), 2)].reshape(2 * size, size)
            share[both] -= times_t(left, panel[col_of(p, b)]).reshape(2, size, size)

        loop(0, (row_blocks - lo) // 2, pair)

    def trail(p, b_from, near):
        loop(b_from, col_blocks, lambda b: update_column(p, b, first_a(b * n_col + col - jnp.where(b == near, 0, 1))))

    def columns_arrived(p, b_from):
        def one(b):
            column_arrived(p, b)
            edge_arrived(p, b)

        loop(b_from, col_blocks, one)

    def prepare(b):
        work[size:, :] = jnp.zeros((BASE, size), F32)
        r_id = lax.broadcasted_iota(jnp.int32, (size + BASE, size), 0)
        c_id = lax.broadcasted_iota(jnp.int32, (size + BASE, size), 1)
        winv[...] = jnp.where(r_id == c_id, 1.0, 0.0).astype(F32)

    def times_winv_t(x):
        hi, mid, lo = split3(x)
        whi, wmid, wlo = winv3[0], winv3[1], winv3[2]
        small = times_t(lo, whi) + times_t(mid, wmid) + times_t(hi, wlo)
        return small + (times_t(mid, whi) + times_t(hi, wmid)) + times_t(hi, whi)

    def solve(k, a, count, near):
        kb = k // n_col
        here = pl.ds(spot(a, kb), count)

        def apply(p):
            left = panel[pl.ds(row_slot(p, a), count)].reshape(count * size, size)
            share[here] -= times_t(left, panel[col_of(p, kb)]).reshape(count, size, size)

        if not near:

            for m in range(count):

                @pl.when(k >= 3)
                def _():
                    receive(k - 3, a + m)

                @pl.when(jnp.logical_and(k >= 2, a + m > last_near(k - 2)))
                def _():
                    receive(k - 2, a + m)

            loop(jnp.maximum(k - 2 - LAG, 0), k - 1, apply)

        @pl.when(k > 0)
        def _():
            for m in range(count):
                receive(k - 1, a + m)
            apply(k - 1)

        x = times_winv_t(share[here].reshape(count * size, size)).reshape(count, size, size)
        panel[pl.ds(row_slot(k, a), count)] = x.astype(BF16)
        share[here] = x
        if near:

            @pl.when(jnp.logical_and(leads, lax.rem(k + 1, n_row) == LEAD))
            def _():
                first[...] = panel[row_slot(k, a)]
                first_out(k, start)

        if count == 1:
            source_sends(k, a, start)
        else:
            loop(a, a + count, lambda n: source_sends(k, n, start))
        for m in range(count):
            pltpu.make_async_copy(share.at[spot(a + m, kb)], home(o_ref, a + m, kb), store_sem).start()

    def update_near(p, b):
        update_diag(p, b)
        update_edge(p, b)

    def first_slot(k, dev_row):
        return jnp.where(lax.rem(k + 1, n_row) == dev_row, row_slot(k, (k + 1) // n_row), col_slot(k, (k + 1) // n_col))

    def first_copy(k, dev_row, sem):
        dst = first_slot(k, dev_row)
        return pltpu.make_async_remote_copy(
            src_ref=first, dst_ref=panel.at[dst], send_sem=sem, recv_sem=recv_sem.at[dst],
            device_id=at(dev_row, lax.rem(col + 1, n_col)), device_id_type=MESH,
        )

    def others_first(k, fn):
        urgent = lax.rem(k + 3, n_row)
        lone = urgent == LEAD
        for m in range(n_row - 1):
            fn(m, lax.rem(jnp.where(lone, LEAD + 1, urgent) + m + jnp.where(lax.rem(jnp.where(lone, LEAD + 1, urgent) - LEAD + n_row, n_row) + m >= n_row, 1, 0), n_row))

    def first_out(k, act):
        act(first_copy(k, LEAD, first_sem.at[0, 0]))

        @pl.when(odd == 0)
        def _():
            others_first(k, lambda m, r: act(first_copy(k, r, first_sem.at[0, 1 + m])))

    def first_down(k, act):
        @pl.when(odd == 0)
        def _():
            others_first(k, lambda m, r: act(copy(first_slot(k, LEAD), first_slot(k, r), first_sem.at[1, 1 + m], at(r, col))))

    def firsts_done(k):
        @pl.when(jnp.logical_and(leads, k + 1 < steps))
        def _():
            first_out(k, finish)

        @pl.when(jnp.logical_and(leads, k > 0))
        def _():
            first_down(k - 1, finish)

    @pl.when(col == 0)
    def _():
        prepare(0)
        work[0:size, :] = diag[0]

    def step(k):
        mine = jnp.logical_and(col == lax.rem(k, n_col), k < steps)
        kb = k // n_col
        last = k - 1
        soon = jnp.logical_and(col == lax.rem(k + 1, n_col), k + 1 < steps)

        @pl.when(mine)
        def _():
            with jax.named_scope("factor"):
                factor_block(work, winv, winv3, prev, fac)

            @pl.when(has_edge(kb))
            def _():
                with jax.named_scope("lead"):

                    @pl.when(k == 0)
                    def _():
                        edge_seeded(kb)

                    @pl.when(k > 0)
                    def _():
                        edge_arrived(last, kb)
                        update_edge(last, kb)

                    first[...] = times_winv_t(edge[kb]).astype(BF16)
                    first_out(k, start)

            lo = first_a(k)
            second = jnp.minimum(lo + 1, row_blocks)
            with jax.named_scope("solve_near"):
                loop(lo, second, lambda a: solve(k, a, 1, True))
            with jax.named_scope("solve_one"):
                third = second + lax.rem(row_blocks - second, 2)
                loop(second, third, lambda a: solve(k, a, 1, False))
            with jax.named_scope("solve_two"):
                loop(0, (row_blocks - third) // 2, lambda m: solve(k, third + 2 * m, 2, False))

        @pl.when(k >= depth)
        def _():
            with jax.named_scope("passed"):
                passed(k - depth)

        @pl.when(mine)
        def _():
            @pl.when(row == lax.rem(k, n_row))
            def _():
                for d in range(1, n_row):
                    seed_copy(kb, lax.rem(row + d, n_row)).wait_send()
                r_id = lax.broadcasted_iota(jnp.int32, (size, size), 0)
                c_id = lax.broadcasted_iota(jnp.int32, (size, size), 1)
                n = spot(k // n_row, kb)
                share[n] = jnp.where(r_id >= c_id, work[0:size, :].T, 0.0)
                pltpu.make_async_copy(share.at[n], home(o_ref, k // n_row, kb), store_sem).start()

            with jax.named_scope("late_trail"):

                def late(p):
                    columns_arrived(p, kb + 1)
                    trail(p, kb + 1, -1)

                loop(jnp.maximum(k - 2 - LAG, 0), k - LAG + 1, late)

            @pl.when(kb + 1 < col_blocks)
            def _():
                hand_out(kb + 1)

        @pl.when(jnp.logical_and(k > 0, jnp.logical_not(jnp.logical_or(mine, soon))))
        def _():
            @pl.when(col != lax.rem(last, n_col))
            def _():
                with jax.named_scope("receive"):
                    end = jnp.where(lead(last) == 3, jnp.minimum(last_near(last) + 1, row_blocks), row_blocks)
                    loop(first_passed(last), end, lambda a: receive_any(last, a))

            @pl.when(jnp.logical_and(k >= LAG, lead(last) != 3))
            def _():
                p = k - LAG
                near = first_b(k)
                with jax.named_scope("columns"):
                    columns_arrived(p, near)

                @pl.when(near < col_blocks)
                def _():
                    age = k + n_col - (near * n_col + col)

                    @pl.when(jnp.logical_and(age == 3, near > 0))
                    def _():
                        with jax.named_scope("seed_late"):
                            seed_arrived(near)
                            edge_seeded(near)

                    @pl.when(age >= 3)
                    def _():
                        oldest = jnp.where(age == 3, jnp.maximum(p - 2, 0), p)
                        loop(oldest, p + 1, lambda q: update_near(q, near))

                with jax.named_scope("trail"):
                    trail(p, near, near)

        @pl.when(soon)
        def _():
            nb = (k + 1) // n_col

            oldest = jnp.maximum(k - 1 - LAG, 0)
            lo = first_a(k + 1)

            def old_diag(p):
                column_arrived(p, nb)
                edge_arrived(p, nb)
                update_near(p, nb)

            def take(a):
                receive(last, a)

                @pl.when(jnp.logical_and(a * n_row + row > k + 1, a <= lo))
                def _():
                    loop(oldest, last, lambda p: update_block(p, a, nb))

            @pl.when(k > 0)
            def _():
                with jax.named_scope("old_diag"):
                    loop(oldest, last, old_diag)
                with jax.named_scope("take"):
                    loop(first_a(k), jnp.minimum(last_near(last) + 1, row_blocks), take)
                with jax.named_scope("take_column"):
                    column_arrived(last, nb)
                    edge_arrived(last, nb)
                with jax.named_scope("catch_up"):
                    update_near(last, nb)
                    loop(first_a(k + 1), jnp.minimum(first_a(k + 1) + 1, row_blocks), lambda a: update_block(last, a, nb))

            prepare(nb)
            slot = col_of(k, nb)
            with jax.named_scope("first_block"):
                arrived(slot)

            @pl.when(leads)
            def _():
                first_down(k, start)

            other = panel[slot]
            work[0:size, :] = diag[nb] - times_t(other, other)

        @pl.when(jnp.logical_and(k >= n_col // 2, col == lax.rem(k + n_col // 2, n_col)))
        def _():
            with jax.named_scope("sends_done"):
                firsts_done(k - n_col // 2)
                loop(first_a(k - n_col // 2), row_blocks, lambda a: source_sends(k - n_col // 2, a, finish))

    loop(0, steps + n_col // 2, step)

    def edges_done(b):
        @pl.when(jnp.logical_and(holds_edge(b), jnp.logical_not(leads)))
        def _():
            edge_copy(b).wait_send()

    loop(0, col_blocks, edges_done)
    with jax.named_scope("stored"):
        pltpu.make_async_copy(share, share, store_sem).wait()


def solution(mesh):
    n_row = mesh.shape["row"]
    n_col = mesh.shape["col"]

    def factor_local(a_loc):
        row_blocks, size, local_cols = a_loc.shape
        col_blocks = local_cols // size
        slots = n_row * (row_blocks * (row_blocks + 1) // 2) + n_col * (col_blocks * (col_blocks + 1) // 2)
        slots += 2 * row_blocks * n_row
        return pl.pallas_call(
            functools.partial(kernel, n_row, n_col, "batch"),
            out_shape=jax.ShapeDtypeStruct(a_loc.shape, F32),
            in_specs=[pl.BlockSpec(memory_space=pl.ANY)],
            out_specs=pl.BlockSpec(memory_space=pl.ANY),
            scratch_shapes=[
                pltpu.VMEM((row_blocks * col_blocks, size, size), F32),
                pltpu.VMEM((col_blocks, size, size), F32),
                pltpu.VMEM((col_blocks, size, size), F32),
                pltpu.VMEM((col_blocks, size, size), F32),
                pltpu.VMEM((size, size), BF16),
                pltpu.VMEM((slots, size, size), BF16),
                pltpu.VMEM((size + BASE, size), F32),
                pltpu.VMEM((size + BASE, size), F32),
                pltpu.VMEM((3, size, size), BF16),
                pltpu.VMEM((BASE, 3 * LANE), F32),
                pltpu.VMEM((4 * SUB, SUB, LANE), F32),
                pltpu.SemaphoreType.DMA,
                pltpu.SemaphoreType.DMA,
                pltpu.SemaphoreType.DMA((col_blocks, n_row)),
                pltpu.SemaphoreType.DMA((col_blocks,)),
                pltpu.SemaphoreType.DMA((col_blocks,)),
                pltpu.SemaphoreType.DMA((col_blocks,)),
                pltpu.SemaphoreType.DMA((2, n_row)),
                pltpu.SemaphoreType.DMA((row_blocks, 9)),
                pltpu.SemaphoreType.DMA((4, row_blocks, 6)),
                pltpu.SemaphoreType.DMA((slots,)),
            ],
            compiler_params=pltpu.CompilerParams(
                collective_id=0, has_side_effects=True, vmem_limit_bytes=60 * 1024 * 1024
            ),
            name="cholesky",
        )(a_loc)

    blk_spec = P(("batch", "row"), None, "col")
    return jax.shard_map(factor_local, mesh=mesh, in_specs=(blk_spec,), out_specs=blk_spec, check_vma=False)
```

```python
import functools

import jax
import jax.numpy as jnp
from jax import lax
from jax.experimental import pallas as pl
from jax.experimental.pallas import tpu as pltpu
from jax.sharding import PartitionSpec as P

F32 = jnp.float32
BF16 = jnp.bfloat16
MESH = pl.DeviceIdType.MESH
SUB = 8
LANE = 128
BASE = 16
LEAD = 1
LAG = 3


def sub_bcast(x, q):
    return jnp.broadcast_to(x[q : q + 1, :], (SUB, LANE))


ALONG_LANES = lax.GatherDimensionNumbers(
    offset_dims=(), collapsed_slice_dims=(1,), start_index_map=(1,), operand_batching_dims=(0,), start_indices_batching_dims=(0,)
)


def lane_bcast(x, lane):
    index = jnp.full((SUB, LANE, 1), lane, jnp.int32)
    return lax.gather(x, index, ALONG_LANES, (1, 1), mode=lax.GatherScatterMode.PROMISE_IN_BOUNDS)


def split3(x):
    high = x.astype(BF16)
    rest = x - high.astype(F32)
    mid = rest.astype(BF16)
    return high, mid, (rest - mid.astype(F32)).astype(BF16)


def swap_rows(x, bit, row_id):
    if bit == SUB // 2:
        return pltpu.roll(x, bit, 0)
    return jnp.where((row_id & bit) == 0, pltpu.roll(x, SUB - bit, 0), pltpu.roll(x, bit, 0))


def stack_sums(parts):
    row_id = lax.broadcasted_iota(jnp.int32, (SUB, LANE), 0)
    for bit in (4, 2, 1):
        low = (row_id & bit) == 0
        half = len(parts) // 2
        parts = [
            jnp.where(low, parts[n], parts[n + half]) + swap_rows(jnp.where(low, parts[n + half], parts[n]), bit, row_id)
            for n in range(half)
        ]
    return parts[0]


def eliminate(rows, lane0):
    row_id = lax.broadcasted_iota(jnp.int32, (SUB, LANE), 0)
    rows = [list(rows[0]), list(rows[1])]
    cols = [
        [lane_bcast(rows[0][0], lane0 + j) for j in range(SUB)],
        [lane_bcast(rows[1][0], lane0 + j) for j in range(BASE)],
    ]
    scale = [jnp.zeros((SUB, LANE), F32), jnp.zeros((SUB, LANE), F32)]
    pivot = sub_bcast(cols[0][0], 0)
    for j in range(BASE):
        t, q = divmod(j, SUB)
        inv = lax.rsqrt(pivot)
        scale[t] = jnp.where(row_id == q, inv, scale[t])
        if j + 1 < BASE:
            tn, qn = divmod(j + 1, SUB)
            near = sub_bcast(cols[tn][j], qn) * inv
            pivot = sub_bcast(cols[tn][j + 1], qn) - near * near
        below = cols[1][j] * inv
        here = cols[0][j] * inv if t == 0 else None
        for n in range(j + 1, BASE):
            tn, qn = divmod(n, SUB)
            other = near if n == j + 1 else sub_bcast(here if tn == 0 else below, qn)
            if t == 0 and tn == 0:
                cols[0][n] = cols[0][n] - here * other
            cols[1][n] = cols[1][n] - below * other
        masked = jnp.where(row_id > q, here if t == 0 else below, 0.0)
        for v in range(len(rows[0])):
            pivot_row = sub_bcast(rows[t][v], q) * inv
            rows[t][v] = rows[t][v] - masked * pivot_row
            if t == 0:
                rows[1][v] = rows[1][v] - below * pivot_row
    return [[x * scale[t] for x in rows[t]] for t in range(2)]


def factor_block(work, winv, winv3, prev, fac):
    size = work.shape[1]
    prev[...] = jnp.zeros(prev.shape, F32)
    fac[...] = jnp.zeros(fac.shape, F32)

    def group(v):
        return slice(LANE * v, LANE * (v + 1))

    def pending(factors, before, t, v):
        above, below = before[:SUB, group(v)], before[SUB:, group(v)]
        at = 2 * SUB * t
        return stack_sums([factors[at + n] * above + factors[at + SUB + n] * below for n in range(SUB)])

    for half in range(size // LANE):
        views = [(work, 0), (work, 1), (winv, 0)] if half == 0 else [(work, 1), (winv, 0), (winv, 1)]
        first = half * LANE
        if half == 1:
            factors, before = fac[...], prev[...]
            work[first : first + BASE, group(1)] -= jnp.concatenate([pending(factors, before, t, 1) for t in range(2)], axis=0)
            prev[...] = jnp.concatenate([before[:, group(1)], before[:, group(2)], jnp.zeros((BASE, LANE), F32)], axis=1)

        def body(s, carry, views=views, first=first):
            lane0 = s * BASE
            row0 = pl.multiple_of(first + lane0, BASE)

            here = pl.ds(row0, BASE)
            then = pl.ds(pl.multiple_of(row0 + BASE, BASE), BASE)
            both = [ref[here, group(g)] for ref, g in views]
            rows = [[x[SUB * t : SUB * (t + 1)] for x in both] for t in range(2)]
            factors, before = fac[...], prev[...]
            for t in range(2):
                for v in (1, 2):
                    rows[t][v] = rows[t][v] - pending(factors, before, t, v)
            hi, mid, lo = split3(before)
            lane = lax.broadcasted_iota(jnp.int32, (BASE, size - first), 1) + first
            after = lane >= row0 + BASE
            lhi, lmid, llo = [jnp.where(after, x[:, : size - first], jnp.zeros((), BF16)) for x in (hi, mid, lo)]
            update = lax.dot_general(
                jnp.concatenate([lhi, lhi, lmid, lhi, llo, lmid], axis=0),
                jnp.concatenate([hi, mid, hi, lo, hi, mid], axis=0),
                (((0,), (0,)), ((), ())),
                preferred_element_type=F32,
            )
            for v, (ref, g) in enumerate(views):
                ref[first:size, group(g)] -= update[:, group(v)]
            done = eliminate(rows, lane0)
            if first == 0:
                source = [jnp.where(s == LANE // BASE - 1, done[t][1], done[t][0]) for t in range(2)]
            else:
                source = [done[t][0] for t in range(2)]
            next_lane = (lane0 + BASE) % LANE
            factors, sums = [], []
            for t in range(2):
                factor = [[lane_bcast(source[m], next_lane + SUB * t + n) for n in range(SUB)] for m in range(2)]
                sums.append(stack_sums([factor[0][n] * done[0][0] + factor[1][n] * done[1][0] for n in range(SUB)]))
                factors += factor[0] + factor[1]
            ref, g = views[0]
            ref[then, group(g)] -= jnp.concatenate(sums, axis=0)
            fac[...] = jnp.stack(factors)
            whole = [jnp.concatenate([done[0][v], done[1][v]], axis=0) for v in range(3)]
            prev[...] = jnp.concatenate(whole, axis=1)
            for (ref, g), x in zip(views, whole):
                ref[here, group(g)] = x
                if ref is winv:
                    for n, part in enumerate(split3(x)):
                        winv3[n, here, group(g)] = part
            return carry

        lax.fori_loop(0, LANE // BASE, body, 0)


def kernel(n_row, n_col, batch_axis, a_ref, o_ref, share, diag, edge, stage, first, panel, work, winv, winv3, prev, fac, load_sem, store_sem,
           seed_send, seed_recv, edge_send, edge_recv, first_sem, send_sem, pass_sem, recv_sem):
    row_blocks, size, local_cols = a_ref.shape
    col_blocks = local_cols // size
    ratio = n_col // n_row
    steps = row_blocks * n_row
    depth = pass_sem.shape[0]
    batch = lax.axis_index(batch_axis)
    row = lax.axis_index("row")
    col = lax.axis_index("col")
    odd = lax.rem(col, 2)
    on_diag = lax.rem(col, n_row) == row
    row_slots = n_row * (row_blocks * (row_blocks + 1) // 2)
    edge_slots = row_slots + n_col * (col_blocks * (col_blocks + 1) // 2)
    leads = row == LEAD

    def at(dev_row, dev_col):
        return (batch, dev_row, dev_col)

    def row_slot(k, a):
        g = k // n_row
        return n_row * (row_blocks * g - (g * (g - 1)) // 2) + (k - g * n_row) * (row_blocks - g) + a - g

    def col_slot(k, b):
        h = k // n_col
        return row_slots + n_col * (col_blocks * h - (h * (h - 1)) // 2) + (k - h * n_col) * (col_blocks - h) + b - h

    def first_a(k):
        return (k + n_row - row) // n_row

    def first_b(k):
        return (k + n_col - col) // n_col

    def home(ref, a, b):
        return ref.at[a, :, pl.ds(pl.multiple_of(b * size, size), size)]

    def spot(a, b):
        return b * row_blocks + a

    def col_of(k, b):
        return jnp.where(on_diag, row_slot(k, ratio * b + col // n_row), col_slot(k, b))

    def edge_slot(k, j):
        return edge_slots + 2 * k + (j - k - 1) // n_col

    def edge_reach(ahead):
        return jnp.logical_and(ahead >= 2, jnp.logical_and(ahead <= n_col + LAG, row != LEAD))

    def copy(src_slot, dst_slot, sem, device):
        return pltpu.make_async_remote_copy(
            src_ref=panel.at[src_slot], dst_ref=panel.at[dst_slot], send_sem=sem, recv_sem=recv_sem.at[dst_slot],
            device_id=device, device_id_type=MESH,
        )

    def arrived(slot):
        copy(slot, slot, send_sem.at[0, 0], at(row, col)).wait_recv()

    def start(c):
        c.start()

    def finish(c):
        c.wait_send()

    def from_maker(ahead, way):
        there = lax.rem(row + way, n_row)
        lead_near = jnp.logical_and(there == LEAD, jnp.logical_and(ahead >= 2, ahead <= n_row))
        soon_needed = jnp.logical_and(ahead == 2, way == 2)
        return jnp.logical_or(lead_near, soon_needed)

    def down_column(k, a, maker, sems, act):
        i = a * n_row + row
        slot = row_slot(k, a)
        dst = col_slot(k, i // n_col)
        for m, way in enumerate((1, n_row - 1, 2)):
            direct = from_maker(i - k, way)

            @pl.when(direct if maker else jnp.logical_not(direct))
            def _():
                act(copy(slot, dst, sems[m], at(lax.rem(row + way, n_row), lax.rem(i, n_col))))

    def last_near(p):
        return first_a(p + 3)

    def to_edge(k, a, sem, act):
        i = a * n_row + row
        act(copy(row_slot(k, a), edge_slot(k, i - 1), sem, at(LEAD, lax.rem(i - 1, n_col))))

    def source_sends(k, a, act):
        ahead = a * n_row + row - k
        slot = row_slot(k, a)
        early = n_row

        @pl.when(jnp.logical_and(edge_reach(ahead), jnp.logical_or(ahead <= early, ahead == n_col)))
        def _():
            to_edge(k, a, send_sem.at[a, 5], act)

        @pl.when(jnp.logical_and(ahead >= 2, ahead <= early))
        def _():
            down_column(k, a, True, [send_sem.at[a, m] for m in range(3)], act)

        @pl.when(lax.rem(ahead, n_col) == 0)
        def _():
            down_column(k, a, False, [send_sem.at[a, m] for m in range(3)], act)

        @pl.when(jnp.logical_or(jnp.logical_and(odd == 0, ahead >= 2), ahead >= n_col - 1))
        def _():
            act(copy(slot, slot, send_sem.at[a, 3], at(row, lax.rem(jnp.where(odd == 0, col + 1, col - 1), n_col))))

        @pl.when(jnp.logical_and(ahead >= 2, a <= last_near(k)))
        def _():
            act(copy(slot, slot, send_sem.at[a, 6], at(row, lax.rem(col - odd + 2, n_col))))

        @pl.when(jnp.logical_and(ahead >= 3 - odd, a <= last_near(k)))
        def _():
            act(copy(slot, slot, send_sem.at[a, 4], at(row, lax.rem(col - odd + 3, n_col))))

        @pl.when(ahead >= n_col // 2 - odd)
        def _():
            act(copy(slot, slot, send_sem.at[a, 7], at(row, lax.rem(col - odd + 5, n_col))))

    def lead(p):
        return lax.rem(col - lax.rem(p, n_col) + n_col, n_col)

    def hops(p):
        return lax.rem(col // 2 - lax.rem(p, n_col) // 2 + n_col // 2, n_col // 2)

    def passes(p):
        return jnp.logical_and(odd == 1, hops(p) > 1)

    def first_passed(p):
        low = jnp.where(passes(p), jnp.maximum(lead(p) - 1, 2), lead(p))
        return (p + low - row + n_row - 1) // n_row

    def pass_down(p, a, act):
        i = a * n_row + row
        ahead = i - p
        sems = pass_sem.at[lax.rem(p, depth), a]

        @pl.when(jnp.logical_and(odd == 0, jnp.logical_and(lead(p) <= 2, a > last_near(p))))
        def _():
            act(copy(row_slot(p, a), row_slot(p, a), sems.at[3], at(row, col + 1)))

        @pl.when(jnp.logical_and(lax.rem(i, n_col) == col, ahead > 1))
        def _():
            @pl.when(jnp.logical_and(ahead > n_row, edge_reach(ahead)))
            def _():
                to_edge(p, a, sems.at[5], act)

            down_column(p, a, False, [sems.at[m] for m in range(3)], act)

    def pass_on(p, a, act):
        slot = row_slot(p, a)
        sems = pass_sem.at[lax.rem(p, depth), a]

        @pl.when(passes(p))
        def _():
            @pl.when(hops(p) == 2)
            def _():
                @pl.when(a * n_row + row - p >= n_col - 2 - lax.rem(p, 2))
                def _():
                    act(copy(slot, slot, sems.at[4], at(row, lax.rem(col + 2, n_col))))

                @pl.when(a > last_near(p))
                def _():
                    act(copy(slot, slot, sems.at[6], at(row, lax.rem(col - 3 + n_col, n_col))))

            act(copy(slot, slot, sems.at[3], at(row, col - 1)))

        pass_down(p, a, act)

    def passed(p):
        @pl.when(lead(p) != 0)
        def _():
            loop(first_passed(p), row_blocks, lambda a: pass_on(p, a, finish))

    def receive(p, a):
        arrived(row_slot(p, a))
        pass_down(p, a, start)

    def receive_any(p, a):
        arrived(row_slot(p, a))
        pass_on(p, a, start)

    def loop(lo, hi, fn):
        lax.fori_loop(lo, hi, lambda n, c: (fn(n), c)[1], 0)

    for a in range(row_blocks):
        for b in range(col_blocks):
            pltpu.make_async_copy(home(a_ref, a, b), share.at[spot(a, b)], load_sem).start()

    barrier = pltpu.get_barrier_semaphore()
    n_dev = n_row * n_col

    def greet(n):
        other = lax.rem(row * n_col + col + n, n_dev)
        pl.semaphore_signal(barrier, inc=1, device_id=at(other // n_col, lax.rem(other, n_col)), device_id_type=MESH)

    loop(1, n_dev, greet)
    with jax.named_scope("all_here"):
        pl.semaphore_wait(barrier, n_dev - 1)
    with jax.named_scope("loaded"):
        pltpu.make_async_copy(share, share, load_sem).wait()

    def seed_copy(b, dev_row):
        return pltpu.make_async_remote_copy(
            src_ref=share.at[spot(ratio * b + col // n_row, b)], dst_ref=diag.at[b],
            send_sem=seed_send.at[b, lax.rem(dev_row - row + n_row, n_row)],
            recv_sem=seed_recv.at[b], device_id=at(dev_row, col), device_id_type=MESH,
        )

    def hand_out(b):
        @pl.when(on_diag)
        def _():
            for d in (1, n_row - 1, 2):
                seed_copy(b, lax.rem(row + d, n_row)).start()
            diag[b] = share[spot(ratio * b + col // n_row, b)]

        @pl.when(jnp.logical_and(holds_edge(b), jnp.logical_not(leads)))
        def _():
            stage[b] = share[spot((b * n_col + col + 1) // n_row, b)]
            edge_copy(b).start()

    def holds_edge(b):
        j = b * n_col + col
        return jnp.logical_and(lax.rem(j + 1, n_row) == row, j + 1 < steps)

    def edge_copy(b):
        return pltpu.make_async_remote_copy(
            src_ref=stage.at[b], dst_ref=edge.at[b], send_sem=edge_send.at[b], recv_sem=edge_recv.at[b],
            device_id=at(LEAD, col), device_id_type=MESH,
        )

    def has_edge(b):
        from_other = jnp.logical_and(leads, lax.rem(col + 1, n_row) != LEAD)
        return jnp.logical_and(from_other, b * n_col + col + 1 < steps)

    def edge_seeded(b):
        @pl.when(has_edge(b))
        def _():
            edge_copy(b).wait_recv()

    def edge_arrived(p, b):
        j = b * n_col + col

        @pl.when(jnp.logical_and(has_edge(b), j + 1 - p <= n_col + LAG))
        def _():
            arrived(edge_slot(p, j))

    hand_out(0)
    winv3[...] = jnp.zeros(winv3.shape, BF16)

    def seed_arrived(b):
        @pl.when(jnp.logical_not(on_diag))
        def _():
            seed_copy(b, row).wait_recv()

    with jax.named_scope("seed"):
        seed_arrived(0)

        @pl.when(col != 0)
        def _():
            edge_seeded(0)

    def clear(n):
        a, b = lax.rem(n, row_blocks), n // row_blocks

        @pl.when(a * n_row + row < b * n_col + col)
        def _():
            share[n] = jnp.zeros((size, size), F32)
            pltpu.make_async_copy(share.at[n], home(o_ref, a, b), store_sem).start()

    loop(0, row_blocks * col_blocks, clear)

    def times_t(x, y):
        return lax.dot_general(x, y, (((1,), (1,)), ((), ())), preferred_element_type=F32)

    def update_block(p, a, b):
        share[spot(a, b)] -= times_t(panel[row_slot(p, a)], panel[col_of(p, b)])

    def update_diag(p, b):
        other = panel[col_of(p, b)]
        diag[b] -= times_t(other, other)

    def update_edge(p, b):
        @pl.when(has_edge(b))
        def _():
            edge[b] -= times_t(panel[edge_slot(p, b * n_col + col)], panel[col_of(p, b)])

    def column_arrived(p, b):
        @pl.when(jnp.logical_not(on_diag))
        def _():
            arrived(col_slot(p, b))

    def update_column(p, b, lo):
        lone = lax.rem(row_blocks - lo, 2)

        @pl.when(lone == 1)
        def _():
            update_block(p, lo, b)

        def pair(m):
            a = lo + lone + 2 * m
            both = pl.ds(spot(a, b), 2)
            left = panel[pl.ds(row_slot(p, a), 2)].reshape(2 * size, size)
            share[both] -= times_t(left, panel[col_of(p, b)]).reshape(2, size, size)

        loop(0, (row_blocks - lo) // 2, pair)

    def trail(p, b_from, near):
        loop(b_from, col_blocks, lambda b: update_column(p, b, first_a(b * n_col + col - jnp.where(b == near, 0, 1))))

    def columns_arrived(p, b_from):
        def one(b):
            column_arrived(p, b)
            edge_arrived(p, b)

        loop(b_from, col_blocks, one)

    def prepare(b):
        work[size:, :] = jnp.zeros((BASE, size), F32)
        r_id = lax.broadcasted_iota(jnp.int32, (size + BASE, size), 0)
        c_id = lax.broadcasted_iota(jnp.int32, (size + BASE, size), 1)
        winv[...] = jnp.where(r_id == c_id, 1.0, 0.0).astype(F32)

    def times_winv_t(x):
        hi, mid, lo = split3(x)
        whi, wmid, wlo = winv3[0], winv3[1], winv3[2]
        small = times_t(lo, whi) + times_t(mid, wmid) + times_t(hi, wlo)
        return small + (times_t(mid, whi) + times_t(hi, wmid)) + times_t(hi, whi)

    def solve(k, a, count, near):
        kb = k // n_col
        here = pl.ds(spot(a, kb), count)

        def apply(p):
            left = panel[pl.ds(row_slot(p, a), count)].reshape(count * size, size)
            share[here] -= times_t(left, panel[col_of(p, kb)]).reshape(count, size, size)

        if not near:

            for m in range(count):

                @pl.when(k >= 3)
                def _():
                    receive(k - 3, a + m)

                @pl.when(jnp.logical_and(k >= 2, a + m > last_near(k - 2)))
                def _():
                    receive(k - 2, a + m)

            loop(jnp.maximum(k - 2 - LAG, 0), k - 1, apply)

        @pl.when(k > 0)
        def _():
            for m in range(count):
                receive(k - 1, a + m)
            apply(k - 1)

        x = times_winv_t(share[here].reshape(count * size, size)).reshape(count, size, size)
        panel[pl.ds(row_slot(k, a), count)] = x.astype(BF16)
        share[here] = x
        if near:

            @pl.when(jnp.logical_and(leads, lax.rem(k + 1, n_row) == LEAD))
            def _():
                first[...] = panel[row_slot(k, a)]
                first_out(k, start)

        if count == 1:
            source_sends(k, a, start)
        else:
            loop(a, a + count, lambda n: source_sends(k, n, start))
        for m in range(count):
            pltpu.make_async_copy(share.at[spot(a + m, kb)], home(o_ref, a + m, kb), store_sem).start()

    def update_near(p, b):
        update_diag(p, b)
        update_edge(p, b)

    def first_slot(k, dev_row):
        return jnp.where(lax.rem(k + 1, n_row) == dev_row, row_slot(k, (k + 1) // n_row), col_slot(k, (k + 1) // n_col))

    def first_copy(k, dev_row, sem):
        dst = first_slot(k, dev_row)
        return pltpu.make_async_remote_copy(
            src_ref=first, dst_ref=panel.at[dst], send_sem=sem, recv_sem=recv_sem.at[dst],
            device_id=at(dev_row, lax.rem(col + 1, n_col)), device_id_type=MESH,
        )

    def others_first(k, fn):
        urgent = lax.rem(k + 3, n_row)
        lone = urgent == LEAD
        for m in range(n_row - 1):
            fn(m, lax.rem(jnp.where(lone, LEAD + 1, urgent) + m + jnp.where(lax.rem(jnp.where(lone, LEAD + 1, urgent) - LEAD + n_row, n_row) + m >= n_row, 1, 0), n_row))

    def first_out(k, act):
        act(first_copy(k, LEAD, first_sem.at[0, 0]))

        @pl.when(odd == 0)
        def _():
            others_first(k, lambda m, r: act(first_copy(k, r, first_sem.at[0, 1 + m])))

    def first_down(k, act):
        @pl.when(odd == 0)
        def _():
            others_first(k, lambda m, r: act(copy(first_slot(k, LEAD), first_slot(k, r), first_sem.at[1, 1 + m], at(r, col))))

    def firsts_done(k):
        @pl.when(jnp.logical_and(leads, k + 1 < steps))
        def _():
            first_out(k, finish)

        @pl.when(jnp.logical_and(leads, k > 0))
        def _():
            first_down(k - 1, finish)

    @pl.when(col == 0)
    def _():
        prepare(0)
        work[0:size, :] = diag[0]

    def step(k):
        mine = jnp.logical_and(col == lax.rem(k, n_col), k < steps)
        kb = k // n_col
        last = k - 1
        soon = jnp.logical_and(col == lax.rem(k + 1, n_col), k + 1 < steps)

        @pl.when(mine)
        def _():
            with jax.named_scope("factor"):
                factor_block(work, winv, winv3, prev, fac)

            @pl.when(has_edge(kb))
            def _():
                with jax.named_scope("lead"):

                    @pl.when(k == 0)
                    def _():
                        edge_seeded(kb)

                    @pl.when(k > 0)
                    def _():
                        edge_arrived(last, kb)
                        update_edge(last, kb)

                    first[...] = times_winv_t(edge[kb]).astype(BF16)
                    first_out(k, start)

            lo = first_a(k)
            second = jnp.minimum(lo + 1, row_blocks)
            with jax.named_scope("solve_near"):
                loop(lo, second, lambda a: solve(k, a, 1, True))
            with jax.named_scope("solve_one"):
                third = second + lax.rem(row_blocks - second, 2)
                loop(second, third, lambda a: solve(k, a, 1, False))
            with jax.named_scope("solve_two"):
                loop(0, (row_blocks - third) // 2, lambda m: solve(k, third + 2 * m, 2, False))

        @pl.when(k >= depth)
        def _():
            with jax.named_scope("passed"):
                passed(k - depth)

        @pl.when(mine)
        def _():
            @pl.when(row == lax.rem(k, n_row))
            def _():
                for d in range(1, n_row):
                    seed_copy(kb, lax.rem(row + d, n_row)).wait_send()
                r_id = lax.broadcasted_iota(jnp.int32, (size, size), 0)
                c_id = lax.broadcasted_iota(jnp.int32, (size, size), 1)
                n = spot(k // n_row, kb)
                share[n] = jnp.where(r_id >= c_id, work[0:size, :].T, 0.0)
                pltpu.make_async_copy(share.at[n], home(o_ref, k // n_row, kb), store_sem).start()

            with jax.named_scope("late_trail"):

                def late(p):
                    columns_arrived(p, kb + 1)
                    trail(p, kb + 1, -1)

                loop(jnp.maximum(k - 2 - LAG, 0), k - LAG + 1, late)

            @pl.when(kb + 1 < col_blocks)
            def _():
                hand_out(kb + 1)

        @pl.when(jnp.logical_and(k > 0, jnp.logical_not(jnp.logical_or(mine, soon))))
        def _():
            @pl.when(col != lax.rem(last, n_col))
            def _():
                with jax.named_scope("receive"):
                    end = jnp.where(lead(last) == 3, jnp.minimum(last_near(last) + 1, row_blocks), row_blocks)
                    loop(first_passed(last), end, lambda a: receive_any(last, a))

            @pl.when(jnp.logical_and(k >= LAG, lead(last) != 3))
            def _():
                p = k - LAG
                near = first_b(k)
                with jax.named_scope("columns"):
                    columns_arrived(p, near)

                @pl.when(near < col_blocks)
                def _():
                    age = k + n_col - (near * n_col + col)

                    @pl.when(jnp.logical_and(age == 3, near > 0))
                    def _():
                        with jax.named_scope("seed_late"):
                            seed_arrived(near)
                            edge_seeded(near)

                    @pl.when(age >= 3)
                    def _():
                        oldest = jnp.where(age == 3, jnp.maximum(p - 2, 0), p)
                        loop(oldest, p + 1, lambda q: update_near(q, near))

                with jax.named_scope("trail"):
                    trail(p, near, near)

        @pl.when(soon)
        def _():
            nb = (k + 1) // n_col

            oldest = jnp.maximum(k - 1 - LAG, 0)
            lo = first_a(k + 1)

            def old_diag(p):
                column_arrived(p, nb)
                edge_arrived(p, nb)
                update_near(p, nb)

            def take(a):
                receive(last, a)

                @pl.when(jnp.logical_and(a * n_row + row > k + 1, a <= lo))
                def _():
                    loop(oldest, last, lambda p: update_block(p, a, nb))

            @pl.when(k > 0)
            def _():
                with jax.named_scope("old_diag"):
                    loop(oldest, last, old_diag)
                with jax.named_scope("take"):
                    loop(first_a(k), jnp.minimum(last_near(last) + 1, row_blocks), take)
                with jax.named_scope("take_column"):
                    column_arrived(last, nb)
                    edge_arrived(last, nb)
                with jax.named_scope("catch_up"):
                    update_near(last, nb)
                    loop(first_a(k + 1), jnp.minimum(first_a(k + 1) + 1, row_blocks), lambda a: update_block(last, a, nb))

            prepare(nb)
            slot = col_of(k, nb)
            with jax.named_scope("first_block"):
                arrived(slot)

            @pl.when(leads)
            def _():
                first_down(k, start)

            other = panel[slot]
            work[0:size, :] = diag[nb] - times_t(other, other)

        @pl.when(jnp.logical_and(k >= n_col // 2, col == lax.rem(k + n_col // 2, n_col)))
        def _():
            with jax.named_scope("sends_done"):
                firsts_done(k - n_col // 2)
                loop(first_a(k - n_col // 2), row_blocks, lambda a: source_sends(k - n_col // 2, a, finish))

    loop(0, steps + n_col // 2, step)

    def edges_done(b):
        @pl.when(jnp.logical_and(holds_edge(b), jnp.logical_not(leads)))
        def _():
            edge_copy(b).wait_send()

    loop(0, col_blocks, edges_done)
    with jax.named_scope("stored"):
        pltpu.make_async_copy(share, share, store_sem).wait()


def solution(mesh):
    n_row = mesh.shape["row"]
    n_col = mesh.shape["col"]

    def factor_local(a_loc):
        row_blocks, size, local_cols = a_loc.shape
        col_blocks = local_cols // size
        slots = n_row * (row_blocks * (row_blocks + 1) // 2) + n_col * (col_blocks * (col_blocks + 1) // 2)
        slots += 2 * row_blocks * n_row
        return pl.pallas_call(
            functools.partial(kernel, n_row, n_col, "batch"),
            out_shape=jax.ShapeDtypeStruct(a_loc.shape, F32),
            in_specs=[pl.BlockSpec(memory_space=pl.ANY)],
            out_specs=pl.BlockSpec(memory_space=pl.ANY),
            scratch_shapes=[
                pltpu.VMEM((row_blocks * col_blocks, size, size), F32),
                pltpu.VMEM((col_blocks, size, size), F32),
                pltpu.VMEM((col_blocks, size, size), F32),
                pltpu.VMEM((col_blocks, size, size), F32),
                pltpu.VMEM((size, size), BF16),
                pltpu.VMEM((slots, size, size), BF16),
                pltpu.VMEM((size + BASE, size), F32),
                pltpu.VMEM((size + BASE, size), F32),
                pltpu.VMEM((3, size, size), BF16),
                pltpu.VMEM((BASE, 3 * LANE), F32),
                pltpu.VMEM((4 * SUB, SUB, LANE), F32),
                pltpu.SemaphoreType.DMA,
                pltpu.SemaphoreType.DMA,
                pltpu.SemaphoreType.DMA((col_blocks, n_row)),
                pltpu.SemaphoreType.DMA((col_blocks,)),
                pltpu.SemaphoreType.DMA((col_blocks,)),
                pltpu.SemaphoreType.DMA((col_blocks,)),
                pltpu.SemaphoreType.DMA((2, n_row)),
                pltpu.SemaphoreType.DMA((row_blocks, 9)),
                pltpu.SemaphoreType.DMA((4, row_blocks, 7)),
                pltpu.SemaphoreType.DMA((slots,)),
            ],
            compiler_params=pltpu.CompilerParams(
                collective_id=0, has_side_effects=True, vmem_limit_bytes=60 * 1024 * 1024
            ),
            name="cholesky",
        )(a_loc)

    blk_spec = P(("batch", "row"), None, "col")
    return jax.shard_map(factor_local, mesh=mesh, in_specs=(blk_spec,), out_specs=blk_spec, check_vma=False)
```

```python
import functools

import jax
import jax.numpy as jnp
from jax import lax
from jax.experimental import pallas as pl
from jax.experimental.pallas import tpu as pltpu
from jax.sharding import PartitionSpec as P

F32 = jnp.float32
BF16 = jnp.bfloat16
MESH = pl.DeviceIdType.MESH
SUB = 8
LANE = 128
BASE = 16
LEAD = 1
LAG = 3


def sub_bcast(x, q):
    return jnp.broadcast_to(x[q : q + 1, :], (SUB, LANE))


ALONG_LANES = lax.GatherDimensionNumbers(
    offset_dims=(), collapsed_slice_dims=(1,), start_index_map=(1,), operand_batching_dims=(0,), start_indices_batching_dims=(0,)
)


def lane_bcast(x, lane):
    index = jnp.full((SUB, LANE, 1), lane, jnp.int32)
    return lax.gather(x, index, ALONG_LANES, (1, 1), mode=lax.GatherScatterMode.PROMISE_IN_BOUNDS)


def split3(x):
    high = x.astype(BF16)
    rest = x - high.astype(F32)
    mid = rest.astype(BF16)
    return high, mid, (rest - mid.astype(F32)).astype(BF16)


def swap_rows(x, bit, row_id):
    if bit == SUB // 2:
        return pltpu.roll(x, bit, 0)
    return jnp.where((row_id & bit) == 0, pltpu.roll(x, SUB - bit, 0), pltpu.roll(x, bit, 0))


def stack_sums(parts):
    row_id = lax.broadcasted_iota(jnp.int32, (SUB, LANE), 0)
    for bit in (4, 2, 1):
        low = (row_id & bit) == 0
        half = len(parts) // 2
        parts = [
            jnp.where(low, parts[n], parts[n + half]) + swap_rows(jnp.where(low, parts[n + half], parts[n]), bit, row_id)
            for n in range(half)
        ]
    return parts[0]


def eliminate(rows, lane0):
    row_id = lax.broadcasted_iota(jnp.int32, (SUB, LANE), 0)
    rows = [list(rows[0]), list(rows[1])]
    cols = [
        [lane_bcast(rows[0][0], lane0 + j) for j in range(SUB)],
        [lane_bcast(rows[1][0], lane0 + j) for j in range(BASE)],
    ]
    scale = [jnp.zeros((SUB, LANE), F32), jnp.zeros((SUB, LANE), F32)]
    pivot = sub_bcast(cols[0][0], 0)
    for j in range(BASE):
        t, q = divmod(j, SUB)
        inv = lax.rsqrt(pivot)
        scale[t] = jnp.where(row_id == q, inv, scale[t])
        if j + 1 < BASE:
            tn, qn = divmod(j + 1, SUB)
            near = sub_bcast(cols[tn][j], qn) * inv
            pivot = sub_bcast(cols[tn][j + 1], qn) - near * near
        below = cols[1][j] * inv
        here = cols[0][j] * inv if t == 0 else None
        for n in range(j + 1, BASE):
            tn, qn = divmod(n, SUB)
            other = near if n == j + 1 else sub_bcast(here if tn == 0 else below, qn)
            if t == 0 and tn == 0:
                cols[0][n] = cols[0][n] - here * other
            cols[1][n] = cols[1][n] - below * other
        masked = jnp.where(row_id > q, here if t == 0 else below, 0.0)
        for v in range(len(rows[0])):
            pivot_row = sub_bcast(rows[t][v], q) * inv
            rows[t][v] = rows[t][v] - masked * pivot_row
            if t == 0:
                rows[1][v] = rows[1][v] - below * pivot_row
    return [[x * scale[t] for x in rows[t]] for t in range(2)]


def factor_block(work, winv, winv3, prev, fac):
    size = work.shape[1]
    prev[...] = jnp.zeros(prev.shape, F32)
    fac[...] = jnp.zeros(fac.shape, F32)

    def group(v):
        return slice(LANE * v, LANE * (v + 1))

    def pending(factors, before, t, v):
        above, below = before[:SUB, group(v)], before[SUB:, group(v)]
        at = 2 * SUB * t
        return stack_sums([factors[at + n] * above + factors[at + SUB + n] * below for n in range(SUB)])

    for half in range(size // LANE):
        views = [(work, 0), (work, 1), (winv, 0)] if half == 0 else [(work, 1), (winv, 0), (winv, 1)]
        first = half * LANE
        if half == 1:
            factors, before = fac[...], prev[...]
            work[first : first + BASE, group(1)] -= jnp.concatenate([pending(factors, before, t, 1) for t in range(2)], axis=0)
            prev[...] = jnp.concatenate([before[:, group(1)], before[:, group(2)], jnp.zeros((BASE, LANE), F32)], axis=1)

        def body(s, carry, views=views, first=first):
            lane0 = s * BASE
            row0 = pl.multiple_of(first + lane0, BASE)

            here = pl.ds(row0, BASE)
            then = pl.ds(pl.multiple_of(row0 + BASE, BASE), BASE)
            both = [ref[here, group(g)] for ref, g in views]
            rows = [[x[SUB * t : SUB * (t + 1)] for x in both] for t in range(2)]
            factors, before = fac[...], prev[...]
            for t in range(2):
                for v in (1, 2):
                    rows[t][v] = rows[t][v] - pending(factors, before, t, v)
            hi, mid, lo = split3(before)
            lane = lax.broadcasted_iota(jnp.int32, (BASE, size - first), 1) + first
            after = lane >= row0 + BASE
            lhi, lmid, llo = [jnp.where(after, x[:, : size - first], jnp.zeros((), BF16)) for x in (hi, mid, lo)]
            update = lax.dot_general(
                jnp.concatenate([lhi, lhi, lmid, lhi, llo, lmid], axis=0),
                jnp.concatenate([hi, mid, hi, lo, hi, mid], axis=0),
                (((0,), (0,)), ((), ())),
                preferred_element_type=F32,
            )
            for v, (ref, g) in enumerate(views):
                ref[first:size, group(g)] -= update[:, group(v)]
            done = eliminate(rows, lane0)
            if first == 0:
                source = [jnp.where(s == LANE // BASE - 1, done[t][1], done[t][0]) for t in range(2)]
            else:
                source = [done[t][0] for t in range(2)]
            next_lane = (lane0 + BASE) % LANE
            factors, sums = [], []
            for t in range(2):
                factor = [[lane_bcast(source[m], next_lane + SUB * t + n) for n in range(SUB)] for m in range(2)]
                sums.append(stack_sums([factor[0][n] * done[0][0] + factor[1][n] * done[1][0] for n in range(SUB)]))
                factors += factor[0] + factor[1]
            ref, g = views[0]
            ref[then, group(g)] -= jnp.concatenate(sums, axis=0)
            fac[...] = jnp.stack(factors)
            whole = [jnp.concatenate([done[0][v], done[1][v]], axis=0) for v in range(3)]
            prev[...] = jnp.concatenate(whole, axis=1)
            for (ref, g), x in zip(views, whole):
                ref[here, group(g)] = x
                if ref is winv:
                    for n, part in enumerate(split3(x)):
                        winv3[n, here, group(g)] = part
            return carry

        lax.fori_loop(0, LANE // BASE, body, 0)


def kernel(n_row, n_col, batch_axis, a_ref, o_ref, share, diag, edge, stage, first, panel, work, winv, winv3, prev, fac, load_sem, store_sem,
           seed_send, seed_recv, edge_send, edge_recv, first_sem, send_sem, pass_sem, recv_sem):
    row_blocks, size, local_cols = a_ref.shape
    col_blocks = local_cols // size
    ratio = n_col // n_row
    steps = row_blocks * n_row
    depth = pass_sem.shape[0]
    batch = lax.axis_index(batch_axis)
    row = lax.axis_index("row")
    col = lax.axis_index("col")
    odd = lax.rem(col, 2)
    on_diag = lax.rem(col, n_row) == row
    row_slots = n_row * (row_blocks * (row_blocks + 1) // 2)
    edge_slots = row_slots + n_col * (col_blocks * (col_blocks + 1) // 2)
    leads = row == LEAD

    def at(dev_row, dev_col):
        return (batch, dev_row, dev_col)

    def row_slot(k, a):
        g = k // n_row
        return n_row * (row_blocks * g - (g * (g - 1)) // 2) + (k - g * n_row) * (row_blocks - g) + a - g

    def col_slot(k, b):
        h = k // n_col
        return row_slots + n_col * (col_blocks * h - (h * (h - 1)) // 2) + (k - h * n_col) * (col_blocks - h) + b - h

    def first_a(k):
        return (k + n_row - row) // n_row

    def first_b(k):
        return (k + n_col - col) // n_col

    def home(ref, a, b):
        return ref.at[a, :, pl.ds(pl.multiple_of(b * size, size), size)]

    def spot(a, b):
        return b * row_blocks + a

    def col_of(k, b):
        return jnp.where(on_diag, row_slot(k, ratio * b + col // n_row), col_slot(k, b))

    def edge_slot(k, j):
        return edge_slots + 2 * k + (j - k - 1) // n_col

    def edge_reach(ahead):
        return jnp.logical_and(ahead >= 2, jnp.logical_and(ahead <= n_col + LAG, row != LEAD))

    def copy(src_slot, dst_slot, sem, device):
        return pltpu.make_async_remote_copy(
            src_ref=panel.at[src_slot], dst_ref=panel.at[dst_slot], send_sem=sem, recv_sem=recv_sem.at[dst_slot],
            device_id=device, device_id_type=MESH,
        )

    def arrived(slot):
        copy(slot, slot, send_sem.at[0, 0], at(row, col)).wait_recv()

    def start(c):
        c.start()

    def finish(c):
        c.wait_send()

    def from_maker(ahead, way):
        there = lax.rem(row + way, n_row)
        lead_near = jnp.logical_and(there == LEAD, jnp.logical_and(ahead >= 2, ahead <= n_row))
        soon_needed = jnp.logical_and(ahead == 2, way == 2)
        return jnp.logical_or(lead_near, soon_needed)

    def down_column(k, a, maker, sems, act):
        i = a * n_row + row
        slot = row_slot(k, a)
        dst = col_slot(k, i // n_col)
        for m, way in enumerate((1, n_row - 1, 2)):
            direct = from_maker(i - k, way)

            @pl.when(direct if maker else jnp.logical_not(direct))
            def _():
                act(copy(slot, dst, sems[m], at(lax.rem(row + way, n_row), lax.rem(i, n_col))))

    def last_near(p):
        return first_a(p + 3)

    def to_edge(k, a, sem, act):
        i = a * n_row + row
        act(copy(row_slot(k, a), edge_slot(k, i - 1), sem, at(LEAD, lax.rem(i - 1, n_col))))

    def source_sends(k, a, act):
        ahead = a * n_row + row - k
        slot = row_slot(k, a)
        early = n_row

        @pl.when(jnp.logical_and(edge_reach(ahead), jnp.logical_or(ahead <= early, ahead == n_col)))
        def _():
            to_edge(k, a, send_sem.at[a, 5], act)

        @pl.when(jnp.logical_and(ahead >= 2, ahead <= early))
        def _():
            down_column(k, a, True, [send_sem.at[a, m] for m in range(3)], act)

        @pl.when(lax.rem(ahead, n_col) == 0)
        def _():
            down_column(k, a, False, [send_sem.at[a, m] for m in range(3)], act)

        @pl.when(jnp.logical_or(jnp.logical_and(odd == 0, ahead >= 2), ahead >= n_col - 1))
        def _():
            act(copy(slot, slot, send_sem.at[a, 3], at(row, lax.rem(jnp.where(odd == 0, col + 1, col - 1), n_col))))

        @pl.when(ahead >= 2)
        def _():
            act(copy(slot, slot, send_sem.at[a, 6], at(row, lax.rem(col - odd + 2, n_col))))

        @pl.when(jnp.logical_and(ahead >= 3 - odd, a <= last_near(k)))
        def _():
            act(copy(slot, slot, send_sem.at[a, 4], at(row, lax.rem(col - odd + 3, n_col))))

        @pl.when(jnp.logical_and(ahead >= n_col // 2 - odd, ahead < n_col - 2 - odd))
        def _():
            act(copy(slot, slot, send_sem.at[a, 7], at(row, lax.rem(col - odd + 5, n_col))))

        @pl.when(ahead >= n_col - 2 - odd)
        def _():
            act(copy(slot, slot, send_sem.at[a, 8], at(row, lax.rem(col - odd - 2 + n_col, n_col))))

    def lead(p):
        return lax.rem(col - lax.rem(p, n_col) + n_col, n_col)

    def hops(p):
        return lax.rem(col // 2 - lax.rem(p, n_col) // 2 + n_col // 2, n_col // 2)

    def passes(p):
        return jnp.where(odd == 1, 2, n_col // 2 - 1) == hops(p)

    def first_passed(p):
        low = jnp.where(jnp.logical_and(passes(p), odd == 1), lead(p) - 1, lead(p))
        return (p + low - row + n_row - 1) // n_row

    def pass_down(p, a, act):
        i = a * n_row + row
        ahead = i - p
        sems = pass_sem.at[lax.rem(p, depth), a]

        @pl.when(jnp.logical_and(odd == 0, jnp.logical_and(lead(p) <= 2, a > last_near(p))))
        def _():
            act(copy(row_slot(p, a), row_slot(p, a), sems.at[3], at(row, col + 1)))

        @pl.when(jnp.logical_and(lax.rem(i, n_col) == col, ahead > 1))
        def _():
            @pl.when(jnp.logical_and(ahead > n_row, edge_reach(ahead)))
            def _():
                to_edge(p, a, sems.at[5], act)

            down_column(p, a, False, [sems.at[m] for m in range(3)], act)

    def pass_on(p, a, act):
        slot = row_slot(p, a)
        sems = pass_sem.at[lax.rem(p, depth), a]

        @pl.when(passes(p))
        def _():
            @pl.when(odd == 0)
            def _():
                act(copy(slot, slot, sems.at[4], at(row, lax.rem(col - 1 + n_col, n_col))))

            @pl.when(jnp.logical_or(odd == 1, a * n_row + row > p + lead(p)))
            def _():
                act(copy(slot, slot, sems.at[3], at(row, col + 1 - 2 * odd)))

        pass_down(p, a, act)

    def passed(p):
        @pl.when(lead(p) != 0)
        def _():
            loop(first_passed(p), row_blocks, lambda a: pass_on(p, a, finish))

    def receive(p, a):
        arrived(row_slot(p, a))
        pass_down(p, a, start)

    def receive_any(p, a):
        arrived(row_slot(p, a))
        pass_on(p, a, start)

    def loop(lo, hi, fn):
        lax.fori_loop(lo, hi, lambda n, c: (fn(n), c)[1], 0)

    for a in range(row_blocks):
        for b in range(col_blocks):
            pltpu.make_async_copy(home(a_ref, a, b), share.at[spot(a, b)], load_sem).start()

    barrier = pltpu.get_barrier_semaphore()
    n_dev = n_row * n_col

    def greet(n):
        other = lax.rem(row * n_col + col + n, n_dev)
        pl.semaphore_signal(barrier, inc=1, device_id=at(other // n_col, lax.rem(other, n_col)), device_id_type=MESH)

    loop(1, n_dev, greet)
    with jax.named_scope("all_here"):
        pl.semaphore_wait(barrier, n_dev - 1)
    with jax.named_scope("loaded"):
        pltpu.make_async_copy(share, share, load_sem).wait()

    def seed_copy(b, dev_row):
        return pltpu.make_async_remote_copy(
            src_ref=share.at[spot(ratio * b + col // n_row, b)], dst_ref=diag.at[b],
            send_sem=seed_send.at[b, lax.rem(dev_row - row + n_row, n_row)],
            recv_sem=seed_recv.at[b], device_id=at(dev_row, col), device_id_type=MESH,
        )

    def hand_out(b):
        @pl.when(on_diag)
        def _():
            for d in (1, n_row - 1, 2):
                seed_copy(b, lax.rem(row + d, n_row)).start()
            diag[b] = share[spot(ratio * b + col // n_row, b)]

        @pl.when(jnp.logical_and(holds_edge(b), jnp.logical_not(leads)))
        def _():
            stage[b] = share[spot((b * n_col + col + 1) // n_row, b)]
            edge_copy(b).start()

    def holds_edge(b):
        j = b * n_col + col
        return jnp.logical_and(lax.rem(j + 1, n_row) == row, j + 1 < steps)

    def edge_copy(b):
        return pltpu.make_async_remote_copy(
            src_ref=stage.at[b], dst_ref=edge.at[b], send_sem=edge_send.at[b], recv_sem=edge_recv.at[b],
            device_id=at(LEAD, col), device_id_type=MESH,
        )

    def has_edge(b):
        from_other = jnp.logical_and(leads, lax.rem(col + 1, n_row) != LEAD)
        return jnp.logical_and(from_other, b * n_col + col + 1 < steps)

    def edge_seeded(b):
        @pl.when(has_edge(b))
        def _():
            edge_copy(b).wait_recv()

    def edge_arrived(p, b):
        j = b * n_col + col

        @pl.when(jnp.logical_and(has_edge(b), j + 1 - p <= n_col + LAG))
        def _():
            arrived(edge_slot(p, j))

    hand_out(0)
    winv3[...] = jnp.zeros(winv3.shape, BF16)

    def seed_arrived(b):
        @pl.when(jnp.logical_not(on_diag))
        def _():
            seed_copy(b, row).wait_recv()

    with jax.named_scope("seed"):
        seed_arrived(0)

        @pl.when(col != 0)
        def _():
            edge_seeded(0)

    def clear(n):
        a, b = lax.rem(n, row_blocks), n // row_blocks

        @pl.when(a * n_row + row < b * n_col + col)
        def _():
            share[n] = jnp.zeros((size, size), F32)
            pltpu.make_async_copy(share.at[n], home(o_ref, a, b), store_sem).start()

    loop(0, row_blocks * col_blocks, clear)

    def times_t(x, y):
        return lax.dot_general(x, y, (((1,), (1,)), ((), ())), preferred_element_type=F32)

    def update_block(p, a, b):
        share[spot(a, b)] -= times_t(panel[row_slot(p, a)], panel[col_of(p, b)])

    def update_diag(p, b):
        other = panel[col_of(p, b)]
        diag[b] -= times_t(other, other)

    def update_edge(p, b):
        @pl.when(has_edge(b))
        def _():
            edge[b] -= times_t(panel[edge_slot(p, b * n_col + col)], panel[col_of(p, b)])

    def column_arrived(p, b):
        @pl.when(jnp.logical_not(on_diag))
        def _():
            arrived(col_slot(p, b))

    def update_column(p, b, lo):
        lone = lax.rem(row_blocks - lo, 2)

        @pl.when(lone == 1)
        def _():
            update_block(p, lo, b)

        def pair(m):
            a = lo + lone + 2 * m
            both = pl.ds(spot(a, b), 2)
            left = panel[pl.ds(row_slot(p, a), 2)].reshape(2 * size, size)
            share[both] -= times_t(left, panel[col_of(p, b)]).reshape(2, size, size)

        loop(0, (row_blocks - lo) // 2, pair)

    def trail(p, b_from, near):
        loop(b_from, col_blocks, lambda b: update_column(p, b, first_a(b * n_col + col - jnp.where(b == near, 0, 1))))

    def columns_arrived(p, b_from):
        def one(b):
            column_arrived(p, b)
            edge_arrived(p, b)

        loop(b_from, col_blocks, one)

    def prepare(b):
        work[size:, :] = jnp.zeros((BASE, size), F32)
        r_id = lax.broadcasted_iota(jnp.int32, (size + BASE, size), 0)
        c_id = lax.broadcasted_iota(jnp.int32, (size + BASE, size), 1)
        winv[...] = jnp.where(r_id == c_id, 1.0, 0.0).astype(F32)

    def times_winv_t(x):
        hi, mid, lo = split3(x)
        whi, wmid, wlo = winv3[0], winv3[1], winv3[2]
        small = times_t(lo, whi) + times_t(mid, wmid) + times_t(hi, wlo)
        return small + (times_t(mid, whi) + times_t(hi, wmid)) + times_t(hi, whi)

    def solve(k, a, count, near):
        kb = k // n_col
        here = pl.ds(spot(a, kb), count)

        def apply(p):
            left = panel[pl.ds(row_slot(p, a), count)].reshape(count * size, size)
            share[here] -= times_t(left, panel[col_of(p, kb)]).reshape(count, size, size)

        if not near:

            for m in range(count):

                @pl.when(k >= 3)
                def _():
                    receive(k - 3, a + m)

                @pl.when(jnp.logical_and(k >= 2, a + m > last_near(k - 2)))
                def _():
                    receive(k - 2, a + m)

            loop(jnp.maximum(k - 2 - LAG, 0), k - 1, apply)

        @pl.when(k > 0)
        def _():
            for m in range(count):
                receive(k - 1, a + m)
            apply(k - 1)

        x = times_winv_t(share[here].reshape(count * size, size)).reshape(count, size, size)
        panel[pl.ds(row_slot(k, a), count)] = x.astype(BF16)
        share[here] = x
        if near:

            @pl.when(jnp.logical_and(leads, lax.rem(k + 1, n_row) == LEAD))
            def _():
                first[...] = panel[row_slot(k, a)]
                first_out(k, start)

        if count == 1:
            source_sends(k, a, start)
        else:
            loop(a, a + count, lambda n: source_sends(k, n, start))
        for m in range(count):
            pltpu.make_async_copy(share.at[spot(a + m, kb)], home(o_ref, a + m, kb), store_sem).start()

    def update_near(p, b):
        update_diag(p, b)
        update_edge(p, b)

    def first_slot(k, dev_row):
        return jnp.where(lax.rem(k + 1, n_row) == dev_row, row_slot(k, (k + 1) // n_row), col_slot(k, (k + 1) // n_col))

    def first_copy(k, dev_row, sem):
        dst = first_slot(k, dev_row)
        return pltpu.make_async_remote_copy(
            src_ref=first, dst_ref=panel.at[dst], send_sem=sem, recv_sem=recv_sem.at[dst],
            device_id=at(dev_row, lax.rem(col + 1, n_col)), device_id_type=MESH,
        )

    def others_first(k, fn):
        urgent = lax.rem(k + 3, n_row)
        lone = urgent == LEAD
        for m in range(n_row - 1):
            fn(m, lax.rem(jnp.where(lone, LEAD + 1, urgent) + m + jnp.where(lax.rem(jnp.where(lone, LEAD + 1, urgent) - LEAD + n_row, n_row) + m >= n_row, 1, 0), n_row))

    def first_out(k, act):
        act(first_copy(k, LEAD, first_sem.at[0, 0]))

        @pl.when(odd == 0)
        def _():
            others_first(k, lambda m, r: act(first_copy(k, r, first_sem.at[0, 1 + m])))

    def first_down(k, act):
        @pl.when(odd == 0)
        def _():
            others_first(k, lambda m, r: act(copy(first_slot(k, LEAD), first_slot(k, r), first_sem.at[1, 1 + m], at(r, col))))

    def firsts_done(k):
        @pl.when(jnp.logical_and(leads, k + 1 < steps))
        def _():
            first_out(k, finish)

        @pl.when(jnp.logical_and(leads, k > 0))
        def _():
            first_down(k - 1, finish)

    @pl.when(col == 0)
    def _():
        prepare(0)
        work[0:size, :] = diag[0]

    def step(k):
        mine = jnp.logical_and(col == lax.rem(k, n_col), k < steps)
        kb = k // n_col
        last = k - 1
        soon = jnp.logical_and(col == lax.rem(k + 1, n_col), k + 1 < steps)

        @pl.when(mine)
        def _():
            with jax.named_scope("factor"):
                factor_block(work, winv, winv3, prev, fac)

            @pl.when(has_edge(kb))
            def _():
                with jax.named_scope("lead"):

                    @pl.when(k == 0)
                    def _():
                        edge_seeded(kb)

                    @pl.when(k > 0)
                    def _():
                        edge_arrived(last, kb)
                        update_edge(last, kb)

                    first[...] = times_winv_t(edge[kb]).astype(BF16)
                    first_out(k, start)

            lo = first_a(k)
            second = jnp.minimum(lo + 1, row_blocks)
            with jax.named_scope("solve_near"):
                loop(lo, second, lambda a: solve(k, a, 1, True))
            with jax.named_scope("solve_one"):
                third = second + lax.rem(row_blocks - second, 2)
                loop(second, third, lambda a: solve(k, a, 1, False))
            with jax.named_scope("solve_two"):
                loop(0, (row_blocks - third) // 2, lambda m: solve(k, third + 2 * m, 2, False))

        @pl.when(k >= depth)
        def _():
            with jax.named_scope("passed"):
                passed(k - depth)

        @pl.when(mine)
        def _():
            @pl.when(row == lax.rem(k, n_row))
            def _():
                for d in range(1, n_row):
                    seed_copy(kb, lax.rem(row + d, n_row)).wait_send()
                r_id = lax.broadcasted_iota(jnp.int32, (size, size), 0)
                c_id = lax.broadcasted_iota(jnp.int32, (size, size), 1)
                n = spot(k // n_row, kb)
                share[n] = jnp.where(r_id >= c_id, work[0:size, :].T, 0.0)
                pltpu.make_async_copy(share.at[n], home(o_ref, k // n_row, kb), store_sem).start()

            with jax.named_scope("late_trail"):

                def late(p):
                    columns_arrived(p, kb + 1)
                    trail(p, kb + 1, -1)

                loop(jnp.maximum(k - 2 - LAG, 0), k - LAG + 1, late)

            @pl.when(kb + 1 < col_blocks)
            def _():
                hand_out(kb + 1)

        @pl.when(jnp.logical_and(k > 0, jnp.logical_not(jnp.logical_or(mine, soon))))
        def _():
            @pl.when(col != lax.rem(last, n_col))
            def _():
                with jax.named_scope("receive"):
                    end = jnp.where(lead(last) == 3, jnp.minimum(last_near(last) + 1, row_blocks), row_blocks)
                    loop(first_passed(last), end, lambda a: receive_any(last, a))

            @pl.when(jnp.logical_and(k >= LAG, lead(last) != 3))
            def _():
                p = k - LAG
                near = first_b(k)
                with jax.named_scope("columns"):
                    columns_arrived(p, near)

                @pl.when(near < col_blocks)
                def _():
                    age = k + n_col - (near * n_col + col)

                    @pl.when(jnp.logical_and(age == 3, near > 0))
                    def _():
                        with jax.named_scope("seed_late"):
                            seed_arrived(near)
                            edge_seeded(near)

                    @pl.when(age >= 3)
                    def _():
                        oldest = jnp.where(age == 3, jnp.maximum(p - 2, 0), p)
                        loop(oldest, p + 1, lambda q: update_near(q, near))

                with jax.named_scope("trail"):
                    trail(p, near, near)

        @pl.when(soon)
        def _():
            nb = (k + 1) // n_col

            oldest = jnp.maximum(k - 1 - LAG, 0)
            lo = first_a(k + 1)

            def old_diag(p):
                column_arrived(p, nb)
                edge_arrived(p, nb)
                update_near(p, nb)

            def take(a):
                receive(last, a)

                @pl.when(jnp.logical_and(a * n_row + row > k + 1, a <= lo))
                def _():
                    loop(oldest, last, lambda p: update_block(p, a, nb))

            @pl.when(k > 0)
            def _():
                with jax.named_scope("old_diag"):
                    loop(oldest, last, old_diag)
                with jax.named_scope("take"):
                    loop(first_a(k), jnp.minimum(last_near(last) + 1, row_blocks), take)
                with jax.named_scope("take_column"):
                    column_arrived(last, nb)
                    edge_arrived(last, nb)
                with jax.named_scope("catch_up"):
                    update_near(last, nb)
                    loop(first_a(k + 1), jnp.minimum(first_a(k + 1) + 1, row_blocks), lambda a: update_block(last, a, nb))

            prepare(nb)
            slot = col_of(k, nb)
            with jax.named_scope("first_block"):
                arrived(slot)

            @pl.when(leads)
            def _():
                first_down(k, start)

            other = panel[slot]
            work[0:size, :] = diag[nb] - times_t(other, other)

        @pl.when(jnp.logical_and(k >= n_col // 2, col == lax.rem(k + n_col // 2, n_col)))
        def _():
            with jax.named_scope("sends_done"):
                firsts_done(k - n_col // 2)
                loop(first_a(k - n_col // 2), row_blocks, lambda a: source_sends(k - n_col // 2, a, finish))

    loop(0, steps + n_col // 2, step)

    def edges_done(b):
        @pl.when(jnp.logical_and(holds_edge(b), jnp.logical_not(leads)))
        def _():
            edge_copy(b).wait_send()

    loop(0, col_blocks, edges_done)
    with jax.named_scope("stored"):
        pltpu.make_async_copy(share, share, store_sem).wait()


def solution(mesh):
    n_row = mesh.shape["row"]
    n_col = mesh.shape["col"]

    def factor_local(a_loc):
        row_blocks, size, local_cols = a_loc.shape
        col_blocks = local_cols // size
        slots = n_row * (row_blocks * (row_blocks + 1) // 2) + n_col * (col_blocks * (col_blocks + 1) // 2)
        slots += 2 * row_blocks * n_row
        return pl.pallas_call(
            functools.partial(kernel, n_row, n_col, "batch"),
            out_shape=jax.ShapeDtypeStruct(a_loc.shape, F32),
            in_specs=[pl.BlockSpec(memory_space=pl.ANY)],
            out_specs=pl.BlockSpec(memory_space=pl.ANY),
            scratch_shapes=[
                pltpu.VMEM((row_blocks * col_blocks, size, size), F32),
                pltpu.VMEM((col_blocks, size, size), F32),
                pltpu.VMEM((col_blocks, size, size), F32),
                pltpu.VMEM((col_blocks, size, size), F32),
                pltpu.VMEM((size, size), BF16),
                pltpu.VMEM((slots, size, size), BF16),
                pltpu.VMEM((size + BASE, size), F32),
                pltpu.VMEM((size + BASE, size), F32),
                pltpu.VMEM((3, size, size), BF16),
                pltpu.VMEM((BASE, 3 * LANE), F32),
                pltpu.VMEM((4 * SUB, SUB, LANE), F32),
                pltpu.SemaphoreType.DMA,
                pltpu.SemaphoreType.DMA,
                pltpu.SemaphoreType.DMA((col_blocks, n_row)),
                pltpu.SemaphoreType.DMA((col_blocks,)),
                pltpu.SemaphoreType.DMA((col_blocks,)),
                pltpu.SemaphoreType.DMA((col_blocks,)),
                pltpu.SemaphoreType.DMA((2, n_row)),
                pltpu.SemaphoreType.DMA((row_blocks, 9)),
                pltpu.SemaphoreType.DMA((4, row_blocks, 6)),
                pltpu.SemaphoreType.DMA((slots,)),
            ],
            compiler_params=pltpu.CompilerParams(
                collective_id=0, has_side_effects=True, vmem_limit_bytes=60 * 1024 * 1024
            ),
            name="cholesky",
        )(a_loc)

    def factor_lower(a_loc):
        row_blocks, size, local_cols = a_loc.shape
        row_of = jnp.arange(row_blocks) * n_row + lax.axis_index("row")
        col_of = jnp.arange(local_cols) // size * n_col + lax.axis_index("col")
        return jnp.where(row_of[:, None, None] >= col_of[None, None, :], factor_local(a_loc), 0.0)

    blk_spec = P(("batch", "row"), None, "col")
    return jax.shard_map(factor_lower, mesh=mesh, in_specs=(blk_spec,), out_specs=blk_spec, check_vma=False)
```

```python
import functools

import jax
import jax.numpy as jnp
from jax import lax
from jax.experimental import pallas as pl
from jax.experimental.pallas import tpu as pltpu
from jax.sharding import PartitionSpec as P

F32 = jnp.float32
BF16 = jnp.bfloat16
MESH = pl.DeviceIdType.MESH
SUB = 8
LANE = 128
BASE = 16
LEAD = 1
SETTLE = 3
LAG = 3


def sub_bcast(x, q):
    return jnp.broadcast_to(x[q : q + 1, :], (SUB, LANE))


ALONG_LANES = lax.GatherDimensionNumbers(
    offset_dims=(), collapsed_slice_dims=(1,), start_index_map=(1,), operand_batching_dims=(0,), start_indices_batching_dims=(0,)
)


def lane_bcast(x, lane):
    index = jnp.full((SUB, LANE, 1), lane, jnp.int32)
    return lax.gather(x, index, ALONG_LANES, (1, 1), mode=lax.GatherScatterMode.PROMISE_IN_BOUNDS)


def split3(x):
    high = x.astype(BF16)
    rest = x - high.astype(F32)
    mid = rest.astype(BF16)
    return high, mid, (rest - mid.astype(F32)).astype(BF16)


def swap_rows(x, bit, row_id):
    if bit == SUB // 2:
        return pltpu.roll(x, bit, 0)
    return jnp.where((row_id & bit) == 0, pltpu.roll(x, SUB - bit, 0), pltpu.roll(x, bit, 0))


def stack_sums(parts):
    row_id = lax.broadcasted_iota(jnp.int32, (SUB, LANE), 0)
    for bit in (4, 2, 1):
        low = (row_id & bit) == 0
        half = len(parts) // 2
        parts = [
            jnp.where(low, parts[n], parts[n + half]) + swap_rows(jnp.where(low, parts[n + half], parts[n]), bit, row_id)
            for n in range(half)
        ]
    return parts[0]


def eliminate(rows, lane0):
    row_id = lax.broadcasted_iota(jnp.int32, (SUB, LANE), 0)
    rows = [list(rows[0]), list(rows[1])]
    cols = [
        [lane_bcast(rows[0][0], lane0 + j) for j in range(SUB)],
        [lane_bcast(rows[1][0], lane0 + j) for j in range(BASE)],
    ]
    scale = [jnp.zeros((SUB, LANE), F32), jnp.zeros((SUB, LANE), F32)]
    pivot = sub_bcast(cols[0][0], 0)
    for j in range(BASE):
        t, q = divmod(j, SUB)
        inv = lax.rsqrt(pivot)
        scale[t] = jnp.where(row_id == q, inv, scale[t])
        if j + 1 < BASE:
            tn, qn = divmod(j + 1, SUB)
            near = sub_bcast(cols[tn][j], qn) * inv
            pivot = sub_bcast(cols[tn][j + 1], qn) - near * near
        below = cols[1][j] * inv
        here = cols[0][j] * inv if t == 0 else None
        for n in range(j + 1, BASE):
            tn, qn = divmod(n, SUB)
            other = near if n == j + 1 else sub_bcast(here if tn == 0 else below, qn)
            if t == 0 and tn == 0:
                cols[0][n] = cols[0][n] - here * other
            cols[1][n] = cols[1][n] - below * other
        masked = jnp.where(row_id > q, here if t == 0 else below, 0.0)
        for v in range(len(rows[0])):
            pivot_row = sub_bcast(rows[t][v], q) * inv
            rows[t][v] = rows[t][v] - masked * pivot_row
            if t == 0:
                rows[1][v] = rows[1][v] - below * pivot_row
    return [[x * scale[t] for x in rows[t]] for t in range(2)]


def factor_block(work, winv, winv3, prev, fac):
    size = work.shape[1]
    prev[...] = jnp.zeros(prev.shape, F32)
    fac[...] = jnp.zeros(fac.shape, F32)

    def group(v):
        return slice(LANE * v, LANE * (v + 1))

    def pending(factors, before, t, v):
        above, below = before[:SUB, group(v)], before[SUB:, group(v)]
        at = 2 * SUB * t
        return stack_sums([factors[at + n] * above + factors[at + SUB + n] * below for n in range(SUB)])

    for half in range(size // LANE):
        views = [(work, 0), (work, 1), (winv, 0)] if half == 0 else [(work, 1), (winv, 0), (winv, 1)]
        first = half * LANE
        if half == 1:
            factors, before = fac[...], prev[...]
            work[first : first + BASE, group(1)] -= jnp.concatenate([pending(factors, before, t, 1) for t in range(2)], axis=0)
            prev[...] = jnp.concatenate([before[:, group(1)], before[:, group(2)], jnp.zeros((BASE, LANE), F32)], axis=1)

        def body(s, carry, views=views, first=first):
            lane0 = s * BASE
            row0 = pl.multiple_of(first + lane0, BASE)

            here = pl.ds(row0, BASE)
            then = pl.ds(pl.multiple_of(row0 + BASE, BASE), BASE)
            both = [ref[here, group(g)] for ref, g in views]
            rows = [[x[SUB * t : SUB * (t + 1)] for x in both] for t in range(2)]
            factors, before = fac[...], prev[...]
            for t in range(2):
                for v in (1, 2):
                    rows[t][v] = rows[t][v] - pending(factors, before, t, v)
            hi, mid, lo = split3(before)
            lane = lax.broadcasted_iota(jnp.int32, (BASE, size - first), 1) + first
            after = lane >= row0 + BASE
            lhi, lmid, llo = [jnp.where(after, x[:, : size - first], jnp.zeros((), BF16)) for x in (hi, mid, lo)]
            update = lax.dot_general(
                jnp.concatenate([lhi, lhi, lmid, lhi, llo, lmid], axis=0),
                jnp.concatenate([hi, mid, hi, lo, hi, mid], axis=0),
                (((0,), (0,)), ((), ())),
                preferred_element_type=F32,
            )
            for v, (ref, g) in enumerate(views):
                ref[first:size, group(g)] -= update[:, group(v)]
            done = eliminate(rows, lane0)
            if first == 0:
                source = [jnp.where(s == LANE // BASE - 1, done[t][1], done[t][0]) for t in range(2)]
            else:
                source = [done[t][0] for t in range(2)]
            next_lane = (lane0 + BASE) % LANE
            factors, sums = [], []
            for t in range(2):
                factor = [[lane_bcast(source[m], next_lane + SUB * t + n) for n in range(SUB)] for m in range(2)]
                sums.append(stack_sums([factor[0][n] * done[0][0] + factor[1][n] * done[1][0] for n in range(SUB)]))
                factors += factor[0] + factor[1]
            ref, g = views[0]
            ref[then, group(g)] -= jnp.concatenate(sums, axis=0)
            fac[...] = jnp.stack(factors)
            whole = [jnp.concatenate([done[0][v], done[1][v]], axis=0) for v in range(3)]
            prev[...] = jnp.concatenate(whole, axis=1)
            for (ref, g), x in zip(views, whole):
                ref[here, group(g)] = x
                if ref is winv:
                    for n, part in enumerate(split3(x)):
                        winv3[n, here, group(g)] = part
            return carry

        lax.fori_loop(0, LANE // BASE, body, 0)


def kernel(n_row, n_col, batch_axis, a_ref, o_ref, share, diag, edge, stage, first, panel, work, winv, winv3, prev, fac, load_sem, store_sem,
           seed_send, seed_recv, edge_send, edge_recv, first_sem, send_sem, pass_sem, recv_sem):
    row_blocks, size, local_cols = a_ref.shape
    col_blocks = local_cols // size
    ratio = n_col // n_row
    steps = row_blocks * n_row
    depth = pass_sem.shape[0]
    batch = lax.axis_index(batch_axis)
    row = lax.axis_index("row")
    col = lax.axis_index("col")
    odd = lax.rem(col, 2)
    on_diag = lax.rem(col, n_row) == row
    row_slots = n_row * (row_blocks * (row_blocks + 1) // 2)
    edge_slots = row_slots + n_col * (col_blocks * (col_blocks + 1) // 2)
    leads = row == LEAD

    def at(dev_row, dev_col):
        return (batch, dev_row, dev_col)

    def row_slot(k, a):
        g = k // n_row
        return n_row * (row_blocks * g - (g * (g - 1)) // 2) + (k - g * n_row) * (row_blocks - g) + a - g

    def col_slot(k, b):
        h = k // n_col
        return row_slots + n_col * (col_blocks * h - (h * (h - 1)) // 2) + (k - h * n_col) * (col_blocks - h) + b - h

    def first_a(k):
        return (k + n_row - row) // n_row

    def first_b(k):
        return (k + n_col - col) // n_col

    def home(ref, a, b):
        return ref.at[a, :, pl.ds(pl.multiple_of(b * size, size), size)]

    def spot(a, b):
        return b * row_blocks + a

    def col_of(k, b):
        return jnp.where(on_diag, row_slot(k, ratio * b + col // n_row), col_slot(k, b))

    def edge_slot(k, j):
        return edge_slots + 2 * k + (j - k - 1) // n_col

    def edge_reach(ahead):
        return jnp.logical_and(ahead >= 2, jnp.logical_and(ahead <= n_col + LAG - SETTLE, row != LEAD))

    def copy(src_slot, dst_slot, sem, device):
        return pltpu.make_async_remote_copy(
            src_ref=panel.at[src_slot], dst_ref=panel.at[dst_slot], send_sem=sem, recv_sem=recv_sem.at[dst_slot],
            device_id=device, device_id_type=MESH,
        )

    def arrived(slot):
        copy(slot, slot, send_sem.at[0, 0], at(row, col)).wait_recv()

    def start(c):
        c.start()

    def finish(c):
        c.wait_send()

    def from_maker(ahead, way):
        there = lax.rem(row + way, n_row)
        lead_near = jnp.logical_and(there == LEAD, jnp.logical_and(ahead >= 2, ahead <= n_row))
        soon_needed = jnp.logical_and(ahead == 2, way == 2)
        return jnp.logical_or(lead_near, soon_needed)

    def down_column(k, a, maker, sems, act):
        i = a * n_row + row
        slot = row_slot(k, a)
        dst = col_slot(k, i // n_col)
        for m, way in enumerate((1, n_row - 1, 2)):
            direct = from_maker(i - k, way)

            @pl.when(direct if maker else jnp.logical_not(direct))
            def _():
                act(copy(slot, dst, sems[m], at(lax.rem(row + way, n_row), lax.rem(i, n_col))))

    def last_near(p):
        return first_a(p + 3)

    def to_edge(k, a, sem, act):
        i = a * n_row + row
        act(copy(row_slot(k, a), edge_slot(k, i - 1), sem, at(LEAD, lax.rem(i - 1, n_col))))

    def source_sends(k, a, act):
        ahead = a * n_row + row - k
        slot = row_slot(k, a)
        early = n_row

        @pl.when(jnp.logical_and(edge_reach(ahead), jnp.logical_or(ahead <= early, ahead == n_col)))
        def _():
            to_edge(k, a, send_sem.at[a, 5], act)

        @pl.when(jnp.logical_and(ahead >= 2, ahead <= early))
        def _():
            down_column(k, a, True, [send_sem.at[a, m] for m in range(3)], act)

        @pl.when(lax.rem(ahead, n_col) == 0)
        def _():
            down_column(k, a, False, [send_sem.at[a, m] for m in range(3)], act)

        @pl.when(jnp.logical_or(jnp.logical_and(odd == 0, ahead >= 2), ahead >= n_col - 1))
        def _():
            act(copy(slot, slot, send_sem.at[a, 3], at(row, lax.rem(jnp.where(odd == 0, col + 1, col - 1), n_col))))

        @pl.when(ahead >= 2)
        def _():
            act(copy(slot, slot, send_sem.at[a, 6], at(row, lax.rem(col - odd + 2, n_col))))

        @pl.when(jnp.logical_and(ahead >= 3 - odd, a <= last_near(k)))
        def _():
            act(copy(slot, slot, send_sem.at[a, 4], at(row, lax.rem(col - odd + 3, n_col))))

        @pl.when(jnp.logical_and(ahead >= n_col // 2 - odd, ahead < n_col - 2 - odd))
        def _():
            act(copy(slot, slot, send_sem.at[a, 7], at(row, lax.rem(col - odd + 5, n_col))))

        @pl.when(ahead >= n_col - 2 - odd)
        def _():
            act(copy(slot, slot, send_sem.at[a, 8], at(row, lax.rem(col - odd - 2 + n_col, n_col))))

    def lead(p):
        return lax.rem(col - lax.rem(p, n_col) + n_col, n_col)

    def hops(p):
        return lax.rem(col // 2 - lax.rem(p, n_col) // 2 + n_col // 2, n_col // 2)

    def passes(p):
        return jnp.where(odd == 1, 2, n_col // 2 - 1) == hops(p)

    def first_passed(p):
        low = jnp.where(jnp.logical_and(passes(p), odd == 1), lead(p) - 1, lead(p))
        return (p + low - row + n_row - 1) // n_row

    def pass_down(p, a, act):
        i = a * n_row + row
        ahead = i - p
        sems = pass_sem.at[lax.rem(p, depth), a]

        @pl.when(jnp.logical_and(odd == 0, jnp.logical_and(lead(p) <= 2, a > last_near(p))))
        def _():
            act(copy(row_slot(p, a), row_slot(p, a), sems.at[3], at(row, col + 1)))

        @pl.when(jnp.logical_and(lax.rem(i, n_col) == col, ahead > 1))
        def _():
            @pl.when(jnp.logical_and(ahead > n_row, edge_reach(ahead)))
            def _():
                to_edge(p, a, sems.at[5], act)

            down_column(p, a, False, [sems.at[m] for m in range(3)], act)

    def pass_on(p, a, act):
        slot = row_slot(p, a)
        sems = pass_sem.at[lax.rem(p, depth), a]

        @pl.when(passes(p))
        def _():
            @pl.when(odd == 0)
            def _():
                act(copy(slot, slot, sems.at[4], at(row, lax.rem(col - 1 + n_col, n_col))))

            @pl.when(jnp.logical_or(odd == 1, a * n_row + row > p + lead(p)))
            def _():
                act(copy(slot, slot, sems.at[3], at(row, col + 1 - 2 * odd)))

        pass_down(p, a, act)

    def passed(p):
        @pl.when(lead(p) != 0)
        def _():
            loop(first_passed(p), row_blocks, lambda a: pass_on(p, a, finish))

    def receive(p, a):
        arrived(row_slot(p, a))
        pass_down(p, a, start)

    def receive_any(p, a):
        arrived(row_slot(p, a))
        pass_on(p, a, start)

    def loop(lo, hi, fn):
        lax.fori_loop(lo, hi, lambda n, c: (fn(n), c)[1], 0)

    for a in range(row_blocks):
        for b in range(col_blocks):
            pltpu.make_async_copy(home(a_ref, a, b), share.at[spot(a, b)], load_sem).start()

    barrier = pltpu.get_barrier_semaphore()
    n_dev = n_row * n_col

    def greet(n):
        other = lax.rem(row * n_col + col + n, n_dev)
        pl.semaphore_signal(barrier, inc=1, device_id=at(other // n_col, lax.rem(other, n_col)), device_id_type=MESH)

    loop(1, n_dev, greet)
    with jax.named_scope("all_here"):
        pl.semaphore_wait(barrier, n_dev - 1)
    with jax.named_scope("loaded"):
        pltpu.make_async_copy(share, share, load_sem).wait()

    def seed_copy(b, dev_row):
        return pltpu.make_async_remote_copy(
            src_ref=share.at[spot(ratio * b + col // n_row, b)], dst_ref=diag.at[b],
            send_sem=seed_send.at[b, lax.rem(dev_row - row + n_row, n_row)],
            recv_sem=seed_recv.at[b], device_id=at(dev_row, col), device_id_type=MESH,
        )

    def hand_out(b):
        @pl.when(on_diag)
        def _():
            for d in (1, n_row - 1, 2):
                seed_copy(b, lax.rem(row + d, n_row)).start()
            diag[b] = share[spot(ratio * b + col // n_row, b)]

        @pl.when(jnp.logical_and(holds_edge(b), jnp.logical_not(leads)))
        def _():
            stage[b] = share[spot((b * n_col + col + 1) // n_row, b)]
            edge_copy(b).start()

    def holds_edge(b):
        j = b * n_col + col
        return jnp.logical_and(lax.rem(j + 1, n_row) == row, j + 1 < steps)

    def edge_copy(b):
        return pltpu.make_async_remote_copy(
            src_ref=stage.at[b], dst_ref=edge.at[b], send_sem=edge_send.at[b], recv_sem=edge_recv.at[b],
            device_id=at(LEAD, col), device_id_type=MESH,
        )

    def has_edge(b):
        from_other = jnp.logical_and(leads, lax.rem(col + 1, n_row) != LEAD)
        return jnp.logical_and(from_other, b * n_col + col + 1 < steps)

    def edge_seeded(b):
        @pl.when(has_edge(b))
        def _():
            edge_copy(b).wait_recv()

    def edge_arrived(p, b):
        j = b * n_col + col

        @pl.when(jnp.logical_and(has_edge(b), j + 1 - p <= n_col + LAG - SETTLE))
        def _():
            arrived(edge_slot(p, j))

    hand_out(0)
    winv3[...] = jnp.zeros(winv3.shape, BF16)

    def seed_arrived(b):
        @pl.when(jnp.logical_not(on_diag))
        def _():
            seed_copy(b, row).wait_recv()

    with jax.named_scope("seed"):
        seed_arrived(0)

        @pl.when(col != 0)
        def _():
            edge_seeded(0)

    def clear(n):
        a, b = lax.rem(n, row_blocks), n // row_blocks

        @pl.when(a * n_row + row < b * n_col + col)
        def _():
            share[n] = jnp.zeros((size, size), F32)
            pltpu.make_async_copy(share.at[n], home(o_ref, a, b), store_sem).start()

    loop(0, row_blocks * col_blocks, clear)

    def times_t(x, y):
        return lax.dot_general(x, y, (((1,), (1,)), ((), ())), preferred_element_type=F32)

    def update_block(p, a, b):
        share[spot(a, b)] -= times_t(panel[row_slot(p, a)], panel[col_of(p, b)])

    def update_diag(p, b):
        other = panel[col_of(p, b)]
        diag[b] -= times_t(other, other)

    def update_edge(p, b):
        @pl.when(has_edge(b))
        def _():
            edge[b] -= times_t(panel[edge_slot(p, b * n_col + col)], panel[col_of(p, b)])

    def column_arrived(p, b):
        @pl.when(jnp.logical_not(on_diag))
        def _():
            arrived(col_slot(p, b))

    def update_column(p, b, lo):
        lone = lax.rem(row_blocks - lo, 2)

        @pl.when(lone == 1)
        def _():
            update_block(p, lo, b)

        def pair(m):
            a = lo + lone + 2 * m
            both = pl.ds(spot(a, b), 2)
            left = panel[pl.ds(row_slot(p, a), 2)].reshape(2 * size, size)
            share[both] -= times_t(left, panel[col_of(p, b)]).reshape(2, size, size)

        loop(0, (row_blocks - lo) // 2, pair)

    def trail(p, b_from, near):
        loop(b_from, col_blocks, lambda b: update_column(p, b, first_a(b * n_col + col - jnp.where(b == near, 0, 1))))

    def columns_arrived(p, b_from):
        def one(b):
            column_arrived(p, b)
            edge_arrived(p, b)

        loop(b_from, col_blocks, one)

    def prepare(b):
        work[size:, :] = jnp.zeros((BASE, size), F32)
        r_id = lax.broadcasted_iota(jnp.int32, (size + BASE, size), 0)
        c_id = lax.broadcasted_iota(jnp.int32, (size + BASE, size), 1)
        winv[...] = jnp.where(r_id == c_id, 1.0, 0.0).astype(F32)

    def times_winv_t(x):
        hi, mid, lo = split3(x)
        whi, wmid, wlo = winv3[0], winv3[1], winv3[2]
        small = times_t(lo, whi) + times_t(mid, wmid) + times_t(hi, wlo)
        return small + (times_t(mid, whi) + times_t(hi, wmid)) + times_t(hi, whi)

    def solve(k, a, count, near):
        kb = k // n_col
        here = pl.ds(spot(a, kb), count)

        def apply(p):
            left = panel[pl.ds(row_slot(p, a), count)].reshape(count * size, size)
            share[here] -= times_t(left, panel[col_of(p, kb)]).reshape(count, size, size)

        if not near:

            for m in range(count):

                @pl.when(k >= 3)
                def _():
                    receive(k - 3, a + m)

                @pl.when(jnp.logical_and(k >= 2, a + m > last_near(k - 2)))
                def _():
                    receive(k - 2, a + m)

            loop(jnp.maximum(k - 2 - LAG, 0), k - 1, apply)

        @pl.when(k > 0)
        def _():
            for m in range(count):
                receive(k - 1, a + m)
            apply(k - 1)

        x = times_winv_t(share[here].reshape(count * size, size)).reshape(count, size, size)
        panel[pl.ds(row_slot(k, a), count)] = x.astype(BF16)
        share[here] = x
        if near:

            @pl.when(jnp.logical_and(leads, lax.rem(k + 1, n_row) == LEAD))
            def _():
                first[...] = panel[row_slot(k, a)]
                first_out(k, start)

        if count == 1:
            source_sends(k, a, start)
        else:
            loop(a, a + count, lambda n: source_sends(k, n, start))
        for m in range(count):
            pltpu.make_async_copy(share.at[spot(a + m, kb)], home(o_ref, a + m, kb), store_sem).start()

    def update_near(p, b):
        update_diag(p, b)
        update_edge(p, b)

    def first_slot(k, dev_row):
        return jnp.where(lax.rem(k + 1, n_row) == dev_row, row_slot(k, (k + 1) // n_row), col_slot(k, (k + 1) // n_col))

    def first_copy(k, dev_row, sem):
        dst = first_slot(k, dev_row)
        return pltpu.make_async_remote_copy(
            src_ref=first, dst_ref=panel.at[dst], send_sem=sem, recv_sem=recv_sem.at[dst],
            device_id=at(dev_row, lax.rem(col + 1, n_col)), device_id_type=MESH,
        )

    def others_first(k, fn):
        urgent = lax.rem(k + 3, n_row)
        lone = urgent == LEAD
        for m in range(n_row - 1):
            fn(m, lax.rem(jnp.where(lone, LEAD + 1, urgent) + m + jnp.where(lax.rem(jnp.where(lone, LEAD + 1, urgent) - LEAD + n_row, n_row) + m >= n_row, 1, 0), n_row))

    def first_out(k, act):
        act(first_copy(k, LEAD, first_sem.at[0, 0]))

        @pl.when(odd == 0)
        def _():
            others_first(k, lambda m, r: act(first_copy(k, r, first_sem.at[0, 1 + m])))

    def first_down(k, act):
        @pl.when(odd == 0)
        def _():
            others_first(k, lambda m, r: act(copy(first_slot(k, LEAD), first_slot(k, r), first_sem.at[1, 1 + m], at(r, col))))

    def firsts_done(k):
        @pl.when(jnp.logical_and(leads, k + 1 < steps))
        def _():
            first_out(k, finish)

        @pl.when(jnp.logical_and(leads, k > 0))
        def _():
            first_down(k - 1, finish)

    @pl.when(col == 0)
    def _():
        prepare(0)
        work[0:size, :] = diag[0]

    def step(k):
        mine = jnp.logical_and(col == lax.rem(k, n_col), k < steps)
        kb = k // n_col
        last = k - 1
        soon = jnp.logical_and(col == lax.rem(k + 1, n_col), k + 1 < steps)

        @pl.when(mine)
        def _():
            with jax.named_scope("factor"):
                factor_block(work, winv, winv3, prev, fac)

            @pl.when(has_edge(kb))
            def _():
                with jax.named_scope("lead"):

                    @pl.when(k == 0)
                    def _():
                        edge_seeded(kb)

                    @pl.when(k > 0)
                    def _():
                        edge_arrived(last, kb)
                        update_edge(last, kb)

                    first[...] = times_winv_t(edge[kb]).astype(BF16)
                    first_out(k, start)

            lo = first_a(k)
            second = jnp.minimum(lo + 1, row_blocks)
            with jax.named_scope("solve_near"):
                loop(lo, second, lambda a: solve(k, a, 1, True))
            with jax.named_scope("solve_one"):
                third = second + lax.rem(row_blocks - second, 2)
                loop(second, third, lambda a: solve(k, a, 1, False))
            with jax.named_scope("solve_two"):
                loop(0, (row_blocks - third) // 2, lambda m: solve(k, third + 2 * m, 2, False))

        @pl.when(k >= depth)
        def _():
            with jax.named_scope("passed"):
                passed(k - depth)

        @pl.when(mine)
        def _():
            @pl.when(row == lax.rem(k, n_row))
            def _():
                for d in range(1, n_row):
                    seed_copy(kb, lax.rem(row + d, n_row)).wait_send()
                r_id = lax.broadcasted_iota(jnp.int32, (size, size), 0)
                c_id = lax.broadcasted_iota(jnp.int32, (size, size), 1)
                n = spot(k // n_row, kb)
                share[n] = jnp.where(r_id >= c_id, work[0:size, :].T, 0.0)
                pltpu.make_async_copy(share.at[n], home(o_ref, k // n_row, kb), store_sem).start()

        @pl.when(jnp.logical_and(k > 0, jnp.logical_not(jnp.logical_or(mine, soon))))
        def _():
            @pl.when(col != lax.rem(last, n_col))
            def _():
                with jax.named_scope("receive"):
                    end = jnp.where(lead(last) == 3, jnp.minimum(last_near(last) + 1, row_blocks), row_blocks)
                    loop(first_passed(last), end, lambda a: receive_any(last, a))

            near = first_b(k)
            age = k + n_col - (near * n_col + col)
            settle = jnp.logical_and(age == SETTLE, jnp.logical_and(near > 0, near < col_blocks))

            @pl.when(settle)
            def _():
                with jax.named_scope("late_trail"):
                    own = k - SETTLE

                    def late(p):
                        columns_arrived(p, near)
                        trail(p, near, -1)

                    loop(jnp.maximum(own - 2 - LAG, 0), own - LAG + 1, late)

            @pl.when(jnp.logical_and(k >= LAG, lead(last) != 3))
            def _():
                p = k - LAG
                with jax.named_scope("columns"):
                    columns_arrived(p, near)

                @pl.when(jnp.logical_and(near < col_blocks, age >= SETTLE + 2))
                def _():
                    @pl.when(jnp.logical_and(age == SETTLE + 2, near > 0))
                    def _():
                        with jax.named_scope("seed_late"):
                            seed_arrived(near)
                            edge_seeded(near)

                    oldest = jnp.where(age == SETTLE + 2, jnp.maximum(p - 1, 0), p)
                    loop(oldest, p + 1, lambda q: update_near(q, near))

                with jax.named_scope("trail"):
                    trail(p, near, jnp.where(jnp.logical_or(age > SETTLE, near == 0), near, -1))

            @pl.when(settle)
            def _():
                hand_out(near)

        @pl.when(soon)
        def _():
            nb = (k + 1) // n_col

            oldest = jnp.maximum(k - 1 - LAG, 0)
            lo = first_a(k + 1)

            def old_diag(p):
                column_arrived(p, nb)
                edge_arrived(p, nb)
                update_near(p, nb)

            def take(a):
                receive(last, a)

                @pl.when(jnp.logical_and(a * n_row + row > k + 1, a <= lo))
                def _():
                    loop(oldest, last, lambda p: update_block(p, a, nb))

            @pl.when(k > 0)
            def _():
                with jax.named_scope("old_diag"):
                    loop(oldest, last, old_diag)
                with jax.named_scope("take"):
                    loop(first_a(k), jnp.minimum(last_near(last) + 1, row_blocks), take)
                with jax.named_scope("take_column"):
                    column_arrived(last, nb)
                    edge_arrived(last, nb)
                with jax.named_scope("catch_up"):
                    update_near(last, nb)
                    loop(first_a(k + 1), jnp.minimum(first_a(k + 1) + 1, row_blocks), lambda a: update_block(last, a, nb))

            prepare(nb)
            slot = col_of(k, nb)
            with jax.named_scope("first_block"):
                arrived(slot)

            @pl.when(leads)
            def _():
                first_down(k, start)

            other = panel[slot]
            work[0:size, :] = diag[nb] - times_t(other, other)

        @pl.when(jnp.logical_and(k >= n_col // 2, col == lax.rem(k + n_col // 2, n_col)))
        def _():
            with jax.named_scope("sends_done"):
                firsts_done(k - n_col // 2)
                loop(first_a(k - n_col // 2), row_blocks, lambda a: source_sends(k - n_col // 2, a, finish))

    loop(0, steps + n_col // 2, step)

    def edges_done(b):
        @pl.when(jnp.logical_and(holds_edge(b), jnp.logical_not(leads)))
        def _():
            edge_copy(b).wait_send()

    loop(0, col_blocks, edges_done)
    with jax.named_scope("stored"):
        pltpu.make_async_copy(share, share, store_sem).wait()


def solution(mesh):
    n_row = mesh.shape["row"]
    n_col = mesh.shape["col"]

    def factor_local(a_loc):
        row_blocks, size, local_cols = a_loc.shape
        col_blocks = local_cols // size
        slots = n_row * (row_blocks * (row_blocks + 1) // 2) + n_col * (col_blocks * (col_blocks + 1) // 2)
        slots += 2 * row_blocks * n_row
        return pl.pallas_call(
            functools.partial(kernel, n_row, n_col, "batch"),
            out_shape=jax.ShapeDtypeStruct(a_loc.shape, F32),
            in_specs=[pl.BlockSpec(memory_space=pl.ANY)],
            out_specs=pl.BlockSpec(memory_space=pl.ANY),
            scratch_shapes=[
                pltpu.VMEM((row_blocks * col_blocks, size, size), F32),
                pltpu.VMEM((col_blocks, size, size), F32),
                pltpu.VMEM((col_blocks, size, size), F32),
                pltpu.VMEM((col_blocks, size, size), F32),
                pltpu.VMEM((size, size), BF16),
                pltpu.VMEM((slots, size, size), BF16),
                pltpu.VMEM((size + BASE, size), F32),
                pltpu.VMEM((size + BASE, size), F32),
                pltpu.VMEM((3, size, size), BF16),
                pltpu.VMEM((BASE, 3 * LANE), F32),
                pltpu.VMEM((4 * SUB, SUB, LANE), F32),
                pltpu.SemaphoreType.DMA,
                pltpu.SemaphoreType.DMA,
                pltpu.SemaphoreType.DMA((col_blocks, n_row)),
                pltpu.SemaphoreType.DMA((col_blocks,)),
                pltpu.SemaphoreType.DMA((col_blocks,)),
                pltpu.SemaphoreType.DMA((col_blocks,)),
                pltpu.SemaphoreType.DMA((2, n_row)),
                pltpu.SemaphoreType.DMA((row_blocks, 9)),
                pltpu.SemaphoreType.DMA((4, row_blocks, 6)),
                pltpu.SemaphoreType.DMA((slots,)),
            ],
            compiler_params=pltpu.CompilerParams(
                collective_id=0, has_side_effects=True, vmem_limit_bytes=60 * 1024 * 1024
            ),
            name="cholesky",
        )(a_loc)

    blk_spec = P(("batch", "row"), None, "col")
    return jax.shard_map(factor_local, mesh=mesh, in_specs=(blk_spec,), out_specs=blk_spec, check_vma=False)
```

```python
import functools

import jax
import jax.numpy as jnp
from jax import lax
from jax.experimental import pallas as pl
from jax.experimental.pallas import tpu as pltpu
from jax.sharding import PartitionSpec as P

F32 = jnp.float32
BF16 = jnp.bfloat16
MESH = pl.DeviceIdType.MESH
SUB = 8
LANE = 128
BASE = 16
LEAD = 1
SETTLE = 3
LAG = 5


def sub_bcast(x, q):
    return jnp.broadcast_to(x[q : q + 1, :], (SUB, LANE))


ALONG_LANES = lax.GatherDimensionNumbers(
    offset_dims=(), collapsed_slice_dims=(1,), start_index_map=(1,), operand_batching_dims=(0,), start_indices_batching_dims=(0,)
)


def lane_bcast(x, lane):
    index = jnp.full((SUB, LANE, 1), lane, jnp.int32)
    return lax.gather(x, index, ALONG_LANES, (1, 1), mode=lax.GatherScatterMode.PROMISE_IN_BOUNDS)


def split3(x):
    high = x.astype(BF16)
    rest = x - high.astype(F32)
    mid = rest.astype(BF16)
    return high, mid, (rest - mid.astype(F32)).astype(BF16)


def swap_rows(x, bit, row_id):
    if bit == SUB // 2:
        return pltpu.roll(x, bit, 0)
    return jnp.where((row_id & bit) == 0, pltpu.roll(x, SUB - bit, 0), pltpu.roll(x, bit, 0))


def stack_sums(parts):
    row_id = lax.broadcasted_iota(jnp.int32, (SUB, LANE), 0)
    for bit in (4, 2, 1):
        low = (row_id & bit) == 0
        half = len(parts) // 2
        parts = [
            jnp.where(low, parts[n], parts[n + half]) + swap_rows(jnp.where(low, parts[n + half], parts[n]), bit, row_id)
            for n in range(half)
        ]
    return parts[0]


def eliminate(rows, lane0):
    row_id = lax.broadcasted_iota(jnp.int32, (SUB, LANE), 0)
    rows = [list(rows[0]), list(rows[1])]
    cols = [
        [lane_bcast(rows[0][0], lane0 + j) for j in range(SUB)],
        [lane_bcast(rows[1][0], lane0 + j) for j in range(BASE)],
    ]
    scale = [jnp.zeros((SUB, LANE), F32), jnp.zeros((SUB, LANE), F32)]
    pivot = sub_bcast(cols[0][0], 0)
    for j in range(BASE):
        t, q = divmod(j, SUB)
        inv = lax.rsqrt(pivot)
        scale[t] = jnp.where(row_id == q, inv, scale[t])
        if j + 1 < BASE:
            tn, qn = divmod(j + 1, SUB)
            near = sub_bcast(cols[tn][j], qn) * inv
            pivot = sub_bcast(cols[tn][j + 1], qn) - near * near
        below = cols[1][j] * inv
        here = cols[0][j] * inv if t == 0 else None
        for n in range(j + 1, BASE):
            tn, qn = divmod(n, SUB)
            other = near if n == j + 1 else sub_bcast(here if tn == 0 else below, qn)
            if t == 0 and tn == 0:
                cols[0][n] = cols[0][n] - here * other
            cols[1][n] = cols[1][n] - below * other
        masked = jnp.where(row_id > q, here if t == 0 else below, 0.0)
        for v in range(len(rows[0])):
            pivot_row = sub_bcast(rows[t][v], q) * inv
            rows[t][v] = rows[t][v] - masked * pivot_row
            if t == 0:
                rows[1][v] = rows[1][v] - below * pivot_row
    return [[x * scale[t] for x in rows[t]] for t in range(2)]


def factor_block(work, winv, winv3, prev, fac):
    size = work.shape[1]
    prev[...] = jnp.zeros(prev.shape, F32)
    fac[...] = jnp.zeros(fac.shape, F32)

    def group(v):
        return slice(LANE * v, LANE * (v + 1))

    def pending(factors, before, t, v):
        above, below = before[:SUB, group(v)], before[SUB:, group(v)]
        at = 2 * SUB * t
        return stack_sums([factors[at + n] * above + factors[at + SUB + n] * below for n in range(SUB)])

    for half in range(size // LANE):
        views = [(work, 0), (work, 1), (winv, 0)] if half == 0 else [(work, 1), (winv, 0), (winv, 1)]
        first = half * LANE
        if half == 1:
            factors, before = fac[...], prev[...]
            work[first : first + BASE, group(1)] -= jnp.concatenate([pending(factors, before, t, 1) for t in range(2)], axis=0)
            prev[...] = jnp.concatenate([before[:, group(1)], before[:, group(2)], jnp.zeros((BASE, LANE), F32)], axis=1)

        def body(s, carry, views=views, first=first):
            lane0 = s * BASE
            row0 = pl.multiple_of(first + lane0, BASE)

            here = pl.ds(row0, BASE)
            then = pl.ds(pl.multiple_of(row0 + BASE, BASE), BASE)
            both = [ref[here, group(g)] for ref, g in views]
            rows = [[x[SUB * t : SUB * (t + 1)] for x in both] for t in range(2)]
            factors, before = fac[...], prev[...]
            for t in range(2):
                for v in (1, 2):
                    rows[t][v] = rows[t][v] - pending(factors, before, t, v)
            hi, mid, lo = split3(before)
            lane = lax.broadcasted_iota(jnp.int32, (BASE, size - first), 1) + first
            after = lane >= row0 + BASE
            lhi, lmid, llo = [jnp.where(after, x[:, : size - first], jnp.zeros((), BF16)) for x in (hi, mid, lo)]
            update = lax.dot_general(
                jnp.concatenate([lhi, lhi, lmid, lhi, llo, lmid], axis=0),
                jnp.concatenate([hi, mid, hi, lo, hi, mid], axis=0),
                (((0,), (0,)), ((), ())),
                preferred_element_type=F32,
            )
            for v, (ref, g) in enumerate(views):
                ref[first:size, group(g)] -= update[:, group(v)]
            done = eliminate(rows, lane0)
            if first == 0:
                source = [jnp.where(s == LANE // BASE - 1, done[t][1], done[t][0]) for t in range(2)]
            else:
                source = [done[t][0] for t in range(2)]
            next_lane = (lane0 + BASE) % LANE
            factors, sums = [], []
            for t in range(2):
                factor = [[lane_bcast(source[m], next_lane + SUB * t + n) for n in range(SUB)] for m in range(2)]
                sums.append(stack_sums([factor[0][n] * done[0][0] + factor[1][n] * done[1][0] for n in range(SUB)]))
                factors += factor[0] + factor[1]
            ref, g = views[0]
            ref[then, group(g)] -= jnp.concatenate(sums, axis=0)
            fac[...] = jnp.stack(factors)
            whole = [jnp.concatenate([done[0][v], done[1][v]], axis=0) for v in range(3)]
            prev[...] = jnp.concatenate(whole, axis=1)
            for (ref, g), x in zip(views, whole):
                ref[here, group(g)] = x
                if ref is winv:
                    for n, part in enumerate(split3(x)):
                        winv3[n, here, group(g)] = part
            return carry

        lax.fori_loop(0, LANE // BASE, body, 0)


def kernel(n_row, n_col, batch_axis, a_ref, o_ref, share, diag, edge, stage, first, panel, work, winv, winv3, prev, fac, load_sem, store_sem,
           seed_send, seed_recv, edge_send, edge_recv, first_sem, send_sem, pass_sem, recv_sem):
    row_blocks, size, local_cols = a_ref.shape
    col_blocks = local_cols // size
    ratio = n_col // n_row
    steps = row_blocks * n_row
    depth = pass_sem.shape[0]
    batch = lax.axis_index(batch_axis)
    row = lax.axis_index("row")
    col = lax.axis_index("col")
    odd = lax.rem(col, 2)
    on_diag = lax.rem(col, n_row) == row
    row_slots = n_row * (row_blocks * (row_blocks + 1) // 2)
    edge_slots = row_slots + n_col * (col_blocks * (col_blocks + 1) // 2)
    leads = row == LEAD

    def at(dev_row, dev_col):
        return (batch, dev_row, dev_col)

    def row_slot(k, a):
        g = k // n_row
        return n_row * (row_blocks * g - (g * (g - 1)) // 2) + (k - g * n_row) * (row_blocks - g) + a - g

    def col_slot(k, b):
        h = k // n_col
        return row_slots + n_col * (col_blocks * h - (h * (h - 1)) // 2) + (k - h * n_col) * (col_blocks - h) + b - h

    def first_a(k):
        return (k + n_row - row) // n_row

    def first_b(k):
        return (k + n_col - col) // n_col

    def home(ref, a, b):
        return ref.at[a, :, pl.ds(pl.multiple_of(b * size, size), size)]

    def spot(a, b):
        return b * row_blocks + a

    def col_of(k, b):
        return jnp.where(on_diag, row_slot(k, ratio * b + col // n_row), col_slot(k, b))

    def edge_slot(k, j):
        return edge_slots + 2 * k + (j - k - 1) // n_col

    def edge_reach(ahead):
        return jnp.logical_and(ahead >= 2, jnp.logical_and(ahead <= n_col + LAG - SETTLE, row != LEAD))

    def copy(src_slot, dst_slot, sem, device):
        return pltpu.make_async_remote_copy(
            src_ref=panel.at[src_slot], dst_ref=panel.at[dst_slot], send_sem=sem, recv_sem=recv_sem.at[dst_slot],
            device_id=device, device_id_type=MESH,
        )

    def arrived(slot):
        copy(slot, slot, send_sem.at[0, 0], at(row, col)).wait_recv()

    def start(c):
        c.start()

    def finish(c):
        c.wait_send()

    def from_maker(ahead, way):
        there = lax.rem(row + way, n_row)
        lead_near = jnp.logical_and(there == LEAD, jnp.logical_and(ahead >= 2, ahead <= n_row))
        soon_needed = jnp.logical_and(ahead == 2, way == 2)
        return jnp.logical_or(lead_near, soon_needed)

    def down_column(k, a, maker, sems, act):
        i = a * n_row + row
        slot = row_slot(k, a)
        dst = col_slot(k, i // n_col)
        for m, way in enumerate((1, n_row - 1, 2)):
            direct = from_maker(i - k, way)

            @pl.when(direct if maker else jnp.logical_not(direct))
            def _():
                act(copy(slot, dst, sems[m], at(lax.rem(row + way, n_row), lax.rem(i, n_col))))

    def last_near(p):
        return first_a(p + 3)

    def to_edge(k, a, sem, act):
        i = a * n_row + row
        act(copy(row_slot(k, a), edge_slot(k, i - 1), sem, at(LEAD, lax.rem(i - 1, n_col))))

    def source_sends(k, a, act):
        ahead = a * n_row + row - k
        slot = row_slot(k, a)
        early = n_row

        @pl.when(jnp.logical_and(edge_reach(ahead), jnp.logical_or(ahead <= early, ahead == n_col)))
        def _():
            to_edge(k, a, send_sem.at[a, 5], act)

        @pl.when(jnp.logical_and(ahead >= 2, ahead <= early))
        def _():
            down_column(k, a, True, [send_sem.at[a, m] for m in range(3)], act)

        @pl.when(lax.rem(ahead, n_col) == 0)
        def _():
            down_column(k, a, False, [send_sem.at[a, m] for m in range(3)], act)

        @pl.when(jnp.logical_or(jnp.logical_and(odd == 0, ahead >= 2), ahead >= n_col - 1))
        def _():
            act(copy(slot, slot, send_sem.at[a, 3], at(row, lax.rem(jnp.where(odd == 0, col + 1, col - 1), n_col))))

        @pl.when(ahead >= 2)
        def _():
            act(copy(slot, slot, send_sem.at[a, 6], at(row, lax.rem(col - odd + 2, n_col))))

        @pl.when(jnp.logical_and(ahead >= 3 - odd, a <= last_near(k)))
        def _():
            act(copy(slot, slot, send_sem.at[a, 4], at(row, lax.rem(col - odd + 3, n_col))))

        @pl.when(jnp.logical_and(ahead >= n_col // 2 - odd, ahead < n_col - 2 - odd))
        def _():
            act(copy(slot, slot, send_sem.at[a, 7], at(row, lax.rem(col - odd + 5, n_col))))

        @pl.when(ahead >= n_col - 2 - odd)
        def _():
            act(copy(slot, slot, send_sem.at[a, 8], at(row, lax.rem(col - odd - 2 + n_col, n_col))))

    def lead(p):
        return lax.rem(col - lax.rem(p, n_col) + n_col, n_col)

    def hops(p):
        return lax.rem(col // 2 - lax.rem(p, n_col) // 2 + n_col // 2, n_col // 2)

    def passes(p):
        return jnp.where(odd == 1, 2, n_col // 2 - 1) == hops(p)

    def first_passed(p):
        low = jnp.where(jnp.logical_and(passes(p), odd == 1), lead(p) - 1, lead(p))
        return (p + low - row + n_row - 1) // n_row

    def pass_down(p, a, act):
        i = a * n_row + row
        ahead = i - p
        sems = pass_sem.at[lax.rem(p, depth), a]

        @pl.when(jnp.logical_and(odd == 0, jnp.logical_and(lead(p) <= 2, a > last_near(p))))
        def _():
            act(copy(row_slot(p, a), row_slot(p, a), sems.at[3], at(row, col + 1)))

        @pl.when(jnp.logical_and(lax.rem(i, n_col) == col, ahead > 1))
        def _():
            @pl.when(jnp.logical_and(ahead > n_row, edge_reach(ahead)))
            def _():
                to_edge(p, a, sems.at[5], act)

            down_column(p, a, False, [sems.at[m] for m in range(3)], act)

    def pass_on(p, a, act):
        slot = row_slot(p, a)
        sems = pass_sem.at[lax.rem(p, depth), a]

        @pl.when(passes(p))
        def _():
            @pl.when(odd == 0)
            def _():
                act(copy(slot, slot, sems.at[4], at(row, lax.rem(col - 1 + n_col, n_col))))

            @pl.when(jnp.logical_or(odd == 1, a * n_row + row > p + lead(p)))
            def _():
                act(copy(slot, slot, sems.at[3], at(row, col + 1 - 2 * odd)))

        pass_down(p, a, act)

    def passed(p):
        @pl.when(lead(p) != 0)
        def _():
            loop(first_passed(p), row_blocks, lambda a: pass_on(p, a, finish))

    def receive(p, a):
        arrived(row_slot(p, a))
        pass_down(p, a, start)

    def receive_any(p, a):
        arrived(row_slot(p, a))
        pass_on(p, a, start)

    def loop(lo, hi, fn):
        lax.fori_loop(lo, hi, lambda n, c: (fn(n), c)[1], 0)

    for a in range(row_blocks):
        for b in range(col_blocks):
            pltpu.make_async_copy(home(a_ref, a, b), share.at[spot(a, b)], load_sem).start()

    barrier = pltpu.get_barrier_semaphore()
    n_dev = n_row * n_col

    def greet(n):
        other = lax.rem(row * n_col + col + n, n_dev)
        pl.semaphore_signal(barrier, inc=1, device_id=at(other // n_col, lax.rem(other, n_col)), device_id_type=MESH)

    loop(1, n_dev, greet)
    with jax.named_scope("all_here"):
        pl.semaphore_wait(barrier, n_dev - 1)
    with jax.named_scope("loaded"):
        pltpu.make_async_copy(share, share, load_sem).wait()

    def seed_copy(b, dev_row):
        return pltpu.make_async_remote_copy(
            src_ref=share.at[spot(ratio * b + col // n_row, b)], dst_ref=diag.at[b],
            send_sem=seed_send.at[b, lax.rem(dev_row - row + n_row, n_row)],
            recv_sem=seed_recv.at[b], device_id=at(dev_row, col), device_id_type=MESH,
        )

    def hand_out(b):
        @pl.when(on_diag)
        def _():
            for d in (1, n_row - 1, 2):
                seed_copy(b, lax.rem(row + d, n_row)).start()
            diag[b] = share[spot(ratio * b + col // n_row, b)]

        @pl.when(jnp.logical_and(holds_edge(b), jnp.logical_not(leads)))
        def _():
            stage[b] = share[spot((b * n_col + col + 1) // n_row, b)]
            edge_copy(b).start()

    def holds_edge(b):
        j = b * n_col + col
        return jnp.logical_and(lax.rem(j + 1, n_row) == row, j + 1 < steps)

    def edge_copy(b):
        return pltpu.make_async_remote_copy(
            src_ref=stage.at[b], dst_ref=edge.at[b], send_sem=edge_send.at[b], recv_sem=edge_recv.at[b],
            device_id=at(LEAD, col), device_id_type=MESH,
        )

    def has_edge(b):
        from_other = jnp.logical_and(leads, lax.rem(col + 1, n_row) != LEAD)
        return jnp.logical_and(from_other, b * n_col + col + 1 < steps)

    def edge_seeded(b):
        @pl.when(has_edge(b))
        def _():
            edge_copy(b).wait_recv()

    def edge_arrived(p, b):
        j = b * n_col + col

        @pl.when(jnp.logical_and(has_edge(b), j + 1 - p <= n_col + LAG - SETTLE))
        def _():
            arrived(edge_slot(p, j))

    hand_out(0)
    winv3[...] = jnp.zeros(winv3.shape, BF16)

    def seed_arrived(b):
        @pl.when(jnp.logical_not(on_diag))
        def _():
            seed_copy(b, row).wait_recv()

    with jax.named_scope("seed"):
        seed_arrived(0)

        @pl.when(col != 0)
        def _():
            edge_seeded(0)

    def clear(n):
        a, b = lax.rem(n, row_blocks), n // row_blocks

        @pl.when(a * n_row + row < b * n_col + col)
        def _():
            share[n] = jnp.zeros((size, size), F32)
            pltpu.make_async_copy(share.at[n], home(o_ref, a, b), store_sem).start()

    loop(0, row_blocks * col_blocks, clear)

    def times_t(x, y):
        return lax.dot_general(x, y, (((1,), (1,)), ((), ())), preferred_element_type=F32)

    def update_block(p, a, b):
        share[spot(a, b)] -= times_t(panel[row_slot(p, a)], panel[col_of(p, b)])

    def update_diag(p, b):
        other = panel[col_of(p, b)]
        diag[b] -= times_t(other, other)

    def update_edge(p, b):
        @pl.when(has_edge(b))
        def _():
            edge[b] -= times_t(panel[edge_slot(p, b * n_col + col)], panel[col_of(p, b)])

    def column_arrived(p, b):
        @pl.when(jnp.logical_not(on_diag))
        def _():
            arrived(col_slot(p, b))

    def update_column(p, b, lo):
        lone = lax.rem(row_blocks - lo, 2)

        @pl.when(lone == 1)
        def _():
            update_block(p, lo, b)

        def pair(m):
            a = lo + lone + 2 * m
            both = pl.ds(spot(a, b), 2)
            left = panel[pl.ds(row_slot(p, a), 2)].reshape(2 * size, size)
            share[both] -= times_t(left, panel[col_of(p, b)]).reshape(2, size, size)

        loop(0, (row_blocks - lo) // 2, pair)

    def trail(p, b_from, near):
        loop(b_from, col_blocks, lambda b: update_column(p, b, first_a(b * n_col + col - jnp.where(b == near, 0, 1))))

    def columns_arrived(p, b_from):
        def one(b):
            column_arrived(p, b)
            edge_arrived(p, b)

        loop(b_from, col_blocks, one)

    def prepare(b):
        work[size:, :] = jnp.zeros((BASE, size), F32)
        r_id = lax.broadcasted_iota(jnp.int32, (size + BASE, size), 0)
        c_id = lax.broadcasted_iota(jnp.int32, (size + BASE, size), 1)
        winv[...] = jnp.where(r_id == c_id, 1.0, 0.0).astype(F32)

    def times_winv_t(x):
        hi, mid, lo = split3(x)
        whi, wmid, wlo = winv3[0], winv3[1], winv3[2]
        small = times_t(lo, whi) + times_t(mid, wmid) + times_t(hi, wlo)
        return small + (times_t(mid, whi) + times_t(hi, wmid)) + times_t(hi, whi)

    def solve(k, a, count, near):
        kb = k // n_col
        here = pl.ds(spot(a, kb), count)

        def apply(p):
            left = panel[pl.ds(row_slot(p, a), count)].reshape(count * size, size)
            share[here] -= times_t(left, panel[col_of(p, kb)]).reshape(count, size, size)

        if not near:

            for m in range(count):

                @pl.when(k >= 3)
                def _():
                    receive(k - 3, a + m)

                @pl.when(jnp.logical_and(k >= 2, a + m > last_near(k - 2)))
                def _():
                    receive(k - 2, a + m)

            loop(jnp.maximum(k - 2 - LAG, 0), k - 1, apply)

        @pl.when(k > 0)
        def _():
            for m in range(count):
                receive(k - 1, a + m)
            apply(k - 1)

        x = times_winv_t(share[here].reshape(count * size, size)).reshape(count, size, size)
        panel[pl.ds(row_slot(k, a), count)] = x.astype(BF16)
        share[here] = x
        if near:

            @pl.when(jnp.logical_and(leads, lax.rem(k + 1, n_row) == LEAD))
            def _():
                first[...] = panel[row_slot(k, a)]
                first_out(k, start)

        if count == 1:
            source_sends(k, a, start)
        else:
            loop(a, a + count, lambda n: source_sends(k, n, start))
        for m in range(count):
            pltpu.make_async_copy(share.at[spot(a + m, kb)], home(o_ref, a + m, kb), store_sem).start()

    def update_near(p, b):
        update_diag(p, b)
        update_edge(p, b)

    def first_slot(k, dev_row):
        return jnp.where(lax.rem(k + 1, n_row) == dev_row, row_slot(k, (k + 1) // n_row), col_slot(k, (k + 1) // n_col))

    def first_copy(k, dev_row, sem):
        dst = first_slot(k, dev_row)
        return pltpu.make_async_remote_copy(
            src_ref=first, dst_ref=panel.at[dst], send_sem=sem, recv_sem=recv_sem.at[dst],
            device_id=at(dev_row, lax.rem(col + 1, n_col)), device_id_type=MESH,
        )

    def others_first(k, fn):
        urgent = lax.rem(k + 3, n_row)
        lone = urgent == LEAD
        for m in range(n_row - 1):
            fn(m, lax.rem(jnp.where(lone, LEAD + 1, urgent) + m + jnp.where(lax.rem(jnp.where(lone, LEAD + 1, urgent) - LEAD + n_row, n_row) + m >= n_row, 1, 0), n_row))

    def first_out(k, act):
        act(first_copy(k, LEAD, first_sem.at[0, 0]))

        @pl.when(odd == 0)
        def _():
            others_first(k, lambda m, r: act(first_copy(k, r, first_sem.at[0, 1 + m])))

    def first_down(k, act):
        @pl.when(odd == 0)
        def _():
            others_first(k, lambda m, r: act(copy(first_slot(k, LEAD), first_slot(k, r), first_sem.at[1, 1 + m], at(r, col))))

    def firsts_done(k):
        @pl.when(jnp.logical_and(leads, k + 1 < steps))
        def _():
            first_out(k, finish)

        @pl.when(jnp.logical_and(leads, k > 0))
        def _():
            first_down(k - 1, finish)

    @pl.when(col == 0)
    def _():
        prepare(0)
        work[0:size, :] = diag[0]

    def step(k):
        mine = jnp.logical_and(col == lax.rem(k, n_col), k < steps)
        kb = k // n_col
        last = k - 1
        soon = jnp.logical_and(col == lax.rem(k + 1, n_col), k + 1 < steps)

        @pl.when(mine)
        def _():
            with jax.named_scope("factor"):
                factor_block(work, winv, winv3, prev, fac)

            @pl.when(has_edge(kb))
            def _():
                with jax.named_scope("lead"):

                    @pl.when(k == 0)
                    def _():
                        edge_seeded(kb)

                    @pl.when(k > 0)
                    def _():
                        edge_arrived(last, kb)
                        update_edge(last, kb)

                    first[...] = times_winv_t(edge[kb]).astype(BF16)
                    first_out(k, start)

            lo = first_a(k)
            second = jnp.minimum(lo + 1, row_blocks)
            with jax.named_scope("solve_near"):
                loop(lo, second, lambda a: solve(k, a, 1, True))
            with jax.named_scope("solve_one"):
                third = second + lax.rem(row_blocks - second, 2)
                loop(second, third, lambda a: solve(k, a, 1, False))
            with jax.named_scope("solve_two"):
                loop(0, (row_blocks - third) // 2, lambda m: solve(k, third + 2 * m, 2, False))

        @pl.when(k >= depth)
        def _():
            with jax.named_scope("passed"):
                passed(k - depth)

        @pl.when(mine)
        def _():
            @pl.when(row == lax.rem(k, n_row))
            def _():
                for d in range(1, n_row):
                    seed_copy(kb, lax.rem(row + d, n_row)).wait_send()
                r_id = lax.broadcasted_iota(jnp.int32, (size, size), 0)
                c_id = lax.broadcasted_iota(jnp.int32, (size, size), 1)
                n = spot(k // n_row, kb)
                share[n] = jnp.where(r_id >= c_id, work[0:size, :].T, 0.0)
                pltpu.make_async_copy(share.at[n], home(o_ref, k // n_row, kb), store_sem).start()

        @pl.when(jnp.logical_and(k > 0, jnp.logical_not(jnp.logical_or(mine, soon))))
        def _():
            @pl.when(col != lax.rem(last, n_col))
            def _():
                with jax.named_scope("receive"):
                    end = jnp.where(lead(last) == 3, jnp.minimum(last_near(last) + 1, row_blocks), row_blocks)
                    loop(first_passed(last), end, lambda a: receive_any(last, a))

            near = first_b(k)
            age = k + n_col - (near * n_col + col)
            settle = jnp.logical_and(age == SETTLE, jnp.logical_and(near > 0, near < col_blocks))

            @pl.when(settle)
            def _():
                with jax.named_scope("late_trail"):
                    own = k - SETTLE

                    def late(p):
                        columns_arrived(p, near)
                        trail(p, near, -1)

                    loop(jnp.maximum(own - 2 - LAG, 0), own - LAG + 1, late)

            @pl.when(jnp.logical_and(k >= LAG, lead(last) != 3))
            def _():
                p = k - LAG
                with jax.named_scope("columns"):
                    columns_arrived(p, near)

                @pl.when(jnp.logical_and(near < col_blocks, age >= SETTLE + 2))
                def _():
                    @pl.when(jnp.logical_and(age == SETTLE + 2, near > 0))
                    def _():
                        with jax.named_scope("seed_late"):
                            seed_arrived(near)
                            edge_seeded(near)

                    oldest = jnp.where(age == SETTLE + 2, jnp.maximum(p - 1, 0), p)
                    loop(oldest, p + 1, lambda q: update_near(q, near))

                with jax.named_scope("trail"):
                    trail(p, near, jnp.where(jnp.logical_or(age > SETTLE, near == 0), near, -1))

            @pl.when(settle)
            def _():
                hand_out(near)

        @pl.when(soon)
        def _():
            nb = (k + 1) // n_col

            oldest = jnp.maximum(k - 1 - LAG, 0)
            lo = first_a(k + 1)

            def old_diag(p):
                column_arrived(p, nb)
                edge_arrived(p, nb)
                update_near(p, nb)

            def take(a):
                receive(last, a)

                @pl.when(jnp.logical_and(a * n_row + row > k + 1, a <= lo))
                def _():
                    loop(oldest, last, lambda p: update_block(p, a, nb))

            @pl.when(k > 0)
            def _():
                with jax.named_scope("old_diag"):
                    loop(oldest, last, old_diag)
                with jax.named_scope("take"):
                    loop(first_a(k), jnp.minimum(last_near(last) + 1, row_blocks), take)
                with jax.named_scope("take_column"):
                    column_arrived(last, nb)
                    edge_arrived(last, nb)
                with jax.named_scope("catch_up"):
                    update_near(last, nb)
                    loop(first_a(k + 1), jnp.minimum(first_a(k + 1) + 1, row_blocks), lambda a: update_block(last, a, nb))

            prepare(nb)
            slot = col_of(k, nb)
            with jax.named_scope("first_block"):
                arrived(slot)

            @pl.when(leads)
            def _():
                first_down(k, start)

            other = panel[slot]
            work[0:size, :] = diag[nb] - times_t(other, other)

        @pl.when(jnp.logical_and(k >= n_col // 2, col == lax.rem(k + n_col // 2, n_col)))
        def _():
            with jax.named_scope("sends_done"):
                firsts_done(k - n_col // 2)
                loop(first_a(k - n_col // 2), row_blocks, lambda a: source_sends(k - n_col // 2, a, finish))

    loop(0, steps + n_col // 2, step)

    def edges_done(b):
        @pl.when(jnp.logical_and(holds_edge(b), jnp.logical_not(leads)))
        def _():
            edge_copy(b).wait_send()

    loop(0, col_blocks, edges_done)
    with jax.named_scope("stored"):
        pltpu.make_async_copy(share, share, store_sem).wait()


def solution(mesh):
    n_row = mesh.shape["row"]
    n_col = mesh.shape["col"]

    def factor_local(a_loc):
        row_blocks, size, local_cols = a_loc.shape
        col_blocks = local_cols // size
        slots = n_row * (row_blocks * (row_blocks + 1) // 2) + n_col * (col_blocks * (col_blocks + 1) // 2)
        slots += 2 * row_blocks * n_row
        return pl.pallas_call(
            functools.partial(kernel, n_row, n_col, "batch"),
            out_shape=jax.ShapeDtypeStruct(a_loc.shape, F32),
            in_specs=[pl.BlockSpec(memory_space=pl.ANY)],
            out_specs=pl.BlockSpec(memory_space=pl.ANY),
            scratch_shapes=[
                pltpu.VMEM((row_blocks * col_blocks, size, size), F32),
                pltpu.VMEM((col_blocks, size, size), F32),
                pltpu.VMEM((col_blocks, size, size), F32),
                pltpu.VMEM((col_blocks, size, size), F32),
                pltpu.VMEM((size, size), BF16),
                pltpu.VMEM((slots, size, size), BF16),
                pltpu.VMEM((size + BASE, size), F32),
                pltpu.VMEM((size + BASE, size), F32),
                pltpu.VMEM((3, size, size), BF16),
                pltpu.VMEM((BASE, 3 * LANE), F32),
                pltpu.VMEM((4 * SUB, SUB, LANE), F32),
                pltpu.SemaphoreType.DMA,
                pltpu.SemaphoreType.DMA,
                pltpu.SemaphoreType.DMA((col_blocks, n_row)),
                pltpu.SemaphoreType.DMA((col_blocks,)),
                pltpu.SemaphoreType.DMA((col_blocks,)),
                pltpu.SemaphoreType.DMA((col_blocks,)),
                pltpu.SemaphoreType.DMA((2, n_row)),
                pltpu.SemaphoreType.DMA((row_blocks, 9)),
                pltpu.SemaphoreType.DMA((4, row_blocks, 6)),
                pltpu.SemaphoreType.DMA((slots,)),
            ],
            compiler_params=pltpu.CompilerParams(
                collective_id=0, has_side_effects=True, vmem_limit_bytes=60 * 1024 * 1024
            ),
            name="cholesky",
        )(a_loc)

    blk_spec = P(("batch", "row"), None, "col")
    return jax.shard_map(factor_local, mesh=mesh, in_specs=(blk_spec,), out_specs=blk_spec, check_vma=False)
```

```python
import functools

import jax
import jax.numpy as jnp
from jax import lax
from jax.experimental import pallas as pl
from jax.experimental.pallas import tpu as pltpu
from jax.sharding import PartitionSpec as P

F32 = jnp.float32
BF16 = jnp.bfloat16
MESH = pl.DeviceIdType.MESH
SUB = 8
LANE = 128
BASE = 16
LEAD = 1
SETTLE = 3
RELAYED = 10
LAG = 3


def sub_bcast(x, q):
    return jnp.broadcast_to(x[q : q + 1, :], (SUB, LANE))


ALONG_LANES = lax.GatherDimensionNumbers(
    offset_dims=(), collapsed_slice_dims=(1,), start_index_map=(1,), operand_batching_dims=(0,), start_indices_batching_dims=(0,)
)


def lane_bcast(x, lane):
    index = jnp.full((SUB, LANE, 1), lane, jnp.int32)
    return lax.gather(x, index, ALONG_LANES, (1, 1), mode=lax.GatherScatterMode.PROMISE_IN_BOUNDS)


def split3(x):
    high = x.astype(BF16)
    rest = x - high.astype(F32)
    mid = rest.astype(BF16)
    return high, mid, (rest - mid.astype(F32)).astype(BF16)


def swap_rows(x, bit, row_id):
    if bit == SUB // 2:
        return pltpu.roll(x, bit, 0)
    return jnp.where((row_id & bit) == 0, pltpu.roll(x, SUB - bit, 0), pltpu.roll(x, bit, 0))


def stack_sums(parts):
    row_id = lax.broadcasted_iota(jnp.int32, (SUB, LANE), 0)
    for bit in (4, 2, 1):
        low = (row_id & bit) == 0
        half = len(parts) // 2
        parts = [
            jnp.where(low, parts[n], parts[n + half]) + swap_rows(jnp.where(low, parts[n + half], parts[n]), bit, row_id)
            for n in range(half)
        ]
    return parts[0]


def eliminate(rows, lane0):
    row_id = lax.broadcasted_iota(jnp.int32, (SUB, LANE), 0)
    rows = [list(rows[0]), list(rows[1])]
    cols = [
        [lane_bcast(rows[0][0], lane0 + j) for j in range(SUB)],
        [lane_bcast(rows[1][0], lane0 + j) for j in range(BASE)],
    ]
    scale = [jnp.zeros((SUB, LANE), F32), jnp.zeros((SUB, LANE), F32)]
    pivot = sub_bcast(cols[0][0], 0)
    for j in range(BASE):
        t, q = divmod(j, SUB)
        inv = lax.rsqrt(pivot)
        scale[t] = jnp.where(row_id == q, inv, scale[t])
        if j + 1 < BASE:
            tn, qn = divmod(j + 1, SUB)
            near = sub_bcast(cols[tn][j], qn) * inv
            pivot = sub_bcast(cols[tn][j + 1], qn) - near * near
        below = cols[1][j] * inv
        here = cols[0][j] * inv if t == 0 else None
        for n in range(j + 1, BASE):
            tn, qn = divmod(n, SUB)
            other = near if n == j + 1 else sub_bcast(here if tn == 0 else below, qn)
            if t == 0 and tn == 0:
                cols[0][n] = cols[0][n] - here * other
            cols[1][n] = cols[1][n] - below * other
        masked = jnp.where(row_id > q, here if t == 0 else below, 0.0)
        for v in range(len(rows[0])):
            pivot_row = sub_bcast(rows[t][v], q) * inv
            rows[t][v] = rows[t][v] - masked * pivot_row
            if t == 0:
                rows[1][v] = rows[1][v] - below * pivot_row
    return [[x * scale[t] for x in rows[t]] for t in range(2)]


def factor_block(work, winv, winv3, prev, fac):
    size = work.shape[1]
    prev[...] = jnp.zeros(prev.shape, F32)
    fac[...] = jnp.zeros(fac.shape, F32)

    def group(v):
        return slice(LANE * v, LANE * (v + 1))

    def pending(factors, before, t, v):
        above, below = before[:SUB, group(v)], before[SUB:, group(v)]
        at = 2 * SUB * t
        return stack_sums([factors[at + n] * above + factors[at + SUB + n] * below for n in range(SUB)])

    for half in range(size // LANE):
        views = [(work, 0), (work, 1), (winv, 0)] if half == 0 else [(work, 1), (winv, 0), (winv, 1)]
        first = half * LANE
        if half == 1:
            factors, before = fac[...], prev[...]
            work[first : first + BASE, group(1)] -= jnp.concatenate([pending(factors, before, t, 1) for t in range(2)], axis=0)
            prev[...] = jnp.concatenate([before[:, group(1)], before[:, group(2)], jnp.zeros((BASE, LANE), F32)], axis=1)

        def body(s, carry, views=views, first=first):
            lane0 = s * BASE
            row0 = pl.multiple_of(first + lane0, BASE)

            here = pl.ds(row0, BASE)
            then = pl.ds(pl.multiple_of(row0 + BASE, BASE), BASE)
            both = [ref[here, group(g)] for ref, g in views]
            rows = [[x[SUB * t : SUB * (t + 1)] for x in both] for t in range(2)]
            factors, before = fac[...], prev[...]
            for t in range(2):
                for v in (1, 2):
                    rows[t][v] = rows[t][v] - pending(factors, before, t, v)
            hi, mid, lo = split3(before)
            lane = lax.broadcasted_iota(jnp.int32, (BASE, size - first), 1) + first
            after = lane >= row0 + BASE
            lhi, lmid, llo = [jnp.where(after, x[:, : size - first], jnp.zeros((), BF16)) for x in (hi, mid, lo)]
            update = lax.dot_general(
                jnp.concatenate([lhi, lhi, lmid, lhi, llo, lmid], axis=0),
                jnp.concatenate([hi, mid, hi, lo, hi, mid], axis=0),
                (((0,), (0,)), ((), ())),
                preferred_element_type=F32,
            )
            for v, (ref, g) in enumerate(views):
                ref[first:size, group(g)] -= update[:, group(v)]
            done = eliminate(rows, lane0)
            if first == 0:
                source = [jnp.where(s == LANE // BASE - 1, done[t][1], done[t][0]) for t in range(2)]
            else:
                source = [done[t][0] for t in range(2)]
            next_lane = (lane0 + BASE) % LANE
            factors, sums = [], []
            for t in range(2):
                factor = [[lane_bcast(source[m], next_lane + SUB * t + n) for n in range(SUB)] for m in range(2)]
                sums.append(stack_sums([factor[0][n] * done[0][0] + factor[1][n] * done[1][0] for n in range(SUB)]))
                factors += factor[0] + factor[1]
            ref, g = views[0]
            ref[then, group(g)] -= jnp.concatenate(sums, axis=0)
            fac[...] = jnp.stack(factors)
            whole = [jnp.concatenate([done[0][v], done[1][v]], axis=0) for v in range(3)]
            prev[...] = jnp.concatenate(whole, axis=1)
            for (ref, g), x in zip(views, whole):
                ref[here, group(g)] = x
                if ref is winv:
                    for n, part in enumerate(split3(x)):
                        winv3[n, here, group(g)] = part
            return carry

        lax.fori_loop(0, LANE // BASE, body, 0)


def kernel(n_row, n_col, batch_axis, a_ref, o_ref, share, diag, edge, stage, first, panel, work, winv, winv3, prev, fac, load_sem, store_sem,
           seed_send, seed_recv, edge_send, edge_recv, first_sem, send_sem, pass_sem, relay_sem, recv_sem):
    row_blocks, size, local_cols = a_ref.shape
    col_blocks = local_cols // size
    ratio = n_col // n_row
    steps = row_blocks * n_row
    depth = pass_sem.shape[0]
    relay_depth = relay_sem.shape[0]
    batch = lax.axis_index(batch_axis)
    row = lax.axis_index("row")
    col = lax.axis_index("col")
    odd = lax.rem(col, 2)
    on_diag = lax.rem(col, n_row) == row
    row_slots = n_row * (row_blocks * (row_blocks + 1) // 2)
    edge_slots = row_slots + n_col * (col_blocks * (col_blocks + 1) // 2)
    leads = row == LEAD

    def at(dev_row, dev_col):
        return (batch, dev_row, dev_col)

    def row_slot(k, a):
        g = k // n_row
        return n_row * (row_blocks * g - (g * (g - 1)) // 2) + (k - g * n_row) * (row_blocks - g) + a - g

    def col_slot(k, b):
        h = k // n_col
        return row_slots + n_col * (col_blocks * h - (h * (h - 1)) // 2) + (k - h * n_col) * (col_blocks - h) + b - h

    def first_a(k):
        return (k + n_row - row) // n_row

    def first_b(k):
        return (k + n_col - col) // n_col

    def home(ref, a, b):
        return ref.at[a, :, pl.ds(pl.multiple_of(b * size, size), size)]

    def spot(a, b):
        return b * row_blocks + a

    def col_of(k, b):
        return jnp.where(on_diag, row_slot(k, ratio * b + col // n_row), col_slot(k, b))

    def edge_slot(k, j):
        return edge_slots + 2 * k + (j - k - 1) // n_col

    def edge_reach(ahead):
        return jnp.logical_and(ahead >= 2, jnp.logical_and(ahead <= n_col + LAG - SETTLE, row != LEAD))

    def copy(src_slot, dst_slot, sem, device):
        return pltpu.make_async_remote_copy(
            src_ref=panel.at[src_slot], dst_ref=panel.at[dst_slot], send_sem=sem, recv_sem=recv_sem.at[dst_slot],
            device_id=device, device_id_type=MESH,
        )

    def arrived(slot):
        copy(slot, slot, send_sem.at[0, 0], at(row, col)).wait_recv()

    def start(c):
        c.start()

    def finish(c):
        c.wait_send()

    def from_maker(ahead, way):
        there = lax.rem(row + way, n_row)
        lead_near = jnp.logical_and(there == LEAD, jnp.logical_and(ahead >= 2, ahead <= n_row))
        soon_needed = jnp.logical_and(ahead == 2, way == 2)
        return jnp.logical_or(lead_near, soon_needed)

    def down_column(k, a, maker, sems, act):
        i = a * n_row + row
        slot = row_slot(k, a)
        dst = col_slot(k, i // n_col)
        for m, way in enumerate((1, n_row - 1, 2)):
            direct = from_maker(i - k, way)
            relayed = jnp.logical_and(way == 2, i - k > n_col)

            @pl.when(jnp.where(maker, direct, jnp.logical_not(jnp.logical_or(direct, relayed))))
            def _():
                act(copy(slot, dst, sems[m], at(lax.rem(row + way, n_row), lax.rem(i, n_col))))

    def last_near(p):
        return first_a(p + 3)

    def to_edge(k, a, sem, act):
        i = a * n_row + row
        act(copy(row_slot(k, a), edge_slot(k, i - 1), sem, at(LEAD, lax.rem(i - 1, n_col))))

    def source_sends(k, a, act):
        ahead = a * n_row + row - k
        slot = row_slot(k, a)
        early = n_row

        @pl.when(jnp.logical_and(edge_reach(ahead), jnp.logical_or(ahead <= early, ahead == n_col)))
        def _():
            to_edge(k, a, send_sem.at[a, 5], act)

        near = jnp.logical_and(ahead >= 2, ahead <= early)

        @pl.when(jnp.logical_or(near, lax.rem(ahead, n_col) == 0))
        def _():
            down_column(k, a, near, [send_sem.at[a, m] for m in range(3)], act)

        @pl.when(jnp.logical_or(jnp.logical_and(odd == 0, ahead >= 2), ahead >= n_col - 1))
        def _():
            act(copy(slot, slot, send_sem.at[a, 3], at(row, lax.rem(jnp.where(odd == 0, col + 1, col - 1), n_col))))

        @pl.when(ahead >= 2)
        def _():
            act(copy(slot, slot, send_sem.at[a, 6], at(row, lax.rem(col - odd + 2, n_col))))

        @pl.when(jnp.logical_and(ahead >= 3 - odd, a <= last_near(k)))
        def _():
            act(copy(slot, slot, send_sem.at[a, 4], at(row, lax.rem(col - odd + 3, n_col))))

        @pl.when(jnp.logical_and(ahead >= n_col // 2 - odd, ahead < n_col - 2 - odd))
        def _():
            act(copy(slot, slot, send_sem.at[a, 7], at(row, lax.rem(col - odd + 5, n_col))))

        @pl.when(ahead >= n_col - 2 - odd)
        def _():
            act(copy(slot, slot, send_sem.at[a, 8], at(row, lax.rem(col - odd - 2 + n_col, n_col))))

    def lead(p):
        return lax.rem(col - lax.rem(p, n_col) + n_col, n_col)

    def hops(p):
        return lax.rem(col // 2 - lax.rem(p, n_col) // 2 + n_col // 2, n_col // 2)

    def passes(p):
        return jnp.where(odd == 1, 2, n_col // 2 - 1) == hops(p)

    def first_passed(p):
        low = jnp.where(jnp.logical_and(passes(p), odd == 1), lead(p) - 1, lead(p))
        return (p + low - row + n_row - 1) // n_row

    def pass_down(p, a, act):
        i = a * n_row + row
        ahead = i - p
        sems = pass_sem.at[lax.rem(p, depth), a]

        @pl.when(jnp.logical_and(odd == 0, jnp.logical_and(lead(p) <= 2, a > last_near(p))))
        def _():
            act(copy(row_slot(p, a), row_slot(p, a), sems.at[3], at(row, col + 1)))

        @pl.when(jnp.logical_and(lax.rem(i, n_col) == col, ahead > 1))
        def _():
            @pl.when(jnp.logical_and(ahead > n_row, edge_reach(ahead)))
            def _():
                to_edge(p, a, sems.at[5], act)

            down_column(p, a, False, [sems.at[m] for m in range(3)], act)

    def pass_on(p, a, act):
        slot = row_slot(p, a)
        sems = pass_sem.at[lax.rem(p, depth), a]

        @pl.when(passes(p))
        def _():
            @pl.when(odd == 0)
            def _():
                act(copy(slot, slot, sems.at[4], at(row, lax.rem(col - 1 + n_col, n_col))))

            @pl.when(jnp.logical_or(odd == 1, a * n_row + row > p + lead(p)))
            def _():
                act(copy(slot, slot, sems.at[3], at(row, col + 1 - 2 * odd)))

        pass_down(p, a, act)

    def column_relay(p, b, act):
        j = b * n_col + col
        away = lax.rem(row - lax.rem(j, n_row) + n_row, n_row)

        @pl.when(jnp.logical_and(j - p > n_col, away == jnp.where(lax.rem(b, 2) == 0, 1, n_row - 1)))
        def _():
            slot = col_slot(p, b)
            act(copy(slot, slot, relay_sem.at[lax.rem(p, relay_depth), b], at(lax.rem(row + away, n_row), col)))

    def passed(p):
        @pl.when(lead(p) != 0)
        def _():
            loop(first_passed(p), row_blocks, lambda a: pass_on(p, a, finish))

    def receive(p, a):
        arrived(row_slot(p, a))
        pass_down(p, a, start)

    def receive_any(p, a):
        arrived(row_slot(p, a))
        pass_on(p, a, start)

    def loop(lo, hi, fn):
        lax.fori_loop(lo, hi, lambda n, c: (fn(n), c)[1], 0)

    for a in range(row_blocks):
        for b in range(col_blocks):
            pltpu.make_async_copy(home(a_ref, a, b), share.at[spot(a, b)], load_sem).start()

    barrier = pltpu.get_barrier_semaphore()
    n_dev = n_row * n_col

    def greet(n):
        other = lax.rem(row * n_col + col + n, n_dev)
        pl.semaphore_signal(barrier, inc=1, device_id=at(other // n_col, lax.rem(other, n_col)), device_id_type=MESH)

    loop(1, n_dev, greet)
    with jax.named_scope("all_here"):
        pl.semaphore_wait(barrier, n_dev - 1)
    with jax.named_scope("loaded"):
        pltpu.make_async_copy(share, share, load_sem).wait()

    def seed_copy(b, dev_row):
        return pltpu.make_async_remote_copy(
            src_ref=share.at[spot(ratio * b + col // n_row, b)], dst_ref=diag.at[b],
            send_sem=seed_send.at[b, lax.rem(dev_row - row + n_row, n_row)],
            recv_sem=seed_recv.at[b], device_id=at(dev_row, col), device_id_type=MESH,
        )

    def hand_out(b):
        @pl.when(on_diag)
        def _():
            for d in (1, n_row - 1, 2):
                seed_copy(b, lax.rem(row + d, n_row)).start()
            diag[b] = share[spot(ratio * b + col // n_row, b)]

        @pl.when(jnp.logical_and(holds_edge(b), jnp.logical_not(leads)))
        def _():
            stage[b] = share[spot((b * n_col + col + 1) // n_row, b)]
            edge_copy(b).start()

    def holds_edge(b):
        j = b * n_col + col
        return jnp.logical_and(lax.rem(j + 1, n_row) == row, j + 1 < steps)

    def edge_copy(b):
        return pltpu.make_async_remote_copy(
            src_ref=stage.at[b], dst_ref=edge.at[b], send_sem=edge_send.at[b], recv_sem=edge_recv.at[b],
            device_id=at(LEAD, col), device_id_type=MESH,
        )

    def has_edge(b):
        from_other = jnp.logical_and(leads, lax.rem(col + 1, n_row) != LEAD)
        return jnp.logical_and(from_other, b * n_col + col + 1 < steps)

    def edge_seeded(b):
        @pl.when(has_edge(b))
        def _():
            edge_copy(b).wait_recv()

    def edge_arrived(p, b):
        j = b * n_col + col

        @pl.when(jnp.logical_and(has_edge(b), j + 1 - p <= n_col + LAG - SETTLE))
        def _():
            arrived(edge_slot(p, j))

    hand_out(0)
    winv3[...] = jnp.zeros(winv3.shape, BF16)

    def seed_arrived(b):
        @pl.when(jnp.logical_not(on_diag))
        def _():
            seed_copy(b, row).wait_recv()

    with jax.named_scope("seed"):
        seed_arrived(0)

        @pl.when(col != 0)
        def _():
            edge_seeded(0)

    def clear(n):
        a, b = lax.rem(n, row_blocks), n // row_blocks

        @pl.when(a * n_row + row < b * n_col + col)
        def _():
            share[n] = jnp.zeros((size, size), F32)
            pltpu.make_async_copy(share.at[n], home(o_ref, a, b), store_sem).start()

    loop(0, row_blocks * col_blocks, clear)

    def times_t(x, y):
        return lax.dot_general(x, y, (((1,), (1,)), ((), ())), preferred_element_type=F32)

    def update_block(p, a, b):
        share[spot(a, b)] -= times_t(panel[row_slot(p, a)], panel[col_of(p, b)])

    def update_diag(p, b):
        other = panel[col_of(p, b)]
        diag[b] -= times_t(other, other)

    def update_edge(p, b):
        @pl.when(has_edge(b))
        def _():
            edge[b] -= times_t(panel[edge_slot(p, b * n_col + col)], panel[col_of(p, b)])

    def column_arrived(p, b):
        @pl.when(jnp.logical_not(on_diag))
        def _():
            arrived(col_slot(p, b))
            column_relay(p, b, start)

    def update_column(p, b, lo):
        lone = lax.rem(row_blocks - lo, 2)

        @pl.when(lone == 1)
        def _():
            update_block(p, lo, b)

        def pair(m):
            a = lo + lone + 2 * m
            both = pl.ds(spot(a, b), 2)
            left = panel[pl.ds(row_slot(p, a), 2)].reshape(2 * size, size)
            share[both] -= times_t(left, panel[col_of(p, b)]).reshape(2, size, size)

        loop(0, (row_blocks - lo) // 2, pair)

    def trail(p, b_from, near):
        loop(b_from, col_blocks, lambda b: update_column(p, b, first_a(b * n_col + col - jnp.where(b == near, 0, 1))))

    def columns_arrived(p, b_from):
        def one(b):
            column_arrived(p, b)
            edge_arrived(p, b)

        loop(b_from, col_blocks, one)

    def prepare(b):
        work[size:, :] = jnp.zeros((BASE, size), F32)
        r_id = lax.broadcasted_iota(jnp.int32, (size + BASE, size), 0)
        c_id = lax.broadcasted_iota(jnp.int32, (size + BASE, size), 1)
        winv[...] = jnp.where(r_id == c_id, 1.0, 0.0).astype(F32)

    def times_winv_t(x):
        hi, mid, lo = split3(x)
        whi, wmid, wlo = winv3[0], winv3[1], winv3[2]
        small = times_t(lo, whi) + times_t(mid, wmid) + times_t(hi, wlo)
        return small + (times_t(mid, whi) + times_t(hi, wmid)) + times_t(hi, whi)

    def solve(k, a, count):
        kb = k // n_col
        near = a == first_a(k)
        here = pl.ds(spot(a, kb), count)

        def apply(p):
            left = panel[pl.ds(row_slot(p, a), count)].reshape(count * size, size)
            share[here] -= times_t(left, panel[col_of(p, kb)]).reshape(count, size, size)

        @pl.when(jnp.logical_not(near))
        def _():
            for m in range(count):

                @pl.when(k >= 3)
                def _():
                    receive(k - 3, a + m)

                @pl.when(jnp.logical_and(k >= 2, a + m > last_near(k - 2)))
                def _():
                    receive(k - 2, a + m)

            loop(jnp.maximum(k - 2 - LAG, 0), k - 1, apply)

        @pl.when(k > 0)
        def _():
            for m in range(count):
                receive(k - 1, a + m)
            apply(k - 1)

        x = times_winv_t(share[here].reshape(count * size, size)).reshape(count, size, size)
        panel[pl.ds(row_slot(k, a), count)] = x.astype(BF16)
        share[here] = x
        if count == 1:

            @pl.when(jnp.logical_and(near, jnp.logical_and(leads, lax.rem(k + 1, n_row) == LEAD)))
            def _():
                first[...] = panel[row_slot(k, a)]
                first_out(k, start)

        if count == 1:
            source_sends(k, a, start)
        else:
            loop(a, a + count, lambda n: source_sends(k, n, start))
        for m in range(count):
            pltpu.make_async_copy(share.at[spot(a + m, kb)], home(o_ref, a + m, kb), store_sem).start()

    def update_near(p, b):
        update_diag(p, b)
        update_edge(p, b)

    def first_slot(k, dev_row):
        return jnp.where(lax.rem(k + 1, n_row) == dev_row, row_slot(k, (k + 1) // n_row), col_slot(k, (k + 1) // n_col))

    def first_copy(k, dev_row, sem):
        dst = first_slot(k, dev_row)
        return pltpu.make_async_remote_copy(
            src_ref=first, dst_ref=panel.at[dst], send_sem=sem, recv_sem=recv_sem.at[dst],
            device_id=at(dev_row, lax.rem(col + 1, n_col)), device_id_type=MESH,
        )

    def others_first(k, fn):
        urgent = lax.rem(k + 3, n_row)
        lone = urgent == LEAD
        for m in range(n_row - 1):
            fn(m, lax.rem(jnp.where(lone, LEAD + 1, urgent) + m + jnp.where(lax.rem(jnp.where(lone, LEAD + 1, urgent) - LEAD + n_row, n_row) + m >= n_row, 1, 0), n_row))

    def first_out(k, act):
        act(first_copy(k, LEAD, first_sem.at[0, 0]))

        @pl.when(odd == 0)
        def _():
            others_first(k, lambda m, r: act(first_copy(k, r, first_sem.at[0, 1 + m])))

    def first_down(k, act):
        @pl.when(odd == 0)
        def _():
            others_first(k, lambda m, r: act(copy(first_slot(k, LEAD), first_slot(k, r), first_sem.at[1, 1 + m], at(r, col))))

    def firsts_done(k):
        @pl.when(jnp.logical_and(leads, k + 1 < steps))
        def _():
            first_out(k, finish)

        @pl.when(jnp.logical_and(leads, k > 0))
        def _():
            first_down(k - 1, finish)

    @pl.when(col == 0)
    def _():
        prepare(0)
        work[0:size, :] = diag[0]

    def step(k):
        mine = jnp.logical_and(col == lax.rem(k, n_col), k < steps)
        kb = k // n_col
        last = k - 1
        soon = jnp.logical_and(col == lax.rem(k + 1, n_col), k + 1 < steps)

        @pl.when(mine)
        def _():
            with jax.named_scope("factor"):
                factor_block(work, winv, winv3, prev, fac)

            @pl.when(has_edge(kb))
            def _():
                with jax.named_scope("lead"):

                    @pl.when(k == 0)
                    def _():
                        edge_seeded(kb)

                    @pl.when(k > 0)
                    def _():
                        edge_arrived(last, kb)
                        update_edge(last, kb)

                    first[...] = times_winv_t(edge[kb]).astype(BF16)
                    first_out(k, start)

            lo = first_a(k)
            second = jnp.minimum(lo + 1, row_blocks)
            third = second + lax.rem(row_blocks - second, 2)
            with jax.named_scope("solve_near"):
                loop(lo, third, lambda a: solve(k, a, 1))
            with jax.named_scope("solve_two"):
                loop(0, (row_blocks - third) // 2, lambda m: solve(k, third + 2 * m, 2))

        @pl.when(k >= depth)
        def _():
            with jax.named_scope("passed"):
                passed(k - depth)

        @pl.when(k >= RELAYED)
        def _():
            loop(first_b(k - RELAYED), col_blocks, lambda b: column_relay(k - RELAYED, b, finish))

        @pl.when(mine)
        def _():
            @pl.when(row == lax.rem(k, n_row))
            def _():
                for d in range(1, n_row):
                    seed_copy(kb, lax.rem(row + d, n_row)).wait_send()
                r_id = lax.broadcasted_iota(jnp.int32, (size, size), 0)
                c_id = lax.broadcasted_iota(jnp.int32, (size, size), 1)
                n = spot(k // n_row, kb)
                share[n] = jnp.where(r_id >= c_id, work[0:size, :].T, 0.0)
                pltpu.make_async_copy(share.at[n], home(o_ref, k // n_row, kb), store_sem).start()

        @pl.when(jnp.logical_and(k > 0, jnp.logical_not(jnp.logical_or(mine, soon))))
        def _():
            @pl.when(col != lax.rem(last, n_col))
            def _():
                with jax.named_scope("receive"):
                    end = jnp.where(lead(last) == 3, jnp.minimum(last_near(last) + 1, row_blocks), row_blocks)
                    loop(first_passed(last), end, lambda a: receive_any(last, a))

            near = first_b(k)
            age = k + n_col - (near * n_col + col)
            settle = jnp.logical_and(age == SETTLE, jnp.logical_and(near > 0, near < col_blocks))

            @pl.when(settle)
            def _():
                with jax.named_scope("late_trail"):
                    own = k - SETTLE

                    for back in (LAG + 2, LAG + 1, LAG):

                        @pl.when(own >= back)
                        def _():
                            columns_arrived(own - back, near)

                    loop(jnp.maximum(own - 2 - LAG, 0), own - LAG + 1, lambda p: trail(p, near, -1))

            @pl.when(jnp.logical_and(k >= LAG, lead(last) != 3))
            def _():
                p = k - LAG
                with jax.named_scope("columns"):
                    columns_arrived(p, near)

                @pl.when(jnp.logical_and(near < col_blocks, age >= SETTLE + 2))
                def _():
                    @pl.when(jnp.logical_and(age == SETTLE + 2, near > 0))
                    def _():
                        with jax.named_scope("seed_late"):
                            seed_arrived(near)
                            edge_seeded(near)

                    oldest = jnp.where(age == SETTLE + 2, jnp.maximum(p - 1, 0), p)
                    loop(oldest, p + 1, lambda q: update_near(q, near))

                with jax.named_scope("trail"):
                    trail(p, near, jnp.where(jnp.logical_or(age > SETTLE, near == 0), near, -1))

            @pl.when(settle)
            def _():
                hand_out(near)

        @pl.when(soon)
        def _():
            nb = (k + 1) // n_col

            oldest = jnp.maximum(k - 1 - LAG, 0)
            lo = first_a(k + 1)

            def old_diag(p):
                column_arrived(p, nb)
                edge_arrived(p, nb)
                update_near(p, nb)

            def take(a):
                receive(last, a)

                @pl.when(jnp.logical_and(a * n_row + row > k + 1, a <= lo))
                def _():
                    loop(oldest, last, lambda p: update_block(p, a, nb))

            @pl.when(k > 0)
            def _():
                with jax.named_scope("old_diag"):
                    loop(oldest, last, old_diag)
                with jax.named_scope("take"):
                    loop(first_a(k), jnp.minimum(last_near(last) + 1, row_blocks), take)
                with jax.named_scope("take_column"):
                    column_arrived(last, nb)
                    edge_arrived(last, nb)
                with jax.named_scope("catch_up"):
                    update_near(last, nb)
                    loop(first_a(k + 1), jnp.minimum(first_a(k + 1) + 1, row_blocks), lambda a: update_block(last, a, nb))

            prepare(nb)
            slot = col_of(k, nb)
            with jax.named_scope("first_block"):
                arrived(slot)

            @pl.when(leads)
            def _():
                first_down(k, start)

            other = panel[slot]
            work[0:size, :] = diag[nb] - times_t(other, other)

        @pl.when(jnp.logical_and(k >= n_col // 2, col == lax.rem(k + n_col // 2, n_col)))
        def _():
            with jax.named_scope("sends_done"):
                firsts_done(k - n_col // 2)
                loop(first_a(k - n_col // 2), row_blocks, lambda a: source_sends(k - n_col // 2, a, finish))

    loop(0, steps + n_col // 2, step)

    def edges_done(b):
        @pl.when(jnp.logical_and(holds_edge(b), jnp.logical_not(leads)))
        def _():
            edge_copy(b).wait_send()

    loop(0, col_blocks, edges_done)
    with jax.named_scope("stored"):
        pltpu.make_async_copy(share, share, store_sem).wait()


def solution(mesh):
    n_row = mesh.shape["row"]
    n_col = mesh.shape["col"]

    def factor_local(a_loc):
        row_blocks, size, local_cols = a_loc.shape
        col_blocks = local_cols // size
        slots = n_row * (row_blocks * (row_blocks + 1) // 2) + n_col * (col_blocks * (col_blocks + 1) // 2)
        slots += 2 * row_blocks * n_row
        return pl.pallas_call(
            functools.partial(kernel, n_row, n_col, "batch"),
            out_shape=jax.ShapeDtypeStruct(a_loc.shape, F32),
            in_specs=[pl.BlockSpec(memory_space=pl.ANY)],
            out_specs=pl.BlockSpec(memory_space=pl.ANY),
            scratch_shapes=[
                pltpu.VMEM((row_blocks * col_blocks, size, size), F32),
                pltpu.VMEM((col_blocks, size, size), F32),
                pltpu.VMEM((col_blocks, size, size), F32),
                pltpu.VMEM((col_blocks, size, size), F32),
                pltpu.VMEM((size, size), BF16),
                pltpu.VMEM((slots, size, size), BF16),
                pltpu.VMEM((size + BASE, size), F32),
                pltpu.VMEM((size + BASE, size), F32),
                pltpu.VMEM((3, size, size), BF16),
                pltpu.VMEM((BASE, 3 * LANE), F32),
                pltpu.VMEM((4 * SUB, SUB, LANE), F32),
                pltpu.SemaphoreType.DMA,
                pltpu.SemaphoreType.DMA,
                pltpu.SemaphoreType.DMA((col_blocks, n_row)),
                pltpu.SemaphoreType.DMA((col_blocks,)),
                pltpu.SemaphoreType.DMA((col_blocks,)),
                pltpu.SemaphoreType.DMA((col_blocks,)),
                pltpu.SemaphoreType.DMA((2, n_row)),
                pltpu.SemaphoreType.DMA((row_blocks, 9)),
                pltpu.SemaphoreType.DMA((4, row_blocks, 6)),
                pltpu.SemaphoreType.DMA((RELAYED + 2, col_blocks)),
                pltpu.SemaphoreType.DMA((slots,)),
            ],
            compiler_params=pltpu.CompilerParams(
                collective_id=0, has_side_effects=True, vmem_limit_bytes=60 * 1024 * 1024
            ),
            name="cholesky",
        )(a_loc)

    blk_spec = P(("batch", "row"), None, "col")
    return jax.shard_map(factor_local, mesh=mesh, in_specs=(blk_spec,), out_specs=blk_spec, check_vma=False)
```

```python
import functools

import jax
import jax.numpy as jnp
from jax import lax
from jax.experimental import pallas as pl
from jax.experimental.pallas import tpu as pltpu
from jax.sharding import PartitionSpec as P

F32 = jnp.float32
BF16 = jnp.bfloat16
MESH = pl.DeviceIdType.MESH
SUB = 8
LANE = 128
BASE = 16
LEAD = 1
SETTLE = 3
LAG = 3


def sub_bcast(x, q):
    return jnp.broadcast_to(x[q : q + 1, :], (SUB, LANE))


ALONG_LANES = lax.GatherDimensionNumbers(
    offset_dims=(), collapsed_slice_dims=(1,), start_index_map=(1,), operand_batching_dims=(0,), start_indices_batching_dims=(0,)
)


def lane_bcast(x, lane):
    index = jnp.full((SUB, LANE, 1), lane, jnp.int32)
    return lax.gather(x, index, ALONG_LANES, (1, 1), mode=lax.GatherScatterMode.PROMISE_IN_BOUNDS)


def split3(x):
    high = x.astype(BF16)
    rest = x - high.astype(F32)
    mid = rest.astype(BF16)
    return high, mid, (rest - mid.astype(F32)).astype(BF16)


def swap_rows(x, bit, row_id):
    if bit == SUB // 2:
        return pltpu.roll(x, bit, 0)
    return jnp.where((row_id & bit) == 0, pltpu.roll(x, SUB - bit, 0), pltpu.roll(x, bit, 0))


def stack_sums(parts):
    row_id = lax.broadcasted_iota(jnp.int32, (SUB, LANE), 0)
    for bit in (4, 2, 1):
        low = (row_id & bit) == 0
        half = len(parts) // 2
        parts = [
            jnp.where(low, parts[n], parts[n + half]) + swap_rows(jnp.where(low, parts[n + half], parts[n]), bit, row_id)
            for n in range(half)
        ]
    return parts[0]


def eliminate(rows, lane0):
    row_id = lax.broadcasted_iota(jnp.int32, (SUB, LANE), 0)
    rows = [list(rows[0]), list(rows[1])]
    cols = [
        [lane_bcast(rows[0][0], lane0 + j) for j in range(SUB)],
        [lane_bcast(rows[1][0], lane0 + j) for j in range(BASE)],
    ]
    scale = [jnp.zeros((SUB, LANE), F32), jnp.zeros((SUB, LANE), F32)]
    pivot = sub_bcast(cols[0][0], 0)
    for j in range(BASE):
        t, q = divmod(j, SUB)
        inv = lax.rsqrt(pivot)
        scale[t] = jnp.where(row_id == q, inv, scale[t])
        if j + 1 < BASE:
            tn, qn = divmod(j + 1, SUB)
            near = sub_bcast(cols[tn][j], qn) * inv
            pivot = sub_bcast(cols[tn][j + 1], qn) - near * near
        below = cols[1][j] * inv
        here = cols[0][j] * inv if t == 0 else None
        for n in range(j + 1, BASE):
            tn, qn = divmod(n, SUB)
            other = near if n == j + 1 else sub_bcast(here if tn == 0 else below, qn)
            if t == 0 and tn == 0:
                cols[0][n] = cols[0][n] - here * other
            cols[1][n] = cols[1][n] - below * other
        masked = jnp.where(row_id > q, here if t == 0 else below, 0.0)
        for v in range(len(rows[0])):
            pivot_row = sub_bcast(rows[t][v], q) * inv
            rows[t][v] = rows[t][v] - masked * pivot_row
            if t == 0:
                rows[1][v] = rows[1][v] - below * pivot_row
    return [[x * scale[t] for x in rows[t]] for t in range(2)]


def factor_block(work, winv, winv3, prev, fac):
    size = work.shape[1]
    prev[...] = jnp.zeros(prev.shape, F32)
    fac[...] = jnp.zeros(fac.shape, F32)

    def group(v):
        return slice(LANE * v, LANE * (v + 1))

    def pending(factors, before, t, v):
        above, below = before[:SUB, group(v)], before[SUB:, group(v)]
        at = 2 * SUB * t
        return stack_sums([factors[at + n] * above + factors[at + SUB + n] * below for n in range(SUB)])

    for half in range(size // LANE):
        views = [(work, 0), (work, 1), (winv, 0)] if half == 0 else [(work, 1), (winv, 0), (winv, 1)]
        first = half * LANE
        if half == 1:
            factors, before = fac[...], prev[...]
            work[first : first + BASE, group(1)] -= jnp.concatenate([pending(factors, before, t, 1) for t in range(2)], axis=0)
            prev[...] = jnp.concatenate([before[:, group(1)], before[:, group(2)], jnp.zeros((BASE, LANE), F32)], axis=1)

        def body(s, carry, views=views, first=first):
            lane0 = s * BASE
            row0 = pl.multiple_of(first + lane0, BASE)

            here = pl.ds(row0, BASE)
            then = pl.ds(pl.multiple_of(row0 + BASE, BASE), BASE)
            both = [ref[here, group(g)] for ref, g in views]
            rows = [[x[SUB * t : SUB * (t + 1)] for x in both] for t in range(2)]
            factors, before = fac[...], prev[...]
            for t in range(2):
                for v in (1, 2):
                    rows[t][v] = rows[t][v] - pending(factors, before, t, v)
            hi, mid, lo = split3(before)
            lane = lax.broadcasted_iota(jnp.int32, (BASE, size - first), 1) + first
            after = lane >= row0 + BASE
            lhi, lmid, llo = [jnp.where(after, x[:, : size - first], jnp.zeros((), BF16)) for x in (hi, mid, lo)]
            update = lax.dot_general(
                jnp.concatenate([lhi, lhi, lmid, lhi, llo, lmid], axis=0),
                jnp.concatenate([hi, mid, hi, lo, hi, mid], axis=0),
                (((0,), (0,)), ((), ())),
                preferred_element_type=F32,
            )
            for v, (ref, g) in enumerate(views):
                ref[first:size, group(g)] -= update[:, group(v)]
            done = eliminate(rows, lane0)
            if first == 0:
                source = [jnp.where(s == LANE // BASE - 1, done[t][1], done[t][0]) for t in range(2)]
            else:
                source = [done[t][0] for t in range(2)]
            next_lane = (lane0 + BASE) % LANE
            factors, sums = [], []
            for t in range(2):
                factor = [[lane_bcast(source[m], next_lane + SUB * t + n) for n in range(SUB)] for m in range(2)]
                sums.append(stack_sums([factor[0][n] * done[0][0] + factor[1][n] * done[1][0] for n in range(SUB)]))
                factors += factor[0] + factor[1]
            ref, g = views[0]
            ref[then, group(g)] -= jnp.concatenate(sums, axis=0)
            fac[...] = jnp.stack(factors)
            whole = [jnp.concatenate([done[0][v], done[1][v]], axis=0) for v in range(3)]
            prev[...] = jnp.concatenate(whole, axis=1)
            for (ref, g), x in zip(views, whole):
                ref[here, group(g)] = x
                if ref is winv:
                    for n, part in enumerate(split3(x)):
                        winv3[n, here, group(g)] = part
            return carry

        lax.fori_loop(0, LANE // BASE, body, 0)


def kernel(n_row, n_col, batch_axis, a_ref, o_ref, share, diag, edge, stage, first, panel, work, winv, winv3, prev, fac, load_sem, store_sem,
           seed_send, seed_recv, edge_send, edge_recv, first_sem, send_sem, pass_sem, recv_sem):
    row_blocks, size, local_cols = a_ref.shape
    col_blocks = local_cols // size
    ratio = n_col // n_row
    steps = row_blocks * n_row
    depth = pass_sem.shape[0]
    batch = lax.axis_index(batch_axis)
    row = lax.axis_index("row")
    col = lax.axis_index("col")
    odd = lax.rem(col, 2)
    on_diag = lax.rem(col, n_row) == row
    row_slots = n_row * (row_blocks * (row_blocks + 1) // 2)
    edge_slots = row_slots + n_col * (col_blocks * (col_blocks + 1) // 2)
    leads = row == LEAD

    def at(dev_row, dev_col):
        return (batch, dev_row, dev_col)

    def row_slot(k, a):
        g = k // n_row
        return n_row * (row_blocks * g - (g * (g - 1)) // 2) + (k - g * n_row) * (row_blocks - g) + a - g

    def col_slot(k, b):
        h = k // n_col
        return row_slots + n_col * (col_blocks * h - (h * (h - 1)) // 2) + (k - h * n_col) * (col_blocks - h) + b - h

    def first_a(k):
        return (k + n_row - row) // n_row

    def first_b(k):
        return (k + n_col - col) // n_col

    def home(ref, a, b):
        return ref.at[a, :, pl.ds(pl.multiple_of(b * size, size), size)]

    def spot(a, b):
        return b * row_blocks + a

    def col_of(k, b):
        return jnp.where(on_diag, row_slot(k, ratio * b + col // n_row), col_slot(k, b))

    def edge_slot(k, j):
        return edge_slots + 2 * k + (j - k - 1) // n_col

    def edge_reach(ahead):
        return jnp.logical_and(ahead >= 2, jnp.logical_and(ahead <= n_col + LAG - SETTLE, row != LEAD))

    def copy(src_slot, dst_slot, sem, device):
        return pltpu.make_async_remote_copy(
            src_ref=panel.at[src_slot], dst_ref=panel.at[dst_slot], send_sem=sem, recv_sem=recv_sem.at[dst_slot],
            device_id=device, device_id_type=MESH,
        )

    def arrived(slot):
        copy(slot, slot, send_sem.at[0, 0], at(row, col)).wait_recv()

    def start(c):
        c.start()

    def finish(c):
        c.wait_send()

    def from_maker(ahead, way):
        there = lax.rem(row + way, n_row)
        lead_near = jnp.logical_and(there == LEAD, jnp.logical_and(ahead >= 2, ahead <= n_row))
        soon_needed = jnp.logical_and(ahead == 2, way == 2)
        return jnp.logical_or(lead_near, soon_needed)

    def down_column(k, a, maker, sems, act):
        i = a * n_row + row
        slot = row_slot(k, a)
        dst = col_slot(k, i // n_col)
        for m, way in enumerate((1, n_row - 1, 2)):
            direct = from_maker(i - k, way)

            @pl.when(jnp.where(maker, direct, jnp.logical_not(direct)))
            def _():
                act(copy(slot, dst, sems[m], at(lax.rem(row + way, n_row), lax.rem(i, n_col))))

    def last_near(p):
        return first_a(p + 2)

    def to_edge(k, a, sem, act):
        i = a * n_row + row
        act(copy(row_slot(k, a), edge_slot(k, i - 1), sem, at(LEAD, lax.rem(i - 1, n_col))))

    def source_sends(k, a, act):
        ahead = a * n_row + row - k
        slot = row_slot(k, a)
        early = n_row

        @pl.when(edge_reach(ahead))
        def _():
            to_edge(k, a, send_sem.at[a, 5], act)

        near = jnp.logical_and(ahead >= 2, ahead <= early)

        @pl.when(jnp.logical_or(near, lax.rem(ahead, n_col) == 0))
        def _():
            down_column(k, a, near, [send_sem.at[a, m] for m in range(3)], act)

        @pl.when(jnp.logical_or(jnp.logical_and(odd == 0, ahead >= 2), ahead >= n_col - 1))
        def _():
            act(copy(slot, slot, send_sem.at[a, 3], at(row, lax.rem(jnp.where(odd == 0, col + 1, col - 1), n_col))))

        @pl.when(ahead >= 2)
        def _():
            act(copy(slot, slot, send_sem.at[a, 6], at(row, lax.rem(col - odd + 2, n_col))))

        @pl.when(jnp.logical_and(ahead >= 3 - odd, a <= last_near(k)))
        def _():
            act(copy(slot, slot, send_sem.at[a, 4], at(row, lax.rem(col - odd + 3, n_col))))

        @pl.when(jnp.logical_and(ahead >= n_col // 2 - odd, ahead < n_col - 2 - odd))
        def _():
            act(copy(slot, slot, send_sem.at[a, 7], at(row, lax.rem(col - odd + 5, n_col))))

        @pl.when(ahead >= n_col - 2 - odd)
        def _():
            act(copy(slot, slot, send_sem.at[a, 8], at(row, lax.rem(col - odd - 2 + n_col, n_col))))

    def lead(p):
        return lax.rem(col - lax.rem(p, n_col) + n_col, n_col)

    def hops(p):
        return lax.rem(col // 2 - lax.rem(p, n_col) // 2 + n_col // 2, n_col // 2)

    def passes(p):
        return jnp.where(odd == 1, 2, n_col // 2 - 1) == hops(p)

    def first_passed(p):
        low = jnp.where(jnp.logical_and(passes(p), odd == 1), lead(p) - 1, lead(p))
        return (p + low - row + n_row - 1) // n_row

    def pass_down(p, a, act):
        i = a * n_row + row
        ahead = i - p
        sems = pass_sem.at[lax.rem(p, depth), a]

        @pl.when(jnp.logical_and(odd == 0, jnp.logical_and(lead(p) <= 2, a > last_near(p))))
        def _():
            act(copy(row_slot(p, a), row_slot(p, a), sems.at[3], at(row, col + 1)))

        @pl.when(jnp.logical_and(lax.rem(i, n_col) == col, ahead > 1))
        def _():
            down_column(p, a, False, [sems.at[m] for m in range(3)], act)

    def pass_on(p, a, act):
        slot = row_slot(p, a)
        sems = pass_sem.at[lax.rem(p, depth), a]

        @pl.when(passes(p))
        def _():
            @pl.when(odd == 0)
            def _():
                act(copy(slot, slot, sems.at[4], at(row, lax.rem(col - 1 + n_col, n_col))))

            @pl.when(jnp.logical_or(odd == 1, a * n_row + row > p + lead(p)))
            def _():
                act(copy(slot, slot, sems.at[3], at(row, col + 1 - 2 * odd)))

        pass_down(p, a, act)

    def passed(p):
        @pl.when(lead(p) != 0)
        def _():
            loop(first_passed(p), row_blocks, lambda a: pass_on(p, a, finish))

    def receive(p, a):
        arrived(row_slot(p, a))
        pass_down(p, a, start)

    def receive_any(p, a):
        arrived(row_slot(p, a))
        pass_on(p, a, start)

    def loop(lo, hi, fn):
        lax.fori_loop(lo, hi, lambda n, c: (fn(n), c)[1], 0)

    for a in range(row_blocks):
        for b in range(col_blocks):
            pltpu.make_async_copy(home(a_ref, a, b), share.at[spot(a, b)], load_sem).start()

    barrier = pltpu.get_barrier_semaphore()
    n_dev = n_row * n_col

    def greet(n):
        other = lax.rem(row * n_col + col + n, n_dev)
        pl.semaphore_signal(barrier, inc=1, device_id=at(other // n_col, lax.rem(other, n_col)), device_id_type=MESH)

    loop(1, n_dev, greet)
    with jax.named_scope("all_here"):
        pl.semaphore_wait(barrier, n_dev - 1)
    with jax.named_scope("loaded"):
        pltpu.make_async_copy(share, share, load_sem).wait()

    def seed_copy(b, dev_row):
        return pltpu.make_async_remote_copy(
            src_ref=share.at[spot(ratio * b + col // n_row, b)], dst_ref=diag.at[b],
            send_sem=seed_send.at[b, lax.rem(dev_row - row + n_row, n_row)],
            recv_sem=seed_recv.at[b], device_id=at(dev_row, col), device_id_type=MESH,
        )

    def hand_out(b):
        @pl.when(on_diag)
        def _():
            for d in (1, n_row - 1, 2):
                seed_copy(b, lax.rem(row + d, n_row)).start()
            diag[b] = share[spot(ratio * b + col // n_row, b)]

        @pl.when(jnp.logical_and(holds_edge(b), jnp.logical_not(leads)))
        def _():
            stage[b] = share[spot((b * n_col + col + 1) // n_row, b)]
            edge_copy(b).start()

    def holds_edge(b):
        j = b * n_col + col
        return jnp.logical_and(lax.rem(j + 1, n_row) == row, j + 1 < steps)

    def edge_copy(b):
        return pltpu.make_async_remote_copy(
            src_ref=stage.at[b], dst_ref=edge.at[b], send_sem=edge_send.at[b], recv_sem=edge_recv.at[b],
            device_id=at(LEAD, col), device_id_type=MESH,
        )

    def has_edge(b):
        from_other = jnp.logical_and(leads, lax.rem(col + 1, n_row) != LEAD)
        return jnp.logical_and(from_other, b * n_col + col + 1 < steps)

    def edge_seeded(b):
        @pl.when(has_edge(b))
        def _():
            edge_copy(b).wait_recv()

    def edge_arrived(p, b):
        j = b * n_col + col

        @pl.when(jnp.logical_and(has_edge(b), j + 1 - p <= n_col + LAG - SETTLE))
        def _():
            arrived(edge_slot(p, j))

    hand_out(0)
    winv3[...] = jnp.zeros(winv3.shape, BF16)

    def seed_arrived(b):
        @pl.when(jnp.logical_not(on_diag))
        def _():
            seed_copy(b, row).wait_recv()

    with jax.named_scope("seed"):
        seed_arrived(0)

        @pl.when(col != 0)
        def _():
            edge_seeded(0)

    def clear(n):
        a, b = lax.rem(n, row_blocks), n // row_blocks

        @pl.when(a * n_row + row < b * n_col + col)
        def _():
            share[n] = jnp.zeros((size, size), F32)
            pltpu.make_async_copy(share.at[n], home(o_ref, a, b), store_sem).start()

    loop(0, row_blocks * col_blocks, clear)

    def times_t(x, y):
        return lax.dot_general(x, y, (((1,), (1,)), ((), ())), preferred_element_type=F32)

    def update_block(p, a, b):
        share[spot(a, b)] -= times_t(panel[row_slot(p, a)], panel[col_of(p, b)])

    def update_diag(p, b):
        other = panel[col_of(p, b)]
        diag[b] -= times_t(other, other)

    def update_edge(p, b):
        @pl.when(has_edge(b))
        def _():
            edge[b] -= times_t(panel[edge_slot(p, b * n_col + col)], panel[col_of(p, b)])

    def column_arrived(p, b):
        @pl.when(jnp.logical_not(on_diag))
        def _():
            arrived(col_slot(p, b))

    def update_column(p, b, lo):
        lone = lax.rem(row_blocks - lo, 2)

        @pl.when(lone == 1)
        def _():
            update_block(p, lo, b)

        def pair(m):
            a = lo + lone + 2 * m
            both = pl.ds(spot(a, b), 2)
            left = panel[pl.ds(row_slot(p, a), 2)].reshape(2 * size, size)
            share[both] -= times_t(left, panel[col_of(p, b)]).reshape(2, size, size)

        loop(0, (row_blocks - lo) // 2, pair)

    def trail(p, b_from, near):
        loop(b_from, col_blocks, lambda b: update_column(p, b, first_a(b * n_col + col - jnp.where(b == near, 0, 1))))

    def columns_arrived(p, b_from):
        def one(b):
            column_arrived(p, b)
            edge_arrived(p, b)

        loop(b_from, col_blocks, one)

    def prepare(b):
        work[size:, :] = jnp.zeros((BASE, size), F32)
        r_id = lax.broadcasted_iota(jnp.int32, (size + BASE, size), 0)
        c_id = lax.broadcasted_iota(jnp.int32, (size + BASE, size), 1)
        winv[...] = jnp.where(r_id == c_id, 1.0, 0.0).astype(F32)

    def times_winv_t(x):
        hi, mid, lo = split3(x)
        whi, wmid, wlo = winv3[0], winv3[1], winv3[2]
        small = times_t(lo, whi) + times_t(mid, wmid) + times_t(hi, wlo)
        return small + (times_t(mid, whi) + times_t(hi, wmid)) + times_t(hi, whi)

    def here_diag(k):
        return row == lax.rem(k, n_row)

    def solve(k, a, count):
        kb = k // n_col
        near = jnp.logical_and(a == first_a(k), jnp.logical_not(here_diag(k)))
        here = pl.ds(spot(a, kb), count)

        def apply(p):
            left = panel[pl.ds(row_slot(p, a), count)].reshape(count * size, size)
            share[here] -= times_t(left, panel[col_of(p, kb)]).reshape(count, size, size)

        @pl.when(jnp.logical_not(near))
        def _():
            for m in range(count):

                @pl.when(k >= 3)
                def _():
                    receive(k - 3, a + m)

                @pl.when(k >= 2)
                def _():
                    receive(k - 2, a + m)

            loop(jnp.maximum(k - 2 - LAG, 0), k - 1, apply)

        @pl.when(k > 0)
        def _():
            for m in range(count):
                receive(k - 1, a + m)
            apply(k - 1)

        x = times_winv_t(share[here].reshape(count * size, size)).reshape(count, size, size)
        panel[pl.ds(row_slot(k, a), count)] = x.astype(BF16)
        share[here] = x
        if count == 1:

            @pl.when(jnp.logical_and(near, jnp.logical_and(leads, lax.rem(k + 1, n_row) == LEAD)))
            def _():
                first[...] = panel[row_slot(k, a)]
                first_out(k, start)

        if count == 1:
            source_sends(k, a, start)
        else:
            loop(a, a + count, lambda n: source_sends(k, n, start))
        for m in range(count):
            pltpu.make_async_copy(share.at[spot(a + m, kb)], home(o_ref, a + m, kb), store_sem).start()

    def update_near(p, b):
        update_diag(p, b)
        update_edge(p, b)

    def first_slot(k, dev_row):
        return jnp.where(lax.rem(k + 1, n_row) == dev_row, row_slot(k, (k + 1) // n_row), col_slot(k, (k + 1) // n_col))

    def first_copy(k, dev_row, sem):
        dst = first_slot(k, dev_row)
        return pltpu.make_async_remote_copy(
            src_ref=first, dst_ref=panel.at[dst], send_sem=sem, recv_sem=recv_sem.at[dst],
            device_id=at(dev_row, lax.rem(col + 1, n_col)), device_id_type=MESH,
        )

    def others_first(k, fn):
        urgent = lax.rem(k + 3, n_row)
        lone = urgent == LEAD
        for m in range(n_row - 1):
            fn(m, lax.rem(jnp.where(lone, LEAD + 1, urgent) + m + jnp.where(lax.rem(jnp.where(lone, LEAD + 1, urgent) - LEAD + n_row, n_row) + m >= n_row, 1, 0), n_row))

    def first_out(k, act):
        act(first_copy(k, LEAD, first_sem.at[0, 0]))

        @pl.when(odd == 0)
        def _():
            others_first(k, lambda m, r: act(first_copy(k, r, first_sem.at[0, 1 + m])))

    def first_down(k, act):
        @pl.when(odd == 0)
        def _():
            others_first(k, lambda m, r: act(copy(first_slot(k, LEAD), first_slot(k, r), first_sem.at[1, 1 + m], at(r, col))))

    def firsts_done(k):
        @pl.when(jnp.logical_and(leads, k + 1 < steps))
        def _():
            first_out(k, finish)

        @pl.when(jnp.logical_and(leads, k > 0))
        def _():
            first_down(k - 1, finish)

    @pl.when(col == 0)
    def _():
        prepare(0)
        work[0:size, :] = diag[0]

    def step(k):
        mine = jnp.logical_and(col == lax.rem(k, n_col), k < steps)
        kb = k // n_col
        last = k - 1
        soon = jnp.logical_and(col == lax.rem(k + 1, n_col), k + 1 < steps)

        @pl.when(mine)
        def _():
            with jax.named_scope("factor"):
                factor_block(work, winv, winv3, prev, fac)

            @pl.when(has_edge(kb))
            def _():
                with jax.named_scope("lead"):

                    @pl.when(k == 0)
                    def _():
                        edge_seeded(kb)

                    @pl.when(k > 0)
                    def _():
                        edge_arrived(last, kb)
                        update_edge(last, kb)

                    first[...] = times_winv_t(edge[kb]).astype(BF16)
                    first_out(k, start)

            lo = first_a(k)
            second = jnp.minimum(lo + 1, row_blocks)
            third = second + lax.rem(row_blocks - second, 2)
            with jax.named_scope("solve_near"):
                loop(lo, third, lambda a: solve(k, a, 1))
            with jax.named_scope("solve_two"):
                loop(0, (row_blocks - third) // 2, lambda m: solve(k, third + 2 * m, 2))

        @pl.when(k >= depth)
        def _():
            with jax.named_scope("passed"):
                passed(k - depth)

        @pl.when(mine)
        def _():
            @pl.when(row == lax.rem(k, n_row))
            def _():
                for d in range(1, n_row):
                    seed_copy(kb, lax.rem(row + d, n_row)).wait_send()
                r_id = lax.broadcasted_iota(jnp.int32, (size, size), 0)
                c_id = lax.broadcasted_iota(jnp.int32, (size, size), 1)
                n = spot(k // n_row, kb)
                share[n] = jnp.where(r_id >= c_id, work[0:size, :].T, 0.0)
                pltpu.make_async_copy(share.at[n], home(o_ref, k // n_row, kb), store_sem).start()

        @pl.when(jnp.logical_and(k > 0, jnp.logical_not(jnp.logical_or(mine, soon))))
        def _():
            @pl.when(col != lax.rem(last, n_col))
            def _():
                with jax.named_scope("receive"):
                    end = jnp.where(lead(last) == 3, jnp.minimum(last_near(last) + 1, row_blocks), row_blocks)
                    loop(first_passed(last), end, lambda a: receive_any(last, a))

            near = first_b(k)
            age = k + n_col - (near * n_col + col)
            settle = jnp.logical_and(age == SETTLE, jnp.logical_and(near > 0, near < col_blocks))

            @pl.when(settle)
            def _():
                with jax.named_scope("late_trail"):
                    own = k - SETTLE

                    for back in (LAG + 2, LAG + 1, LAG):

                        @pl.when(own >= back)
                        def _():
                            columns_arrived(own - back, near)

                    loop(jnp.maximum(own - 2 - LAG, 0), own - LAG + 1, lambda p: trail(p, near, -1))

            @pl.when(jnp.logical_and(k >= LAG, lead(last) != 3))
            def _():
                p = k - LAG
                with jax.named_scope("columns"):
                    columns_arrived(p, near)

                @pl.when(jnp.logical_and(near < col_blocks, age >= SETTLE + 2))
                def _():
                    @pl.when(jnp.logical_and(age == SETTLE + 2, near > 0))
                    def _():
                        with jax.named_scope("seed_late"):
                            seed_arrived(near)
                            edge_seeded(near)

                    oldest = jnp.where(age == SETTLE + 2, jnp.maximum(p - 1, 0), p)
                    loop(oldest, p + 1, lambda q: update_near(q, near))

                with jax.named_scope("trail"):
                    trail(p, near, jnp.where(jnp.logical_or(age > SETTLE, near == 0), near, -1))

            @pl.when(settle)
            def _():
                hand_out(near)

        @pl.when(soon)
        def _():
            nb = (k + 1) // n_col

            oldest = jnp.maximum(k - 1 - LAG, 0)
            lo = first_a(k + 1)

            def old_diag(p):
                column_arrived(p, nb)
                edge_arrived(p, nb)
                update_near(p, nb)

            def take(a):
                receive(last, a)

                @pl.when(jnp.logical_not(here_diag(k + 1)))
                def _():
                    loop(oldest, last, lambda p: update_block(p, a, nb))

            @pl.when(k > 0)
            def _():
                with jax.named_scope("old_diag"):
                    loop(oldest, last, old_diag)
                with jax.named_scope("take"):
                    loop(first_a(k), jnp.minimum(first_a(k) + 1, row_blocks), take)
                with jax.named_scope("take_column"):
                    column_arrived(last, nb)
                    edge_arrived(last, nb)
                with jax.named_scope("catch_up"):
                    update_near(last, nb)
                    @pl.when(jnp.logical_and(jnp.logical_not(here_diag(k + 1)), lo < row_blocks))
                    def _():
                        update_block(last, lo, nb)

            prepare(nb)
            slot = col_of(k, nb)
            with jax.named_scope("first_block"):
                arrived(slot)

            @pl.when(leads)
            def _():
                first_down(k, start)

            other = panel[slot]
            work[0:size, :] = diag[nb] - times_t(other, other)

        @pl.when(jnp.logical_and(k >= n_col // 2, col == lax.rem(k + n_col // 2, n_col)))
        def _():
            with jax.named_scope("sends_done"):
                firsts_done(k - n_col // 2)
                loop(first_a(k - n_col // 2), row_blocks, lambda a: source_sends(k - n_col // 2, a, finish))

    loop(0, steps + n_col // 2, step)

    def edges_done(b):
        @pl.when(jnp.logical_and(holds_edge(b), jnp.logical_not(leads)))
        def _():
            edge_copy(b).wait_send()

    loop(0, col_blocks, edges_done)
    with jax.named_scope("stored"):
        pltpu.make_async_copy(share, share, store_sem).wait()


def solution(mesh):
    n_row = mesh.shape["row"]
    n_col = mesh.shape["col"]

    def factor_local(a_loc):
        row_blocks, size, local_cols = a_loc.shape
        col_blocks = local_cols // size
        slots = n_row * (row_blocks * (row_blocks + 1) // 2) + n_col * (col_blocks * (col_blocks + 1) // 2)
        slots += 2 * row_blocks * n_row
        return pl.pallas_call(
            functools.partial(kernel, n_row, n_col, "batch"),
            out_shape=jax.ShapeDtypeStruct(a_loc.shape, F32),
            in_specs=[pl.BlockSpec(memory_space=pl.ANY)],
            out_specs=pl.BlockSpec(memory_space=pl.ANY),
            scratch_shapes=[
                pltpu.VMEM((row_blocks * col_blocks, size, size), F32),
                pltpu.VMEM((col_blocks, size, size), F32),
                pltpu.VMEM((col_blocks, size, size), F32),
                pltpu.VMEM((col_blocks, size, size), F32),
                pltpu.VMEM((size, size), BF16),
                pltpu.VMEM((slots, size, size), BF16),
                pltpu.VMEM((size + BASE, size), F32),
                pltpu.VMEM((size + BASE, size), F32),
                pltpu.VMEM((3, size, size), BF16),
                pltpu.VMEM((BASE, 3 * LANE), F32),
                pltpu.VMEM((4 * SUB, SUB, LANE), F32),
                pltpu.SemaphoreType.DMA,
                pltpu.SemaphoreType.DMA,
                pltpu.SemaphoreType.DMA((col_blocks, n_row)),
                pltpu.SemaphoreType.DMA((col_blocks,)),
                pltpu.SemaphoreType.DMA((col_blocks,)),
                pltpu.SemaphoreType.DMA((col_blocks,)),
                pltpu.SemaphoreType.DMA((2, n_row)),
                pltpu.SemaphoreType.DMA((row_blocks, 9)),
                pltpu.SemaphoreType.DMA((4, row_blocks, 6)),
                pltpu.SemaphoreType.DMA((slots,)),
            ],
            compiler_params=pltpu.CompilerParams(
                collective_id=0, has_side_effects=True, vmem_limit_bytes=60 * 1024 * 1024
            ),
            name="cholesky",
        )(a_loc)

    blk_spec = P(("batch", "row"), None, "col")
    return jax.shard_map(factor_local, mesh=mesh, in_specs=(blk_spec,), out_specs=blk_spec, check_vma=False)
```

```python
import functools

import jax
import jax.numpy as jnp
from jax import lax
from jax.experimental import pallas as pl
from jax.experimental.pallas import tpu as pltpu
from jax.sharding import PartitionSpec as P

F32 = jnp.float32
BF16 = jnp.bfloat16
MESH = pl.DeviceIdType.MESH
SUB = 8
LANE = 128
BASE = 16
LEAD = 1
SETTLE = 3
LAG = 3


def sub_bcast(x, q):
    return jnp.broadcast_to(x[q : q + 1, :], (SUB, LANE))


ALONG_LANES = lax.GatherDimensionNumbers(
    offset_dims=(), collapsed_slice_dims=(1,), start_index_map=(1,), operand_batching_dims=(0,), start_indices_batching_dims=(0,)
)


def lane_bcast(x, lane):
    index = jnp.full((SUB, LANE, 1), lane, jnp.int32)
    return lax.gather(x, index, ALONG_LANES, (1, 1), mode=lax.GatherScatterMode.PROMISE_IN_BOUNDS)


def split3(x):
    high = x.astype(BF16)
    rest = x - high.astype(F32)
    mid = rest.astype(BF16)
    return high, mid, (rest - mid.astype(F32)).astype(BF16)


def swap_rows(x, bit, row_id):
    if bit == SUB // 2:
        return pltpu.roll(x, bit, 0)
    return jnp.where((row_id & bit) == 0, pltpu.roll(x, SUB - bit, 0), pltpu.roll(x, bit, 0))


def stack_sums(parts):
    row_id = lax.broadcasted_iota(jnp.int32, (SUB, LANE), 0)
    for bit in (4, 2, 1):
        low = (row_id & bit) == 0
        half = len(parts) // 2
        parts = [
            jnp.where(low, parts[n], parts[n + half]) + swap_rows(jnp.where(low, parts[n + half], parts[n]), bit, row_id)
            for n in range(half)
        ]
    return parts[0]


def eliminate(rows, lane0):
    row_id = lax.broadcasted_iota(jnp.int32, (SUB, LANE), 0)
    rows = [list(rows[0]), list(rows[1])]
    cols = [
        [lane_bcast(rows[0][0], lane0 + j) for j in range(SUB)],
        [lane_bcast(rows[1][0], lane0 + j) for j in range(BASE)],
    ]
    scale = [jnp.zeros((SUB, LANE), F32), jnp.zeros((SUB, LANE), F32)]
    pivot = sub_bcast(cols[0][0], 0)
    for j in range(BASE):
        t, q = divmod(j, SUB)
        inv = lax.rsqrt(pivot)
        scale[t] = jnp.where(row_id == q, inv, scale[t])
        if j + 1 < BASE:
            tn, qn = divmod(j + 1, SUB)
            near = sub_bcast(cols[tn][j], qn) * inv
            pivot = sub_bcast(cols[tn][j + 1], qn) - near * near
        below = cols[1][j] * inv
        here = cols[0][j] * inv if t == 0 else None
        for n in range(j + 1, BASE):
            tn, qn = divmod(n, SUB)
            other = near if n == j + 1 else sub_bcast(here if tn == 0 else below, qn)
            if t == 0 and tn == 0:
                cols[0][n] = cols[0][n] - here * other
            cols[1][n] = cols[1][n] - below * other
        masked = jnp.where(row_id > q, here if t == 0 else below, 0.0)
        for v in range(len(rows[0])):
            pivot_row = sub_bcast(rows[t][v], q) * inv
            rows[t][v] = rows[t][v] - masked * pivot_row
            if t == 0:
                rows[1][v] = rows[1][v] - below * pivot_row
    return [[x * scale[t] for x in rows[t]] for t in range(2)]


def factor_block(work, winv, winv3, prev, fac):
    size = work.shape[1]
    prev[...] = jnp.zeros(prev.shape, F32)
    fac[...] = jnp.zeros(fac.shape, F32)

    def group(v):
        return slice(LANE * v, LANE * (v + 1))

    def pending(factors, before, t, v):
        above, below = before[:SUB, group(v)], before[SUB:, group(v)]
        at = 2 * SUB * t
        return stack_sums([factors[at + n] * above + factors[at + SUB + n] * below for n in range(SUB)])

    for half in range(size // LANE):
        views = [(work, 0), (work, 1), (winv, 0)] if half == 0 else [(work, 1), (winv, 0), (winv, 1)]
        first = half * LANE
        if half == 1:
            factors, before = fac[...], prev[...]
            work[first : first + BASE, group(1)] -= jnp.concatenate([pending(factors, before, t, 1) for t in range(2)], axis=0)
            prev[...] = jnp.concatenate([before[:, group(1)], before[:, group(2)], jnp.zeros((BASE, LANE), F32)], axis=1)

        def body(s, carry, views=views, first=first):
            lane0 = s * BASE
            row0 = pl.multiple_of(first + lane0, BASE)

            here = pl.ds(row0, BASE)
            then = pl.ds(pl.multiple_of(row0 + BASE, BASE), BASE)
            both = [ref[here, group(g)] for ref, g in views]
            rows = [[x[SUB * t : SUB * (t + 1)] for x in both] for t in range(2)]
            factors, before = fac[...], prev[...]
            for t in range(2):
                for v in (1, 2):
                    rows[t][v] = rows[t][v] - pending(factors, before, t, v)
            hi, mid, lo = split3(before)
            lane = lax.broadcasted_iota(jnp.int32, (BASE, size - first), 1) + first
            after = lane >= row0 + BASE
            lhi, lmid, llo = [jnp.where(after, x[:, : size - first], jnp.zeros((), BF16)) for x in (hi, mid, lo)]
            update = lax.dot_general(
                jnp.concatenate([lhi, lhi, lmid, lhi, llo, lmid], axis=0),
                jnp.concatenate([hi, mid, hi, lo, hi, mid], axis=0),
                (((0,), (0,)), ((), ())),
                preferred_element_type=F32,
            )
            for v, (ref, g) in enumerate(views):
                ref[first:size, group(g)] -= update[:, group(v)]
            done = eliminate(rows, lane0)
            if first == 0:
                source = [jnp.where(s == LANE // BASE - 1, done[t][1], done[t][0]) for t in range(2)]
            else:
                source = [done[t][0] for t in range(2)]
            next_lane = (lane0 + BASE) % LANE
            factors, sums = [], []
            for t in range(2):
                factor = [[lane_bcast(source[m], next_lane + SUB * t + n) for n in range(SUB)] for m in range(2)]
                sums.append(stack_sums([factor[0][n] * done[0][0] + factor[1][n] * done[1][0] for n in range(SUB)]))
                factors += factor[0] + factor[1]
            ref, g = views[0]
            ref[then, group(g)] -= jnp.concatenate(sums, axis=0)
            fac[...] = jnp.stack(factors)
            whole = [jnp.concatenate([done[0][v], done[1][v]], axis=0) for v in range(3)]
            prev[...] = jnp.concatenate(whole, axis=1)
            for (ref, g), x in zip(views, whole):
                ref[here, group(g)] = x
                if ref is winv:
                    for n, part in enumerate(split3(x)):
                        winv3[n, here, group(g)] = part
            return carry

        lax.fori_loop(0, LANE // BASE, body, 0)


def kernel(n_row, n_col, batch_axis, a_ref, o_ref, share, diag, edge, stage, first, panel, work, winv, winv3, prev, fac, load_sem, store_sem,
           seed_send, seed_recv, edge_send, edge_recv, first_sem, send_sem, pass_sem, recv_sem):
    row_blocks, size, local_cols = a_ref.shape
    col_blocks = local_cols // size
    ratio = n_col // n_row
    steps = row_blocks * n_row
    depth = pass_sem.shape[0]
    batch = lax.axis_index(batch_axis)
    row = lax.axis_index("row")
    col = lax.axis_index("col")
    odd = lax.rem(col, 2)
    on_diag = lax.rem(col, n_row) == row
    row_slots = n_row * (row_blocks * (row_blocks + 1) // 2)
    edge_slots = row_slots + n_col * (col_blocks * (col_blocks + 1) // 2)
    leads = row == LEAD

    def at(dev_row, dev_col):
        return (batch, dev_row, dev_col)

    def row_slot(k, a):
        g = k // n_row
        return n_row * (row_blocks * g - (g * (g - 1)) // 2) + (k - g * n_row) * (row_blocks - g) + a - g

    def col_slot(k, b):
        h = k // n_col
        return row_slots + n_col * (col_blocks * h - (h * (h - 1)) // 2) + (k - h * n_col) * (col_blocks - h) + b - h

    def first_a(k):
        return (k + n_row - row) // n_row

    def first_b(k):
        return (k + n_col - col) // n_col

    def home(ref, a, b):
        return ref.at[a, :, pl.ds(pl.multiple_of(b * size, size), size)]

    def spot(a, b):
        return b * row_blocks + a

    def col_of(k, b):
        return jnp.where(on_diag, row_slot(k, ratio * b + col // n_row), col_slot(k, b))

    def edge_slot(k, j):
        return edge_slots + 2 * k + (j - k - 1) // n_col

    def edge_reach(ahead):
        return jnp.logical_and(ahead >= 2, jnp.logical_and(ahead <= n_col + LAG - SETTLE, row != LEAD))

    def copy(src_slot, dst_slot, sem, device):
        return pltpu.make_async_remote_copy(
            src_ref=panel.at[src_slot], dst_ref=panel.at[dst_slot], send_sem=sem, recv_sem=recv_sem.at[dst_slot],
            device_id=device, device_id_type=MESH,
        )

    def arrived(slot):
        copy(slot, slot, send_sem.at[0, 0], at(row, col)).wait_recv()

    def start(c):
        c.start()

    def finish(c):
        c.wait_send()

    def from_maker(ahead, way):
        there = lax.rem(row + way, n_row)
        lead_near = jnp.logical_and(there == LEAD, jnp.logical_and(ahead >= 2, ahead <= n_row))
        soon_needed = jnp.logical_and(ahead == 2, way == 2)
        return jnp.logical_or(lead_near, soon_needed)

    def down_column(k, a, maker, sems, act):
        i = a * n_row + row
        slot = row_slot(k, a)
        dst = col_slot(k, i // n_col)
        for m, way in enumerate((2, 1, n_row - 1)):
            direct = from_maker(i - k, way)

            @pl.when(jnp.where(maker, direct, jnp.logical_not(direct)))
            def _():
                act(copy(slot, dst, sems[m], at(lax.rem(row + way, n_row), lax.rem(i, n_col))))

    def last_near(p):
        return first_a(p + 2)

    def to_edge(k, a, sem, act):
        i = a * n_row + row
        act(copy(row_slot(k, a), edge_slot(k, i - 1), sem, at(LEAD, lax.rem(i - 1, n_col))))

    def source_sends(k, a, act):
        ahead = a * n_row + row - k
        slot = row_slot(k, a)
        early = n_row

        @pl.when(edge_reach(ahead))
        def _():
            to_edge(k, a, send_sem.at[a, 5], act)

        near = jnp.logical_and(ahead >= 2, ahead <= early)

        @pl.when(jnp.logical_or(near, lax.rem(ahead, n_col) == 0))
        def _():
            down_column(k, a, near, [send_sem.at[a, m] for m in range(3)], act)

        @pl.when(jnp.logical_or(jnp.logical_and(odd == 0, ahead >= 2), ahead >= n_col - 1))
        def _():
            act(copy(slot, slot, send_sem.at[a, 3], at(row, lax.rem(jnp.where(odd == 0, col + 1, col - 1), n_col))))

        @pl.when(ahead >= 2)
        def _():
            act(copy(slot, slot, send_sem.at[a, 6], at(row, lax.rem(col - odd + 2, n_col))))

        @pl.when(jnp.logical_and(ahead >= 3 - odd, a <= last_near(k)))
        def _():
            act(copy(slot, slot, send_sem.at[a, 4], at(row, lax.rem(col - odd + 3, n_col))))

        @pl.when(jnp.logical_and(ahead >= n_col // 2 - odd, ahead < n_col - 2 - odd))
        def _():
            act(copy(slot, slot, send_sem.at[a, 7], at(row, lax.rem(col - odd + 5, n_col))))

        @pl.when(ahead >= n_col - 2 - odd)
        def _():
            act(copy(slot, slot, send_sem.at[a, 8], at(row, lax.rem(col - odd - 2 + n_col, n_col))))

    def lead(p):
        return lax.rem(col - lax.rem(p, n_col) + n_col, n_col)

    def hops(p):
        return lax.rem(col // 2 - lax.rem(p, n_col) // 2 + n_col // 2, n_col // 2)

    def passes(p):
        return jnp.where(odd == 1, 2, n_col // 2 - 1) == hops(p)

    def first_passed(p):
        low = jnp.where(jnp.logical_and(passes(p), odd == 1), lead(p) - 1, lead(p))
        return (p + low - row + n_row - 1) // n_row

    def pass_down(p, a, act):
        i = a * n_row + row
        ahead = i - p
        sems = pass_sem.at[lax.rem(p, depth), a]

        @pl.when(jnp.logical_and(odd == 0, jnp.logical_and(lead(p) <= 2, a > last_near(p))))
        def _():
            act(copy(row_slot(p, a), row_slot(p, a), sems.at[3], at(row, col + 1)))

        @pl.when(jnp.logical_and(lax.rem(i, n_col) == col, ahead > 1))
        def _():
            down_column(p, a, False, [sems.at[m] for m in range(3)], act)

    def pass_on(p, a, act):
        slot = row_slot(p, a)
        sems = pass_sem.at[lax.rem(p, depth), a]

        @pl.when(passes(p))
        def _():
            @pl.when(odd == 0)
            def _():
                act(copy(slot, slot, sems.at[4], at(row, lax.rem(col - 1 + n_col, n_col))))

            @pl.when(jnp.logical_or(odd == 1, a * n_row + row > p + lead(p)))
            def _():
                act(copy(slot, slot, sems.at[3], at(row, col + 1 - 2 * odd)))

        pass_down(p, a, act)

    def passed(p):
        @pl.when(lead(p) != 0)
        def _():
            loop(first_passed(p), row_blocks, lambda a: pass_on(p, a, finish))

    def receive(p, a):
        arrived(row_slot(p, a))
        pass_down(p, a, start)

    def receive_any(p, a):
        arrived(row_slot(p, a))
        pass_on(p, a, start)

    def loop(lo, hi, fn):
        lax.fori_loop(lo, hi, lambda n, c: (fn(n), c)[1], 0)

    for a in range(row_blocks):
        for b in range(col_blocks):
            pltpu.make_async_copy(home(a_ref, a, b), share.at[spot(a, b)], load_sem).start()

    barrier = pltpu.get_barrier_semaphore()
    n_dev = n_row * n_col

    def greet(n):
        other = lax.rem(row * n_col + col + n, n_dev)
        pl.semaphore_signal(barrier, inc=1, device_id=at(other // n_col, lax.rem(other, n_col)), device_id_type=MESH)

    loop(1, n_dev, greet)
    with jax.named_scope("all_here"):
        pl.semaphore_wait(barrier, n_dev - 1)
    with jax.named_scope("loaded"):
        pltpu.make_async_copy(share, share, load_sem).wait()

    def seed_copy(b, dev_row):
        return pltpu.make_async_remote_copy(
            src_ref=share.at[spot(ratio * b + col // n_row, b)], dst_ref=diag.at[b],
            send_sem=seed_send.at[b, lax.rem(dev_row - row + n_row, n_row)],
            recv_sem=seed_recv.at[b], device_id=at(dev_row, col), device_id_type=MESH,
        )

    def hand_out(b):
        @pl.when(on_diag)
        def _():
            for d in (1, n_row - 1, 2):
                seed_copy(b, lax.rem(row + d, n_row)).start()
            diag[b] = share[spot(ratio * b + col // n_row, b)]

        @pl.when(jnp.logical_and(holds_edge(b), jnp.logical_not(leads)))
        def _():
            stage[b] = share[spot((b * n_col + col + 1) // n_row, b)]
            edge_copy(b).start()

    def holds_edge(b):
        j = b * n_col + col
        return jnp.logical_and(lax.rem(j + 1, n_row) == row, j + 1 < steps)

    def edge_copy(b):
        return pltpu.make_async_remote_copy(
            src_ref=stage.at[b], dst_ref=edge.at[b], send_sem=edge_send.at[b], recv_sem=edge_recv.at[b],
            device_id=at(LEAD, col), device_id_type=MESH,
        )

    def has_edge(b):
        from_other = jnp.logical_and(leads, lax.rem(col + 1, n_row) != LEAD)
        return jnp.logical_and(from_other, b * n_col + col + 1 < steps)

    def edge_seeded(b):
        @pl.when(has_edge(b))
        def _():
            edge_copy(b).wait_recv()

    def edge_arrived(p, b):
        j = b * n_col + col

        @pl.when(jnp.logical_and(has_edge(b), j + 1 - p <= n_col + LAG - SETTLE))
        def _():
            arrived(edge_slot(p, j))

    hand_out(0)
    winv3[...] = jnp.zeros(winv3.shape, BF16)

    def seed_arrived(b):
        @pl.when(jnp.logical_not(on_diag))
        def _():
            seed_copy(b, row).wait_recv()

    with jax.named_scope("seed"):
        seed_arrived(0)

        @pl.when(col != 0)
        def _():
            edge_seeded(0)

    def clear(n):
        a, b = lax.rem(n, row_blocks), n // row_blocks

        @pl.when(a * n_row + row < b * n_col + col)
        def _():
            share[n] = jnp.zeros((size, size), F32)
            pltpu.make_async_copy(share.at[n], home(o_ref, a, b), store_sem).start()

    loop(0, row_blocks * col_blocks, clear)

    def times_t(x, y):
        return lax.dot_general(x, y, (((1,), (1,)), ((), ())), preferred_element_type=F32)

    def update_block(p, a, b):
        share[spot(a, b)] -= times_t(panel[row_slot(p, a)], panel[col_of(p, b)])

    def update_diag(p, b):
        other = panel[col_of(p, b)]
        diag[b] -= times_t(other, other)

    def update_edge(p, b):
        @pl.when(has_edge(b))
        def _():
            edge[b] -= times_t(panel[edge_slot(p, b * n_col + col)], panel[col_of(p, b)])

    def column_arrived(p, b):
        @pl.when(jnp.logical_not(on_diag))
        def _():
            arrived(col_slot(p, b))

    def update_column(p, b, lo):
        lone = lax.rem(row_blocks - lo, 2)

        @pl.when(lone == 1)
        def _():
            update_block(p, lo, b)

        def pair(m):
            a = lo + lone + 2 * m
            both = pl.ds(spot(a, b), 2)
            left = panel[pl.ds(row_slot(p, a), 2)].reshape(2 * size, size)
            share[both] -= times_t(left, panel[col_of(p, b)]).reshape(2, size, size)

        loop(0, (row_blocks - lo) // 2, pair)

    def trail(p, b_from, near):
        loop(b_from, col_blocks, lambda b: update_column(p, b, first_a(b * n_col + col - jnp.where(b == near, 0, 1))))

    def columns_arrived(p, b_from):
        def one(b):
            column_arrived(p, b)
            edge_arrived(p, b)

        loop(b_from, col_blocks, one)

    def prepare(b):
        work[size:, :] = jnp.zeros((BASE, size), F32)
        r_id = lax.broadcasted_iota(jnp.int32, (size + BASE, size), 0)
        c_id = lax.broadcasted_iota(jnp.int32, (size + BASE, size), 1)
        winv[...] = jnp.where(r_id == c_id, 1.0, 0.0).astype(F32)

    def times_winv_t(x):
        hi, mid, lo = split3(x)
        whi, wmid, wlo = winv3[0], winv3[1], winv3[2]
        small = times_t(lo, whi) + times_t(mid, wmid) + times_t(hi, wlo)
        return small + (times_t(mid, whi) + times_t(hi, wmid)) + times_t(hi, whi)

    def here_diag(k):
        return row == lax.rem(k, n_row)

    def solve(k, a, count):
        kb = k // n_col
        near = jnp.logical_and(a == first_a(k), jnp.logical_not(here_diag(k)))
        here = pl.ds(spot(a, kb), count)

        def apply(p):
            left = panel[pl.ds(row_slot(p, a), count)].reshape(count * size, size)
            share[here] -= times_t(left, panel[col_of(p, kb)]).reshape(count, size, size)

        @pl.when(jnp.logical_not(near))
        def _():
            for m in range(count):

                @pl.when(k >= 3)
                def _():
                    receive(k - 3, a + m)

                @pl.when(k >= 2)
                def _():
                    receive(k - 2, a + m)

            loop(jnp.maximum(k - 2 - LAG, 0), k - 1, apply)

        @pl.when(k > 0)
        def _():
            for m in range(count):
                receive(k - 1, a + m)
            apply(k - 1)

        x = times_winv_t(share[here].reshape(count * size, size)).reshape(count, size, size)
        panel[pl.ds(row_slot(k, a), count)] = x.astype(BF16)
        share[here] = x
        if count == 1:

            @pl.when(jnp.logical_and(near, jnp.logical_and(leads, lax.rem(k + 1, n_row) == LEAD)))
            def _():
                first[...] = panel[row_slot(k, a)]
                first_out(k, start)

        if count == 1:
            source_sends(k, a, start)
        else:
            loop(a, a + count, lambda n: source_sends(k, n, start))
        for m in range(count):
            pltpu.make_async_copy(share.at[spot(a + m, kb)], home(o_ref, a + m, kb), store_sem).start()

    def update_near(p, b):
        update_diag(p, b)
        update_edge(p, b)

    def first_slot(k, dev_row):
        return jnp.where(lax.rem(k + 1, n_row) == dev_row, row_slot(k, (k + 1) // n_row), col_slot(k, (k + 1) // n_col))

    def first_copy(k, dev_row, sem):
        dst = first_slot(k, dev_row)
        return pltpu.make_async_remote_copy(
            src_ref=first, dst_ref=panel.at[dst], send_sem=sem, recv_sem=recv_sem.at[dst],
            device_id=at(dev_row, lax.rem(col + 1, n_col)), device_id_type=MESH,
        )

    def others_first(k, fn):
        urgent = lax.rem(k + 3, n_row)
        lone = urgent == LEAD
        for m in range(n_row - 1):
            fn(m, lax.rem(jnp.where(lone, LEAD + 1, urgent) + m + jnp.where(lax.rem(jnp.where(lone, LEAD + 1, urgent) - LEAD + n_row, n_row) + m >= n_row, 1, 0), n_row))

    def first_out(k, act):
        act(first_copy(k, LEAD, first_sem.at[0, 0]))

        @pl.when(odd == 0)
        def _():
            others_first(k, lambda m, r: act(first_copy(k, r, first_sem.at[0, 1 + m])))

    def first_down(k, act):
        @pl.when(odd == 0)
        def _():
            others_first(k, lambda m, r: act(copy(first_slot(k, LEAD), first_slot(k, r), first_sem.at[1, 1 + m], at(r, col))))

    def firsts_done(k):
        @pl.when(jnp.logical_and(leads, k + 1 < steps))
        def _():
            first_out(k, finish)

        @pl.when(jnp.logical_and(leads, k > 0))
        def _():
            first_down(k - 1, finish)

    @pl.when(col == 0)
    def _():
        prepare(0)
        work[0:size, :] = diag[0]

    def step(k):
        mine = jnp.logical_and(col == lax.rem(k, n_col), k < steps)
        kb = k // n_col
        last = k - 1
        soon = jnp.logical_and(col == lax.rem(k + 1, n_col), k + 1 < steps)

        @pl.when(mine)
        def _():
            with jax.named_scope("factor"):
                factor_block(work, winv, winv3, prev, fac)

            @pl.when(has_edge(kb))
            def _():
                with jax.named_scope("lead"):

                    @pl.when(k == 0)
                    def _():
                        edge_seeded(kb)

                    @pl.when(k > 0)
                    def _():
                        edge_arrived(last, kb)
                        update_edge(last, kb)

                    first[...] = times_winv_t(edge[kb]).astype(BF16)
                    first_out(k, start)

            lo = first_a(k)
            second = jnp.minimum(lo + 1, row_blocks)
            third = second + lax.rem(row_blocks - second, 2)
            with jax.named_scope("solve_near"):
                loop(lo, third, lambda a: solve(k, a, 1))
            with jax.named_scope("solve_two"):
                loop(0, (row_blocks - third) // 2, lambda m: solve(k, third + 2 * m, 2))

        @pl.when(k >= depth)
        def _():
            with jax.named_scope("passed"):
                passed(k - depth)

        @pl.when(mine)
        def _():
            @pl.when(row == lax.rem(k, n_row))
            def _():
                for d in range(1, n_row):
                    seed_copy(kb, lax.rem(row + d, n_row)).wait_send()
                r_id = lax.broadcasted_iota(jnp.int32, (size, size), 0)
                c_id = lax.broadcasted_iota(jnp.int32, (size, size), 1)
                n = spot(k // n_row, kb)
                share[n] = jnp.where(r_id >= c_id, work[0:size, :].T, 0.0)
                pltpu.make_async_copy(share.at[n], home(o_ref, k // n_row, kb), store_sem).start()

        @pl.when(jnp.logical_and(k > 0, jnp.logical_not(jnp.logical_or(mine, soon))))
        def _():
            @pl.when(col != lax.rem(last, n_col))
            def _():
                with jax.named_scope("receive"):
                    end = jnp.where(lead(last) == 3, jnp.minimum(last_near(last) + 1, row_blocks), row_blocks)
                    loop(first_passed(last), end, lambda a: receive_any(last, a))

            near = first_b(k)
            age = k + n_col - (near * n_col + col)
            settle = jnp.logical_and(age == SETTLE, jnp.logical_and(near > 0, near < col_blocks))

            @pl.when(settle)
            def _():
                with jax.named_scope("late_trail"):
                    own = k - SETTLE

                    for back in (LAG + 2, LAG + 1, LAG):

                        @pl.when(own >= back)
                        def _():
                            columns_arrived(own - back, near)

                    loop(jnp.maximum(own - 2 - LAG, 0), own - LAG + 1, lambda p: trail(p, near, -1))

            @pl.when(jnp.logical_and(k >= LAG, lead(last) != 3))
            def _():
                p = k - LAG
                with jax.named_scope("columns"):
                    columns_arrived(p, near)

                with jax.named_scope("trail"):
                    trail(p, near, jnp.where(jnp.logical_or(age > SETTLE, near == 0), near, -1))

            @pl.when(settle)
            def _():
                hand_out(near)

        @pl.when(soon)
        def _():
            nb = (k + 1) // n_col

            oldest = jnp.maximum(k - 1 - LAG, 0)
            lo = first_a(k + 1)

            @pl.when(nb > 0)
            def _():
                with jax.named_scope("seed_late"):
                    seed_arrived(nb)
                    edge_seeded(nb)

            handed = jnp.maximum(k + 1 - n_col + SETTLE - LAG + 1, 0)

            def old_diag(p):
                column_arrived(p, nb)
                edge_arrived(p, nb)
                update_near(p, nb)

            def take(a):
                receive(last, a)

                @pl.when(jnp.logical_not(here_diag(k + 1)))
                def _():
                    loop(oldest, last, lambda p: update_block(p, a, nb))

            @pl.when(k > 0)
            def _():
                with jax.named_scope("older"):
                    loop(handed, oldest, lambda p: update_near(p, nb))
                with jax.named_scope("old_diag"):
                    loop(oldest, last, old_diag)
                with jax.named_scope("take"):
                    loop(first_a(k), jnp.minimum(first_a(k) + 1, row_blocks), take)
                with jax.named_scope("take_column"):
                    column_arrived(last, nb)
                    edge_arrived(last, nb)
                with jax.named_scope("catch_up"):
                    update_near(last, nb)
                    @pl.when(jnp.logical_and(jnp.logical_not(here_diag(k + 1)), lo < row_blocks))
                    def _():
                        update_block(last, lo, nb)

            prepare(nb)
            slot = col_of(k, nb)
            with jax.named_scope("first_block"):
                arrived(slot)

            @pl.when(leads)
            def _():
                first_down(k, start)

            other = panel[slot]
            work[0:size, :] = diag[nb] - times_t(other, other)

        @pl.when(jnp.logical_and(k >= n_col // 2, col == lax.rem(k + n_col // 2, n_col)))
        def _():
            with jax.named_scope("sends_done"):
                firsts_done(k - n_col // 2)
                loop(first_a(k - n_col // 2), row_blocks, lambda a: source_sends(k - n_col // 2, a, finish))

    loop(0, steps + n_col // 2, step)

    def edges_done(b):
        @pl.when(jnp.logical_and(holds_edge(b), jnp.logical_not(leads)))
        def _():
            edge_copy(b).wait_send()

    loop(0, col_blocks, edges_done)
    with jax.named_scope("stored"):
        pltpu.make_async_copy(share, share, store_sem).wait()


def solution(mesh):
    n_row = mesh.shape["row"]
    n_col = mesh.shape["col"]

    def factor_local(a_loc):
        row_blocks, size, local_cols = a_loc.shape
        col_blocks = local_cols // size
        slots = n_row * (row_blocks * (row_blocks + 1) // 2) + n_col * (col_blocks * (col_blocks + 1) // 2)
        slots += 2 * row_blocks * n_row
        return pl.pallas_call(
            functools.partial(kernel, n_row, n_col, "batch"),
            out_shape=jax.ShapeDtypeStruct(a_loc.shape, F32),
            in_specs=[pl.BlockSpec(memory_space=pl.ANY)],
            out_specs=pl.BlockSpec(memory_space=pl.ANY),
            scratch_shapes=[
                pltpu.VMEM((row_blocks * col_blocks, size, size), F32),
                pltpu.VMEM((col_blocks, size, size), F32),
                pltpu.VMEM((col_blocks, size, size), F32),
                pltpu.VMEM((col_blocks, size, size), F32),
                pltpu.VMEM((size, size), BF16),
                pltpu.VMEM((slots, size, size), BF16),
                pltpu.VMEM((size + BASE, size), F32),
                pltpu.VMEM((size + BASE, size), F32),
                pltpu.VMEM((3, size, size), BF16),
                pltpu.VMEM((BASE, 3 * LANE), F32),
                pltpu.VMEM((4 * SUB, SUB, LANE), F32),
                pltpu.SemaphoreType.DMA,
                pltpu.SemaphoreType.DMA,
                pltpu.SemaphoreType.DMA((col_blocks, n_row)),
                pltpu.SemaphoreType.DMA((col_blocks,)),
                pltpu.SemaphoreType.DMA((col_blocks,)),
                pltpu.SemaphoreType.DMA((col_blocks,)),
                pltpu.SemaphoreType.DMA((2, n_row)),
                pltpu.SemaphoreType.DMA((row_blocks, 9)),
                pltpu.SemaphoreType.DMA((4, row_blocks, 6)),
                pltpu.SemaphoreType.DMA((slots,)),
            ],
            compiler_params=pltpu.CompilerParams(
                collective_id=0, has_side_effects=True, vmem_limit_bytes=60 * 1024 * 1024
            ),
            name="cholesky",
        )(a_loc)

    blk_spec = P(("batch", "row"), None, "col")
    return jax.shard_map(factor_local, mesh=mesh, in_specs=(blk_spec,), out_specs=blk_spec, check_vma=False)
```

```python
import functools

import jax
import jax.numpy as jnp
from jax import lax
from jax.experimental import pallas as pl
from jax.experimental.pallas import tpu as pltpu
from jax.sharding import PartitionSpec as P

F32 = jnp.float32
BF16 = jnp.bfloat16
MESH = pl.DeviceIdType.MESH
SUB = 8
LANE = 128
BASE = 16
LEAD = 1
SETTLE = 3
LAG = 3


def sub_bcast(x, q):
    return jnp.broadcast_to(x[q : q + 1, :], (SUB, LANE))


ALONG_LANES = lax.GatherDimensionNumbers(
    offset_dims=(), collapsed_slice_dims=(1,), start_index_map=(1,), operand_batching_dims=(0,), start_indices_batching_dims=(0,)
)


def lane_bcast(x, lane):
    index = jnp.full((SUB, LANE, 1), lane, jnp.int32)
    return lax.gather(x, index, ALONG_LANES, (1, 1), mode=lax.GatherScatterMode.PROMISE_IN_BOUNDS)


def split3(x):
    high = x.astype(BF16)
    rest = x - high.astype(F32)
    mid = rest.astype(BF16)
    return high, mid, (rest - mid.astype(F32)).astype(BF16)


def swap_rows(x, bit, row_id):
    if bit == SUB // 2:
        return pltpu.roll(x, bit, 0)
    return jnp.where((row_id & bit) == 0, pltpu.roll(x, SUB - bit, 0), pltpu.roll(x, bit, 0))


def stack_sums(parts):
    row_id = lax.broadcasted_iota(jnp.int32, (SUB, LANE), 0)
    for bit in (4, 2, 1):
        low = (row_id & bit) == 0
        half = len(parts) // 2
        parts = [
            jnp.where(low, parts[n], parts[n + half]) + swap_rows(jnp.where(low, parts[n + half], parts[n]), bit, row_id)
            for n in range(half)
        ]
    return parts[0]


def eliminate(rows, lane0):
    row_id = lax.broadcasted_iota(jnp.int32, (SUB, LANE), 0)
    rows = [list(rows[0]), list(rows[1])]
    cols = [
        [lane_bcast(rows[0][0], lane0 + j) for j in range(SUB)],
        [lane_bcast(rows[1][0], lane0 + j) for j in range(BASE)],
    ]
    scale = [jnp.zeros((SUB, LANE), F32), jnp.zeros((SUB, LANE), F32)]
    pivot = sub_bcast(cols[0][0], 0)
    for j in range(BASE):
        t, q = divmod(j, SUB)
        inv = lax.rsqrt(pivot)
        scale[t] = jnp.where(row_id == q, inv, scale[t])
        if j + 1 < BASE:
            tn, qn = divmod(j + 1, SUB)
            near = sub_bcast(cols[tn][j], qn) * inv
            pivot = sub_bcast(cols[tn][j + 1], qn) - near * near
        below = cols[1][j] * inv
        here = cols[0][j] * inv if t == 0 else None
        for n in range(j + 1, BASE):
            tn, qn = divmod(n, SUB)
            other = near if n == j + 1 else sub_bcast(here if tn == 0 else below, qn)
            if t == 0 and tn == 0:
                cols[0][n] = cols[0][n] - here * other
            cols[1][n] = cols[1][n] - below * other
        masked = jnp.where(row_id > q, here if t == 0 else below, 0.0)
        for v in range(len(rows[0])):
            pivot_row = sub_bcast(rows[t][v], q) * inv
            rows[t][v] = rows[t][v] - masked * pivot_row
            if t == 0:
                rows[1][v] = rows[1][v] - below * pivot_row
    return [[x * scale[t] for x in rows[t]] for t in range(2)]


def factor_block(work, winv, winv3, prev, fac):
    size = work.shape[1]
    prev[...] = jnp.zeros(prev.shape, F32)
    fac[...] = jnp.zeros(fac.shape, F32)

    def group(v):
        return slice(LANE * v, LANE * (v + 1))

    def pending(factors, before, t, v):
        above, below = before[:SUB, group(v)], before[SUB:, group(v)]
        at = 2 * SUB * t
        return stack_sums([factors[at + n] * above + factors[at + SUB + n] * below for n in range(SUB)])

    for half in range(size // LANE):
        views = [(work, 0), (work, 1), (winv, 0)] if half == 0 else [(work, 1), (winv, 0), (winv, 1)]
        first = half * LANE
        if half == 1:
            factors, before = fac[...], prev[...]
            work[first : first + BASE, group(1)] -= jnp.concatenate([pending(factors, before, t, 1) for t in range(2)], axis=0)
            prev[...] = jnp.concatenate([before[:, group(1)], before[:, group(2)], jnp.zeros((BASE, LANE), F32)], axis=1)

        def body(s, carry, views=views, first=first):
            lane0 = s * BASE
            row0 = pl.multiple_of(first + lane0, BASE)

            here = pl.ds(row0, BASE)
            then = pl.ds(pl.multiple_of(row0 + BASE, BASE), BASE)
            both = [ref[here, group(g)] for ref, g in views]
            rows = [[x[SUB * t : SUB * (t + 1)] for x in both] for t in range(2)]
            factors, before = fac[...], prev[...]
            for t in range(2):
                for v in (1, 2):
                    rows[t][v] = rows[t][v] - pending(factors, before, t, v)
            hi, mid, lo = split3(before)
            lane = lax.broadcasted_iota(jnp.int32, (BASE, size - first), 1) + first
            after = lane >= row0 + BASE
            lhi, lmid, llo = [jnp.where(after, x[:, : size - first], jnp.zeros((), BF16)) for x in (hi, mid, lo)]
            update = lax.dot_general(
                jnp.concatenate([lhi, lhi, lmid, lhi, llo, lmid], axis=0),
                jnp.concatenate([hi, mid, hi, lo, hi, mid], axis=0),
                (((0,), (0,)), ((), ())),
                preferred_element_type=F32,
            )
            for v, (ref, g) in enumerate(views):
                ref[first:size, group(g)] -= update[:, group(v)]
            done = eliminate(rows, lane0)
            if first == 0:
                source = [jnp.where(s == LANE // BASE - 1, done[t][1], done[t][0]) for t in range(2)]
            else:
                source = [done[t][0] for t in range(2)]
            next_lane = (lane0 + BASE) % LANE
            factors, sums = [], []
            for t in range(2):
                factor = [[lane_bcast(source[m], next_lane + SUB * t + n) for n in range(SUB)] for m in range(2)]
                sums.append(stack_sums([factor[0][n] * done[0][0] + factor[1][n] * done[1][0] for n in range(SUB)]))
                factors += factor[0] + factor[1]
            ref, g = views[0]
            ref[then, group(g)] -= jnp.concatenate(sums, axis=0)
            fac[...] = jnp.stack(factors)
            whole = [jnp.concatenate([done[0][v], done[1][v]], axis=0) for v in range(3)]
            prev[...] = jnp.concatenate(whole, axis=1)
            for (ref, g), x in zip(views, whole):
                ref[here, group(g)] = x
                if ref is winv:
                    for n, part in enumerate(split3(x)):
                        winv3[n, here, group(g)] = part
            return carry

        lax.fori_loop(0, LANE // BASE, body, 0)


def kernel(n_row, n_col, batch_axis, a_ref, o_ref, share, diag, edge, stage, first, panel, work, winv, winv3, prev, fac, load_sem, store_sem,
           seed_send, seed_recv, edge_send, edge_recv, first_sem, send_sem, pass_sem, recv_sem):
    row_blocks, size, local_cols = a_ref.shape
    col_blocks = local_cols // size
    ratio = n_col // n_row
    steps = row_blocks * n_row
    depth = pass_sem.shape[0]
    batch = lax.axis_index(batch_axis)
    row = lax.axis_index("row")
    col = lax.axis_index("col")
    odd = lax.rem(col, 2)
    on_diag = lax.rem(col, n_row) == row
    row_slots = n_row * (row_blocks * (row_blocks + 1) // 2)
    edge_slots = row_slots + n_col * (col_blocks * (col_blocks + 1) // 2)
    leads = row == LEAD

    def at(dev_row, dev_col):
        return (batch, dev_row, dev_col)

    def row_slot(k, a):
        g = k // n_row
        return n_row * (row_blocks * g - (g * (g - 1)) // 2) + (k - g * n_row) * (row_blocks - g) + a - g

    def col_slot(k, b):
        h = k // n_col
        return row_slots + n_col * (col_blocks * h - (h * (h - 1)) // 2) + (k - h * n_col) * (col_blocks - h) + b - h

    def first_a(k):
        return (k + n_row - row) // n_row

    def first_b(k):
        return (k + n_col - col) // n_col

    def home(ref, a, b):
        return ref.at[a, :, pl.ds(pl.multiple_of(b * size, size), size)]

    def spot(a, b):
        return b * row_blocks + a

    def col_of(k, b):
        return jnp.where(on_diag, row_slot(k, ratio * b + col // n_row), col_slot(k, b))

    def edge_slot(k, j):
        return edge_slots + 2 * k + (j - k - 1) // n_col

    def edge_reach(ahead):
        return jnp.logical_and(ahead >= 2, jnp.logical_and(ahead <= n_col + LAG - SETTLE, row != LEAD))

    def copy(src_slot, dst_slot, sem, device):
        return pltpu.make_async_remote_copy(
            src_ref=panel.at[src_slot], dst_ref=panel.at[dst_slot], send_sem=sem, recv_sem=recv_sem.at[dst_slot],
            device_id=device, device_id_type=MESH,
        )

    def arrived(slot):
        copy(slot, slot, send_sem.at[0, 0], at(row, col)).wait_recv()

    def start(c):
        c.start()

    def finish(c):
        c.wait_send()

    def from_maker(ahead, way):
        there = lax.rem(row + way, n_row)
        lead_near = jnp.logical_and(there == LEAD, jnp.logical_and(ahead >= 2, ahead <= n_row))
        soon_needed = jnp.logical_and(jnp.logical_and(ahead >= 2, ahead <= n_row), way == 2)
        return jnp.logical_or(lead_near, soon_needed)

    def down_column(k, a, maker, sems, act):
        i = a * n_row + row
        slot = row_slot(k, a)
        dst = col_slot(k, i // n_col)
        for m, way in enumerate((2, 1, n_row - 1)):
            direct = from_maker(i - k, way)

            @pl.when(jnp.where(maker, direct, jnp.logical_not(direct)))
            def _():
                act(copy(slot, dst, sems[m], at(lax.rem(row + way, n_row), lax.rem(i, n_col))))

    def last_near(p):
        return first_a(p + 2)

    def to_edge(k, a, sem, act):
        i = a * n_row + row
        act(copy(row_slot(k, a), edge_slot(k, i - 1), sem, at(LEAD, lax.rem(i - 1, n_col))))

    def source_sends(k, a, act):
        ahead = a * n_row + row - k
        slot = row_slot(k, a)
        early = n_row

        @pl.when(edge_reach(ahead))
        def _():
            to_edge(k, a, send_sem.at[a, 5], act)

        near = jnp.logical_and(ahead >= 2, ahead <= early)

        @pl.when(jnp.logical_or(near, lax.rem(ahead, n_col) == 0))
        def _():
            down_column(k, a, near, [send_sem.at[a, m] for m in range(3)], act)

        @pl.when(jnp.logical_or(jnp.logical_and(odd == 0, ahead >= 2), ahead >= n_col - 1))
        def _():
            act(copy(slot, slot, send_sem.at[a, 3], at(row, lax.rem(jnp.where(odd == 0, col + 1, col - 1), n_col))))

        @pl.when(ahead >= 2)
        def _():
            act(copy(slot, slot, send_sem.at[a, 6], at(row, lax.rem(col - odd + 2, n_col))))

        @pl.when(jnp.logical_and(ahead >= 3 - odd, a <= last_near(k)))
        def _():
            act(copy(slot, slot, send_sem.at[a, 4], at(row, lax.rem(col - odd + 3, n_col))))

        @pl.when(jnp.logical_and(ahead >= n_col // 2 - odd, ahead < n_col - 2 - odd))
        def _():
            act(copy(slot, slot, send_sem.at[a, 7], at(row, lax.rem(col - odd + 5, n_col))))

        @pl.when(ahead >= n_col - 2 - odd)
        def _():
            act(copy(slot, slot, send_sem.at[a, 8], at(row, lax.rem(col - odd - 2 + n_col, n_col))))

    def lead(p):
        return lax.rem(col - lax.rem(p, n_col) + n_col, n_col)

    def hops(p):
        return lax.rem(col // 2 - lax.rem(p, n_col) // 2 + n_col // 2, n_col // 2)

    def passes(p):
        return jnp.where(odd == 1, 2, n_col // 2 - 1) == hops(p)

    def first_passed(p):
        low = jnp.where(jnp.logical_and(passes(p), odd == 1), lead(p) - 1, lead(p))
        return (p + low - row + n_row - 1) // n_row

    def pass_down(p, a, act):
        i = a * n_row + row
        ahead = i - p
        sems = pass_sem.at[lax.rem(p, depth), a]

        @pl.when(jnp.logical_and(odd == 0, jnp.logical_and(lead(p) <= 2, a > last_near(p))))
        def _():
            act(copy(row_slot(p, a), row_slot(p, a), sems.at[3], at(row, col + 1)))

        @pl.when(jnp.logical_and(lax.rem(i, n_col) == col, ahead > 1))
        def _():
            down_column(p, a, False, [sems.at[m] for m in range(3)], act)

    def pass_on(p, a, act):
        slot = row_slot(p, a)
        sems = pass_sem.at[lax.rem(p, depth), a]

        @pl.when(passes(p))
        def _():
            @pl.when(odd == 0)
            def _():
                act(copy(slot, slot, sems.at[4], at(row, lax.rem(col - 1 + n_col, n_col))))

            @pl.when(jnp.logical_or(odd == 1, a * n_row + row > p + lead(p)))
            def _():
                act(copy(slot, slot, sems.at[3], at(row, col + 1 - 2 * odd)))

        pass_down(p, a, act)

    def passed(p):
        @pl.when(lead(p) != 0)
        def _():
            loop(first_passed(p), row_blocks, lambda a: pass_on(p, a, finish))

    def receive(p, a):
        arrived(row_slot(p, a))
        pass_down(p, a, start)

    def receive_any(p, a):
        arrived(row_slot(p, a))
        pass_on(p, a, start)

    def loop(lo, hi, fn):
        lax.fori_loop(lo, hi, lambda n, c: (fn(n), c)[1], 0)

    for a in range(row_blocks):
        for b in range(col_blocks):
            pltpu.make_async_copy(home(a_ref, a, b), share.at[spot(a, b)], load_sem).start()

    barrier = pltpu.get_barrier_semaphore()
    n_dev = n_row * n_col

    def greet(n):
        other = lax.rem(row * n_col + col + n, n_dev)
        pl.semaphore_signal(barrier, inc=1, device_id=at(other // n_col, lax.rem(other, n_col)), device_id_type=MESH)

    loop(1, n_dev, greet)
    with jax.named_scope("all_here"):
        pl.semaphore_wait(barrier, n_dev - 1)
    with jax.named_scope("loaded"):
        pltpu.make_async_copy(share, share, load_sem).wait()

    def seed_copy(b, dev_row):
        return pltpu.make_async_remote_copy(
            src_ref=share.at[spot(ratio * b + col // n_row, b)], dst_ref=diag.at[b],
            send_sem=seed_send.at[b, lax.rem(dev_row - row + n_row, n_row)],
            recv_sem=seed_recv.at[b], device_id=at(dev_row, col), device_id_type=MESH,
        )

    def hand_out(b):
        @pl.when(on_diag)
        def _():
            for d in (1, n_row - 1, 2):
                seed_copy(b, lax.rem(row + d, n_row)).start()
            diag[b] = share[spot(ratio * b + col // n_row, b)]

        @pl.when(jnp.logical_and(holds_edge(b), jnp.logical_not(leads)))
        def _():
            stage[b] = share[spot((b * n_col + col + 1) // n_row, b)]
            edge_copy(b).start()

    def holds_edge(b):
        j = b * n_col + col
        return jnp.logical_and(lax.rem(j + 1, n_row) == row, j + 1 < steps)

    def edge_copy(b):
        return pltpu.make_async_remote_copy(
            src_ref=stage.at[b], dst_ref=edge.at[b], send_sem=edge_send.at[b], recv_sem=edge_recv.at[b],
            device_id=at(LEAD, col), device_id_type=MESH,
        )

    def has_edge(b):
        from_other = jnp.logical_and(leads, lax.rem(col + 1, n_row) != LEAD)
        return jnp.logical_and(from_other, b * n_col + col + 1 < steps)

    def edge_seeded(b):
        @pl.when(has_edge(b))
        def _():
            edge_copy(b).wait_recv()

    def edge_arrived(p, b):
        j = b * n_col + col

        @pl.when(jnp.logical_and(has_edge(b), j + 1 - p <= n_col + LAG - SETTLE))
        def _():
            arrived(edge_slot(p, j))

    hand_out(0)
    winv3[...] = jnp.zeros(winv3.shape, BF16)

    def seed_arrived(b):
        @pl.when(jnp.logical_not(on_diag))
        def _():
            seed_copy(b, row).wait_recv()

    with jax.named_scope("seed"):
        seed_arrived(0)

        @pl.when(col != 0)
        def _():
            edge_seeded(0)

    def clear(n):
        a, b = lax.rem(n, row_blocks), n // row_blocks

        @pl.when(a * n_row + row < b * n_col + col)
        def _():
            share[n] = jnp.zeros((size, size), F32)
            pltpu.make_async_copy(share.at[n], home(o_ref, a, b), store_sem).start()

    loop(0, row_blocks * col_blocks, clear)

    def times_t(x, y):
        return lax.dot_general(x, y, (((1,), (1,)), ((), ())), preferred_element_type=F32)

    def update_block(p, a, b):
        share[spot(a, b)] -= times_t(panel[row_slot(p, a)], panel[col_of(p, b)])

    def update_diag(p, b):
        other = panel[col_of(p, b)]
        diag[b] -= times_t(other, other)

    def update_edge(p, b):
        @pl.when(has_edge(b))
        def _():
            edge[b] -= times_t(panel[edge_slot(p, b * n_col + col)], panel[col_of(p, b)])

    def column_arrived(p, b):
        @pl.when(jnp.logical_not(on_diag))
        def _():
            arrived(col_slot(p, b))

    def update_column(p, b, lo):
        lone = lax.rem(row_blocks - lo, 2)

        @pl.when(lone == 1)
        def _():
            update_block(p, lo, b)

        def pair(m):
            a = lo + lone + 2 * m
            both = pl.ds(spot(a, b), 2)
            left = panel[pl.ds(row_slot(p, a), 2)].reshape(2 * size, size)
            share[both] -= times_t(left, panel[col_of(p, b)]).reshape(2, size, size)

        loop(0, (row_blocks - lo) // 2, pair)

    def trail(p, b_from, near):
        loop(b_from, col_blocks, lambda b: update_column(p, b, first_a(b * n_col + col - jnp.where(b == near, 0, 1))))

    def columns_arrived(p, b_from):
        def one(b):
            column_arrived(p, b)
            edge_arrived(p, b)

        loop(b_from, col_blocks, one)

    def prepare(b):
        work[size:, :] = jnp.zeros((BASE, size), F32)
        r_id = lax.broadcasted_iota(jnp.int32, (size + BASE, size), 0)
        c_id = lax.broadcasted_iota(jnp.int32, (size + BASE, size), 1)
        winv[...] = jnp.where(r_id == c_id, 1.0, 0.0).astype(F32)

    def times_winv_t(x):
        hi, mid, lo = split3(x)
        whi, wmid, wlo = winv3[0], winv3[1], winv3[2]
        small = times_t(lo, whi) + times_t(mid, wmid) + times_t(hi, wlo)
        return small + (times_t(mid, whi) + times_t(hi, wmid)) + times_t(hi, whi)

    def here_diag(k):
        return row == lax.rem(k, n_row)

    def solve(k, a, count):
        kb = k // n_col
        near = jnp.logical_and(a == first_a(k), jnp.logical_not(here_diag(k)))
        here = pl.ds(spot(a, kb), count)

        def apply(p):
            left = panel[pl.ds(row_slot(p, a), count)].reshape(count * size, size)
            share[here] -= times_t(left, panel[col_of(p, kb)]).reshape(count, size, size)

        @pl.when(jnp.logical_not(near))
        def _():
            for m in range(count):

                @pl.when(k >= 3)
                def _():
                    receive(k - 3, a + m)

                @pl.when(k >= 2)
                def _():
                    receive(k - 2, a + m)

            loop(jnp.maximum(k - 2 - LAG, 0), k - 1, apply)

        @pl.when(k > 0)
        def _():
            for m in range(count):
                receive(k - 1, a + m)
            apply(k - 1)

        x = times_winv_t(share[here].reshape(count * size, size)).reshape(count, size, size)
        panel[pl.ds(row_slot(k, a), count)] = x.astype(BF16)
        share[here] = x
        if count == 1:

            @pl.when(jnp.logical_and(near, jnp.logical_and(leads, lax.rem(k + 1, n_row) == LEAD)))
            def _():
                first[...] = panel[row_slot(k, a)]
                first_out(k, start)

        if count == 1:
            source_sends(k, a, start)
        else:
            loop(a, a + count, lambda n: source_sends(k, n, start))
        for m in range(count):
            pltpu.make_async_copy(share.at[spot(a + m, kb)], home(o_ref, a + m, kb), store_sem).start()

    def update_near(p, b):
        update_diag(p, b)
        update_edge(p, b)

    def first_slot(k, dev_row):
        return jnp.where(lax.rem(k + 1, n_row) == dev_row, row_slot(k, (k + 1) // n_row), col_slot(k, (k + 1) // n_col))

    def first_copy(k, dev_row, sem):
        dst = first_slot(k, dev_row)
        return pltpu.make_async_remote_copy(
            src_ref=first, dst_ref=panel.at[dst], send_sem=sem, recv_sem=recv_sem.at[dst],
            device_id=at(dev_row, lax.rem(col + 1, n_col)), device_id_type=MESH,
        )

    def others_first(k, fn):
        urgent = lax.rem(k + 3, n_row)
        lone = urgent == LEAD
        for m in range(n_row - 1):
            fn(m, lax.rem(jnp.where(lone, LEAD + 1, urgent) + m + jnp.where(lax.rem(jnp.where(lone, LEAD + 1, urgent) - LEAD + n_row, n_row) + m >= n_row, 1, 0), n_row))

    def first_out(k, act):
        act(first_copy(k, LEAD, first_sem.at[0, 0]))

        @pl.when(odd == 0)
        def _():
            others_first(k, lambda m, r: act(first_copy(k, r, first_sem.at[0, 1 + m])))

    def first_down(k, act):
        @pl.when(odd == 0)
        def _():
            others_first(k, lambda m, r: act(copy(first_slot(k, LEAD), first_slot(k, r), first_sem.at[1, 1 + m], at(r, col))))

    def firsts_done(k):
        @pl.when(jnp.logical_and(leads, k + 1 < steps))
        def _():
            first_out(k, finish)

        @pl.when(jnp.logical_and(leads, k > 0))
        def _():
            first_down(k - 1, finish)

    @pl.when(col == 0)
    def _():
        prepare(0)
        work[0:size, :] = diag[0]

    def step(k):
        mine = jnp.logical_and(col == lax.rem(k, n_col), k < steps)
        kb = k // n_col
        last = k - 1
        soon = jnp.logical_and(col == lax.rem(k + 1, n_col), k + 1 < steps)

        @pl.when(mine)
        def _():
            with jax.named_scope("factor"):
                factor_block(work, winv, winv3, prev, fac)

            @pl.when(has_edge(kb))
            def _():
                with jax.named_scope("lead"):

                    @pl.when(k == 0)
                    def _():
                        edge_seeded(kb)

                    @pl.when(k > 0)
                    def _():
                        edge_arrived(last, kb)
                        update_edge(last, kb)

                    first[...] = times_winv_t(edge[kb]).astype(BF16)
                    first_out(k, start)

            lo = first_a(k)
            second = jnp.minimum(lo + 1, row_blocks)
            third = second + lax.rem(row_blocks - second, 2)
            with jax.named_scope("solve_near"):
                loop(lo, third, lambda a: solve(k, a, 1))
            with jax.named_scope("solve_two"):
                loop(0, (row_blocks - third) // 2, lambda m: solve(k, third + 2 * m, 2))

        @pl.when(k >= depth)
        def _():
            with jax.named_scope("passed"):
                passed(k - depth)

        @pl.when(mine)
        def _():
            @pl.when(row == lax.rem(k, n_row))
            def _():
                for d in range(1, n_row):
                    seed_copy(kb, lax.rem(row + d, n_row)).wait_send()
                r_id = lax.broadcasted_iota(jnp.int32, (size, size), 0)
                c_id = lax.broadcasted_iota(jnp.int32, (size, size), 1)
                n = spot(k // n_row, kb)
                share[n] = jnp.where(r_id >= c_id, work[0:size, :].T, 0.0)
                pltpu.make_async_copy(share.at[n], home(o_ref, k // n_row, kb), store_sem).start()

        @pl.when(jnp.logical_and(k > 0, jnp.logical_not(jnp.logical_or(mine, soon))))
        def _():
            @pl.when(col != lax.rem(last, n_col))
            def _():
                with jax.named_scope("receive"):
                    end = jnp.where(lead(last) == 3, jnp.minimum(last_near(last) + 1, row_blocks), row_blocks)
                    loop(first_passed(last), end, lambda a: receive_any(last, a))

            near = first_b(k)
            age = k + n_col - (near * n_col + col)
            settle = jnp.logical_and(age == SETTLE, jnp.logical_and(near > 0, near < col_blocks))

            @pl.when(settle)
            def _():
                with jax.named_scope("late_trail"):
                    own = k - SETTLE

                    for back in (LAG + 2, LAG + 1, LAG):

                        @pl.when(own >= back)
                        def _():
                            columns_arrived(own - back, near)

                    loop(jnp.maximum(own - 2 - LAG, 0), own - LAG + 1, lambda p: trail(p, near, -1))

            @pl.when(jnp.logical_and(k >= LAG, lead(last) != 3))
            def _():
                p = k - LAG
                with jax.named_scope("columns"):
                    columns_arrived(p, near)

                with jax.named_scope("trail"):
                    trail(p, near, jnp.where(jnp.logical_or(age > SETTLE, near == 0), near, -1))

            @pl.when(settle)
            def _():
                hand_out(near)

        @pl.when(soon)
        def _():
            nb = (k + 1) // n_col

            oldest = jnp.maximum(k - 1 - LAG, 0)
            lo = first_a(k + 1)

            @pl.when(nb > 0)
            def _():
                with jax.named_scope("seed_late"):
                    seed_arrived(nb)
                    edge_seeded(nb)

            handed = jnp.maximum(k + 1 - n_col + SETTLE - LAG + 1, 0)

            def old_diag(p):
                column_arrived(p, nb)
                edge_arrived(p, nb)
                update_near(p, nb)

            def take(a):
                receive(last, a)

                @pl.when(jnp.logical_not(here_diag(k + 1)))
                def _():
                    loop(oldest, last, lambda p: update_block(p, a, nb))

            @pl.when(k > 0)
            def _():
                with jax.named_scope("older"):
                    loop(handed, oldest, lambda p: update_near(p, nb))
                with jax.named_scope("old_diag"):
                    loop(oldest, last, old_diag)
                with jax.named_scope("take"):
                    loop(first_a(k), jnp.minimum(first_a(k) + 1, row_blocks), take)
                with jax.named_scope("take_column"):
                    column_arrived(last, nb)
                    edge_arrived(last, nb)
                with jax.named_scope("catch_up"):
                    update_near(last, nb)
                    @pl.when(jnp.logical_and(jnp.logical_not(here_diag(k + 1)), lo < row_blocks))
                    def _():
                        update_block(last, lo, nb)

            prepare(nb)
            slot = col_of(k, nb)
            with jax.named_scope("first_block"):
                arrived(slot)

            @pl.when(leads)
            def _():
                first_down(k, start)

            other = panel[slot]
            work[0:size, :] = diag[nb] - times_t(other, other)

        @pl.when(jnp.logical_and(k >= n_col // 2, col == lax.rem(k + n_col // 2, n_col)))
        def _():
            with jax.named_scope("sends_done"):
                firsts_done(k - n_col // 2)
                loop(first_a(k - n_col // 2), row_blocks, lambda a: source_sends(k - n_col // 2, a, finish))

    loop(0, steps + n_col // 2, step)

    def edges_done(b):
        @pl.when(jnp.logical_and(holds_edge(b), jnp.logical_not(leads)))
        def _():
            edge_copy(b).wait_send()

    loop(0, col_blocks, edges_done)
    with jax.named_scope("stored"):
        pltpu.make_async_copy(share, share, store_sem).wait()


def solution(mesh):
    n_row = mesh.shape["row"]
    n_col = mesh.shape["col"]

    def factor_local(a_loc):
        row_blocks, size, local_cols = a_loc.shape
        col_blocks = local_cols // size
        slots = n_row * (row_blocks * (row_blocks + 1) // 2) + n_col * (col_blocks * (col_blocks + 1) // 2)
        slots += 2 * row_blocks * n_row
        return pl.pallas_call(
            functools.partial(kernel, n_row, n_col, "batch"),
            out_shape=jax.ShapeDtypeStruct(a_loc.shape, F32),
            in_specs=[pl.BlockSpec(memory_space=pl.ANY)],
            out_specs=pl.BlockSpec(memory_space=pl.ANY),
            scratch_shapes=[
                pltpu.VMEM((row_blocks * col_blocks, size, size), F32),
                pltpu.VMEM((col_blocks, size, size), F32),
                pltpu.VMEM((col_blocks, size, size), F32),
                pltpu.VMEM((col_blocks, size, size), F32),
                pltpu.VMEM((size, size), BF16),
                pltpu.VMEM((slots, size, size), BF16),
                pltpu.VMEM((size + BASE, size), F32),
                pltpu.VMEM((size + BASE, size), F32),
                pltpu.VMEM((3, size, size), BF16),
                pltpu.VMEM((BASE, 3 * LANE), F32),
                pltpu.VMEM((4 * SUB, SUB, LANE), F32),
                pltpu.SemaphoreType.DMA,
                pltpu.SemaphoreType.DMA,
                pltpu.SemaphoreType.DMA((col_blocks, n_row)),
                pltpu.SemaphoreType.DMA((col_blocks,)),
                pltpu.SemaphoreType.DMA((col_blocks,)),
                pltpu.SemaphoreType.DMA((col_blocks,)),
                pltpu.SemaphoreType.DMA((2, n_row)),
                pltpu.SemaphoreType.DMA((row_blocks, 9)),
                pltpu.SemaphoreType.DMA((4, row_blocks, 6)),
                pltpu.SemaphoreType.DMA((slots,)),
            ],
            compiler_params=pltpu.CompilerParams(
                collective_id=0, has_side_effects=True, vmem_limit_bytes=60 * 1024 * 1024
            ),
            name="cholesky",
        )(a_loc)

    blk_spec = P(("batch", "row"), None, "col")
    return jax.shard_map(factor_local, mesh=mesh, in_specs=(blk_spec,), out_specs=blk_spec, check_vma=False)
```

```python
import functools

import jax
import jax.numpy as jnp
from jax import lax
from jax.experimental import pallas as pl
from jax.experimental.pallas import tpu as pltpu
from jax.sharding import PartitionSpec as P

F32 = jnp.float32
BF16 = jnp.bfloat16
MESH = pl.DeviceIdType.MESH
SUB = 8
LANE = 128
BASE = 16
LEAD = 1
SETTLE = 3
LAG = 3


def sub_bcast(x, q):
    return jnp.broadcast_to(x[q : q + 1, :], (SUB, LANE))


ALONG_LANES = lax.GatherDimensionNumbers(
    offset_dims=(), collapsed_slice_dims=(1,), start_index_map=(1,), operand_batching_dims=(0,), start_indices_batching_dims=(0,)
)


def lane_bcast(x, lane):
    index = jnp.full((SUB, LANE, 1), lane, jnp.int32)
    return lax.gather(x, index, ALONG_LANES, (1, 1), mode=lax.GatherScatterMode.PROMISE_IN_BOUNDS)


def split3(x):
    high = x.astype(BF16)
    rest = x - high.astype(F32)
    mid = rest.astype(BF16)
    return high, mid, (rest - mid.astype(F32)).astype(BF16)


def swap_rows(x, bit, row_id):
    if bit == SUB // 2:
        return pltpu.roll(x, bit, 0)
    return jnp.where((row_id & bit) == 0, pltpu.roll(x, SUB - bit, 0), pltpu.roll(x, bit, 0))


def stack_sums(parts):
    row_id = lax.broadcasted_iota(jnp.int32, (SUB, LANE), 0)
    for bit in (4, 2, 1):
        low = (row_id & bit) == 0
        half = len(parts) // 2
        parts = [
            jnp.where(low, parts[n], parts[n + half]) + swap_rows(jnp.where(low, parts[n + half], parts[n]), bit, row_id)
            for n in range(half)
        ]
    return parts[0]


def eliminate(rows, lane0):
    row_id = lax.broadcasted_iota(jnp.int32, (SUB, LANE), 0)
    rows = [list(rows[0]), list(rows[1])]
    cols = [
        [lane_bcast(rows[0][0], lane0 + j) for j in range(SUB)],
        [lane_bcast(rows[1][0], lane0 + j) for j in range(BASE)],
    ]
    scale = [jnp.zeros((SUB, LANE), F32), jnp.zeros((SUB, LANE), F32)]
    pivot = sub_bcast(cols[0][0], 0)
    for j in range(BASE):
        t, q = divmod(j, SUB)
        inv = lax.rsqrt(pivot)
        scale[t] = jnp.where(row_id == q, inv, scale[t])
        if j + 1 < BASE:
            tn, qn = divmod(j + 1, SUB)
            near = sub_bcast(cols[tn][j], qn) * inv
            pivot = sub_bcast(cols[tn][j + 1], qn) - near * near
        below = cols[1][j] * inv
        here = cols[0][j] * inv if t == 0 else None
        for n in range(j + 1, BASE):
            tn, qn = divmod(n, SUB)
            other = near if n == j + 1 else sub_bcast(here if tn == 0 else below, qn)
            if t == 0 and tn == 0:
                cols[0][n] = cols[0][n] - here * other
            cols[1][n] = cols[1][n] - below * other
        masked = jnp.where(row_id > q, here if t == 0 else below, 0.0)
        for v in range(len(rows[0])):
            pivot_row = sub_bcast(rows[t][v], q) * inv
            rows[t][v] = rows[t][v] - masked * pivot_row
            if t == 0:
                rows[1][v] = rows[1][v] - below * pivot_row
    return [[x * scale[t] for x in rows[t]] for t in range(2)]


def factor_block(work, winv, winv3, prev, fac):
    size = work.shape[1]
    prev[...] = jnp.zeros(prev.shape, F32)
    fac[...] = jnp.zeros(fac.shape, F32)

    def group(v):
        return slice(LANE * v, LANE * (v + 1))

    def pending(factors, before, t, v):
        above, below = before[:SUB, group(v)], before[SUB:, group(v)]
        at = 2 * SUB * t
        return stack_sums([factors[at + n] * above + factors[at + SUB + n] * below for n in range(SUB)])

    for half in range(size // LANE):
        views = [(work, 0), (work, 1), (winv, 0)] if half == 0 else [(work, 1), (winv, 0), (winv, 1)]
        first = half * LANE
        if half == 1:
            factors, before = fac[...], prev[...]
            work[first : first + BASE, group(1)] -= jnp.concatenate([pending(factors, before, t, 1) for t in range(2)], axis=0)
            prev[...] = jnp.concatenate([before[:, group(1)], before[:, group(2)], jnp.zeros((BASE, LANE), F32)], axis=1)

        def body(s, carry, views=views, first=first):
            lane0 = s * BASE
            row0 = pl.multiple_of(first + lane0, BASE)

            here = pl.ds(row0, BASE)
            then = pl.ds(pl.multiple_of(row0 + BASE, BASE), BASE)
            both = [ref[here, group(g)] for ref, g in views]
            rows = [[x[SUB * t : SUB * (t + 1)] for x in both] for t in range(2)]
            factors, before = fac[...], prev[...]
            for t in range(2):
                for v in (1, 2):
                    rows[t][v] = rows[t][v] - pending(factors, before, t, v)
            hi, mid, lo = split3(before)
            lane = lax.broadcasted_iota(jnp.int32, (BASE, size - first), 1) + first
            after = lane >= row0 + BASE
            lhi, lmid, llo = [jnp.where(after, x[:, : size - first], jnp.zeros((), BF16)) for x in (hi, mid, lo)]
            update = lax.dot_general(
                jnp.concatenate([lhi, lhi, lmid, lhi, llo, lmid], axis=0),
                jnp.concatenate([hi, mid, hi, lo, hi, mid], axis=0),
                (((0,), (0,)), ((), ())),
                preferred_element_type=F32,
            )
            for v, (ref, g) in enumerate(views):
                ref[first:size, group(g)] -= update[:, group(v)]
            done = eliminate(rows, lane0)
            if first == 0:
                source = [jnp.where(s == LANE // BASE - 1, done[t][1], done[t][0]) for t in range(2)]
            else:
                source = [done[t][0] for t in range(2)]
            next_lane = (lane0 + BASE) % LANE
            factors, sums = [], []
            for t in range(2):
                factor = [[lane_bcast(source[m], next_lane + SUB * t + n) for n in range(SUB)] for m in range(2)]
                sums.append(stack_sums([factor[0][n] * done[0][0] + factor[1][n] * done[1][0] for n in range(SUB)]))
                factors += factor[0] + factor[1]
            ref, g = views[0]
            ref[then, group(g)] -= jnp.concatenate(sums, axis=0)
            fac[...] = jnp.stack(factors)
            whole = [jnp.concatenate([done[0][v], done[1][v]], axis=0) for v in range(3)]
            prev[...] = jnp.concatenate(whole, axis=1)
            for (ref, g), x in zip(views, whole):
                ref[here, group(g)] = x
                if ref is winv:
                    for n, part in enumerate(split3(x)):
                        winv3[n, here, group(g)] = part
            return carry

        lax.fori_loop(0, LANE // BASE, body, 0)


def kernel(n_row, n_col, batch_axis, a_ref, share, diag, edge, stage, first, panel, work, winv, winv3, prev, fac, load_sem,
           seed_send, seed_recv, edge_send, edge_recv, first_sem, send_sem, pass_sem, down_sem, recv_sem):
    row_blocks, size, local_cols = a_ref.shape
    col_blocks = local_cols // size
    ratio = n_col // n_row
    steps = row_blocks * n_row
    depth = pass_sem.shape[0]
    batch = lax.axis_index(batch_axis)
    row = lax.axis_index("row")
    col = lax.axis_index("col")
    odd = lax.rem(col, 2)
    on_diag = lax.rem(col, n_row) == row
    row_slots = n_row * (row_blocks * (row_blocks + 1) // 2)
    edge_slots = row_slots + n_col * (col_blocks * (col_blocks + 1) // 2)
    leads = row == LEAD

    def at(dev_row, dev_col):
        return (batch, dev_row, dev_col)

    def row_slot(k, a):
        g = k // n_row
        return n_row * (row_blocks * g - (g * (g - 1)) // 2) + (k - g * n_row) * (row_blocks - g) + a - g

    def col_slot(k, b):
        h = k // n_col
        return row_slots + n_col * (col_blocks * h - (h * (h - 1)) // 2) + (k - h * n_col) * (col_blocks - h) + b - h

    def first_a(k):
        return (k + n_row - row) // n_row

    def first_b(k):
        return (k + n_col - col) // n_col

    def spot(a, b, count=1):
        return (a if count == 1 else pl.ds(a, count), slice(None), pl.ds(pl.multiple_of(b * size, size), size))

    def col_of(k, b):
        return jnp.where(on_diag, row_slot(k, ratio * b + col // n_row), col_slot(k, b))

    def edge_slot(k):
        return edge_slots + k

    def edge_reach(ahead):
        return jnp.logical_and(ahead >= 2, jnp.logical_and(ahead <= n_col + LAG - SETTLE, row != LEAD))

    def copy(src_slot, dst_slot, sem, device):
        return pltpu.make_async_remote_copy(
            src_ref=panel.at[src_slot], dst_ref=panel.at[dst_slot], send_sem=sem, recv_sem=recv_sem.at[dst_slot],
            device_id=device, device_id_type=MESH,
        )

    def arrived(slot):
        copy(slot, slot, send_sem.at[0, 0], at(row, col)).wait_recv()

    def start(c):
        c.start()

    def finish(c):
        c.wait_send()

    def from_maker(ahead, way):
        there = lax.rem(row + way, n_row)
        lead_near = jnp.logical_and(there == LEAD, jnp.logical_and(ahead >= 2, ahead <= n_row))
        soon_needed = jnp.logical_and(ahead == 2, way == 2)
        return jnp.logical_or(lead_near, soon_needed)

    def down_column(k, a, maker, sems, act):
        i = a * n_row + row
        slot = row_slot(k, a)
        dst = col_slot(k, i // n_col)
        for m, way in enumerate((1, n_row - 1, 2)):
            direct = from_maker(i - k, way)

            @pl.when(jnp.where(maker, direct, jnp.logical_not(direct)))
            def _():
                act(copy(slot, dst, sems[m], at(lax.rem(row + way, n_row), lax.rem(i, n_col))))

    def last_near(p):
        return first_a(p + 2)

    def to_edge(k, a, sem, act):
        i = a * n_row + row
        act(copy(row_slot(k, a), edge_slot(k), sem, at(LEAD, lax.rem(i - 1, n_col))))

    def source_sends(k, a, act):
        ahead = a * n_row + row - k
        slot = row_slot(k, a)
        early = n_row

        @pl.when(edge_reach(ahead))
        def _():
            to_edge(k, a, send_sem.at[a, 5], act)

        near = jnp.logical_and(ahead >= 2, ahead <= early)

        @pl.when(jnp.logical_or(near, lax.rem(ahead, n_col) == 0))
        def _():
            down_column(k, a, near, [send_sem.at[a, m] for m in range(3)], act)

        @pl.when(jnp.logical_or(jnp.logical_and(odd == 0, ahead >= 2), ahead >= n_col - 1))
        def _():
            act(copy(slot, slot, send_sem.at[a, 3], at(row, lax.rem(jnp.where(odd == 0, col + 1, col - 1), n_col))))

        @pl.when(ahead >= 2)
        def _():
            act(copy(slot, slot, send_sem.at[a, 6], at(row, lax.rem(col - odd + 2, n_col))))

        @pl.when(jnp.logical_and(ahead >= 3 - odd, a <= last_near(k)))
        def _():
            act(copy(slot, slot, send_sem.at[a, 4], at(row, lax.rem(col - odd + 3, n_col))))

        @pl.when(jnp.logical_and(ahead >= n_col // 2 - odd, ahead < n_col - 2 - odd))
        def _():
            act(copy(slot, slot, send_sem.at[a, 7], at(row, lax.rem(col - odd + 5, n_col))))

        @pl.when(ahead >= n_col - 2 - odd)
        def _():
            act(copy(slot, slot, send_sem.at[a, 8], at(row, lax.rem(col - odd - 2 + n_col, n_col))))

    def lead(p):
        return lax.rem(col - lax.rem(p, n_col) + n_col, n_col)

    def hops(p):
        return lax.rem(col // 2 - lax.rem(p, n_col) // 2 + n_col // 2, n_col // 2)

    def passes(p):
        return jnp.where(odd == 1, 2, n_col // 2 - 1) == hops(p)

    def first_passed(p):
        low = jnp.where(jnp.logical_and(passes(p), odd == 1), lead(p) - 1, lead(p))
        return (p + low - row + n_row - 1) // n_row

    def pass_down(p, a, act):
        i = a * n_row + row
        ahead = i - p
        sems = pass_sem.at[lax.rem(p, depth), a]

        @pl.when(jnp.logical_and(odd == 0, jnp.logical_and(lead(p) <= 2, a > last_near(p))))
        def _():
            act(copy(row_slot(p, a), row_slot(p, a), sems.at[0], at(row, col + 1)))

        @pl.when(jnp.logical_and(lax.rem(i, n_col) == col, ahead > 1))
        def _():
            downs = down_sem.at[lax.rem(p, depth), i // n_col]
            down_column(p, a, False, [downs.at[m] for m in range(3)], act)

    def pass_on(p, a, act):
        slot = row_slot(p, a)
        sems = pass_sem.at[lax.rem(p, depth), a]

        @pl.when(passes(p))
        def _():
            @pl.when(odd == 0)
            def _():
                act(copy(slot, slot, sems.at[1], at(row, lax.rem(col - 1 + n_col, n_col))))

            @pl.when(jnp.logical_or(odd == 1, a * n_row + row > p + lead(p)))
            def _():
                act(copy(slot, slot, sems.at[0], at(row, col + 1 - 2 * odd)))

        pass_down(p, a, act)

    def passed(p):
        @pl.when(lead(p) != 0)
        def _():
            loop(first_passed(p), row_blocks, lambda a: pass_on(p, a, finish))

    def receive(p, a):
        arrived(row_slot(p, a))
        pass_down(p, a, start)

    def receive_any(p, a):
        arrived(row_slot(p, a))
        pass_on(p, a, start)

    def loop(lo, hi, fn):
        lax.fori_loop(lo, hi, lambda n, c: (fn(n), c)[1], 0)

    load = pltpu.make_async_copy(a_ref, share, load_sem)
    load.start()

    barrier = pltpu.get_barrier_semaphore()
    n_dev = n_row * n_col

    def greet(n):
        other = lax.rem(row * n_col + col + n, n_dev)
        pl.semaphore_signal(barrier, inc=1, device_id=at(other // n_col, lax.rem(other, n_col)), device_id_type=MESH)

    loop(1, n_dev, greet)
    with jax.named_scope("all_here"):
        pl.semaphore_wait(barrier, n_dev - 1)
    with jax.named_scope("loaded"):
        load.wait()

    def seed_copy(b, dev_row):
        return pltpu.make_async_remote_copy(
            src_ref=share.at[spot(ratio * b + col // n_row, b)], dst_ref=diag.at[b],
            send_sem=seed_send.at[b, lax.rem(dev_row - row + n_row, n_row)],
            recv_sem=seed_recv.at[b], device_id=at(dev_row, col), device_id_type=MESH,
        )

    def hand_out(b):
        @pl.when(on_diag)
        def _():
            for d in (1, n_row - 1, 2):
                seed_copy(b, lax.rem(row + d, n_row)).start()
            diag[b] = share[spot(ratio * b + col // n_row, b)]

        @pl.when(jnp.logical_and(holds_edge(b), jnp.logical_not(leads)))
        def _():
            stage[b] = share[spot((b * n_col + col + 1) // n_row, b)]
            edge_copy(b).start()

    def holds_edge(b):
        j = b * n_col + col
        return jnp.logical_and(lax.rem(j + 1, n_row) == row, j + 1 < steps)

    def edge_copy(b):
        return pltpu.make_async_remote_copy(
            src_ref=stage.at[b], dst_ref=edge.at[b], send_sem=edge_send.at[b], recv_sem=edge_recv.at[b],
            device_id=at(LEAD, col), device_id_type=MESH,
        )

    def has_edge(b):
        from_other = jnp.logical_and(leads, lax.rem(col + 1, n_row) != LEAD)
        return jnp.logical_and(from_other, b * n_col + col + 1 < steps)

    def edge_seeded(b):
        @pl.when(has_edge(b))
        def _():
            edge_copy(b).wait_recv()

    def edge_arrived(p, b):
        j = b * n_col + col

        @pl.when(jnp.logical_and(has_edge(b), j + 1 - p <= n_col + LAG - SETTLE))
        def _():
            arrived(edge_slot(p))

    hand_out(0)
    winv3[...] = jnp.zeros(winv3.shape, BF16)

    def seed_arrived(b):
        @pl.when(jnp.logical_not(on_diag))
        def _():
            seed_copy(b, row).wait_recv()

    with jax.named_scope("seed"):
        seed_arrived(0)

        @pl.when(col != 0)
        def _():
            edge_seeded(0)

    def clear(n):
        a, b = lax.rem(n, row_blocks), n // row_blocks

        @pl.when(a * n_row + row < b * n_col + col)
        def _():
            share[spot(a, b)] = jnp.zeros((size, size), F32)

    loop(0, row_blocks * col_blocks, clear)

    def times_t(x, y):
        return lax.dot_general(x, y, (((1,), (1,)), ((), ())), preferred_element_type=F32)

    def update_block(p, a, b):
        share[spot(a, b)] -= times_t(panel[row_slot(p, a)], panel[col_of(p, b)])

    def update_diag(p, b):
        other = panel[col_of(p, b)]
        diag[b] -= times_t(other, other)

    def update_edge(p, b):
        @pl.when(has_edge(b))
        def _():
            edge[b] -= times_t(panel[edge_slot(p)], panel[col_of(p, b)])

    def column_arrived(p, b):
        @pl.when(jnp.logical_not(on_diag))
        def _():
            arrived(col_slot(p, b))

    def update_column(p, b, lo):
        lone = lax.rem(row_blocks - lo, 2)

        @pl.when(lone == 1)
        def _():
            update_block(p, lo, b)

        def pair(m):
            a = lo + lone + 2 * m
            both = spot(a, b, 2)
            left = panel[pl.ds(row_slot(p, a), 2)].reshape(2 * size, size)
            share[both] -= times_t(left, panel[col_of(p, b)]).reshape(2, size, size)

        loop(0, (row_blocks - lo) // 2, pair)

    def trail(p, b_from, near):
        loop(b_from, col_blocks, lambda b: update_column(p, b, first_a(b * n_col + col - jnp.where(b == near, 0, 1))))

    def columns_arrived(p, b_from):
        def one(b):
            column_arrived(p, b)
            edge_arrived(p, b)

        loop(b_from, col_blocks, one)

    def prepare(b):
        work[size:, :] = jnp.zeros((BASE, size), F32)
        r_id = lax.broadcasted_iota(jnp.int32, (size + BASE, size), 0)
        c_id = lax.broadcasted_iota(jnp.int32, (size + BASE, size), 1)
        winv[...] = jnp.where(r_id == c_id, 1.0, 0.0).astype(F32)

    def times_winv_t(x):
        hi, mid, lo = split3(x)
        whi, wmid, wlo = winv3[0], winv3[1], winv3[2]
        small = times_t(lo, whi) + times_t(mid, wmid) + times_t(hi, wlo)
        return small + (times_t(mid, whi) + times_t(hi, wmid)) + times_t(hi, whi)

    def here_diag(k):
        return row == lax.rem(k, n_row)

    def solve(k, a, count):
        kb = k // n_col
        near = jnp.logical_and(a == first_a(k), jnp.logical_not(here_diag(k)))
        here = spot(a, kb, count)

        def shaped(x):
            return x if count == 1 else x.reshape(count, size, size)

        def apply(p):
            left = panel[pl.ds(row_slot(p, a), count)].reshape(count * size, size)
            share[here] -= shaped(times_t(left, panel[col_of(p, kb)]))

        @pl.when(jnp.logical_not(near))
        def _():
            for m in range(count):

                @pl.when(k >= 3)
                def _():
                    receive(k - 3, a + m)

                @pl.when(k >= 2)
                def _():
                    receive(k - 2, a + m)

            loop(jnp.maximum(k - 2 - LAG, 0), k - 1, apply)

        @pl.when(k > 0)
        def _():
            for m in range(count):
                receive(k - 1, a + m)
            apply(k - 1)

        x = times_winv_t(share[here].reshape(count * size, size))
        panel[pl.ds(row_slot(k, a), count)] = x.astype(BF16).reshape(count, size, size)
        share[here] = shaped(x)
        if count == 1:

            @pl.when(jnp.logical_and(near, jnp.logical_and(leads, lax.rem(k + 1, n_row) == LEAD)))
            def _():
                first[...] = panel[row_slot(k, a)]
                first_out(k, start)

        if count == 1:
            source_sends(k, a, start)
        else:
            loop(a, a + count, lambda n: source_sends(k, n, start))

    def update_near(p, b):
        update_diag(p, b)
        update_edge(p, b)

    def first_slot(k, dev_row):
        return jnp.where(lax.rem(k + 1, n_row) == dev_row, row_slot(k, (k + 1) // n_row), col_slot(k, (k + 1) // n_col))

    def first_copy(k, dev_row, sem):
        dst = first_slot(k, dev_row)
        return pltpu.make_async_remote_copy(
            src_ref=first, dst_ref=panel.at[dst], send_sem=sem, recv_sem=recv_sem.at[dst],
            device_id=at(dev_row, lax.rem(col + 1, n_col)), device_id_type=MESH,
        )

    def others_first(k, fn):
        urgent = lax.rem(k + 3, n_row)
        lone = urgent == LEAD
        for m in range(n_row - 1):
            fn(m, lax.rem(jnp.where(lone, LEAD + 1, urgent) + m + jnp.where(lax.rem(jnp.where(lone, LEAD + 1, urgent) - LEAD + n_row, n_row) + m >= n_row, 1, 0), n_row))

    def first_out(k, act):
        act(first_copy(k, LEAD, first_sem.at[0, 0]))

        @pl.when(odd == 0)
        def _():
            others_first(k, lambda m, r: act(first_copy(k, r, first_sem.at[0, 1 + m])))

    def first_down(k, act):
        @pl.when(odd == 0)
        def _():
            others_first(k, lambda m, r: act(copy(first_slot(k, LEAD), first_slot(k, r), first_sem.at[1, 1 + m], at(r, col))))

    def firsts_done(k):
        @pl.when(jnp.logical_and(leads, k + 1 < steps))
        def _():
            first_out(k, finish)

        @pl.when(jnp.logical_and(leads, k > 0))
        def _():
            first_down(k - 1, finish)

    @pl.when(col == 0)
    def _():
        prepare(0)
        work[0:size, :] = diag[0]

    def step(k):
        mine = jnp.logical_and(col == lax.rem(k, n_col), k < steps)
        kb = k // n_col
        last = k - 1
        soon = jnp.logical_and(col == lax.rem(k + 1, n_col), k + 1 < steps)

        @pl.when(mine)
        def _():
            with jax.named_scope("factor"):
                factor_block(work, winv, winv3, prev, fac)

            @pl.when(has_edge(kb))
            def _():
                with jax.named_scope("lead"):

                    @pl.when(k == 0)
                    def _():
                        edge_seeded(kb)

                    @pl.when(k > 0)
                    def _():
                        edge_arrived(last, kb)
                        update_edge(last, kb)

                    first[...] = times_winv_t(edge[kb]).astype(BF16)
                    first_out(k, start)

            lo = first_a(k)
            second = jnp.minimum(lo + 1, row_blocks)
            third = second + lax.rem(row_blocks - second, 2)
            with jax.named_scope("solve_near"):
                loop(lo, third, lambda a: solve(k, a, 1))
            with jax.named_scope("solve_two"):
                loop(0, (row_blocks - third) // 2, lambda m: solve(k, third + 2 * m, 2))

        @pl.when(k >= depth)
        def _():
            with jax.named_scope("passed"):
                passed(k - depth)

        @pl.when(mine)
        def _():
            @pl.when(row == lax.rem(k, n_row))
            def _():
                for d in range(1, n_row):
                    seed_copy(kb, lax.rem(row + d, n_row)).wait_send()
                r_id = lax.broadcasted_iota(jnp.int32, (size, size), 0)
                c_id = lax.broadcasted_iota(jnp.int32, (size, size), 1)
                share[spot(k // n_row, kb)] = jnp.where(r_id >= c_id, work[0:size, :].T, 0.0)

        @pl.when(jnp.logical_and(k > 0, jnp.logical_not(jnp.logical_or(mine, soon))))
        def _():
            @pl.when(col != lax.rem(last, n_col))
            def _():
                with jax.named_scope("receive"):
                    end = jnp.where(lead(last) == 3, jnp.minimum(last_near(last) + 1, row_blocks), row_blocks)
                    loop(first_passed(last), end, lambda a: receive_any(last, a))

            near = first_b(k)
            age = k + n_col - (near * n_col + col)
            settle = jnp.logical_and(age == SETTLE, jnp.logical_and(near > 0, near < col_blocks))

            @pl.when(settle)
            def _():
                with jax.named_scope("late_trail"):
                    own = k - SETTLE

                    for back in (LAG + 2, LAG + 1, LAG):

                        @pl.when(own >= back)
                        def _():
                            columns_arrived(own - back, near)

                    loop(jnp.maximum(own - 2 - LAG, 0), own - LAG + 1, lambda p: trail(p, near, -1))

            @pl.when(jnp.logical_and(k >= LAG, lead(last) != 3))
            def _():
                p = k - LAG
                with jax.named_scope("columns"):
                    columns_arrived(p, near)

                @pl.when(jnp.logical_and(near < col_blocks, age >= SETTLE + 2))
                def _():
                    @pl.when(jnp.logical_and(age == SETTLE + 2, near > 0))
                    def _():
                        with jax.named_scope("seed_late"):
                            seed_arrived(near)
                            edge_seeded(near)

                    oldest = jnp.where(age == SETTLE + 2, jnp.maximum(p - 1, 0), p)
                    loop(oldest, p + 1, lambda q: update_near(q, near))

                with jax.named_scope("trail"):
                    trail(p, near, jnp.where(jnp.logical_or(age > SETTLE, near == 0), near, -1))

            @pl.when(settle)
            def _():
                hand_out(near)

        @pl.when(soon)
        def _():
            nb = (k + 1) // n_col

            oldest = jnp.maximum(k - 1 - LAG, 0)
            lo = first_a(k + 1)

            def old_diag(p):
                column_arrived(p, nb)
                edge_arrived(p, nb)
                update_near(p, nb)

            def take(a):
                receive(last, a)

                @pl.when(jnp.logical_not(here_diag(k + 1)))
                def _():
                    loop(oldest, last, lambda p: update_block(p, a, nb))

            @pl.when(k > 0)
            def _():
                with jax.named_scope("old_diag"):
                    loop(oldest, last, old_diag)
                with jax.named_scope("take"):
                    loop(first_a(k), jnp.minimum(first_a(k) + 1, row_blocks), take)
                with jax.named_scope("take_column"):
                    column_arrived(last, nb)
                    edge_arrived(last, nb)
                with jax.named_scope("catch_up"):
                    update_near(last, nb)
                    @pl.when(jnp.logical_and(jnp.logical_not(here_diag(k + 1)), lo < row_blocks))
                    def _():
                        update_block(last, lo, nb)

            prepare(nb)
            slot = col_of(k, nb)
            with jax.named_scope("first_block"):
                arrived(slot)

            @pl.when(leads)
            def _():
                first_down(k, start)

            other = panel[slot]
            work[0:size, :] = diag[nb] - times_t(other, other)

        @pl.when(jnp.logical_and(k >= n_col // 2, col == lax.rem(k + n_col // 2, n_col)))
        def _():
            with jax.named_scope("sends_done"):
                firsts_done(k - n_col // 2)
                loop(first_a(k - n_col // 2), row_blocks, lambda a: source_sends(k - n_col // 2, a, finish))

    loop(0, steps + n_col // 2, step)

    def edges_done(b):
        @pl.when(jnp.logical_and(holds_edge(b), jnp.logical_not(leads)))
        def _():
            edge_copy(b).wait_send()

    loop(0, col_blocks, edges_done)


def solution(mesh):
    n_row = mesh.shape["row"]
    n_col = mesh.shape["col"]

    def factor_local(a_loc):
        row_blocks, size, local_cols = a_loc.shape
        col_blocks = local_cols // size
        slots = n_row * (row_blocks * (row_blocks + 1) // 2) + n_col * (col_blocks * (col_blocks + 1) // 2)
        slots += row_blocks * n_row
        return pl.pallas_call(
            functools.partial(kernel, n_row, n_col, "batch"),
            out_shape=pltpu.VMEM(a_loc.shape, F32),
            in_specs=[pl.BlockSpec(memory_space=pl.ANY)],
            scratch_shapes=[
                pltpu.VMEM((col_blocks, size, size), F32),
                pltpu.VMEM((col_blocks, size, size), F32),
                pltpu.VMEM((col_blocks, size, size), F32),
                pltpu.VMEM((size, size), BF16),
                pltpu.VMEM((slots, size, size), BF16),
                pltpu.VMEM((size + BASE, size), F32),
                pltpu.VMEM((size + BASE, size), F32),
                pltpu.VMEM((3, size, size), BF16),
                pltpu.VMEM((BASE, 3 * LANE), F32),
                pltpu.VMEM((4 * SUB, SUB, LANE), F32),
                pltpu.SemaphoreType.DMA,
                pltpu.SemaphoreType.DMA((col_blocks, n_row)),
                pltpu.SemaphoreType.DMA((col_blocks,)),
                pltpu.SemaphoreType.DMA((col_blocks,)),
                pltpu.SemaphoreType.DMA((col_blocks,)),
                pltpu.SemaphoreType.DMA((2, n_row)),
                pltpu.SemaphoreType.DMA((row_blocks, 9)),
                pltpu.SemaphoreType.DMA((4, row_blocks, 2)),
                pltpu.SemaphoreType.DMA((4, col_blocks, 3)),
                pltpu.SemaphoreType.DMA((slots,)),
            ],
            compiler_params=pltpu.CompilerParams(
                collective_id=0, has_side_effects=True, vmem_limit_bytes=50 * 1024 * 1024
            ),
            name="cholesky",
        )(a_loc)

    blk_spec = P(("batch", "row"), None, "col")
    return jax.shard_map(factor_local, mesh=mesh, in_specs=(blk_spec,), out_specs=blk_spec, check_vma=False)
```

```python
import functools

import jax
import jax.numpy as jnp
from jax import lax
from jax.experimental import pallas as pl
from jax.experimental.pallas import tpu as pltpu
from jax.sharding import PartitionSpec as P

F32 = jnp.float32
BF16 = jnp.bfloat16
MESH = pl.DeviceIdType.MESH
SUB = 8
LANE = 128
BASE = 16
LEAD = 1
SETTLE = 3
LAG = 3


def sub_bcast(x, q):
    return jnp.broadcast_to(x[q : q + 1, :], (SUB, LANE))


ALONG_LANES = lax.GatherDimensionNumbers(
    offset_dims=(), collapsed_slice_dims=(1,), start_index_map=(1,), operand_batching_dims=(0,), start_indices_batching_dims=(0,)
)


def lane_bcast(x, lane):
    index = jnp.full((SUB, LANE, 1), lane, jnp.int32)
    return lax.gather(x, index, ALONG_LANES, (1, 1), mode=lax.GatherScatterMode.PROMISE_IN_BOUNDS)


def split3(x):
    high = x.astype(BF16)
    rest = x - high.astype(F32)
    mid = rest.astype(BF16)
    return high, mid, (rest - mid.astype(F32)).astype(BF16)


def swap_rows(x, bit, row_id):
    if bit == SUB // 2:
        return pltpu.roll(x, bit, 0)
    return jnp.where((row_id & bit) == 0, pltpu.roll(x, SUB - bit, 0), pltpu.roll(x, bit, 0))


def stack_sums(parts):
    row_id = lax.broadcasted_iota(jnp.int32, (SUB, LANE), 0)
    for bit in (4, 2, 1):
        low = (row_id & bit) == 0
        half = len(parts) // 2
        parts = [
            jnp.where(low, parts[n], parts[n + half]) + swap_rows(jnp.where(low, parts[n + half], parts[n]), bit, row_id)
            for n in range(half)
        ]
    return parts[0]


def eliminate(rows, lane0):
    row_id = lax.broadcasted_iota(jnp.int32, (SUB, LANE), 0)
    rows = [list(rows[0]), list(rows[1])]
    cols = [
        [lane_bcast(rows[0][0], lane0 + j) for j in range(SUB)],
        [lane_bcast(rows[1][0], lane0 + j) for j in range(BASE)],
    ]
    scale = [jnp.zeros((SUB, LANE), F32), jnp.zeros((SUB, LANE), F32)]
    pivot = sub_bcast(cols[0][0], 0)
    for j in range(BASE):
        t, q = divmod(j, SUB)
        inv = lax.rsqrt(pivot)
        scale[t] = jnp.where(row_id == q, inv, scale[t])
        if j + 1 < BASE:
            tn, qn = divmod(j + 1, SUB)
            near = sub_bcast(cols[tn][j], qn) * inv
            pivot = sub_bcast(cols[tn][j + 1], qn) - near * near
        below = cols[1][j] * inv
        here = cols[0][j] * inv if t == 0 else None
        for n in range(j + 1, BASE):
            tn, qn = divmod(n, SUB)
            other = near if n == j + 1 else sub_bcast(here if tn == 0 else below, qn)
            if t == 0 and tn == 0:
                cols[0][n] = cols[0][n] - here * other
            cols[1][n] = cols[1][n] - below * other
        masked = jnp.where(row_id > q, here if t == 0 else below, 0.0)
        for v in range(len(rows[0])):
            pivot_row = sub_bcast(rows[t][v], q) * inv
            rows[t][v] = rows[t][v] - masked * pivot_row
            if t == 0:
                rows[1][v] = rows[1][v] - below * pivot_row
    return [[x * scale[t] for x in rows[t]] for t in range(2)]


def factor_block(work, winv, winv3, prev, fac):
    size = work.shape[1]
    prev[...] = jnp.zeros(prev.shape, F32)
    fac[...] = jnp.zeros(fac.shape, F32)

    def group(v):
        return slice(LANE * v, LANE * (v + 1))

    def pending(factors, before, t, v):
        above, below = before[:SUB, group(v)], before[SUB:, group(v)]
        at = 2 * SUB * t
        return stack_sums([factors[at + n] * above + factors[at + SUB + n] * below for n in range(SUB)])

    for half in range(size // LANE):
        views = [(work, 0), (work, 1), (winv, 0)] if half == 0 else [(work, 1), (winv, 0), (winv, 1)]
        first = half * LANE
        if half == 1:
            factors, before = fac[...], prev[...]
            work[first : first + BASE, group(1)] -= jnp.concatenate([pending(factors, before, t, 1) for t in range(2)], axis=0)
            prev[...] = jnp.concatenate([before[:, group(1)], before[:, group(2)], jnp.zeros((BASE, LANE), F32)], axis=1)

        def body(s, carry, views=views, first=first):
            lane0 = s * BASE
            row0 = pl.multiple_of(first + lane0, BASE)

            here = pl.ds(row0, BASE)
            then = pl.ds(pl.multiple_of(row0 + BASE, BASE), BASE)
            both = [ref[here, group(g)] for ref, g in views]
            rows = [[x[SUB * t : SUB * (t + 1)] for x in both] for t in range(2)]
            factors, before = fac[...], prev[...]
            for t in range(2):
                for v in (1, 2):
                    rows[t][v] = rows[t][v] - pending(factors, before, t, v)
            hi, mid, lo = split3(before)
            lane = lax.broadcasted_iota(jnp.int32, (BASE, size - first), 1) + first
            after = lane >= row0 + BASE
            lhi, lmid, llo = [jnp.where(after, x[:, : size - first], jnp.zeros((), BF16)) for x in (hi, mid, lo)]
            update = lax.dot_general(
                jnp.concatenate([lhi, lhi, lmid, lhi, llo, lmid], axis=0),
                jnp.concatenate([hi, mid, hi, lo, hi, mid], axis=0),
                (((0,), (0,)), ((), ())),
                preferred_element_type=F32,
            )
            for v, (ref, g) in enumerate(views):
                ref[first:size, group(g)] -= update[:, group(v)]
            done = eliminate(rows, lane0)
            if first == 0:
                source = [jnp.where(s == LANE // BASE - 1, done[t][1], done[t][0]) for t in range(2)]
            else:
                source = [done[t][0] for t in range(2)]
            next_lane = (lane0 + BASE) % LANE
            factors, sums = [], []
            for t in range(2):
                factor = [[lane_bcast(source[m], next_lane + SUB * t + n) for n in range(SUB)] for m in range(2)]
                sums.append(stack_sums([factor[0][n] * done[0][0] + factor[1][n] * done[1][0] for n in range(SUB)]))
                factors += factor[0] + factor[1]
            ref, g = views[0]
            ref[then, group(g)] -= jnp.concatenate(sums, axis=0)
            fac[...] = jnp.stack(factors)
            whole = [jnp.concatenate([done[0][v], done[1][v]], axis=0) for v in range(3)]
            prev[...] = jnp.concatenate(whole, axis=1)
            for (ref, g), x in zip(views, whole):
                ref[here, group(g)] = x
                if ref is winv:
                    for n, part in enumerate(split3(x)):
                        winv3[n, here, group(g)] = part
            return carry

        lax.fori_loop(0, LANE // BASE, body, 0, unroll=2)


def kernel(n_row, n_col, batch_axis, a_ref, share, diag, edge, stage, first, panel, work, winv, winv3, prev, fac, load_sem,
           seed_send, seed_recv, edge_send, edge_recv, first_sem, send_sem, pass_sem, down_sem, recv_sem):
    row_blocks, size, local_cols = a_ref.shape
    col_blocks = local_cols // size
    ratio = n_col // n_row
    steps = row_blocks * n_row
    depth = pass_sem.shape[0]
    batch = lax.axis_index(batch_axis)
    row = lax.axis_index("row")
    col = lax.axis_index("col")
    odd = lax.rem(col, 2)
    on_diag = lax.rem(col, n_row) == row
    row_slots = n_row * (row_blocks * (row_blocks + 1) // 2)
    edge_slots = row_slots + n_col * (col_blocks * (col_blocks + 1) // 2)
    leads = row == LEAD

    def at(dev_row, dev_col):
        return (batch, dev_row, dev_col)

    def row_slot(k, a):
        g = k // n_row
        return n_row * (row_blocks * g - (g * (g - 1)) // 2) + (k - g * n_row) * (row_blocks - g) + a - g

    def col_slot(k, b):
        h = k // n_col
        return row_slots + n_col * (col_blocks * h - (h * (h - 1)) // 2) + (k - h * n_col) * (col_blocks - h) + b - h

    def first_a(k):
        return (k + n_row - row) // n_row

    def first_b(k):
        return (k + n_col - col) // n_col

    def spot(a, b, count=1):
        return (a if count == 1 else pl.ds(a, count), slice(None), pl.ds(pl.multiple_of(b * size, size), size))

    def col_of(k, b):
        return jnp.where(on_diag, row_slot(k, ratio * b + col // n_row), col_slot(k, b))

    def edge_slot(k):
        return edge_slots + k

    def edge_reach(ahead):
        return jnp.logical_and(ahead >= 2, jnp.logical_and(ahead <= n_col + LAG - SETTLE, row != LEAD))

    def copy(src_slot, dst_slot, sem, device):
        return pltpu.make_async_remote_copy(
            src_ref=panel.at[src_slot], dst_ref=panel.at[dst_slot], send_sem=sem, recv_sem=recv_sem.at[dst_slot],
            device_id=device, device_id_type=MESH,
        )

    def arrived(slot):
        copy(slot, slot, send_sem.at[0, 0], at(row, col)).wait_recv()

    def start(c):
        c.start()

    def finish(c):
        c.wait_send()

    def from_maker(ahead, way):
        there = lax.rem(row + way, n_row)
        lead_near = jnp.logical_and(there == LEAD, jnp.logical_and(ahead >= 2, ahead <= n_row))
        soon_needed = jnp.logical_and(ahead == 2, way == 2)
        return jnp.logical_or(lead_near, soon_needed)

    def down_column(k, a, maker, sems, act):
        i = a * n_row + row
        slot = row_slot(k, a)
        dst = col_slot(k, i // n_col)
        for m, way in enumerate((1, n_row - 1, 2)):
            direct = from_maker(i - k, way)

            @pl.when(jnp.where(maker, direct, jnp.logical_not(direct)))
            def _():
                act(copy(slot, dst, sems[m], at(lax.rem(row + way, n_row), lax.rem(i, n_col))))

    def last_near(p):
        return first_a(p + 2)

    def to_edge(k, a, sem, act):
        i = a * n_row + row
        act(copy(row_slot(k, a), edge_slot(k), sem, at(LEAD, lax.rem(i - 1, n_col))))

    def source_sends(k, a, act):
        ahead = a * n_row + row - k
        slot = row_slot(k, a)
        early = n_row

        @pl.when(edge_reach(ahead))
        def _():
            to_edge(k, a, send_sem.at[a, 5], act)

        near = jnp.logical_and(ahead >= 2, ahead <= early)

        @pl.when(jnp.logical_or(near, lax.rem(ahead, n_col) == 0))
        def _():
            down_column(k, a, near, [send_sem.at[a, m] for m in range(3)], act)

        @pl.when(jnp.logical_or(jnp.logical_and(odd == 0, ahead >= 2), ahead >= n_col - 1))
        def _():
            act(copy(slot, slot, send_sem.at[a, 3], at(row, lax.rem(jnp.where(odd == 0, col + 1, col - 1), n_col))))

        @pl.when(ahead >= 2)
        def _():
            act(copy(slot, slot, send_sem.at[a, 6], at(row, lax.rem(col - odd + 2, n_col))))

        @pl.when(jnp.logical_and(ahead >= 3 - odd, a <= last_near(k)))
        def _():
            act(copy(slot, slot, send_sem.at[a, 4], at(row, lax.rem(col - odd + 3, n_col))))

        @pl.when(jnp.logical_and(ahead >= n_col // 2 - odd, ahead < n_col - 2 - odd))
        def _():
            act(copy(slot, slot, send_sem.at[a, 7], at(row, lax.rem(col - odd + 5, n_col))))

        @pl.when(ahead >= n_col - 2 - odd)
        def _():
            act(copy(slot, slot, send_sem.at[a, 8], at(row, lax.rem(col - odd - 2 + n_col, n_col))))

    def lead(p):
        return lax.rem(col - lax.rem(p, n_col) + n_col, n_col)

    def hops(p):
        return lax.rem(col // 2 - lax.rem(p, n_col) // 2 + n_col // 2, n_col // 2)

    def passes(p):
        return jnp.where(odd == 1, 2, n_col // 2 - 1) == hops(p)

    def first_passed(p):
        low = jnp.where(jnp.logical_and(passes(p), odd == 1), lead(p) - 1, lead(p))
        return (p + low - row + n_row - 1) // n_row

    def pass_down(p, a, act):
        i = a * n_row + row
        ahead = i - p
        sems = pass_sem.at[lax.rem(p, depth), a]

        @pl.when(jnp.logical_and(odd == 0, jnp.logical_and(lead(p) <= 2, a > last_near(p))))
        def _():
            act(copy(row_slot(p, a), row_slot(p, a), sems.at[0], at(row, col + 1)))

        @pl.when(jnp.logical_and(lax.rem(i, n_col) == col, ahead > 1))
        def _():
            downs = down_sem.at[lax.rem(p, depth), i // n_col]
            down_column(p, a, False, [downs.at[m] for m in range(3)], act)

    def pass_on(p, a, act):
        slot = row_slot(p, a)
        sems = pass_sem.at[lax.rem(p, depth), a]

        @pl.when(passes(p))
        def _():
            @pl.when(odd == 0)
            def _():
                act(copy(slot, slot, sems.at[1], at(row, lax.rem(col - 1 + n_col, n_col))))

            @pl.when(jnp.logical_or(odd == 1, a * n_row + row > p + lead(p)))
            def _():
                act(copy(slot, slot, sems.at[0], at(row, col + 1 - 2 * odd)))

        pass_down(p, a, act)

    def passed(p):
        @pl.when(lead(p) != 0)
        def _():
            loop(first_passed(p), row_blocks, lambda a: pass_on(p, a, finish))

    def receive(p, a):
        arrived(row_slot(p, a))
        pass_down(p, a, start)

    def receive_any(p, a):
        arrived(row_slot(p, a))
        pass_on(p, a, start)

    def loop(lo, hi, fn):
        lax.fori_loop(lo, hi, lambda n, c: (fn(n), c)[1], 0)

    load = pltpu.make_async_copy(a_ref, share, load_sem)
    load.start()

    barrier = pltpu.get_barrier_semaphore()
    n_dev = n_row * n_col

    def greet(n):
        other = lax.rem(row * n_col + col + n, n_dev)
        pl.semaphore_signal(barrier, inc=1, device_id=at(other // n_col, lax.rem(other, n_col)), device_id_type=MESH)

    loop(1, n_dev, greet)
    with jax.named_scope("all_here"):
        pl.semaphore_wait(barrier, n_dev - 1)
    with jax.named_scope("loaded"):
        load.wait()

    def seed_copy(b, dev_row):
        return pltpu.make_async_remote_copy(
            src_ref=share.at[spot(ratio * b + col // n_row, b)], dst_ref=diag.at[b],
            send_sem=seed_send.at[b, lax.rem(dev_row - row + n_row, n_row)],
            recv_sem=seed_recv.at[b], device_id=at(dev_row, col), device_id_type=MESH,
        )

    def hand_out(b):
        @pl.when(on_diag)
        def _():
            for d in (1, n_row - 1, 2):
                seed_copy(b, lax.rem(row + d, n_row)).start()
            diag[b] = share[spot(ratio * b + col // n_row, b)]

        @pl.when(jnp.logical_and(holds_edge(b), jnp.logical_not(leads)))
        def _():
            stage[b] = share[spot((b * n_col + col + 1) // n_row, b)]
            edge_copy(b).start()

    def holds_edge(b):
        j = b * n_col + col
        return jnp.logical_and(lax.rem(j + 1, n_row) == row, j + 1 < steps)

    def edge_copy(b):
        return pltpu.make_async_remote_copy(
            src_ref=stage.at[b], dst_ref=edge.at[b], send_sem=edge_send.at[b], recv_sem=edge_recv.at[b],
            device_id=at(LEAD, col), device_id_type=MESH,
        )

    def has_edge(b):
        from_other = jnp.logical_and(leads, lax.rem(col + 1, n_row) != LEAD)
        return jnp.logical_and(from_other, b * n_col + col + 1 < steps)

    def edge_seeded(b):
        @pl.when(has_edge(b))
        def _():
            edge_copy(b).wait_recv()

    def edge_arrived(p, b):
        j = b * n_col + col

        @pl.when(jnp.logical_and(has_edge(b), j + 1 - p <= n_col + LAG - SETTLE))
        def _():
            arrived(edge_slot(p))

    hand_out(0)
    winv3[...] = jnp.zeros(winv3.shape, BF16)

    def seed_arrived(b):
        @pl.when(jnp.logical_not(on_diag))
        def _():
            seed_copy(b, row).wait_recv()

    with jax.named_scope("seed"):
        seed_arrived(0)

        @pl.when(col != 0)
        def _():
            edge_seeded(0)

    def clear(n):
        a, b = lax.rem(n, row_blocks), n // row_blocks

        @pl.when(a * n_row + row < b * n_col + col)
        def _():
            share[spot(a, b)] = jnp.zeros((size, size), F32)

    loop(0, row_blocks * col_blocks, clear)

    def times_t(x, y):
        return lax.dot_general(x, y, (((1,), (1,)), ((), ())), preferred_element_type=F32)

    def update_block(p, a, b):
        share[spot(a, b)] -= times_t(panel[row_slot(p, a)], panel[col_of(p, b)])

    def update_diag(p, b):
        other = panel[col_of(p, b)]
        diag[b] -= times_t(other, other)

    def update_edge(p, b):
        @pl.when(has_edge(b))
        def _():
            edge[b] -= times_t(panel[edge_slot(p)], panel[col_of(p, b)])

    def column_arrived(p, b):
        @pl.when(jnp.logical_not(on_diag))
        def _():
            arrived(col_slot(p, b))

    def update_column(p, b, lo):
        lone = lax.rem(row_blocks - lo, 2)

        @pl.when(lone == 1)
        def _():
            update_block(p, lo, b)

        def pair(m):
            a = lo + lone + 2 * m
            both = spot(a, b, 2)
            left = panel[pl.ds(row_slot(p, a), 2)].reshape(2 * size, size)
            share[both] -= times_t(left, panel[col_of(p, b)]).reshape(2, size, size)

        loop(0, (row_blocks - lo) // 2, pair)

    def trail(p, b_from, near):
        loop(b_from, col_blocks, lambda b: update_column(p, b, first_a(b * n_col + col - jnp.where(b == near, 0, 1))))

    def columns_arrived(p, b_from):
        def one(b):
            column_arrived(p, b)
            edge_arrived(p, b)

        loop(b_from, col_blocks, one)

    def prepare(b):
        work[size:, :] = jnp.zeros((BASE, size), F32)
        r_id = lax.broadcasted_iota(jnp.int32, (size + BASE, size), 0)
        c_id = lax.broadcasted_iota(jnp.int32, (size + BASE, size), 1)
        winv[...] = jnp.where(r_id == c_id, 1.0, 0.0).astype(F32)

    def times_winv_t(x):
        hi, mid, lo = split3(x)
        whi, wmid, wlo = winv3[0], winv3[1], winv3[2]
        small = times_t(lo, whi) + times_t(mid, wmid) + times_t(hi, wlo)
        return small + (times_t(mid, whi) + times_t(hi, wmid)) + times_t(hi, whi)

    def here_diag(k):
        return row == lax.rem(k, n_row)

    def solve(k, a, count):
        kb = k // n_col
        near = jnp.logical_and(a == first_a(k), jnp.logical_not(here_diag(k)))
        here = spot(a, kb, count)

        def shaped(x):
            return x if count == 1 else x.reshape(count, size, size)

        def apply(p):
            left = panel[pl.ds(row_slot(p, a), count)].reshape(count * size, size)
            share[here] -= shaped(times_t(left, panel[col_of(p, kb)]))

        @pl.when(jnp.logical_not(near))
        def _():
            for m in range(count):

                @pl.when(k >= 3)
                def _():
                    receive(k - 3, a + m)

                @pl.when(k >= 2)
                def _():
                    receive(k - 2, a + m)

            loop(jnp.maximum(k - 2 - LAG, 0), k - 1, apply)

        @pl.when(k > 0)
        def _():
            for m in range(count):
                receive(k - 1, a + m)
            apply(k - 1)

        x = times_winv_t(share[here].reshape(count * size, size))
        panel[pl.ds(row_slot(k, a), count)] = x.astype(BF16).reshape(count, size, size)
        share[here] = shaped(x)
        if count == 1:

            @pl.when(jnp.logical_and(near, jnp.logical_and(leads, lax.rem(k + 1, n_row) == LEAD)))
            def _():
                first[...] = panel[row_slot(k, a)]
                first_out(k, start)

        if count == 1:
            source_sends(k, a, start)
        else:
            loop(a, a + count, lambda n: source_sends(k, n, start))

    def update_near(p, b):
        update_diag(p, b)
        update_edge(p, b)

    def first_slot(k, dev_row):
        return jnp.where(lax.rem(k + 1, n_row) == dev_row, row_slot(k, (k + 1) // n_row), col_slot(k, (k + 1) // n_col))

    def first_copy(k, dev_row, sem):
        dst = first_slot(k, dev_row)
        return pltpu.make_async_remote_copy(
            src_ref=first, dst_ref=panel.at[dst], send_sem=sem, recv_sem=recv_sem.at[dst],
            device_id=at(dev_row, lax.rem(col + 1, n_col)), device_id_type=MESH,
        )

    def others_first(k, fn):
        urgent = lax.rem(k + 3, n_row)
        lone = urgent == LEAD
        for m in range(n_row - 1):
            fn(m, lax.rem(jnp.where(lone, LEAD + 1, urgent) + m + jnp.where(lax.rem(jnp.where(lone, LEAD + 1, urgent) - LEAD + n_row, n_row) + m >= n_row, 1, 0), n_row))

    def first_out(k, act):
        act(first_copy(k, LEAD, first_sem.at[0, 0]))

        @pl.when(odd == 0)
        def _():
            others_first(k, lambda m, r: act(first_copy(k, r, first_sem.at[0, 1 + m])))

    def first_down(k, act):
        @pl.when(odd == 0)
        def _():
            others_first(k, lambda m, r: act(copy(first_slot(k, LEAD), first_slot(k, r), first_sem.at[1, 1 + m], at(r, col))))

    def firsts_done(k):
        @pl.when(jnp.logical_and(leads, k + 1 < steps))
        def _():
            first_out(k, finish)

        @pl.when(jnp.logical_and(leads, k > 0))
        def _():
            first_down(k - 1, finish)

    @pl.when(col == 0)
    def _():
        prepare(0)
        work[0:size, :] = diag[0]

    def step(k):
        mine = jnp.logical_and(col == lax.rem(k, n_col), k < steps)
        kb = k // n_col
        last = k - 1
        soon = jnp.logical_and(col == lax.rem(k + 1, n_col), k + 1 < steps)

        @pl.when(mine)
        def _():
            with jax.named_scope("factor"):
                factor_block(work, winv, winv3, prev, fac)

            @pl.when(has_edge(kb))
            def _():
                with jax.named_scope("lead"):

                    @pl.when(k == 0)
                    def _():
                        edge_seeded(kb)

                    @pl.when(k > 0)
                    def _():
                        edge_arrived(last, kb)
                        update_edge(last, kb)

                    first[...] = times_winv_t(edge[kb]).astype(BF16)
                    first_out(k, start)

            lo = first_a(k)
            second = jnp.minimum(lo + 1, row_blocks)
            third = second + lax.rem(row_blocks - second, 2)
            with jax.named_scope("solve_near"):
                loop(lo, third, lambda a: solve(k, a, 1))
            with jax.named_scope("solve_two"):
                loop(0, (row_blocks - third) // 2, lambda m: solve(k, third + 2 * m, 2))

        @pl.when(k >= depth)
        def _():
            with jax.named_scope("passed"):
                passed(k - depth)

        @pl.when(mine)
        def _():
            @pl.when(row == lax.rem(k, n_row))
            def _():
                for d in range(1, n_row):
                    seed_copy(kb, lax.rem(row + d, n_row)).wait_send()
                r_id = lax.broadcasted_iota(jnp.int32, (size, size), 0)
                c_id = lax.broadcasted_iota(jnp.int32, (size, size), 1)
                share[spot(k // n_row, kb)] = jnp.where(r_id >= c_id, work[0:size, :].T, 0.0)

        @pl.when(jnp.logical_and(k > 0, jnp.logical_not(jnp.logical_or(mine, soon))))
        def _():
            @pl.when(col != lax.rem(last, n_col))
            def _():
                with jax.named_scope("receive"):
                    end = jnp.where(lead(last) == 3, jnp.minimum(last_near(last) + 1, row_blocks), row_blocks)
                    loop(first_passed(last), end, lambda a: receive_any(last, a))

            near = first_b(k)
            age = k + n_col - (near * n_col + col)
            settle = jnp.logical_and(age == SETTLE, jnp.logical_and(near > 0, near < col_blocks))

            @pl.when(settle)
            def _():
                with jax.named_scope("late_trail"):
                    own = k - SETTLE

                    for back in (LAG + 2, LAG + 1, LAG):

                        @pl.when(own >= back)
                        def _():
                            columns_arrived(own - back, near)

                    loop(jnp.maximum(own - 2 - LAG, 0), own - LAG + 1, lambda p: trail(p, near, -1))

            @pl.when(jnp.logical_and(k >= LAG, lead(last) != 3))
            def _():
                p = k - LAG
                with jax.named_scope("columns"):
                    columns_arrived(p, near)

                @pl.when(jnp.logical_and(near < col_blocks, age >= SETTLE + 2))
                def _():
                    @pl.when(jnp.logical_and(age == SETTLE + 2, near > 0))
                    def _():
                        with jax.named_scope("seed_late"):
                            seed_arrived(near)
                            edge_seeded(near)

                    oldest = jnp.where(age == SETTLE + 2, jnp.maximum(p - 1, 0), p)
                    loop(oldest, p + 1, lambda q: update_near(q, near))

                with jax.named_scope("trail"):
                    trail(p, near, jnp.where(jnp.logical_or(age > SETTLE, near == 0), near, -1))

            @pl.when(settle)
            def _():
                hand_out(near)

        @pl.when(soon)
        def _():
            nb = (k + 1) // n_col

            oldest = jnp.maximum(k - 1 - LAG, 0)
            lo = first_a(k + 1)

            def old_diag(p):
                column_arrived(p, nb)
                edge_arrived(p, nb)
                update_near(p, nb)

            def take(a):
                receive(last, a)

                @pl.when(jnp.logical_not(here_diag(k + 1)))
                def _():
                    loop(oldest, last, lambda p: update_block(p, a, nb))

            @pl.when(k > 0)
            def _():
                with jax.named_scope("old_diag"):
                    loop(oldest, last, old_diag)
                with jax.named_scope("take"):
                    loop(first_a(k), jnp.minimum(first_a(k) + 1, row_blocks), take)
                with jax.named_scope("take_column"):
                    column_arrived(last, nb)
                    edge_arrived(last, nb)
                with jax.named_scope("catch_up"):
                    update_near(last, nb)
                    @pl.when(jnp.logical_and(jnp.logical_not(here_diag(k + 1)), lo < row_blocks))
                    def _():
                        update_block(last, lo, nb)

            prepare(nb)
            slot = col_of(k, nb)
            with jax.named_scope("first_block"):
                arrived(slot)

            @pl.when(leads)
            def _():
                first_down(k, start)

            other = panel[slot]
            work[0:size, :] = diag[nb] - times_t(other, other)

        @pl.when(jnp.logical_and(k >= n_col // 2, col == lax.rem(k + n_col // 2, n_col)))
        def _():
            with jax.named_scope("sends_done"):
                firsts_done(k - n_col // 2)
                loop(first_a(k - n_col // 2), row_blocks, lambda a: source_sends(k - n_col // 2, a, finish))

    loop(0, steps + n_col // 2, step)

    def edges_done(b):
        @pl.when(jnp.logical_and(holds_edge(b), jnp.logical_not(leads)))
        def _():
            edge_copy(b).wait_send()

    loop(0, col_blocks, edges_done)


def solution(mesh):
    n_row = mesh.shape["row"]
    n_col = mesh.shape["col"]

    def factor_local(a_loc):
        row_blocks, size, local_cols = a_loc.shape
        col_blocks = local_cols // size
        slots = n_row * (row_blocks * (row_blocks + 1) // 2) + n_col * (col_blocks * (col_blocks + 1) // 2)
        slots += row_blocks * n_row
        return pl.pallas_call(
            functools.partial(kernel, n_row, n_col, "batch"),
            out_shape=pltpu.VMEM(a_loc.shape, F32),
            in_specs=[pl.BlockSpec(memory_space=pl.ANY)],
            scratch_shapes=[
                pltpu.VMEM((col_blocks, size, size), F32),
                pltpu.VMEM((col_blocks, size, size), F32),
                pltpu.VMEM((col_blocks, size, size), F32),
                pltpu.VMEM((size, size), BF16),
                pltpu.VMEM((slots, size, size), BF16),
                pltpu.VMEM((size + BASE, size), F32),
                pltpu.VMEM((size + BASE, size), F32),
                pltpu.VMEM((3, size, size), BF16),
                pltpu.VMEM((BASE, 3 * LANE), F32),
                pltpu.VMEM((4 * SUB, SUB, LANE), F32),
                pltpu.SemaphoreType.DMA,
                pltpu.SemaphoreType.DMA((col_blocks, n_row)),
                pltpu.SemaphoreType.DMA((col_blocks,)),
                pltpu.SemaphoreType.DMA((col_blocks,)),
                pltpu.SemaphoreType.DMA((col_blocks,)),
                pltpu.SemaphoreType.DMA((2, n_row)),
                pltpu.SemaphoreType.DMA((row_blocks, 9)),
                pltpu.SemaphoreType.DMA((4, row_blocks, 2)),
                pltpu.SemaphoreType.DMA((4, col_blocks, 3)),
                pltpu.SemaphoreType.DMA((slots,)),
            ],
            compiler_params=pltpu.CompilerParams(
                collective_id=0, has_side_effects=True, vmem_limit_bytes=50 * 1024 * 1024
            ),
            name="cholesky",
        )(a_loc)

    blk_spec = P(("batch", "row"), None, "col")
    return jax.shard_map(factor_local, mesh=mesh, in_specs=(blk_spec,), out_specs=blk_spec, check_vma=False)
```

```python
import functools

import jax
import jax.numpy as jnp
from jax import lax
from jax.experimental import pallas as pl
from jax.experimental.pallas import tpu as pltpu
from jax.sharding import PartitionSpec as P

F32 = jnp.float32
BF16 = jnp.bfloat16
MESH = pl.DeviceIdType.MESH
SUB = 8
LANE = 128
BASE = 16
LEAD = 1
SETTLE = 2
LAG = 3


def sub_bcast(x, q):
    return jnp.broadcast_to(x[q : q + 1, :], (SUB, LANE))


ALONG_LANES = lax.GatherDimensionNumbers(
    offset_dims=(), collapsed_slice_dims=(1,), start_index_map=(1,), operand_batching_dims=(0,), start_indices_batching_dims=(0,)
)


def lane_bcast(x, lane):
    index = jnp.full((SUB, LANE, 1), lane, jnp.int32)
    return lax.gather(x, index, ALONG_LANES, (1, 1), mode=lax.GatherScatterMode.PROMISE_IN_BOUNDS)


def split3(x):
    high = x.astype(BF16)
    rest = x - high.astype(F32)
    mid = rest.astype(BF16)
    return high, mid, (rest - mid.astype(F32)).astype(BF16)


def swap_rows(x, bit, row_id):
    if bit == SUB // 2:
        return pltpu.roll(x, bit, 0)
    return jnp.where((row_id & bit) == 0, pltpu.roll(x, SUB - bit, 0), pltpu.roll(x, bit, 0))


def stack_sums(parts):
    row_id = lax.broadcasted_iota(jnp.int32, (SUB, LANE), 0)
    for bit in (4, 2, 1):
        low = (row_id & bit) == 0
        half = len(parts) // 2
        parts = [
            jnp.where(low, parts[n], parts[n + half]) + swap_rows(jnp.where(low, parts[n + half], parts[n]), bit, row_id)
            for n in range(half)
        ]
    return parts[0]


def eliminate(rows, lane0):
    row_id = lax.broadcasted_iota(jnp.int32, (SUB, LANE), 0)
    rows = [list(rows[0]), list(rows[1])]
    cols = [
        [lane_bcast(rows[0][0], lane0 + j) for j in range(SUB)],
        [lane_bcast(rows[1][0], lane0 + j) for j in range(BASE)],
    ]
    scale = [jnp.zeros((SUB, LANE), F32), jnp.zeros((SUB, LANE), F32)]
    pivot = sub_bcast(cols[0][0], 0)
    for j in range(BASE):
        t, q = divmod(j, SUB)
        inv = lax.rsqrt(pivot)
        scale[t] = jnp.where(row_id == q, inv, scale[t])
        if j + 1 < BASE:
            tn, qn = divmod(j + 1, SUB)
            near = sub_bcast(cols[tn][j], qn) * inv
            pivot = sub_bcast(cols[tn][j + 1], qn) - near * near
        below = cols[1][j] * inv
        here = cols[0][j] * inv if t == 0 else None
        for n in range(j + 1, BASE):
            tn, qn = divmod(n, SUB)
            other = near if n == j + 1 else sub_bcast(here if tn == 0 else below, qn)
            if t == 0 and tn == 0:
                cols[0][n] = cols[0][n] - here * other
            cols[1][n] = cols[1][n] - below * other
        masked = jnp.where(row_id > q, here if t == 0 else below, 0.0)
        for v in range(len(rows[0])):
            pivot_row = sub_bcast(rows[t][v], q) * inv
            rows[t][v] = rows[t][v] - masked * pivot_row
            if t == 0:
                rows[1][v] = rows[1][v] - below * pivot_row
    return [[x * scale[t] for x in rows[t]] for t in range(2)]


def factor_block(work, winv, winv3, prev, fac):
    size = work.shape[1]
    prev[...] = jnp.zeros(prev.shape, F32)
    fac[...] = jnp.zeros(fac.shape, F32)

    def group(v):
        return slice(LANE * v, LANE * (v + 1))

    def pending(factors, before, t, v):
        above, below = before[:SUB, group(v)], before[SUB:, group(v)]
        at = 2 * SUB * t
        return stack_sums([factors[at + n] * above + factors[at + SUB + n] * below for n in range(SUB)])

    for half in range(size // LANE):
        views = [(work, 0), (work, 1), (winv, 0)] if half == 0 else [(work, 1), (winv, 0), (winv, 1)]
        first = half * LANE
        if half == 1:
            factors, before = fac[...], prev[...]
            work[first : first + BASE, group(1)] -= jnp.concatenate([pending(factors, before, t, 1) for t in range(2)], axis=0)
            prev[...] = jnp.concatenate([before[:, group(1)], before[:, group(2)], jnp.zeros((BASE, LANE), F32)], axis=1)

        def body(s, carry, views=views, first=first):
            lane0 = s * BASE
            row0 = pl.multiple_of(first + lane0, BASE)

            here = pl.ds(row0, BASE)
            then = pl.ds(pl.multiple_of(row0 + BASE, BASE), BASE)
            both = [ref[here, group(g)] for ref, g in views]
            rows = [[x[SUB * t : SUB * (t + 1)] for x in both] for t in range(2)]
            factors, before = fac[...], prev[...]
            for t in range(2):
                for v in (1, 2):
                    rows[t][v] = rows[t][v] - pending(factors, before, t, v)
            hi, mid, lo = split3(before)
            lane = lax.broadcasted_iota(jnp.int32, (BASE, size - first), 1) + first
            after = lane >= row0 + BASE
            lhi, lmid, llo = [jnp.where(after, x[:, : size - first], jnp.zeros((), BF16)) for x in (hi, mid, lo)]
            update = lax.dot_general(
                jnp.concatenate([lhi, lhi, lmid, lhi, llo, lmid], axis=0),
                jnp.concatenate([hi, mid, hi, lo, hi, mid], axis=0),
                (((0,), (0,)), ((), ())),
                preferred_element_type=F32,
            )
            for v, (ref, g) in enumerate(views):
                ref[first:size, group(g)] -= update[:, group(v)]
            done = eliminate(rows, lane0)
            if first == 0:
                source = [jnp.where(s == LANE // BASE - 1, done[t][1], done[t][0]) for t in range(2)]
            else:
                source = [done[t][0] for t in range(2)]
            next_lane = (lane0 + BASE) % LANE
            factors, sums = [], []
            for t in range(2):
                factor = [[lane_bcast(source[m], next_lane + SUB * t + n) for n in range(SUB)] for m in range(2)]
                sums.append(stack_sums([factor[0][n] * done[0][0] + factor[1][n] * done[1][0] for n in range(SUB)]))
                factors += factor[0] + factor[1]
            ref, g = views[0]
            ref[then, group(g)] -= jnp.concatenate(sums, axis=0)
            fac[...] = jnp.stack(factors)
            whole = [jnp.concatenate([done[0][v], done[1][v]], axis=0) for v in range(3)]
            prev[...] = jnp.concatenate(whole, axis=1)
            for (ref, g), x in zip(views, whole):
                ref[here, group(g)] = x
                if ref is winv:
                    for n, part in enumerate(split3(x)):
                        winv3[n, here, group(g)] = part
            return carry

        lax.fori_loop(0, LANE // BASE, body, 0, unroll=2)


def kernel(n_row, n_col, batch_axis, a_ref, share, diag, edge, stage, first, panel, work, winv, winv3, prev, fac, load_sem,
           seed_send, seed_recv, edge_send, edge_recv, first_sem, send_sem, pass_sem, down_sem, recv_sem):
    row_blocks, size, local_cols = a_ref.shape
    col_blocks = local_cols // size
    ratio = n_col // n_row
    steps = row_blocks * n_row
    depth = pass_sem.shape[0]
    batch = lax.axis_index(batch_axis)
    row = lax.axis_index("row")
    col = lax.axis_index("col")
    odd = lax.rem(col, 2)
    on_diag = lax.rem(col, n_row) == row
    row_slots = n_row * (row_blocks * (row_blocks + 1) // 2)
    edge_slots = row_slots + n_col * (col_blocks * (col_blocks + 1) // 2)
    leads = row == LEAD

    def at(dev_row, dev_col):
        return (batch, dev_row, dev_col)

    def row_slot(k, a):
        g = k // n_row
        return n_row * (row_blocks * g - (g * (g - 1)) // 2) + (k - g * n_row) * (row_blocks - g) + a - g

    def col_slot(k, b):
        h = k // n_col
        return row_slots + n_col * (col_blocks * h - (h * (h - 1)) // 2) + (k - h * n_col) * (col_blocks - h) + b - h

    def first_a(k):
        return (k + n_row - row) // n_row

    def first_b(k):
        return (k + n_col - col) // n_col

    def spot(a, b, count=1):
        return (a if count == 1 else pl.ds(a, count), slice(None), pl.ds(pl.multiple_of(b * size, size), size))

    def col_of(k, b):
        return jnp.where(on_diag, row_slot(k, ratio * b + col // n_row), col_slot(k, b))

    def edge_slot(k):
        return edge_slots + k

    def edge_reach(ahead):
        return jnp.logical_and(ahead >= 2, jnp.logical_and(ahead <= n_col + LAG - SETTLE, row != LEAD))

    def copy(src_slot, dst_slot, sem, device):
        return pltpu.make_async_remote_copy(
            src_ref=panel.at[src_slot], dst_ref=panel.at[dst_slot], send_sem=sem, recv_sem=recv_sem.at[dst_slot],
            device_id=device, device_id_type=MESH,
        )

    def arrived(slot):
        copy(slot, slot, send_sem.at[0, 0], at(row, col)).wait_recv()

    def start(c):
        c.start()

    def finish(c):
        c.wait_send()

    def from_maker(ahead, way):
        there = lax.rem(row + way, n_row)
        lead_near = jnp.logical_and(there == LEAD, jnp.logical_and(ahead >= 2, ahead <= n_row))
        soon_needed = jnp.logical_and(ahead == 2, way == 2)
        return jnp.logical_or(lead_near, soon_needed)

    def down_column(k, a, maker, sems, act):
        i = a * n_row + row
        slot = row_slot(k, a)
        dst = col_slot(k, i // n_col)
        for m, way in enumerate((1, n_row - 1, 2)):
            direct = from_maker(i - k, way)

            @pl.when(jnp.where(maker, direct, jnp.logical_not(direct)))
            def _():
                act(copy(slot, dst, sems[m], at(lax.rem(row + way, n_row), lax.rem(i, n_col))))

    def last_near(p):
        return first_a(p + 2)

    def to_edge(k, a, sem, act):
        i = a * n_row + row
        act(copy(row_slot(k, a), edge_slot(k), sem, at(LEAD, lax.rem(i - 1, n_col))))

    def source_sends(k, a, act):
        ahead = a * n_row + row - k
        slot = row_slot(k, a)
        early = n_row

        @pl.when(edge_reach(ahead))
        def _():
            to_edge(k, a, send_sem.at[a, 5], act)

        near = jnp.logical_and(ahead >= 2, ahead <= early)

        @pl.when(jnp.logical_or(near, lax.rem(ahead, n_col) == 0))
        def _():
            down_column(k, a, near, [send_sem.at[a, m] for m in range(3)], act)

        @pl.when(jnp.logical_or(jnp.logical_and(odd == 0, ahead >= 2), ahead >= n_col - 1))
        def _():
            act(copy(slot, slot, send_sem.at[a, 3], at(row, lax.rem(jnp.where(odd == 0, col + 1, col - 1), n_col))))

        @pl.when(ahead >= 2)
        def _():
            act(copy(slot, slot, send_sem.at[a, 6], at(row, lax.rem(col - odd + 2, n_col))))

        @pl.when(jnp.logical_and(ahead >= 3 - odd, a <= last_near(k)))
        def _():
            act(copy(slot, slot, send_sem.at[a, 4], at(row, lax.rem(col - odd + 3, n_col))))

        @pl.when(jnp.logical_and(ahead >= n_col // 2 - odd, ahead < n_col - 2 - odd))
        def _():
            act(copy(slot, slot, send_sem.at[a, 7], at(row, lax.rem(col - odd + 5, n_col))))

        @pl.when(ahead >= n_col - 2 - odd)
        def _():
            act(copy(slot, slot, send_sem.at[a, 8], at(row, lax.rem(col - odd - 2 + n_col, n_col))))

    def lead(p):
        return lax.rem(col - lax.rem(p, n_col) + n_col, n_col)

    def hops(p):
        return lax.rem(col // 2 - lax.rem(p, n_col) // 2 + n_col // 2, n_col // 2)

    def passes(p):
        return jnp.where(odd == 1, 2, n_col // 2 - 1) == hops(p)

    def first_passed(p):
        low = jnp.where(jnp.logical_and(passes(p), odd == 1), lead(p) - 1, lead(p))
        return (p + low - row + n_row - 1) // n_row

    def pass_down(p, a, act):
        i = a * n_row + row
        ahead = i - p
        sems = pass_sem.at[lax.rem(p, depth), a]

        @pl.when(jnp.logical_and(odd == 0, jnp.logical_and(lead(p) <= 2, a > last_near(p))))
        def _():
            act(copy(row_slot(p, a), row_slot(p, a), sems.at[0], at(row, col + 1)))

        @pl.when(jnp.logical_and(lax.rem(i, n_col) == col, ahead > 1))
        def _():
            downs = down_sem.at[lax.rem(p, depth), i // n_col]
            down_column(p, a, False, [downs.at[m] for m in range(3)], act)

    def pass_on(p, a, act):
        slot = row_slot(p, a)
        sems = pass_sem.at[lax.rem(p, depth), a]

        @pl.when(passes(p))
        def _():
            @pl.when(odd == 0)
            def _():
                act(copy(slot, slot, sems.at[1], at(row, lax.rem(col - 1 + n_col, n_col))))

            @pl.when(jnp.logical_or(odd == 1, a * n_row + row > p + lead(p)))
            def _():
                act(copy(slot, slot, sems.at[0], at(row, col + 1 - 2 * odd)))

        pass_down(p, a, act)

    def passed(p):
        @pl.when(lead(p) != 0)
        def _():
            loop(first_passed(p), row_blocks, lambda a: pass_on(p, a, finish))

    def receive(p, a):
        arrived(row_slot(p, a))
        pass_down(p, a, start)

    def receive_any(p, a):
        arrived(row_slot(p, a))
        pass_on(p, a, start)

    def loop(lo, hi, fn):
        lax.fori_loop(lo, hi, lambda n, c: (fn(n), c)[1], 0)

    load = pltpu.make_async_copy(a_ref, share, load_sem)
    load.start()

    barrier = pltpu.get_barrier_semaphore()
    n_dev = n_row * n_col

    def greet(n):
        other = lax.rem(row * n_col + col + n, n_dev)
        pl.semaphore_signal(barrier, inc=1, device_id=at(other // n_col, lax.rem(other, n_col)), device_id_type=MESH)

    loop(1, n_dev, greet)
    with jax.named_scope("all_here"):
        pl.semaphore_wait(barrier, n_dev - 1)
    with jax.named_scope("loaded"):
        load.wait()

    def seed_copy(b, dev_row):
        return pltpu.make_async_remote_copy(
            src_ref=share.at[spot(ratio * b + col // n_row, b)], dst_ref=diag.at[b],
            send_sem=seed_send.at[b, lax.rem(dev_row - row + n_row, n_row)],
            recv_sem=seed_recv.at[b], device_id=at(dev_row, col), device_id_type=MESH,
        )

    def hand_out(b):
        @pl.when(on_diag)
        def _():
            for d in (1, n_row - 1, 2):
                seed_copy(b, lax.rem(row + d, n_row)).start()
            diag[b] = share[spot(ratio * b + col // n_row, b)]

        @pl.when(jnp.logical_and(holds_edge(b), jnp.logical_not(leads)))
        def _():
            stage[b] = share[spot((b * n_col + col + 1) // n_row, b)]
            edge_copy(b).start()

    def holds_edge(b):
        j = b * n_col + col
        return jnp.logical_and(lax.rem(j + 1, n_row) == row, j + 1 < steps)

    def edge_copy(b):
        return pltpu.make_async_remote_copy(
            src_ref=stage.at[b], dst_ref=edge.at[b], send_sem=edge_send.at[b], recv_sem=edge_recv.at[b],
            device_id=at(LEAD, col), device_id_type=MESH,
        )

    def has_edge(b):
        from_other = jnp.logical_and(leads, lax.rem(col + 1, n_row) != LEAD)
        return jnp.logical_and(from_other, b * n_col + col + 1 < steps)

    def edge_seeded(b):
        @pl.when(has_edge(b))
        def _():
            edge_copy(b).wait_recv()

    def edge_arrived(p, b):
        j = b * n_col + col

        @pl.when(jnp.logical_and(has_edge(b), j + 1 - p <= n_col + LAG - SETTLE))
        def _():
            arrived(edge_slot(p))

    hand_out(0)
    winv3[...] = jnp.zeros(winv3.shape, BF16)

    def seed_arrived(b):
        @pl.when(jnp.logical_not(on_diag))
        def _():
            seed_copy(b, row).wait_recv()

    with jax.named_scope("seed"):
        seed_arrived(0)

        @pl.when(col != 0)
        def _():
            edge_seeded(0)

    def clear(n):
        a, b = lax.rem(n, row_blocks), n // row_blocks

        @pl.when(a * n_row + row < b * n_col + col)
        def _():
            share[spot(a, b)] = jnp.zeros((size, size), F32)

    loop(0, row_blocks * col_blocks, clear)

    def times_t(x, y):
        return lax.dot_general(x, y, (((1,), (1,)), ((), ())), preferred_element_type=F32)

    def update_block(p, a, b):
        share[spot(a, b)] -= times_t(panel[row_slot(p, a)], panel[col_of(p, b)])

    def update_diag(p, b):
        other = panel[col_of(p, b)]
        diag[b] -= times_t(other, other)

    def update_edge(p, b):
        @pl.when(has_edge(b))
        def _():
            edge[b] -= times_t(panel[edge_slot(p)], panel[col_of(p, b)])

    def column_arrived(p, b):
        @pl.when(jnp.logical_not(on_diag))
        def _():
            arrived(col_slot(p, b))

    def update_column(p, b, lo):
        lone = lax.rem(row_blocks - lo, 2)

        @pl.when(lone == 1)
        def _():
            update_block(p, lo, b)

        def pair(m):
            a = lo + lone + 2 * m
            both = spot(a, b, 2)
            left = panel[pl.ds(row_slot(p, a), 2)].reshape(2 * size, size)
            share[both] -= times_t(left, panel[col_of(p, b)]).reshape(2, size, size)

        loop(0, (row_blocks - lo) // 2, pair)

    def trail(p, b_from, near):
        loop(b_from, col_blocks, lambda b: update_column(p, b, first_a(b * n_col + col - jnp.where(b == near, 0, 1))))

    def columns_arrived(p, b_from):
        def one(b):
            column_arrived(p, b)
            edge_arrived(p, b)

        loop(b_from, col_blocks, one)

    def prepare(b):
        work[size:, :] = jnp.zeros((BASE, size), F32)
        r_id = lax.broadcasted_iota(jnp.int32, (size + BASE, size), 0)
        c_id = lax.broadcasted_iota(jnp.int32, (size + BASE, size), 1)
        winv[...] = jnp.where(r_id == c_id, 1.0, 0.0).astype(F32)

    def times_winv_t(x):
        hi, mid, lo = split3(x)
        whi, wmid, wlo = winv3[0], winv3[1], winv3[2]
        small = times_t(lo, whi) + times_t(mid, wmid) + times_t(hi, wlo)
        return small + (times_t(mid, whi) + times_t(hi, wmid)) + times_t(hi, whi)

    def here_diag(k):
        return row == lax.rem(k, n_row)

    def solve(k, a, count):
        kb = k // n_col
        near = jnp.logical_and(a == first_a(k), jnp.logical_not(here_diag(k)))
        here = spot(a, kb, count)

        def shaped(x):
            return x if count == 1 else x.reshape(count, size, size)

        def apply(p):
            left = panel[pl.ds(row_slot(p, a), count)].reshape(count * size, size)
            share[here] -= shaped(times_t(left, panel[col_of(p, kb)]))

        @pl.when(jnp.logical_not(near))
        def _():
            for m in range(count):

                @pl.when(k >= 3)
                def _():
                    receive(k - 3, a + m)

                @pl.when(k >= 2)
                def _():
                    receive(k - 2, a + m)

            loop(jnp.maximum(k - 2 - LAG, 0), k - 1, apply)

        @pl.when(k > 0)
        def _():
            for m in range(count):
                receive(k - 1, a + m)
            apply(k - 1)

        x = times_winv_t(share[here].reshape(count * size, size))
        panel[pl.ds(row_slot(k, a), count)] = x.astype(BF16).reshape(count, size, size)
        share[here] = shaped(x)
        if count == 1:

            @pl.when(jnp.logical_and(near, jnp.logical_and(leads, lax.rem(k + 1, n_row) == LEAD)))
            def _():
                first[...] = panel[row_slot(k, a)]
                first_out(k, start)

        if count == 1:
            source_sends(k, a, start)
        else:
            loop(a, a + count, lambda n: source_sends(k, n, start))

    def update_near(p, b):
        update_diag(p, b)
        update_edge(p, b)

    def first_slot(k, dev_row):
        return jnp.where(lax.rem(k + 1, n_row) == dev_row, row_slot(k, (k + 1) // n_row), col_slot(k, (k + 1) // n_col))

    def first_copy(k, dev_row, sem):
        dst = first_slot(k, dev_row)
        return pltpu.make_async_remote_copy(
            src_ref=first, dst_ref=panel.at[dst], send_sem=sem, recv_sem=recv_sem.at[dst],
            device_id=at(dev_row, lax.rem(col + 1, n_col)), device_id_type=MESH,
        )

    def others_first(k, fn):
        urgent = lax.rem(k + 3, n_row)
        lone = urgent == LEAD
        for m in range(n_row - 1):
            fn(m, lax.rem(jnp.where(lone, LEAD + 1, urgent) + m + jnp.where(lax.rem(jnp.where(lone, LEAD + 1, urgent) - LEAD + n_row, n_row) + m >= n_row, 1, 0), n_row))

    def first_out(k, act):
        act(first_copy(k, LEAD, first_sem.at[0, 0]))

        @pl.when(odd == 0)
        def _():
            others_first(k, lambda m, r: act(first_copy(k, r, first_sem.at[0, 1 + m])))

    def first_down(k, act):
        @pl.when(odd == 0)
        def _():
            others_first(k, lambda m, r: act(copy(first_slot(k, LEAD), first_slot(k, r), first_sem.at[1, 1 + m], at(r, col))))

    def firsts_done(k):
        @pl.when(jnp.logical_and(leads, k + 1 < steps))
        def _():
            first_out(k, finish)

        @pl.when(jnp.logical_and(leads, k > 0))
        def _():
            first_down(k - 1, finish)

    @pl.when(col == 0)
    def _():
        prepare(0)
        work[0:size, :] = diag[0]

    def step(k):
        mine = jnp.logical_and(col == lax.rem(k, n_col), k < steps)
        kb = k // n_col
        last = k - 1
        soon = jnp.logical_and(col == lax.rem(k + 1, n_col), k + 1 < steps)

        @pl.when(mine)
        def _():
            with jax.named_scope("factor"):
                factor_block(work, winv, winv3, prev, fac)

            @pl.when(has_edge(kb))
            def _():
                with jax.named_scope("lead"):

                    @pl.when(k == 0)
                    def _():
                        edge_seeded(kb)

                    @pl.when(k > 0)
                    def _():
                        edge_arrived(last, kb)
                        update_edge(last, kb)

                    first[...] = times_winv_t(edge[kb]).astype(BF16)
                    first_out(k, start)

            lo = first_a(k)
            second = jnp.minimum(lo + 1, row_blocks)
            third = second + lax.rem(row_blocks - second, 2)
            with jax.named_scope("solve_near"):
                loop(lo, third, lambda a: solve(k, a, 1))
            with jax.named_scope("solve_two"):
                loop(0, (row_blocks - third) // 2, lambda m: solve(k, third + 2 * m, 2))

        @pl.when(k >= depth)
        def _():
            with jax.named_scope("passed"):
                passed(k - depth)

        @pl.when(mine)
        def _():
            @pl.when(row == lax.rem(k, n_row))
            def _():
                for d in range(1, n_row):
                    seed_copy(kb, lax.rem(row + d, n_row)).wait_send()
                r_id = lax.broadcasted_iota(jnp.int32, (size, size), 0)
                c_id = lax.broadcasted_iota(jnp.int32, (size, size), 1)
                share[spot(k // n_row, kb)] = jnp.where(r_id >= c_id, work[0:size, :].T, 0.0)

        @pl.when(jnp.logical_and(k > 0, jnp.logical_not(jnp.logical_or(mine, soon))))
        def _():
            @pl.when(col != lax.rem(last, n_col))
            def _():
                with jax.named_scope("receive"):
                    end = jnp.where(lead(last) == 3, jnp.minimum(last_near(last) + 1, row_blocks), row_blocks)
                    loop(first_passed(last), end, lambda a: receive_any(last, a))

            near = first_b(k)
            age = k + n_col - (near * n_col + col)
            settle = jnp.logical_and(age == SETTLE, jnp.logical_and(near > 0, near < col_blocks))

            @pl.when(settle)
            def _():
                with jax.named_scope("late_trail"):
                    own = k - SETTLE

                    for back in (LAG + 2, LAG + 1, LAG):

                        @pl.when(own >= back)
                        def _():
                            columns_arrived(own - back, near)

                    loop(jnp.maximum(own - 2 - LAG, 0), own - LAG + 1, lambda p: trail(p, near, -1))

            @pl.when(jnp.logical_and(k >= LAG, lead(last) != 3))
            def _():
                p = k - LAG
                with jax.named_scope("columns"):
                    columns_arrived(p, near)

                @pl.when(jnp.logical_and(near < col_blocks, age >= SETTLE + 2))
                def _():
                    @pl.when(jnp.logical_and(age == SETTLE + 2, near > 0))
                    def _():
                        with jax.named_scope("seed_late"):
                            seed_arrived(near)
                            edge_seeded(near)

                    oldest = jnp.where(age == SETTLE + 2, jnp.maximum(p - 1, 0), p)
                    loop(oldest, p + 1, lambda q: update_near(q, near))

                with jax.named_scope("trail"):
                    trail(p, near, jnp.where(jnp.logical_or(age > SETTLE, near == 0), near, -1))

            @pl.when(settle)
            def _():
                hand_out(near)

        @pl.when(soon)
        def _():
            nb = (k + 1) // n_col

            oldest = jnp.maximum(k - 1 - LAG, 0)
            lo = first_a(k + 1)

            def old_diag(p):
                column_arrived(p, nb)
                edge_arrived(p, nb)
                update_near(p, nb)

            def take(a):
                receive(last, a)

                @pl.when(jnp.logical_not(here_diag(k + 1)))
                def _():
                    loop(oldest, last, lambda p: update_block(p, a, nb))

            @pl.when(k > 0)
            def _():
                with jax.named_scope("old_diag"):
                    loop(oldest, last, old_diag)
                with jax.named_scope("take"):
                    loop(first_a(k), jnp.minimum(first_a(k) + 1, row_blocks), take)
                with jax.named_scope("take_column"):
                    column_arrived(last, nb)
                    edge_arrived(last, nb)
                with jax.named_scope("catch_up"):
                    update_near(last, nb)
                    @pl.when(jnp.logical_and(jnp.logical_not(here_diag(k + 1)), lo < row_blocks))
                    def _():
                        update_block(last, lo, nb)

            prepare(nb)
            slot = col_of(k, nb)
            with jax.named_scope("first_block"):
                arrived(slot)

            @pl.when(leads)
            def _():
                first_down(k, start)

            other = panel[slot]
            work[0:size, :] = diag[nb] - times_t(other, other)

        @pl.when(jnp.logical_and(k >= n_col // 2, col == lax.rem(k + n_col // 2, n_col)))
        def _():
            with jax.named_scope("sends_done"):
                firsts_done(k - n_col // 2)
                loop(first_a(k - n_col // 2), row_blocks, lambda a: source_sends(k - n_col // 2, a, finish))

    loop(0, steps + n_col // 2, step)

    def edges_done(b):
        @pl.when(jnp.logical_and(holds_edge(b), jnp.logical_not(leads)))
        def _():
            edge_copy(b).wait_send()

    loop(0, col_blocks, edges_done)


def solution(mesh):
    n_row = mesh.shape["row"]
    n_col = mesh.shape["col"]

    def factor_local(a_loc):
        row_blocks, size, local_cols = a_loc.shape
        col_blocks = local_cols // size
        slots = n_row * (row_blocks * (row_blocks + 1) // 2) + n_col * (col_blocks * (col_blocks + 1) // 2)
        slots += row_blocks * n_row
        return pl.pallas_call(
            functools.partial(kernel, n_row, n_col, "batch"),
            out_shape=pltpu.VMEM(a_loc.shape, F32),
            in_specs=[pl.BlockSpec(memory_space=pl.ANY)],
            scratch_shapes=[
                pltpu.VMEM((col_blocks, size, size), F32),
                pltpu.VMEM((col_blocks, size, size), F32),
                pltpu.VMEM((col_blocks, size, size), F32),
                pltpu.VMEM((size, size), BF16),
                pltpu.VMEM((slots, size, size), BF16),
                pltpu.VMEM((size + BASE, size), F32),
                pltpu.VMEM((size + BASE, size), F32),
                pltpu.VMEM((3, size, size), BF16),
                pltpu.VMEM((BASE, 3 * LANE), F32),
                pltpu.VMEM((4 * SUB, SUB, LANE), F32),
                pltpu.SemaphoreType.DMA,
                pltpu.SemaphoreType.DMA((col_blocks, n_row)),
                pltpu.SemaphoreType.DMA((col_blocks,)),
                pltpu.SemaphoreType.DMA((col_blocks,)),
                pltpu.SemaphoreType.DMA((col_blocks,)),
                pltpu.SemaphoreType.DMA((2, n_row)),
                pltpu.SemaphoreType.DMA((row_blocks, 9)),
                pltpu.SemaphoreType.DMA((4, row_blocks, 2)),
                pltpu.SemaphoreType.DMA((4, col_blocks, 3)),
                pltpu.SemaphoreType.DMA((slots,)),
            ],
            compiler_params=pltpu.CompilerParams(
                collective_id=0, has_side_effects=True, vmem_limit_bytes=50 * 1024 * 1024
            ),
            name="cholesky",
        )(a_loc)

    blk_spec = P(("batch", "row"), None, "col")
    return jax.shard_map(factor_local, mesh=mesh, in_specs=(blk_spec,), out_specs=blk_spec, check_vma=False)
```

```python
import functools

import jax
import jax.numpy as jnp
from jax import lax
from jax.experimental import pallas as pl
from jax.experimental.pallas import tpu as pltpu
from jax.sharding import PartitionSpec as P

F32 = jnp.float32
BF16 = jnp.bfloat16
MESH = pl.DeviceIdType.MESH
SUB = 8
LANE = 128
BASE = 16
LEAD = 1
SETTLE = 3
LAG = 3


def sub_bcast(x, q):
    return jnp.broadcast_to(x[q : q + 1, :], (SUB, LANE))


ALONG_LANES = lax.GatherDimensionNumbers(
    offset_dims=(), collapsed_slice_dims=(1,), start_index_map=(1,), operand_batching_dims=(0,), start_indices_batching_dims=(0,)
)


def lane_bcast(x, lane):
    index = jnp.full((SUB, LANE, 1), lane, jnp.int32)
    return lax.gather(x, index, ALONG_LANES, (1, 1), mode=lax.GatherScatterMode.PROMISE_IN_BOUNDS)


def split3(x):
    high = x.astype(BF16)
    rest = x - high.astype(F32)
    mid = rest.astype(BF16)
    return high, mid, (rest - mid.astype(F32)).astype(BF16)


def swap_rows(x, bit, row_id):
    if bit == SUB // 2:
        return pltpu.roll(x, bit, 0)
    return jnp.where((row_id & bit) == 0, pltpu.roll(x, SUB - bit, 0), pltpu.roll(x, bit, 0))


def stack_sums(parts):
    row_id = lax.broadcasted_iota(jnp.int32, (SUB, LANE), 0)
    for bit in (4, 2, 1):
        low = (row_id & bit) == 0
        half = len(parts) // 2
        parts = [
            jnp.where(low, parts[n], parts[n + half]) + swap_rows(jnp.where(low, parts[n + half], parts[n]), bit, row_id)
            for n in range(half)
        ]
    return parts[0]


def eliminate(rows, lane0):
    row_id = lax.broadcasted_iota(jnp.int32, (SUB, LANE), 0)
    rows = [list(rows[0]), list(rows[1])]
    cols = [
        [lane_bcast(rows[0][0], lane0 + j) for j in range(SUB)],
        [lane_bcast(rows[1][0], lane0 + j) for j in range(BASE)],
    ]
    scale = [jnp.zeros((SUB, LANE), F32), jnp.zeros((SUB, LANE), F32)]
    pivot = sub_bcast(cols[0][0], 0)
    for j in range(BASE):
        t, q = divmod(j, SUB)
        inv = lax.rsqrt(pivot)
        scale[t] = jnp.where(row_id == q, inv, scale[t])
        if j + 1 < BASE:
            tn, qn = divmod(j + 1, SUB)
            near = sub_bcast(cols[tn][j], qn) * inv
            pivot = sub_bcast(cols[tn][j + 1], qn) - near * near
        below = cols[1][j] * inv
        here = cols[0][j] * inv if t == 0 else None
        for n in range(j + 1, BASE):
            tn, qn = divmod(n, SUB)
            other = near if n == j + 1 else sub_bcast(here if tn == 0 else below, qn)
            if t == 0 and tn == 0:
                cols[0][n] = cols[0][n] - here * other
            cols[1][n] = cols[1][n] - below * other
        masked = jnp.where(row_id > q, here if t == 0 else below, 0.0)
        for v in range(len(rows[0])):
            pivot_row = sub_bcast(rows[t][v], q) * inv
            rows[t][v] = rows[t][v] - masked * pivot_row
            if t == 0:
                rows[1][v] = rows[1][v] - below * pivot_row
    return [[x * scale[t] for x in rows[t]] for t in range(2)]


def factor_block(work, winv, winv3, prev, fac):
    size = work.shape[1]
    prev[...] = jnp.zeros(prev.shape, F32)
    fac[...] = jnp.zeros(fac.shape, F32)

    def group(v):
        return slice(LANE * v, LANE * (v + 1))

    def pending(factors, before, t, v):
        above, below = before[:SUB, group(v)], before[SUB:, group(v)]
        at = 2 * SUB * t
        return stack_sums([factors[at + n] * above + factors[at + SUB + n] * below for n in range(SUB)])

    for half in range(size // LANE):
        views = [(work, 0), (work, 1), (winv, 0)] if half == 0 else [(work, 1), (winv, 0), (winv, 1)]
        first = half * LANE
        if half == 1:
            factors, before = fac[...], prev[...]
            work[first : first + BASE, group(1)] -= jnp.concatenate([pending(factors, before, t, 1) for t in range(2)], axis=0)
            prev[...] = jnp.concatenate([before[:, group(1)], before[:, group(2)], jnp.zeros((BASE, LANE), F32)], axis=1)

        def body(s, carry, views=views, first=first):
            lane0 = s * BASE
            row0 = pl.multiple_of(first + lane0, BASE)

            here = pl.ds(row0, BASE)
            then = pl.ds(pl.multiple_of(row0 + BASE, BASE), BASE)
            both = [ref[here, group(g)] for ref, g in views]
            rows = [[x[SUB * t : SUB * (t + 1)] for x in both] for t in range(2)]
            factors, before = fac[...], prev[...]
            for t in range(2):
                for v in (1, 2):
                    rows[t][v] = rows[t][v] - pending(factors, before, t, v)
            hi, mid, lo = split3(before)
            lane = lax.broadcasted_iota(jnp.int32, (BASE, size - first), 1) + first
            after = lane >= row0 + BASE
            lhi, lmid, llo = [jnp.where(after, x[:, : size - first], jnp.zeros((), BF16)) for x in (hi, mid, lo)]
            update = lax.dot_general(
                jnp.concatenate([lhi, lhi, lmid, lhi, llo, lmid], axis=0),
                jnp.concatenate([hi, mid, hi, lo, hi, mid], axis=0),
                (((0,), (0,)), ((), ())),
                preferred_element_type=F32,
            )
            for v, (ref, g) in enumerate(views):
                ref[first:size, group(g)] -= update[:, group(v)]
            done = eliminate(rows, lane0)
            if first == 0:
                source = [jnp.where(s == LANE // BASE - 1, done[t][1], done[t][0]) for t in range(2)]
            else:
                source = [done[t][0] for t in range(2)]
            next_lane = (lane0 + BASE) % LANE
            factors, sums = [], []
            for t in range(2):
                factor = [[lane_bcast(source[m], next_lane + SUB * t + n) for n in range(SUB)] for m in range(2)]
                sums.append(stack_sums([factor[0][n] * done[0][0] + factor[1][n] * done[1][0] for n in range(SUB)]))
                factors += factor[0] + factor[1]
            ref, g = views[0]
            ref[then, group(g)] -= jnp.concatenate(sums, axis=0)
            fac[...] = jnp.stack(factors)
            whole = [jnp.concatenate([done[0][v], done[1][v]], axis=0) for v in range(3)]
            prev[...] = jnp.concatenate(whole, axis=1)
            for (ref, g), x in zip(views, whole):
                ref[here, group(g)] = x
                if ref is winv:
                    for n, part in enumerate(split3(x)):
                        winv3[n, here, group(g)] = part
            return carry

        lax.fori_loop(0, LANE // BASE, body, 0, unroll=2)


def kernel(n_row, n_col, batch_axis, a_ref, share, diag, edge, stage, first, panel, work, winv, winv3, prev, fac, load_sem,
           seed_send, seed_recv, edge_send, edge_recv, first_sem, send_sem, pass_sem, down_sem, recv_sem):
    row_blocks, size, local_cols = a_ref.shape
    col_blocks = local_cols // size
    ratio = n_col // n_row
    steps = row_blocks * n_row
    depth = pass_sem.shape[0]
    batch = lax.axis_index(batch_axis)
    row = lax.axis_index("row")
    col = lax.axis_index("col")
    odd = lax.rem(col, 2)
    on_diag = lax.rem(col, n_row) == row
    row_slots = n_row * (row_blocks * (row_blocks + 1) // 2)
    edge_slots = row_slots + n_col * (col_blocks * (col_blocks + 1) // 2)
    leads = row == LEAD

    def at(dev_row, dev_col):
        return (batch, dev_row, dev_col)

    def row_slot(k, a):
        g = k // n_row
        return n_row * (row_blocks * g - (g * (g - 1)) // 2) + (k - g * n_row) * (row_blocks - g) + a - g

    def col_slot(k, b):
        h = k // n_col
        return row_slots + n_col * (col_blocks * h - (h * (h - 1)) // 2) + (k - h * n_col) * (col_blocks - h) + b - h

    def first_a(k):
        return (k + n_row - row) // n_row

    def first_b(k):
        return (k + n_col - col) // n_col

    def spot(a, b, count=1):
        return (a if count == 1 else pl.ds(a, count), slice(None), pl.ds(pl.multiple_of(b * size, size), size))

    def col_of(k, b):
        return jnp.where(on_diag, row_slot(k, ratio * b + col // n_row), col_slot(k, b))

    def edge_slot(k):
        return edge_slots + k

    def edge_reach(ahead):
        return jnp.logical_and(ahead >= 2, jnp.logical_and(ahead <= n_col + LAG - SETTLE, row != LEAD))

    def copy(src_slot, dst_slot, sem, device):
        return pltpu.make_async_remote_copy(
            src_ref=panel.at[src_slot], dst_ref=panel.at[dst_slot], send_sem=sem, recv_sem=recv_sem.at[dst_slot],
            device_id=device, device_id_type=MESH,
        )

    def arrived(slot):
        copy(slot, slot, send_sem.at[0, 0], at(row, col)).wait_recv()

    def start(c):
        c.start()

    def finish(c):
        c.wait_send()

    def from_maker(ahead, way):
        there = lax.rem(row + way, n_row)
        lead_near = jnp.logical_and(there == LEAD, jnp.logical_and(ahead >= 2, ahead <= n_row))
        soon_needed = jnp.logical_and(jnp.logical_and(ahead >= 2, ahead <= 3), way == 2)
        return jnp.logical_or(lead_near, soon_needed)

    def down_column(k, a, maker, sems, act):
        i = a * n_row + row
        slot = row_slot(k, a)
        dst = col_slot(k, i // n_col)
        for m, way in enumerate((1, n_row - 1, 2)):
            direct = from_maker(i - k, way)

            @pl.when(jnp.where(maker, direct, jnp.logical_not(direct)))
            def _():
                act(copy(slot, dst, sems[m], at(lax.rem(row + way, n_row), lax.rem(i, n_col))))

    def last_near(p):
        return first_a(p + 2)

    def to_edge(k, a, sem, act):
        i = a * n_row + row
        act(copy(row_slot(k, a), edge_slot(k), sem, at(LEAD, lax.rem(i - 1, n_col))))

    def source_sends(k, a, act):
        ahead = a * n_row + row - k
        slot = row_slot(k, a)
        early = n_row

        @pl.when(edge_reach(ahead))
        def _():
            to_edge(k, a, send_sem.at[a, 5], act)

        near = jnp.logical_and(ahead >= 2, ahead <= early)

        @pl.when(jnp.logical_or(near, lax.rem(ahead, n_col) == 0))
        def _():
            down_column(k, a, near, [send_sem.at[a, m] for m in range(3)], act)

        @pl.when(jnp.logical_or(jnp.logical_and(odd == 0, ahead >= 2), ahead >= n_col - 1))
        def _():
            act(copy(slot, slot, send_sem.at[a, 3], at(row, lax.rem(jnp.where(odd == 0, col + 1, col - 1), n_col))))

        @pl.when(ahead >= 2)
        def _():
            act(copy(slot, slot, send_sem.at[a, 6], at(row, lax.rem(col - odd + 2, n_col))))

        @pl.when(jnp.logical_and(ahead >= 3 - odd, a <= last_near(k)))
        def _():
            act(copy(slot, slot, send_sem.at[a, 4], at(row, lax.rem(col - odd + 3, n_col))))

        @pl.when(jnp.logical_and(ahead >= n_col // 2 - odd, ahead < n_col - 2 - odd))
        def _():
            act(copy(slot, slot, send_sem.at[a, 7], at(row, lax.rem(col - odd + 5, n_col))))

        @pl.when(ahead >= n_col - 2 - odd)
        def _():
            act(copy(slot, slot, send_sem.at[a, 8], at(row, lax.rem(col - odd - 2 + n_col, n_col))))

    def lead(p):
        return lax.rem(col - lax.rem(p, n_col) + n_col, n_col)

    def hops(p):
        return lax.rem(col // 2 - lax.rem(p, n_col) // 2 + n_col // 2, n_col // 2)

    def passes(p):
        return jnp.where(odd == 1, 2, n_col // 2 - 1) == hops(p)

    def first_passed(p):
        low = jnp.where(jnp.logical_and(passes(p), odd == 1), lead(p) - 1, lead(p))
        return (p + low - row + n_row - 1) // n_row

    def pass_down(p, a, act):
        i = a * n_row + row
        ahead = i - p
        sems = pass_sem.at[lax.rem(p, depth), a]

        @pl.when(jnp.logical_and(odd == 0, jnp.logical_and(lead(p) <= 2, a > last_near(p))))
        def _():
            act(copy(row_slot(p, a), row_slot(p, a), sems.at[0], at(row, col + 1)))

        @pl.when(jnp.logical_and(lax.rem(i, n_col) == col, ahead > 1))
        def _():
            downs = down_sem.at[lax.rem(p, depth), i // n_col]
            down_column(p, a, False, [downs.at[m] for m in range(3)], act)

    def pass_on(p, a, act):
        slot = row_slot(p, a)
        sems = pass_sem.at[lax.rem(p, depth), a]

        @pl.when(passes(p))
        def _():
            @pl.when(odd == 0)
            def _():
                act(copy(slot, slot, sems.at[1], at(row, lax.rem(col - 1 + n_col, n_col))))

            @pl.when(jnp.logical_or(odd == 1, a * n_row + row > p + lead(p)))
            def _():
                act(copy(slot, slot, sems.at[0], at(row, col + 1 - 2 * odd)))

        pass_down(p, a, act)

    def passed(p):
        @pl.when(lead(p) != 0)
        def _():
            loop(first_passed(p), row_blocks, lambda a: pass_on(p, a, finish))

    def receive(p, a):
        arrived(row_slot(p, a))
        pass_down(p, a, start)

    def receive_any(p, a):
        arrived(row_slot(p, a))
        pass_on(p, a, start)

    def loop(lo, hi, fn):
        lax.fori_loop(lo, hi, lambda n, c: (fn(n), c)[1], 0)

    load = pltpu.make_async_copy(a_ref, share, load_sem)
    load.start()

    barrier = pltpu.get_barrier_semaphore()
    n_dev = n_row * n_col

    def greet(n):
        other = lax.rem(row * n_col + col + n, n_dev)
        pl.semaphore_signal(barrier, inc=1, device_id=at(other // n_col, lax.rem(other, n_col)), device_id_type=MESH)

    loop(1, n_dev, greet)
    with jax.named_scope("all_here"):
        pl.semaphore_wait(barrier, n_dev - 1)
    with jax.named_scope("loaded"):
        load.wait()

    def seed_copy(b, dev_row):
        return pltpu.make_async_remote_copy(
            src_ref=share.at[spot(ratio * b + col // n_row, b)], dst_ref=diag.at[b],
            send_sem=seed_send.at[b, lax.rem(dev_row - row + n_row, n_row)],
            recv_sem=seed_recv.at[b], device_id=at(dev_row, col), device_id_type=MESH,
        )

    def hand_out(b):
        @pl.when(on_diag)
        def _():
            for d in (1, n_row - 1, 2):
                seed_copy(b, lax.rem(row + d, n_row)).start()
            diag[b] = share[spot(ratio * b + col // n_row, b)]

        @pl.when(jnp.logical_and(holds_edge(b), jnp.logical_not(leads)))
        def _():
            stage[b] = share[spot((b * n_col + col + 1) // n_row, b)]
            edge_copy(b).start()

    def holds_edge(b):
        j = b * n_col + col
        return jnp.logical_and(lax.rem(j + 1, n_row) == row, j + 1 < steps)

    def edge_copy(b):
        return pltpu.make_async_remote_copy(
            src_ref=stage.at[b], dst_ref=edge.at[b], send_sem=edge_send.at[b], recv_sem=edge_recv.at[b],
            device_id=at(LEAD, col), device_id_type=MESH,
        )

    def has_edge(b):
        from_other = jnp.logical_and(leads, lax.rem(col + 1, n_row) != LEAD)
        return jnp.logical_and(from_other, b * n_col + col + 1 < steps)

    def edge_seeded(b):
        @pl.when(has_edge(b))
        def _():
            edge_copy(b).wait_recv()

    def edge_arrived(p, b):
        j = b * n_col + col

        @pl.when(jnp.logical_and(has_edge(b), j + 1 - p <= n_col + LAG - SETTLE))
        def _():
            arrived(edge_slot(p))

    hand_out(0)
    winv3[...] = jnp.zeros(winv3.shape, BF16)

    def seed_arrived(b):
        @pl.when(jnp.logical_not(on_diag))
        def _():
            seed_copy(b, row).wait_recv()

    with jax.named_scope("seed"):
        seed_arrived(0)

        @pl.when(col != 0)
        def _():
            edge_seeded(0)

    def clear(n):
        a, b = lax.rem(n, row_blocks), n // row_blocks

        @pl.when(a * n_row + row < b * n_col + col)
        def _():
            share[spot(a, b)] = jnp.zeros((size, size), F32)

    loop(0, row_blocks * col_blocks, clear)

    def times_t(x, y):
        return lax.dot_general(x, y, (((1,), (1,)), ((), ())), preferred_element_type=F32)

    def update_block(p, a, b):
        share[spot(a, b)] -= times_t(panel[row_slot(p, a)], panel[col_of(p, b)])

    def update_diag(p, b):
        other = panel[col_of(p, b)]
        diag[b] -= times_t(other, other)

    def update_edge(p, b):
        @pl.when(has_edge(b))
        def _():
            edge[b] -= times_t(panel[edge_slot(p)], panel[col_of(p, b)])

    def column_arrived(p, b):
        @pl.when(jnp.logical_not(on_diag))
        def _():
            arrived(col_slot(p, b))

    def update_column(p, b, lo):
        lone = lax.rem(row_blocks - lo, 2)

        @pl.when(lone == 1)
        def _():
            update_block(p, lo, b)

        def pair(m):
            a = lo + lone + 2 * m
            both = spot(a, b, 2)
            left = panel[pl.ds(row_slot(p, a), 2)].reshape(2 * size, size)
            share[both] -= times_t(left, panel[col_of(p, b)]).reshape(2, size, size)

        loop(0, (row_blocks - lo) // 2, pair)

    def trail(p, b_from, near):
        loop(b_from, col_blocks, lambda b: update_column(p, b, first_a(b * n_col + col - jnp.where(b == near, 0, 1))))

    def columns_arrived(p, b_from):
        def one(b):
            column_arrived(p, b)
            edge_arrived(p, b)

        loop(b_from, col_blocks, one)

    def prepare(b):
        work[size:, :] = jnp.zeros((BASE, size), F32)
        r_id = lax.broadcasted_iota(jnp.int32, (size + BASE, size), 0)
        c_id = lax.broadcasted_iota(jnp.int32, (size + BASE, size), 1)
        winv[...] = jnp.where(r_id == c_id, 1.0, 0.0).astype(F32)

    def times_winv_t(x):
        hi, mid, lo = split3(x)
        whi, wmid, wlo = winv3[0], winv3[1], winv3[2]
        small = times_t(lo, whi) + times_t(mid, wmid) + times_t(hi, wlo)
        return small + (times_t(mid, whi) + times_t(hi, wmid)) + times_t(hi, whi)

    def here_diag(k):
        return row == lax.rem(k, n_row)

    def solve(k, a, count):
        kb = k // n_col
        near = jnp.logical_and(a == first_a(k), jnp.logical_not(here_diag(k)))
        here = spot(a, kb, count)

        def shaped(x):
            return x if count == 1 else x.reshape(count, size, size)

        def apply(p):
            left = panel[pl.ds(row_slot(p, a), count)].reshape(count * size, size)
            share[here] -= shaped(times_t(left, panel[col_of(p, kb)]))

        @pl.when(jnp.logical_not(near))
        def _():
            for m in range(count):

                @pl.when(k >= 3)
                def _():
                    receive(k - 3, a + m)

                @pl.when(k >= 2)
                def _():
                    receive(k - 2, a + m)

            loop(jnp.maximum(k - 2 - LAG, 0), k - 1, apply)

        @pl.when(k > 0)
        def _():
            for m in range(count):
                receive(k - 1, a + m)
            apply(k - 1)

        x = times_winv_t(share[here].reshape(count * size, size))
        panel[pl.ds(row_slot(k, a), count)] = x.astype(BF16).reshape(count, size, size)
        share[here] = shaped(x)
        if count == 1:

            @pl.when(jnp.logical_and(near, jnp.logical_and(leads, lax.rem(k + 1, n_row) == LEAD)))
            def _():
                first[...] = panel[row_slot(k, a)]
                first_out(k, start)

        if count == 1:
            source_sends(k, a, start)
        else:
            loop(a, a + count, lambda n: source_sends(k, n, start))

    def update_near(p, b):
        update_diag(p, b)
        update_edge(p, b)

    def first_slot(k, dev_row):
        return jnp.where(lax.rem(k + 1, n_row) == dev_row, row_slot(k, (k + 1) // n_row), col_slot(k, (k + 1) // n_col))

    def first_copy(k, dev_row, sem):
        dst = first_slot(k, dev_row)
        return pltpu.make_async_remote_copy(
            src_ref=first, dst_ref=panel.at[dst], send_sem=sem, recv_sem=recv_sem.at[dst],
            device_id=at(dev_row, lax.rem(col + 1, n_col)), device_id_type=MESH,
        )

    def others_first(k, fn):
        urgent = lax.rem(k + 3, n_row)
        lone = urgent == LEAD
        for m in range(n_row - 1):
            fn(m, lax.rem(jnp.where(lone, LEAD + 1, urgent) + m + jnp.where(lax.rem(jnp.where(lone, LEAD + 1, urgent) - LEAD + n_row, n_row) + m >= n_row, 1, 0), n_row))

    def first_out(k, act):
        act(first_copy(k, LEAD, first_sem.at[0, 0]))

        @pl.when(odd == 0)
        def _():
            others_first(k, lambda m, r: act(first_copy(k, r, first_sem.at[0, 1 + m])))

    def first_down(k, act):
        @pl.when(odd == 0)
        def _():
            others_first(k, lambda m, r: act(copy(first_slot(k, LEAD), first_slot(k, r), first_sem.at[1, 1 + m], at(r, col))))

    def firsts_done(k):
        @pl.when(jnp.logical_and(leads, k + 1 < steps))
        def _():
            first_out(k, finish)

        @pl.when(jnp.logical_and(leads, k > 0))
        def _():
            first_down(k - 1, finish)

    @pl.when(col == 0)
    def _():
        prepare(0)
        work[0:size, :] = diag[0]

    def step(k):
        mine = jnp.logical_and(col == lax.rem(k, n_col), k < steps)
        kb = k // n_col
        last = k - 1
        soon = jnp.logical_and(col == lax.rem(k + 1, n_col), k + 1 < steps)

        @pl.when(mine)
        def _():
            with jax.named_scope("factor"):
                factor_block(work, winv, winv3, prev, fac)

            @pl.when(has_edge(kb))
            def _():
                with jax.named_scope("lead"):

                    @pl.when(k == 0)
                    def _():
                        edge_seeded(kb)

                    @pl.when(k > 0)
                    def _():
                        edge_arrived(last, kb)
                        update_edge(last, kb)

                    first[...] = times_winv_t(edge[kb]).astype(BF16)
                    first_out(k, start)

            lo = first_a(k)
            second = jnp.minimum(lo + 1, row_blocks)
            third = second + lax.rem(row_blocks - second, 2)
            with jax.named_scope("solve_near"):
                loop(lo, third, lambda a: solve(k, a, 1))
            with jax.named_scope("solve_two"):
                loop(0, (row_blocks - third) // 2, lambda m: solve(k, third + 2 * m, 2))

        @pl.when(k >= depth)
        def _():
            with jax.named_scope("passed"):
                passed(k - depth)

        @pl.when(mine)
        def _():
            @pl.when(row == lax.rem(k, n_row))
            def _():
                for d in range(1, n_row):
                    seed_copy(kb, lax.rem(row + d, n_row)).wait_send()
                r_id = lax.broadcasted_iota(jnp.int32, (size, size), 0)
                c_id = lax.broadcasted_iota(jnp.int32, (size, size), 1)
                share[spot(k // n_row, kb)] = jnp.where(r_id >= c_id, work[0:size, :].T, 0.0)

        @pl.when(jnp.logical_and(k > 0, jnp.logical_not(jnp.logical_or(mine, soon))))
        def _():
            @pl.when(col != lax.rem(last, n_col))
            def _():
                with jax.named_scope("receive"):
                    end = jnp.where(lead(last) == 3, jnp.minimum(last_near(last) + 1, row_blocks), row_blocks)
                    loop(first_passed(last), end, lambda a: receive_any(last, a))

            near = first_b(k)
            age = k + n_col - (near * n_col + col)
            settle = jnp.logical_and(age == SETTLE, jnp.logical_and(near > 0, near < col_blocks))

            @pl.when(settle)
            def _():
                with jax.named_scope("late_trail"):
                    own = k - SETTLE

                    for back in (LAG + 2, LAG + 1, LAG):

                        @pl.when(own >= back)
                        def _():
                            columns_arrived(own - back, near)

                    loop(jnp.maximum(own - 2 - LAG, 0), own - LAG + 1, lambda p: trail(p, near, -1))

            @pl.when(jnp.logical_and(k >= LAG, lead(last) != 3))
            def _():
                p = k - LAG
                with jax.named_scope("columns"):
                    columns_arrived(p, near)

                @pl.when(jnp.logical_and(near < col_blocks, age >= SETTLE + 2))
                def _():
                    @pl.when(jnp.logical_and(age == SETTLE + 2, near > 0))
                    def _():
                        with jax.named_scope("seed_late"):
                            seed_arrived(near)
                            edge_seeded(near)

                    oldest = jnp.where(age == SETTLE + 2, jnp.maximum(p - 1, 0), p)
                    loop(oldest, p + 1, lambda q: update_near(q, near))

                with jax.named_scope("trail"):
                    trail(p, near, jnp.where(jnp.logical_or(age > SETTLE, near == 0), near, -1))

            @pl.when(settle)
            def _():
                hand_out(near)

        @pl.when(soon)
        def _():
            nb = (k + 1) // n_col

            oldest = jnp.maximum(k - 1 - LAG, 0)
            lo = first_a(k + 1)

            def old_diag(p):
                column_arrived(p, nb)
                edge_arrived(p, nb)
                update_near(p, nb)

            def take(a):
                receive(last, a)

                @pl.when(jnp.logical_not(here_diag(k + 1)))
                def _():
                    loop(oldest, last, lambda p: update_block(p, a, nb))

            @pl.when(k > 0)
            def _():
                with jax.named_scope("old_diag"):
                    loop(oldest, last, old_diag)
                with jax.named_scope("take"):
                    loop(first_a(k), jnp.minimum(first_a(k) + 1, row_blocks), take)
                with jax.named_scope("take_column"):
                    column_arrived(last, nb)
                    edge_arrived(last, nb)
                with jax.named_scope("catch_up"):
                    update_near(last, nb)
                    @pl.when(jnp.logical_and(jnp.logical_not(here_diag(k + 1)), lo < row_blocks))
                    def _():
                        update_block(last, lo, nb)

            prepare(nb)
            slot = col_of(k, nb)
            with jax.named_scope("first_block"):
                arrived(slot)

            @pl.when(leads)
            def _():
                first_down(k, start)

            other = panel[slot]
            work[0:size, :] = diag[nb] - times_t(other, other)

        @pl.when(jnp.logical_and(k >= n_col // 2, col == lax.rem(k + n_col // 2, n_col)))
        def _():
            with jax.named_scope("sends_done"):
                firsts_done(k - n_col // 2)
                loop(first_a(k - n_col // 2), row_blocks, lambda a: source_sends(k - n_col // 2, a, finish))

    loop(0, steps + n_col // 2, step)

    def edges_done(b):
        @pl.when(jnp.logical_and(holds_edge(b), jnp.logical_not(leads)))
        def _():
            edge_copy(b).wait_send()

    loop(0, col_blocks, edges_done)


def solution(mesh):
    n_row = mesh.shape["row"]
    n_col = mesh.shape["col"]

    def factor_local(a_loc):
        row_blocks, size, local_cols = a_loc.shape
        col_blocks = local_cols // size
        slots = n_row * (row_blocks * (row_blocks + 1) // 2) + n_col * (col_blocks * (col_blocks + 1) // 2)
        slots += row_blocks * n_row
        return pl.pallas_call(
            functools.partial(kernel, n_row, n_col, "batch"),
            out_shape=pltpu.VMEM(a_loc.shape, F32),
            in_specs=[pl.BlockSpec(memory_space=pl.ANY)],
            scratch_shapes=[
                pltpu.VMEM((col_blocks, size, size), F32),
                pltpu.VMEM((col_blocks, size, size), F32),
                pltpu.VMEM((col_blocks, size, size), F32),
                pltpu.VMEM((size, size), BF16),
                pltpu.VMEM((slots, size, size), BF16),
                pltpu.VMEM((size + BASE, size), F32),
                pltpu.VMEM((size + BASE, size), F32),
                pltpu.VMEM((3, size, size), BF16),
                pltpu.VMEM((BASE, 3 * LANE), F32),
                pltpu.VMEM((4 * SUB, SUB, LANE), F32),
                pltpu.SemaphoreType.DMA,
                pltpu.SemaphoreType.DMA((col_blocks, n_row)),
                pltpu.SemaphoreType.DMA((col_blocks,)),
                pltpu.SemaphoreType.DMA((col_blocks,)),
                pltpu.SemaphoreType.DMA((col_blocks,)),
                pltpu.SemaphoreType.DMA((2, n_row)),
                pltpu.SemaphoreType.DMA((row_blocks, 9)),
                pltpu.SemaphoreType.DMA((4, row_blocks, 2)),
                pltpu.SemaphoreType.DMA((4, col_blocks, 3)),
                pltpu.SemaphoreType.DMA((slots,)),
            ],
            compiler_params=pltpu.CompilerParams(
                collective_id=0, has_side_effects=True, vmem_limit_bytes=50 * 1024 * 1024
            ),
            name="cholesky",
        )(a_loc)

    blk_spec = P(("batch", "row"), None, "col")
    return jax.shard_map(factor_local, mesh=mesh, in_specs=(blk_spec,), out_specs=blk_spec, check_vma=False)
```

```python
import functools

import jax
import jax.numpy as jnp
from jax import lax
from jax.experimental import pallas as pl
from jax.experimental.pallas import tpu as pltpu
from jax.sharding import PartitionSpec as P

F32 = jnp.float32
BF16 = jnp.bfloat16
MESH = pl.DeviceIdType.MESH
SUB = 8
LANE = 128
BASE = 16
LEAD = 1
SETTLE = 3
LAG = 3


def sub_bcast(x, q):
    return jnp.broadcast_to(x[q : q + 1, :], (SUB, LANE))


ALONG_LANES = lax.GatherDimensionNumbers(
    offset_dims=(), collapsed_slice_dims=(1,), start_index_map=(1,), operand_batching_dims=(0,), start_indices_batching_dims=(0,)
)


def lane_bcast(x, lane):
    index = jnp.full((SUB, LANE, 1), lane, jnp.int32)
    return lax.gather(x, index, ALONG_LANES, (1, 1), mode=lax.GatherScatterMode.PROMISE_IN_BOUNDS)


def split3(x):
    high = x.astype(BF16)
    rest = x - high.astype(F32)
    mid = rest.astype(BF16)
    return high, mid, (rest - mid.astype(F32)).astype(BF16)


def swap_rows(x, bit, row_id):
    if bit == SUB // 2:
        return pltpu.roll(x, bit, 0)
    return jnp.where((row_id & bit) == 0, pltpu.roll(x, SUB - bit, 0), pltpu.roll(x, bit, 0))


def stack_sums(parts):
    row_id = lax.broadcasted_iota(jnp.int32, (SUB, LANE), 0)
    for bit in (4, 2, 1):
        low = (row_id & bit) == 0
        half = len(parts) // 2
        parts = [
            jnp.where(low, parts[n], parts[n + half]) + swap_rows(jnp.where(low, parts[n + half], parts[n]), bit, row_id)
            for n in range(half)
        ]
    return parts[0]


def eliminate(rows, lane0):
    row_id = lax.broadcasted_iota(jnp.int32, (SUB, LANE), 0)
    rows = [list(rows[0]), list(rows[1])]
    cols = [
        [lane_bcast(rows[0][0], lane0 + j) for j in range(SUB)],
        [lane_bcast(rows[1][0], lane0 + j) for j in range(BASE)],
    ]
    scale = [jnp.zeros((SUB, LANE), F32), jnp.zeros((SUB, LANE), F32)]
    pivot = sub_bcast(cols[0][0], 0)
    for j in range(BASE):
        t, q = divmod(j, SUB)
        inv = lax.rsqrt(pivot)
        scale[t] = jnp.where(row_id == q, inv, scale[t])
        if j + 1 < BASE:
            tn, qn = divmod(j + 1, SUB)
            near = sub_bcast(cols[tn][j], qn) * inv
            pivot = sub_bcast(cols[tn][j + 1], qn) - near * near
        below = cols[1][j] * inv
        here = cols[0][j] * inv if t == 0 else None
        for n in range(j + 1, BASE):
            tn, qn = divmod(n, SUB)
            other = near if n == j + 1 else sub_bcast(here if tn == 0 else below, qn)
            if t == 0 and tn == 0:
                cols[0][n] = cols[0][n] - here * other
            cols[1][n] = cols[1][n] - below * other
        masked = jnp.where(row_id > q, here if t == 0 else below, 0.0)
        for v in range(len(rows[0])):
            pivot_row = sub_bcast(rows[t][v], q) * inv
            rows[t][v] = rows[t][v] - masked * pivot_row
            if t == 0:
                rows[1][v] = rows[1][v] - below * pivot_row
    return [[x * scale[t] for x in rows[t]] for t in range(2)]


def factor_block(work, winv, winv3, prev, fac):
    size = work.shape[1]
    prev[...] = jnp.zeros(prev.shape, F32)
    fac[...] = jnp.zeros(fac.shape, F32)

    def group(v):
        return slice(LANE * v, LANE * (v + 1))

    def pending(factors, before, t, v):
        above, below = before[:SUB, group(v)], before[SUB:, group(v)]
        at = 2 * SUB * t
        return stack_sums([factors[at + n] * above + factors[at + SUB + n] * below for n in range(SUB)])

    for half in range(size // LANE):
        views = [(work, 0), (work, 1), (winv, 0)] if half == 0 else [(work, 1), (winv, 0), (winv, 1)]
        first = half * LANE
        if half == 1:
            factors, before = fac[...], prev[...]
            work[first : first + BASE, group(1)] -= jnp.concatenate([pending(factors, before, t, 1) for t in range(2)], axis=0)
            prev[...] = jnp.concatenate([before[:, group(1)], before[:, group(2)], jnp.zeros((BASE, LANE), F32)], axis=1)

        def body(s, carry, views=views, first=first):
            lane0 = s * BASE
            row0 = pl.multiple_of(first + lane0, BASE)

            here = pl.ds(row0, BASE)
            then = pl.ds(pl.multiple_of(row0 + BASE, BASE), BASE)
            both = [ref[here, group(g)] for ref, g in views]
            rows = [[x[SUB * t : SUB * (t + 1)] for x in both] for t in range(2)]
            factors, before = fac[...], prev[...]
            for t in range(2):
                for v in (1, 2):
                    rows[t][v] = rows[t][v] - pending(factors, before, t, v)
            hi, mid, lo = split3(before)
            lane = lax.broadcasted_iota(jnp.int32, (BASE, size - first), 1) + first
            after = lane >= row0 + BASE
            lhi, lmid, llo = [jnp.where(after, x[:, : size - first], jnp.zeros((), BF16)) for x in (hi, mid, lo)]
            update = lax.dot_general(
                jnp.concatenate([lhi, lhi, lmid, lhi, llo, lmid], axis=0),
                jnp.concatenate([hi, mid, hi, lo, hi, mid], axis=0),
                (((0,), (0,)), ((), ())),
                preferred_element_type=F32,
            )
            for v, (ref, g) in enumerate(views):
                ref[first:size, group(g)] -= update[:, group(v)]
            done = eliminate(rows, lane0)
            if first == 0:
                source = [jnp.where(s == LANE // BASE - 1, done[t][1], done[t][0]) for t in range(2)]
            else:
                source = [done[t][0] for t in range(2)]
            next_lane = (lane0 + BASE) % LANE
            factors, sums = [], []
            for t in range(2):
                factor = [[lane_bcast(source[m], next_lane + SUB * t + n) for n in range(SUB)] for m in range(2)]
                sums.append(stack_sums([factor[0][n] * done[0][0] + factor[1][n] * done[1][0] for n in range(SUB)]))
                factors += factor[0] + factor[1]
            ref, g = views[0]
            ref[then, group(g)] -= jnp.concatenate(sums, axis=0)
            fac[...] = jnp.stack(factors)
            whole = [jnp.concatenate([done[0][v], done[1][v]], axis=0) for v in range(3)]
            prev[...] = jnp.concatenate(whole, axis=1)
            for (ref, g), x in zip(views, whole):
                ref[here, group(g)] = x
                if ref is winv:
                    for n, part in enumerate(split3(x)):
                        winv3[n, here, group(g)] = part
            return carry

        lax.fori_loop(0, LANE // BASE, body, 0, unroll=2)


def kernel(n_row, n_col, batch_axis, a_ref, share, diag, edge, stage, first, panel, work, winv, winv3, prev, fac, load_sem,
           seed_send, seed_recv, edge_send, edge_recv, first_sem, send_sem, pass_sem, down_sem, recv_sem):
    row_blocks, size, local_cols = a_ref.shape
    col_blocks = local_cols // size
    ratio = n_col // n_row
    steps = row_blocks * n_row
    depth = pass_sem.shape[0]
    batch = lax.axis_index(batch_axis)
    row = lax.axis_index("row")
    col = lax.axis_index("col")
    odd = lax.rem(col, 2)
    on_diag = lax.rem(col, n_row) == row
    row_slots = n_row * (row_blocks * (row_blocks + 1) // 2)
    edge_slots = row_slots + n_col * (col_blocks * (col_blocks + 1) // 2)
    leads = row == LEAD

    def at(dev_row, dev_col):
        return (batch, dev_row, dev_col)

    def row_slot(k, a):
        g = k // n_row
        return n_row * (row_blocks * g - (g * (g - 1)) // 2) + (k - g * n_row) * (row_blocks - g) + a - g

    def col_slot(k, b):
        h = k // n_col
        return row_slots + n_col * (col_blocks * h - (h * (h - 1)) // 2) + (k - h * n_col) * (col_blocks - h) + b - h

    def first_a(k):
        return (k + n_row - row) // n_row

    def first_b(k):
        return (k + n_col - col) // n_col

    def spot(a, b, count=1):
        return (a if count == 1 else pl.ds(a, count), slice(None), pl.ds(pl.multiple_of(b * size, size), size))

    def col_of(k, b):
        return jnp.where(on_diag, row_slot(k, ratio * b + col // n_row), col_slot(k, b))

    def edge_slot(k):
        return edge_slots + k

    def edge_reach(ahead):
        return jnp.logical_and(ahead >= 2, jnp.logical_and(ahead <= n_col + LAG - SETTLE, row != LEAD))

    def copy(src_slot, dst_slot, sem, device):
        return pltpu.make_async_remote_copy(
            src_ref=panel.at[src_slot], dst_ref=panel.at[dst_slot], send_sem=sem, recv_sem=recv_sem.at[dst_slot],
            device_id=device, device_id_type=MESH,
        )

    def arrived(slot):
        copy(slot, slot, send_sem.at[0, 0], at(row, col)).wait_recv()

    def start(c):
        c.start()

    def finish(c):
        c.wait_send()

    def from_maker(ahead, way):
        there = lax.rem(row + way, n_row)
        lead_near = jnp.logical_and(there == LEAD, jnp.logical_and(ahead >= 2, ahead <= n_row))
        soon_needed = jnp.logical_and(jnp.logical_and(ahead >= 2, ahead <= 3), way == 2)
        return jnp.logical_or(lead_near, soon_needed)

    def down_column(k, a, maker, sems, act):
        i = a * n_row + row
        slot = row_slot(k, a)
        dst = col_slot(k, i // n_col)
        for m, way in enumerate((1, n_row - 1, 2)):
            direct = from_maker(i - k, way)

            @pl.when(jnp.where(maker, direct, jnp.logical_not(direct)))
            def _():
                act(copy(slot, dst, sems[m], at(lax.rem(row + way, n_row), lax.rem(i, n_col))))

    def last_near(p):
        return first_a(p + 2)

    def to_edge(k, a, sem, act):
        i = a * n_row + row
        act(copy(row_slot(k, a), edge_slot(k), sem, at(LEAD, lax.rem(i - 1, n_col))))

    def source_sends(k, a, act):
        ahead = a * n_row + row - k
        slot = row_slot(k, a)
        early = n_row

        @pl.when(edge_reach(ahead))
        def _():
            to_edge(k, a, send_sem.at[a, 5], act)

        near = jnp.logical_and(ahead >= 2, ahead <= early)

        @pl.when(jnp.logical_or(near, lax.rem(ahead, n_col) == 0))
        def _():
            down_column(k, a, near, [send_sem.at[a, m] for m in range(3)], act)

        @pl.when(jnp.logical_or(jnp.logical_and(odd == 0, ahead >= 2), ahead >= n_col - 1))
        def _():
            act(copy(slot, slot, send_sem.at[a, 3], at(row, lax.rem(jnp.where(odd == 0, col + 1, col - 1), n_col))))

        @pl.when(ahead >= 2)
        def _():
            act(copy(slot, slot, send_sem.at[a, 6], at(row, lax.rem(col - odd + 2, n_col))))

        @pl.when(jnp.logical_and(ahead >= 3 - odd, a <= last_near(k)))
        def _():
            act(copy(slot, slot, send_sem.at[a, 4], at(row, lax.rem(col - odd + 3, n_col))))

        @pl.when(jnp.logical_and(ahead >= n_col // 2 - odd, ahead < n_col - 2 - odd))
        def _():
            act(copy(slot, slot, send_sem.at[a, 7], at(row, lax.rem(col - odd + 5, n_col))))

        @pl.when(ahead >= n_col - 2 - odd)
        def _():
            act(copy(slot, slot, send_sem.at[a, 8], at(row, lax.rem(col - odd - 2 + n_col, n_col))))

    def lead(p):
        return lax.rem(col - lax.rem(p, n_col) + n_col, n_col)

    def hops(p):
        return lax.rem(col // 2 - lax.rem(p, n_col) // 2 + n_col // 2, n_col // 2)

    def passes(p):
        return jnp.where(odd == 1, 2, n_col // 2 - 1) == hops(p)

    def first_passed(p):
        low = jnp.where(jnp.logical_and(passes(p), odd == 1), lead(p) - 1, lead(p))
        return (p + low - row + n_row - 1) // n_row

    def pass_down(p, a, act):
        i = a * n_row + row
        ahead = i - p
        sems = pass_sem.at[lax.rem(p, depth), a]

        @pl.when(jnp.logical_and(odd == 0, jnp.logical_and(lead(p) <= 2, a > last_near(p))))
        def _():
            act(copy(row_slot(p, a), row_slot(p, a), sems.at[0], at(row, col + 1)))

        @pl.when(jnp.logical_and(lax.rem(i, n_col) == col, ahead > 1))
        def _():
            downs = down_sem.at[lax.rem(p, depth), i // n_col]
            down_column(p, a, False, [downs.at[m] for m in range(3)], act)

    def pass_on(p, a, act):
        slot = row_slot(p, a)
        sems = pass_sem.at[lax.rem(p, depth), a]

        @pl.when(passes(p))
        def _():
            @pl.when(odd == 0)
            def _():
                act(copy(slot, slot, sems.at[1], at(row, lax.rem(col - 1 + n_col, n_col))))

            @pl.when(jnp.logical_or(odd == 1, a * n_row + row > p + lead(p)))
            def _():
                act(copy(slot, slot, sems.at[0], at(row, col + 1 - 2 * odd)))

        pass_down(p, a, act)

    def passed(p):
        @pl.when(lead(p) != 0)
        def _():
            loop(first_passed(p), row_blocks, lambda a: pass_on(p, a, finish))

    def receive(p, a):
        arrived(row_slot(p, a))
        pass_down(p, a, start)

    def receive_any(p, a):
        arrived(row_slot(p, a))
        pass_on(p, a, start)

    def loop(lo, hi, fn):
        lax.fori_loop(lo, hi, lambda n, c: (fn(n), c)[1], 0)

    load = pltpu.make_async_copy(a_ref, share, load_sem)
    load.start()

    barrier = pltpu.get_barrier_semaphore()
    n_dev = n_row * n_col

    def greet(n):
        other = lax.rem(row * n_col + col + n, n_dev)
        pl.semaphore_signal(barrier, inc=1, device_id=at(other // n_col, lax.rem(other, n_col)), device_id_type=MESH)

    loop(1, n_dev, greet)
    with jax.named_scope("all_here"):
        pl.semaphore_wait(barrier, n_dev - 1)
    with jax.named_scope("loaded"):
        load.wait()

    def seed_copy(b, dev_row):
        return pltpu.make_async_remote_copy(
            src_ref=share.at[spot(ratio * b + col // n_row, b)], dst_ref=diag.at[b],
            send_sem=seed_send.at[b, lax.rem(dev_row - row + n_row, n_row)],
            recv_sem=seed_recv.at[b], device_id=at(dev_row, col), device_id_type=MESH,
        )

    def hand_out(b):
        @pl.when(on_diag)
        def _():
            for d in (1, n_row - 1, 2):
                seed_copy(b, lax.rem(row + d, n_row)).start()
            diag[b] = share[spot(ratio * b + col // n_row, b)]

        @pl.when(jnp.logical_and(holds_edge(b), jnp.logical_not(leads)))
        def _():
            stage[b] = share[spot((b * n_col + col + 1) // n_row, b)]
            edge_copy(b).start()

    def holds_edge(b):
        j = b * n_col + col
        return jnp.logical_and(lax.rem(j + 1, n_row) == row, j + 1 < steps)

    def edge_copy(b):
        return pltpu.make_async_remote_copy(
            src_ref=stage.at[b], dst_ref=edge.at[b], send_sem=edge_send.at[b], recv_sem=edge_recv.at[b],
            device_id=at(LEAD, col), device_id_type=MESH,
        )

    def has_edge(b):
        from_other = jnp.logical_and(leads, lax.rem(col + 1, n_row) != LEAD)
        return jnp.logical_and(from_other, b * n_col + col + 1 < steps)

    def edge_seeded(b):
        @pl.when(has_edge(b))
        def _():
            edge_copy(b).wait_recv()

    def edge_arrived(p, b):
        j = b * n_col + col

        @pl.when(jnp.logical_and(has_edge(b), j + 1 - p <= n_col + LAG - SETTLE))
        def _():
            arrived(edge_slot(p))

    hand_out(0)
    winv3[...] = jnp.zeros(winv3.shape, BF16)

    def seed_arrived(b):
        @pl.when(jnp.logical_not(on_diag))
        def _():
            seed_copy(b, row).wait_recv()

    with jax.named_scope("seed"):
        seed_arrived(0)

        @pl.when(col != 0)
        def _():
            edge_seeded(0)

    def clear(n):
        a, b = lax.rem(n, row_blocks), n // row_blocks

        @pl.when(a * n_row + row < b * n_col + col)
        def _():
            share[spot(a, b)] = jnp.zeros((size, size), F32)

    loop(0, row_blocks * col_blocks, clear)

    def times_t(x, y):
        return lax.dot_general(x, y, (((1,), (1,)), ((), ())), preferred_element_type=F32)

    def update_block(p, a, b):
        share[spot(a, b)] -= times_t(panel[row_slot(p, a)], panel[col_of(p, b)])

    def update_diag(p, b):
        other = panel[col_of(p, b)]
        diag[b] -= times_t(other, other)

    def update_edge(p, b):
        @pl.when(has_edge(b))
        def _():
            edge[b] -= times_t(panel[edge_slot(p)], panel[col_of(p, b)])

    def column_arrived(p, b):
        @pl.when(jnp.logical_not(on_diag))
        def _():
            arrived(col_slot(p, b))

    def update_column(p, b, lo):
        lone = lax.rem(row_blocks - lo, 2)

        @pl.when(lone == 1)
        def _():
            update_block(p, lo, b)

        def pair(m):
            a = lo + lone + 2 * m
            both = spot(a, b, 2)
            left = panel[pl.ds(row_slot(p, a), 2)].reshape(2 * size, size)
            share[both] -= times_t(left, panel[col_of(p, b)]).reshape(2, size, size)

        loop(0, (row_blocks - lo) // 2, pair)

    def trail(p, b_from, near):
        loop(b_from, col_blocks, lambda b: update_column(p, b, first_a(b * n_col + col - jnp.where(b == near, 0, 1))))

    def columns_arrived(p, b_from):
        def one(b):
            column_arrived(p, b)
            edge_arrived(p, b)

        loop(b_from, col_blocks, one)

    def prepare(b):
        work[size:, :] = jnp.zeros((BASE, size), F32)
        r_id = lax.broadcasted_iota(jnp.int32, (size + BASE, size), 0)
        c_id = lax.broadcasted_iota(jnp.int32, (size + BASE, size), 1)
        winv[...] = jnp.where(r_id == c_id, 1.0, 0.0).astype(F32)

    def times_winv_t(x):
        hi, mid, lo = split3(x)
        whi, wmid, wlo = winv3[0], winv3[1], winv3[2]
        small = times_t(lo, whi) + times_t(mid, wmid) + times_t(hi, wlo)
        return small + (times_t(mid, whi) + times_t(hi, wmid)) + times_t(hi, whi)

    def here_diag(k):
        return row == lax.rem(k, n_row)

    def solve(k, a, count):
        kb = k // n_col
        near = jnp.logical_and(a == first_a(k), jnp.logical_not(here_diag(k)))
        here = spot(a, kb, count)

        def shaped(x):
            return x if count == 1 else x.reshape(count, size, size)

        def apply(p):
            left = panel[pl.ds(row_slot(p, a), count)].reshape(count * size, size)
            share[here] -= shaped(times_t(left, panel[col_of(p, kb)]))

        @pl.when(jnp.logical_not(near))
        def _():
            for m in range(count):

                @pl.when(k >= 3)
                def _():
                    receive(k - 3, a + m)

                @pl.when(k >= 2)
                def _():
                    receive(k - 2, a + m)

            loop(jnp.maximum(k - 2 - LAG, 0), k - 1, apply)

        @pl.when(k > 0)
        def _():
            for m in range(count):
                receive(k - 1, a + m)
            apply(k - 1)

        x = times_winv_t(share[here].reshape(count * size, size))
        panel[pl.ds(row_slot(k, a), count)] = x.astype(BF16).reshape(count, size, size)
        share[here] = shaped(x)
        if count == 1:

            @pl.when(jnp.logical_and(near, jnp.logical_and(leads, lax.rem(k + 1, n_row) == LEAD)))
            def _():
                first[...] = panel[row_slot(k, a)]
                first_out(k, start)

        if count == 1:
            source_sends(k, a, start)
        else:
            loop(a, a + count, lambda n: source_sends(k, n, start))

    def update_near(p, b):
        update_diag(p, b)
        update_edge(p, b)

    def first_slot(k, dev_row):
        return jnp.where(lax.rem(k + 1, n_row) == dev_row, row_slot(k, (k + 1) // n_row), col_slot(k, (k + 1) // n_col))

    def first_copy(k, dev_row, sem):
        dst = first_slot(k, dev_row)
        return pltpu.make_async_remote_copy(
            src_ref=first, dst_ref=panel.at[dst], send_sem=sem, recv_sem=recv_sem.at[dst],
            device_id=at(dev_row, lax.rem(col + 1, n_col)), device_id_type=MESH,
        )

    def others_first(k, fn):
        urgent = lax.rem(k + 3, n_row)
        lone = urgent == LEAD
        for m in range(n_row - 1):
            fn(m, lax.rem(jnp.where(lone, LEAD + 1, urgent) + m + jnp.where(lax.rem(jnp.where(lone, LEAD + 1, urgent) - LEAD + n_row, n_row) + m >= n_row, 1, 0), n_row))

    def first_out(k, act):
        act(first_copy(k, LEAD, first_sem.at[0, 0]))

        @pl.when(odd == 0)
        def _():
            others_first(k, lambda m, r: act(first_copy(k, r, first_sem.at[0, 1 + m])))

    def first_down(k, act):
        @pl.when(odd == 0)
        def _():
            others_first(k, lambda m, r: act(copy(first_slot(k, LEAD), first_slot(k, r), first_sem.at[1, 1 + m], at(r, col))))

    def firsts_done(k):
        @pl.when(jnp.logical_and(leads, k + 1 < steps))
        def _():
            first_out(k, finish)

        @pl.when(jnp.logical_and(leads, k > 0))
        def _():
            first_down(k - 1, finish)

    @pl.when(col == 0)
    def _():
        prepare(0)
        work[0:size, :] = diag[0]

    def step(k):
        mine = jnp.logical_and(col == lax.rem(k, n_col), k < steps)
        kb = k // n_col
        last = k - 1
        soon = jnp.logical_and(col == lax.rem(k + 1, n_col), k + 1 < steps)

        @pl.when(mine)
        def _():
            with jax.named_scope("factor"):
                factor_block(work, winv, winv3, prev, fac)

            @pl.when(has_edge(kb))
            def _():
                with jax.named_scope("lead"):

                    @pl.when(k == 0)
                    def _():
                        edge_seeded(kb)

                    @pl.when(k > 0)
                    def _():
                        edge_arrived(last, kb)
                        update_edge(last, kb)

                    first[...] = times_winv_t(edge[kb]).astype(BF16)
                    first_out(k, start)

            lo = first_a(k)
            second = jnp.minimum(lo + 1, row_blocks)
            third = second + lax.rem(row_blocks - second, 2)
            with jax.named_scope("solve_near"):
                loop(lo, third, lambda a: solve(k, a, 1))
            with jax.named_scope("solve_two"):
                loop(0, (row_blocks - third) // 2, lambda m: solve(k, third + 2 * m, 2))

        @pl.when(k >= depth)
        def _():
            with jax.named_scope("passed"):
                passed(k - depth)

        @pl.when(mine)
        def _():
            @pl.when(row == lax.rem(k, n_row))
            def _():
                for d in range(1, n_row):
                    seed_copy(kb, lax.rem(row + d, n_row)).wait_send()
                r_id = lax.broadcasted_iota(jnp.int32, (size, size), 0)
                c_id = lax.broadcasted_iota(jnp.int32, (size, size), 1)
                share[spot(k // n_row, kb)] = jnp.where(r_id >= c_id, work[0:size, :].T, 0.0)

        @pl.when(jnp.logical_and(k > 0, jnp.logical_not(jnp.logical_or(mine, soon))))
        def _():
            @pl.when(col != lax.rem(last, n_col))
            def _():
                with jax.named_scope("receive"):
                    end = jnp.where(lead(last) == 3, jnp.minimum(last_near(last) + 1, row_blocks), row_blocks)
                    loop(first_passed(last), end, lambda a: receive_any(last, a))

            near = first_b(k)
            age = k + n_col - (near * n_col + col)
            settle = jnp.logical_and(age == SETTLE, jnp.logical_and(near > 0, near < col_blocks))

            @pl.when(settle)
            def _():
                with jax.named_scope("late_trail"):
                    own = k - SETTLE

                    for back in (LAG + 2, LAG + 1, LAG):

                        @pl.when(own >= back)
                        def _():
                            columns_arrived(own - back, near)

                    loop(jnp.maximum(own - 2 - LAG, 0), own - LAG + 1, lambda p: trail(p, near, -1))

            @pl.when(jnp.logical_and(k >= LAG, lead(last) != 3))
            def _():
                p = k - LAG
                with jax.named_scope("columns"):
                    columns_arrived(p, near)

                with jax.named_scope("trail"):
                    trail(p, near, jnp.where(jnp.logical_or(age > SETTLE, near == 0), near, -1))

            @pl.when(settle)
            def _():
                hand_out(near)

        @pl.when(soon)
        def _():
            nb = (k + 1) // n_col

            oldest = jnp.maximum(k - 1 - LAG, 0)
            lo = first_a(k + 1)

            @pl.when(nb > 0)
            def _():
                with jax.named_scope("seed_late"):
                    seed_arrived(nb)
                    edge_seeded(nb)

            handed = jnp.maximum(k + 1 - n_col + SETTLE - LAG + 1, 0)

            def old_diag(p):
                column_arrived(p, nb)
                edge_arrived(p, nb)
                update_near(p, nb)

            def take(a):
                receive(last, a)

                @pl.when(jnp.logical_not(here_diag(k + 1)))
                def _():
                    loop(oldest, last, lambda p: update_block(p, a, nb))

            @pl.when(k > 0)
            def _():
                with jax.named_scope("older"):
                    loop(handed, oldest, lambda p: update_near(p, nb))
                with jax.named_scope("old_diag"):
                    loop(oldest, last, old_diag)
                with jax.named_scope("take"):
                    loop(first_a(k), jnp.minimum(first_a(k) + 1, row_blocks), take)
                with jax.named_scope("take_column"):
                    column_arrived(last, nb)
                    edge_arrived(last, nb)
                with jax.named_scope("catch_up"):
                    update_near(last, nb)
                    @pl.when(jnp.logical_and(jnp.logical_not(here_diag(k + 1)), lo < row_blocks))
                    def _():
                        update_block(last, lo, nb)

            prepare(nb)
            slot = col_of(k, nb)
            with jax.named_scope("first_block"):
                arrived(slot)

            @pl.when(leads)
            def _():
                first_down(k, start)

            other = panel[slot]
            work[0:size, :] = diag[nb] - times_t(other, other)

        @pl.when(jnp.logical_and(k >= n_col // 2, col == lax.rem(k + n_col // 2, n_col)))
        def _():
            with jax.named_scope("sends_done"):
                firsts_done(k - n_col // 2)
                loop(first_a(k - n_col // 2), row_blocks, lambda a: source_sends(k - n_col // 2, a, finish))

    loop(0, steps + n_col // 2, step)

    def edges_done(b):
        @pl.when(jnp.logical_and(holds_edge(b), jnp.logical_not(leads)))
        def _():
            edge_copy(b).wait_send()

    loop(0, col_blocks, edges_done)


def solution(mesh):
    n_row = mesh.shape["row"]
    n_col = mesh.shape["col"]

    def factor_local(a_loc):
        row_blocks, size, local_cols = a_loc.shape
        col_blocks = local_cols // size
        slots = n_row * (row_blocks * (row_blocks + 1) // 2) + n_col * (col_blocks * (col_blocks + 1) // 2)
        slots += row_blocks * n_row
        return pl.pallas_call(
            functools.partial(kernel, n_row, n_col, "batch"),
            out_shape=pltpu.VMEM(a_loc.shape, F32),
            in_specs=[pl.BlockSpec(memory_space=pl.ANY)],
            scratch_shapes=[
                pltpu.VMEM((col_blocks, size, size), F32),
                pltpu.VMEM((col_blocks, size, size), F32),
                pltpu.VMEM((col_blocks, size, size), F32),
                pltpu.VMEM((size, size), BF16),
                pltpu.VMEM((slots, size, size), BF16),
                pltpu.VMEM((size + BASE, size), F32),
                pltpu.VMEM((size + BASE, size), F32),
                pltpu.VMEM((3, size, size), BF16),
                pltpu.VMEM((BASE, 3 * LANE), F32),
                pltpu.VMEM((4 * SUB, SUB, LANE), F32),
                pltpu.SemaphoreType.DMA,
                pltpu.SemaphoreType.DMA((col_blocks, n_row)),
                pltpu.SemaphoreType.DMA((col_blocks,)),
                pltpu.SemaphoreType.DMA((col_blocks,)),
                pltpu.SemaphoreType.DMA((col_blocks,)),
                pltpu.SemaphoreType.DMA((2, n_row)),
                pltpu.SemaphoreType.DMA((row_blocks, 9)),
                pltpu.SemaphoreType.DMA((4, row_blocks, 2)),
                pltpu.SemaphoreType.DMA((4, col_blocks, 3)),
                pltpu.SemaphoreType.DMA((slots,)),
            ],
            compiler_params=pltpu.CompilerParams(
                collective_id=0, has_side_effects=True, vmem_limit_bytes=50 * 1024 * 1024
            ),
            name="cholesky",
        )(a_loc)

    blk_spec = P(("batch", "row"), None, "col")
    return jax.shard_map(factor_local, mesh=mesh, in_specs=(blk_spec,), out_specs=blk_spec, check_vma=False)
```

```python
import functools

import jax
import jax.numpy as jnp
from jax import lax
from jax.experimental import pallas as pl
from jax.experimental.pallas import tpu as pltpu
from jax.sharding import PartitionSpec as P

F32 = jnp.float32
BF16 = jnp.bfloat16
MESH = pl.DeviceIdType.MESH
SUB = 8
LANE = 128
BASE = 16
LEAD = 1
SETTLE = 3
LAG = 3


def sub_bcast(x, q):
    return jnp.broadcast_to(x[q : q + 1, :], (SUB, LANE))


ALONG_LANES = lax.GatherDimensionNumbers(
    offset_dims=(), collapsed_slice_dims=(1,), start_index_map=(1,), operand_batching_dims=(0,), start_indices_batching_dims=(0,)
)


def lane_bcast(x, lane):
    index = jnp.full((SUB, LANE, 1), lane, jnp.int32)
    return lax.gather(x, index, ALONG_LANES, (1, 1), mode=lax.GatherScatterMode.PROMISE_IN_BOUNDS)


def split3(x):
    high = x.astype(BF16)
    rest = x - high.astype(F32)
    mid = rest.astype(BF16)
    return high, mid, (rest - mid.astype(F32)).astype(BF16)


def swap_rows(x, bit, row_id):
    if bit == SUB // 2:
        return pltpu.roll(x, bit, 0)
    return jnp.where((row_id & bit) == 0, pltpu.roll(x, SUB - bit, 0), pltpu.roll(x, bit, 0))


def stack_sums(parts):
    row_id = lax.broadcasted_iota(jnp.int32, (SUB, LANE), 0)
    for bit in (4, 2, 1):
        low = (row_id & bit) == 0
        half = len(parts) // 2
        parts = [
            jnp.where(low, parts[n], parts[n + half]) + swap_rows(jnp.where(low, parts[n + half], parts[n]), bit, row_id)
            for n in range(half)
        ]
    return parts[0]


def eliminate(rows, lane0):
    row_id = lax.broadcasted_iota(jnp.int32, (SUB, LANE), 0)
    rows = [list(rows[0]), list(rows[1])]
    cols = [
        [lane_bcast(rows[0][0], lane0 + j) for j in range(SUB)],
        [lane_bcast(rows[1][0], lane0 + j) for j in range(BASE)],
    ]
    scale = [jnp.zeros((SUB, LANE), F32), jnp.zeros((SUB, LANE), F32)]
    pivot = sub_bcast(cols[0][0], 0)
    for j in range(BASE):
        t, q = divmod(j, SUB)
        inv = lax.rsqrt(pivot)
        scale[t] = jnp.where(row_id == q, inv, scale[t])
        if j + 1 < BASE:
            tn, qn = divmod(j + 1, SUB)
            near = sub_bcast(cols[tn][j], qn) * inv
            pivot = sub_bcast(cols[tn][j + 1], qn) - near * near
        below = cols[1][j] * inv
        here = cols[0][j] * inv if t == 0 else None
        for n in range(j + 1, BASE):
            tn, qn = divmod(n, SUB)
            other = near if n == j + 1 else sub_bcast(here if tn == 0 else below, qn)
            if t == 0 and tn == 0:
                cols[0][n] = cols[0][n] - here * other
            cols[1][n] = cols[1][n] - below * other
        masked = jnp.where(row_id > q, here if t == 0 else below, 0.0)
        for v in range(len(rows[0])):
            pivot_row = sub_bcast(rows[t][v], q) * inv
            rows[t][v] = rows[t][v] - masked * pivot_row
            if t == 0:
                rows[1][v] = rows[1][v] - below * pivot_row
    return [[x * scale[t] for x in rows[t]] for t in range(2)]


def factor_block(work, winv, winv3, prev, fac):
    size = work.shape[1]

    def group(v):
        return slice(LANE * v, LANE * (v + 1))

    def pending(factors, before, t, v):
        above, below = before[:SUB, group(v)], before[SUB:, group(v)]
        at = 2 * SUB * t
        return stack_sums([factors[at + n] * above + factors[at + SUB + n] * below for n in range(SUB)])

    for half in range(size // LANE):
        views = [(work, 0), (work, 1), (winv, 0)] if half == 0 else [(work, 1), (winv, 0), (winv, 1)]
        first = half * LANE
        if half == 1:
            factors, before = fac[...], prev[...]
            work[first : first + BASE, group(1)] -= jnp.concatenate([pending(factors, before, t, 1) for t in range(2)], axis=0)
            prev[...] = jnp.concatenate([before[:, group(1)], before[:, group(2)], jnp.zeros((BASE, LANE), F32)], axis=1)

        def body(s, carry, views=views, first=first):
            lane0 = s * BASE
            row0 = pl.multiple_of(first + lane0, BASE)

            here = pl.ds(row0, BASE)
            then = pl.ds(pl.multiple_of(row0 + BASE, BASE), BASE)
            both = [ref[here, group(g)] for ref, g in views]
            rows = [[x[SUB * t : SUB * (t + 1)] for x in both] for t in range(2)]
            factors, before = fac[...], prev[...]
            for t in range(2):
                for v in (1, 2):
                    rows[t][v] = rows[t][v] - pending(factors, before, t, v)
            hi, mid, lo = split3(before)
            lane = lax.broadcasted_iota(jnp.int32, (BASE, size - first), 1) + first
            after = lane >= row0 + BASE
            lhi, lmid, llo = [jnp.where(after, x[:, : size - first], jnp.zeros((), BF16)) for x in (hi, mid, lo)]
            update = lax.dot_general(
                jnp.concatenate([lhi, lhi, lmid, lhi, llo, lmid], axis=0),
                jnp.concatenate([hi, mid, hi, lo, hi, mid], axis=0),
                (((0,), (0,)), ((), ())),
                preferred_element_type=F32,
            )
            for v, (ref, g) in enumerate(views):
                ref[first:size, group(g)] -= update[:, group(v)]
            done = eliminate(rows, lane0)
            if first == 0:
                source = [jnp.where(s == LANE // BASE - 1, done[t][1], done[t][0]) for t in range(2)]
            else:
                source = [done[t][0] for t in range(2)]
            next_lane = (lane0 + BASE) % LANE
            factors, sums = [], []
            for t in range(2):
                factor = [[lane_bcast(source[m], next_lane + SUB * t + n) for n in range(SUB)] for m in range(2)]
                sums.append(stack_sums([factor[0][n] * done[0][0] + factor[1][n] * done[1][0] for n in range(SUB)]))
                factors += factor[0] + factor[1]
            ref, g = views[0]
            ref[then, group(g)] -= jnp.concatenate(sums, axis=0)
            fac[...] = jnp.stack(factors)
            whole = [jnp.concatenate([done[0][v], done[1][v]], axis=0) for v in range(3)]
            prev[...] = jnp.concatenate(whole, axis=1)
            for (ref, g), x in zip(views, whole):
                ref[here, group(g)] = x
                if ref is winv:
                    for n, part in enumerate(split3(x)):
                        winv3[n, here, group(g)] = part
            return carry

        lax.fori_loop(0, LANE // BASE, body, 0, unroll=2)


def kernel(n_row, n_col, batch_axis, a_ref, share, diag, edge, stage, first, panel, work, winv, winv3, prev, fac, load_sem,
           seed_send, seed_recv, edge_send, edge_recv, first_sem, send_sem, pass_sem, down_sem, recv_sem):
    row_blocks, size, local_cols = a_ref.shape
    col_blocks = local_cols // size
    ratio = n_col // n_row
    steps = row_blocks * n_row
    depth = pass_sem.shape[0]
    batch = lax.axis_index(batch_axis)
    row = lax.axis_index("row")
    col = lax.axis_index("col")
    odd = lax.rem(col, 2)
    on_diag = lax.rem(col, n_row) == row
    row_slots = n_row * (row_blocks * (row_blocks + 1) // 2)
    edge_slots = row_slots + n_col * (col_blocks * (col_blocks + 1) // 2)
    leads = row == LEAD

    def at(dev_row, dev_col):
        return (batch, dev_row, dev_col)

    def row_slot(k, a):
        g = k // n_row
        return n_row * (row_blocks * g - (g * (g - 1)) // 2) + (k - g * n_row) * (row_blocks - g) + a - g

    def col_slot(k, b):
        h = k // n_col
        return row_slots + n_col * (col_blocks * h - (h * (h - 1)) // 2) + (k - h * n_col) * (col_blocks - h) + b - h

    def first_a(k):
        return (k + n_row - row) // n_row

    def first_b(k):
        return (k + n_col - col) // n_col

    def spot(a, b, count=1):
        return (a if count == 1 else pl.ds(a, count), slice(None), pl.ds(pl.multiple_of(b * size, size), size))

    def col_of(k, b):
        return jnp.where(on_diag, row_slot(k, ratio * b + col // n_row), col_slot(k, b))

    def edge_slot(k):
        return edge_slots + k

    def edge_reach(ahead):
        return jnp.logical_and(ahead >= 2, jnp.logical_and(ahead <= n_col + LAG - SETTLE, row != LEAD))

    def copy(src_slot, dst_slot, sem, device):
        return pltpu.make_async_remote_copy(
            src_ref=panel.at[src_slot], dst_ref=panel.at[dst_slot], send_sem=sem, recv_sem=recv_sem.at[dst_slot],
            device_id=device, device_id_type=MESH,
        )

    def arrived(slot):
        copy(slot, slot, send_sem.at[0, 0], at(row, col)).wait_recv()

    def start(c):
        c.start()

    def finish(c):
        c.wait_send()

    def from_maker(ahead, way):
        there = lax.rem(row + way, n_row)
        lead_near = jnp.logical_and(there == LEAD, jnp.logical_and(ahead >= 2, ahead <= n_row))
        soon_needed = jnp.logical_and(ahead == 2, way == 2)
        return jnp.logical_or(lead_near, soon_needed)

    def down_column(k, a, maker, sems, act):
        i = a * n_row + row
        slot = row_slot(k, a)
        dst = col_slot(k, i // n_col)
        for m, way in enumerate((1, n_row - 1, 2)):
            direct = from_maker(i - k, way)

            @pl.when(jnp.where(maker, direct, jnp.logical_not(direct)))
            def _():
                act(copy(slot, dst, sems[m], at(lax.rem(row + way, n_row), lax.rem(i, n_col))))

    def last_near(p):
        return first_a(p + 2)

    def to_edge(k, a, sem, act):
        i = a * n_row + row
        act(copy(row_slot(k, a), edge_slot(k), sem, at(LEAD, lax.rem(i - 1, n_col))))

    def source_sends(k, a, act):
        ahead = a * n_row + row - k
        slot = row_slot(k, a)
        early = n_row

        @pl.when(edge_reach(ahead))
        def _():
            to_edge(k, a, send_sem.at[a, 5], act)

        near = jnp.logical_and(ahead >= 2, ahead <= early)

        @pl.when(jnp.logical_or(near, lax.rem(ahead, n_col) == 0))
        def _():
            down_column(k, a, near, [send_sem.at[a, m] for m in range(3)], act)

        @pl.when(jnp.logical_or(jnp.logical_and(odd == 0, ahead >= 2), ahead >= n_col - 1))
        def _():
            act(copy(slot, slot, send_sem.at[a, 3], at(row, lax.rem(jnp.where(odd == 0, col + 1, col - 1), n_col))))

        @pl.when(ahead >= 2)
        def _():
            act(copy(slot, slot, send_sem.at[a, 6], at(row, lax.rem(col - odd + 2, n_col))))

        @pl.when(jnp.logical_and(ahead >= 3 - odd, a <= last_near(k)))
        def _():
            act(copy(slot, slot, send_sem.at[a, 4], at(row, lax.rem(col - odd + 3, n_col))))

        @pl.when(jnp.logical_and(ahead >= n_col // 2 - odd, ahead < n_col - 2 - odd))
        def _():
            act(copy(slot, slot, send_sem.at[a, 7], at(row, lax.rem(col - odd + 5, n_col))))

        @pl.when(ahead >= n_col - 2 - odd)
        def _():
            act(copy(slot, slot, send_sem.at[a, 8], at(row, lax.rem(col - odd - 2 + n_col, n_col))))

    def lead(p):
        return lax.rem(col - lax.rem(p, n_col) + n_col, n_col)

    def hops(p):
        return lax.rem(col // 2 - lax.rem(p, n_col) // 2 + n_col // 2, n_col // 2)

    def passes(p):
        return jnp.where(odd == 1, 2, n_col // 2 - 1) == hops(p)

    def first_passed(p):
        low = jnp.where(jnp.logical_and(passes(p), odd == 1), lead(p) - 1, lead(p))
        return (p + low - row + n_row - 1) // n_row

    def pass_down(p, a, act):
        i = a * n_row + row
        ahead = i - p
        sems = pass_sem.at[lax.rem(p, depth), a]

        @pl.when(jnp.logical_and(odd == 0, jnp.logical_and(lead(p) <= 2, a > last_near(p))))
        def _():
            act(copy(row_slot(p, a), row_slot(p, a), sems.at[0], at(row, col + 1)))

        @pl.when(jnp.logical_and(lax.rem(i, n_col) == col, ahead > 1))
        def _():
            downs = down_sem.at[lax.rem(p, depth), i // n_col]
            down_column(p, a, False, [downs.at[m] for m in range(3)], act)

    def pass_on(p, a, act):
        slot = row_slot(p, a)
        sems = pass_sem.at[lax.rem(p, depth), a]

        @pl.when(passes(p))
        def _():
            @pl.when(odd == 0)
            def _():
                act(copy(slot, slot, sems.at[1], at(row, lax.rem(col - 1 + n_col, n_col))))

            @pl.when(jnp.logical_or(odd == 1, a * n_row + row > p + lead(p)))
            def _():
                act(copy(slot, slot, sems.at[0], at(row, col + 1 - 2 * odd)))

        pass_down(p, a, act)

    def passed(p):
        @pl.when(lead(p) != 0)
        def _():
            loop(first_passed(p), row_blocks, lambda a: pass_on(p, a, finish))

    def receive(p, a):
        arrived(row_slot(p, a))
        pass_down(p, a, start)

    def receive_any(p, a):
        arrived(row_slot(p, a))
        pass_on(p, a, start)

    def loop(lo, hi, fn):
        lax.fori_loop(lo, hi, lambda n, c: (fn(n), c)[1], 0)

    load = pltpu.make_async_copy(a_ref, share, load_sem)
    load.start()

    barrier = pltpu.get_barrier_semaphore()
    n_dev = n_row * n_col

    def greet(n):
        other = lax.rem(row * n_col + col + n, n_dev)
        pl.semaphore_signal(barrier, inc=1, device_id=at(other // n_col, lax.rem(other, n_col)), device_id_type=MESH)

    loop(1, n_dev, greet)
    with jax.named_scope("all_here"):
        pl.semaphore_wait(barrier, n_dev - 1)
    with jax.named_scope("loaded"):
        load.wait()

    def seed_copy(b, dev_row):
        return pltpu.make_async_remote_copy(
            src_ref=share.at[spot(ratio * b + col // n_row, b)], dst_ref=diag.at[b],
            send_sem=seed_send.at[b, lax.rem(dev_row - row + n_row, n_row)],
            recv_sem=seed_recv.at[b], device_id=at(dev_row, col), device_id_type=MESH,
        )

    def hand_out(b):
        @pl.when(on_diag)
        def _():
            for d in (1, n_row - 1, 2):
                seed_copy(b, lax.rem(row + d, n_row)).start()
            diag[b] = share[spot(ratio * b + col // n_row, b)]

        @pl.when(jnp.logical_and(holds_edge(b), jnp.logical_not(leads)))
        def _():
            stage[b] = share[spot((b * n_col + col + 1) // n_row, b)]
            edge_copy(b).start()

    def holds_edge(b):
        j = b * n_col + col
        return jnp.logical_and(lax.rem(j + 1, n_row) == row, j + 1 < steps)

    def edge_copy(b):
        return pltpu.make_async_remote_copy(
            src_ref=stage.at[b], dst_ref=edge.at[b], send_sem=edge_send.at[b], recv_sem=edge_recv.at[b],
            device_id=at(LEAD, col), device_id_type=MESH,
        )

    def has_edge(b):
        from_other = jnp.logical_and(leads, lax.rem(col + 1, n_row) != LEAD)
        return jnp.logical_and(from_other, b * n_col + col + 1 < steps)

    def edge_seeded(b):
        @pl.when(has_edge(b))
        def _():
            edge_copy(b).wait_recv()

    def edge_arrived(p, b):
        j = b * n_col + col

        @pl.when(jnp.logical_and(has_edge(b), j + 1 - p <= n_col + LAG - SETTLE))
        def _():
            arrived(edge_slot(p))

    hand_out(0)
    winv3[...] = jnp.zeros(winv3.shape, BF16)

    def seed_arrived(b):
        @pl.when(jnp.logical_not(on_diag))
        def _():
            seed_copy(b, row).wait_recv()

    with jax.named_scope("seed"):
        seed_arrived(0)

        @pl.when(col != 0)
        def _():
            edge_seeded(0)

    def clear(n):
        a, b = lax.rem(n, row_blocks), n // row_blocks

        @pl.when(a * n_row + row < b * n_col + col)
        def _():
            share[spot(a, b)] = jnp.zeros((size, size), F32)

    loop(0, row_blocks * col_blocks, clear)

    def times_t(x, y):
        return lax.dot_general(x, y, (((1,), (1,)), ((), ())), preferred_element_type=F32)

    def update_block(p, a, b):
        share[spot(a, b)] -= times_t(panel[row_slot(p, a)], panel[col_of(p, b)])

    def update_diag(p, b):
        other = panel[col_of(p, b)]
        diag[b] -= times_t(other, other)

    def update_edge(p, b):
        @pl.when(has_edge(b))
        def _():
            edge[b] -= times_t(panel[edge_slot(p)], panel[col_of(p, b)])

    def column_arrived(p, b):
        @pl.when(jnp.logical_not(on_diag))
        def _():
            arrived(col_slot(p, b))

    def update_column(p, b, lo):
        lone = lax.rem(row_blocks - lo, 2)

        @pl.when(lone == 1)
        def _():
            update_block(p, lo, b)

        def pair(m):
            a = lo + lone + 2 * m
            both = spot(a, b, 2)
            left = panel[pl.ds(row_slot(p, a), 2)].reshape(2 * size, size)
            share[both] -= times_t(left, panel[col_of(p, b)]).reshape(2, size, size)

        loop(0, (row_blocks - lo) // 2, pair)

    def trail(p, b_from, near):
        loop(b_from, col_blocks, lambda b: update_column(p, b, first_a(b * n_col + col - jnp.where(b == near, 0, 1))))

    def columns_arrived(p, b_from):
        def one(b):
            column_arrived(p, b)
            edge_arrived(p, b)

        loop(b_from, col_blocks, one)

    def prepare(b):
        prev[...] = jnp.zeros(prev.shape, F32)
        fac[...] = jnp.zeros(fac.shape, F32)
        work[size:, :] = jnp.zeros((BASE, size), F32)
        r_id = lax.broadcasted_iota(jnp.int32, (size + BASE, size), 0)
        c_id = lax.broadcasted_iota(jnp.int32, (size + BASE, size), 1)
        winv[...] = jnp.where(r_id == c_id, 1.0, 0.0).astype(F32)

    def times_winv_t(x):
        hi, mid, lo = split3(x)
        whi, wmid, wlo = winv3[0], winv3[1], winv3[2]
        small = times_t(lo, whi) + times_t(mid, wmid) + times_t(hi, wlo)
        return small + (times_t(mid, whi) + times_t(hi, wmid)) + times_t(hi, whi)

    def here_diag(k):
        return row == lax.rem(k, n_row)

    def solve(k, a, count):
        kb = k // n_col
        near = jnp.logical_and(a == first_a(k), jnp.logical_not(here_diag(k)))
        here = spot(a, kb, count)

        def shaped(x):
            return x if count == 1 else x.reshape(count, size, size)

        def apply(p):
            left = panel[pl.ds(row_slot(p, a), count)].reshape(count * size, size)
            share[here] -= shaped(times_t(left, panel[col_of(p, kb)]))

        @pl.when(jnp.logical_not(near))
        def _():
            for m in range(count):

                @pl.when(k >= 3)
                def _():
                    receive(k - 3, a + m)

                @pl.when(k >= 2)
                def _():
                    receive(k - 2, a + m)

            loop(jnp.maximum(k - 2 - LAG, 0), k - 1, apply)

        @pl.when(k > 0)
        def _():
            for m in range(count):
                receive(k - 1, a + m)
            apply(k - 1)

        x = times_winv_t(share[here].reshape(count * size, size))
        panel[pl.ds(row_slot(k, a), count)] = x.astype(BF16).reshape(count, size, size)
        share[here] = shaped(x)
        if count == 1:

            @pl.when(jnp.logical_and(near, jnp.logical_and(leads, lax.rem(k + 1, n_row) == LEAD)))
            def _():
                first[...] = panel[row_slot(k, a)]
                first_out(k, start)

        if count == 1:
            source_sends(k, a, start)
        else:
            loop(a, a + count, lambda n: source_sends(k, n, start))

    def update_near(p, b):
        update_diag(p, b)
        update_edge(p, b)

    def first_slot(k, dev_row):
        return jnp.where(lax.rem(k + 1, n_row) == dev_row, row_slot(k, (k + 1) // n_row), col_slot(k, (k + 1) // n_col))

    def first_copy(k, dev_row, sem):
        dst = first_slot(k, dev_row)
        return pltpu.make_async_remote_copy(
            src_ref=first, dst_ref=panel.at[dst], send_sem=sem, recv_sem=recv_sem.at[dst],
            device_id=at(dev_row, lax.rem(col + 1, n_col)), device_id_type=MESH,
        )

    def others_first(k, fn):
        urgent = lax.rem(k + 3, n_row)
        lone = urgent == LEAD
        for m in range(n_row - 1):
            fn(m, lax.rem(jnp.where(lone, LEAD + 1, urgent) + m + jnp.where(lax.rem(jnp.where(lone, LEAD + 1, urgent) - LEAD + n_row, n_row) + m >= n_row, 1, 0), n_row))

    def first_out(k, act):
        act(first_copy(k, LEAD, first_sem.at[0, 0]))

        @pl.when(odd == 0)
        def _():
            others_first(k, lambda m, r: act(first_copy(k, r, first_sem.at[0, 1 + m])))

    def first_down(k, act):
        @pl.when(odd == 0)
        def _():
            others_first(k, lambda m, r: act(copy(first_slot(k, LEAD), first_slot(k, r), first_sem.at[1, 1 + m], at(r, col))))

    def firsts_done(k):
        @pl.when(jnp.logical_and(leads, k + 1 < steps))
        def _():
            first_out(k, finish)

        @pl.when(jnp.logical_and(leads, k > 0))
        def _():
            first_down(k - 1, finish)

    @pl.when(col == 0)
    def _():
        prepare(0)
        work[0:size, :] = diag[0]

    def step(k):
        mine = jnp.logical_and(col == lax.rem(k, n_col), k < steps)
        kb = k // n_col
        last = k - 1
        soon = jnp.logical_and(col == lax.rem(k + 1, n_col), k + 1 < steps)

        @pl.when(mine)
        def _():
            with jax.named_scope("factor"):
                factor_block(work, winv, winv3, prev, fac)

            @pl.when(has_edge(kb))
            def _():
                with jax.named_scope("lead"):

                    @pl.when(k == 0)
                    def _():
                        edge_seeded(kb)

                    @pl.when(k > 0)
                    def _():
                        edge_arrived(last, kb)
                        update_edge(last, kb)

                    first[...] = times_winv_t(edge[kb]).astype(BF16)
                    first_out(k, start)

            lo = first_a(k)
            second = jnp.minimum(lo + 1, row_blocks)
            third = second + lax.rem(row_blocks - second, 2)
            with jax.named_scope("solve_near"):
                loop(lo, third, lambda a: solve(k, a, 1))
            with jax.named_scope("solve_two"):
                loop(0, (row_blocks - third) // 2, lambda m: solve(k, third + 2 * m, 2))

        @pl.when(k >= depth)
        def _():
            with jax.named_scope("passed"):
                passed(k - depth)

        @pl.when(mine)
        def _():
            @pl.when(row == lax.rem(k, n_row))
            def _():
                for d in range(1, n_row):
                    seed_copy(kb, lax.rem(row + d, n_row)).wait_send()
                r_id = lax.broadcasted_iota(jnp.int32, (size, size), 0)
                c_id = lax.broadcasted_iota(jnp.int32, (size, size), 1)
                share[spot(k // n_row, kb)] = jnp.where(r_id >= c_id, work[0:size, :].T, 0.0)

        @pl.when(jnp.logical_and(k > 0, jnp.logical_not(jnp.logical_or(mine, soon))))
        def _():
            @pl.when(col != lax.rem(last, n_col))
            def _():
                with jax.named_scope("receive"):
                    end = jnp.where(lead(last) == 3, jnp.minimum(last_near(last) + 1, row_blocks), row_blocks)
                    loop(first_passed(last), end, lambda a: receive_any(last, a))

            near = first_b(k)
            age = k + n_col - (near * n_col + col)
            settle = jnp.logical_and(age == SETTLE, jnp.logical_and(near > 0, near < col_blocks))

            @pl.when(settle)
            def _():
                with jax.named_scope("late_trail"):
                    own = k - SETTLE

                    for back in (LAG + 2, LAG + 1, LAG):

                        @pl.when(own >= back)
                        def _():
                            columns_arrived(own - back, near)

                    loop(jnp.maximum(own - 2 - LAG, 0), own - LAG + 1, lambda p: trail(p, near, -1))

            @pl.when(jnp.logical_and(k >= LAG, lead(last) != 3))
            def _():
                p = k - LAG
                with jax.named_scope("columns"):
                    columns_arrived(p, near)

                @pl.when(jnp.logical_and(near < col_blocks, age >= SETTLE + 2))
                def _():
                    @pl.when(jnp.logical_and(age == SETTLE + 2, near > 0))
                    def _():
                        with jax.named_scope("seed_late"):
                            seed_arrived(near)
                            edge_seeded(near)

                    oldest = jnp.where(age == SETTLE + 2, jnp.maximum(p - 1, 0), p)
                    loop(oldest, p + 1, lambda q: update_near(q, near))

                with jax.named_scope("trail"):
                    trail(p, near, jnp.where(jnp.logical_or(age > SETTLE, near == 0), near, -1))

            @pl.when(settle)
            def _():
                hand_out(near)

        @pl.when(soon)
        def _():
            nb = (k + 1) // n_col

            oldest = jnp.maximum(k - 1 - LAG, 0)
            lo = first_a(k + 1)

            def old_diag(p):
                column_arrived(p, nb)
                edge_arrived(p, nb)
                update_near(p, nb)

            def take(a):
                receive(last, a)

                @pl.when(jnp.logical_not(here_diag(k + 1)))
                def _():
                    loop(oldest, last, lambda p: update_block(p, a, nb))

            @pl.when(k > 0)
            def _():
                with jax.named_scope("old_diag"):
                    loop(oldest, last, old_diag)
                with jax.named_scope("take"):
                    loop(first_a(k), jnp.minimum(first_a(k) + 1, row_blocks), take)
                with jax.named_scope("take_column"):
                    column_arrived(last, nb)
                    edge_arrived(last, nb)
                with jax.named_scope("catch_up"):
                    update_near(last, nb)
                    @pl.when(jnp.logical_and(jnp.logical_not(here_diag(k + 1)), lo < row_blocks))
                    def _():
                        update_block(last, lo, nb)

            prepare(nb)
            slot = col_of(k, nb)
            with jax.named_scope("first_block"):
                arrived(slot)

            @pl.when(leads)
            def _():
                first_down(k, start)

            other = panel[slot]
            work[0:size, :] = diag[nb] - times_t(other, other)

        @pl.when(jnp.logical_and(k >= n_col // 2, col == lax.rem(k + n_col // 2, n_col)))
        def _():
            with jax.named_scope("sends_done"):
                firsts_done(k - n_col // 2)
                loop(first_a(k - n_col // 2), row_blocks, lambda a: source_sends(k - n_col // 2, a, finish))

    loop(0, steps + n_col // 2, step)

    def edges_done(b):
        @pl.when(jnp.logical_and(holds_edge(b), jnp.logical_not(leads)))
        def _():
            edge_copy(b).wait_send()

    loop(0, col_blocks, edges_done)


def solution(mesh):
    n_row = mesh.shape["row"]
    n_col = mesh.shape["col"]

    def factor_local(a_loc):
        row_blocks, size, local_cols = a_loc.shape
        col_blocks = local_cols // size
        slots = n_row * (row_blocks * (row_blocks + 1) // 2) + n_col * (col_blocks * (col_blocks + 1) // 2)
        slots += row_blocks * n_row
        return pl.pallas_call(
            functools.partial(kernel, n_row, n_col, "batch"),
            out_shape=pltpu.VMEM(a_loc.shape, F32),
            in_specs=[pl.BlockSpec(memory_space=pl.ANY)],
            scratch_shapes=[
                pltpu.VMEM((col_blocks, size, size), F32),
                pltpu.VMEM((col_blocks, size, size), F32),
                pltpu.VMEM((col_blocks, size, size), F32),
                pltpu.VMEM((size, size), BF16),
                pltpu.VMEM((slots, size, size), BF16),
                pltpu.VMEM((size + BASE, size), F32),
                pltpu.VMEM((size + BASE, size), F32),
                pltpu.VMEM((3, size, size), BF16),
                pltpu.VMEM((BASE, 3 * LANE), F32),
                pltpu.VMEM((4 * SUB, SUB, LANE), F32),
                pltpu.SemaphoreType.DMA,
                pltpu.SemaphoreType.DMA((col_blocks, n_row)),
                pltpu.SemaphoreType.DMA((col_blocks,)),
                pltpu.SemaphoreType.DMA((col_blocks,)),
                pltpu.SemaphoreType.DMA((col_blocks,)),
                pltpu.SemaphoreType.DMA((2, n_row)),
                pltpu.SemaphoreType.DMA((row_blocks, 9)),
                pltpu.SemaphoreType.DMA((4, row_blocks, 2)),
                pltpu.SemaphoreType.DMA((4, col_blocks, 3)),
                pltpu.SemaphoreType.DMA((slots,)),
            ],
            compiler_params=pltpu.CompilerParams(
                collective_id=0, has_side_effects=True, vmem_limit_bytes=50 * 1024 * 1024
            ),
            name="cholesky",
        )(a_loc)

    blk_spec = P(("batch", "row"), None, "col")
    return jax.shard_map(factor_local, mesh=mesh, in_specs=(blk_spec,), out_specs=blk_spec, check_vma=False)
```

```python
import functools

import jax
import jax.numpy as jnp
from jax import lax
from jax.experimental import pallas as pl
from jax.experimental.pallas import tpu as pltpu
from jax.sharding import PartitionSpec as P

F32 = jnp.float32
BF16 = jnp.bfloat16
MESH = pl.DeviceIdType.MESH
SUB = 8
LANE = 128
BASE = 16
LEAD = 3
SETTLE = 3
LAG = 3


def sub_bcast(x, q):
    return jnp.broadcast_to(x[q : q + 1, :], (SUB, LANE))


ALONG_LANES = lax.GatherDimensionNumbers(
    offset_dims=(), collapsed_slice_dims=(1,), start_index_map=(1,), operand_batching_dims=(0,), start_indices_batching_dims=(0,)
)


def lane_bcast(x, lane):
    index = jnp.full((SUB, LANE, 1), lane, jnp.int32)
    return lax.gather(x, index, ALONG_LANES, (1, 1), mode=lax.GatherScatterMode.PROMISE_IN_BOUNDS)


def split3(x):
    high = x.astype(BF16)
    rest = x - high.astype(F32)
    mid = rest.astype(BF16)
    return high, mid, (rest - mid.astype(F32)).astype(BF16)


def swap_rows(x, bit, row_id):
    if bit == SUB // 2:
        return pltpu.roll(x, bit, 0)
    return jnp.where((row_id & bit) == 0, pltpu.roll(x, SUB - bit, 0), pltpu.roll(x, bit, 0))


def stack_sums(parts):
    row_id = lax.broadcasted_iota(jnp.int32, (SUB, LANE), 0)
    for bit in (4, 2, 1):
        low = (row_id & bit) == 0
        half = len(parts) // 2
        parts = [
            jnp.where(low, parts[n], parts[n + half]) + swap_rows(jnp.where(low, parts[n + half], parts[n]), bit, row_id)
            for n in range(half)
        ]
    return parts[0]


def eliminate(rows, lane0):
    row_id = lax.broadcasted_iota(jnp.int32, (SUB, LANE), 0)
    rows = [list(rows[0]), list(rows[1])]
    cols = [
        [lane_bcast(rows[0][0], lane0 + j) for j in range(SUB)],
        [lane_bcast(rows[1][0], lane0 + j) for j in range(BASE)],
    ]
    scale = [jnp.zeros((SUB, LANE), F32), jnp.zeros((SUB, LANE), F32)]
    pivot = sub_bcast(cols[0][0], 0)
    for j in range(BASE):
        t, q = divmod(j, SUB)
        inv = lax.rsqrt(pivot)
        scale[t] = jnp.where(row_id == q, inv, scale[t])
        if j + 1 < BASE:
            tn, qn = divmod(j + 1, SUB)
            near = sub_bcast(cols[tn][j], qn) * inv
            pivot = sub_bcast(cols[tn][j + 1], qn) - near * near
        below = cols[1][j] * inv
        here = cols[0][j] * inv if t == 0 else None
        for n in range(j + 1, BASE):
            tn, qn = divmod(n, SUB)
            other = near if n == j + 1 else sub_bcast(here if tn == 0 else below, qn)
            if t == 0 and tn == 0:
                cols[0][n] = cols[0][n] - here * other
            cols[1][n] = cols[1][n] - below * other
        masked = jnp.where(row_id > q, here if t == 0 else below, 0.0)
        for v in range(len(rows[0])):
            pivot_row = sub_bcast(rows[t][v], q) * inv
            rows[t][v] = rows[t][v] - masked * pivot_row
            if t == 0:
                rows[1][v] = rows[1][v] - below * pivot_row
    return [[x * scale[t] for x in rows[t]] for t in range(2)]


def factor_block(work, winv, winv3, prev, fac):
    size = work.shape[1]

    def group(v):
        return slice(LANE * v, LANE * (v + 1))

    def pending(factors, before, t, v):
        above, below = before[:SUB, group(v)], before[SUB:, group(v)]
        at = 2 * SUB * t
        return stack_sums([factors[at + n] * above + factors[at + SUB + n] * below for n in range(SUB)])

    for half in range(size // LANE):
        views = [(work, 0), (work, 1), (winv, 0)] if half == 0 else [(work, 1), (winv, 0), (winv, 1)]
        first = half * LANE
        if half == 1:
            factors, before = fac[...], prev[...]
            work[first : first + BASE, group(1)] -= jnp.concatenate([pending(factors, before, t, 1) for t in range(2)], axis=0)
            prev[...] = jnp.concatenate([before[:, group(1)], before[:, group(2)], jnp.zeros((BASE, LANE), F32)], axis=1)

        def body(s, carry, views=views, first=first):
            lane0 = s * BASE
            row0 = pl.multiple_of(first + lane0, BASE)

            here = pl.ds(row0, BASE)
            then = pl.ds(pl.multiple_of(row0 + BASE, BASE), BASE)
            both = [ref[here, group(g)] for ref, g in views]
            rows = [[x[SUB * t : SUB * (t + 1)] for x in both] for t in range(2)]
            factors, before = fac[...], prev[...]
            for t in range(2):
                for v in (1, 2):
                    rows[t][v] = rows[t][v] - pending(factors, before, t, v)
            hi, mid, lo = split3(before)
            lane = lax.broadcasted_iota(jnp.int32, (BASE, size - first), 1) + first
            after = lane >= row0 + BASE
            lhi, lmid, llo = [jnp.where(after, x[:, : size - first], jnp.zeros((), BF16)) for x in (hi, mid, lo)]
            update = lax.dot_general(
                jnp.concatenate([lhi, lhi, lmid, lhi, llo, lmid], axis=0),
                jnp.concatenate([hi, mid, hi, lo, hi, mid], axis=0),
                (((0,), (0,)), ((), ())),
                preferred_element_type=F32,
            )
            for v, (ref, g) in enumerate(views):
                ref[first:size, group(g)] -= update[:, group(v)]
            done = eliminate(rows, lane0)
            if first == 0:
                source = [jnp.where(s == LANE // BASE - 1, done[t][1], done[t][0]) for t in range(2)]
            else:
                source = [done[t][0] for t in range(2)]
            next_lane = (lane0 + BASE) % LANE
            factors, sums = [], []
            for t in range(2):
                factor = [[lane_bcast(source[m], next_lane + SUB * t + n) for n in range(SUB)] for m in range(2)]
                sums.append(stack_sums([factor[0][n] * done[0][0] + factor[1][n] * done[1][0] for n in range(SUB)]))
                factors += factor[0] + factor[1]
            ref, g = views[0]
            ref[then, group(g)] -= jnp.concatenate(sums, axis=0)
            fac[...] = jnp.stack(factors)
            whole = [jnp.concatenate([done[0][v], done[1][v]], axis=0) for v in range(3)]
            prev[...] = jnp.concatenate(whole, axis=1)
            for (ref, g), x in zip(views, whole):
                ref[here, group(g)] = x
                if ref is winv:
                    for n, part in enumerate(split3(x)):
                        winv3[n, here, group(g)] = part
            return carry

        lax.fori_loop(0, LANE // BASE, body, 0, unroll=2)


def kernel(n_row, n_col, batch_axis, a_ref, share, diag, edge, stage, first, panel, work, winv, winv3, prev, fac, load_sem,
           seed_send, seed_recv, edge_send, edge_recv, first_sem, send_sem, pass_sem, down_sem, recv_sem):
    row_blocks, size, local_cols = a_ref.shape
    col_blocks = local_cols // size
    ratio = n_col // n_row
    steps = row_blocks * n_row
    depth = pass_sem.shape[0]
    batch = lax.axis_index(batch_axis)
    row = lax.axis_index("row")
    col = lax.axis_index("col")
    odd = lax.rem(col, 2)
    on_diag = lax.rem(col, n_row) == row
    row_slots = n_row * (row_blocks * (row_blocks + 1) // 2)
    edge_slots = row_slots + n_col * (col_blocks * (col_blocks + 1) // 2)
    leads = row == LEAD

    def at(dev_row, dev_col):
        return (batch, dev_row, dev_col)

    def row_slot(k, a):
        g = k // n_row
        return n_row * (row_blocks * g - (g * (g - 1)) // 2) + (k - g * n_row) * (row_blocks - g) + a - g

    def col_slot(k, b):
        h = k // n_col
        return row_slots + n_col * (col_blocks * h - (h * (h - 1)) // 2) + (k - h * n_col) * (col_blocks - h) + b - h

    def first_a(k):
        return (k + n_row - row) // n_row

    def first_b(k):
        return (k + n_col - col) // n_col

    def spot(a, b, count=1):
        return (a if count == 1 else pl.ds(a, count), slice(None), pl.ds(pl.multiple_of(b * size, size), size))

    def col_of(k, b):
        return jnp.where(on_diag, row_slot(k, ratio * b + col // n_row), col_slot(k, b))

    def edge_slot(k):
        return edge_slots + k

    def edge_reach(ahead):
        return jnp.logical_and(ahead >= 2, jnp.logical_and(ahead <= n_col + LAG - SETTLE, row != LEAD))

    def copy(src_slot, dst_slot, sem, device):
        return pltpu.make_async_remote_copy(
            src_ref=panel.at[src_slot], dst_ref=panel.at[dst_slot], send_sem=sem, recv_sem=recv_sem.at[dst_slot],
            device_id=device, device_id_type=MESH,
        )

    def arrived(slot):
        copy(slot, slot, send_sem.at[0, 0], at(row, col)).wait_recv()

    def start(c):
        c.start()

    def finish(c):
        c.wait_send()

    def from_maker(ahead, way):
        there = lax.rem(row + way, n_row)
        lead_near = jnp.logical_and(there == LEAD, jnp.logical_and(ahead >= 2, ahead <= n_row))
        soon_needed = jnp.logical_and(ahead == 2, way == 2)
        return jnp.logical_or(lead_near, soon_needed)

    def down_column(k, a, maker, sems, act):
        i = a * n_row + row
        slot = row_slot(k, a)
        dst = col_slot(k, i // n_col)
        for m, way in enumerate((1, n_row - 1, 2)):
            direct = from_maker(i - k, way)

            @pl.when(jnp.where(maker, direct, jnp.logical_not(direct)))
            def _():
                act(copy(slot, dst, sems[m], at(lax.rem(row + way, n_row), lax.rem(i, n_col))))

    def last_near(p):
        return first_a(p + 2)

    def to_edge(k, a, sem, act):
        i = a * n_row + row
        act(copy(row_slot(k, a), edge_slot(k), sem, at(LEAD, lax.rem(i - 1, n_col))))

    def source_sends(k, a, act):
        ahead = a * n_row + row - k
        slot = row_slot(k, a)
        early = n_row

        @pl.when(edge_reach(ahead))
        def _():
            to_edge(k, a, send_sem.at[a, 5], act)

        near = jnp.logical_and(ahead >= 2, ahead <= early)

        @pl.when(jnp.logical_or(near, lax.rem(ahead, n_col) == 0))
        def _():
            down_column(k, a, near, [send_sem.at[a, m] for m in range(3)], act)

        @pl.when(jnp.logical_or(jnp.logical_and(odd == 0, ahead >= 2), ahead >= n_col - 1))
        def _():
            act(copy(slot, slot, send_sem.at[a, 3], at(row, lax.rem(jnp.where(odd == 0, col + 1, col - 1), n_col))))

        @pl.when(ahead >= 2)
        def _():
            act(copy(slot, slot, send_sem.at[a, 6], at(row, lax.rem(col - odd + 2, n_col))))

        @pl.when(jnp.logical_and(ahead >= 3 - odd, a <= last_near(k)))
        def _():
            act(copy(slot, slot, send_sem.at[a, 4], at(row, lax.rem(col - odd + 3, n_col))))

        @pl.when(jnp.logical_and(ahead >= n_col // 2 - odd, ahead < n_col - 2 - odd))
        def _():
            act(copy(slot, slot, send_sem.at[a, 7], at(row, lax.rem(col - odd + 5, n_col))))

        @pl.when(ahead >= n_col - 2 - odd)
        def _():
            act(copy(slot, slot, send_sem.at[a, 8], at(row, lax.rem(col - odd - 2 + n_col, n_col))))

    def lead(p):
        return lax.rem(col - lax.rem(p, n_col) + n_col, n_col)

    def hops(p):
        return lax.rem(col // 2 - lax.rem(p, n_col) // 2 + n_col // 2, n_col // 2)

    def passes(p):
        return jnp.where(odd == 1, 2, n_col // 2 - 1) == hops(p)

    def first_passed(p):
        low = jnp.where(jnp.logical_and(passes(p), odd == 1), lead(p) - 1, lead(p))
        return (p + low - row + n_row - 1) // n_row

    def pass_down(p, a, act):
        i = a * n_row + row
        ahead = i - p
        sems = pass_sem.at[lax.rem(p, depth), a]

        @pl.when(jnp.logical_and(odd == 0, jnp.logical_and(lead(p) <= 2, a > last_near(p))))
        def _():
            act(copy(row_slot(p, a), row_slot(p, a), sems.at[0], at(row, col + 1)))

        @pl.when(jnp.logical_and(lax.rem(i, n_col) == col, ahead > 1))
        def _():
            downs = down_sem.at[lax.rem(p, depth), i // n_col]
            down_column(p, a, False, [downs.at[m] for m in range(3)], act)

    def pass_on(p, a, act):
        slot = row_slot(p, a)
        sems = pass_sem.at[lax.rem(p, depth), a]

        @pl.when(passes(p))
        def _():
            @pl.when(odd == 0)
            def _():
                act(copy(slot, slot, sems.at[1], at(row, lax.rem(col - 1 + n_col, n_col))))

            @pl.when(jnp.logical_or(odd == 1, a * n_row + row > p + lead(p)))
            def _():
                act(copy(slot, slot, sems.at[0], at(row, col + 1 - 2 * odd)))

        pass_down(p, a, act)

    def passed(p):
        @pl.when(lead(p) != 0)
        def _():
            loop(first_passed(p), row_blocks, lambda a: pass_on(p, a, finish))

    def receive(p, a):
        arrived(row_slot(p, a))
        pass_down(p, a, start)

    def receive_any(p, a):
        arrived(row_slot(p, a))
        pass_on(p, a, start)

    def loop(lo, hi, fn):
        lax.fori_loop(lo, hi, lambda n, c: (fn(n), c)[1], 0)

    load = pltpu.make_async_copy(a_ref, share, load_sem)
    load.start()

    barrier = pltpu.get_barrier_semaphore()
    n_dev = n_row * n_col

    def greet(n):
        other = lax.rem(row * n_col + col + n, n_dev)
        pl.semaphore_signal(barrier, inc=1, device_id=at(other // n_col, lax.rem(other, n_col)), device_id_type=MESH)

    loop(1, n_dev, greet)
    with jax.named_scope("all_here"):
        pl.semaphore_wait(barrier, n_dev - 1)
    with jax.named_scope("loaded"):
        load.wait()

    def seed_copy(b, dev_row):
        return pltpu.make_async_remote_copy(
            src_ref=share.at[spot(ratio * b + col // n_row, b)], dst_ref=diag.at[b],
            send_sem=seed_send.at[b, lax.rem(dev_row - row + n_row, n_row)],
            recv_sem=seed_recv.at[b], device_id=at(dev_row, col), device_id_type=MESH,
        )

    def hand_out(b):
        @pl.when(on_diag)
        def _():
            for d in (1, n_row - 1, 2):
                seed_copy(b, lax.rem(row + d, n_row)).start()
            diag[b] = share[spot(ratio * b + col // n_row, b)]

        @pl.when(jnp.logical_and(holds_edge(b), jnp.logical_not(leads)))
        def _():
            stage[b] = share[spot((b * n_col + col + 1) // n_row, b)]
            edge_copy(b).start()

    def holds_edge(b):
        j = b * n_col + col
        return jnp.logical_and(lax.rem(j + 1, n_row) == row, j + 1 < steps)

    def edge_copy(b):
        return pltpu.make_async_remote_copy(
            src_ref=stage.at[b], dst_ref=edge.at[b], send_sem=edge_send.at[b], recv_sem=edge_recv.at[b],
            device_id=at(LEAD, col), device_id_type=MESH,
        )

    def has_edge(b):
        from_other = jnp.logical_and(leads, lax.rem(col + 1, n_row) != LEAD)
        return jnp.logical_and(from_other, b * n_col + col + 1 < steps)

    def edge_seeded(b):
        @pl.when(has_edge(b))
        def _():
            edge_copy(b).wait_recv()

    def edge_arrived(p, b):
        j = b * n_col + col

        @pl.when(jnp.logical_and(has_edge(b), j + 1 - p <= n_col + LAG - SETTLE))
        def _():
            arrived(edge_slot(p))

    hand_out(0)
    winv3[...] = jnp.zeros(winv3.shape, BF16)

    def seed_arrived(b):
        @pl.when(jnp.logical_not(on_diag))
        def _():
            seed_copy(b, row).wait_recv()

    with jax.named_scope("seed"):
        seed_arrived(0)

        @pl.when(col != 0)
        def _():
            edge_seeded(0)

    def clear(n):
        a, b = lax.rem(n, row_blocks), n // row_blocks

        @pl.when(a * n_row + row < b * n_col + col)
        def _():
            share[spot(a, b)] = jnp.zeros((size, size), F32)

    loop(0, row_blocks * col_blocks, clear)

    def times_t(x, y):
        return lax.dot_general(x, y, (((1,), (1,)), ((), ())), preferred_element_type=F32)

    def update_block(p, a, b):
        share[spot(a, b)] -= times_t(panel[row_slot(p, a)], panel[col_of(p, b)])

    def update_diag(p, b):
        other = panel[col_of(p, b)]
        diag[b] -= times_t(other, other)

    def update_edge(p, b):
        @pl.when(has_edge(b))
        def _():
            edge[b] -= times_t(panel[edge_slot(p)], panel[col_of(p, b)])

    def column_arrived(p, b):
        @pl.when(jnp.logical_not(on_diag))
        def _():
            arrived(col_slot(p, b))

    def update_column(p, b, lo):
        lone = lax.rem(row_blocks - lo, 2)

        @pl.when(lone == 1)
        def _():
            update_block(p, lo, b)

        def pair(m):
            a = lo + lone + 2 * m
            both = spot(a, b, 2)
            left = panel[pl.ds(row_slot(p, a), 2)].reshape(2 * size, size)
            share[both] -= times_t(left, panel[col_of(p, b)]).reshape(2, size, size)

        loop(0, (row_blocks - lo) // 2, pair)

    def trail(p, b_from, near):
        loop(b_from, col_blocks, lambda b: update_column(p, b, first_a(b * n_col + col - jnp.where(b == near, 0, 1))))

    def columns_arrived(p, b_from):
        def one(b):
            column_arrived(p, b)
            edge_arrived(p, b)

        loop(b_from, col_blocks, one)

    def prepare(b):
        prev[...] = jnp.zeros(prev.shape, F32)
        fac[...] = jnp.zeros(fac.shape, F32)
        work[size:, :] = jnp.zeros((BASE, size), F32)
        r_id = lax.broadcasted_iota(jnp.int32, (size + BASE, size), 0)
        c_id = lax.broadcasted_iota(jnp.int32, (size + BASE, size), 1)
        winv[...] = jnp.where(r_id == c_id, 1.0, 0.0).astype(F32)

    def times_winv_t(x):
        hi, mid, lo = split3(x)
        whi, wmid, wlo = winv3[0], winv3[1], winv3[2]
        small = times_t(lo, whi) + times_t(mid, wmid) + times_t(hi, wlo)
        return small + (times_t(mid, whi) + times_t(hi, wmid)) + times_t(hi, whi)

    def here_diag(k):
        return row == lax.rem(k, n_row)

    def solve(k, a, count):
        kb = k // n_col
        near = jnp.logical_and(a == first_a(k), jnp.logical_not(here_diag(k)))
        here = spot(a, kb, count)

        def shaped(x):
            return x if count == 1 else x.reshape(count, size, size)

        def apply(p):
            left = panel[pl.ds(row_slot(p, a), count)].reshape(count * size, size)
            share[here] -= shaped(times_t(left, panel[col_of(p, kb)]))

        @pl.when(jnp.logical_not(near))
        def _():
            for m in range(count):

                @pl.when(k >= 3)
                def _():
                    receive(k - 3, a + m)

                @pl.when(k >= 2)
                def _():
                    receive(k - 2, a + m)

            loop(jnp.maximum(k - 2 - LAG, 0), k - 1, apply)

        @pl.when(k > 0)
        def _():
            for m in range(count):
                receive(k - 1, a + m)
            apply(k - 1)

        x = times_winv_t(share[here].reshape(count * size, size))
        panel[pl.ds(row_slot(k, a), count)] = x.astype(BF16).reshape(count, size, size)
        share[here] = shaped(x)
        if count == 1:

            @pl.when(jnp.logical_and(near, jnp.logical_and(leads, lax.rem(k + 1, n_row) == LEAD)))
            def _():
                first[...] = panel[row_slot(k, a)]
                first_out(k, start)

        if count == 1:
            source_sends(k, a, start)
        else:
            loop(a, a + count, lambda n: source_sends(k, n, start))

    def update_near(p, b):
        update_diag(p, b)
        update_edge(p, b)

    def first_slot(k, dev_row):
        return jnp.where(lax.rem(k + 1, n_row) == dev_row, row_slot(k, (k + 1) // n_row), col_slot(k, (k + 1) // n_col))

    def first_copy(k, dev_row, sem):
        dst = first_slot(k, dev_row)
        return pltpu.make_async_remote_copy(
            src_ref=first, dst_ref=panel.at[dst], send_sem=sem, recv_sem=recv_sem.at[dst],
            device_id=at(dev_row, lax.rem(col + 1, n_col)), device_id_type=MESH,
        )

    def others_first(k, fn):
        urgent = lax.rem(k + 3, n_row)
        lone = urgent == LEAD
        for m in range(n_row - 1):
            fn(m, lax.rem(jnp.where(lone, LEAD + 1, urgent) + m + jnp.where(lax.rem(jnp.where(lone, LEAD + 1, urgent) - LEAD + n_row, n_row) + m >= n_row, 1, 0), n_row))

    def first_out(k, act):
        act(first_copy(k, LEAD, first_sem.at[0, 0]))

        @pl.when(odd == 0)
        def _():
            others_first(k, lambda m, r: act(first_copy(k, r, first_sem.at[0, 1 + m])))

    def first_down(k, act):
        @pl.when(odd == 0)
        def _():
            others_first(k, lambda m, r: act(copy(first_slot(k, LEAD), first_slot(k, r), first_sem.at[1, 1 + m], at(r, col))))

    def firsts_done(k):
        @pl.when(jnp.logical_and(leads, k + 1 < steps))
        def _():
            first_out(k, finish)

        @pl.when(jnp.logical_and(leads, k > 0))
        def _():
            first_down(k - 1, finish)

    @pl.when(col == 0)
    def _():
        prepare(0)
        work[0:size, :] = diag[0]

    def step(k):
        mine = jnp.logical_and(col == lax.rem(k, n_col), k < steps)
        kb = k // n_col
        last = k - 1
        soon = jnp.logical_and(col == lax.rem(k + 1, n_col), k + 1 < steps)

        @pl.when(mine)
        def _():
            with jax.named_scope("factor"):
                factor_block(work, winv, winv3, prev, fac)

            @pl.when(has_edge(kb))
            def _():
                with jax.named_scope("lead"):

                    @pl.when(k == 0)
                    def _():
                        edge_seeded(kb)

                    @pl.when(k > 0)
                    def _():
                        edge_arrived(last, kb)
                        update_edge(last, kb)

                    first[...] = times_winv_t(edge[kb]).astype(BF16)
                    first_out(k, start)

            lo = first_a(k)
            second = jnp.minimum(lo + 1, row_blocks)
            third = second + lax.rem(row_blocks - second, 2)
            with jax.named_scope("solve_near"):
                loop(lo, third, lambda a: solve(k, a, 1))
            with jax.named_scope("solve_two"):
                loop(0, (row_blocks - third) // 2, lambda m: solve(k, third + 2 * m, 2))

        @pl.when(k >= depth)
        def _():
            with jax.named_scope("passed"):
                passed(k - depth)

        @pl.when(mine)
        def _():
            @pl.when(row == lax.rem(k, n_row))
            def _():
                for d in range(1, n_row):
                    seed_copy(kb, lax.rem(row + d, n_row)).wait_send()
                r_id = lax.broadcasted_iota(jnp.int32, (size, size), 0)
                c_id = lax.broadcasted_iota(jnp.int32, (size, size), 1)
                share[spot(k // n_row, kb)] = jnp.where(r_id >= c_id, work[0:size, :].T, 0.0)

        @pl.when(jnp.logical_and(k > 0, jnp.logical_not(jnp.logical_or(mine, soon))))
        def _():
            @pl.when(col != lax.rem(last, n_col))
            def _():
                with jax.named_scope("receive"):
                    end = jnp.where(lead(last) == 3, jnp.minimum(last_near(last) + 1, row_blocks), row_blocks)
                    loop(first_passed(last), end, lambda a: receive_any(last, a))

            near = first_b(k)
            age = k + n_col - (near * n_col + col)
            settle = jnp.logical_and(age == SETTLE, jnp.logical_and(near > 0, near < col_blocks))

            @pl.when(settle)
            def _():
                with jax.named_scope("late_trail"):
                    own = k - SETTLE

                    for back in (LAG + 2, LAG + 1, LAG):

                        @pl.when(own >= back)
                        def _():
                            columns_arrived(own - back, near)

                    loop(jnp.maximum(own - 2 - LAG, 0), own - LAG + 1, lambda p: trail(p, near, -1))

            @pl.when(jnp.logical_and(k >= LAG, lead(last) != 3))
            def _():
                p = k - LAG
                with jax.named_scope("columns"):
                    columns_arrived(p, near)

                @pl.when(jnp.logical_and(near < col_blocks, age >= SETTLE + 2))
                def _():
                    @pl.when(jnp.logical_and(age == SETTLE + 2, near > 0))
                    def _():
                        with jax.named_scope("seed_late"):
                            seed_arrived(near)
                            edge_seeded(near)

                    oldest = jnp.where(age == SETTLE + 2, jnp.maximum(p - 1, 0), p)
                    loop(oldest, p + 1, lambda q: update_near(q, near))

                with jax.named_scope("trail"):
                    trail(p, near, jnp.where(jnp.logical_or(age > SETTLE, near == 0), near, -1))

            @pl.when(settle)
            def _():
                hand_out(near)

        @pl.when(soon)
        def _():
            nb = (k + 1) // n_col

            oldest = jnp.maximum(k - 1 - LAG, 0)
            lo = first_a(k + 1)

            def old_diag(p):
                column_arrived(p, nb)
                edge_arrived(p, nb)
                update_near(p, nb)

            def take(a):
                receive(last, a)

                @pl.when(jnp.logical_not(here_diag(k + 1)))
                def _():
                    loop(oldest, last, lambda p: update_block(p, a, nb))

            @pl.when(k > 0)
            def _():
                with jax.named_scope("old_diag"):
                    loop(oldest, last, old_diag)
                with jax.named_scope("take"):
                    loop(first_a(k), jnp.minimum(first_a(k) + 1, row_blocks), take)
                with jax.named_scope("take_column"):
                    column_arrived(last, nb)
                    edge_arrived(last, nb)
                with jax.named_scope("catch_up"):
                    update_near(last, nb)
                    @pl.when(jnp.logical_and(jnp.logical_not(here_diag(k + 1)), lo < row_blocks))
                    def _():
                        update_block(last, lo, nb)

            prepare(nb)
            slot = col_of(k, nb)
            with jax.named_scope("first_block"):
                arrived(slot)

            @pl.when(leads)
            def _():
                first_down(k, start)

            other = panel[slot]
            work[0:size, :] = diag[nb] - times_t(other, other)

        @pl.when(jnp.logical_and(k >= n_col // 2, col == lax.rem(k + n_col // 2, n_col)))
        def _():
            with jax.named_scope("sends_done"):
                firsts_done(k - n_col // 2)
                loop(first_a(k - n_col // 2), row_blocks, lambda a: source_sends(k - n_col // 2, a, finish))

    loop(0, steps + n_col // 2, step)

    def edges_done(b):
        @pl.when(jnp.logical_and(holds_edge(b), jnp.logical_not(leads)))
        def _():
            edge_copy(b).wait_send()

    loop(0, col_blocks, edges_done)


def solution(mesh):
    n_row = mesh.shape["row"]
    n_col = mesh.shape["col"]

    def factor_local(a_loc):
        row_blocks, size, local_cols = a_loc.shape
        col_blocks = local_cols // size
        slots = n_row * (row_blocks * (row_blocks + 1) // 2) + n_col * (col_blocks * (col_blocks + 1) // 2)
        slots += row_blocks * n_row
        return pl.pallas_call(
            functools.partial(kernel, n_row, n_col, "batch"),
            out_shape=pltpu.VMEM(a_loc.shape, F32),
            in_specs=[pl.BlockSpec(memory_space=pl.ANY)],
            scratch_shapes=[
                pltpu.VMEM((col_blocks, size, size), F32),
                pltpu.VMEM((col_blocks, size, size), F32),
                pltpu.VMEM((col_blocks, size, size), F32),
                pltpu.VMEM((size, size), BF16),
                pltpu.VMEM((slots, size, size), BF16),
                pltpu.VMEM((size + BASE, size), F32),
                pltpu.VMEM((size + BASE, size), F32),
                pltpu.VMEM((3, size, size), BF16),
                pltpu.VMEM((BASE, 3 * LANE), F32),
                pltpu.VMEM((4 * SUB, SUB, LANE), F32),
                pltpu.SemaphoreType.DMA,
                pltpu.SemaphoreType.DMA((col_blocks, n_row)),
                pltpu.SemaphoreType.DMA((col_blocks,)),
                pltpu.SemaphoreType.DMA((col_blocks,)),
                pltpu.SemaphoreType.DMA((col_blocks,)),
                pltpu.SemaphoreType.DMA((2, n_row)),
                pltpu.SemaphoreType.DMA((row_blocks, 9)),
                pltpu.SemaphoreType.DMA((4, row_blocks, 2)),
                pltpu.SemaphoreType.DMA((4, col_blocks, 3)),
                pltpu.SemaphoreType.DMA((slots,)),
            ],
            compiler_params=pltpu.CompilerParams(
                collective_id=0, has_side_effects=True, vmem_limit_bytes=50 * 1024 * 1024
            ),
            name="cholesky",
        )(a_loc)

    blk_spec = P(("batch", "row"), None, "col")
    return jax.shard_map(factor_local, mesh=mesh, in_specs=(blk_spec,), out_specs=blk_spec, check_vma=False)
```
